32 devices in a mesh: dp: 8 (over z, y), tp: 4 (over x, core).
Axes of the slice: x: 2, y: 2, z: 4, core: 2. Of those that a mesh axis runs over, the one named last changes fastest.
Arguments:
- node_lat: bfloat16 [16, 1885, 128], P('dp', None, 'tp')
- edge_lat: bfloat16 [16, 10910, 128], P('dp', None, 'tp')
- senders: int32 [10910], replicated
- receivers: int32 [10910], replicated
- grad_node: bfloat16 [16, 1885, 128], P('dp', None, 'tp')
- grad_edge: bfloat16 [16, 10910, 128], P('dp', None, 'tp')
- edge_w1: bfloat16 [2, 3, 128, 128], P(None, None, 'tp')
- edge_b1: float32 [2, 128], replicated
- edge_w2: bfloat16 [2, 128, 128], P(None, None, 'tp')
- edge_vec: float32 [2, 3, 128], P(None, None, 'tp')
- node_w1: bfloat16 [2, 2, 128, 128], P(None, None, 'tp')
- node_b1: float32 [2, 128], replicated
- node_w2: bfloat16 [2, 128, 128], P(None, None, 'tp')
- node_vec: float32 [2, 3, 128], P(None, None, 'tp')
Outputs:
- output 1: bfloat16 [16, 1885, 128], P('dp', None, 'tp')
- output 2: bfloat16 [16, 10910, 128], P('dp', None, 'tp')
- output 3: bfloat16 [16, 1885, 128], P('dp', None, 'tp')
- output 4: bfloat16 [16, 10910, 128], P('dp', None, 'tp')
- output 5: float32 [2, 3, 128, 128], P(None, None, 'tp')
- output 6: float32 [2, 128], replicated
- output 7: float32 [2, 128, 128], P(None, None, 'tp')
- output 8: float32 [2, 3, 128], P(None, None, 'tp')
- output 9: float32 [2, 2, 128, 128], P(None, None, 'tp')
- output 10: float32 [2, 128], replicated
- output 11: float32 [2, 128, 128], P(None, None, 'tp')
- output 12: float32 [2, 3, 128], P(None, None, 'tp')
All inputs are finite; a program needn't handle non-finite values.
Results may differ from the reference program's by a relative error of at most 0.0186387.
Values sent between devices are 32-bit elements.
A program may use at most 1 GiB of HBM per device.

```python
import jax
import jax.numpy as jnp
from jax import lax

D = 128
NODES = 1885
EDGES = 10910
BATCH = 16
LAYERS = 2
LN_EPS = 1e-5


def normal_draw(base_key, arr_shape):
    return jax.random.normal(base_key, arr_shape, jnp.float32)


def vec_draw(base_key):
    noise_val = normal_draw(base_key, (LAYERS, 3, D))
    scales = jnp.array([0.5, 0.3, 0.3], jnp.float32)[None, :, None]
    shifts = jnp.array([0.0, 1.0, 0.0], jnp.float32)[None, :, None]
    return noise_val * scales + shifts


def index_draw(base_key):
    idx_keys = jax.random.split(base_key, 4)
    extra_edges = EDGES - NODES
    senders = jnp.concatenate([
        jax.random.randint(idx_keys[0], (extra_edges,), 0, NODES, dtype=jnp.int32),
        jax.random.permutation(idx_keys[1], NODES).astype(jnp.int32)])
    receivers = jnp.concatenate([
        jax.random.permutation(idx_keys[2], NODES).astype(jnp.int32),
        jax.random.randint(idx_keys[3], (extra_edges,), 0, NODES, dtype=jnp.int32)])
    return senders, receivers


def setup_inputs(seed: int = 0) -> dict:
    sub_keys = jax.random.split(jax.random.key(seed), 13)
    senders, receivers = index_draw(sub_keys[12])
    node_shape = (BATCH, NODES, D)
    edge_shape = (BATCH, EDGES, D)
    return {
        'node_lat': normal_draw(sub_keys[0], node_shape).astype(jnp.bfloat16),
        'edge_lat': normal_draw(sub_keys[1], edge_shape).astype(jnp.bfloat16),
        'senders': senders,
        'receivers': receivers,
        'grad_node': normal_draw(sub_keys[2], node_shape).astype(jnp.bfloat16),
        'grad_edge': normal_draw(sub_keys[3], edge_shape).astype(jnp.bfloat16),
        'edge_w1': (normal_draw(sub_keys[4], (LAYERS, 3, D, D)) * (3 * D) ** -0.5).astype(jnp.bfloat16),
        'edge_b1': 0.5 * normal_draw(sub_keys[5], (LAYERS, D)),
        'edge_w2': (normal_draw(sub_keys[6], (LAYERS, D, D)) * D ** -0.5).astype(jnp.bfloat16),
        'edge_vec': vec_draw(sub_keys[7]),
        'node_w1': (normal_draw(sub_keys[8], (LAYERS, 2, D, D)) * (2 * D) ** -0.5).astype(jnp.bfloat16),
        'node_b1': 0.5 * normal_draw(sub_keys[9], (LAYERS, D)),
        'node_w2': (normal_draw(sub_keys[10], (LAYERS, D, D)) * D ** -0.5).astype(jnp.bfloat16),
        'node_vec': vec_draw(sub_keys[11]),
    }


def mlp_norm(inputs, w_first, b_first, w_second, norm_vec):
    hidden = b_first
    for block_id in range(len(inputs)):
        hidden = hidden + jnp.dot(inputs[block_id], w_first[block_id].astype(jnp.bfloat16), preferred_element_type=jnp.float32)
    act_bf = jax.nn.silu(hidden).astype(jnp.bfloat16)
    out_f32 = jnp.dot(act_bf, w_second.astype(jnp.bfloat16), preferred_element_type=jnp.float32) + norm_vec[0]
    row_mean = jnp.mean(out_f32, axis=-1, keepdims=True)
    centered = out_f32 - row_mean
    row_var = jnp.mean(centered * centered, axis=-1, keepdims=True)
    return (centered * lax.rsqrt(row_var + LN_EPS) * norm_vec[1] + norm_vec[2]).astype(jnp.bfloat16)


def layer_step(node_lat, edge_lat, senders, receivers, layer_par):
    edge_w1, edge_b1, edge_w2, edge_vec, node_w1, node_b1, node_w2, node_vec = layer_par
    send_lat = jnp.take(node_lat, senders, axis=0)
    recv_lat = jnp.take(node_lat, receivers, axis=0)
    edge_msg = mlp_norm((edge_lat, send_lat, recv_lat), edge_w1, edge_b1, edge_w2, edge_vec)
    node_agg = jax.ops.segment_sum(edge_msg.astype(jnp.float32), receivers, num_segments=node_lat.shape[0]).astype(jnp.bfloat16)
    node_msg = mlp_norm((node_lat, node_agg), node_w1, node_b1, node_w2, node_vec)
    new_node = (node_lat.astype(jnp.float32) + node_msg.astype(jnp.float32)).astype(jnp.bfloat16)
    new_edge = (edge_lat.astype(jnp.float32) + edge_msg.astype(jnp.float32)).astype(jnp.bfloat16)
    return new_node, new_edge


def sample_forward(node_lat, edge_lat, senders, receivers, params):
    def layer_body(carry_lat, layer_par):
        return layer_step(carry_lat[0], carry_lat[1], senders, receivers, layer_par), None
    final_lat, unused_out = lax.scan(layer_body, (node_lat, edge_lat), params)
    return final_lat


def reference(node_lat, edge_lat, senders, receivers, grad_node, grad_edge, edge_w1, edge_b1, edge_w2, edge_vec, node_w1, node_b1, node_w2, node_vec):
    params = (edge_w1.astype(jnp.float32), edge_b1, edge_w2.astype(jnp.float32), edge_vec,
              node_w1.astype(jnp.float32), node_b1, node_w2.astype(jnp.float32), node_vec)

    def forward_fn(node_one, edge_one, par_f32):
        return sample_forward(node_one, edge_one, senders, receivers, par_f32)

    def per_sample(grad_acc, sample):
        node_one, edge_one, gnode_one, gedge_one = sample
        fwd_outs, pullback = jax.vjp(forward_fn, node_one, edge_one, params)
        d_node, d_edge, d_params = pullback((gnode_one, gedge_one))
        grad_acc = tuple(acc_part + new_part for acc_part, new_part in zip(grad_acc, d_params))
        return grad_acc, (fwd_outs[0], fwd_outs[1], d_node, d_edge)

    zero_acc = tuple(jnp.zeros(par_arr.shape, jnp.float32) for par_arr in params)
    grad_acc, per_out = lax.scan(per_sample, zero_acc, (node_lat, edge_lat, grad_node, grad_edge))
    return (per_out[0], per_out[1], per_out[2], per_out[3],
            grad_acc[0], grad_acc[1], grad_acc[2], grad_acc[3],
            grad_acc[4], grad_acc[5], grad_acc[6], grad_acc[7])
```

```python
import jax
import jax.numpy as jnp
from jax import lax
from jax.experimental import pallas as pl
from jax.experimental.pallas import tpu as pltpu
from jax.sharding import PartitionSpec as P

LN_EPS = 1e-5
D = 128
T = 256
TN = 384
BF = jnp.bfloat16
F32 = jnp.float32
VM = pl.BlockSpec(memory_space=pltpu.VMEM)


def dot(a, b):
    return jnp.dot(a, b, preferred_element_type=F32)


def dot_nt(a, b):
    return lax.dot_general(a, b, (((1,), (1,)), ((), ())), preferred_element_type=F32)


def gather(table, row, iota):
    acc = None
    nodes = table.shape[1]
    one, zero = jnp.ones((), BF), jnp.zeros((), BF)
    for base in range(0, nodes, T):
        width = min(T, nodes - base)
        key = (row - float(base)).astype(BF)
        hot = jnp.where(iota[:width, :] == key, one, zero)
        part = dot(table[:, base:base + width], hot)
        acc = part if acc is None else acc + part
    return acc


def scatter(acc_ref, val, low, high, lanes):
    nodes = acc_ref.shape[1]
    one, zero = jnp.ones((), BF), jnp.zeros((), BF)
    none = jnp.full((), -1, BF)
    for block, base in enumerate(range(0, nodes, T)):
        width = min(T, nodes - base)
        key = jnp.where(high == jnp.full((), block, BF), low, none)
        hot = jnp.concatenate([jnp.where(lanes[0:1, s:s + D] == key, one, zero) for s in range(0, width, D)], axis=1)
        acc_ref[:, base:base + width] += dot(val, hot)


def sigmoid(hidden):
    return 1.0 / (1.0 + jnp.exp(-hidden))


def mlp_tail(hidden, w2t, vec):
    act = (hidden * sigmoid(hidden)).astype(BF)
    out = dot(w2t[...], act) + vec[:, 0:1]
    mean = jnp.sum(out, axis=0, keepdims=True) * (1.0 / D)
    centered = out - mean
    var = jnp.sum(centered * centered, axis=0, keepdims=True) * (1.0 / D)
    inv = lax.rsqrt(var + LN_EPS)
    normed = centered * inv
    message = (normed * vec[:, 1:2] + vec[:, 2:3]).astype(BF)
    return message, normed, inv


def fold(val):
    total = val[:, 0:D]
    for start in range(D, val.shape[1], D):
        total = total + val[:, start:start + D]
    return total


def mlp_back(d_msg, hidden, normed, inv, w2, vec, dw2, sums):
    sums[D:2 * D, :] += fold(d_msg * normed)
    sums[2 * D:3 * D, :] += fold(d_msg)
    d_normed = d_msg * vec[:, 1:2]
    mean0 = jnp.sum(d_normed, axis=0, keepdims=True) * (1.0 / D)
    mean1 = jnp.sum(d_normed * normed, axis=0, keepdims=True) * (1.0 / D)
    d_out = inv * (d_normed - mean0 - normed * mean1)
    sums[0:D, :] += fold(d_out)
    d_out_bf = d_out.astype(BF)
    sig = sigmoid(hidden)
    act = (hidden * sig).astype(BF)
    dw2[...] += dot_nt(d_out_bf, act)
    d_hidden = dot(w2[...], d_out_bf) * (sig * (1.0 + hidden * (1.0 - sig)))
    sums[3 * D:4 * D, :] += fold(d_hidden)
    return d_hidden.astype(BF)


def finish_sums(sums, out):
    for q in range(4):
        out[:, q:q + 1] = jnp.sum(sums[q * D:(q + 1) * D, :], axis=1, keepdims=True)


def swap_halves(val):
    q = D // 4
    return jnp.concatenate([val[q:2 * q], val[0:q], val[3 * q:], val[2 * q:3 * q]], axis=0)


def edge_forward_kernel(srow, rrow, rlow, rhigh, iota, lanes, table, edge, w1t, b1, w2t, vec,
                        edge_out, hidden, normed, inv, agg):
    agg[...] = jnp.zeros_like(agg)

    def body(step, _):
        at = pl.ds(pl.multiple_of(step * T, T), T)
        e_in = edge[:, at]
        xs = gather(table, srow[:, at], iota).astype(BF)
        xr = gather(table, rrow[:, at], iota).astype(BF)
        hid = dot(w1t[...], jnp.concatenate([e_in, xs, xr], axis=0)) + b1[...]
        hidden[:, at] = hid
        msg, nrm, std = mlp_tail(hid, w2t, vec)
        normed[:, at] = nrm
        inv[:, at] = std
        edge_out[:, at] = (e_in.astype(F32) + msg.astype(F32)).astype(BF)
        scatter(agg, msg, rlow[at, :], rhigh[at, :], lanes)
        return 0

    lax.fori_loop(0, edge.shape[1] // T, body, 0)


def node_forward_kernel(table, agg_own, agg_other, w1t, b1, w2t, vec, node_out, agg, hidden, normed, inv):
    def body(step, _):
        at = pl.ds(pl.multiple_of(step * TN, D), TN)
        v_in = table[:, at]
        agg_bf = (agg_own[:, at] + swap_halves(agg_other[:, at])).astype(BF)
        agg[:, at] = agg_bf
        hid = dot(w1t[...], jnp.concatenate([v_in, agg_bf], axis=0)) + b1[...]
        hidden[:, at] = hid
        msg, nrm, std = mlp_tail(hid, w2t, vec)
        normed[:, at] = nrm
        inv[:, at] = std
        node_out[:, at] = (v_in.astype(F32) + msg.astype(F32)).astype(BF)
        return 0

    lax.fori_loop(0, table.shape[1] // TN, body, 0)


def node_backward_kernel(d_part, d_own, d_other, table, agg, hidden, normed, inv, w1, w2, vec,
                         d_agg, d_node, dw1, dw2, dvec, sums):
    dw1[...] = jnp.zeros_like(dw1)
    dw2[...] = jnp.zeros_like(dw2)
    sums[...] = jnp.zeros_like(sums)

    def body(step, _):
        at = pl.ds(pl.multiple_of(step * TN, D), TN)
        d_in = (d_part[:, at] + d_own[:, at] + swap_halves(d_other[:, at])).astype(BF).astype(F32)
        d_hid = mlp_back(d_in, hidden[:, at], normed[:, at], inv[:, at], w2, vec, dw2, sums)
        dw1[0:D, :] += dot_nt(table[:, at], d_hid)
        dw1[D:2 * D, :] += dot_nt(agg[:, at], d_hid)
        d_node[:, at] = d_in + dot(w1[0:D, :], d_hid)
        d_agg[:, at] = dot(w1[D:2 * D, :], d_hid).astype(BF)
        return 0

    lax.fori_loop(0, table.shape[1] // TN, body, 0)
    finish_sums(sums, dvec)


def edge_backward_kernel(rrow, slow, shigh, rlow, rhigh, iota, lanes, d_agg, d_edge, table, edge, hidden, normed, inv,
                         w1, w2, vec, d_edge_in, d_node, dw1, dw2, dvec, sums, send_sum, recv_sum):
    dw1[...] = jnp.zeros_like(dw1)
    dw2[...] = jnp.zeros_like(dw2)
    sums[...] = jnp.zeros_like(sums)
    send_sum[...] = jnp.zeros_like(send_sum)
    recv_sum[...] = jnp.zeros_like(recv_sum)

    def body(step, _):
        at = pl.ds(pl.multiple_of(step * T, T), T)
        d_out = d_edge[:, at].astype(F32)
        d_msg = d_out + gather(d_agg, rrow[:, at], iota)
        d_hid = mlp_back(d_msg, hidden[:, at], normed[:, at], inv[:, at], w2, vec, dw2, sums)
        dw1[0:D, :] += dot_nt(edge[:, at], d_hid)
        d_edge_in[:, at] = (d_out + dot(w1[0:D, :], d_hid)).astype(BF)
        scatter(send_sum, d_hid, slow[at, :], shigh[at, :], lanes)
        scatter(recv_sum, d_hid, rlow[at, :], rhigh[at, :], lanes)
        return 0

    lax.fori_loop(0, edge.shape[1] // T, body, 0)

    def project(step, _):
        at = pl.ds(pl.multiple_of(step * TN, D), TN)
        s_bf = send_sum[:, at].astype(BF)
        r_bf = recv_sum[:, at].astype(BF)
        v_in = table[:, at]
        d_node[:, at] = dot(w1[D:2 * D, :], s_bf) + dot(w1[2 * D:3 * D, :], r_bf)
        dw1[D:2 * D, :] += dot_nt(v_in, s_bf)
        dw1[2 * D:3 * D, :] += dot_nt(v_in, r_bf)
        return 0

    lax.fori_loop(0, table.shape[1] // TN, project, 0)
    finish_sums(sums, dvec)


def join_kernel(*refs):
    out = refs[-1]
    rows = refs[0].shape[0]
    for d, piece in enumerate(refs[:-1]):
        out[d * rows:(d + 1) * rows, :] = piece[...].astype(out.dtype)


def place_edges_kernel(where, *refs):
    out = refs[-1]
    for d, piece in enumerate(refs[:-1]):
        width = piece.shape[1]
        for half in range(2):
            used = min(width, out.shape[2] - half * width)

            @pl.when((where[1] ^ (d & 1)) == half)
            def _():
                out[where[0] ^ (d >> 1), :, half * width:half * width + used] = piece[:, 0:used].astype(out.dtype)


def place_nodes_kernel(where, *refs):
    out = refs[-1]
    for d, piece in enumerate(refs[:-1]):
        out[where[0] ^ d] = piece[:, 0:out.shape[2]].astype(out.dtype)


def call(kernel, name, outs, args, flops, scratch=()):
    moved = sum(a.size * a.dtype.itemsize for a in args) + sum(s.size * s.dtype.itemsize for s in outs)
    return pl.pallas_call(
        kernel,
        name=name,
        out_shape=outs,
        in_specs=[VM] * len(args),
        out_specs=[VM] * len(outs),
        scratch_shapes=list(scratch),
        compiler_params=pltpu.CompilerParams(vmem_limit_bytes=56 * 1024 * 1024),
        cost_estimate=pl.CostEstimate(flops=flops, bytes_accessed=moved, transcendentals=0),
    )(*args)


def solution(mesh):
    lat_spec = P('dp', None, 'tp')
    first_spec = P(None, None, 'tp', None)
    col_spec = P(None, None, 'tp')
    param_specs = (first_spec, P(), col_spec, col_spec, first_spec, P(), col_spec, col_spec)
    in_specs = (lat_spec, lat_spec, P(), P(), lat_spec, lat_spec) + param_specs
    out_specs = (lat_spec, lat_spec, lat_spec, lat_spec) + param_specs
    tp = mesh.shape['tp']
    shape = jax.ShapeDtypeStruct

    def exchange(val, d):
        return lax.ppermute(val, 'tp', [(t, t ^ d) for t in range(tp)])

    def local_step(node_lat, edge_lat, senders, receivers, grad_node, grad_edge, edge_w1, edge_b1, edge_w2, edge_vec, node_w1, node_b1, node_w2, node_vec):
        layers = edge_w1.shape[0]
        cols = node_lat.shape[2]
        nodes, edges = node_lat.shape[1], edge_lat.shape[1]
        np_ = -(-nodes // TN) * TN
        eh = -(-edges // (2 * T)) * T
        tpi = lax.axis_index('tp')
        x, c = tpi // 2, tpi % 2

        def edge_pieces(arr):
            wide = jnp.pad(jnp.swapaxes(arr, 1, 2).astype(F32), ((0, 0), (0, 0), (0, 2 * eh - edges)))
            got = []
            for d in range(4):
                piece = lax.dynamic_slice(wide, (x ^ (d >> 1), 0, (c ^ (d & 1)) * eh), (1, cols, eh))[0]
                got.append(exchange(piece, d) if d else piece)
            return call(join_kernel, 'join_edges', [shape((D, eh), BF)], got, 0)[0]

        def node_pieces(arr, kind):
            wide = jnp.pad(jnp.swapaxes(arr, 1, 2).astype(F32), ((0, 0), (0, 0), (0, np_ - nodes)))
            got = []
            for d in range(4):
                piece = lax.dynamic_slice(wide, (x ^ (d >> 1), 0, 0), (1, cols, np_))[0]
                got.append(exchange(piece, d) if d else piece)
            return call(join_kernel, 'join_nodes', [shape((D, np_), kind)], got, 0)[0]

        lane_pad = ((0, 0), (0, 0), (0, D - 3))
        pack = jnp.concatenate([
            edge_w1.astype(F32).reshape(-1, D),
            jnp.swapaxes(edge_w2, 1, 2).astype(F32).reshape(-1, D),
            node_w1.astype(F32).reshape(-1, D),
            jnp.swapaxes(node_w2, 1, 2).astype(F32).reshape(-1, D),
            jnp.pad(jnp.swapaxes(edge_vec, 1, 2), lane_pad).reshape(-1, D),
            jnp.pad(jnp.swapaxes(node_vec, 1, 2), lane_pad).reshape(-1, D)], axis=0)
        packs = jnp.stack([exchange(pack, d) if d else pack for d in range(4)])
        sizes = [layers * 3 * cols, layers * cols, layers * 2 * cols, layers * cols, layers * cols, layers * cols]
        starts = [sum(sizes[:q]) for q in range(6)]
        parts = [packs[:, s:s + n] for s, n in zip(starts, sizes)]

        def full_first(part, k):
            return jnp.transpose(part.reshape(4, layers, k, cols, D), (1, 2, 0, 3, 4)).reshape(layers, k * D, D).astype(BF)

        def full_second(part):
            return jnp.transpose(part.reshape(4, layers, cols, D), (1, 0, 2, 3)).reshape(layers, D, D)

        ew1, nw1 = full_first(parts[0], 3), full_first(parts[2], 2)
        ew2t, nw2t = full_second(parts[1]).astype(BF), full_second(parts[3]).astype(BF)
        evec, nvec = full_second(parts[4]), full_second(parts[5])
        ew1t, nw1t = jnp.swapaxes(ew1, 1, 2), jnp.swapaxes(nw1, 1, 2)
        ew2, nw2 = jnp.swapaxes(ew2t, 1, 2), jnp.swapaxes(nw2t, 1, 2)
        eb1 = edge_b1[:, :, None]
        nb1 = node_b1[:, :, None]

        def ids(arr):
            wide = jnp.pad(arr, (0, 2 * eh - edges), constant_values=-1)
            return lax.dynamic_slice(wide, (c * eh,), (eh,))

        def row_form(idx):
            return idx.astype(F32)[None, :]

        def col_form(idx):
            low = jnp.where(idx < 0, -1, idx % T).astype(BF)
            high = (idx // T).astype(BF)
            return jnp.broadcast_to(low[:, None], (eh, D)), jnp.broadcast_to(high[:, None], (eh, D))

        sid, rid = ids(senders), ids(receivers)
        srow, rrow = row_form(sid), row_form(rid)
        slow, shigh = col_form(sid)
        rlow, rhigh = col_form(rid)
        iota = lax.broadcasted_iota(jnp.int32, (T, T), 0).astype(BF)
        lanes = lax.broadcasted_iota(jnp.int32, (16, T), 1).astype(BF)

        table = node_pieces(node_lat, BF)
        edge = edge_pieces(edge_lat)
        g_node = node_pieces(grad_node, F32)
        g_edge = edge_pieces(grad_edge)
        where = jnp.stack([x, c]).astype(jnp.int32)

        e_flops = 2 * eh * D * (2 * np_ + 4 * D + np_)
        n_flops = 2 * np_ * D * 6 * D

        saved = []
        for l in range(layers):
            e_outs = [shape((D, eh), BF), shape((D, eh), F32), shape((D, eh), F32), shape((1, eh), F32), shape((D, np_), F32)]
            e_next, hid, nrm, inv, agg_own = call(
                edge_forward_kernel, f'edge_fwd{l}', e_outs,
                (srow, rrow, rlow, rhigh, iota, lanes, table, edge, ew1t[l], eb1[l], ew2t[l], evec[l]), e_flops)
            agg_other = exchange(agg_own, 1)
            n_outs = [shape((D, np_), BF), shape((D, np_), BF), shape((D, np_), F32), shape((D, np_), F32), shape((1, np_), F32)]
            v_next, agg, nhid, nnrm, ninv = call(
                node_forward_kernel, f'node_fwd{l}', n_outs,
                (table, agg_own, agg_other, nw1t[l], nb1[l], nw2t[l], nvec[l]), n_flops)
            saved.append((table, edge, hid, nrm, inv, agg, nhid, nnrm, ninv))
            table, edge = v_next, e_next

        def place(kernel, name, pieces, out):
            return pl.pallas_call(
                kernel, name=name, out_shape=out, in_specs=[pl.BlockSpec(memory_space=pltpu.SMEM)] + [VM] * len(pieces), out_specs=VM,
                compiler_params=pltpu.CompilerParams(vmem_limit_bytes=32 * 1024 * 1024),
            )(where, *pieces).swapaxes(1, 2)

        def spread_edges(arr):
            wide = arr.astype(F32).reshape(4, cols, eh)
            got = [exchange(wide[d], d) if d else wide[0] for d in range(4)]
            return place(place_edges_kernel, 'place_edges', got, shape((2, cols, edges), BF))

        def spread_nodes(arr):
            wide = arr.astype(F32).reshape(4, cols, np_)
            return place(place_nodes_kernel, 'place_nodes', [wide[0], exchange(wide[2], 2)], shape((2, cols, nodes), BF))

        node_out, edge_out = spread_nodes(table), spread_edges(edge)

        zero = jnp.zeros((D, np_), F32)
        d_part, d_own, d_other = g_node, zero, zero
        d_edge = g_edge
        grads = []
        for l in reversed(range(layers)):
            table_l, edge_l, hid, nrm, inv, agg, nhid, nnrm, ninv = saved[l]
            nb_outs = [shape((D, np_), BF), shape((D, np_), F32), shape((2 * D, D), F32), shape((D, D), F32), shape((D, 4), F32)]
            d_agg, d_part, ndw1, ndw2, ndvec = call(
                node_backward_kernel, f'node_bwd{l}', nb_outs,
                (d_part, d_own, d_other, table_l, agg, nhid, nnrm, ninv, nw1[l], nw2[l], nvec[l]), 2 * n_flops,
                [pltpu.VMEM((4 * D, D), F32)])
            eb_outs = [shape((D, eh), BF), shape((D, np_), F32), shape((3 * D, D), F32), shape((D, D), F32), shape((D, 4), F32)]
            d_edge, d_own, edw1, edw2, edvec = call(
                edge_backward_kernel, f'edge_bwd{l}', eb_outs,
                (rrow, slow, shigh, rlow, rhigh, iota, lanes, d_agg, d_edge, table_l, edge_l, hid, nrm, inv, ew1[l], ew2[l], evec[l]),
                e_flops, [pltpu.VMEM((4 * D, D), F32), pltpu.VMEM((D, np_), F32), pltpu.VMEM((D, np_), F32)])
            d_other = exchange(d_own, 1)
            grads.append((edw1, edw2, edvec, ndw1, ndw2, ndvec))
        grads = grads[::-1]
        d_node = (d_part + d_own + d_other.reshape(2, 2, cols, np_)[:, ::-1].reshape(D, np_)).astype(BF)
        d_node_out, d_edge_out = spread_nodes(d_node), spread_edges(d_edge)

        half = jnp.where(c == 0, 1.0, 0.0).astype(F32)

        def stack(q, k):
            return jnp.stack([g[q] for g in grads]).reshape(layers, k, 4, cols, -1)

        blocks = []
        ew, ew2g, ev = stack(0, 3), stack(1, 1), stack(2, 1)
        nw, nw2g, nv = stack(3, 2), stack(4, 1), stack(5, 1)
        for d in range(4):
            pad = lambda a: jnp.pad(a, ((0, 0), (0, 0), (0, 0), (0, D - a.shape[-1])))
            blocks.append(jnp.concatenate([
                ew[:, :, d].reshape(-1, D), ew2g[:, :, d].reshape(-1, D), pad(ev[:, :, d]).reshape(-1, D),
                half * nw[:, :, d].reshape(-1, D), half * nw2g[:, :, d].reshape(-1, D), half * pad(nv[:, :, d]).reshape(-1, D)], axis=0))
        total = blocks[0]
        for d in range(1, 4):
            total = total + exchange(blocks[d], d)
        b1_sum = jnp.stack([jnp.stack([g[2][:, 3] for g in grads]), half * jnp.stack([g[5][:, 3] for g in grads])])
        b1_sum = lax.psum(b1_sum, ('dp', 'tp'))
        total = lax.psum(total, 'dp')
        rows = [layers * 3 * cols, layers * cols, layers * cols, layers * 2 * cols, layers * cols, layers * cols]
        offs = [sum(rows[:q]) for q in range(6)]
        ew, ew2g, ev, nw, nw2g, nv = [total[o:o + n] for o, n in zip(offs, rows)]
        return (node_out, edge_out, d_node_out, d_edge_out,
                ew.reshape(layers, 3, cols, D), b1_sum[0], jnp.swapaxes(ew2g.reshape(layers, cols, D), 1, 2),
                jnp.swapaxes(ev.reshape(layers, cols, D)[:, :, :3], 1, 2),
                nw.reshape(layers, 2, cols, D), b1_sum[1], jnp.swapaxes(nw2g.reshape(layers, cols, D), 1, 2),
                jnp.swapaxes(nv.reshape(layers, cols, D)[:, :, :3], 1, 2))

    return jax.shard_map(local_step, mesh=mesh, in_specs=in_specs, out_specs=out_specs, check_vma=False)
```

```python
import jax
import jax.numpy as jnp
from jax import lax
from jax.experimental import pallas as pl
from jax.experimental.pallas import tpu as pltpu
from jax.sharding import PartitionSpec as P

LN_EPS = 1e-5
D = 128
T = 256
TN = 384
EC = 512
KS = 1408
BF = jnp.bfloat16
F32 = jnp.float32
I16 = jnp.int16
MESH = pl.DeviceIdType.MESH
VM = pl.BlockSpec(memory_space=pltpu.VMEM)
HB = pl.BlockSpec(memory_space=pl.ANY)
GROUP = 4
BOTH = (0, 1)
THREE = (0, 1, 2)
OTHERS = (1, 2, 3)
EDGE_IN, GRAD_IN, EDGE_OUT, GRAD_OUT = range(4)
SEND_ORDER = (2, 3, 1)
LROWS = 7 * (D // 4)
HEAD = 16
SLABS = 8


def dot(a, b):
    return jnp.dot(a, b, preferred_element_type=F32)


def dot_nt(a, b):
    return lax.dot_general(a, b, (((1,), (1,)), ((), ())), preferred_element_type=F32)


def mat(k, n=1):
    return slice(k * D, (k + n) * D)


def rows_of(d):
    q = D // 4
    return slice(d * q, (d + 1) * q)


def at(step, width):
    return pl.ds(pl.multiple_of(step * width, width), width)


def loop(stop, body, start=0):
    def step(j, carry):
        body(j)
        return carry

    lax.fori_loop(start, stop, step, 0)


def column_sum(val):
    return jnp.sum(val, axis=0, keepdims=True)


def flip(val):
    return jnp.swapaxes(val, 0, 1)


def stacked(parts):
    return jnp.concatenate(parts, axis=0)


def beside(parts):
    return jnp.concatenate(parts, axis=1)


def slot(d):
    return d - 1


def sigmoid(hidden):
    return 1.0 / (1.0 + jnp.exp(-hidden))


def fold(val):
    total = val[:, mat(0)]
    for start in range(D, val.shape[1], D):
        total = total + val[:, start:start + D]
    return total


def swap_halves(val):
    return stacked([val[rows_of(d)] for d in (1, 0, 3, 2)])


def gather(table, keys, iota):
    acc = None
    nodes = table.shape[1]
    one, zero = jnp.ones((), BF), jnp.zeros((), BF)
    for base in range(0, nodes, T):
        width = min(T, nodes - base)
        ids = iota[0:width, :]
        hot = beside([jnp.where(ids == (key - jnp.asarray(base, I16)), one, zero) for key in keys])
        part = dot(table[:, base:base + width], hot)
        acc = part if acc is None else acc + part
    return acc


def scatter(acc_ref, val, cols, lanes):
    nodes = acc_ref.shape[1]
    one, zero = jnp.ones((), BF), jnp.zeros((), BF)
    row = lanes[0:1, :]
    for base in range(0, nodes, T):
        width = min(T, nodes - base)
        hot = beside([jnp.where((row + jnp.asarray(base + s, I16)) == cols, one, zero) for s in range(0, width, D)])
        acc_ref[:, base:base + width] += dot(val, hot)


def mlp_tail(hidden, w2t, vec):
    act = (hidden * sigmoid(hidden)).astype(BF)
    out = dot(w2t, act) + vec[0]
    mean = column_sum(out) / D
    centered = out - mean
    var = column_sum(centered * centered) / D
    inv = lax.rsqrt(var + LN_EPS)
    normed = centered * inv
    message = (normed * vec[1] + vec[2]).astype(BF)
    return message, normed, inv


def mlp_back(d_msg, hidden, normed, inv, w2, vec):
    d_normed = d_msg * vec[1]
    mean0 = column_sum(d_normed) / D
    mean1 = column_sum(d_normed * normed) / D
    d_out = inv * (d_normed - mean0 - normed * mean1)
    d_out_bf = d_out.astype(BF)
    sig = sigmoid(hidden)
    act = (hidden * sig).astype(BF)
    d_w2 = dot_nt(d_out_bf, act)
    d_hidden = dot(w2, d_out_bf) * (sig * (1.0 + hidden * (1.0 - sig)))
    sums = (fold(d_out), fold(d_msg * normed), fold(d_msg), fold(d_hidden))
    return d_hidden.astype(BF), d_w2, sums


def add_sums(ref, parts):
    for q in range(4):
        total = parts[0][q]
        for other in parts[1:]:
            total = total + other[q]
        ref[mat(q), :] += total


def step_kernel(dims, *refs):
    layers, cols, nodes, edges, npad, eh, dpn = dims
    nch = eh // EC
    top = layers - 1
    n_in = 11
    (node_in, edge_in, gnode_in, gedge_in, idx, ew1_in, ew2_in, nw1_in, nw2_in, vec_in, b1_in) = refs[:n_in]
    n_out = 12
    (node_out, edge_out, dnode_out, dedge_out, ew1_out, eb1_out, ew2_out, evec_out, nw1_out, nb1_out, nw2_out, nvec_out) = refs[n_in:n_in + n_out]
    (node_raw, gnode_raw, edge_raw, gedge_raw, w_send, w_recv, n_send, n_recv, gn_send, gn_recv, no_send, no_recv, dn_send, dn_recv,
     e_send, g_send, e_recv, g_recv, eo_recv, de_recv, part, part_recv, hidden, normed, inv, nhid, nnrm, ninv, d_part, s_sum, r_sum,
     sums, grad, core_recv, half, dp_recv, cross_send, cross_recv, own_sum, gathered,
     core_ss, core_rs, dp_ss, dp_rs, cross_ss, cross_rs, load_sem, w_ss, w_rs, n_ss, n_rs, e_ss, e_rs, p_ss, p_rs, out_sem) = refs[n_in + n_out:]

    t = lax.axis_index('tp')
    p = lax.axis_index('dp')
    per = SLABS // dpn
    dp_others = range(1, dpn)
    x, c = t // 2, lax.rem(t, 2)
    ox, oc = 1 - x, 1 - c
    peer = [t, t + 1 - 2 * c, t + 2 - 4 * x, t + 3 - 2 * c - 4 * x]

    def remote(src, dst, ssem, rsem, d):
        return pltpu.make_async_remote_copy(src_ref=src, dst_ref=dst, send_sem=ssem, recv_sem=rsem,
                                            device_id={'tp': peer[d]}, device_id_type=MESH)

    loads = [pltpu.make_async_copy(src, dst, load_sem.at[q]) for q, (src, dst) in enumerate(
        [(node_in, node_raw), (edge_in, edge_raw), (gnode_in, gnode_raw), (gedge_in, gedge_raw)])]
    for copy in loads:
        copy.start()

    barrier = pltpu.get_barrier_semaphore()
    for d in OTHERS:
        pl.semaphore_signal(barrier, inc=1, device_id={'tp': peer[d]}, device_id_type=MESH)
    for i in dp_others:
        pl.semaphore_signal(barrier, inc=1, device_id={'dp': lax.rem(p + i, dpn)}, device_id_type=MESH)
    pl.semaphore_wait(barrier, len(OTHERS) + dpn - 1)

    def node_copies(send, recv, kind):
        return (remote(send.at[1], recv.at[0], n_ss.at[kind, 0], n_rs.at[kind, 0], 1),
                remote(send.at[0], recv.at[1], n_ss.at[kind, 1], n_rs.at[kind, 1], 2),
                remote(recv.at[1], recv.at[2], n_ss.at[kind, 2], n_rs.at[kind, 2], 1))

    def weight_copies(kind):
        rows = (pl.ds(0, HEAD + LROWS), pl.ds(HEAD + LROWS, LROWS * (top)))[kind]
        return (remote(w_send.at[rows], w_recv.at[0, rows], w_ss.at[kind, 0], w_rs.at[kind, 0], 1),
                remote(w_send.at[rows], w_recv.at[1, rows], w_ss.at[kind, 1], w_rs.at[kind, 1], 2),
                remote(w_recv.at[1, rows], w_recv.at[2, rows], w_ss.at[kind, 2], w_rs.at[kind, 2], 1))

    def edge_copy(kind, j, d):
        src, dst = ((e_send, e_recv), (g_send, g_recv), (e_send, eo_recv), (g_send, de_recv))[kind]
        lanes_j = at(j, EC)
        return remote(src.at[slot(d), :, lanes_j], dst.at[slot(d), :, lanes_j], e_ss.at[kind, slot(d), j], e_rs.at[kind, slot(d), j], d)

    def core_copy(l, b):
        return remote(grad.at[l, :, pl.ds((2 * b + 1) * cols, cols), :], core_recv.at[l, b], core_ss.at[l, b], core_rs.at[l, b], 1)

    def dp_remote(src, dst, stage, l, i):
        return pltpu.make_async_remote_copy(src_ref=src, dst_ref=dst, send_sem=dp_ss.at[stage, l, i - 1], recv_sem=dp_rs.at[stage, l, i - 1],
                                            device_id={'dp': lax.rem(p + i, dpn)}, device_id_type=MESH)

    def spread_copy(l, i):
        return dp_remote(half.at[l, pl.ds(lax.rem(p + i, dpn) * per, per)], dp_recv.at[l, i - 1], 0, l, i)

    def cross_copy(l):
        return remote(cross_send.at[l], cross_recv.at[l], cross_ss.at[l], cross_rs.at[l], 2)

    def gather_copy(l, i, owner):
        return dp_remote(own_sum.at[l], gathered.at[l, pl.ds(owner * per, per)], 1, l, i)

    def part_copy(q):
        return remote(part.at[q], part_recv.at[q], p_ss.at[q], p_rs.at[q], 1)

    def load_nodes(raw, send, own):
        send[...] = jnp.zeros_like(send)
        send[0, :, :nodes] = raw[ox].astype(F32)
        send[1, :, :nodes] = raw[x].astype(F32)
        own[:cols, :] = send[1].astype(own.dtype)

    def load_edges(raw, send, own, kind):
        def put(j, lanes_j, val_of):
            for d in OTHERS:
                sample = x if d < 2 else ox
                send[slot(d), :, lanes_j] = val_of(sample, oc if d % 2 else c).astype(F32)
            own[:cols, lanes_j] = val_of(x, c)

        def chunk(j):
            put(j, at(j, EC), lambda s, h: raw[s, :, pl.ds(pl.multiple_of(h * eh + j * EC, D), EC)])
            for d in SEND_ORDER:
                edge_copy(kind, j, d).start()

        loop(nch - 1, chunk)
        first = (nch - 1) * EC
        used = edges - eh - first
        last = pl.ds(first, EC)

        def tail(s, h):
            left = raw[s, :, pl.ds(first, EC)]
            right = beside([raw[s, :, pl.ds(eh + first, used)], jnp.zeros((cols, EC - used), BF)])
            return jnp.where(h == 0, left.astype(F32), right.astype(F32)).astype(BF)

        put(nch - 1, last, tail)
        for d in SEND_ORDER:
            edge_copy(kind, nch - 1, d).start()

    def place_edges(raw, block, d, j):
        s = x if d < 2 else ox
        h = oc if d % 2 else c
        val = block.astype(BF)
        first = (nch - 1) * EC
        used = edges - eh - first

        @pl.when(jnp.logical_or(j < nch - 1, h == 0))
        def _():
            raw[s, :, pl.ds(pl.multiple_of(h * eh + j * EC, D), EC)] = val

        @pl.when(jnp.logical_and(j == nch - 1, h == 1))
        def _():
            raw[s, :, pl.ds(eh + first, used)] = val[:, :used]

    def scoped(e0, e1, ge, msg, v0, v1, v2, agg0, agg1, d_agg, scol, rcol, srow, rrow, iota, lanes, ew1, ew1t, ew2, ew2t, nw1, nw1t, nw2, nw2t, vecs):
        tables = (v0, v1, v2)
        aggs = (agg0, agg1)
        edges_in = (e0, e1)

        loads[0].wait()
        load_nodes(node_raw, n_send, v0)
        ncop = node_copies(n_send, n_recv, 0)
        ncop[1].start()
        ncop[0].start()
        q = cols
        w_send[:HEAD, :cols] = vec_in[...]
        for l in range(layers):
            off = HEAD + l * LROWS
            w_send[off:off + 3 * q, :] = ew1_in[l * 3 * q:(l + 1) * 3 * q, :].astype(F32)
            w_send[off + 3 * q:off + 4 * q, :] = ew2_in[l * q:(l + 1) * q, :].astype(F32)
            w_send[off + 4 * q:off + 6 * q, :] = nw1_in[l * 2 * q:(l + 1) * 2 * q, :].astype(F32)
            w_send[off + 6 * q:off + 7 * q, :] = nw2_in[l * q:(l + 1) * q, :].astype(F32)
        wcop = [weight_copies(kind) for kind in range(2)]
        wcop[0][1].start()
        wcop[0][0].start()
        loads[1].wait()
        load_edges(edge_raw, e_send, e0, EDGE_IN)
        wcop[1][1].start()
        wcop[1][0].start()
        loads[2].wait()
        load_nodes(gnode_raw, gn_send, d_part)
        gcop = node_copies(gn_send, gn_recv, 1)
        gcop[1].start()
        gcop[0].start()
        loads[3].wait()
        load_edges(gedge_raw, g_send, ge, GRAD_IN)

        iota[...] = lax.broadcasted_iota(jnp.int32, (T, D), 0).astype(I16)
        lanes[...] = lax.broadcasted_iota(jnp.int32, (16, D), 1).astype(I16)

        def ids(b):
            for which, (row_ref, col_ref) in enumerate(((srow, scol), (rrow, rcol))):
                row = idx[which, pl.ds(c * (eh // D) + b, 1), :]
                wide = jnp.broadcast_to(row, (D, D))
                row_ref[at(b, 16), :] = wide[:16].astype(I16)
                col_ref[at(b, D), :] = flip(wide.astype(F32)).astype(jnp.int32).astype(I16)

        loop(eh // D, ids)

        def keys(ref, step):
            return [ref[pl.ds(pl.multiple_of(step * (T // D) * 16 + 16 * h, 16), 1), :] for h in range(T // D)]

        def join_weights(l):
            off = HEAD + l * LROWS
            for d in range(GROUP):
                src = w_send if d == 0 else w_recv.at[slot(d)]
                r = slice(d * q, (d + 1) * q)
                for k in THREE:
                    ew1[l, k * D + d * q:k * D + (d + 1) * q, :] = src[off + k * q:off + (k + 1) * q, :].astype(BF)
                ew2t[l, r, :] = src[off + 3 * q:off + 4 * q, :].astype(BF)
                for k in range(2):
                    nw1[l, k * D + d * q:k * D + (d + 1) * q, :] = src[off + (4 + k) * q:off + (5 + k) * q, :].astype(BF)
                nw2t[l, r, :] = src[off + 6 * q:off + 7 * q, :].astype(BF)

            def flip_bf(mat):
                return flip(mat.astype(F32)).astype(BF)

            for k in THREE:
                ew1t[l, :, mat(k)] = flip_bf(ew1[l, mat(k), :])
            for k in range(2):
                nw1t[l, :, mat(k)] = flip_bf(nw1[l, mat(k), :])
            ew2[l] = flip_bf(ew2t[l])
            nw2[l] = flip_bf(nw2t[l])

        def wait_recvs(copies):
            copies[1].wait_recv()
            copies[2].start()
            copies[0].wait_recv()
            copies[2].wait_recv()

        wait_recvs(ncop)
        for d in OTHERS:
            v0[rows_of(d), :] = n_recv[slot(d)].astype(BF)
        wait_recvs(wcop[0])
        rows_all = beside([w_send[:HEAD, :cols]] + [w_recv[d, :HEAD, :cols] for d in range(3)])
        vecs[...] = flip(stacked([rows_all, jnp.zeros((D - HEAD, D), F32)]))
        join_weights(0)

        def vec(l, node):
            first = 6 * node + l
            return [vecs[:, first + 2 * k:first + 2 * k + 1] for k in THREE]

        def bias(l, node):
            return b1_in[:, 2 * node + l:2 * node + l + 1]

        def hidden_of_nodes(l):
            table, b1 = tables[l], bias(l, 0)

            def body(step):
                xs = gather(table, keys(srow, step), iota).astype(BF)
                xr = gather(table, keys(rrow, step), iota).astype(BF)
                hidden[l, :, at(step, T)] = dot(ew1t[l, :, mat(1, 2)], stacked([xs, xr])) + b1

            loop(eh // T, body)

        def edge_forward(l):
            e_in = edges_in[l]

            def body(j):
                for sub in range(EC // T):
                    a = at(j * (EC // T) + sub, T)
                    if l == 0:
                        if sub == 0:
                            for d in OTHERS:
                                edge_copy(EDGE_IN, j, d).wait_recv()
                        for d in OTHERS:
                            e_in[rows_of(d), a] = e_recv[slot(d), :, a].astype(BF)
                    e_val = e_in[:, a]
                    hid = hidden[l, :, a] + dot(ew1t[l, :, mat(0)], e_val)
                    hidden[l, :, a] = hid
                    message, nrm, std = mlp_tail(hid, ew2t[l], vec(l, 0))
                    normed[l, :, a] = nrm
                    inv[l:l + 1, a] = std
                    msg[:, a] = message
                    e_new = (e_val.astype(F32) + message.astype(F32)).astype(BF)
                    if l < top:
                        edges_in[l + 1][:, a] = e_new
                    else:
                        for d in OTHERS:
                            e_send[slot(d), :, a] = e_new[rows_of(d)].astype(F32)
                        if sub == 0:
                            own_parts = []
                        own_parts.append(e_new[:q])
                if l == top:
                    for d in SEND_ORDER:
                        edge_copy(EDGE_OUT, j, d).start()
                    place_edges(edge_raw, beside(own_parts), 0, j)

            loop(nch, body)

        def segment_sum(acc, ids_ref):
            acc[...] = jnp.zeros(acc.shape, F32)

            def body(step):
                scatter(acc, msg[:, at(step, KS)], ids_ref[at(step, KS), :], lanes)

            loop(eh // KS, body)

        def node_forward(l):
            table, agg, out = tables[l], aggs[l], tables[l + 1]

            def body(step):
                a = pl.ds(pl.multiple_of(step * TN, D), TN)
                v_in = table[:, a]
                agg_bf = (part[l, :, a] + swap_halves(part_recv[l, :, a])).astype(BF)
                agg[:, a] = agg_bf
                hid = dot(nw1t[l], stacked([v_in, agg_bf])) + bias(l, 1)
                nhid[l, :, a] = hid
                message, nrm, std = mlp_tail(hid, nw2t[l], vec(l, 1))
                nnrm[l, :, a] = nrm
                ninv[l:l + 1, a] = std
                out[:, a] = (v_in.astype(F32) + message.astype(F32)).astype(BF)

            loop(npad // TN, body)

        for l in range(layers):
            hidden_of_nodes(l)
            if l == top:
                def drain(j):
                    for d in OTHERS:
                        edge_copy(EDGE_IN, j, d).wait_send()
                loop(nch, drain)
            edge_forward(l)
            segment_sum(part.at[l], rcol)
            part_copy(l).start()
            if l == 0:
                wait_recvs(wcop[1])
                join_weights(1)
            part_copy(l).wait_recv()
            node_forward(l)
        no_send[...] = tables[layers][2 * q:3 * q, :].astype(F32)
        no_copy = remote(no_send, no_recv, n_ss.at[2, 0], n_rs.at[2, 0], 2)
        no_copy.start()
        node_raw[x] = tables[layers][:q, :nodes]

        hold = nch // 2
        grad[...] = jnp.zeros_like(grad)
        sums[...] = jnp.zeros_like(sums)
        wait_recvs(gcop)
        for d in OTHERS:
            d_part[rows_of(d), :] = gn_recv[slot(d)]

        def node_backward(l):
            table, agg = tables[l], aggs[l]

            def body(step):
                a = pl.ds(pl.multiple_of(step * TN, D), TN)
                d_in = d_part[:, a]
                if l < top:
                    d_in = d_in + part[layers + l + 1, :, a] + swap_halves(part_recv[layers + l + 1, :, a])
                    d_in = d_in.astype(BF).astype(F32)
                d_hid, d_w2, parts = mlp_back(d_in, nhid[l, :, a], nnrm[l, :, a], ninv[l:l + 1, a], nw2[l], vec(l, 1))
                add_sums(sums.at[l, 1], [parts])
                grad[l, 6] += d_w2
                grad[l, 4] += dot_nt(table[:, a], d_hid)
                grad[l, 5] += dot_nt(agg[:, a], d_hid)
                d_part[:, a] = d_in + dot(nw1[l, mat(0), :], d_hid)
                d_agg[:, a] = dot(nw1[l, mat(1), :], d_hid).astype(BF)

            loop(npad // TN, body)

        def gather_back():
            def body(step):
                msg[:, at(step, T)] = gather(d_agg, keys(rrow, step), iota).astype(BF)

            loop(eh // T, body)

        def edge_backward(l):
            e_in = edges_in[l]

            def body(j):
                all_parts, d_w2s, d_w1s, own_parts = [], [], [], []
                for sub in range(EC // T):
                    a = at(j * (EC // T) + sub, T)
                    if l == top:
                        if sub == 0:
                            for d in OTHERS:
                                edge_copy(GRAD_IN, j, d).wait_recv()
                        for d in OTHERS:
                            ge[rows_of(d), a] = g_recv[slot(d), :, a].astype(BF)
                    d_res = ge[:, a].astype(F32)
                    d_msg = d_res + msg[:, a].astype(F32)
                    d_hid, d_w2, parts = mlp_back(d_msg, hidden[l, :, a], normed[l, :, a], inv[l:l + 1, a], ew2[l], vec(l, 0))
                    all_parts.append(parts)
                    d_w2s.append(d_w2)
                    d_w1s.append(dot_nt(e_in[:, a], d_hid))
                    msg[:, a] = d_hid
                    d_new = (d_res + dot(ew1[l, mat(0), :], d_hid)).astype(BF)
                    if l > 0:
                        ge[:, a] = d_new
                    else:
                        for d in OTHERS:
                            g_send[slot(d), :, a] = d_new[rows_of(d)].astype(F32)
                        own_parts.append(d_new[:q])
                add_sums(sums.at[l, 0], all_parts)
                grad[l, 3] += sum(d_w2s[1:], d_w2s[0])
                grad[l, 0] += sum(d_w1s[1:], d_w1s[0])
                if l == 0:
                    @pl.when(j < hold)
                    def _():
                        for d in SEND_ORDER:
                            edge_copy(GRAD_OUT, j, d).start()
                    place_edges(gedge_raw, beside(own_parts), 0, j)

            loop(nch, body)

        def reduce_start(l):
            def total(node, k):
                return column_sum(flip(sums[l, node, mat(k), :]))

            lat = stacked([total(node, k) for node in BOTH for k in THREE])
            biases = stacked([total(node, 3) for node in BOTH])
            n_lat = lat.shape[0]
            for d in range(GROUP):
                grad[l, SLABS - 1, d * cols:d * cols + n_lat, :cols] = lat[:, rows_of(d)]
                grad[l, SLABS - 1, d * cols + n_lat:d * cols + n_lat + 2, :] = biases
            for b in BOTH:
                core_copy(l, b).start()

        def chip_sum(l):
            row = lax.broadcasted_iota(jnp.int32, (cols, D), 0)
            edge_row = jnp.logical_or(row < 3, row == 6)
            for b in BOTH:
                core_copy(l, b).wait_recv()
                for k in range(SLABS):
                    own = grad[l, k, rows_of(2 * b), :]
                    if k < 4:
                        own = own + core_recv[l, b, k]
                    elif k == SLABS - 1:
                        own = own + jnp.where(edge_row, core_recv[l, b, k], 0.0)
                    half[l, k, b] = own
            for i in dp_others:
                spread_copy(l, i).start()

        def dp_sum(l):
            total = half[l, pl.ds(p * per, per)]
            for i in dp_others:
                spread_copy(l, i).wait_recv()
                total = total + dp_recv[l, i - 1]
            own_sum[l] = total[:, 0]
            cross_send[l] = total[:, 1]
            cross_copy(l).start()

        def cross_sum(l):
            cross_copy(l).wait_recv()
            total = own_sum[l] + cross_recv[l]
            own_sum[l] = total
            gathered[l, pl.ds(p * per, per)] = total
            for i in dp_others:
                gather_copy(l, i, p).start()

        def project(l):
            table = tables[l]

            def body(step):
                a = pl.ds(pl.multiple_of(step * TN, D), TN)
                s_bf, r_bf, v_in = s_sum[:, a].astype(BF), r_sum[:, a].astype(BF), table[:, a]
                part[layers + l, :, a] = dot(ew1[l, mat(1), :], s_bf) + dot(ew1[l, mat(2), :], r_bf)
                grad[l, 1] += dot_nt(v_in, s_bf)
                grad[l, 2] += dot_nt(v_in, r_bf)

            loop(npad // TN, body)

        for l in reversed(range(layers)):
            node_backward(l)
            if l < top:
                chip_sum(l + 1)
            gather_back()
            if l == 0:
                def drain_g(j):
                    for d in OTHERS:
                        edge_copy(GRAD_IN, j, d).wait_send()
                loop(nch, drain_g)
            edge_backward(l)
            if l < top:
                dp_sum(l + 1)
            segment_sum(s_sum, scol)
            segment_sum(r_sum, rcol)
            project(l)
            part_copy(layers + l).start()
            reduce_start(l)
            part_copy(layers + l).wait_recv()

        def final(step):
            a = pl.ds(pl.multiple_of(step * TN, D), TN)
            d_in = (d_part[:, a] + part[layers, :, a] + swap_halves(part_recv[layers, :, a])).astype(BF)
            v2[:, a] = d_in

        loop(npad // TN, final)
        dn_send[...] = v2[2 * q:3 * q, :].astype(F32)
        dn_copy = remote(dn_send, dn_recv, n_ss.at[2, 1], n_rs.at[2, 1], 2)
        dn_copy.start()
        gnode_raw[x] = v2[:q, :nodes]
        chip_sum(0)

        no_copy.wait_recv()
        node_raw[ox] = no_recv[:, :nodes].astype(BF)

        def place_e(j):
            for d in OTHERS:
                edge_copy(EDGE_OUT, j, d).wait_recv()
                place_edges(edge_raw, eo_recv[slot(d), :, at(j, EC)], d, j)

        loop(nch, place_e)
        outs = [pltpu.make_async_copy(src, dst, out_sem.at[k]) for k, (src, dst) in enumerate(
            [(node_raw, node_out), (edge_raw, edge_out), (gnode_raw, dnode_out), (gedge_raw, dedge_out)])]
        outs[0].start()
        outs[1].start()

        dp_sum(0)

        def send_rest(j):
            for d in SEND_ORDER:
                edge_copy(GRAD_OUT, j, d).start()

        loop(nch, send_rest, hold)

        def place_g(j):
            for d in OTHERS:
                edge_copy(GRAD_OUT, j, d).wait_recv()
                place_edges(gedge_raw, de_recv[slot(d), :, at(j, EC)], d, j)

        loop(hold, place_g)
        for l in range(layers):
            cross_sum(l)
        loop(nch, place_g, hold)
        outs[3].start()
        dn_copy.wait_recv()
        gnode_raw[ox] = dn_recv[:, :nodes].astype(BF)
        outs[2].start()

        for l in range(layers):
            for i in dp_others:
                gather_copy(l, i, lax.rem(p + dpn - i, dpn)).wait_recv()
            ew1_out[l] = gathered[l, 0:3]
            ew2_out[l] = gathered[l, 3]
            nw1_out[l] = gathered[l, 4:6]
            nw2_out[l] = gathered[l, 6]
            small = gathered[l, SLABS - 1]
            for k in THREE:
                evec_out[k, l:l + 1, :] = small[k:k + 1, :cols]
                nvec_out[k, l:l + 1, :] = small[3 + k:4 + k, :cols]
            eb1_out[l:l + 1, :] = small[6:7]
            nb1_out[l:l + 1, :] = small[7:8]

        for l in range(layers):
            for b in BOTH:
                core_copy(l, b).wait_send()
            cross_copy(l).wait_send()
            for i in dp_others:
                spread_copy(l, i).wait_send()
                gather_copy(l, i, p).wait_send()
        for copies in (ncop, gcop, wcop[0], wcop[1]):
            for copy in copies:
                copy.wait_send()
        no_copy.wait_send()
        dn_copy.wait_send()
        for k in range(2 * layers):
            part_copy(k).wait_send()

        def drain_out(j):
            for kind in (EDGE_OUT, GRAD_OUT):
                for d in OTHERS:
                    edge_copy(kind, j, d).wait_send()

        loop(nch, drain_out)
        for copy in outs:
            copy.wait()

    bf = lambda *s: pltpu.VMEM(s, BF)
    pl.run_scoped(
        scoped, bf(D, eh), bf(D, eh), bf(D, eh), bf(D, eh), bf(D, npad), bf(D, npad), bf(D, npad), bf(D, npad), bf(D, npad), bf(D, npad),
        pltpu.VMEM((eh, D), I16), pltpu.VMEM((eh, D), I16), pltpu.VMEM((eh // D * 16, D), I16), pltpu.VMEM((eh // D * 16, D), I16),
        pltpu.VMEM((T, D), I16), pltpu.VMEM((16, D), I16),
        bf(layers, 3 * D, D), bf(layers, D, 3 * D), bf(layers, D, D), bf(layers, D, D),
        bf(layers, 2 * D, D), bf(layers, D, 2 * D), bf(layers, D, D), bf(layers, D, D), pltpu.VMEM((D, D), F32))


def solution(mesh):
    lat_spec = P('dp', None, 'tp')
    first_spec = P(None, None, 'tp', None)
    col_spec = P(None, None, 'tp')
    param_specs = (first_spec, P(), col_spec, col_spec, first_spec, P(), col_spec, col_spec)
    in_specs = (lat_spec, lat_spec, P(), P(), lat_spec, lat_spec) + param_specs
    out_specs = (lat_spec, lat_spec, lat_spec, lat_spec) + param_specs
    shape = jax.ShapeDtypeStruct

    def local_step(node_lat, edge_lat, senders, receivers, grad_node, grad_edge, edge_w1, edge_b1, edge_w2, edge_vec, node_w1, node_b1, node_w2, node_vec):
        layers = edge_w1.shape[0]
        cols = node_lat.shape[2]
        nodes, edges = node_lat.shape[1], edge_lat.shape[1]
        npad = -(-nodes // TN) * TN
        eh = -(-edges // (2 * EC)) * EC
        nch = eh // EC
        dpn = mesh.shape['dp']
        per = SLABS // dpn
        dims = (layers, cols, nodes, edges, npad, eh, dpn)
        flat = lambda arr: jnp.swapaxes(arr, 1, 2)
        idx = jnp.pad(jnp.stack([senders, receivers]), ((0, 0), (0, 2 * eh - edges)), constant_values=-1).reshape(2, 2 * eh // D, D)
        vec_in = jnp.concatenate([jnp.transpose(edge_vec, (1, 0, 2)).reshape(-1, cols), jnp.transpose(node_vec, (1, 0, 2)).reshape(-1, cols),
                                  jnp.zeros((HEAD - 6 * layers, cols), F32)], axis=0)
        b1_in = jnp.transpose(stacked([edge_b1, node_b1]))
        args = (flat(node_lat), flat(edge_lat), flat(grad_node), flat(grad_edge), idx,
                edge_w1.reshape(-1, D), flat(edge_w2).reshape(-1, D), node_w1.reshape(-1, D), flat(node_w2).reshape(-1, D), vec_in, b1_in)
        vm, sem = pltpu.VMEM, pltpu.SemaphoreType.DMA
        wrows = HEAD + layers * LROWS
        lat_n, lat_e = (2, cols, nodes), (2, cols, edges)
        scratch = [
            vm(lat_n, BF), vm(lat_n, BF), vm(lat_e, BF), vm(lat_e, BF), vm((wrows, D), F32), vm((3, wrows, D), F32),
            vm((2, cols, npad), F32), vm((3, cols, npad), F32), vm((2, cols, npad), F32), vm((3, cols, npad), F32),
            vm((cols, npad), F32), vm((cols, npad), F32), vm((cols, npad), F32), vm((cols, npad), F32),
            vm((3, cols, eh), F32), vm((3, cols, eh), F32), vm((3, cols, eh), F32), vm((3, cols, eh), F32), vm((3, cols, eh), F32), vm((3, cols, eh), F32),
            vm((2 * layers, D, npad), F32), vm((2 * layers, D, npad), F32),
            vm((layers, D, eh), F32), vm((layers, D, eh), F32), vm((8, eh), F32),
            vm((layers, D, npad), F32), vm((layers, D, npad), F32), vm((8, npad), F32),
            vm((D, npad), F32), vm((D, npad), F32), vm((D, npad), F32), vm((layers, 2, 4 * D, D), F32),
            vm((layers, SLABS, D, D), F32), vm((layers, 2, SLABS, cols, D), F32), vm((layers, SLABS, 2, cols, D), F32),
            vm((layers, dpn - 1, per, 2, cols, D), F32), vm((layers, per, cols, D), F32), vm((layers, per, cols, D), F32),
            vm((layers, per, cols, D), F32), vm((layers, SLABS, cols, D), F32),
            sem((layers, 2)), sem((layers, 2)), sem((2, layers, dpn - 1)), sem((2, layers, dpn - 1)), sem((layers,)), sem((layers,)),
            sem((4,)), sem((2, 3)), sem((2, 3)), sem((3, 3)), sem((3, 3)), sem((4, 3, nch)), sem((4, 3, nch)),
            sem((2 * layers,)), sem((2 * layers,)), sem((4,))]
        outs = [shape(lat_n, BF), shape(lat_e, BF), shape(lat_n, BF), shape(lat_e, BF),
                shape((layers, 3, cols, D), F32), shape((layers, D), F32), shape((layers, cols, D), F32), shape((3, layers, cols), F32),
                shape((layers, 2, cols, D), F32), shape((layers, D), F32), shape((layers, cols, D), F32), shape((3, layers, cols), F32)]
        res = pl.pallas_call(
            lambda *refs: step_kernel(dims, *refs),
            name='graph_step',
            out_shape=outs,
            in_specs=[HB] * 4 + [VM] * 7,
            out_specs=[HB] * 4 + [VM] * 8,
            scratch_shapes=scratch,
            compiler_params=pltpu.CompilerParams(collective_id=0, has_side_effects=True, vmem_limit_bytes=67_043_328),
        )(*args)

        lead = lambda arr: jnp.transpose(arr, (1, 0, 2))
        return (flat(res[0]), flat(res[1]), flat(res[2]), flat(res[3]),
                res[4], res[5], flat(res[6]), lead(res[7]), res[8], res[9], flat(res[10]), lead(res[11]))

    return jax.shard_map(local_step, mesh=mesh, in_specs=in_specs, out_specs=out_specs, check_vma=False)
```

```python
import jax
import jax.numpy as jnp
from jax import lax
from jax.experimental import pallas as pl
from jax.experimental.pallas import tpu as pltpu
from jax.sharding import PartitionSpec as P

LN_EPS = 1e-5
D = 128
T = 256
TN = 384
EC = 512
KS = 1408
BF = jnp.bfloat16
F32 = jnp.float32
I16 = jnp.int16
MESH = pl.DeviceIdType.MESH
VM = pl.BlockSpec(memory_space=pltpu.VMEM)
HB = pl.BlockSpec(memory_space=pl.ANY)
GROUP = 4
BOTH = (0, 1)
THREE = (0, 1, 2)
OTHERS = (1, 2, 3)
EDGE_IN, GRAD_IN, EDGE_OUT, GRAD_OUT = range(4)
SEND_ORDER = (2, 3, 1)
LROWS = 7 * (D // 4)
HEAD = 16
SLABS = 8


def dot(a, b):
    return jnp.dot(a, b, preferred_element_type=F32)


def dot_nt(a, b):
    return lax.dot_general(a, b, (((1,), (1,)), ((), ())), preferred_element_type=F32)


def mat(k, n=1):
    return slice(k * D, (k + n) * D)


def rows_of(d):
    q = D // 4
    return slice(d * q, (d + 1) * q)


def at(step, width):
    return pl.ds(pl.multiple_of(step * width, width), width)


def loop(stop, body, start=0):
    def step(j, carry):
        body(j)
        return carry

    lax.fori_loop(start, stop, step, 0)


def column_sum(val):
    return jnp.sum(val, axis=0, keepdims=True)


def flip(val):
    return jnp.swapaxes(val, 0, 1)


def stacked(parts):
    return jnp.concatenate(parts, axis=0)


def beside(parts):
    return jnp.concatenate(parts, axis=1)


def slot(d):
    return d - 1


def sigmoid(hidden):
    return 1.0 / (1.0 + jnp.exp(-hidden))


def fold(val):
    total = val[:, mat(0)]
    for start in range(D, val.shape[1], D):
        total = total + val[:, start:start + D]
    return total


def swap_halves(val):
    return stacked([val[rows_of(d)] for d in (1, 0, 3, 2)])


def gather(table, keys, iota):
    acc = None
    nodes = table.shape[1]
    one, zero = jnp.ones((), BF), jnp.zeros((), BF)
    for base in range(0, nodes, T):
        width = min(T, nodes - base)
        ids = iota[0:width, :]
        hot = beside([jnp.where(ids == (key - jnp.asarray(base, I16)), one, zero) for key in keys])
        part = dot(table[:, base:base + width], hot)
        acc = part if acc is None else acc + part
    return acc


def scatter(acc_ref, val, cols, lanes):
    nodes = acc_ref.shape[1]
    one, zero = jnp.ones((), BF), jnp.zeros((), BF)
    row = lanes[0:1, :]
    for base in range(0, nodes, T):
        width = min(T, nodes - base)
        hot = beside([jnp.where((row + jnp.asarray(base + s, I16)) == cols, one, zero) for s in range(0, width, D)])
        acc_ref[:, base:base + width] += dot(val, hot)


def mlp_tail(hidden, w2t, vec):
    act = (hidden * sigmoid(hidden)).astype(BF)
    out = dot(w2t, act) + vec[0]
    mean = column_sum(out) / D
    centered = out - mean
    var = column_sum(centered * centered) / D
    inv = lax.rsqrt(var + LN_EPS)
    normed = centered * inv
    message = (normed * vec[1] + vec[2]).astype(BF)
    return message, normed, inv


def mlp_back(d_msg, hidden, normed, inv, w2, vec):
    d_normed = d_msg * vec[1]
    mean0 = column_sum(d_normed) / D
    mean1 = column_sum(d_normed * normed) / D
    d_out = inv * (d_normed - mean0 - normed * mean1)
    d_out_bf = d_out.astype(BF)
    sig = sigmoid(hidden)
    act = (hidden * sig).astype(BF)
    d_w2 = dot_nt(d_out_bf, act)
    d_hidden = dot(w2, d_out_bf) * (sig * (1.0 + hidden * (1.0 - sig)))
    sums = (fold(d_out), fold(d_msg * normed), fold(d_msg), fold(d_hidden))
    return d_hidden.astype(BF), d_w2, sums


def add_sums(ref, parts):
    for q in range(4):
        total = parts[0][q]
        for other in parts[1:]:
            total = total + other[q]
        ref[mat(q), :] += total


def step_kernel(dims, *refs):
    layers, cols, nodes, edges, npad, eh, dpn = dims
    nch = eh // EC
    top = layers - 1
    n_in = 14
    (node_in, edge_in, gnode_in, gedge_in, send_ids, recv_ids, ew1_in, ew2_in, nw1_in, nw2_in, evec_in, nvec_in, eb1_in, nb1_in) = refs[:n_in]
    n_out = 12
    (node_out, edge_out, dnode_out, dedge_out, ew1_out, eb1_out, ew2_out, evec_out, nw1_out, nb1_out, nw2_out, nvec_out) = refs[n_in:n_in + n_out]
    (node_raw, gnode_raw, edge_raw, gedge_raw, w_send, w_recv, n_send, n_recv, gn_send, gn_recv, no_send, no_recv, dn_send, dn_recv,
     e_send, g_send, e_recv, g_recv, eo_recv, de_recv, part, part_recv, hidden, normed, inv, nhid, nnrm, ninv, d_part, s_sum, r_sum,
     ids_raw, bias_cols, sums, grad, core_recv, half, dp_recv, cross_send, cross_recv, own_sum, gathered,
     core_ss, core_rs, dp_ss, dp_rs, cross_ss, cross_rs, load_sem, w_ss, w_rs, n_ss, n_rs, e_ss, e_rs, p_ss, p_rs, out_sem) = refs[n_in + n_out:]

    t = lax.axis_index('tp')
    p = lax.axis_index('dp')
    per = SLABS // dpn
    dp_others = range(1, dpn)
    x, c = t // 2, lax.rem(t, 2)
    ox, oc = 1 - x, 1 - c
    peer = [t, t + 1 - 2 * c, t + 2 - 4 * x, t + 3 - 2 * c - 4 * x]

    def remote(src, dst, ssem, rsem, d):
        return pltpu.make_async_remote_copy(src_ref=src, dst_ref=dst, send_sem=ssem, recv_sem=rsem,
                                            device_id={'tp': peer[d]}, device_id_type=MESH)

    loads = [pltpu.make_async_copy(src, dst, load_sem.at[q]) for q, (src, dst) in enumerate(
        [(node_in, node_raw), (edge_in, edge_raw), (gnode_in, gnode_raw), (gedge_in, gedge_raw)])]
    for copy in loads:
        copy.start()

    barrier = pltpu.get_barrier_semaphore()
    for d in OTHERS:
        pl.semaphore_signal(barrier, inc=1, device_id={'tp': peer[d]}, device_id_type=MESH)
    for i in dp_others:
        pl.semaphore_signal(barrier, inc=1, device_id={'dp': lax.rem(p + i, dpn)}, device_id_type=MESH)
    with jax.named_scope('barrier'):
        pl.semaphore_wait(barrier, len(OTHERS) + dpn - 1)

    def node_copies(send, recv, kind):
        return (remote(send.at[1], recv.at[0], n_ss.at[kind, 0], n_rs.at[kind, 0], 1),
                remote(send.at[0], recv.at[1], n_ss.at[kind, 1], n_rs.at[kind, 1], 2),
                remote(recv.at[1], recv.at[2], n_ss.at[kind, 2], n_rs.at[kind, 2], 1))

    def weight_copies(kind):
        rows = (pl.ds(0, HEAD + LROWS), pl.ds(HEAD + LROWS, LROWS * (top)))[kind]
        return (remote(w_send.at[rows], w_recv.at[0, rows], w_ss.at[kind, 0], w_rs.at[kind, 0], 1),
                remote(w_send.at[rows], w_recv.at[1, rows], w_ss.at[kind, 1], w_rs.at[kind, 1], 2),
                remote(w_recv.at[1, rows], w_recv.at[2, rows], w_ss.at[kind, 2], w_rs.at[kind, 2], 1))

    def edge_copy(kind, j, d):
        src, dst = ((e_send, e_recv), (g_send, g_recv), (e_send, eo_recv), (g_send, de_recv))[kind]
        lanes_j = at(j, EC)
        return remote(src.at[slot(d), :, lanes_j], dst.at[slot(d), :, lanes_j], e_ss.at[kind, slot(d), j], e_rs.at[kind, slot(d), j], d)

    def core_copy(l, b):
        return remote(grad.at[l, :, pl.ds((2 * b + 1) * cols, cols), :], core_recv.at[l, b], core_ss.at[l, b], core_rs.at[l, b], 1)

    def dp_remote(src, dst, stage, l, i):
        return pltpu.make_async_remote_copy(src_ref=src, dst_ref=dst, send_sem=dp_ss.at[stage, l, i - 1], recv_sem=dp_rs.at[stage, l, i - 1],
                                            device_id={'dp': lax.rem(p + i, dpn)}, device_id_type=MESH)

    def spread_copy(l, i):
        return dp_remote(half.at[l, pl.ds(lax.rem(p + i, dpn) * per, per)], dp_recv.at[l, i - 1], 0, l, i)

    def cross_copy(l):
        return remote(cross_send.at[l], cross_recv.at[l], cross_ss.at[l], cross_rs.at[l], 2)

    def gather_copy(l, i, owner):
        return dp_remote(own_sum.at[l], gathered.at[l, pl.ds(owner * per, per)], 1, l, i)

    def part_copy(q):
        return remote(part.at[q], part_recv.at[q], p_ss.at[q], p_rs.at[q], 1)

    def load_nodes(raw, send, own):
        send[...] = jnp.zeros_like(send)
        send[0, :, :nodes] = raw[ox].astype(F32)
        send[1, :, :nodes] = raw[x].astype(F32)
        own[:cols, :] = send[1].astype(own.dtype)

    def load_edges(raw, send, own, kind):
        def put(j, lanes_j, val_of):
            for d in OTHERS:
                sample = x if d < 2 else ox
                send[slot(d), :, lanes_j] = val_of(sample, oc if d % 2 else c).astype(F32)
            own[:cols, lanes_j] = val_of(x, c)

        def chunk(j):
            put(j, at(j, EC), lambda s, h: raw[s, :, pl.ds(pl.multiple_of(h * eh + j * EC, D), EC)])
            for d in SEND_ORDER:
                edge_copy(kind, j, d).start()

        loop(nch - 1, chunk)
        first = (nch - 1) * EC
        used = edges - eh - first
        last = pl.ds(first, EC)

        def tail(s, h):
            left = raw[s, :, pl.ds(first, EC)]
            right = beside([raw[s, :, pl.ds(eh + first, used)], jnp.zeros((cols, EC - used), BF)])
            return jnp.where(h == 0, left.astype(F32), right.astype(F32)).astype(BF)

        put(nch - 1, last, tail)
        for d in SEND_ORDER:
            edge_copy(kind, nch - 1, d).start()

    def place_edges(raw, block, d, j):
        s = x if d < 2 else ox
        h = oc if d % 2 else c
        val = block.astype(BF)
        first = (nch - 1) * EC
        used = edges - eh - first

        @pl.when(jnp.logical_or(j < nch - 1, h == 0))
        def _():
            raw[s, :, pl.ds(pl.multiple_of(h * eh + j * EC, D), EC)] = val

        @pl.when(jnp.logical_and(j == nch - 1, h == 1))
        def _():
            raw[s, :, pl.ds(eh + first, used)] = val[:, :used]

    def scoped(e0, e1, ge, msg, v0, v1, v2, agg0, agg1, d_agg, scol, rcol, srow, rrow, iota, lanes, ew1, ew1t, ew2, ew2t, nw1, nw1t, nw2, nw2t, vecs):
        tables = (v0, v1, v2)
        aggs = (agg0, agg1)
        edges_in = (e0, e1)

        loads[0].wait()
        with jax.named_scope('send_nodes'):
            load_nodes(node_raw, n_send, v0)
        ncop = node_copies(n_send, n_recv, 0)
        ncop[1].start()
        ncop[0].start()
        q = cols
        w_send[:HEAD, :] = jnp.zeros((HEAD, D), F32)
        for k in THREE:
            w_send[k * layers:(k + 1) * layers, :cols] = evec_in[k]
            w_send[(3 + k) * layers:(4 + k) * layers, :cols] = nvec_in[k]
        for l in range(layers):
            off = HEAD + l * LROWS
            w_send[off:off + 3 * q, :] = ew1_in[l * 3 * q:(l + 1) * 3 * q, :].astype(F32)
            w_send[off + 3 * q:off + 4 * q, :] = ew2_in[l * q:(l + 1) * q, :].astype(F32)
            w_send[off + 4 * q:off + 6 * q, :] = nw1_in[l * 2 * q:(l + 1) * 2 * q, :].astype(F32)
            w_send[off + 6 * q:off + 7 * q, :] = nw2_in[l * q:(l + 1) * q, :].astype(F32)
        wcop = [weight_copies(kind) for kind in range(2)]
        wcop[0][1].start()
        wcop[0][0].start()
        loads[1].wait()
        with jax.named_scope('send_edges'):
            load_edges(edge_raw, e_send, e0, EDGE_IN)
        wcop[1][1].start()
        wcop[1][0].start()
        loads[2].wait()
        load_nodes(gnode_raw, gn_send, d_part)
        gcop = node_copies(gn_send, gn_recv, 1)
        gcop[1].start()
        gcop[0].start()
        loads[3].wait()
        with jax.named_scope('send_grads'):
            load_edges(gedge_raw, g_send, ge, GRAD_IN)

        iota[...] = lax.broadcasted_iota(jnp.int32, (T, D), 0).astype(I16)
        lanes[...] = lax.broadcasted_iota(jnp.int32, (16, D), 1).astype(I16)

        ids_raw[...] = jnp.full(ids_raw.shape, -1, jnp.int32)
        for which, src in enumerate((send_ids, recv_ids)):
            ids_raw[which:which + 1, :edges] = src[...].reshape(1, edges)

        def ids(b):
            for which, (row_ref, col_ref) in enumerate(((srow, scol), (rrow, rcol))):
                wide = jnp.broadcast_to(ids_raw[which:which + 1, pl.ds(pl.multiple_of(c * eh + b * D, D), D)], (D, D))
                row_ref[at(b, 16), :] = wide[:16].astype(I16)
                col_ref[at(b, D), :] = flip(wide.astype(F32)).astype(jnp.int32).astype(I16)

        with jax.named_scope('ids'):
            loop(eh // D, ids)

        def keys(ref, step):
            return [ref[pl.ds(pl.multiple_of(step * (T // D) * 16 + 16 * h, 16), 1), :] for h in range(T // D)]

        bias_cols[...] = flip(stacked([eb1_in[...], nb1_in[...], jnp.zeros((D - 2 * layers, D), F32)]))

        def join_weights(l):
            off = HEAD + l * LROWS
            for d in range(GROUP):
                src = w_send if d == 0 else w_recv.at[slot(d)]
                r = slice(d * q, (d + 1) * q)
                for k in THREE:
                    ew1[l, k * D + d * q:k * D + (d + 1) * q, :] = src[off + k * q:off + (k + 1) * q, :].astype(BF)
                ew2t[l, r, :] = src[off + 3 * q:off + 4 * q, :].astype(BF)
                for k in range(2):
                    nw1[l, k * D + d * q:k * D + (d + 1) * q, :] = src[off + (4 + k) * q:off + (5 + k) * q, :].astype(BF)
                nw2t[l, r, :] = src[off + 6 * q:off + 7 * q, :].astype(BF)

            def flip_bf(mat):
                return flip(mat.astype(F32)).astype(BF)

            for k in THREE:
                ew1t[l, :, mat(k)] = flip_bf(ew1[l, mat(k), :])
            for k in range(2):
                nw1t[l, :, mat(k)] = flip_bf(nw1[l, mat(k), :])
            ew2[l] = flip_bf(ew2t[l])
            nw2[l] = flip_bf(nw2t[l])

        def wait_recvs(copies):
            copies[1].wait_recv()
            copies[2].start()
            copies[0].wait_recv()
            copies[2].wait_recv()

        with jax.named_scope('node_wait'):
            wait_recvs(ncop)
        for d in OTHERS:
            v0[rows_of(d), :] = n_recv[slot(d)].astype(BF)
        with jax.named_scope('weight_wait'):
            wait_recvs(wcop[0])
        rows_all = beside([w_send[:HEAD, :cols]] + [w_recv[d, :HEAD, :cols] for d in range(3)])
        vecs[...] = flip(stacked([rows_all, jnp.zeros((D - HEAD, D), F32)]))
        join_weights(0)

        def vec(l, node):
            first = 6 * node + l
            return [vecs[:, first + 2 * k:first + 2 * k + 1] for k in THREE]

        def bias(l, node):
            return bias_cols[:, node * layers + l:node * layers + l + 1]

        def hidden_of_nodes(l):
            table, b1 = tables[l], bias(l, 0)

            def body(step):
                xs = gather(table, keys(srow, step), iota).astype(BF)
                xr = gather(table, keys(rrow, step), iota).astype(BF)
                hidden[l, :, at(step, T)] = dot(ew1t[l, :, mat(1, 2)], stacked([xs, xr])) + b1

            loop(eh // T, body)

        def edge_forward(l):
            e_in = edges_in[l]

            def body(j):
                for sub in range(EC // T):
                    a = at(j * (EC // T) + sub, T)
                    if l == 0:
                        if sub == 0:
                            for d in OTHERS:
                                edge_copy(EDGE_IN, j, d).wait_recv()
                        for d in OTHERS:
                            e_in[rows_of(d), a] = e_recv[slot(d), :, a].astype(BF)
                    e_val = e_in[:, a]
                    hid = hidden[l, :, a] + dot(ew1t[l, :, mat(0)], e_val)
                    hidden[l, :, a] = hid
                    message, nrm, std = mlp_tail(hid, ew2t[l], vec(l, 0))
                    normed[l, :, a] = nrm
                    inv[l:l + 1, a] = std
                    msg[:, a] = message
                    e_new = (e_val.astype(F32) + message.astype(F32)).astype(BF)
                    if l < top:
                        edges_in[l + 1][:, a] = e_new
                    else:
                        for d in OTHERS:
                            e_send[slot(d), :, a] = e_new[rows_of(d)].astype(F32)
                        if sub == 0:
                            own_parts = []
                        own_parts.append(e_new[:q])
                if l == top:
                    for d in SEND_ORDER:
                        edge_copy(EDGE_OUT, j, d).start()
                    place_edges(edge_raw, beside(own_parts), 0, j)

            loop(nch, body)

        def segment_sum(acc, ids_ref):
            acc[...] = jnp.zeros(acc.shape, F32)

            def body(step):
                scatter(acc, msg[:, at(step, KS)], ids_ref[at(step, KS), :], lanes)

            loop(eh // KS, body)

        def node_forward(l):
            table, agg, out = tables[l], aggs[l], tables[l + 1]

            def body(step):
                a = pl.ds(pl.multiple_of(step * TN, D), TN)
                v_in = table[:, a]
                agg_bf = (part[l, :, a] + swap_halves(part_recv[l, :, a])).astype(BF)
                agg[:, a] = agg_bf
                hid = dot(nw1t[l], stacked([v_in, agg_bf])) + bias(l, 1)
                nhid[l, :, a] = hid
                message, nrm, std = mlp_tail(hid, nw2t[l], vec(l, 1))
                nnrm[l, :, a] = nrm
                ninv[l:l + 1, a] = std
                out[:, a] = (v_in.astype(F32) + message.astype(F32)).astype(BF)

            loop(npad // TN, body)

        for l in range(layers):
            with jax.named_scope(f'gather_{l}'):
                hidden_of_nodes(l)
            if l == top:
                def drain(j):
                    for d in OTHERS:
                        edge_copy(EDGE_IN, j, d).wait_send()
                loop(nch, drain)
            with jax.named_scope(f'edge_forward_{l}'):
                edge_forward(l)
            with jax.named_scope(f'sum_{l}'):
                segment_sum(part.at[l], rcol)
            part_copy(l).start()
            if l == 0:
                wait_recvs(wcop[1])
                join_weights(1)
            with jax.named_scope(f'part_wait_{l}'):
                part_copy(l).wait_recv()
            with jax.named_scope(f'node_forward_{l}'):
                node_forward(l)
        no_send[...] = tables[layers][2 * q:3 * q, :].astype(F32)
        no_copy = remote(no_send, no_recv, n_ss.at[2, 0], n_rs.at[2, 0], 2)
        no_copy.start()
        node_raw[x] = tables[layers][:q, :nodes]

        hold = nch // 2
        grad[...] = jnp.zeros_like(grad)
        sums[...] = jnp.zeros_like(sums)
        with jax.named_scope('grad_node_wait'):
            wait_recvs(gcop)
        for d in OTHERS:
            d_part[rows_of(d), :] = gn_recv[slot(d)]

        def node_backward(l):
            table, agg = tables[l], aggs[l]

            def body(step):
                a = pl.ds(pl.multiple_of(step * TN, D), TN)
                d_in = d_part[:, a]
                if l < top:
                    d_in = d_in + part[layers + l + 1, :, a] + swap_halves(part_recv[layers + l + 1, :, a])
                    d_in = d_in.astype(BF).astype(F32)
                d_hid, d_w2, parts = mlp_back(d_in, nhid[l, :, a], nnrm[l, :, a], ninv[l:l + 1, a], nw2[l], vec(l, 1))
                add_sums(sums.at[l, 1], [parts])
                grad[l, 6] += d_w2
                grad[l, 4] += dot_nt(table[:, a], d_hid)
                grad[l, 5] += dot_nt(agg[:, a], d_hid)
                d_part[:, a] = d_in + dot(nw1[l, mat(0), :], d_hid)
                d_agg[:, a] = dot(nw1[l, mat(1), :], d_hid).astype(BF)

            loop(npad // TN, body)

        def gather_back():
            def body(step):
                msg[:, at(step, T)] = gather(d_agg, keys(rrow, step), iota).astype(BF)

            loop(eh // T, body)

        def edge_backward(l):
            e_in = edges_in[l]

            def body(j):
                all_parts, d_w2s, d_w1s, own_parts = [], [], [], []
                for sub in range(EC // T):
                    a = at(j * (EC // T) + sub, T)
                    if l == top:
                        if sub == 0:
                            for d in OTHERS:
                                edge_copy(GRAD_IN, j, d).wait_recv()
                        for d in OTHERS:
                            ge[rows_of(d), a] = g_recv[slot(d), :, a].astype(BF)
                    d_res = ge[:, a].astype(F32)
                    d_msg = d_res + msg[:, a].astype(F32)
                    d_hid, d_w2, parts = mlp_back(d_msg, hidden[l, :, a], normed[l, :, a], inv[l:l + 1, a], ew2[l], vec(l, 0))
                    all_parts.append(parts)
                    d_w2s.append(d_w2)
                    d_w1s.append(dot_nt(e_in[:, a], d_hid))
                    msg[:, a] = d_hid
                    d_new = (d_res + dot(ew1[l, mat(0), :], d_hid)).astype(BF)
                    if l > 0:
                        ge[:, a] = d_new
                    else:
                        for d in OTHERS:
                            g_send[slot(d), :, a] = d_new[rows_of(d)].astype(F32)
                        own_parts.append(d_new[:q])
                add_sums(sums.at[l, 0], all_parts)
                grad[l, 3] += sum(d_w2s[1:], d_w2s[0])
                grad[l, 0] += sum(d_w1s[1:], d_w1s[0])
                if l == 0:
                    @pl.when(j < hold)
                    def _():
                        for d in SEND_ORDER:
                            edge_copy(GRAD_OUT, j, d).start()
                    place_edges(gedge_raw, beside(own_parts), 0, j)

            loop(nch, body)

        def reduce_start(l):
            def total(node, k):
                return column_sum(flip(sums[l, node, mat(k), :]))

            lat = stacked([total(node, k) for node in BOTH for k in THREE])
            biases = stacked([total(node, 3) for node in BOTH])
            n_lat = lat.shape[0]
            for d in range(GROUP):
                grad[l, SLABS - 1, d * cols:d * cols + n_lat, :cols] = lat[:, rows_of(d)]
                grad[l, SLABS - 1, d * cols + n_lat:d * cols + n_lat + 2, :] = biases
            for b in BOTH:
                core_copy(l, b).start()

        def chip_sum(l):
            row = lax.broadcasted_iota(jnp.int32, (cols, D), 0)
            edge_row = jnp.logical_or(row < 3, row == 6)
            for b in BOTH:
                core_copy(l, b).wait_recv()
                for k in range(SLABS):
                    own = grad[l, k, rows_of(2 * b), :]
                    if k < 4:
                        own = own + core_recv[l, b, k]
                    elif k == SLABS - 1:
                        own = own + jnp.where(edge_row, core_recv[l, b, k], 0.0)
                    half[l, k, b] = own
            for i in dp_others:
                spread_copy(l, i).start()

        def dp_sum(l):
            total = half[l, pl.ds(p * per, per)]
            for i in dp_others:
                spread_copy(l, i).wait_recv()
                total = total + dp_recv[l, i - 1]
            own_sum[l] = total[:, 0]
            cross_send[l] = total[:, 1]
            cross_copy(l).start()

        def cross_sum(l):
            cross_copy(l).wait_recv()
            total = own_sum[l] + cross_recv[l]
            own_sum[l] = total
            gathered[l, pl.ds(p * per, per)] = total
            for i in dp_others:
                gather_copy(l, i, p).start()

        def project(l):
            table = tables[l]

            def body(step):
                a = pl.ds(pl.multiple_of(step * TN, D), TN)
                s_bf, r_bf, v_in = s_sum[:, a].astype(BF), r_sum[:, a].astype(BF), table[:, a]
                part[layers + l, :, a] = dot(ew1[l, mat(1), :], s_bf) + dot(ew1[l, mat(2), :], r_bf)
                grad[l, 1] += dot_nt(v_in, s_bf)
                grad[l, 2] += dot_nt(v_in, r_bf)

            loop(npad // TN, body)

        for l in reversed(range(layers)):
            with jax.named_scope(f'node_backward_{l}'):
                node_backward(l)
            if l < top:
                with jax.named_scope('chip_sum_1'):
                    chip_sum(l + 1)
            with jax.named_scope(f'gather_back_{l}'):
                gather_back()
            if l == 0:
                def drain_g(j):
                    for d in OTHERS:
                        edge_copy(GRAD_IN, j, d).wait_send()
                loop(nch, drain_g)
            with jax.named_scope(f'edge_backward_{l}'):
                edge_backward(l)
            if l < top:
                with jax.named_scope('dp_sum_1'):
                    dp_sum(l + 1)
            with jax.named_scope(f'sum_send_{l}'):
                segment_sum(s_sum, scol)
            with jax.named_scope(f'sum_recv_{l}'):
                segment_sum(r_sum, rcol)
            with jax.named_scope(f'project_{l}'):
                project(l)
            part_copy(layers + l).start()
            with jax.named_scope(f'reduce_start_{l}'):
                reduce_start(l)
            with jax.named_scope(f'back_wait_{l}'):
                part_copy(layers + l).wait_recv()

        def final(step):
            a = pl.ds(pl.multiple_of(step * TN, D), TN)
            d_in = (d_part[:, a] + part[layers, :, a] + swap_halves(part_recv[layers, :, a])).astype(BF)
            v2[:, a] = d_in

        loop(npad // TN, final)
        dn_send[...] = v2[2 * q:3 * q, :].astype(F32)
        dn_copy = remote(dn_send, dn_recv, n_ss.at[2, 1], n_rs.at[2, 1], 2)
        dn_copy.start()
        gnode_raw[x] = v2[:q, :nodes]
        with jax.named_scope('chip_sum_0'):
            chip_sum(0)

        with jax.named_scope('node_out_wait'):
            no_copy.wait_recv()
        node_raw[ox] = no_recv[:, :nodes].astype(BF)

        def place_e(j):
            for d in OTHERS:
                edge_copy(EDGE_OUT, j, d).wait_recv()
                place_edges(edge_raw, eo_recv[slot(d), :, at(j, EC)], d, j)

        with jax.named_scope('place_edge_out'):
            loop(nch, place_e)
        outs = [pltpu.make_async_copy(src, dst, out_sem.at[k]) for k, (src, dst) in enumerate(
            [(node_raw, node_out), (edge_raw, edge_out), (gnode_raw, dnode_out), (gedge_raw, dedge_out)])]
        outs[0].start()
        outs[1].start()

        with jax.named_scope('dp_sum_0'):
            dp_sum(0)

        def send_rest(j):
            for d in SEND_ORDER:
                edge_copy(GRAD_OUT, j, d).start()

        loop(nch, send_rest, hold)

        def place_g(j):
            for d in OTHERS:
                edge_copy(GRAD_OUT, j, d).wait_recv()
                place_edges(gedge_raw, de_recv[slot(d), :, at(j, EC)], d, j)

        with jax.named_scope('place_first'):
            loop(hold, place_g)
        for l in range(layers):
            with jax.named_scope(f'cross_sum_{l}'):
                cross_sum(l)
        with jax.named_scope('place_rest'):
            loop(nch, place_g, hold)
        outs[3].start()
        with jax.named_scope('d_node_wait'):
            dn_copy.wait_recv()
        gnode_raw[ox] = dn_recv[:, :nodes].astype(BF)
        outs[2].start()

        for l in range(layers):
            for i in dp_others:
                gather_copy(l, i, lax.rem(p + dpn - i, dpn)).wait_recv()
            ew1_out[l] = gathered[l, 0:3]
            ew2_out[l] = gathered[l, 3]
            nw1_out[l] = gathered[l, 4:6]
            nw2_out[l] = gathered[l, 6]
            small = gathered[l, SLABS - 1]
            for k in THREE:
                evec_out[k, l:l + 1, :] = small[k:k + 1, :cols]
                nvec_out[k, l:l + 1, :] = small[3 + k:4 + k, :cols]
            eb1_out[l:l + 1, :] = small[6:7]
            nb1_out[l:l + 1, :] = small[7:8]

        for l in range(layers):
            for b in BOTH:
                core_copy(l, b).wait_send()
            cross_copy(l).wait_send()
            for i in dp_others:
                spread_copy(l, i).wait_send()
                gather_copy(l, i, p).wait_send()
        for copies in (ncop, gcop, wcop[0], wcop[1]):
            for copy in copies:
                copy.wait_send()
        no_copy.wait_send()
        dn_copy.wait_send()
        for k in range(2 * layers):
            part_copy(k).wait_send()

        def drain_out(j):
            for kind in (EDGE_OUT, GRAD_OUT):
                for d in OTHERS:
                    edge_copy(kind, j, d).wait_send()

        loop(nch, drain_out)
        for copy in outs:
            copy.wait()

    bf = lambda *s: pltpu.VMEM(s, BF)
    pl.run_scoped(
        scoped, bf(D, eh), bf(D, eh), bf(D, eh), bf(D, eh), bf(D, npad), bf(D, npad), bf(D, npad), bf(D, npad), bf(D, npad), bf(D, npad),
        pltpu.VMEM((eh, D), I16), pltpu.VMEM((eh, D), I16), pltpu.VMEM((eh // D * 16, D), I16), pltpu.VMEM((eh // D * 16, D), I16),
        pltpu.VMEM((T, D), I16), pltpu.VMEM((16, D), I16),
        bf(layers, 3 * D, D), bf(layers, D, 3 * D), bf(layers, D, D), bf(layers, D, D),
        bf(layers, 2 * D, D), bf(layers, D, 2 * D), bf(layers, D, D), bf(layers, D, D), pltpu.VMEM((D, D), F32))


def finish_kernel(*refs):
    count = (len(refs) - 2) // 3
    srcs, dsts, bufs, (in_sem, out_sem) = refs[:count], refs[count:2 * count], refs[2 * count:3 * count], refs[3 * count:]
    pulls = [pltpu.make_async_copy(src, buf, in_sem.at[k]) for k, (src, buf) in enumerate(zip(srcs, bufs))]
    puts = [pltpu.make_async_copy(buf, dst, out_sem.at[k]) for k, (buf, dst) in enumerate(zip(bufs, dsts))]
    for pull in pulls:
        pull.start()
    for pull, put in zip(pulls, puts):
        pull.wait()
        put.start()
    for put in puts:
        put.wait()


def finish(arrays):
    sems = pltpu.SemaphoreType.DMA((len(arrays),))
    return pl.pallas_call(
        finish_kernel,
        name='finish',
        out_shape=[jax.ShapeDtypeStruct(a.shape, a.dtype) for a in arrays],
        in_specs=[HB] * len(arrays),
        out_specs=[HB] * len(arrays),
        scratch_shapes=[pltpu.VMEM(a.shape, a.dtype) for a in arrays] + [sems, sems],
    )(*arrays)


def solution(mesh):
    lat_spec = P('dp', None, 'tp')
    first_spec = P(None, None, 'tp', None)
    col_spec = P(None, None, 'tp')
    param_specs = (first_spec, P(), col_spec, col_spec, first_spec, P(), col_spec, col_spec)
    in_specs = (lat_spec, lat_spec, P(), P(), lat_spec, lat_spec) + param_specs
    out_specs = (lat_spec, lat_spec, lat_spec, lat_spec) + param_specs
    shape = jax.ShapeDtypeStruct

    def local_step(node_lat, edge_lat, senders, receivers, grad_node, grad_edge, edge_w1, edge_b1, edge_w2, edge_vec, node_w1, node_b1, node_w2, node_vec):
        layers = edge_w1.shape[0]
        cols = node_lat.shape[2]
        nodes, edges = node_lat.shape[1], edge_lat.shape[1]
        npad = -(-nodes // TN) * TN
        eh = -(-edges // (2 * EC)) * EC
        nch = eh // EC
        dpn = mesh.shape['dp']
        per = SLABS // dpn
        dims = (layers, cols, nodes, edges, npad, eh, dpn)
        flat = lambda arr: jnp.swapaxes(arr, 1, 2)
        lead = lambda arr: jnp.transpose(arr, (1, 0, 2))
        args = (flat(node_lat), flat(edge_lat), flat(grad_node), flat(grad_edge), senders, receivers,
                edge_w1.reshape(-1, D), flat(edge_w2).reshape(-1, D), node_w1.reshape(-1, D), flat(node_w2).reshape(-1, D),
                lead(edge_vec), lead(node_vec), edge_b1, node_b1)
        vm, sem = pltpu.VMEM, pltpu.SemaphoreType.DMA
        wrows = HEAD + layers * LROWS
        lat_n, lat_e = (2, cols, nodes), (2, cols, edges)
        scratch = [
            vm(lat_n, BF), vm(lat_n, BF), vm(lat_e, BF), vm(lat_e, BF), vm((wrows, D), F32), vm((3, wrows, D), F32),
            vm((2, cols, npad), F32), vm((3, cols, npad), F32), vm((2, cols, npad), F32), vm((3, cols, npad), F32),
            vm((cols, npad), F32), vm((cols, npad), F32), vm((cols, npad), F32), vm((cols, npad), F32),
            vm((3, cols, eh), F32), vm((3, cols, eh), F32), vm((3, cols, eh), F32), vm((3, cols, eh), F32), vm((3, cols, eh), F32), vm((3, cols, eh), F32),
            vm((2 * layers, D, npad), F32), vm((2 * layers, D, npad), F32),
            vm((layers, D, eh), F32), vm((layers, D, eh), F32), vm((8, eh), F32),
            vm((layers, D, npad), F32), vm((layers, D, npad), F32), vm((8, npad), F32),
            vm((D, npad), F32), vm((D, npad), F32), vm((D, npad), F32), vm((8, 2 * eh), jnp.int32), vm((D, D), F32), vm((layers, 2, 4 * D, D), F32),
            vm((layers, SLABS, D, D), F32), vm((layers, 2, SLABS, cols, D), F32), vm((layers, SLABS, 2, cols, D), F32),
            vm((layers, dpn - 1, per, 2, cols, D), F32), vm((layers, per, cols, D), F32), vm((layers, per, cols, D), F32),
            vm((layers, per, cols, D), F32), vm((layers, SLABS, cols, D), F32),
            sem((layers, 2)), sem((layers, 2)), sem((2, layers, dpn - 1)), sem((2, layers, dpn - 1)), sem((layers,)), sem((layers,)),
            sem((4,)), sem((2, 3)), sem((2, 3)), sem((3, 3)), sem((3, 3)), sem((4, 3, nch)), sem((4, 3, nch)),
            sem((2 * layers,)), sem((2 * layers,)), sem((4,))]
        outs = [shape(lat_n, BF), shape(lat_e, BF), shape(lat_n, BF), shape(lat_e, BF),
                shape((layers, 3, cols, D), F32), shape((layers, D), F32), shape((layers, cols, D), F32), shape((3, layers, cols), F32),
                shape((layers, 2, cols, D), F32), shape((layers, D), F32), shape((layers, cols, D), F32), shape((3, layers, cols), F32)]
        res = pl.pallas_call(
            lambda *refs: step_kernel(dims, *refs),
            name='graph_step',
            out_shape=outs,
            in_specs=[HB] * 4 + [VM] * 10,
            out_specs=[HB] * 4 + [VM] * 8,
            scratch_shapes=scratch,
            compiler_params=pltpu.CompilerParams(collective_id=0, has_side_effects=True, vmem_limit_bytes=67_043_328),
        )(*args)

        res = finish(res)
        return (flat(res[0]), flat(res[1]), flat(res[2]), flat(res[3]),
                res[4], res[5], flat(res[6]), lead(res[7]), res[8], res[9], flat(res[10]), lead(res[11]))

    return jax.shard_map(local_step, mesh=mesh, in_specs=in_specs, out_specs=out_specs, check_vma=False)
```

```python
import jax
import jax.numpy as jnp
from jax import lax
from jax.experimental import pallas as pl
from jax.experimental.pallas import tpu as pltpu
from jax.sharding import PartitionSpec as P

LN_EPS = 1e-5
D = 128
T = 256
TN = 384
EC = 512
KS = 1408
BF = jnp.bfloat16
F32 = jnp.float32
I16 = jnp.int16
MESH = pl.DeviceIdType.MESH
VM = pl.BlockSpec(memory_space=pltpu.VMEM)
HB = pl.BlockSpec(memory_space=pl.ANY)
GROUP = 4
BOTH = (0, 1)
THREE = (0, 1, 2)
OTHERS = (1, 2, 3)
EDGE_IN, GRAD_IN, EDGE_OUT, GRAD_OUT = range(4)
SEND_ORDER = (2, 3, 1)
LROWS = 7 * (D // 4)
HEAD = 16
SLABS = 8


def dot(a, b):
    return jnp.dot(a, b, preferred_element_type=F32)


def dot_nt(a, b):
    return lax.dot_general(a, b, (((1,), (1,)), ((), ())), preferred_element_type=F32)


def mat(k, n=1):
    return slice(k * D, (k + n) * D)


def rows_of(d):
    q = D // 4
    return slice(d * q, (d + 1) * q)


def at(step, width):
    return pl.ds(pl.multiple_of(step * width, width), width)


def loop(stop, body, start=0):
    def step(j, carry):
        body(j)
        return carry

    lax.fori_loop(start, stop, step, 0)


def column_sum(val):
    return jnp.sum(val, axis=0, keepdims=True)


def flip(val):
    return jnp.swapaxes(val, 0, 1)


def stacked(parts):
    return jnp.concatenate(parts, axis=0)


def beside(parts):
    return jnp.concatenate(parts, axis=1)


def slot(d):
    return d - 1


def sigmoid(hidden):
    return 1.0 / (1.0 + jnp.exp(-hidden))


def fold(val):
    total = val[:, mat(0)]
    for start in range(D, val.shape[1], D):
        total = total + val[:, start:start + D]
    return total


def swap_halves(val):
    return stacked([val[rows_of(d)] for d in (1, 0, 3, 2)])


def gather(table, keys, iota):
    acc = None
    nodes = table.shape[1]
    one, zero = jnp.ones((), BF), jnp.zeros((), BF)
    for base in range(0, nodes, T):
        width = min(T, nodes - base)
        ids = iota[0:width, :]
        hot = beside([jnp.where(ids == (key - jnp.asarray(base, I16)), one, zero) for key in keys])
        part = dot(table[:, base:base + width], hot)
        acc = part if acc is None else acc + part
    return acc


def scatter(acc_ref, val, cols, lanes):
    nodes = acc_ref.shape[1]
    one, zero = jnp.ones((), BF), jnp.zeros((), BF)
    row = lanes[0:1, :]
    for base in range(0, nodes, T):
        width = min(T, nodes - base)
        hot = beside([jnp.where((row + jnp.asarray(base + s, I16)) == cols, one, zero) for s in range(0, width, D)])
        acc_ref[:, base:base + width] += dot(val, hot)


def mlp_tail(hidden, w2t, vec):
    act = (hidden * sigmoid(hidden)).astype(BF)
    out = dot(w2t, act) + vec[0]
    mean = column_sum(out) / D
    centered = out - mean
    var = column_sum(centered * centered) / D
    inv = lax.rsqrt(var + LN_EPS)
    normed = centered * inv
    message = (normed * vec[1] + vec[2]).astype(BF)
    return message, normed, inv


def mlp_back(d_msg, hidden, normed, inv, w2, vec):
    d_normed = d_msg * vec[1]
    mean0 = column_sum(d_normed) / D
    mean1 = column_sum(d_normed * normed) / D
    d_out = inv * (d_normed - mean0 - normed * mean1)
    d_out_bf = d_out.astype(BF)
    sig = sigmoid(hidden)
    act = (hidden * sig).astype(BF)
    d_w2 = dot_nt(d_out_bf, act)
    d_hidden = dot(w2, d_out_bf) * (sig * (1.0 + hidden * (1.0 - sig)))
    sums = (fold(d_out), fold(d_msg * normed), fold(d_msg), fold(d_hidden))
    return d_hidden.astype(BF), d_w2, sums


def add_sums(ref, parts):
    for q in range(4):
        total = parts[0][q]
        for other in parts[1:]:
            total = total + other[q]
        ref[mat(q), :] += total


def step_kernel(dims, *refs):
    layers, cols, nodes, edges, npad, eh, dpn = dims
    nch = eh // EC
    top = layers - 1
    n_in = 14
    (node_in, edge_in, gnode_in, gedge_in, send_ids, recv_ids, ew1_in, ew2_in, nw1_in, nw2_in, evec_in, nvec_in, eb1_in, nb1_in) = refs[:n_in]
    n_out = 12
    (node_out, edge_out, dnode_out, dedge_out, ew1_out, eb1_out, ew2_out, evec_out, nw1_out, nb1_out, nw2_out, nvec_out) = refs[n_in:n_in + n_out]
    (node_raw, gnode_raw, edge_raw, gedge_raw, w_send, w_recv, n_send, n_recv, gn_send, gn_recv, no_send, no_recv, dn_send, dn_recv,
     e_send, g_send, e_recv, g_recv, eo_recv, de_recv, part, part_recv, hidden, normed, inv, nhid, nnrm, ninv, d_part, s_sum, r_sum,
     ew1_buf, eb1_buf, ew2_buf, evec_buf, nw1_buf, nb1_buf, nw2_buf, nvec_buf, ids_raw, bias_cols, sums, grad, core_recv, half, dp_recv, cross_send, cross_recv, own_sum, gathered,
     core_ss, core_rs, dp_ss, dp_rs, cross_ss, cross_rs, load_sem, w_ss, w_rs, n_ss, n_rs, e_ss, e_rs, p_ss, p_rs, out_sem) = refs[n_in + n_out:]

    t = lax.axis_index('tp')
    p = lax.axis_index('dp')
    per = SLABS // dpn
    dp_others = range(1, dpn)
    x, c = t // 2, lax.rem(t, 2)
    ox, oc = 1 - x, 1 - c
    peer = [t, t + 1 - 2 * c, t + 2 - 4 * x, t + 3 - 2 * c - 4 * x]

    def remote(src, dst, ssem, rsem, d):
        return pltpu.make_async_remote_copy(src_ref=src, dst_ref=dst, send_sem=ssem, recv_sem=rsem,
                                            device_id={'tp': peer[d]}, device_id_type=MESH)

    loads = [pltpu.make_async_copy(src, dst, load_sem.at[q]) for q, (src, dst) in enumerate(
        [(node_in, node_raw), (edge_in, edge_raw), (gnode_in, gnode_raw), (gedge_in, gedge_raw)])]
    for copy in loads:
        copy.start()

    def node_copies(send, recv, kind):
        return (remote(send.at[1], recv.at[0], n_ss.at[kind, 0], n_rs.at[kind, 0], 1),
                remote(send.at[0], recv.at[1], n_ss.at[kind, 1], n_rs.at[kind, 1], 2),
                remote(recv.at[1], recv.at[2], n_ss.at[kind, 2], n_rs.at[kind, 2], 1))

    piece = w_send.shape[0] // dpn

    def weight_rows(owner):
        return pl.ds(pl.multiple_of(owner * piece, 8), piece)

    w_pair = remote(w_send, w_recv.at[0], w_ss.at[0], w_rs.at[0], 1)
    w_cross = remote(w_send.at[weight_rows(p)], w_recv.at[1, weight_rows(p)], w_ss.at[1], w_rs.at[1], 2)
    w_relay = remote(w_recv.at[1], w_recv.at[2], w_ss.at[2], w_rs.at[2], 1)

    def weight_copy(i, owner):
        rows = w_recv.at[1, weight_rows(owner)]
        return dp_remote(rows, rows, 2, 0, i)

    def edge_copy(kind, j, d, width):
        src, dst = ((e_send, e_recv), (g_send, g_recv), (e_send, eo_recv), (g_send, de_recv))[kind]
        place = (slot(d), j) if width == EC else (slot(d), j, slice(None), slice(width))
        return remote(src.at[place], dst.at[place], e_ss.at[kind, slot(d), j], e_rs.at[kind, slot(d), j], d)

    def edge_do(kind, j, d, action):
        outward = kind in (EDGE_OUT, GRAD_OUT)
        other = oc if d % 2 else c
        half_id = c if outward == (action != 'wait_recv') else other
        narrow = jnp.logical_and(j == nch - 1, half_id == 1)

        @pl.when(jnp.logical_not(narrow))
        def _():
            getattr(edge_copy(kind, j, d, EC), action)()

        @pl.when(narrow)
        def _():
            getattr(edge_copy(kind, j, d, T), action)()

    def core_copy(l, b):
        return remote(grad.at[l, :, pl.ds((2 * b + 1) * cols, cols), :], core_recv.at[l, b], core_ss.at[l, b], core_rs.at[l, b], 1)

    def dp_remote(src, dst, stage, l, i):
        return pltpu.make_async_remote_copy(src_ref=src, dst_ref=dst, send_sem=dp_ss.at[stage, l, i - 1], recv_sem=dp_rs.at[stage, l, i - 1],
                                            device_id={'dp': lax.rem(p + i, dpn)}, device_id_type=MESH)

    def spread_copy(l, i):
        return dp_remote(half.at[l, pl.ds(lax.rem(p + i, dpn) * per, per)], dp_recv.at[l, i - 1], 0, l, i)

    def cross_copy(l):
        return remote(cross_send.at[l], cross_recv.at[l], cross_ss.at[l], cross_rs.at[l], 2)

    def gather_copy(l, i, owner):
        return dp_remote(own_sum.at[l], gathered.at[l, pl.ds(owner * per, per)], 1, l, i)

    def part_copy(q):
        return remote(part.at[q], part_recv.at[q], p_ss.at[q], p_rs.at[q], 1)

    def load_nodes(raw, send, own):
        send[...] = jnp.zeros_like(send)
        send[0, :, :nodes] = raw[ox].astype(F32)
        send[1, :, :nodes] = raw[x].astype(F32)
        own[:cols, :] = send[1].astype(own.dtype)

    def load_edges(raw, send, own, kind):
        def put(j, lanes_j, val_of):
            for d in OTHERS:
                sample = x if d < 2 else ox
                send[slot(d), j] = val_of(sample, oc if d % 2 else c).astype(F32)
            own[:cols, lanes_j] = val_of(x, c)

        def chunk(j):
            put(j, at(j, EC), lambda s, h: raw[s, :, pl.ds(pl.multiple_of(h * eh + j * EC, D), EC)])
            for d in SEND_ORDER:
                edge_do(kind, j, d, 'start')

        loop(nch - 1, chunk)
        first = (nch - 1) * EC
        used = edges - eh - first
        last = pl.ds(first, EC)

        def tail(s, h):
            left = raw[s, :, pl.ds(first, EC)]
            right = beside([raw[s, :, pl.ds(eh + first, used)], jnp.zeros((cols, EC - used), BF)])
            return jnp.where(h == 0, left.astype(F32), right.astype(F32)).astype(BF)

        put(nch - 1, last, tail)
        for d in SEND_ORDER:
            edge_do(kind, nch - 1, d, 'start')

    def place_edges(raw, block, d, j):
        s = x if d < 2 else ox
        h = oc if d % 2 else c
        val = block.astype(BF)
        first = (nch - 1) * EC
        used = edges - eh - first

        @pl.when(jnp.logical_or(j < nch - 1, h == 0))
        def _():
            raw[s, :, pl.ds(pl.multiple_of(h * eh + j * EC, D), EC)] = val

        @pl.when(jnp.logical_and(j == nch - 1, h == 1))
        def _():
            raw[s, :, pl.ds(eh + first, used)] = val[:, :used]

    def scoped(e0, e1, ge, msg, v0, v1, v2, agg0, agg1, d_agg, scol, rcol, srow, rrow, iota, lanes, ew1, ew1t, ew2, ew2t, nw1, nw1t, nw2, nw2t, vecs):
        tables = (v0, v1, v2)
        aggs = (agg0, agg1)
        edges_in = (e0, e1)

        barrier = pltpu.get_barrier_semaphore()
        for d in OTHERS:
            pl.semaphore_signal(barrier, inc=1, device_id={'tp': peer[d]}, device_id_type=MESH)
        for i in dp_others:
            pl.semaphore_signal(barrier, inc=1, device_id={'dp': lax.rem(p + i, dpn)}, device_id_type=MESH)
        loads[0].wait()
        with jax.named_scope('send_nodes'):
            load_nodes(node_raw, n_send, v0)
        ncop = node_copies(n_send, n_recv, 0)
        q = cols
        w_send[:HEAD, :] = jnp.zeros((HEAD, D), F32)
        for k in THREE:
            w_send[k * layers:(k + 1) * layers, :cols] = evec_in[k]
            w_send[(3 + k) * layers:(4 + k) * layers, :cols] = nvec_in[k]
        for l in range(layers):
            off = HEAD + l * LROWS
            w_send[off:off + 3 * q, :] = ew1_in[l * 3 * q:(l + 1) * 3 * q, :].astype(F32)
            w_send[off + 3 * q:off + 4 * q, :] = ew2_in[l * q:(l + 1) * q, :].astype(F32)
            w_send[off + 4 * q:off + 6 * q, :] = nw1_in[l * 2 * q:(l + 1) * 2 * q, :].astype(F32)
            w_send[off + 6 * q:off + 7 * q, :] = nw2_in[l * q:(l + 1) * q, :].astype(F32)
        with jax.named_scope('barrier'):
            pl.semaphore_wait(barrier, len(OTHERS) + dpn - 1)
        w_cross.start()
        w_pair.start()
        ncop[1].start()
        ncop[0].start()
        loads[1].wait()
        with jax.named_scope('send_edges'):
            load_edges(edge_raw, e_send, e0, EDGE_IN)
        loads[2].wait()
        load_nodes(gnode_raw, gn_send, d_part)
        gcop = node_copies(gn_send, gn_recv, 1)
        gcop[1].start()
        gcop[0].start()
        loads[3].wait()
        with jax.named_scope('send_grads'):
            load_edges(gedge_raw, g_send, ge, GRAD_IN)

        w_cross.wait_recv()
        for i in dp_others:
            weight_copy(i, p).start()

        @pl.when(c == 1)
        def _():
            for recv in (e_recv, g_recv):
                recv[:, nch - 1, :, T:] = jnp.zeros((3, cols, EC - T), F32)

        iota[...] = lax.broadcasted_iota(jnp.int32, (T, D), 0).astype(I16)
        lanes[...] = lax.broadcasted_iota(jnp.int32, (16, D), 1).astype(I16)

        ids_raw[...] = jnp.full(ids_raw.shape, -1, jnp.int32)
        for which, src in enumerate((send_ids, recv_ids)):
            ids_raw[which:which + 1, :edges] = src[...].reshape(1, edges)

        def ids(b):
            for which, (row_ref, col_ref) in enumerate(((srow, scol), (rrow, rcol))):
                wide = jnp.broadcast_to(ids_raw[which:which + 1, pl.ds(pl.multiple_of(c * eh + b * D, D), D)], (D, D))
                row_ref[at(b, 16), :] = wide[:16].astype(I16)
                col_ref[at(b, D), :] = flip(wide.astype(F32)).astype(jnp.int32).astype(I16)

        with jax.named_scope('ids'):
            loop(eh // D, ids)

        def keys(ref, step):
            return [ref[pl.ds(pl.multiple_of(step * (KS // D) * 16 + 16 * h, 16), 1), :] for h in range(KS // D)]

        bias_cols[...] = flip(stacked([eb1_in[...], nb1_in[...], jnp.zeros((D - 2 * layers, D), F32)]))

        def join_weights(l):
            off = HEAD + l * LROWS
            for d in range(GROUP):
                src = w_send if d == 0 else w_recv.at[slot(d)]
                r = slice(d * q, (d + 1) * q)
                for k in THREE:
                    ew1[l, k * D + d * q:k * D + (d + 1) * q, :] = src[off + k * q:off + (k + 1) * q, :].astype(BF)
                ew2t[l, r, :] = src[off + 3 * q:off + 4 * q, :].astype(BF)
                for k in range(2):
                    nw1[l, k * D + d * q:k * D + (d + 1) * q, :] = src[off + (4 + k) * q:off + (5 + k) * q, :].astype(BF)
                nw2t[l, r, :] = src[off + 6 * q:off + 7 * q, :].astype(BF)

            def flip_bf(mat):
                return flip(mat.astype(F32)).astype(BF)

            for k in THREE:
                ew1t[l, :, mat(k)] = flip_bf(ew1[l, mat(k), :])
            for k in range(2):
                nw1t[l, :, mat(k)] = flip_bf(nw1[l, mat(k), :])
            ew2[l] = flip_bf(ew2t[l])
            nw2[l] = flip_bf(nw2t[l])

        def wait_recvs(copies):
            copies[1].wait_recv()
            copies[2].start()
            copies[0].wait_recv()
            copies[2].wait_recv()

        with jax.named_scope('node_wait'):
            wait_recvs(ncop)
        for d in OTHERS:
            v0[rows_of(d), :] = n_recv[slot(d)].astype(BF)
        with jax.named_scope('weight_wait'):
            for i in dp_others:
                weight_copy(i, lax.rem(p + dpn - i, dpn)).wait_recv()
            w_relay.start()
            w_pair.wait_recv()
            w_relay.wait_recv()
        rows_all = beside([w_send[:HEAD, :cols]] + [w_recv[d, :HEAD, :cols] for d in range(3)])
        vecs[...] = flip(stacked([rows_all, jnp.zeros((D - HEAD, D), F32)]))
        join_weights(0)

        def vec(l, node):
            first = 6 * node + l
            return [vecs[:, first + 2 * k:first + 2 * k + 1] for k in THREE]

        def bias(l, node):
            return bias_cols[:, node * layers + l:node * layers + l + 1]

        def hidden_of_nodes(l):
            table, b1 = tables[l], bias(l, 0)

            def body(step):
                xs = gather(table, keys(srow, step), iota).astype(BF)
                xr = gather(table, keys(rrow, step), iota).astype(BF)
                hidden[l, :, at(step, KS)] = dot(ew1t[l, :, mat(1, 2)], stacked([xs, xr])) + b1

            loop(eh // KS, body)

        def edge_forward(l):
            e_in = edges_in[l]

            def body(j):
                for sub in range(EC // T):
                    a = at(j * (EC // T) + sub, T)
                    if l == 0:
                        if sub == 0:
                            for d in OTHERS:
                                edge_do(EDGE_IN, j, d, 'wait_recv')
                        for d in OTHERS:
                            e_in[rows_of(d), a] = e_recv[slot(d), j, :, sub * T:(sub + 1) * T].astype(BF)
                    e_val = e_in[:, a]
                    hid = hidden[l, :, a] + dot(ew1t[l, :, mat(0)], e_val)
                    hidden[l, :, a] = hid
                    message, nrm, std = mlp_tail(hid, ew2t[l], vec(l, 0))
                    normed[l, :, a] = nrm
                    inv[l:l + 1, a] = std
                    msg[:, a] = message
                    e_new = (e_val.astype(F32) + message.astype(F32)).astype(BF)
                    if l < top:
                        edges_in[l + 1][:, a] = e_new
                    else:
                        for d in OTHERS:
                            e_send[slot(d), j, :, sub * T:(sub + 1) * T] = e_new[rows_of(d)].astype(F32)
                        if sub == 0:
                            own_parts = []
                        own_parts.append(e_new[:q])
                if l == top:
                    for d in SEND_ORDER:
                        edge_do(EDGE_OUT, j, d, 'start')
                    place_edges(edge_raw, beside(own_parts), 0, j)

            loop(nch, body)

        def segment_sum(acc, ids_ref):
            acc[...] = jnp.zeros(acc.shape, F32)

            def body(step):
                scatter(acc, msg[:, at(step, KS)], ids_ref[at(step, KS), :], lanes)

            loop(eh // KS, body)

        def node_forward(l):
            table, agg, out = tables[l], aggs[l], tables[l + 1]

            def body(step):
                a = pl.ds(pl.multiple_of(step * TN, D), TN)
                v_in = table[:, a]
                agg_bf = (part[l, :, a] + swap_halves(part_recv[l, :, a])).astype(BF)
                agg[:, a] = agg_bf
                hid = dot(nw1t[l], stacked([v_in, agg_bf])) + bias(l, 1)
                nhid[l, :, a] = hid
                message, nrm, std = mlp_tail(hid, nw2t[l], vec(l, 1))
                nnrm[l, :, a] = nrm
                ninv[l:l + 1, a] = std
                out[:, a] = (v_in.astype(F32) + message.astype(F32)).astype(BF)

            loop(npad // TN, body)

        for l in range(layers):
            with jax.named_scope(f'gather_{l}'):
                hidden_of_nodes(l)
            if l == top:
                def drain(j):
                    for d in OTHERS:
                        edge_do(EDGE_IN, j, d, 'wait_send')
                loop(nch, drain)
            with jax.named_scope(f'edge_forward_{l}'):
                edge_forward(l)
            with jax.named_scope(f'sum_{l}'):
                segment_sum(part.at[l], rcol)
            part_copy(l).start()
            if l == 0:
                join_weights(1)
                gcop[1].wait_recv()
                gcop[2].start()
            with jax.named_scope(f'part_wait_{l}'):
                part_copy(l).wait_recv()
            with jax.named_scope(f'node_forward_{l}'):
                node_forward(l)
        no_send[...] = tables[layers][2 * q:3 * q, :].astype(F32)
        no_copy = remote(no_send, no_recv, n_ss.at[2, 0], n_rs.at[2, 0], 2)
        no_copy.start()
        node_raw[x] = tables[layers][:q, :nodes]

        hold = nch - 3
        grad[...] = jnp.zeros_like(grad)
        sums[...] = jnp.zeros_like(sums)
        with jax.named_scope('grad_node_wait'):
            gcop[0].wait_recv()
            gcop[2].wait_recv()
        for d in OTHERS:
            d_part[rows_of(d), :] = gn_recv[slot(d)]

        def node_backward(l):
            table, agg = tables[l], aggs[l]

            def body(step):
                a = pl.ds(pl.multiple_of(step * TN, D), TN)
                d_in = d_part[:, a]
                if l < top:
                    d_in = d_in + part[layers + l + 1, :, a] + swap_halves(part_recv[layers + l + 1, :, a])
                    d_in = d_in.astype(BF).astype(F32)
                d_hid, d_w2, parts = mlp_back(d_in, nhid[l, :, a], nnrm[l, :, a], ninv[l:l + 1, a], nw2[l], vec(l, 1))
                add_sums(sums.at[l, 1], [parts])
                grad[l, 6] += d_w2
                grad[l, 4] += dot_nt(table[:, a], d_hid)
                grad[l, 5] += dot_nt(agg[:, a], d_hid)
                d_part[:, a] = d_in + dot(nw1[l, mat(0), :], d_hid)
                d_agg[:, a] = dot(nw1[l, mat(1), :], d_hid).astype(BF)

            loop(npad // TN, body)

        def gather_back():
            def body(step):
                msg[:, at(step, KS)] = gather(d_agg, keys(rrow, step), iota).astype(BF)

            loop(eh // KS, body)

        def edge_backward(l):
            e_in = edges_in[l]

            def body(j):
                all_parts, d_w2s, d_w1s, own_parts = [], [], [], []
                for sub in range(EC // T):
                    a = at(j * (EC // T) + sub, T)
                    if l == top:
                        if sub == 0:
                            for d in OTHERS:
                                edge_do(GRAD_IN, j, d, 'wait_recv')
                        for d in OTHERS:
                            ge[rows_of(d), a] = g_recv[slot(d), j, :, sub * T:(sub + 1) * T].astype(BF)
                    d_res = ge[:, a].astype(F32)
                    d_msg = d_res + msg[:, a].astype(F32)
                    d_hid, d_w2, parts = mlp_back(d_msg, hidden[l, :, a], normed[l, :, a], inv[l:l + 1, a], ew2[l], vec(l, 0))
                    all_parts.append(parts)
                    d_w2s.append(d_w2)
                    d_w1s.append(dot_nt(e_in[:, a], d_hid))
                    msg[:, a] = d_hid
                    d_new = (d_res + dot(ew1[l, mat(0), :], d_hid)).astype(BF)
                    if l > 0:
                        ge[:, a] = d_new
                    else:
                        for d in OTHERS:
                            g_send[slot(d), j, :, sub * T:(sub + 1) * T] = d_new[rows_of(d)].astype(F32)
                        own_parts.append(d_new[:q])
                add_sums(sums.at[l, 0], all_parts)
                grad[l, 3] += sum(d_w2s[1:], d_w2s[0])
                grad[l, 0] += sum(d_w1s[1:], d_w1s[0])
                if l == 0:
                    @pl.when(j < hold)
                    def _():
                        for d in SEND_ORDER:
                            edge_do(GRAD_OUT, j, d, 'start')
                    place_edges(gedge_raw, beside(own_parts), 0, j)

            loop(nch, body)

        def reduce_start(l):
            def total(node, k):
                return column_sum(flip(sums[l, node, mat(k), :]))

            lat = stacked([total(node, k) for node in BOTH for k in THREE])
            biases = stacked([total(node, 3) for node in BOTH])
            n_lat = lat.shape[0]
            for d in range(GROUP):
                grad[l, SLABS - 1, d * cols:d * cols + n_lat, :cols] = lat[:, rows_of(d)]
                grad[l, SLABS - 1, d * cols + n_lat:d * cols + n_lat + 2, :] = biases
            for b in BOTH:
                core_copy(l, b).start()

        def chip_sum(l):
            row = lax.broadcasted_iota(jnp.int32, (cols, D), 0)
            edge_row = jnp.logical_or(row < 3, row == 6)
            for b in BOTH:
                core_copy(l, b).wait_recv()
                for k in range(SLABS):
                    own = grad[l, k, rows_of(2 * b), :]
                    if k < 4:
                        own = own + core_recv[l, b, k]
                    elif k == SLABS - 1:
                        own = own + jnp.where(edge_row, core_recv[l, b, k], 0.0)
                    half[l, k, b] = own
            for i in dp_others:
                spread_copy(l, i).start()

        def dp_sum(l):
            total = half[l, pl.ds(p * per, per)]
            for i in dp_others:
                spread_copy(l, i).wait_recv()
                total = total + dp_recv[l, i - 1]
            own_sum[l] = total[:, 0]
            cross_send[l] = total[:, 1]
            cross_copy(l).start()

        def cross_sum(l):
            cross_copy(l).wait_recv()
            total = own_sum[l] + cross_recv[l]
            own_sum[l] = total
            gathered[l, pl.ds(p * per, per)] = total
            for i in dp_others:
                gather_copy(l, i, p).start()

        def project(l):
            table = tables[l]

            def body(step):
                a = pl.ds(pl.multiple_of(step * TN, D), TN)
                s_bf, r_bf, v_in = s_sum[:, a].astype(BF), r_sum[:, a].astype(BF), table[:, a]
                part[layers + l, :, a] = dot(ew1[l, mat(1), :], s_bf) + dot(ew1[l, mat(2), :], r_bf)
                grad[l, 1] += dot_nt(v_in, s_bf)
                grad[l, 2] += dot_nt(v_in, r_bf)

            loop(npad // TN, body)

        for l in reversed(range(layers)):
            with jax.named_scope(f'node_backward_{l}'):
                node_backward(l)
            if l < top:
                with jax.named_scope('chip_sum_1'):
                    chip_sum(l + 1)
            with jax.named_scope(f'gather_back_{l}'):
                gather_back()
            if l == 0:
                def drain_g(j):
                    for d in OTHERS:
                        edge_do(GRAD_IN, j, d, 'wait_send')
                loop(nch, drain_g)
            with jax.named_scope(f'edge_backward_{l}'):
                edge_backward(l)
            if l < top:
                with jax.named_scope('dp_sum_1'):
                    dp_sum(l + 1)
            with jax.named_scope(f'sum_send_{l}'):
                segment_sum(s_sum, scol)
            with jax.named_scope(f'sum_recv_{l}'):
                segment_sum(r_sum, rcol)
            with jax.named_scope(f'project_{l}'):
                project(l)
            part_copy(layers + l).start()
            with jax.named_scope(f'reduce_start_{l}'):
                reduce_start(l)
            with jax.named_scope(f'back_wait_{l}'):
                part_copy(layers + l).wait_recv()

        def final(step):
            a = pl.ds(pl.multiple_of(step * TN, D), TN)
            d_in = (d_part[:, a] + part[layers, :, a] + swap_halves(part_recv[layers, :, a])).astype(BF)
            v2[:, a] = d_in

        loop(npad // TN, final)
        dn_send[...] = v2[2 * q:3 * q, :].astype(F32)
        dn_copy = remote(dn_send, dn_recv, n_ss.at[2, 1], n_rs.at[2, 1], 2)
        dn_copy.start()
        gnode_raw[x] = v2[:q, :nodes]
        with jax.named_scope('chip_sum_0'):
            chip_sum(0)

        with jax.named_scope('node_out_wait'):
            no_copy.wait_recv()
        node_raw[ox] = no_recv[:, :nodes].astype(BF)

        def place_e(j):
            for d in OTHERS:
                edge_do(EDGE_OUT, j, d, 'wait_recv')
                place_edges(edge_raw, eo_recv[slot(d), j], d, j)

        with jax.named_scope('place_edge_out'):
            loop(nch, place_e)
        outs = [pltpu.make_async_copy(src, dst, out_sem.at[k]) for k, (src, dst) in enumerate(
            [(node_raw, node_out), (edge_raw, edge_out), (gnode_raw, dnode_out), (gedge_raw, dedge_out)])]
        outs[0].start()
        outs[1].start()
        small_outs = [pltpu.make_async_copy(src, dst, out_sem.at[4 + k]) for k, (src, dst) in enumerate(
            [(ew1_buf, ew1_out), (eb1_buf, eb1_out), (ew2_buf, ew2_out), (evec_buf, evec_out),
             (nw1_buf, nw1_out), (nb1_buf, nb1_out), (nw2_buf, nw2_out), (nvec_buf, nvec_out)])]

        with jax.named_scope('dp_sum_0'):
            dp_sum(0)

        def send_rest(j):
            for d in SEND_ORDER:
                edge_do(GRAD_OUT, j, d, 'start')

        loop(nch, send_rest, hold)

        def place_g(j):
            for d in OTHERS:
                edge_do(GRAD_OUT, j, d, 'wait_recv')
                place_edges(gedge_raw, de_recv[slot(d), j], d, j)

        with jax.named_scope('place_first'):
            loop(hold, place_g)
        for l in range(layers):
            with jax.named_scope(f'cross_sum_{l}'):
                cross_sum(l)
        with jax.named_scope('place_rest'):
            loop(nch - 1, place_g, hold)
        for l in range(layers):
            for i in dp_others:
                gather_copy(l, i, lax.rem(p + dpn - i, dpn)).wait_recv()
            ew1_buf[l] = gathered[l, 0:3]
            ew2_buf[l] = gathered[l, 3]
            nw1_buf[l] = gathered[l, 4:6]
            nw2_buf[l] = gathered[l, 6]
            small = gathered[l, SLABS - 1]
            for k in THREE:
                evec_buf[k, l:l + 1, :] = small[k:k + 1, :cols]
                nvec_buf[k, l:l + 1, :] = small[3 + k:4 + k, :cols]
            eb1_buf[l:l + 1, :] = small[6:7]
            nb1_buf[l:l + 1, :] = small[7:8]
        for copy in small_outs:
            copy.start()
        with jax.named_scope('place_last'):
            loop(nch, place_g, nch - 1)
        outs[3].start()
        with jax.named_scope('d_node_wait'):
            dn_copy.wait_recv()
        gnode_raw[ox] = dn_recv[:, :nodes].astype(BF)
        outs[2].start()

        for l in range(layers):
            for b in BOTH:
                core_copy(l, b).wait_send()
            cross_copy(l).wait_send()
            for i in dp_others:
                spread_copy(l, i).wait_send()
                gather_copy(l, i, p).wait_send()
        for copy in ncop + gcop + (w_pair, w_cross, w_relay):
            copy.wait_send()
        for i in dp_others:
            weight_copy(i, p).wait_send()
        no_copy.wait_send()
        dn_copy.wait_send()
        for k in range(2 * layers):
            part_copy(k).wait_send()

        def drain_out(j):
            for kind in (EDGE_OUT, GRAD_OUT):
                for d in OTHERS:
                    edge_do(kind, j, d, 'wait_send')

        loop(nch, drain_out)
        for copy in outs + small_outs:
            copy.wait()

    bf = lambda *s: pltpu.VMEM(s, BF)
    pl.run_scoped(
        scoped, bf(D, eh), bf(D, eh), bf(D, eh), bf(D, eh), bf(D, npad), bf(D, npad), bf(D, npad), bf(D, npad), bf(D, npad), bf(D, npad),
        pltpu.VMEM((eh, D), I16), pltpu.VMEM((eh, D), I16), pltpu.VMEM((eh // D * 16, D), I16), pltpu.VMEM((eh // D * 16, D), I16),
        pltpu.VMEM((T, D), I16), pltpu.VMEM((16, D), I16),
        bf(layers, 3 * D, D), bf(layers, D, 3 * D), bf(layers, D, D), bf(layers, D, D),
        bf(layers, 2 * D, D), bf(layers, D, 2 * D), bf(layers, D, D), bf(layers, D, D), pltpu.VMEM((D, D), F32))


def finish_kernel(*refs):
    count = (len(refs) - 2) // 3
    in_sem, out_sem = refs[3 * count:]
    moves = []
    for k in range(count):
        trio = refs[k], refs[2 * count + k], refs[count + k]
        if k < 4:
            rows = trio[0].shape[1] // 2
            parts = [[ref.at[s, pl.ds(r * rows, rows)] for ref in trio] for s in BOTH for r in BOTH]
        else:
            parts = [trio]
        moves += parts
    pulls = [pltpu.make_async_copy(src, buf, in_sem.at[k]) for k, (src, buf, _) in enumerate(moves)]
    puts = [pltpu.make_async_copy(buf, dst, out_sem.at[k]) for k, (_, buf, dst) in enumerate(moves)]
    for pull in pulls:
        pull.start()
    for pull, put in zip(pulls, puts):
        pull.wait()
        put.start()
    for put in puts:
        put.wait()


def finish(arrays):
    sems = pltpu.SemaphoreType.DMA((2 * len(arrays),))
    return pl.pallas_call(
        finish_kernel,
        name='finish',
        out_shape=[jax.ShapeDtypeStruct(a.shape, a.dtype) for a in arrays],
        in_specs=[HB] * len(arrays),
        out_specs=[HB] * len(arrays),
        scratch_shapes=[pltpu.VMEM(a.shape, a.dtype) for a in arrays] + [sems, sems],
    )(*arrays)


def solution(mesh):
    lat_spec = P('dp', None, 'tp')
    first_spec = P(None, None, 'tp', None)
    col_spec = P(None, None, 'tp')
    param_specs = (first_spec, P(), col_spec, col_spec, first_spec, P(), col_spec, col_spec)
    in_specs = (lat_spec, lat_spec, P(), P(), lat_spec, lat_spec) + param_specs
    out_specs = (lat_spec, lat_spec, lat_spec, lat_spec) + param_specs
    shape = jax.ShapeDtypeStruct

    def local_step(node_lat, edge_lat, senders, receivers, grad_node, grad_edge, edge_w1, edge_b1, edge_w2, edge_vec, node_w1, node_b1, node_w2, node_vec):
        layers = edge_w1.shape[0]
        cols = node_lat.shape[2]
        nodes, edges = node_lat.shape[1], edge_lat.shape[1]
        npad = -(-nodes // TN) * TN
        eh = -(-edges // (2 * EC)) * EC
        nch = eh // EC
        dpn = mesh.shape['dp']
        per = SLABS // dpn
        dims = (layers, cols, nodes, edges, npad, eh, dpn)
        flat = lambda arr: jnp.swapaxes(arr, 1, 2)
        lead = lambda arr: jnp.transpose(arr, (1, 0, 2))
        args = (flat(node_lat), flat(edge_lat), flat(grad_node), flat(grad_edge), senders, receivers,
                edge_w1.reshape(-1, D), flat(edge_w2).reshape(-1, D), node_w1.reshape(-1, D), flat(node_w2).reshape(-1, D),
                lead(edge_vec), lead(node_vec), edge_b1, node_b1)
        vm, sem = pltpu.VMEM, pltpu.SemaphoreType.DMA
        wrows = -(-(HEAD + layers * LROWS) // (8 * dpn)) * 8 * dpn
        lat_n, lat_e = (2, cols, nodes), (2, cols, edges)
        outs = [shape(lat_n, BF), shape(lat_e, BF), shape(lat_n, BF), shape(lat_e, BF),
                shape((layers, 3, cols, D), F32), shape((layers, D), F32), shape((layers, cols, D), F32), shape((3, layers, cols), F32),
                shape((layers, 2, cols, D), F32), shape((layers, D), F32), shape((layers, cols, D), F32), shape((3, layers, cols), F32)]
        scratch = [
            vm(lat_n, BF), vm(lat_n, BF), vm(lat_e, BF), vm(lat_e, BF), vm((wrows, D), F32), vm((3, wrows, D), F32),
            vm((2, cols, npad), F32), vm((3, cols, npad), F32), vm((2, cols, npad), F32), vm((3, cols, npad), F32),
            vm((cols, npad), F32), vm((cols, npad), F32), vm((cols, npad), F32), vm((cols, npad), F32),
            *[vm((3, nch, cols, EC), F32)] * 6,
            vm((2 * layers, D, npad), F32), vm((2 * layers, D, npad), F32),
            vm((layers, D, eh), F32), vm((layers, D, eh), F32), vm((8, eh), F32),
            vm((layers, D, npad), F32), vm((layers, D, npad), F32), vm((8, npad), F32),
            vm((D, npad), F32), vm((D, npad), F32), vm((D, npad), F32), *[vm(o.shape, F32) for o in outs[4:]], vm((8, 2 * eh), jnp.int32), vm((D, D), F32), vm((layers, 2, 4 * D, D), F32),
            vm((layers, SLABS, D, D), F32), vm((layers, 2, SLABS, cols, D), F32), vm((layers, SLABS, 2, cols, D), F32),
            vm((layers, dpn - 1, per, 2, cols, D), F32), vm((layers, per, cols, D), F32), vm((layers, per, cols, D), F32),
            vm((layers, per, cols, D), F32), vm((layers, SLABS, cols, D), F32),
            sem((layers, 2)), sem((layers, 2)), sem((3, layers, dpn - 1)), sem((3, layers, dpn - 1)), sem((layers,)), sem((layers,)),
            sem((4,)), sem((3,)), sem((3,)), sem((3, 3)), sem((3, 3)), sem((4, 3, nch)), sem((4, 3, nch)),
            sem((2 * layers,)), sem((2 * layers,)), sem((12,))]
        res = pl.pallas_call(
            lambda *refs: step_kernel(dims, *refs),
            name='graph_step',
            out_shape=outs,
            in_specs=[HB] * 4 + [VM] * 10,
            out_specs=[HB] * 12,
            scratch_shapes=scratch,
            compiler_params=pltpu.CompilerParams(collective_id=0, has_side_effects=True, vmem_limit_bytes=67_043_328),
        )(*args)

        res = finish(res)
        return (flat(res[0]), flat(res[1]), flat(res[2]), flat(res[3]),
                res[4], res[5], flat(res[6]), lead(res[7]), res[8], res[9], flat(res[10]), lead(res[11]))

    return jax.shard_map(local_step, mesh=mesh, in_specs=in_specs, out_specs=out_specs, check_vma=False)
```

```python
import jax
import jax.numpy as jnp
from jax import lax
from jax.experimental import pallas as pl
from jax.experimental.pallas import tpu as pltpu
from jax.sharding import PartitionSpec as P

LN_EPS = 1e-5
D = 128
T = 256
TN = 384
EC = 512
KS = 1408
BF = jnp.bfloat16
F32 = jnp.float32
I16 = jnp.int16
MESH = pl.DeviceIdType.MESH
VM = pl.BlockSpec(memory_space=pltpu.VMEM)
HB = pl.BlockSpec(memory_space=pl.ANY)
RESULT = pltpu.VMEM
GROUP = 4
BOTH = (0, 1)
THREE = (0, 1, 2)
OTHERS = (1, 2, 3)
EDGE_IN, GRAD_IN, EDGE_OUT, GRAD_OUT = range(4)
SEND_ORDER = (2, 3, 1)
LROWS = 7 * (D // 4)
HEAD = 16
VMEM_LIMIT = 63_000_000
SLABS = 8


def dot(a, b):
    return jnp.dot(a, b, preferred_element_type=F32)


def dot_nt(a, b):
    return lax.dot_general(a, b, (((1,), (1,)), ((), ())), preferred_element_type=F32)


def mat(k, n=1):
    return slice(k * D, (k + n) * D)


def rows_of(d):
    q = D // 4
    return slice(d * q, (d + 1) * q)


def at(step, width):
    return pl.ds(pl.multiple_of(step * width, width), width)


def loop(stop, body, start=0):
    def step(j, carry):
        body(j)
        return carry

    lax.fori_loop(start, stop, step, 0)


def column_sum(val):
    return jnp.sum(val, axis=0, keepdims=True)


def flip(val):
    return jnp.swapaxes(val, 0, 1)


def stacked(parts):
    return jnp.concatenate(parts, axis=0)


def beside(parts):
    return jnp.concatenate(parts, axis=1)


def slot(d):
    return d - 1


def sigmoid(hidden):
    return 1.0 / (1.0 + jnp.exp(-hidden))


def fold(val):
    total = val[:, mat(0)]
    for start in range(D, val.shape[1], D):
        total = total + val[:, start:start + D]
    return total


def swap_halves(val):
    return stacked([val[rows_of(d)] for d in (1, 0, 3, 2)])


def gather(table, keys, iota):
    acc = None
    nodes = table.shape[1]
    one, zero = jnp.ones((), BF), jnp.zeros((), BF)
    for base in range(0, nodes, T):
        width = min(T, nodes - base)
        ids = iota[0:width, :]
        hot = beside([jnp.where(ids == (key - jnp.asarray(base, I16)), one, zero) for key in keys])
        part = dot(table[:, base:base + width], hot)
        acc = part if acc is None else acc + part
    return acc


def scatter(acc_ref, val, cols, lanes):
    nodes = acc_ref.shape[1]
    one, zero = jnp.ones((), BF), jnp.zeros((), BF)
    row = lanes[0:1, :]
    for base in range(0, nodes, T):
        width = min(T, nodes - base)
        hot = beside([jnp.where((row + jnp.asarray(base + s, I16)) == cols, one, zero) for s in range(0, width, D)])
        acc_ref[:, base:base + width] += dot(val, hot)


def mlp_tail(hidden, w2t, vec):
    act = (hidden * sigmoid(hidden)).astype(BF)
    out = dot(w2t, act) + vec[0]
    mean = column_sum(out) / D
    centered = out - mean
    var = column_sum(centered * centered) / D
    inv = lax.rsqrt(var + LN_EPS)
    normed = centered * inv
    message = (normed * vec[1] + vec[2]).astype(BF)
    return message, normed, inv


def mlp_back(d_msg, hidden, normed, inv, w2, vec):
    d_normed = d_msg * vec[1]
    mean0 = column_sum(d_normed) / D
    mean1 = column_sum(d_normed * normed) / D
    d_out = inv * (d_normed - mean0 - normed * mean1)
    d_out_bf = d_out.astype(BF)
    sig = sigmoid(hidden)
    act = (hidden * sig).astype(BF)
    d_w2 = dot_nt(d_out_bf, act)
    d_hidden = dot(w2, d_out_bf) * (sig * (1.0 + hidden * (1.0 - sig)))
    sums = (fold(d_out), fold(d_msg * normed), fold(d_msg), fold(d_hidden))
    return d_hidden.astype(BF), d_w2, sums


def add_sums(ref, parts):
    for q in range(4):
        total = parts[0][q]
        for other in parts[1:]:
            total = total + other[q]
        ref[mat(q), :] += total


def step_kernel(dims, *refs):
    layers, cols, nodes, edges, npad, eh, dpn = dims
    nch = eh // EC
    top = layers - 1
    n_in = 14
    (node_in, edge_in, gnode_in, gedge_in, send_ids, recv_ids, ew1_in, ew2_in, nw1_in, nw2_in, evec_in, nvec_in, eb1_in, nb1_in) = refs[:n_in]
    n_out = 12
    (node_raw, edge_raw, gnode_raw, gedge_raw, ew1_buf, eb1_buf, ew2_buf, evec_buf, nw1_buf, nb1_buf, nw2_buf, nvec_buf) = refs[n_in:n_in + n_out]
    (w_send, w_recv, n_send, n_recv, gn_send, gn_recv, no_send, no_recv, dn_send, dn_recv,
     e_send, g_send, e_recv, g_recv, eo_recv, de_recv, part, part_recv, hidden, normed, inv, nhid, nnrm, ninv, d_part, s_sum, r_sum,
     ids_raw, bias_cols, sums, grad, core_recv, half, dp_recv, cross_send, cross_recv, own_sum, gathered,
     core_ss, core_rs, dp_ss, dp_rs, cross_ss, cross_rs, load_sem, w_ss, w_rs, n_ss, n_rs, e_ss, e_rs, p_ss, p_rs) = refs[n_in + n_out:]

    t = lax.axis_index('tp')
    p = lax.axis_index('dp')
    per = SLABS // dpn
    dp_others = range(1, dpn)
    x, c = t // 2, lax.rem(t, 2)
    ox, oc = 1 - x, 1 - c
    peer = [t, t + 1 - 2 * c, t + 2 - 4 * x, t + 3 - 2 * c - 4 * x]

    def remote(src, dst, ssem, rsem, d):
        return pltpu.make_async_remote_copy(src_ref=src, dst_ref=dst, send_sem=ssem, recv_sem=rsem,
                                            device_id={'tp': peer[d]}, device_id_type=MESH)

    loads = [pltpu.make_async_copy(src, dst, load_sem.at[q]) for q, (src, dst) in enumerate(
        [(node_in, node_raw), (edge_in, edge_raw), (gnode_in, gnode_raw), (gedge_in, gedge_raw)])]
    for copy in loads:
        copy.start()

    def node_copies(send, recv, kind):
        return (remote(send.at[1], recv.at[0], n_ss.at[kind, 0], n_rs.at[kind, 0], 1),
                remote(send.at[0], recv.at[1], n_ss.at[kind, 1], n_rs.at[kind, 1], 2),
                remote(recv.at[1], recv.at[2], n_ss.at[kind, 2], n_rs.at[kind, 2], 1))

    piece = w_send.shape[0] // dpn

    def weight_rows(owner):
        return pl.ds(pl.multiple_of(owner * piece, 8), piece)

    w_pair = remote(w_send, w_recv.at[0], w_ss.at[0], w_rs.at[0], 1)
    w_cross = remote(w_send.at[weight_rows(p)], w_recv.at[1, weight_rows(p)], w_ss.at[1], w_rs.at[1], 2)
    w_relay = remote(w_recv.at[1], w_recv.at[2], w_ss.at[2], w_rs.at[2], 1)

    def weight_copy(i, owner):
        rows = w_recv.at[1, weight_rows(owner)]
        return dp_remote(rows, rows, 2, 0, i)

    def edge_copy(kind, j, d, width):
        src, dst = ((e_send, e_recv), (g_send, g_recv), (e_send, eo_recv), (g_send, de_recv))[kind]
        place = (slot(d), j) if width == EC else (slot(d), j, slice(None), slice(width))
        return remote(src.at[place], dst.at[place], e_ss.at[kind, slot(d), jnp.where(j == nch - 1, 1, 0)], e_rs.at[kind, slot(d), j], d)

    def edge_do(kind, j, d, action):
        outward = kind in (EDGE_OUT, GRAD_OUT)
        other = oc if d % 2 else c
        half_id = c if outward == (action != 'wait_recv') else other
        narrow = jnp.logical_and(j == nch - 1, half_id == 1)

        @pl.when(jnp.logical_not(narrow))
        def _():
            getattr(edge_copy(kind, j, d, EC), action)()

        @pl.when(narrow)
        def _():
            getattr(edge_copy(kind, j, d, T), action)()

    def edges_sent(kind):
        src, dst = ((e_send, e_recv), (g_send, g_recv), (e_send, eo_recv), (g_send, de_recv))[kind]
        for d in OTHERS:
            most = (slot(d), pl.ds(0, nch - 1))
            remote(src.at[most], dst.at[most], e_ss.at[kind, slot(d), 0], e_rs.at[kind, slot(d), 0], d).wait_send()
            edge_do(kind, nch - 1, d, 'wait_send')

    def core_copy(l, b):
        return remote(grad.at[l, :, pl.ds((2 * b + 1) * cols, cols), :], core_recv.at[l, b], core_ss.at[l, b], core_rs.at[l, b], 1)

    def dp_remote(src, dst, stage, l, i):
        return pltpu.make_async_remote_copy(src_ref=src, dst_ref=dst, send_sem=dp_ss.at[stage, l, i - 1], recv_sem=dp_rs.at[stage, l, i - 1],
                                            device_id={'dp': lax.rem(p + i, dpn)}, device_id_type=MESH)

    def spread_copy(l, i):
        return dp_remote(half.at[l, pl.ds(lax.rem(p + i, dpn) * per, per)], dp_recv.at[l, i - 1], 0, l, i)

    def cross_copy(l):
        return remote(cross_send.at[l], cross_recv.at[l], cross_ss.at[l], cross_rs.at[l], 2)

    def gather_copy(l, i, owner):
        return dp_remote(own_sum.at[l], gathered.at[l, pl.ds(owner * per, per)], 1, l, i)

    def part_copy(q):
        return remote(part.at[q], part_recv.at[q], p_ss.at[q], p_rs.at[q], 1)

    def load_nodes(raw, send, own):
        send[...] = jnp.zeros_like(send)
        send[0, :, :nodes] = raw[ox].astype(F32)
        send[1, :, :nodes] = raw[x].astype(F32)
        own[:cols, :] = send[1].astype(own.dtype)

    def load_edges(raw, send, own, kind):
        def put(j, lanes_j, val_of):
            for d in OTHERS:
                sample = x if d < 2 else ox
                send[slot(d), j] = val_of(sample, oc if d % 2 else c).astype(F32)
            own[:cols, lanes_j] = val_of(x, c)

        def chunk(j):
            put(j, at(j, EC), lambda s, h: raw[s, :, pl.ds(pl.multiple_of(h * eh + j * EC, D), EC)])
            for d in SEND_ORDER:
                edge_do(kind, j, d, 'start')

        loop(nch - 1, chunk)
        first = (nch - 1) * EC
        used = edges - eh - first
        last = pl.ds(first, EC)

        def tail(s, h):
            left = raw[s, :, pl.ds(first, EC)]
            right = beside([raw[s, :, pl.ds(eh + first, used)], jnp.zeros((cols, EC - used), BF)])
            return jnp.where(h == 0, left.astype(F32), right.astype(F32)).astype(BF)

        put(nch - 1, last, tail)
        for d in SEND_ORDER:
            edge_do(kind, nch - 1, d, 'start')

    def place_edges(raw, block, d, j):
        s = x if d < 2 else ox
        h = oc if d % 2 else c
        val = block.astype(BF)
        first = (nch - 1) * EC
        used = edges - eh - first

        @pl.when(jnp.logical_or(j < nch - 1, h == 0))
        def _():
            raw[s, :, pl.ds(pl.multiple_of(h * eh + j * EC, D), EC)] = val

        @pl.when(jnp.logical_and(j == nch - 1, h == 1))
        def _():
            raw[s, :, pl.ds(eh + first, used)] = val[:, :used]

    def scoped(e0, e1, ge, msg, v0, v1, v2, agg0, agg1, d_agg, scol, rcol, srow, rrow, iota, lanes, ew1, ew1t, ew2, ew2t, nw1, nw1t, nw2, nw2t, vecs):
        tables = (v0, v1, v2)
        aggs = (agg0, agg1)
        edges_in = (e0, e1)

        barrier = pltpu.get_barrier_semaphore()
        for d in OTHERS:
            pl.semaphore_signal(barrier, inc=1, device_id={'tp': peer[d]}, device_id_type=MESH)
        for i in dp_others:
            pl.semaphore_signal(barrier, inc=1, device_id={'dp': lax.rem(p + i, dpn)}, device_id_type=MESH)
        loads[0].wait()
        with jax.named_scope('send_nodes'):
            load_nodes(node_raw, n_send, v0)
        ncop = node_copies(n_send, n_recv, 0)
        q = cols
        w_send[:HEAD, :] = jnp.zeros((HEAD, D), F32)
        for k in THREE:
            w_send[k * layers:(k + 1) * layers, :cols] = evec_in[k]
            w_send[(3 + k) * layers:(4 + k) * layers, :cols] = nvec_in[k]
        for l in range(layers):
            off = HEAD + l * LROWS
            w_send[off:off + 3 * q, :] = ew1_in[l * 3 * q:(l + 1) * 3 * q, :].astype(F32)
            w_send[off + 3 * q:off + 4 * q, :] = ew2_in[l * q:(l + 1) * q, :].astype(F32)
            w_send[off + 4 * q:off + 6 * q, :] = nw1_in[l * 2 * q:(l + 1) * 2 * q, :].astype(F32)
            w_send[off + 6 * q:off + 7 * q, :] = nw2_in[l * q:(l + 1) * q, :].astype(F32)
        with jax.named_scope('barrier'):
            pl.semaphore_wait(barrier, len(OTHERS) + dpn - 1)
        w_cross.start()
        w_pair.start()
        ncop[1].start()
        ncop[0].start()
        loads[1].wait()
        with jax.named_scope('send_edges'):
            load_edges(edge_raw, e_send, e0, EDGE_IN)
        loads[2].wait()
        load_nodes(gnode_raw, gn_send, d_part)
        gcop = node_copies(gn_send, gn_recv, 1)
        gcop[1].start()
        gcop[0].start()
        loads[3].wait()
        with jax.named_scope('send_grads'):
            load_edges(gedge_raw, g_send, ge, GRAD_IN)

        w_cross.wait_recv()
        for i in dp_others:
            weight_copy(i, p).start()

        @pl.when(c == 1)
        def _():
            for recv in (e_recv, g_recv):
                recv[:, nch - 1, :, T:] = jnp.zeros((3, cols, EC - T), F32)

        iota[...] = lax.broadcasted_iota(jnp.int32, (T, D), 0).astype(I16)
        lanes[...] = lax.broadcasted_iota(jnp.int32, (16, D), 1).astype(I16)

        ids_raw[...] = jnp.full(ids_raw.shape, -1, jnp.int32)
        for which, src in enumerate((send_ids, recv_ids)):
            ids_raw[which:which + 1, :edges] = src[...].reshape(1, edges)

        def ids(b):
            for which, (row_ref, col_ref) in enumerate(((srow, scol), (rrow, rcol))):
                wide = jnp.broadcast_to(ids_raw[which:which + 1, pl.ds(pl.multiple_of(c * eh + b * D, D), D)], (D, D))
                row_ref[at(b, 16), :] = wide[:16].astype(I16)
                col_ref[at(b, D), :] = flip(wide.astype(F32)).astype(jnp.int32).astype(I16)

        with jax.named_scope('ids'):
            loop(eh // D, ids)

        def keys(ref, step):
            return [ref[pl.ds(pl.multiple_of(step * (KS // D) * 16 + 16 * h, 16), 1), :] for h in range(KS // D)]

        bias_cols[...] = flip(stacked([eb1_in[...], nb1_in[...], jnp.zeros((D - 2 * layers, D), F32)]))

        def join_weights(l):
            off = HEAD + l * LROWS
            for d in range(GROUP):
                src = w_send if d == 0 else w_recv.at[slot(d)]
                r = slice(d * q, (d + 1) * q)
                for k in THREE:
                    ew1[l, k * D + d * q:k * D + (d + 1) * q, :] = src[off + k * q:off + (k + 1) * q, :].astype(BF)
                ew2t[l, r, :] = src[off + 3 * q:off + 4 * q, :].astype(BF)
                for k in range(2):
                    nw1[l, k * D + d * q:k * D + (d + 1) * q, :] = src[off + (4 + k) * q:off + (5 + k) * q, :].astype(BF)
                nw2t[l, r, :] = src[off + 6 * q:off + 7 * q, :].astype(BF)

            def flip_bf(mat):
                return flip(mat.astype(F32)).astype(BF)

            for k in THREE:
                ew1t[l, :, mat(k)] = flip_bf(ew1[l, mat(k), :])
            for k in range(2):
                nw1t[l, :, mat(k)] = flip_bf(nw1[l, mat(k), :])
            ew2[l] = flip_bf(ew2t[l])
            nw2[l] = flip_bf(nw2t[l])

        def wait_recvs(copies):
            copies[1].wait_recv()
            copies[2].start()
            copies[0].wait_recv()
            copies[2].wait_recv()

        with jax.named_scope('node_wait'):
            wait_recvs(ncop)
        for d in OTHERS:
            v0[rows_of(d), :] = n_recv[slot(d)].astype(BF)
        with jax.named_scope('weight_wait'):
            for i in dp_others:
                weight_copy(i, lax.rem(p + dpn - i, dpn)).wait_recv()
            w_relay.start()
            w_pair.wait_recv()
            w_relay.wait_recv()
        rows_all = beside([w_send[:HEAD, :cols]] + [w_recv[d, :HEAD, :cols] for d in range(3)])
        vecs[...] = flip(stacked([rows_all, jnp.zeros((D - HEAD, D), F32)]))
        join_weights(0)

        def vec(l, node):
            first = 6 * node + l
            return [vecs[:, first + 2 * k:first + 2 * k + 1] for k in THREE]

        def bias(l, node):
            return bias_cols[:, node * layers + l:node * layers + l + 1]

        def hidden_of_nodes(l):
            table, b1 = tables[l], bias(l, 0)

            def body(step):
                xs = gather(table, keys(srow, step), iota).astype(BF)
                xr = gather(table, keys(rrow, step), iota).astype(BF)
                hidden[l, :, at(step, KS)] = dot(ew1t[l, :, mat(1, 2)], stacked([xs, xr])) + b1

            loop(eh // KS, body)

        def edge_forward(l):
            e_in = edges_in[l]

            def body(j):
                for sub in range(EC // T):
                    a = at(j * (EC // T) + sub, T)
                    if l == 0:
                        if sub == 0:
                            for d in OTHERS:
                                edge_do(EDGE_IN, j, d, 'wait_recv')
                        for d in OTHERS:
                            e_in[rows_of(d), a] = e_recv[slot(d), j, :, sub * T:(sub + 1) * T].astype(BF)
                    e_val = e_in[:, a]
                    hid = hidden[l, :, a] + dot(ew1t[l, :, mat(0)], e_val)
                    hidden[l, :, a] = hid
                    message, nrm, std = mlp_tail(hid, ew2t[l], vec(l, 0))
                    normed[l, :, a] = nrm
                    inv[l:l + 1, a] = std
                    msg[:, a] = message
                    e_new = (e_val.astype(F32) + message.astype(F32)).astype(BF)
                    if l < top:
                        edges_in[l + 1][:, a] = e_new
                    else:
                        for d in OTHERS:
                            e_send[slot(d), j, :, sub * T:(sub + 1) * T] = e_new[rows_of(d)].astype(F32)
                        if sub == 0:
                            own_parts = []
                        own_parts.append(e_new[:q])
                if l == top:
                    for d in SEND_ORDER:
                        edge_do(EDGE_OUT, j, d, 'start')
                    place_edges(edge_raw, beside(own_parts), 0, j)

            loop(nch, body)

        def segment_sum(acc, ids_ref):
            acc[...] = jnp.zeros(acc.shape, F32)

            def body(step):
                scatter(acc, msg[:, at(step, KS)], ids_ref[at(step, KS), :], lanes)

            loop(eh // KS, body)

        def node_forward(l):
            table, agg, out = tables[l], aggs[l], tables[l + 1]

            def body(step):
                a = pl.ds(pl.multiple_of(step * TN, D), TN)
                v_in = table[:, a]
                agg_bf = (part[l, :, a] + swap_halves(part_recv[l, :, a])).astype(BF)
                agg[:, a] = agg_bf
                hid = dot(nw1t[l], stacked([v_in, agg_bf])) + bias(l, 1)
                nhid[l, :, a] = hid
                message, nrm, std = mlp_tail(hid, nw2t[l], vec(l, 1))
                nnrm[l, :, a] = nrm
                ninv[l:l + 1, a] = std
                out[:, a] = (v_in.astype(F32) + message.astype(F32)).astype(BF)

            loop(npad // TN, body)

        for l in range(layers):
            with jax.named_scope(f'gather_{l}'):
                hidden_of_nodes(l)
            if l == top:
                edges_sent(EDGE_IN)
            with jax.named_scope(f'edge_forward_{l}'):
                edge_forward(l)
            with jax.named_scope(f'sum_{l}'):
                segment_sum(part.at[l], rcol)
            part_copy(l).start()
            if l == 0:
                join_weights(1)
                gcop[1].wait_recv()
                gcop[2].start()
            with jax.named_scope(f'part_wait_{l}'):
                part_copy(l).wait_recv()
            with jax.named_scope(f'node_forward_{l}'):
                node_forward(l)
        no_send[...] = tables[layers][2 * q:3 * q, :].astype(F32)
        no_copy = remote(no_send, no_recv, n_ss.at[2, 0], n_rs.at[2, 0], 2)
        no_copy.start()
        node_raw[x] = tables[layers][:q, :nodes]

        hold = nch - 3
        grad[...] = jnp.zeros_like(grad)
        sums[...] = jnp.zeros_like(sums)
        with jax.named_scope('grad_node_wait'):
            gcop[0].wait_recv()
            gcop[2].wait_recv()
        for d in OTHERS:
            d_part[rows_of(d), :] = gn_recv[slot(d)]

        def node_backward(l):
            table, agg = tables[l], aggs[l]

            def body(step):
                a = pl.ds(pl.multiple_of(step * TN, D), TN)
                d_in = d_part[:, a]
                if l < top:
                    d_in = d_in + part[layers + l + 1, :, a] + swap_halves(part_recv[layers + l + 1, :, a])
                    d_in = d_in.astype(BF).astype(F32)
                d_hid, d_w2, parts = mlp_back(d_in, nhid[l, :, a], nnrm[l, :, a], ninv[l:l + 1, a], nw2[l], vec(l, 1))
                add_sums(sums.at[l, 1], [parts])
                grad[l, 6] += d_w2
                grad[l, 4] += dot_nt(table[:, a], d_hid)
                grad[l, 5] += dot_nt(agg[:, a], d_hid)
                d_part[:, a] = d_in + dot(nw1[l, mat(0), :], d_hid)
                d_agg[:, a] = dot(nw1[l, mat(1), :], d_hid).astype(BF)

            loop(npad // TN, body)

        def gather_back():
            def body(step):
                msg[:, at(step, KS)] = gather(d_agg, keys(rrow, step), iota).astype(BF)

            loop(eh // KS, body)

        def edge_backward(l):
            e_in = edges_in[l]

            def body(j):
                all_parts, d_w2s, d_w1s, own_parts = [], [], [], []
                for sub in range(EC // T):
                    a = at(j * (EC // T) + sub, T)
                    if l == top:
                        if sub == 0:
                            for d in OTHERS:
                                edge_do(GRAD_IN, j, d, 'wait_recv')
                        for d in OTHERS:
                            ge[rows_of(d), a] = g_recv[slot(d), j, :, sub * T:(sub + 1) * T].astype(BF)
                    d_res = ge[:, a].astype(F32)
                    d_msg = d_res + msg[:, a].astype(F32)
                    d_hid, d_w2, parts = mlp_back(d_msg, hidden[l, :, a], normed[l, :, a], inv[l:l + 1, a], ew2[l], vec(l, 0))
                    all_parts.append(parts)
                    d_w2s.append(d_w2)
                    d_w1s.append(dot_nt(e_in[:, a], d_hid))
                    msg[:, a] = d_hid
                    d_new = (d_res + dot(ew1[l, mat(0), :], d_hid)).astype(BF)
                    if l > 0:
                        ge[:, a] = d_new
                    else:
                        for d in OTHERS:
                            g_send[slot(d), j, :, sub * T:(sub + 1) * T] = d_new[rows_of(d)].astype(F32)
                        own_parts.append(d_new[:q])
                add_sums(sums.at[l, 0], all_parts)
                grad[l, 3] += sum(d_w2s[1:], d_w2s[0])
                grad[l, 0] += sum(d_w1s[1:], d_w1s[0])
                if l == 0:
                    @pl.when(j < hold)
                    def _():
                        for d in SEND_ORDER:
                            edge_do(GRAD_OUT, j, d, 'start')
                    place_edges(gedge_raw, beside(own_parts), 0, j)

            loop(nch, body)

        def reduce_start(l):
            def total(node, k):
                return column_sum(flip(sums[l, node, mat(k), :]))

            lat = stacked([total(node, k) for node in BOTH for k in THREE])
            biases = stacked([total(node, 3) for node in BOTH])
            n_lat = lat.shape[0]
            for d in range(GROUP):
                grad[l, SLABS - 1, d * cols:d * cols + n_lat, :cols] = lat[:, rows_of(d)]
                grad[l, SLABS - 1, d * cols + n_lat:d * cols + n_lat + 2, :] = biases
            for b in BOTH:
                core_copy(l, b).start()

        def chip_sum(l):
            row = lax.broadcasted_iota(jnp.int32, (cols, D), 0)
            edge_row = jnp.logical_or(row < 3, row == 6)
            for b in BOTH:
                core_copy(l, b).wait_recv()
                for k in range(SLABS):
                    own = grad[l, k, rows_of(2 * b), :]
                    if k < 4:
                        own = own + core_recv[l, b, k]
                    elif k == SLABS - 1:
                        own = own + jnp.where(edge_row, core_recv[l, b, k], 0.0)
                    half[l, k, b] = own
            for i in dp_others:
                spread_copy(l, i).start()

        def dp_sum(l):
            total = half[l, pl.ds(p * per, per)]
            for i in dp_others:
                spread_copy(l, i).wait_recv()
                total = total + dp_recv[l, i - 1]
            own_sum[l] = total[:, 0]
            cross_send[l] = total[:, 1]
            cross_copy(l).start()

        def cross_sum(l):
            cross_copy(l).wait_recv()
            total = own_sum[l] + cross_recv[l]
            own_sum[l] = total
            gathered[l, pl.ds(p * per, per)] = total
            for i in dp_others:
                gather_copy(l, i, p).start()

        def project(l):
            table = tables[l]

            def body(step):
                a = pl.ds(pl.multiple_of(step * TN, D), TN)
                s_bf, r_bf, v_in = s_sum[:, a].astype(BF), r_sum[:, a].astype(BF), table[:, a]
                part[layers + l, :, a] = dot(ew1[l, mat(1), :], s_bf) + dot(ew1[l, mat(2), :], r_bf)
                grad[l, 1] += dot_nt(v_in, s_bf)
                grad[l, 2] += dot_nt(v_in, r_bf)

            loop(npad // TN, body)

        for l in reversed(range(layers)):
            with jax.named_scope(f'node_backward_{l}'):
                node_backward(l)
            if l < top:
                with jax.named_scope('chip_sum_1'):
                    chip_sum(l + 1)
            with jax.named_scope(f'gather_back_{l}'):
                gather_back()
            if l == 0:
                edges_sent(GRAD_IN)
            with jax.named_scope(f'edge_backward_{l}'):
                edge_backward(l)
            if l < top:
                with jax.named_scope('dp_sum_1'):
                    dp_sum(l + 1)
            with jax.named_scope(f'sum_send_{l}'):
                segment_sum(s_sum, scol)
            with jax.named_scope(f'sum_recv_{l}'):
                segment_sum(r_sum, rcol)
            with jax.named_scope(f'project_{l}'):
                project(l)
            part_copy(layers + l).start()
            with jax.named_scope(f'reduce_start_{l}'):
                reduce_start(l)
            with jax.named_scope(f'back_wait_{l}'):
                part_copy(layers + l).wait_recv()

        def final(step):
            a = pl.ds(pl.multiple_of(step * TN, D), TN)
            d_in = (d_part[:, a] + part[layers, :, a] + swap_halves(part_recv[layers, :, a])).astype(BF)
            v2[:, a] = d_in

        loop(npad // TN, final)
        dn_send[...] = v2[2 * q:3 * q, :].astype(F32)
        dn_copy = remote(dn_send, dn_recv, n_ss.at[2, 1], n_rs.at[2, 1], 2)
        dn_copy.start()
        gnode_raw[x] = v2[:q, :nodes]
        with jax.named_scope('chip_sum_0'):
            chip_sum(0)

        with jax.named_scope('node_out_wait'):
            no_copy.wait_recv()
        node_raw[ox] = no_recv[:, :nodes].astype(BF)

        def place_e(j):
            for d in OTHERS:
                edge_do(EDGE_OUT, j, d, 'wait_recv')
                place_edges(edge_raw, eo_recv[slot(d), j], d, j)

        with jax.named_scope('place_edge_out'):
            loop(nch, place_e)
        with jax.named_scope('dp_sum_0'):
            dp_sum(0)

        def send_rest(j):
            for d in SEND_ORDER:
                edge_do(GRAD_OUT, j, d, 'start')

        loop(nch, send_rest, hold)

        def place_g(j):
            for d in OTHERS:
                edge_do(GRAD_OUT, j, d, 'wait_recv')
                place_edges(gedge_raw, de_recv[slot(d), j], d, j)

        with jax.named_scope('place_first'):
            loop(hold, place_g)
        for l in range(layers):
            with jax.named_scope(f'cross_sum_{l}'):
                cross_sum(l)
        with jax.named_scope('d_node_wait'):
            dn_copy.wait_recv()
        gnode_raw[ox] = dn_recv[:, :nodes].astype(BF)
        with jax.named_scope('place_rest'):
            loop(nch - 1, place_g, hold)
        for l in range(layers):
            for i in dp_others:
                gather_copy(l, i, lax.rem(p + dpn - i, dpn)).wait_recv()
            ew1_buf[l] = gathered[l, 0:3]
            ew2_buf[l] = gathered[l, 3]
            nw1_buf[l] = gathered[l, 4:6]
            nw2_buf[l] = gathered[l, 6]
            small = gathered[l, SLABS - 1]
            for k in THREE:
                evec_buf[k, l:l + 1, :] = small[k:k + 1, :cols]
                nvec_buf[k, l:l + 1, :] = small[3 + k:4 + k, :cols]
            eb1_buf[l:l + 1, :] = small[6:7]
            nb1_buf[l:l + 1, :] = small[7:8]
        for l in range(layers):
            for b in BOTH:
                core_copy(l, b).wait_send()
            cross_copy(l).wait_send()
            for i in dp_others:
                spread_copy(l, i).wait_send()
                gather_copy(l, i, p).wait_send()
        for copy in ncop + gcop + (w_pair, w_cross, w_relay):
            copy.wait_send()
        for i in dp_others:
            weight_copy(i, p).wait_send()
        no_copy.wait_send()
        dn_copy.wait_send()
        for k in range(2 * layers):
            part_copy(k).wait_send()
        edges_sent(EDGE_OUT)
        with jax.named_scope('place_last'):
            loop(nch, place_g, nch - 1)
        edges_sent(GRAD_OUT)

    bf = lambda *s: pltpu.VMEM(s, BF)
    pl.run_scoped(
        scoped, bf(D, eh), bf(D, eh), bf(D, eh), bf(D, eh), bf(D, npad), bf(D, npad), bf(D, npad), bf(D, npad), bf(D, npad), bf(D, npad),
        pltpu.VMEM((eh, D), I16), pltpu.VMEM((eh, D), I16), pltpu.VMEM((eh // D * 16, D), I16), pltpu.VMEM((eh // D * 16, D), I16),
        pltpu.VMEM((T, D), I16), pltpu.VMEM((16, D), I16),
        bf(layers, 3 * D, D), bf(layers, D, 3 * D), bf(layers, D, D), bf(layers, D, D),
        bf(layers, 2 * D, D), bf(layers, D, 2 * D), bf(layers, D, D), bf(layers, D, D), pltpu.VMEM((D, D), F32))


def finish_kernel(*refs):
    count = len(refs) // 2
    sem = refs[-1]
    puts = [pltpu.make_async_copy(refs[k], refs[count + k], sem.at[k]) for k in range(count)]
    for put in puts:
        put.start()
    for put in puts:
        put.wait()


def keep_in_vmem(val):
    return pltpu.with_memory_space_constraint(val, pltpu.VMEM)


def finish(arrays):
    return pl.pallas_call(
        finish_kernel,
        name='finish',
        out_shape=[jax.ShapeDtypeStruct(a.shape, a.dtype) for a in arrays],
        in_specs=[VM] * len(arrays),
        out_specs=[HB] * len(arrays),
        scratch_shapes=[pltpu.SemaphoreType.DMA((len(arrays),))],
        compiler_params=pltpu.CompilerParams(vmem_limit_bytes=1 << 20),
    )(*[keep_in_vmem(a) for a in arrays])


def solution(mesh):
    lat_spec = P('dp', None, 'tp')
    first_spec = P(None, None, 'tp', None)
    col_spec = P(None, None, 'tp')
    param_specs = (first_spec, P(), col_spec, col_spec, first_spec, P(), col_spec, col_spec)
    in_specs = (lat_spec, lat_spec, P(), P(), lat_spec, lat_spec) + param_specs
    out_specs = (lat_spec, lat_spec, lat_spec, lat_spec) + param_specs
    shape = jax.ShapeDtypeStruct

    def local_step(node_lat, edge_lat, senders, receivers, grad_node, grad_edge, edge_w1, edge_b1, edge_w2, edge_vec, node_w1, node_b1, node_w2, node_vec):
        layers = edge_w1.shape[0]
        cols = node_lat.shape[2]
        nodes, edges = node_lat.shape[1], edge_lat.shape[1]
        npad = -(-nodes // TN) * TN
        eh = -(-edges // (2 * EC)) * EC
        nch = eh // EC
        dpn = mesh.shape['dp']
        per = SLABS // dpn
        dims = (layers, cols, nodes, edges, npad, eh, dpn)
        flat = lambda arr: jnp.swapaxes(arr, 1, 2)
        lead = lambda arr: jnp.transpose(arr, (1, 0, 2))
        args = (flat(node_lat), flat(edge_lat), flat(grad_node), flat(grad_edge), senders, receivers,
                edge_w1.reshape(-1, D), flat(edge_w2).reshape(-1, D), node_w1.reshape(-1, D), flat(node_w2).reshape(-1, D),
                lead(edge_vec), lead(node_vec), edge_b1, node_b1)
        vm, sem = pltpu.VMEM, pltpu.SemaphoreType.DMA
        wrows = -(-(HEAD + layers * LROWS) // (8 * dpn)) * 8 * dpn
        lat_n, lat_e = (2, cols, nodes), (2, cols, edges)
        outs = [RESULT(lat_n, BF), RESULT(lat_e, BF), RESULT(lat_n, BF), RESULT(lat_e, BF),
                RESULT((layers, 3, cols, D), F32), RESULT((layers, D), F32), RESULT((layers, cols, D), F32), RESULT((3, layers, cols), F32),
                RESULT((layers, 2, cols, D), F32), RESULT((layers, D), F32), RESULT((layers, cols, D), F32), RESULT((3, layers, cols), F32)]
        scratch = [
            vm((wrows, D), F32), vm((3, wrows, D), F32),
            vm((2, cols, npad), F32), vm((3, cols, npad), F32), vm((2, cols, npad), F32), vm((3, cols, npad), F32),
            vm((cols, npad), F32), vm((cols, npad), F32), vm((cols, npad), F32), vm((cols, npad), F32),
            *[vm((3, nch, cols, EC), F32)] * 6,
            vm((2 * layers, D, npad), F32), vm((2 * layers, D, npad), F32),
            vm((layers, D, eh), F32), vm((layers, D, eh), F32), vm((8, eh), F32),
            vm((layers, D, npad), F32), vm((layers, D, npad), F32), vm((8, npad), F32),
            vm((D, npad), F32), vm((D, npad), F32), vm((D, npad), F32), vm((8, 2 * eh), jnp.int32), vm((D, D), F32), vm((layers, 2, 4 * D, D), F32),
            vm((layers, SLABS, D, D), F32), vm((layers, 2, SLABS, cols, D), F32), vm((layers, SLABS, 2, cols, D), F32),
            vm((layers, dpn - 1, per, 2, cols, D), F32), vm((layers, per, cols, D), F32), vm((layers, per, cols, D), F32),
            vm((layers, per, cols, D), F32), vm((layers, SLABS, cols, D), F32),
            sem((layers, 2)), sem((layers, 2)), sem((3, layers, dpn - 1)), sem((3, layers, dpn - 1)), sem((layers,)), sem((layers,)),
            sem((4,)), sem((3,)), sem((3,)), sem((3, 3)), sem((3, 3)), sem((4, 3, 2)), sem((4, 3, nch)),
            sem((2 * layers,)), sem((2 * layers,))]
        res = pl.pallas_call(
            lambda *refs: step_kernel(dims, *refs),
            name='graph_step',
            out_shape=outs,
            in_specs=[HB] * 4 + [VM] * 10,
            out_specs=[VM] * len(outs),
            scratch_shapes=scratch,
            compiler_params=pltpu.CompilerParams(collective_id=0, has_side_effects=True, vmem_limit_bytes=VMEM_LIMIT),
        )(*args)

        res = finish(res)
        return (flat(res[0]), flat(res[1]), flat(res[2]), flat(res[3]),
                res[4], res[5], flat(res[6]), lead(res[7]), res[8], res[9], flat(res[10]), lead(res[11]))

    return jax.shard_map(local_step, mesh=mesh, in_specs=in_specs, out_specs=out_specs, check_vma=False)
```

```python
import jax
import jax.numpy as jnp
from jax import lax
from jax.experimental import pallas as pl
from jax.experimental.pallas import tpu as pltpu
from jax.sharding import PartitionSpec as P

LN_EPS = 1e-5
D = 128
T = 256
TN = 384
EC = 512
KS = 1408
BF = jnp.bfloat16
F32 = jnp.float32
I16 = jnp.int16
MESH = pl.DeviceIdType.MESH
VM = pl.BlockSpec(memory_space=pltpu.VMEM)
HB = pl.BlockSpec(memory_space=pl.ANY)
RESULT = pltpu.VMEM
GROUP = 4
BOTH = (0, 1)
THREE = (0, 1, 2)
OTHERS = (1, 2, 3)
EDGE_IN, GRAD_IN, EDGE_OUT, GRAD_OUT = range(4)
SEND_ORDER = (2, 3, 1)
LROWS = 7 * (D // 4)
HEAD = 16
LEADER = GROUP - 1
VMEM_LIMIT = 63_000_000
SLABS = 8


def dot(a, b):
    return jnp.dot(a, b, preferred_element_type=F32)


def dot_nt(a, b):
    return lax.dot_general(a, b, (((1,), (1,)), ((), ())), preferred_element_type=F32)


def mat(k, n=1):
    return slice(k * D, (k + n) * D)


def rows_of(d):
    q = D // 4
    return slice(d * q, (d + 1) * q)


def at(step, width):
    return pl.ds(pl.multiple_of(step * width, width), width)


def loop(stop, body, start=0):
    def step(j, carry):
        body(j)
        return carry

    lax.fori_loop(start, stop, step, 0)


def column_sum(val):
    return jnp.sum(val, axis=0, keepdims=True)


def flip(val):
    return jnp.swapaxes(val, 0, 1)


def stacked(parts):
    return jnp.concatenate(parts, axis=0)


def beside(parts):
    return jnp.concatenate(parts, axis=1)


def slot(d):
    return d - 1


def sigmoid(hidden):
    return 1.0 / (1.0 + jnp.exp(-hidden))


def fold(val):
    total = val[:, mat(0)]
    for start in range(D, val.shape[1], D):
        total = total + val[:, start:start + D]
    return total


def swap_halves(val):
    return stacked([val[rows_of(d)] for d in (1, 0, 3, 2)])


def gather(table, keys, iota):
    acc = None
    nodes = table.shape[1]
    one, zero = jnp.ones((), BF), jnp.zeros((), BF)
    for base in range(0, nodes, T):
        width = min(T, nodes - base)
        ids = iota[0:width, :]
        hot = beside([jnp.where(ids == (key - jnp.asarray(base, I16)), one, zero) for key in keys])
        part = dot(table[:, base:base + width], hot)
        acc = part if acc is None else acc + part
    return acc


def scatter(acc_ref, val, cols, lanes):
    nodes = acc_ref.shape[1]
    one, zero = jnp.ones((), BF), jnp.zeros((), BF)
    row = lanes[0:1, :]
    for base in range(0, nodes, T):
        width = min(T, nodes - base)
        hot = beside([jnp.where((row + jnp.asarray(base + s, I16)) == cols, one, zero) for s in range(0, width, D)])
        acc_ref[:, base:base + width] += dot(val, hot)


def mlp_tail(hidden, w2t, vec):
    act = (hidden * sigmoid(hidden)).astype(BF)
    out = dot(w2t, act) + vec[0]
    mean = column_sum(out) / D
    centered = out - mean
    var = column_sum(centered * centered) / D
    inv = lax.rsqrt(var + LN_EPS)
    normed = centered * inv
    message = (normed * vec[1] + vec[2]).astype(BF)
    return message, normed, inv


def mlp_back(d_msg, hidden, normed, inv, w2, vec):
    d_normed = d_msg * vec[1]
    mean0 = column_sum(d_normed) / D
    mean1 = column_sum(d_normed * normed) / D
    d_out = inv * (d_normed - mean0 - normed * mean1)
    d_out_bf = d_out.astype(BF)
    sig = sigmoid(hidden)
    act = (hidden * sig).astype(BF)
    d_w2 = dot_nt(d_out_bf, act)
    d_hidden = dot(w2, d_out_bf) * (sig * (1.0 + hidden * (1.0 - sig)))
    sums = (fold(d_out), fold(d_msg * normed), fold(d_msg), fold(d_hidden))
    return d_hidden.astype(BF), d_w2, sums


def add_sums(ref, parts):
    for q in range(4):
        total = parts[0][q]
        for other in parts[1:]:
            total = total + other[q]
        ref[mat(q), :] += total


def step_kernel(dims, *refs):
    layers, cols, nodes, edges, npad, eh, dpn = dims
    nch = eh // EC
    top = layers - 1
    n_in = 14
    hbm_in = refs[:n_in]
    n_out = 12
    (node_raw, edge_raw, gnode_raw, gedge_raw, ew1_buf, eb1_buf, ew2_buf, evec_buf, nw1_buf, nb1_buf, nw2_buf, nvec_buf) = refs[n_in:n_in + n_out]
    (send_ids, recv_ids, ew1_in, ew2_in, nw1_in, nw2_in, evec_in, nvec_in, eb1_in, nb1_in, w_send, w_recv, n_send, n_recv, gn_send, gn_recv, no_send, no_recv, dn_send, dn_recv,
     e_send, g_send, e_recv, g_recv, eo_recv, de_recv, part, part_recv, hidden, normed, inv, nhid, nnrm, ninv, d_part, s_sum, r_sum,
     ids_raw, bias_cols, sums, grad, core_recv, half, dp_recv, cross_send, cross_recv, own_sum, gathered,
     core_ss, core_rs, dp_ss, dp_rs, cross_ss, cross_rs, load_sem, w_ss, w_rs, n_ss, n_rs, e_ss, e_rs, p_ss, p_rs, ready) = refs[n_in + n_out:]

    t = lax.axis_index('tp')
    p = lax.axis_index('dp')
    per = SLABS // dpn
    dp_others = range(1, dpn)
    x, c = t // 2, lax.rem(t, 2)
    ox, oc = 1 - x, 1 - c
    peer = [t, t + 1 - 2 * c, t + 2 - 4 * x, t + 3 - 2 * c - 4 * x]

    def remote(src, dst, ssem, rsem, d):
        return pltpu.make_async_remote_copy(src_ref=src, dst_ref=dst, send_sem=ssem, recv_sem=rsem,
                                            device_id={'tp': peer[d]}, device_id_type=MESH)

    small_in = (send_ids, recv_ids, ew1_in, ew2_in, nw1_in, nw2_in, evec_in, nvec_in, eb1_in, nb1_in)
    loads = [pltpu.make_async_copy(src, dst, load_sem.at[q]) for q, (src, dst) in enumerate(
        zip(hbm_in, (node_raw, edge_raw, gnode_raw, gedge_raw) + small_in))]

    def node_copies(send, recv, kind):
        return (remote(send.at[1], recv.at[0], n_ss.at[kind, 0], n_rs.at[kind, 0], 1),
                remote(send.at[0], recv.at[1], n_ss.at[kind, 1], n_rs.at[kind, 1], 2),
                remote(recv.at[1], recv.at[2], n_ss.at[kind, 2], n_rs.at[kind, 2], 1))

    piece = w_send.shape[0] // dpn

    def weight_rows(owner):
        return pl.ds(pl.multiple_of(owner * piece, 8), piece)

    w_pair = remote(w_send, w_recv.at[0], w_ss.at[0], w_rs.at[0], 1)
    w_cross = remote(w_send.at[weight_rows(p)], w_recv.at[1, weight_rows(p)], w_ss.at[1], w_rs.at[1], 2)
    w_relay = remote(w_recv.at[1], w_recv.at[2], w_ss.at[2], w_rs.at[2], 1)

    def weight_copy(i, owner):
        rows = w_recv.at[1, weight_rows(owner)]
        return dp_remote(rows, rows, 2, 0, i)

    def edge_copy(kind, j, d, width):
        src, dst = ((e_send, e_recv), (g_send, g_recv), (e_send, eo_recv), (g_send, de_recv))[kind]
        place = (slot(d), j) if width == EC else (slot(d), j, slice(None), slice(width))
        return remote(src.at[place], dst.at[place], e_ss.at[kind, slot(d), jnp.where(j == nch - 1, 1, 0)], e_rs.at[kind, slot(d), j], d)

    def edge_do(kind, j, d, action):
        outward = kind in (EDGE_OUT, GRAD_OUT)
        other = oc if d % 2 else c
        half_id = c if outward == (action != 'wait_recv') else other
        narrow = jnp.logical_and(j == nch - 1, half_id == 1)

        @pl.when(jnp.logical_not(narrow))
        def _():
            getattr(edge_copy(kind, j, d, EC), action)()

        @pl.when(narrow)
        def _():
            getattr(edge_copy(kind, j, d, T), action)()

    def edges_sent(kind):
        src, dst = ((e_send, e_recv), (g_send, g_recv), (e_send, eo_recv), (g_send, de_recv))[kind]
        for d in OTHERS:
            most = (slot(d), pl.ds(0, nch - 1))
            remote(src.at[most], dst.at[most], e_ss.at[kind, slot(d), 0], e_rs.at[kind, slot(d), 0], d).wait_send()
            edge_do(kind, nch - 1, d, 'wait_send')

    def core_copy(l, b):
        return remote(grad.at[l, :, pl.ds((2 * b + 1) * cols, cols), :], core_recv.at[l, b], core_ss.at[l, b], core_rs.at[l, b], 1)

    def dp_remote(src, dst, stage, l, i):
        return pltpu.make_async_remote_copy(src_ref=src, dst_ref=dst, send_sem=dp_ss.at[stage, l, i - 1], recv_sem=dp_rs.at[stage, l, i - 1],
                                            device_id={'dp': lax.rem(p + i, dpn)}, device_id_type=MESH)

    def spread_copy(l, i):
        return dp_remote(half.at[l, pl.ds(lax.rem(p + i, dpn) * per, per)], dp_recv.at[l, i - 1], 0, l, i)

    def cross_copy(l):
        return remote(cross_send.at[l], cross_recv.at[l], cross_ss.at[l], cross_rs.at[l], 2)

    def gather_copy(l, i, owner):
        return dp_remote(own_sum.at[l], gathered.at[l, pl.ds(owner * per, per)], 1, l, i)

    def part_copy(q):
        return remote(part.at[q], part_recv.at[q], p_ss.at[q], p_rs.at[q], 1)

    def load_nodes(raw, send, own):
        send[...] = jnp.zeros_like(send)
        send[0, :, :nodes] = raw[ox].astype(F32)
        send[1, :, :nodes] = raw[x].astype(F32)
        own[:cols, :] = send[1].astype(own.dtype)

    def load_edges(raw, send, own, kind):
        def put(j, lanes_j, val_of):
            for d in OTHERS:
                sample = x if d < 2 else ox
                send[slot(d), j] = val_of(sample, oc if d % 2 else c).astype(F32)
            own[:cols, lanes_j] = val_of(x, c)

        def chunk(j):
            put(j, at(j, EC), lambda s, h: raw[s, :, pl.ds(pl.multiple_of(h * eh + j * EC, D), EC)])
            for d in SEND_ORDER:
                edge_do(kind, j, d, 'start')

        loop(nch - 1, chunk)
        first = (nch - 1) * EC
        used = edges - eh - first
        last = pl.ds(first, EC)

        def tail(s, h):
            left = raw[s, :, pl.ds(first, EC)]
            right = beside([raw[s, :, pl.ds(eh + first, used)], jnp.zeros((cols, EC - used), BF)])
            return jnp.where(h == 0, left.astype(F32), right.astype(F32)).astype(BF)

        put(nch - 1, last, tail)
        for d in SEND_ORDER:
            edge_do(kind, nch - 1, d, 'start')

    def place_edges(raw, block, d, j):
        s = x if d < 2 else ox
        h = oc if d % 2 else c
        val = block.astype(BF)
        first = (nch - 1) * EC
        used = edges - eh - first

        @pl.when(jnp.logical_or(j < nch - 1, h == 0))
        def _():
            raw[s, :, pl.ds(pl.multiple_of(h * eh + j * EC, D), EC)] = val

        @pl.when(jnp.logical_and(j == nch - 1, h == 1))
        def _():
            raw[s, :, pl.ds(eh + first, used)] = val[:, :used]

    def scoped(e0, e1, ge, msg, v0, v1, v2, agg0, agg1, d_agg, scol, rcol, srow, rrow, iota, lanes, ew1, ew1t, ew2, ew2t, nw1, nw1t, nw2, nw2t, vecs):
        tables = (v0, v1, v2)
        aggs = (agg0, agg1)
        edges_in = (e0, e1)

        barrier = pltpu.get_barrier_semaphore()
        for d in OTHERS:
            pl.semaphore_signal(barrier, inc=1, device_id={'tp': peer[d]}, device_id_type=MESH)
        for copy in loads[:1] + loads[4:] + loads[1:4]:
            copy.start()
        loads[0].wait()
        with jax.named_scope('send_nodes'):
            load_nodes(node_raw, n_send, v0)
        ncop = node_copies(n_send, n_recv, 0)
        for copy in loads[4:]:
            copy.wait()
        q = cols
        w_send[:HEAD, :] = jnp.zeros((HEAD, D), F32)
        for k in THREE:
            w_send[k * layers:(k + 1) * layers, :cols] = evec_in[k]
            w_send[(3 + k) * layers:(4 + k) * layers, :cols] = nvec_in[k]
        for l in range(layers):
            off = HEAD + l * LROWS
            w_send[off:off + 3 * q, :] = ew1_in[l * 3 * q:(l + 1) * 3 * q, :].astype(F32)
            w_send[off + 3 * q:off + 4 * q, :] = ew2_in[l * q:(l + 1) * q, :].astype(F32)
            w_send[off + 4 * q:off + 6 * q, :] = nw1_in[l * 2 * q:(l + 1) * 2 * q, :].astype(F32)
            w_send[off + 6 * q:off + 7 * q, :] = nw2_in[l * q:(l + 1) * q, :].astype(F32)
        with jax.named_scope('barrier'):
            @pl.when(t != LEADER)
            def _():
                pl.semaphore_wait(barrier, len(OTHERS))
                pl.semaphore_signal(ready, inc=1, device_id={'tp': LEADER}, device_id_type=MESH)

            @pl.when(t == LEADER)
            def _():
                pl.semaphore_wait(ready, len(OTHERS))
                for i in dp_others:
                    pl.semaphore_signal(barrier, inc=1, device_id={'dp': lax.rem(p + i, dpn)}, device_id_type=MESH)

        w_cross.start()
        w_pair.start()
        ncop[1].start()
        ncop[0].start()
        loads[1].wait()
        with jax.named_scope('send_edges'):
            load_edges(edge_raw, e_send, e0, EDGE_IN)
        loads[2].wait()
        load_nodes(gnode_raw, gn_send, d_part)
        gcop = node_copies(gn_send, gn_recv, 1)
        gcop[1].start()
        gcop[0].start()
        loads[3].wait()
        with jax.named_scope('send_grads'):
            load_edges(gedge_raw, g_send, ge, GRAD_IN)

        with jax.named_scope('dp_barrier'):
            @pl.when(t == LEADER)
            def _():
                pl.semaphore_wait(barrier, len(OTHERS) + dpn - 1)
                for d in OTHERS:
                    pl.semaphore_signal(ready, inc=1, device_id={'tp': peer[d]}, device_id_type=MESH)

            @pl.when(t != LEADER)
            def _():
                pl.semaphore_wait(ready, 1)

        w_cross.wait_recv()
        for i in dp_others:
            weight_copy(i, p).start()

        @pl.when(c == 1)
        def _():
            for recv in (e_recv, g_recv):
                recv[:, nch - 1, :, T:] = jnp.zeros((3, cols, EC - T), F32)

        iota[...] = lax.broadcasted_iota(jnp.int32, (T, D), 0).astype(I16)
        lanes[...] = lax.broadcasted_iota(jnp.int32, (16, D), 1).astype(I16)

        ids_raw[...] = jnp.full(ids_raw.shape, -1, jnp.int32)
        for which, src in enumerate((send_ids, recv_ids)):
            ids_raw[which:which + 1, :edges] = src[...].reshape(1, edges)

        def ids(b):
            for which, (row_ref, col_ref) in enumerate(((srow, scol), (rrow, rcol))):
                wide = jnp.broadcast_to(ids_raw[which:which + 1, pl.ds(pl.multiple_of(c * eh + b * D, D), D)], (D, D))
                row_ref[at(b, 16), :] = wide[:16].astype(I16)
                col_ref[at(b, D), :] = flip(wide.astype(F32)).astype(jnp.int32).astype(I16)

        with jax.named_scope('ids'):
            loop(eh // D, ids)

        def keys(ref, step):
            return [ref[pl.ds(pl.multiple_of(step * (KS // D) * 16 + 16 * h, 16), 1), :] for h in range(KS // D)]

        bias_cols[...] = flip(stacked([eb1_in[...], nb1_in[...], jnp.zeros((D - 2 * layers, D), F32)]))

        def join_weights(l):
            off = HEAD + l * LROWS
            for d in range(GROUP):
                src = w_send if d == 0 else w_recv.at[slot(d)]
                r = slice(d * q, (d + 1) * q)
                for k in THREE:
                    ew1[l, k * D + d * q:k * D + (d + 1) * q, :] = src[off + k * q:off + (k + 1) * q, :].astype(BF)
                ew2t[l, r, :] = src[off + 3 * q:off + 4 * q, :].astype(BF)
                for k in range(2):
                    nw1[l, k * D + d * q:k * D + (d + 1) * q, :] = src[off + (4 + k) * q:off + (5 + k) * q, :].astype(BF)
                nw2t[l, r, :] = src[off + 6 * q:off + 7 * q, :].astype(BF)

            def flip_bf(mat):
                return flip(mat.astype(F32)).astype(BF)

            for k in THREE:
                ew1t[l, :, mat(k)] = flip_bf(ew1[l, mat(k), :])
            for k in range(2):
                nw1t[l, :, mat(k)] = flip_bf(nw1[l, mat(k), :])
            ew2[l] = flip_bf(ew2t[l])
            nw2[l] = flip_bf(nw2t[l])

        def wait_recvs(copies):
            copies[1].wait_recv()
            copies[2].start()
            copies[0].wait_recv()
            copies[2].wait_recv()

        with jax.named_scope('node_wait'):
            wait_recvs(ncop)
        for d in OTHERS:
            v0[rows_of(d), :] = n_recv[slot(d)].astype(BF)
        with jax.named_scope('weight_wait'):
            for i in dp_others:
                weight_copy(i, lax.rem(p + dpn - i, dpn)).wait_recv()
            w_relay.start()
            w_pair.wait_recv()
            w_relay.wait_recv()
        rows_all = beside([w_send[:HEAD, :cols]] + [w_recv[d, :HEAD, :cols] for d in range(3)])
        vecs[...] = flip(stacked([rows_all, jnp.zeros((D - HEAD, D), F32)]))
        join_weights(0)

        def vec(l, node):
            first = 6 * node + l
            return [vecs[:, first + 2 * k:first + 2 * k + 1] for k in THREE]

        def bias(l, node):
            return bias_cols[:, node * layers + l:node * layers + l + 1]

        def hidden_of_nodes(l):
            table, b1 = tables[l], bias(l, 0)

            def body(step):
                xs = gather(table, keys(srow, step), iota).astype(BF)
                xr = gather(table, keys(rrow, step), iota).astype(BF)
                hidden[l, :, at(step, KS)] = dot(ew1t[l, :, mat(1, 2)], stacked([xs, xr])) + b1

            loop(eh // KS, body)

        def edge_forward(l):
            e_in = edges_in[l]

            def body(j):
                for sub in range(EC // T):
                    a = at(j * (EC // T) + sub, T)
                    if l == 0:
                        if sub == 0:
                            for d in OTHERS:
                                edge_do(EDGE_IN, j, d, 'wait_recv')
                        for d in OTHERS:
                            e_in[rows_of(d), a] = e_recv[slot(d), j, :, sub * T:(sub + 1) * T].astype(BF)
                    e_val = e_in[:, a]
                    hid = hidden[l, :, a] + dot(ew1t[l, :, mat(0)], e_val)
                    hidden[l, :, a] = hid
                    message, nrm, std = mlp_tail(hid, ew2t[l], vec(l, 0))
                    normed[l, :, a] = nrm
                    inv[l:l + 1, a] = std
                    msg[:, a] = message
                    e_new = (e_val.astype(F32) + message.astype(F32)).astype(BF)
                    if l < top:
                        edges_in[l + 1][:, a] = e_new
                    else:
                        for d in OTHERS:
                            e_send[slot(d), j, :, sub * T:(sub + 1) * T] = e_new[rows_of(d)].astype(F32)
                        if sub == 0:
                            own_parts = []
                        own_parts.append(e_new[:q])
                if l == top:
                    for d in SEND_ORDER:
                        edge_do(EDGE_OUT, j, d, 'start')
                    place_edges(edge_raw, beside(own_parts), 0, j)

            loop(nch, body)

        def segment_sum(acc, ids_ref):
            acc[...] = jnp.zeros(acc.shape, F32)

            def body(step):
                scatter(acc, msg[:, at(step, KS)], ids_ref[at(step, KS), :], lanes)

            loop(eh // KS, body)

        def node_forward(l):
            table, agg, out = tables[l], aggs[l], tables[l + 1]

            def body(step):
                a = pl.ds(pl.multiple_of(step * TN, D), TN)
                v_in = table[:, a]
                agg_bf = (part[l, :, a] + swap_halves(part_recv[l, :, a])).astype(BF)
                agg[:, a] = agg_bf
                hid = dot(nw1t[l], stacked([v_in, agg_bf])) + bias(l, 1)
                nhid[l, :, a] = hid
                message, nrm, std = mlp_tail(hid, nw2t[l], vec(l, 1))
                nnrm[l, :, a] = nrm
                ninv[l:l + 1, a] = std
                out[:, a] = (v_in.astype(F32) + message.astype(F32)).astype(BF)

            loop(npad // TN, body)

        for l in range(layers):
            with jax.named_scope(f'gather_{l}'):
                hidden_of_nodes(l)
            if l == top:
                edges_sent(EDGE_IN)
            with jax.named_scope(f'edge_forward_{l}'):
                edge_forward(l)
            with jax.named_scope(f'sum_{l}'):
                segment_sum(part.at[l], rcol)
            part_copy(l).start()
            if l == 0:
                join_weights(1)
                gcop[1].wait_recv()
                gcop[2].start()
            with jax.named_scope(f'part_wait_{l}'):
                part_copy(l).wait_recv()
            with jax.named_scope(f'node_forward_{l}'):
                node_forward(l)
        no_send[...] = tables[layers][2 * q:3 * q, :].astype(F32)
        no_copy = remote(no_send, no_recv, n_ss.at[2, 0], n_rs.at[2, 0], 2)
        no_copy.start()
        node_raw[x] = tables[layers][:q, :nodes]

        hold = nch - 3
        grad[...] = jnp.zeros_like(grad)
        sums[...] = jnp.zeros_like(sums)
        with jax.named_scope('grad_node_wait'):
            gcop[0].wait_recv()
            gcop[2].wait_recv()
        for d in OTHERS:
            d_part[rows_of(d), :] = gn_recv[slot(d)]

        def node_backward(l):
            table, agg = tables[l], aggs[l]

            def body(step):
                a = pl.ds(pl.multiple_of(step * TN, D), TN)
                d_in = d_part[:, a]
                if l < top:
                    d_in = d_in + part[layers + l + 1, :, a] + swap_halves(part_recv[layers + l + 1, :, a])
                    d_in = d_in.astype(BF).astype(F32)
                d_hid, d_w2, parts = mlp_back(d_in, nhid[l, :, a], nnrm[l, :, a], ninv[l:l + 1, a], nw2[l], vec(l, 1))
                add_sums(sums.at[l, 1], [parts])
                grad[l, 6] += d_w2
                grad[l, 4] += dot_nt(table[:, a], d_hid)
                grad[l, 5] += dot_nt(agg[:, a], d_hid)
                d_part[:, a] = d_in + dot(nw1[l, mat(0), :], d_hid)
                d_agg[:, a] = dot(nw1[l, mat(1), :], d_hid).astype(BF)

            loop(npad // TN, body)

        def gather_back():
            def body(step):
                msg[:, at(step, KS)] = gather(d_agg, keys(rrow, step), iota).astype(BF)

            loop(eh // KS, body)

        def edge_backward(l):
            e_in = edges_in[l]

            def body(j):
                all_parts, d_w2s, d_w1s, own_parts = [], [], [], []
                for sub in range(EC // T):
                    a = at(j * (EC // T) + sub, T)
                    if l == top:
                        if sub == 0:
                            for d in OTHERS:
                                edge_do(GRAD_IN, j, d, 'wait_recv')
                        for d in OTHERS:
                            ge[rows_of(d), a] = g_recv[slot(d), j, :, sub * T:(sub + 1) * T].astype(BF)
                    d_res = ge[:, a].astype(F32)
                    d_msg = d_res + msg[:, a].astype(F32)
                    d_hid, d_w2, parts = mlp_back(d_msg, hidden[l, :, a], normed[l, :, a], inv[l:l + 1, a], ew2[l], vec(l, 0))
                    all_parts.append(parts)
                    d_w2s.append(d_w2)
                    d_w1s.append(dot_nt(e_in[:, a], d_hid))
                    msg[:, a] = d_hid
                    d_new = (d_res + dot(ew1[l, mat(0), :], d_hid)).astype(BF)
                    if l > 0:
                        ge[:, a] = d_new
                    else:
                        for d in OTHERS:
                            g_send[slot(d), j, :, sub * T:(sub + 1) * T] = d_new[rows_of(d)].astype(F32)
                        own_parts.append(d_new[:q])
                add_sums(sums.at[l, 0], all_parts)
                grad[l, 3] += sum(d_w2s[1:], d_w2s[0])
                grad[l, 0] += sum(d_w1s[1:], d_w1s[0])
                if l == 0:
                    @pl.when(j < hold)
                    def _():
                        for d in SEND_ORDER:
                            edge_do(GRAD_OUT, j, d, 'start')
                    place_edges(gedge_raw, beside(own_parts), 0, j)

            loop(nch, body)

        def reduce_start(l):
            def total(node, k):
                return column_sum(flip(sums[l, node, mat(k), :]))

            lat = stacked([total(node, k) for node in BOTH for k in THREE])
            biases = stacked([total(node, 3) for node in BOTH])
            n_lat = lat.shape[0]
            for d in range(GROUP):
                grad[l, SLABS - 1, d * cols:d * cols + n_lat, :cols] = lat[:, rows_of(d)]
                grad[l, SLABS - 1, d * cols + n_lat:d * cols + n_lat + 2, :] = biases
            for b in BOTH:
                core_copy(l, b).start()

        def chip_sum(l):
            row = lax.broadcasted_iota(jnp.int32, (cols, D), 0)
            edge_row = jnp.logical_or(row < 3, row == 6)
            for b in BOTH:
                core_copy(l, b).wait_recv()
                for k in range(SLABS):
                    own = grad[l, k, rows_of(2 * b), :]
                    if k < 4:
                        own = own + core_recv[l, b, k]
                    elif k == SLABS - 1:
                        own = own + jnp.where(edge_row, core_recv[l, b, k], 0.0)
                    half[l, k, b] = own
            for i in dp_others:
                spread_copy(l, i).start()

        def dp_sum(l):
            total = half[l, pl.ds(p * per, per)]
            for i in dp_others:
                spread_copy(l, i).wait_recv()
                total = total + dp_recv[l, i - 1]
            own_sum[l] = total[:, 0]
            cross_send[l] = total[:, 1]
            cross_copy(l).start()

        def cross_sum(l):
            cross_copy(l).wait_recv()
            total = own_sum[l] + cross_recv[l]
            own_sum[l] = total
            gathered[l, pl.ds(p * per, per)] = total
            for i in dp_others:
                gather_copy(l, i, p).start()

        def project(l):
            table = tables[l]

            def body(step):
                a = pl.ds(pl.multiple_of(step * TN, D), TN)
                s_bf, r_bf, v_in = s_sum[:, a].astype(BF), r_sum[:, a].astype(BF), table[:, a]
                part[layers + l, :, a] = dot(ew1[l, mat(1), :], s_bf) + dot(ew1[l, mat(2), :], r_bf)
                grad[l, 1] += dot_nt(v_in, s_bf)
                grad[l, 2] += dot_nt(v_in, r_bf)

            loop(npad // TN, body)

        for l in reversed(range(layers)):
            with jax.named_scope(f'node_backward_{l}'):
                node_backward(l)
            if l < top:
                with jax.named_scope('chip_sum_1'):
                    chip_sum(l + 1)
            with jax.named_scope(f'gather_back_{l}'):
                gather_back()
            if l == 0:
                edges_sent(GRAD_IN)
            with jax.named_scope(f'edge_backward_{l}'):
                edge_backward(l)
            if l < top:
                with jax.named_scope('dp_sum_1'):
                    dp_sum(l + 1)
            with jax.named_scope(f'sum_send_{l}'):
                segment_sum(s_sum, scol)
            with jax.named_scope(f'sum_recv_{l}'):
                segment_sum(r_sum, rcol)
            with jax.named_scope(f'project_{l}'):
                project(l)
            part_copy(layers + l).start()
            with jax.named_scope(f'reduce_start_{l}'):
                reduce_start(l)
            with jax.named_scope(f'back_wait_{l}'):
                part_copy(layers + l).wait_recv()

        def final(step):
            a = pl.ds(pl.multiple_of(step * TN, D), TN)
            d_in = (d_part[:, a] + part[layers, :, a] + swap_halves(part_recv[layers, :, a])).astype(BF)
            v2[:, a] = d_in

        loop(npad // TN, final)
        dn_send[...] = v2[2 * q:3 * q, :].astype(F32)
        dn_copy = remote(dn_send, dn_recv, n_ss.at[2, 1], n_rs.at[2, 1], 2)
        dn_copy.start()
        gnode_raw[x] = v2[:q, :nodes]
        with jax.named_scope('chip_sum_0'):
            chip_sum(0)

        with jax.named_scope('node_out_wait'):
            no_copy.wait_recv()
        node_raw[ox] = no_recv[:, :nodes].astype(BF)

        def place_e(j):
            for d in OTHERS:
                edge_do(EDGE_OUT, j, d, 'wait_recv')
                place_edges(edge_raw, eo_recv[slot(d), j], d, j)

        with jax.named_scope('place_edge_out'):
            loop(nch, place_e)
        with jax.named_scope('dp_sum_0'):
            dp_sum(0)

        def send_rest(j):
            for d in SEND_ORDER:
                edge_do(GRAD_OUT, j, d, 'start')

        loop(nch, send_rest, hold)

        def place_g(j):
            for d in OTHERS:
                edge_do(GRAD_OUT, j, d, 'wait_recv')
                place_edges(gedge_raw, de_recv[slot(d), j], d, j)

        with jax.named_scope('place_first'):
            loop(hold, place_g)
        for l in range(layers):
            with jax.named_scope(f'cross_sum_{l}'):
                cross_sum(l)
        with jax.named_scope('d_node_wait'):
            dn_copy.wait_recv()
        gnode_raw[ox] = dn_recv[:, :nodes].astype(BF)
        with jax.named_scope('place_rest'):
            loop(nch - 1, place_g, hold)
        for l in range(layers):
            for i in dp_others:
                gather_copy(l, i, lax.rem(p + dpn - i, dpn)).wait_recv()
            ew1_buf[l] = gathered[l, 0:3]
            ew2_buf[l] = gathered[l, 3]
            nw1_buf[l] = gathered[l, 4:6]
            nw2_buf[l] = gathered[l, 6]
            small = gathered[l, SLABS - 1]
            for k in THREE:
                evec_buf[k, l:l + 1, :] = small[k:k + 1, :cols]
                nvec_buf[k, l:l + 1, :] = small[3 + k:4 + k, :cols]
            eb1_buf[l:l + 1, :] = small[6:7]
            nb1_buf[l:l + 1, :] = small[7:8]
        for l in range(layers):
            for b in BOTH:
                core_copy(l, b).wait_send()
            cross_copy(l).wait_send()
            for i in dp_others:
                spread_copy(l, i).wait_send()
                gather_copy(l, i, p).wait_send()
        for copy in ncop + gcop + (w_pair, w_cross, w_relay):
            copy.wait_send()
        for i in dp_others:
            weight_copy(i, p).wait_send()
        no_copy.wait_send()
        dn_copy.wait_send()
        for k in range(2 * layers):
            part_copy(k).wait_send()
        edges_sent(EDGE_OUT)
        with jax.named_scope('place_last'):
            loop(nch, place_g, nch - 1)
        edges_sent(GRAD_OUT)

    bf = lambda *s: pltpu.VMEM(s, BF)
    pl.run_scoped(
        scoped, bf(D, eh), bf(D, eh), bf(D, eh), bf(D, eh), bf(D, npad), bf(D, npad), bf(D, npad), bf(D, npad), bf(D, npad), bf(D, npad),
        pltpu.VMEM((eh, D), I16), pltpu.VMEM((eh, D), I16), pltpu.VMEM((eh // D * 16, D), I16), pltpu.VMEM((eh // D * 16, D), I16),
        pltpu.VMEM((T, D), I16), pltpu.VMEM((16, D), I16),
        bf(layers, 3 * D, D), bf(layers, D, 3 * D), bf(layers, D, D), bf(layers, D, D),
        bf(layers, 2 * D, D), bf(layers, D, 2 * D), bf(layers, D, D), bf(layers, D, D), pltpu.VMEM((D, D), F32))


def finish_kernel(*refs):
    count = len(refs) // 2
    sem = refs[-1]
    puts = [pltpu.make_async_copy(refs[k], refs[count + k], sem.at[k]) for k in range(count)]
    for put in puts:
        put.start()
    for put in puts:
        put.wait()


def keep_in_vmem(val):
    return pltpu.with_memory_space_constraint(val, pltpu.VMEM)


def finish(arrays):
    return pl.pallas_call(
        finish_kernel,
        name='finish',
        out_shape=[jax.ShapeDtypeStruct(a.shape, a.dtype) for a in arrays],
        in_specs=[VM] * len(arrays),
        out_specs=[HB] * len(arrays),
        scratch_shapes=[pltpu.SemaphoreType.DMA((len(arrays),))],
        compiler_params=pltpu.CompilerParams(vmem_limit_bytes=1 << 20),
    )(*[keep_in_vmem(a) for a in arrays])


def solution(mesh):
    lat_spec = P('dp', None, 'tp')
    first_spec = P(None, None, 'tp', None)
    col_spec = P(None, None, 'tp')
    param_specs = (first_spec, P(), col_spec, col_spec, first_spec, P(), col_spec, col_spec)
    in_specs = (lat_spec, lat_spec, P(), P(), lat_spec, lat_spec) + param_specs
    out_specs = (lat_spec, lat_spec, lat_spec, lat_spec) + param_specs
    shape = jax.ShapeDtypeStruct

    def local_step(node_lat, edge_lat, senders, receivers, grad_node, grad_edge, edge_w1, edge_b1, edge_w2, edge_vec, node_w1, node_b1, node_w2, node_vec):
        layers = edge_w1.shape[0]
        cols = node_lat.shape[2]
        nodes, edges = node_lat.shape[1], edge_lat.shape[1]
        npad = -(-nodes // TN) * TN
        eh = -(-edges // (2 * EC)) * EC
        nch = eh // EC
        dpn = mesh.shape['dp']
        per = SLABS // dpn
        dims = (layers, cols, nodes, edges, npad, eh, dpn)
        flat = lambda arr: jnp.swapaxes(arr, 1, 2)
        lead = lambda arr: jnp.transpose(arr, (1, 0, 2))
        args = (flat(node_lat), flat(edge_lat), flat(grad_node), flat(grad_edge), senders, receivers,
                edge_w1.reshape(-1, D), flat(edge_w2).reshape(-1, D), node_w1.reshape(-1, D), flat(node_w2).reshape(-1, D),
                lead(edge_vec), lead(node_vec), edge_b1, node_b1)
        vm, sem = pltpu.VMEM, pltpu.SemaphoreType.DMA
        wrows = -(-(HEAD + layers * LROWS) // (8 * dpn)) * 8 * dpn
        lat_n, lat_e = (2, cols, nodes), (2, cols, edges)
        outs = [RESULT(lat_n, BF), RESULT(lat_e, BF), RESULT(lat_n, BF), RESULT(lat_e, BF),
                RESULT((layers, 3, cols, D), F32), RESULT((layers, D), F32), RESULT((layers, cols, D), F32), RESULT((3, layers, cols), F32),
                RESULT((layers, 2, cols, D), F32), RESULT((layers, D), F32), RESULT((layers, cols, D), F32), RESULT((3, layers, cols), F32)]
        scratch = [
            *[vm(a.shape, a.dtype) for a in args[4:]], vm((wrows, D), F32), vm((3, wrows, D), F32),
            vm((2, cols, npad), F32), vm((3, cols, npad), F32), vm((2, cols, npad), F32), vm((3, cols, npad), F32),
            vm((cols, npad), F32), vm((cols, npad), F32), vm((cols, npad), F32), vm((cols, npad), F32),
            *[vm((3, nch, cols, EC), F32)] * 6,
            vm((2 * layers, D, npad), F32), vm((2 * layers, D, npad), F32),
            vm((layers, D, eh), F32), vm((layers, D, eh), F32), vm((8, eh), F32),
            vm((layers, D, npad), F32), vm((layers, D, npad), F32), vm((8, npad), F32),
            vm((D, npad), F32), vm((D, npad), F32), vm((D, npad), F32), vm((8, 2 * eh), jnp.int32), vm((D, D), F32), vm((layers, 2, 4 * D, D), F32),
            vm((layers, SLABS, D, D), F32), vm((layers, 2, SLABS, cols, D), F32), vm((layers, SLABS, 2, cols, D), F32),
            vm((layers, dpn - 1, per, 2, cols, D), F32), vm((layers, per, cols, D), F32), vm((layers, per, cols, D), F32),
            vm((layers, per, cols, D), F32), vm((layers, SLABS, cols, D), F32),
            sem((layers, 2)), sem((layers, 2)), sem((3, layers, dpn - 1)), sem((3, layers, dpn - 1)), sem((layers,)), sem((layers,)),
            sem((len(args),)), sem((3,)), sem((3,)), sem((3, 3)), sem((3, 3)), sem((4, 3, 2)), sem((4, 3, nch)),
            sem((2 * layers,)), sem((2 * layers,)), pltpu.SemaphoreType.REGULAR]
        res = pl.pallas_call(
            lambda *refs: step_kernel(dims, *refs),
            name='graph_step',
            out_shape=outs,
            in_specs=[HB] * len(args),
            out_specs=[VM] * len(outs),
            scratch_shapes=scratch,
            compiler_params=pltpu.CompilerParams(collective_id=0, has_side_effects=True, vmem_limit_bytes=VMEM_LIMIT),
        )(*args)

        res = finish(res)
        return (flat(res[0]), flat(res[1]), flat(res[2]), flat(res[3]),
                res[4], res[5], flat(res[6]), lead(res[7]), res[8], res[9], flat(res[10]), lead(res[11]))

    return jax.shard_map(local_step, mesh=mesh, in_specs=in_specs, out_specs=out_specs, check_vma=False)
```

```python
import jax
import jax.numpy as jnp
from jax import lax
from jax.experimental import pallas as pl
from jax.experimental.pallas import tpu as pltpu
from jax.sharding import PartitionSpec as P

LN_EPS = 1e-5
D = 128
T = 256
TN = 384
EC = 512
KS = 1408
BF = jnp.bfloat16
F32 = jnp.float32
I16 = jnp.int16
MESH = pl.DeviceIdType.MESH
VM = pl.BlockSpec(memory_space=pltpu.VMEM)
HB = pl.BlockSpec(memory_space=pl.ANY)
RESULT = pltpu.VMEM
GROUP = 4
BOTH = (0, 1)
THREE = (0, 1, 2)
OTHERS = (1, 2, 3)
EDGE_IN, GRAD_IN, EDGE_OUT, GRAD_OUT = range(4)
SEND_ORDER = (2, 3, 1)
LROWS = 7 * (D // 4)
HEAD = 16
LEADER = GROUP - 1
VMEM_LIMIT = 63_000_000
SLABS = 8
EARLY = 6
VEC_SLAB = 5
EDGE_SLABS = (0, 1, 6, 7)
STAGES = (slice(0, EARLY), slice(EARLY, SLABS))


def dot(a, b):
    return jnp.dot(a, b, preferred_element_type=F32)


def dot_nt(a, b):
    return lax.dot_general(a, b, (((1,), (1,)), ((), ())), preferred_element_type=F32)


def mat(k, n=1):
    return slice(k * D, (k + n) * D)


def rows_of(d):
    q = D // 4
    return slice(d * q, (d + 1) * q)


def at(step, width):
    return pl.ds(pl.multiple_of(step * width, width), width)


def loop(stop, body, start=0):
    def step(j, carry):
        body(j)
        return carry

    lax.fori_loop(start, stop, step, 0)


def column_sum(val):
    return jnp.sum(val, axis=0, keepdims=True)


def flip(val):
    return jnp.swapaxes(val, 0, 1)


def stacked(parts):
    return jnp.concatenate(parts, axis=0)


def beside(parts):
    return jnp.concatenate(parts, axis=1)


def slot(d):
    return d - 1


def sigmoid(hidden):
    return 1.0 / (1.0 + jnp.exp(-hidden))


def fold(val):
    total = val[:, mat(0)]
    for start in range(D, val.shape[1], D):
        total = total + val[:, start:start + D]
    return total


def swap_halves(val):
    return stacked([val[rows_of(d)] for d in (1, 0, 3, 2)])


def gather(table, keys, iota):
    acc = None
    nodes = table.shape[1]
    one, zero = jnp.ones((), BF), jnp.zeros((), BF)
    for base in range(0, nodes, T):
        width = min(T, nodes - base)
        ids = iota[0:width, :]
        hot = beside([jnp.where(ids == (key - jnp.asarray(base, I16)), one, zero) for key in keys])
        part = dot(table[:, base:base + width], hot)
        acc = part if acc is None else acc + part
    return acc


def scatter(acc_ref, val, cols, lanes):
    nodes = acc_ref.shape[1]
    one, zero = jnp.ones((), BF), jnp.zeros((), BF)
    row = lanes[0:1, :]
    for base in range(0, nodes, T):
        width = min(T, nodes - base)
        hot = beside([jnp.where((row + jnp.asarray(base + s, I16)) == cols, one, zero) for s in range(0, width, D)])
        acc_ref[:, base:base + width] += dot(val, hot)


def mlp_tail(hidden, w2t, vec):
    act = (hidden * sigmoid(hidden)).astype(BF)
    out = dot(w2t, act) + vec[0]
    mean = column_sum(out) / D
    centered = out - mean
    var = column_sum(centered * centered) / D
    inv = lax.rsqrt(var + LN_EPS)
    normed = centered * inv
    message = (normed * vec[1] + vec[2]).astype(BF)
    return message, normed, inv


def mlp_back(d_msg, hidden, normed, inv, w2, vec):
    d_normed = d_msg * vec[1]
    mean0 = column_sum(d_normed) / D
    mean1 = column_sum(d_normed * normed) / D
    d_out = inv * (d_normed - mean0 - normed * mean1)
    d_out_bf = d_out.astype(BF)
    sig = sigmoid(hidden)
    act = (hidden * sig).astype(BF)
    d_w2 = dot_nt(d_out_bf, act)
    d_hidden = dot(w2, d_out_bf) * (sig * (1.0 + hidden * (1.0 - sig)))
    sums = (fold(d_out), fold(d_msg * normed), fold(d_msg), fold(d_hidden))
    return d_hidden.astype(BF), d_w2, sums


def add_sums(ref, parts):
    for q in range(4):
        total = parts[0][q]
        for other in parts[1:]:
            total = total + other[q]
        ref[mat(q), :] += total


def step_kernel(dims, *refs):
    layers, cols, nodes, edges, npad, eh, dpn = dims
    nch = eh // EC
    top = layers - 1
    n_in = 14
    hbm_in = refs[:n_in]
    n_out = 12
    (node_raw, edge_raw, gnode_raw, gedge_raw, ew1_buf, eb1_buf, ew2_buf, evec_buf, nw1_buf, nb1_buf, nw2_buf, nvec_buf) = refs[n_in:n_in + n_out]
    (send_ids, recv_ids, ew1_in, ew2_in, nw1_in, nw2_in, evec_in, nvec_in, eb1_in, nb1_in, w_send, w_recv, n_send, n_recv, gn_send, gn_recv, no_send, no_recv, dn_send, dn_recv,
     e_send, g_send, e_recv, g_recv, eo_recv, de_recv, part, part_recv, hidden, normed, inv, nhid, nnrm, ninv, d_part, s_sum, r_sum,
     ids_raw, bias_cols, sums, grad, core_recv, half, dp_recv, cross_send, cross_recv, own_sum, gathered,
     core_ss, core_rs, dp_ss, dp_rs, cross_ss, cross_rs, load_sem, w_ss, w_rs, n_ss, n_rs, e_ss, e_rs, p_ss, p_rs, ready) = refs[n_in + n_out:]

    t = lax.axis_index('tp')
    p = lax.axis_index('dp')
    per = SLABS // dpn
    dp_others = range(1, dpn)
    x, c = t // 2, lax.rem(t, 2)
    ox, oc = 1 - x, 1 - c
    peer = [t, t + 1 - 2 * c, t + 2 - 4 * x, t + 3 - 2 * c - 4 * x]

    def remote(src, dst, ssem, rsem, d):
        return pltpu.make_async_remote_copy(src_ref=src, dst_ref=dst, send_sem=ssem, recv_sem=rsem,
                                            device_id={'tp': peer[d]}, device_id_type=MESH)

    small_in = (send_ids, recv_ids, ew1_in, ew2_in, nw1_in, nw2_in, evec_in, nvec_in, eb1_in, nb1_in)
    loads = [pltpu.make_async_copy(src, dst, load_sem.at[q]) for q, (src, dst) in enumerate(
        zip(hbm_in, (node_raw, edge_raw, gnode_raw, gedge_raw) + small_in))]

    def node_copies(send, recv, kind):
        return (remote(send.at[1], recv.at[0], n_ss.at[kind, 0], n_rs.at[kind, 0], 1),
                remote(send.at[0], recv.at[1], n_ss.at[kind, 1], n_rs.at[kind, 1], 2),
                remote(recv.at[1], recv.at[2], n_ss.at[kind, 2], n_rs.at[kind, 2], 1))

    piece = w_send.shape[0] // dpn

    def weight_rows(owner):
        return pl.ds(pl.multiple_of(owner * piece, 8), piece)

    w_pair = remote(w_send, w_recv.at[0], w_ss.at[0], w_rs.at[0], 1)
    w_cross = remote(w_send.at[weight_rows(p)], w_recv.at[1, weight_rows(p)], w_ss.at[1], w_rs.at[1], 2)
    w_relay = remote(w_recv.at[1], w_recv.at[2], w_ss.at[2], w_rs.at[2], 1)

    def weight_copy(i, owner):
        rows = w_recv.at[1, weight_rows(owner)]
        return dp_remote(rows, rows, 2, 0, i)

    def edge_copy(kind, j, d, width):
        src, dst = ((e_send, e_recv), (g_send, g_recv), (e_send, eo_recv), (g_send, de_recv))[kind]
        place = (slot(d), j) if width == EC else (slot(d), j, slice(None), slice(width))
        return remote(src.at[place], dst.at[place], e_ss.at[kind, slot(d), jnp.where(j == nch - 1, 1, 0)], e_rs.at[kind, slot(d), j], d)

    def edge_do(kind, j, d, action):
        outward = kind in (EDGE_OUT, GRAD_OUT)
        other = oc if d % 2 else c
        half_id = c if outward == (action != 'wait_recv') else other
        narrow = jnp.logical_and(j == nch - 1, half_id == 1)

        @pl.when(jnp.logical_not(narrow))
        def _():
            getattr(edge_copy(kind, j, d, EC), action)()

        @pl.when(narrow)
        def _():
            getattr(edge_copy(kind, j, d, T), action)()

    def edges_sent(kind):
        src, dst = ((e_send, e_recv), (g_send, g_recv), (e_send, eo_recv), (g_send, de_recv))[kind]
        for d in OTHERS:
            most = (slot(d), pl.ds(0, nch - 1))
            remote(src.at[most], dst.at[most], e_ss.at[kind, slot(d), 0], e_rs.at[kind, slot(d), 0], d).wait_send()
            edge_do(kind, nch - 1, d, 'wait_send')

    def core_copy(l, b, stage):
        first, count = ((0, EARLY), (EARLY, SLABS - EARLY))[stage]
        return remote(grad.at[l, pl.ds(first, count), pl.ds((2 * b + 1) * cols, cols), :], core_recv.at[l, b, pl.ds(first, count)],
                      core_ss.at[l, b, stage], core_rs.at[l, b, stage], 1)

    def in_stage(device, stage):
        early = (device + 1) * per <= EARLY
        return jnp.logical_not(early) if stage else early

    def dp_remote(src, dst, stage, l, i):
        return pltpu.make_async_remote_copy(src_ref=src, dst_ref=dst, send_sem=dp_ss.at[stage, l, i - 1], recv_sem=dp_rs.at[stage, l, i - 1],
                                            device_id={'dp': lax.rem(p + i, dpn)}, device_id_type=MESH)

    def spread_copy(l, i):
        return dp_remote(half.at[l, pl.ds(lax.rem(p + i, dpn) * per, per)], dp_recv.at[l, i - 1], 0, l, i)

    def cross_copy(l):
        return remote(cross_send.at[l], cross_recv.at[l], cross_ss.at[l], cross_rs.at[l], 2)

    def gather_copy(l, i, owner):
        return dp_remote(own_sum.at[l], gathered.at[l, pl.ds(owner * per, per)], 1, l, i)

    def part_copy(q):
        return remote(part.at[q], part_recv.at[q], p_ss.at[q], p_rs.at[q], 1)

    def load_nodes(raw, send, own):
        send[...] = jnp.zeros_like(send)
        send[0, :, :nodes] = raw[ox].astype(F32)
        send[1, :, :nodes] = raw[x].astype(F32)
        own[:cols, :] = send[1].astype(own.dtype)

    def load_edges(raw, send, own, kind):
        def put(j, lanes_j, val_of):
            for d in OTHERS:
                sample = x if d < 2 else ox
                send[slot(d), j] = val_of(sample, oc if d % 2 else c).astype(F32)
            own[:cols, lanes_j] = val_of(x, c)

        def chunk(j):
            put(j, at(j, EC), lambda s, h: raw[s, :, pl.ds(pl.multiple_of(h * eh + j * EC, D), EC)])
            for d in SEND_ORDER:
                edge_do(kind, j, d, 'start')

        loop(nch - 1, chunk)
        first = (nch - 1) * EC
        used = edges - eh - first
        last = pl.ds(first, EC)

        def tail(s, h):
            left = raw[s, :, pl.ds(first, EC)]
            right = beside([raw[s, :, pl.ds(eh + first, used)], jnp.zeros((cols, EC - used), BF)])
            return jnp.where(h == 0, left.astype(F32), right.astype(F32)).astype(BF)

        put(nch - 1, last, tail)
        for d in SEND_ORDER:
            edge_do(kind, nch - 1, d, 'start')

    def place_edges(raw, block, d, j):
        s = x if d < 2 else ox
        h = oc if d % 2 else c
        val = block.astype(BF)
        first = (nch - 1) * EC
        used = edges - eh - first

        @pl.when(jnp.logical_or(j < nch - 1, h == 0))
        def _():
            raw[s, :, pl.ds(pl.multiple_of(h * eh + j * EC, D), EC)] = val

        @pl.when(jnp.logical_and(j == nch - 1, h == 1))
        def _():
            raw[s, :, pl.ds(eh + first, used)] = val[:, :used]

    def scoped(e0, e1, ge, msg, v0, v1, v2, agg0, agg1, d_agg, scol, rcol, srow, rrow, iota, lanes, ew1, ew1t, ew2, ew2t, nw1, nw1t, nw2, nw2t, vecs):
        tables = (v0, v1, v2)
        aggs = (agg0, agg1)
        edges_in = (e0, e1)

        barrier = pltpu.get_barrier_semaphore()
        for d in OTHERS:
            pl.semaphore_signal(barrier, inc=1, device_id={'tp': peer[d]}, device_id_type=MESH)
        for copy in loads[:1] + loads[4:] + loads[1:4]:
            copy.start()
        loads[0].wait()
        with jax.named_scope('send_nodes'):
            load_nodes(node_raw, n_send, v0)
        ncop = node_copies(n_send, n_recv, 0)
        for copy in loads[4:]:
            copy.wait()
        q = cols
        w_send[:HEAD, :] = jnp.zeros((HEAD, D), F32)
        for k in THREE:
            w_send[k * layers:(k + 1) * layers, :cols] = evec_in[k]
            w_send[(3 + k) * layers:(4 + k) * layers, :cols] = nvec_in[k]
        for l in range(layers):
            off = HEAD + l * LROWS
            w_send[off:off + 3 * q, :] = ew1_in[l * 3 * q:(l + 1) * 3 * q, :].astype(F32)
            w_send[off + 3 * q:off + 4 * q, :] = ew2_in[l * q:(l + 1) * q, :].astype(F32)
            w_send[off + 4 * q:off + 6 * q, :] = nw1_in[l * 2 * q:(l + 1) * 2 * q, :].astype(F32)
            w_send[off + 6 * q:off + 7 * q, :] = nw2_in[l * q:(l + 1) * q, :].astype(F32)
        with jax.named_scope('barrier'):
            @pl.when(t != LEADER)
            def _():
                pl.semaphore_wait(barrier, len(OTHERS))
                pl.semaphore_signal(ready, inc=1, device_id={'tp': LEADER}, device_id_type=MESH)

            @pl.when(t == LEADER)
            def _():
                pl.semaphore_wait(ready, len(OTHERS))
                for i in dp_others:
                    pl.semaphore_signal(barrier, inc=1, device_id={'dp': lax.rem(p + i, dpn)}, device_id_type=MESH)

        w_cross.start()
        w_pair.start()
        ncop[1].start()
        ncop[0].start()
        loads[1].wait()
        with jax.named_scope('send_edges'):
            load_edges(edge_raw, e_send, e0, EDGE_IN)
        loads[2].wait()
        load_nodes(gnode_raw, gn_send, d_part)
        gcop = node_copies(gn_send, gn_recv, 1)
        gcop[1].start()
        gcop[0].start()
        loads[3].wait()
        with jax.named_scope('send_grads'):
            load_edges(gedge_raw, g_send, ge, GRAD_IN)

        with jax.named_scope('dp_barrier'):
            @pl.when(t == LEADER)
            def _():
                pl.semaphore_wait(barrier, len(OTHERS) + dpn - 1)
                for d in OTHERS:
                    pl.semaphore_signal(ready, inc=1, device_id={'tp': peer[d]}, device_id_type=MESH)

            @pl.when(t != LEADER)
            def _():
                pl.semaphore_wait(ready, 1)

        w_cross.wait_recv()
        for i in dp_others:
            weight_copy(i, p).start()

        @pl.when(c == 1)
        def _():
            for recv in (e_recv, g_recv):
                recv[:, nch - 1, :, T:] = jnp.zeros((3, cols, EC - T), F32)

        iota[...] = lax.broadcasted_iota(jnp.int32, (T, D), 0).astype(I16)
        lanes[...] = lax.broadcasted_iota(jnp.int32, (16, D), 1).astype(I16)

        ids_raw[...] = jnp.full(ids_raw.shape, -1, jnp.int32)
        for which, src in enumerate((send_ids, recv_ids)):
            ids_raw[which:which + 1, :edges] = src[...].reshape(1, edges)

        def ids(b):
            for which, (row_ref, col_ref) in enumerate(((srow, scol), (rrow, rcol))):
                wide = jnp.broadcast_to(ids_raw[which:which + 1, pl.ds(pl.multiple_of(c * eh + b * D, D), D)], (D, D))
                row_ref[at(b, 16), :] = wide[:16].astype(I16)
                col_ref[at(b, D), :] = flip(wide.astype(F32)).astype(jnp.int32).astype(I16)

        with jax.named_scope('ids'):
            loop(eh // D, ids)

        def keys(ref, step):
            return [ref[pl.ds(pl.multiple_of(step * (KS // D) * 16 + 16 * h, 16), 1), :] for h in range(KS // D)]

        bias_cols[...] = flip(stacked([eb1_in[...], nb1_in[...], jnp.zeros((D - 2 * layers, D), F32)]))

        def join_weights(l):
            off = HEAD + l * LROWS
            for d in range(GROUP):
                src = w_send if d == 0 else w_recv.at[slot(d)]
                r = slice(d * q, (d + 1) * q)
                for k in THREE:
                    ew1[l, k * D + d * q:k * D + (d + 1) * q, :] = src[off + k * q:off + (k + 1) * q, :].astype(BF)
                ew2t[l, r, :] = src[off + 3 * q:off + 4 * q, :].astype(BF)
                for k in range(2):
                    nw1[l, k * D + d * q:k * D + (d + 1) * q, :] = src[off + (4 + k) * q:off + (5 + k) * q, :].astype(BF)
                nw2t[l, r, :] = src[off + 6 * q:off + 7 * q, :].astype(BF)

            def flip_bf(mat):
                return flip(mat.astype(F32)).astype(BF)

            for k in THREE:
                ew1t[l, :, mat(k)] = flip_bf(ew1[l, mat(k), :])
            for k in range(2):
                nw1t[l, :, mat(k)] = flip_bf(nw1[l, mat(k), :])
            ew2[l] = flip_bf(ew2t[l])
            nw2[l] = flip_bf(nw2t[l])

        def wait_recvs(copies):
            copies[1].wait_recv()
            copies[2].start()
            copies[0].wait_recv()
            copies[2].wait_recv()

        with jax.named_scope('node_wait'):
            wait_recvs(ncop)
        for d in OTHERS:
            v0[rows_of(d), :] = n_recv[slot(d)].astype(BF)
        with jax.named_scope('weight_wait'):
            for i in dp_others:
                weight_copy(i, lax.rem(p + dpn - i, dpn)).wait_recv()
            w_relay.start()
            w_pair.wait_recv()
            w_relay.wait_recv()
        rows_all = beside([w_send[:HEAD, :cols]] + [w_recv[d, :HEAD, :cols] for d in range(3)])
        vecs[...] = flip(stacked([rows_all, jnp.zeros((D - HEAD, D), F32)]))
        join_weights(0)

        def vec(l, node):
            first = 6 * node + l
            return [vecs[:, first + 2 * k:first + 2 * k + 1] for k in THREE]

        def bias(l, node):
            return bias_cols[:, node * layers + l:node * layers + l + 1]

        def hidden_of_nodes(l):
            table, b1 = tables[l], bias(l, 0)

            def body(step):
                xs = gather(table, keys(srow, step), iota).astype(BF)
                xr = gather(table, keys(rrow, step), iota).astype(BF)
                hidden[l, :, at(step, KS)] = dot(ew1t[l, :, mat(1, 2)], stacked([xs, xr])) + b1

            loop(eh // KS, body)

        def edge_forward(l):
            e_in = edges_in[l]

            def body(j):
                for sub in range(EC // T):
                    a = at(j * (EC // T) + sub, T)
                    if l == 0:
                        if sub == 0:
                            for d in OTHERS:
                                edge_do(EDGE_IN, j, d, 'wait_recv')
                        for d in OTHERS:
                            e_in[rows_of(d), a] = e_recv[slot(d), j, :, sub * T:(sub + 1) * T].astype(BF)
                    e_val = e_in[:, a]
                    hid = hidden[l, :, a] + dot(ew1t[l, :, mat(0)], e_val)
                    hidden[l, :, a] = hid
                    message, nrm, std = mlp_tail(hid, ew2t[l], vec(l, 0))
                    normed[l, :, a] = nrm
                    inv[l:l + 1, a] = std
                    msg[:, a] = message
                    e_new = (e_val.astype(F32) + message.astype(F32)).astype(BF)
                    if l < top:
                        edges_in[l + 1][:, a] = e_new
                    else:
                        for d in OTHERS:
                            e_send[slot(d), j, :, sub * T:(sub + 1) * T] = e_new[rows_of(d)].astype(F32)
                        if sub == 0:
                            own_parts = []
                        own_parts.append(e_new[:q])
                if l == top:
                    for d in SEND_ORDER:
                        edge_do(EDGE_OUT, j, d, 'start')
                    place_edges(edge_raw, beside(own_parts), 0, j)

            loop(nch, body)

        def segment_sum(acc, ids_ref):
            acc[...] = jnp.zeros(acc.shape, F32)

            def body(step):
                scatter(acc, msg[:, at(step, KS)], ids_ref[at(step, KS), :], lanes)

            loop(eh // KS, body)

        def node_forward(l):
            table, agg, out = tables[l], aggs[l], tables[l + 1]

            def body(step):
                a = pl.ds(pl.multiple_of(step * TN, D), TN)
                v_in = table[:, a]
                agg_bf = (part[l, :, a] + swap_halves(part_recv[l, :, a])).astype(BF)
                agg[:, a] = agg_bf
                hid = dot(nw1t[l], stacked([v_in, agg_bf])) + bias(l, 1)
                nhid[l, :, a] = hid
                message, nrm, std = mlp_tail(hid, nw2t[l], vec(l, 1))
                nnrm[l, :, a] = nrm
                ninv[l:l + 1, a] = std
                out[:, a] = (v_in.astype(F32) + message.astype(F32)).astype(BF)

            loop(npad // TN, body)

        for l in range(layers):
            with jax.named_scope(f'gather_{l}'):
                hidden_of_nodes(l)
            if l == top:
                edges_sent(EDGE_IN)
            with jax.named_scope(f'edge_forward_{l}'):
                edge_forward(l)
            with jax.named_scope(f'sum_{l}'):
                segment_sum(part.at[l], rcol)
            part_copy(l).start()
            if l == 0:
                join_weights(1)
                gcop[1].wait_recv()
                gcop[2].start()
            with jax.named_scope(f'part_wait_{l}'):
                part_copy(l).wait_recv()
            with jax.named_scope(f'node_forward_{l}'):
                node_forward(l)
        no_send[...] = tables[layers][2 * q:3 * q, :].astype(F32)
        no_copy = remote(no_send, no_recv, n_ss.at[2, 0], n_rs.at[2, 0], 2)
        no_copy.start()
        node_raw[x] = tables[layers][:q, :nodes]

        hold = nch - 3
        grad[...] = jnp.zeros_like(grad)
        sums[...] = jnp.zeros_like(sums)
        with jax.named_scope('grad_node_wait'):
            gcop[0].wait_recv()
            gcop[2].wait_recv()
        for d in OTHERS:
            d_part[rows_of(d), :] = gn_recv[slot(d)]

        def node_backward(l):
            table, agg = tables[l], aggs[l]

            def body(step):
                a = pl.ds(pl.multiple_of(step * TN, D), TN)
                d_in = d_part[:, a]
                if l < top:
                    d_in = d_in + part[layers + l + 1, :, a] + swap_halves(part_recv[layers + l + 1, :, a])
                    d_in = d_in.astype(BF).astype(F32)
                d_hid, d_w2, parts = mlp_back(d_in, nhid[l, :, a], nnrm[l, :, a], ninv[l:l + 1, a], nw2[l], vec(l, 1))
                add_sums(sums.at[l, 1], [parts])
                grad[l, 4] += d_w2
                grad[l, 2] += dot_nt(table[:, a], d_hid)
                grad[l, 3] += dot_nt(agg[:, a], d_hid)
                d_part[:, a] = d_in + dot(nw1[l, mat(0), :], d_hid)
                d_agg[:, a] = dot(nw1[l, mat(1), :], d_hid).astype(BF)

            loop(npad // TN, body)

        def gather_back():
            def body(step):
                msg[:, at(step, KS)] = gather(d_agg, keys(rrow, step), iota).astype(BF)

            loop(eh // KS, body)

        def edge_backward(l):
            e_in = edges_in[l]

            def body(j):
                all_parts, d_w2s, d_w1s, own_parts = [], [], [], []
                for sub in range(EC // T):
                    a = at(j * (EC // T) + sub, T)
                    if l == top:
                        if sub == 0:
                            for d in OTHERS:
                                edge_do(GRAD_IN, j, d, 'wait_recv')
                        for d in OTHERS:
                            ge[rows_of(d), a] = g_recv[slot(d), j, :, sub * T:(sub + 1) * T].astype(BF)
                    d_res = ge[:, a].astype(F32)
                    d_msg = d_res + msg[:, a].astype(F32)
                    d_hid, d_w2, parts = mlp_back(d_msg, hidden[l, :, a], normed[l, :, a], inv[l:l + 1, a], ew2[l], vec(l, 0))
                    all_parts.append(parts)
                    d_w2s.append(d_w2)
                    d_w1s.append(dot_nt(e_in[:, a], d_hid))
                    msg[:, a] = d_hid
                    d_new = (d_res + dot(ew1[l, mat(0), :], d_hid)).astype(BF)
                    if l > 0:
                        ge[:, a] = d_new
                    else:
                        for d in OTHERS:
                            g_send[slot(d), j, :, sub * T:(sub + 1) * T] = d_new[rows_of(d)].astype(F32)
                        own_parts.append(d_new[:q])
                add_sums(sums.at[l, 0], all_parts)
                grad[l, 1] += sum(d_w2s[1:], d_w2s[0])
                grad[l, 0] += sum(d_w1s[1:], d_w1s[0])
                if l == 0:
                    @pl.when(j < hold)
                    def _():
                        for d in SEND_ORDER:
                            edge_do(GRAD_OUT, j, d, 'start')
                    place_edges(gedge_raw, beside(own_parts), 0, j)

            loop(nch, body)

        def vector_slab(l):
            def total(node, k):
                return column_sum(flip(sums[l, node, mat(k), :]))

            lat = stacked([total(node, k) for node in BOTH for k in THREE])
            biases = stacked([total(node, 3) for node in BOTH])
            n_lat = lat.shape[0]
            for d in range(GROUP):
                grad[l, VEC_SLAB, d * cols:d * cols + n_lat, :cols] = lat[:, rows_of(d)]
                grad[l, VEC_SLAB, d * cols + n_lat:d * cols + n_lat + 2, :] = biases

        def reduce_start(l, stage):
            for b in BOTH:
                core_copy(l, b, stage).start()

        def chip_sum(l, stage):
            row = lax.broadcasted_iota(jnp.int32, (cols, D), 0)
            edge_row = jnp.logical_or(row < 3, row == 6)
            for b in BOTH:
                core_copy(l, b, stage).wait_recv()
                for k in range(SLABS)[STAGES[stage]]:
                    own = grad[l, k, rows_of(2 * b), :]
                    if k in EDGE_SLABS:
                        own = own + core_recv[l, b, k]
                    elif k == VEC_SLAB:
                        own = own + jnp.where(edge_row, core_recv[l, b, k], 0.0)
                    half[l, k, b] = own
            for i in dp_others:
                @pl.when(in_stage(lax.rem(p + i, dpn), stage))
                def _():
                    spread_copy(l, i).start()

        def dp_sum(l, stage):
            @pl.when(in_stage(p, stage))
            def _():
                total = half[l, pl.ds(p * per, per)]
                for i in dp_others:
                    spread_copy(l, i).wait_recv()
                    total = total + dp_recv[l, i - 1]
                own_sum[l] = total[:, 0]
                cross_send[l] = total[:, 1]
                cross_copy(l).start()

        def cross_sum(l):
            cross_copy(l).wait_recv()
            total = own_sum[l] + cross_recv[l]
            own_sum[l] = total
            gathered[l, pl.ds(p * per, per)] = total
            for i in dp_others:
                gather_copy(l, i, p).start()

        def project(l):
            table = tables[l]

            def body(step):
                a = pl.ds(pl.multiple_of(step * TN, D), TN)
                s_bf, r_bf, v_in = s_sum[:, a].astype(BF), r_sum[:, a].astype(BF), table[:, a]
                part[layers + l, :, a] = dot(ew1[l, mat(1), :], s_bf) + dot(ew1[l, mat(2), :], r_bf)
                grad[l, 6] += dot_nt(v_in, s_bf)
                grad[l, 7] += dot_nt(v_in, r_bf)

            loop(npad // TN, body)

        for l in reversed(range(layers)):
            last = l == 0
            with jax.named_scope(f'node_backward_{l}'):
                node_backward(l)
            if last:
                with jax.named_scope('chip_sum_1'):
                    chip_sum(1, 0)
                    chip_sum(1, 1)
            with jax.named_scope(f'gather_back_{l}'):
                gather_back()
            if last:
                edges_sent(GRAD_IN)
            with jax.named_scope(f'edge_backward_{l}'):
                edge_backward(l)
            vector_slab(l)
            reduce_start(l, 0)
            if last:
                with jax.named_scope('dp_sum_1'):
                    dp_sum(1, 0)
                    dp_sum(1, 1)
            with jax.named_scope(f'sum_send_{l}'):
                segment_sum(s_sum, scol)
            if last:
                with jax.named_scope('chip_sum_0'):
                    chip_sum(0, 0)
            with jax.named_scope(f'sum_recv_{l}'):
                segment_sum(r_sum, rcol)
            if last:
                with jax.named_scope('dp_sum_0'):
                    dp_sum(0, 0)
            with jax.named_scope(f'project_{l}'):
                project(l)
            part_copy(layers + l).start()
            reduce_start(l, 1)
            with jax.named_scope(f'back_wait_{l}'):
                part_copy(layers + l).wait_recv()

        def final(step):
            a = pl.ds(pl.multiple_of(step * TN, D), TN)
            d_in = (d_part[:, a] + part[layers, :, a] + swap_halves(part_recv[layers, :, a])).astype(BF)
            v2[:, a] = d_in

        loop(npad // TN, final)
        dn_send[...] = v2[2 * q:3 * q, :].astype(F32)
        dn_copy = remote(dn_send, dn_recv, n_ss.at[2, 1], n_rs.at[2, 1], 2)
        dn_copy.start()
        gnode_raw[x] = v2[:q, :nodes]
        with jax.named_scope('chip_sum_late'):
            chip_sum(0, 1)

        with jax.named_scope('node_out_wait'):
            no_copy.wait_recv()
        node_raw[ox] = no_recv[:, :nodes].astype(BF)

        def place_e(j):
            for d in OTHERS:
                edge_do(EDGE_OUT, j, d, 'wait_recv')
                place_edges(edge_raw, eo_recv[slot(d), j], d, j)

        with jax.named_scope('place_edge_out'):
            loop(nch, place_e)
        with jax.named_scope('dp_sum_late'):
            dp_sum(0, 1)

        def send_rest(j):
            for d in SEND_ORDER:
                edge_do(GRAD_OUT, j, d, 'start')

        loop(nch, send_rest, hold)

        def place_g(j):
            for d in OTHERS:
                edge_do(GRAD_OUT, j, d, 'wait_recv')
                place_edges(gedge_raw, de_recv[slot(d), j], d, j)

        with jax.named_scope('place_first'):
            loop(hold, place_g)
        for l in range(layers):
            with jax.named_scope(f'cross_sum_{l}'):
                cross_sum(l)
        with jax.named_scope('d_node_wait'):
            dn_copy.wait_recv()
        gnode_raw[ox] = dn_recv[:, :nodes].astype(BF)
        with jax.named_scope('place_rest'):
            loop(nch - 1, place_g, hold)
        for l in range(layers):
            for i in dp_others:
                gather_copy(l, i, lax.rem(p + dpn - i, dpn)).wait_recv()
            ew1_buf[l, 0] = gathered[l, 0]
            ew1_buf[l, 1:] = gathered[l, EARLY:]
            ew2_buf[l] = gathered[l, 1]
            nw1_buf[l] = gathered[l, 2:4]
            nw2_buf[l] = gathered[l, 4]
            small = gathered[l, VEC_SLAB]
            for k in THREE:
                evec_buf[k, l:l + 1, :] = small[k:k + 1, :cols]
                nvec_buf[k, l:l + 1, :] = small[3 + k:4 + k, :cols]
            eb1_buf[l:l + 1, :] = small[6:7]
            nb1_buf[l:l + 1, :] = small[7:8]
        for l in range(layers):
            for b in BOTH:
                for stage in BOTH:
                    core_copy(l, b, stage).wait_send()
            cross_copy(l).wait_send()
            for i in dp_others:
                spread_copy(l, i).wait_send()
                gather_copy(l, i, p).wait_send()
        for copy in ncop + gcop + (w_pair, w_cross, w_relay):
            copy.wait_send()
        for i in dp_others:
            weight_copy(i, p).wait_send()
        no_copy.wait_send()
        dn_copy.wait_send()
        for k in range(2 * layers):
            part_copy(k).wait_send()
        edges_sent(EDGE_OUT)
        with jax.named_scope('place_last'):
            loop(nch, place_g, nch - 1)
        edges_sent(GRAD_OUT)

    bf = lambda *s: pltpu.VMEM(s, BF)
    pl.run_scoped(
        scoped, bf(D, eh), bf(D, eh), bf(D, eh), bf(D, eh), bf(D, npad), bf(D, npad), bf(D, npad), bf(D, npad), bf(D, npad), bf(D, npad),
        pltpu.VMEM((eh, D), I16), pltpu.VMEM((eh, D), I16), pltpu.VMEM((eh // D * 16, D), I16), pltpu.VMEM((eh // D * 16, D), I16),
        pltpu.VMEM((T, D), I16), pltpu.VMEM((16, D), I16),
        bf(layers, 3 * D, D), bf(layers, D, 3 * D), bf(layers, D, D), bf(layers, D, D),
        bf(layers, 2 * D, D), bf(layers, D, 2 * D), bf(layers, D, D), bf(layers, D, D), pltpu.VMEM((D, D), F32))


def finish_kernel(*refs):
    count = len(refs) // 2
    sem = refs[-1]
    puts = [pltpu.make_async_copy(refs[k], refs[count + k], sem.at[k]) for k in range(count)]
    for put in puts:
        put.start()
    for put in puts:
        put.wait()


def keep_in_vmem(val):
    return pltpu.with_memory_space_constraint(val, pltpu.VMEM)


def finish(arrays):
    return pl.pallas_call(
        finish_kernel,
        name='finish',
        out_shape=[jax.ShapeDtypeStruct(a.shape, a.dtype) for a in arrays],
        in_specs=[VM] * len(arrays),
        out_specs=[HB] * len(arrays),
        scratch_shapes=[pltpu.SemaphoreType.DMA((len(arrays),))],
        compiler_params=pltpu.CompilerParams(vmem_limit_bytes=1 << 20),
    )(*[keep_in_vmem(a) for a in arrays])


def solution(mesh):
    lat_spec = P('dp', None, 'tp')
    first_spec = P(None, None, 'tp', None)
    col_spec = P(None, None, 'tp')
    param_specs = (first_spec, P(), col_spec, col_spec, first_spec, P(), col_spec, col_spec)
    in_specs = (lat_spec, lat_spec, P(), P(), lat_spec, lat_spec) + param_specs
    out_specs = (lat_spec, lat_spec, lat_spec, lat_spec) + param_specs
    shape = jax.ShapeDtypeStruct

    def local_step(node_lat, edge_lat, senders, receivers, grad_node, grad_edge, edge_w1, edge_b1, edge_w2, edge_vec, node_w1, node_b1, node_w2, node_vec):
        layers = edge_w1.shape[0]
        cols = node_lat.shape[2]
        nodes, edges = node_lat.shape[1], edge_lat.shape[1]
        npad = -(-nodes // TN) * TN
        eh = -(-edges // (2 * EC)) * EC
        nch = eh // EC
        dpn = mesh.shape['dp']
        per = SLABS // dpn
        dims = (layers, cols, nodes, edges, npad, eh, dpn)
        flat = lambda arr: jnp.swapaxes(arr, 1, 2)
        lead = lambda arr: jnp.transpose(arr, (1, 0, 2))
        args = (flat(node_lat), flat(edge_lat), flat(grad_node), flat(grad_edge), senders, receivers,
                edge_w1.reshape(-1, D), flat(edge_w2).reshape(-1, D), node_w1.reshape(-1, D), flat(node_w2).reshape(-1, D),
                lead(edge_vec), lead(node_vec), edge_b1, node_b1)
        vm, sem = pltpu.VMEM, pltpu.SemaphoreType.DMA
        wrows = -(-(HEAD + layers * LROWS) // (8 * dpn)) * 8 * dpn
        lat_n, lat_e = (2, cols, nodes), (2, cols, edges)
        outs = [RESULT(lat_n, BF), RESULT(lat_e, BF), RESULT(lat_n, BF), RESULT(lat_e, BF),
                RESULT((layers, 3, cols, D), F32), RESULT((layers, D), F32), RESULT((layers, cols, D), F32), RESULT((3, layers, cols), F32),
                RESULT((layers, 2, cols, D), F32), RESULT((layers, D), F32), RESULT((layers, cols, D), F32), RESULT((3, layers, cols), F32)]
        scratch = [
            *[vm(a.shape, a.dtype) for a in args[4:]], vm((wrows, D), F32), vm((3, wrows, D), F32),
            vm((2, cols, npad), F32), vm((3, cols, npad), F32), vm((2, cols, npad), F32), vm((3, cols, npad), F32),
            vm((cols, npad), F32), vm((cols, npad), F32), vm((cols, npad), F32), vm((cols, npad), F32),
            *[vm((3, nch, cols, EC), F32)] * 6,
            vm((2 * layers, D, npad), F32), vm((2 * layers, D, npad), F32),
            vm((layers, D, eh), F32), vm((layers, D, eh), F32), vm((8, eh), F32),
            vm((layers, D, npad), F32), vm((layers, D, npad), F32), vm((8, npad), F32),
            vm((D, npad), F32), vm((D, npad), F32), vm((D, npad), F32), vm((8, 2 * eh), jnp.int32), vm((D, D), F32), vm((layers, 2, 4 * D, D), F32),
            vm((layers, SLABS, D, D), F32), vm((layers, 2, SLABS, cols, D), F32), vm((layers, SLABS, 2, cols, D), F32),
            vm((layers, dpn - 1, per, 2, cols, D), F32), vm((layers, per, cols, D), F32), vm((layers, per, cols, D), F32),
            vm((layers, per, cols, D), F32), vm((layers, SLABS, cols, D), F32),
            sem((layers, 2, 2)), sem((layers, 2, 2)), sem((3, layers, dpn - 1)), sem((3, layers, dpn - 1)), sem((layers,)), sem((layers,)),
            sem((len(args),)), sem((3,)), sem((3,)), sem((3, 3)), sem((3, 3)), sem((4, 3, 2)), sem((4, 3, nch)),
            sem((2 * layers,)), sem((2 * layers,)), pltpu.SemaphoreType.REGULAR]
        res = pl.pallas_call(
            lambda *refs: step_kernel(dims, *refs),
            name='graph_step',
            out_shape=outs,
            in_specs=[HB] * len(args),
            out_specs=[VM] * len(outs),
            scratch_shapes=scratch,
            compiler_params=pltpu.CompilerParams(collective_id=0, has_side_effects=True, vmem_limit_bytes=VMEM_LIMIT),
        )(*args)

        res = finish(res)
        return (flat(res[0]), flat(res[1]), flat(res[2]), flat(res[3]),
                res[4], res[5], flat(res[6]), lead(res[7]), res[8], res[9], flat(res[10]), lead(res[11]))

    return jax.shard_map(local_step, mesh=mesh, in_specs=in_specs, out_specs=out_specs, check_vma=False)
```

```python
import jax
import jax.numpy as jnp
from jax import lax
from jax.experimental import pallas as pl
from jax.experimental.pallas import tpu as pltpu
from jax.sharding import PartitionSpec as P

LN_EPS = 1e-5
D = 128
T = 256
TN = 384
EC = 512
KS = 1408
BF = jnp.bfloat16
F32 = jnp.float32
I16 = jnp.int16
MESH = pl.DeviceIdType.MESH
VM = pl.BlockSpec(memory_space=pltpu.VMEM)
HB = pl.BlockSpec(memory_space=pl.ANY)
RESULT = pltpu.VMEM
GROUP = 4
BOTH = (0, 1)
THREE = (0, 1, 2)
OTHERS = (1, 2, 3)
EDGE_IN, GRAD_IN, EDGE_OUT, GRAD_OUT = range(4)
SEND_ORDER = (2, 3, 1)
LROWS = 7 * (D // 4)
HEAD = 16
LEADER = GROUP - 1
VMEM_LIMIT = 63_000_000
SLABS = 8
EARLY = 6
VEC_SLAB = 5
EDGE_SLABS = (0, 1, 6, 7)
STAGES = (slice(0, EARLY), slice(EARLY, SLABS))


def dot(a, b):
    return jnp.dot(a, b, preferred_element_type=F32)


def dot_nt(a, b):
    return lax.dot_general(a, b, (((1,), (1,)), ((), ())), preferred_element_type=F32)


def mat(k, n=1):
    return slice(k * D, (k + n) * D)


def rows_of(d):
    q = D // 4
    return slice(d * q, (d + 1) * q)


def at(step, width):
    return pl.ds(pl.multiple_of(step * width, width), width)


def loop(stop, body, start=0):
    def step(j, carry):
        body(j)
        return carry

    lax.fori_loop(start, stop, step, 0)


def column_sum(val):
    return jnp.sum(val, axis=0, keepdims=True)


def flip(val):
    return jnp.swapaxes(val, 0, 1)


def stacked(parts):
    return jnp.concatenate(parts, axis=0)


def beside(parts):
    return jnp.concatenate(parts, axis=1)


def slot(d):
    return d - 1


def sigmoid(hidden):
    return 1.0 / (1.0 + jnp.exp(-hidden))


def fold(val):
    total = val[:, mat(0)]
    for start in range(D, val.shape[1], D):
        total = total + val[:, start:start + D]
    return total


def swap_halves(val):
    return stacked([val[rows_of(d)] for d in (1, 0, 3, 2)])


def gather(table, keys, iota):
    acc = None
    nodes = table.shape[1]
    one, zero = jnp.ones((), BF), jnp.zeros((), BF)
    for base in range(0, nodes, T):
        width = min(T, nodes - base)
        ids = iota[0:width, :]
        hot = beside([jnp.where(ids == (key - jnp.asarray(base, I16)), one, zero) for key in keys])
        part = dot(table[:, base:base + width], hot)
        acc = part if acc is None else acc + part
    return acc


def scatter(acc_ref, val, cols, lanes):
    nodes = acc_ref.shape[1]
    one, zero = jnp.ones((), BF), jnp.zeros((), BF)
    row = lanes[0:1, :]
    for base in range(0, nodes, T):
        width = min(T, nodes - base)
        hot = beside([jnp.where((row + jnp.asarray(base + s, I16)) == cols, one, zero) for s in range(0, width, D)])
        acc_ref[:, base:base + width] += dot(val, hot)


def mlp_tail(hidden, w2t, vec):
    act = (hidden * sigmoid(hidden)).astype(BF)
    out = dot(w2t, act) + vec[0]
    mean = column_sum(out) / D
    centered = out - mean
    var = column_sum(centered * centered) / D
    inv = lax.rsqrt(var + LN_EPS)
    normed = centered * inv
    message = (normed * vec[1] + vec[2]).astype(BF)
    return message, normed, inv


def mlp_back(d_msg, hidden, normed, inv, w2, vec):
    d_normed = d_msg * vec[1]
    mean0 = column_sum(d_normed) / D
    mean1 = column_sum(d_normed * normed) / D
    d_out = inv * (d_normed - mean0 - normed * mean1)
    d_out_bf = d_out.astype(BF)
    sig = sigmoid(hidden)
    act = (hidden * sig).astype(BF)
    d_w2 = dot_nt(d_out_bf, act)
    d_hidden = dot(w2, d_out_bf) * (sig * (1.0 + hidden * (1.0 - sig)))
    sums = (fold(d_out), fold(d_msg * normed), fold(d_msg), fold(d_hidden))
    return d_hidden.astype(BF), d_w2, sums


def add_sums(ref, parts):
    for q in range(4):
        total = parts[0][q]
        for other in parts[1:]:
            total = total + other[q]
        ref[mat(q), :] += total


def step_kernel(dims, *refs):
    layers, cols, nodes, edges, npad, eh, dpn = dims
    nch = eh // EC
    top = layers - 1
    n_in = 14
    hbm_in = refs[:n_in]
    n_out = 12
    (node_raw, edge_raw, gnode_raw, gedge_raw, ew1_buf, eb1_buf, ew2_buf, evec_buf, nw1_buf, nb1_buf, nw2_buf, nvec_buf) = refs[n_in:n_in + n_out]
    (send_ids, recv_ids, ew1_in, ew2_in, nw1_in, nw2_in, evec_in, nvec_in, eb1_in, nb1_in, w_send, w_recv, n_send, n_recv, gn_send, gn_recv, no_send, no_recv, dn_send, dn_recv,
     e_send, g_send, e_recv, g_recv, eo_recv, de_recv, part, part_recv, hidden, normed, inv, nhid, nnrm, ninv, d_part, s_sum, r_sum,
     ids_raw, bias_cols, sums, grad, core_recv, half, dp_recv, cross_send, cross_recv, own_sum, gathered,
     core_ss, core_rs, dp_ss, dp_rs, cross_ss, cross_rs, load_sem, w_ss, w_rs, n_ss, n_rs, e_ss, e_rs, p_ss, p_rs, ready) = refs[n_in + n_out:]

    t = lax.axis_index('tp')
    p = lax.axis_index('dp')
    per = SLABS // dpn
    dp_others = range(1, dpn)
    x, c = t // 2, lax.rem(t, 2)
    ox, oc = 1 - x, 1 - c
    peer = [t, t + 1 - 2 * c, t + 2 - 4 * x, t + 3 - 2 * c - 4 * x]

    def remote(src, dst, ssem, rsem, d):
        return pltpu.make_async_remote_copy(src_ref=src, dst_ref=dst, send_sem=ssem, recv_sem=rsem,
                                            device_id={'tp': peer[d]}, device_id_type=MESH)

    small_in = (send_ids, recv_ids, ew1_in, ew2_in, nw1_in, nw2_in, evec_in, nvec_in, eb1_in, nb1_in)
    loads = [pltpu.make_async_copy(src, dst, load_sem.at[q]) for q, (src, dst) in enumerate(
        zip(hbm_in, (node_raw, edge_raw, gnode_raw, gedge_raw) + small_in))]

    def node_copies(send, recv, kind):
        return (remote(send.at[1], recv.at[0], n_ss.at[kind, 0], n_rs.at[kind, 0], 1),
                remote(send.at[0], recv.at[1], n_ss.at[kind, 1], n_rs.at[kind, 1], 2),
                remote(recv.at[1], recv.at[2], n_ss.at[kind, 2], n_rs.at[kind, 2], 1))

    piece = w_send.shape[0] // dpn

    def weight_rows(owner):
        return pl.ds(pl.multiple_of(owner * piece, 8), piece)

    w_pair = remote(w_send, w_recv.at[0], w_ss.at[0], w_rs.at[0], 1)
    w_cross = remote(w_send.at[weight_rows(p)], w_recv.at[1, weight_rows(p)], w_ss.at[1], w_rs.at[1], 2)
    w_relay = remote(w_recv.at[1], w_recv.at[2], w_ss.at[2], w_rs.at[2], 1)

    def weight_copy(i, owner):
        rows = w_recv.at[1, weight_rows(owner)]
        return dp_remote(rows, rows, 2, 0, i)

    last = nch - 1
    hold = nch - 3
    buffers = ((e_send, e_recv), (g_send, g_recv), (e_send, eo_recv), (g_send, de_recv))

    def outward(kind):
        return kind in (EDGE_OUT, GRAD_OUT)

    def edge_part(kind, index, send_sem, recv_sem, d):
        src, dst = buffers[kind]
        return remote(src.at[index], dst.at[index], e_ss.at[kind, send_sem], e_rs.at[kind, recv_sem], d)

    def by_half(half_id, j, action):
        narrow = jnp.logical_and(j == last, half_id == 1)

        @pl.when(jnp.logical_not(narrow))
        def _():
            action(slice(None))

        @pl.when(narrow)
        def _():
            action(slice(T))

    def edge_start(kind, j, d):
        other = oc if d % 2 else c
        if outward(kind):
            send_sem, recv_sem = jnp.where(j == last, 1, 0), jnp.where(j == last, 2 + slot(d), jnp.where(j < hold, 0, 1))
        else:
            send_sem, recv_sem = jnp.where(j == last, d, 0), j
        by_half(c if outward(kind) else other, j,
                lambda used: edge_part(kind, (slot(d), j, slice(None), used), send_sem, recv_sem, d).start())

    def edges_sent(kind):
        every = slice(None)
        edge_part(kind, (every, slice(0, last)), 0, 0, 1).wait_send()
        if outward(kind):
            by_half(c, last, lambda used: edge_part(kind, (every, last, every, used), 1, 0, 1).wait_send())
        else:
            for d in OTHERS:
                by_half(oc if d % 2 else c, last, lambda used: edge_part(kind, (slot(d), last, every, used), d, 0, d).wait_send())

    def chunk_arrived(kind, j):
        every = slice(None)
        by_half(c, j, lambda used: edge_part(kind, (every, j, every, used), 0, j, 1).wait_recv())

    def group_arrived(kind, group):
        every = slice(None)
        if group < 2:
            edge_part(kind, (every, (slice(0, hold), slice(hold, last))[group]), 0, group, 1).wait_recv()
        else:
            for d in OTHERS:
                by_half(oc if d % 2 else c, last, lambda used: edge_part(kind, (slot(d), last, every, used), 0, 2 + slot(d), d).wait_recv())

    def core_copy(l, b, stage):
        first, count = ((0, EARLY), (EARLY, SLABS - EARLY))[stage]
        return remote(grad.at[l, pl.ds(first, count), pl.ds((2 * b + 1) * cols, cols), :], core_recv.at[l, b, pl.ds(first, count)],
                      core_ss.at[l, stage], core_rs.at[l, stage], 1)

    def core_all(l, stage):
        part_of = core_recv.at[l, :, (slice(0, EARLY), slice(EARLY, SLABS))[stage]]
        return remote(part_of, part_of, core_ss.at[l, stage], core_rs.at[l, stage], 1)

    def seat(device):
        return lax.rem(device + dpn // 2, dpn)

    def in_stage(device, stage):
        early = (seat(device) + 1) * per <= EARLY
        return jnp.logical_not(early) if stage else early

    def dp_remote(src, dst, stage, l, i):
        return pltpu.make_async_remote_copy(src_ref=src, dst_ref=dst, send_sem=dp_ss.at[stage, l], recv_sem=dp_rs.at[stage, l],
                                            device_id={'dp': lax.rem(p + i, dpn)}, device_id_type=MESH)

    def spread_copy(l, i):
        return dp_remote(half.at[l, pl.ds(seat(lax.rem(p + i, dpn)) * per, per)], dp_recv.at[l, pl.ds((i - 1) * per, per)], 0, l, i)

    def dp_all(l, stage):
        most = (dpn - 1) * per
        part_of = (dp_recv.at[l], gathered.at[l, pl.ds(0, most)], w_recv.at[1, pl.ds(0, (dpn - 1) * piece)])[stage]
        return dp_remote(part_of, part_of, stage, l, 1)

    def cross_copy(l):
        return remote(cross_send.at[l], cross_recv.at[l], cross_ss.at[l], cross_rs.at[l], 2)

    def gather_copy(l, i, owner):
        return dp_remote(own_sum.at[l], gathered.at[l, pl.ds(seat(owner) * per, per)], 1, l, i)

    def part_copy(q):
        return remote(part.at[q], part_recv.at[q], p_ss.at[q], p_rs.at[q], 1)

    def load_nodes(raw, send, own):
        send[...] = jnp.zeros_like(send)
        send[0, :, :nodes] = raw[ox].astype(F32)
        send[1, :, :nodes] = raw[x].astype(F32)
        own[:cols, :] = send[1].astype(own.dtype)

    def load_edges(raw, send, own, kind):
        def put(j, lanes_j, val_of):
            for d in OTHERS:
                sample = x if d < 2 else ox
                send[slot(d), j] = val_of(sample, oc if d % 2 else c).astype(F32)
            own[:cols, lanes_j] = val_of(x, c)

        def chunk(j):
            put(j, at(j, EC), lambda s, h: raw[s, :, pl.ds(pl.multiple_of(h * eh + j * EC, D), EC)])
            for d in SEND_ORDER:
                edge_start(kind, j, d)

        loop(nch - 1, chunk)
        first = (nch - 1) * EC
        used = edges - eh - first
        last = pl.ds(first, EC)

        def tail(s, h):
            left = raw[s, :, pl.ds(first, EC)]
            right = beside([raw[s, :, pl.ds(eh + first, used)], jnp.zeros((cols, EC - used), BF)])
            return jnp.where(h == 0, left.astype(F32), right.astype(F32)).astype(BF)

        put(nch - 1, last, tail)
        for d in SEND_ORDER:
            edge_start(kind, nch - 1, d)

    def place_edges(raw, block, d, j):
        s = x if d < 2 else ox
        h = oc if d % 2 else c
        val = block.astype(BF)
        first = (nch - 1) * EC
        used = edges - eh - first

        @pl.when(jnp.logical_or(j < nch - 1, h == 0))
        def _():
            raw[s, :, pl.ds(pl.multiple_of(h * eh + j * EC, D), EC)] = val

        @pl.when(jnp.logical_and(j == nch - 1, h == 1))
        def _():
            raw[s, :, pl.ds(eh + first, used)] = val[:, :used]

    def scoped(e0, e1, ge, msg, v0, v1, v2, agg0, agg1, d_agg, scol, rcol, srow, rrow, iota, lanes, ew1, ew1t, ew2, ew2t, nw1, nw1t, nw2, nw2t, vecs):
        tables = (v0, v1, v2)
        aggs = (agg0, agg1)
        edges_in = (e0, e1)

        barrier = pltpu.get_barrier_semaphore()
        for d in OTHERS:
            pl.semaphore_signal(barrier, inc=1, device_id={'tp': peer[d]}, device_id_type=MESH)
        for copy in loads[:1] + loads[4:] + loads[1:4]:
            copy.start()
        loads[0].wait()
        with jax.named_scope('send_nodes'):
            load_nodes(node_raw, n_send, v0)
        ncop = node_copies(n_send, n_recv, 0)
        for copy in loads[4:]:
            copy.wait()
        q = cols
        w_send[:HEAD, :] = jnp.zeros((HEAD, D), F32)
        for k in THREE:
            w_send[k * layers:(k + 1) * layers, :cols] = evec_in[k]
            w_send[(3 + k) * layers:(4 + k) * layers, :cols] = nvec_in[k]
        for l in range(layers):
            off = HEAD + l * LROWS
            w_send[off:off + 3 * q, :] = ew1_in[l * 3 * q:(l + 1) * 3 * q, :].astype(F32)
            w_send[off + 3 * q:off + 4 * q, :] = ew2_in[l * q:(l + 1) * q, :].astype(F32)
            w_send[off + 4 * q:off + 6 * q, :] = nw1_in[l * 2 * q:(l + 1) * 2 * q, :].astype(F32)
            w_send[off + 6 * q:off + 7 * q, :] = nw2_in[l * q:(l + 1) * q, :].astype(F32)
        with jax.named_scope('barrier'):
            @pl.when(t != LEADER)
            def _():
                pl.semaphore_wait(barrier, len(OTHERS))
                pl.semaphore_signal(ready, inc=1, device_id={'tp': LEADER}, device_id_type=MESH)

            @pl.when(t == LEADER)
            def _():
                pl.semaphore_wait(ready, len(OTHERS))
                for i in dp_others:
                    pl.semaphore_signal(barrier, inc=1, device_id={'dp': lax.rem(p + i, dpn)}, device_id_type=MESH)

        w_cross.start()
        w_pair.start()
        ncop[1].start()
        ncop[0].start()
        loads[1].wait()
        with jax.named_scope('send_edges'):
            load_edges(edge_raw, e_send, e0, EDGE_IN)
        loads[2].wait()
        load_nodes(gnode_raw, gn_send, d_part)
        gcop = node_copies(gn_send, gn_recv, 1)
        gcop[1].start()
        gcop[0].start()
        loads[3].wait()
        with jax.named_scope('send_grads'):
            load_edges(gedge_raw, g_send, ge, GRAD_IN)

        with jax.named_scope('dp_barrier'):
            @pl.when(t == LEADER)
            def _():
                pl.semaphore_wait(barrier, len(OTHERS) + dpn - 1)
                for d in OTHERS:
                    pl.semaphore_signal(ready, inc=1, device_id={'tp': peer[d]}, device_id_type=MESH)

            @pl.when(t != LEADER)
            def _():
                pl.semaphore_wait(ready, 1)

        w_cross.wait_recv()
        for i in dp_others:
            weight_copy(i, p).start()

        @pl.when(c == 1)
        def _():
            for recv in (e_recv, g_recv):
                recv[:, nch - 1, :, T:] = jnp.zeros((3, cols, EC - T), F32)

        iota[...] = lax.broadcasted_iota(jnp.int32, (T, D), 0).astype(I16)
        lanes[...] = lax.broadcasted_iota(jnp.int32, (16, D), 1).astype(I16)

        ids_raw[...] = jnp.full(ids_raw.shape, -1, jnp.int32)
        for which, src in enumerate((send_ids, recv_ids)):
            ids_raw[which:which + 1, :edges] = src[...].reshape(1, edges)

        def ids(b):
            for which, (row_ref, col_ref) in enumerate(((srow, scol), (rrow, rcol))):
                wide = jnp.broadcast_to(ids_raw[which:which + 1, pl.ds(pl.multiple_of(c * eh + b * D, D), D)], (D, D))
                row_ref[at(b, 16), :] = wide[:16].astype(I16)
                col_ref[at(b, D), :] = flip(wide.astype(F32)).astype(jnp.int32).astype(I16)

        with jax.named_scope('ids'):
            loop(eh // D, ids)

        def keys(ref, step):
            return [ref[pl.ds(pl.multiple_of(step * (KS // D) * 16 + 16 * h, 16), 1), :] for h in range(KS // D)]

        bias_cols[...] = flip(stacked([eb1_in[...], nb1_in[...], jnp.zeros((D - 2 * layers, D), F32)]))

        def join_weights(l):
            off = HEAD + l * LROWS
            for d in range(GROUP):
                src = w_send if d == 0 else w_recv.at[slot(d)]
                r = slice(d * q, (d + 1) * q)
                for k in THREE:
                    ew1[l, k * D + d * q:k * D + (d + 1) * q, :] = src[off + k * q:off + (k + 1) * q, :].astype(BF)
                ew2t[l, r, :] = src[off + 3 * q:off + 4 * q, :].astype(BF)
                for k in range(2):
                    nw1[l, k * D + d * q:k * D + (d + 1) * q, :] = src[off + (4 + k) * q:off + (5 + k) * q, :].astype(BF)
                nw2t[l, r, :] = src[off + 6 * q:off + 7 * q, :].astype(BF)

            def flip_bf(mat):
                return flip(mat.astype(F32)).astype(BF)

            for k in THREE:
                ew1t[l, :, mat(k)] = flip_bf(ew1[l, mat(k), :])
            for k in range(2):
                nw1t[l, :, mat(k)] = flip_bf(nw1[l, mat(k), :])
            ew2[l] = flip_bf(ew2t[l])
            nw2[l] = flip_bf(nw2t[l])

        def wait_recvs(copies):
            copies[1].wait_recv()
            copies[2].start()
            copies[0].wait_recv()
            copies[2].wait_recv()

        with jax.named_scope('node_wait'):
            wait_recvs(ncop)
        for d in OTHERS:
            v0[rows_of(d), :] = n_recv[slot(d)].astype(BF)
        with jax.named_scope('weight_wait'):
            dp_all(0, 2).wait_recv()
            w_relay.start()
            w_pair.wait_recv()
            w_relay.wait_recv()
        rows_all = beside([w_send[:HEAD, :cols]] + [w_recv[d, :HEAD, :cols] for d in range(3)])
        vecs[...] = flip(stacked([rows_all, jnp.zeros((D - HEAD, D), F32)]))
        join_weights(0)

        def vec(l, node):
            first = 6 * node + l
            return [vecs[:, first + 2 * k:first + 2 * k + 1] for k in THREE]

        def bias(l, node):
            return bias_cols[:, node * layers + l:node * layers + l + 1]

        def hidden_of_nodes(l):
            table, b1 = tables[l], bias(l, 0)

            def body(step):
                xs = gather(table, keys(srow, step), iota).astype(BF)
                xr = gather(table, keys(rrow, step), iota).astype(BF)
                hidden[l, :, at(step, KS)] = dot(ew1t[l, :, mat(1, 2)], stacked([xs, xr])) + b1

            loop(eh // KS, body)

        def edge_forward(l):
            e_in = edges_in[l]

            def body(j):
                for sub in range(EC // T):
                    a = at(j * (EC // T) + sub, T)
                    if l == 0:
                        if sub == 0:
                            chunk_arrived(EDGE_IN, j)
                        for d in OTHERS:
                            e_in[rows_of(d), a] = e_recv[slot(d), j, :, sub * T:(sub + 1) * T].astype(BF)
                    e_val = e_in[:, a]
                    hid = hidden[l, :, a] + dot(ew1t[l, :, mat(0)], e_val)
                    hidden[l, :, a] = hid
                    message, nrm, std = mlp_tail(hid, ew2t[l], vec(l, 0))
                    normed[l, :, a] = nrm
                    inv[l:l + 1, a] = std
                    msg[:, a] = message
                    e_new = (e_val.astype(F32) + message.astype(F32)).astype(BF)
                    if l < top:
                        edges_in[l + 1][:, a] = e_new
                    else:
                        for d in OTHERS:
                            e_send[slot(d), j, :, sub * T:(sub + 1) * T] = e_new[rows_of(d)].astype(F32)
                        if sub == 0:
                            own_parts = []
                        own_parts.append(e_new[:q])
                if l == top:
                    for d in SEND_ORDER:
                        edge_start(EDGE_OUT, j, d)
                    place_edges(edge_raw, beside(own_parts), 0, j)

            loop(nch, body)

        def segment_sum(acc, ids_ref):
            acc[...] = jnp.zeros(acc.shape, F32)

            def body(step):
                scatter(acc, msg[:, at(step, KS)], ids_ref[at(step, KS), :], lanes)

            loop(eh // KS, body)

        def node_forward(l):
            table, agg, out = tables[l], aggs[l], tables[l + 1]

            def body(step):
                a = pl.ds(pl.multiple_of(step * TN, D), TN)
                v_in = table[:, a]
                agg_bf = (part[l, :, a] + swap_halves(part_recv[l, :, a])).astype(BF)
                agg[:, a] = agg_bf
                hid = dot(nw1t[l], stacked([v_in, agg_bf])) + bias(l, 1)
                nhid[l, :, a] = hid
                message, nrm, std = mlp_tail(hid, nw2t[l], vec(l, 1))
                nnrm[l, :, a] = nrm
                ninv[l:l + 1, a] = std
                out[:, a] = (v_in.astype(F32) + message.astype(F32)).astype(BF)

            loop(npad // TN, body)

        for l in range(layers):
            with jax.named_scope(f'gather_{l}'):
                hidden_of_nodes(l)
            if l == top:
                edges_sent(EDGE_IN)
            with jax.named_scope(f'edge_forward_{l}'):
                edge_forward(l)
            with jax.named_scope(f'sum_{l}'):
                segment_sum(part.at[l], rcol)
            part_copy(l).start()
            if l == 0:
                join_weights(1)
                gcop[1].wait_recv()
                gcop[2].start()
            with jax.named_scope(f'part_wait_{l}'):
                part_copy(l).wait_recv()
            with jax.named_scope(f'node_forward_{l}'):
                node_forward(l)
        no_send[...] = tables[layers][2 * q:3 * q, :].astype(F32)
        no_copy = remote(no_send, no_recv, n_ss.at[2, 0], n_rs.at[2, 0], 2)
        no_copy.start()
        node_raw[x] = tables[layers][:q, :nodes]

        grad[...] = jnp.zeros_like(grad)
        sums[...] = jnp.zeros_like(sums)
        with jax.named_scope('grad_node_wait'):
            gcop[0].wait_recv()
            gcop[2].wait_recv()
        for d in OTHERS:
            d_part[rows_of(d), :] = gn_recv[slot(d)]

        def node_backward(l):
            table, agg = tables[l], aggs[l]

            def body(step):
                a = pl.ds(pl.multiple_of(step * TN, D), TN)
                d_in = d_part[:, a]
                if l < top:
                    d_in = d_in + part[layers + l + 1, :, a] + swap_halves(part_recv[layers + l + 1, :, a])
                    d_in = d_in.astype(BF).astype(F32)
                d_hid, d_w2, parts = mlp_back(d_in, nhid[l, :, a], nnrm[l, :, a], ninv[l:l + 1, a], nw2[l], vec(l, 1))
                add_sums(sums.at[l, 1], [parts])
                grad[l, 4] += d_w2
                grad[l, 2] += dot_nt(table[:, a], d_hid)
                grad[l, 3] += dot_nt(agg[:, a], d_hid)
                d_part[:, a] = d_in + dot(nw1[l, mat(0), :], d_hid)
                d_agg[:, a] = dot(nw1[l, mat(1), :], d_hid).astype(BF)

            loop(npad // TN, body)

        def gather_back():
            def body(step):
                msg[:, at(step, KS)] = gather(d_agg, keys(rrow, step), iota).astype(BF)

            loop(eh // KS, body)

        def edge_backward(l):
            e_in = edges_in[l]

            def body(j):
                all_parts, d_w2s, d_w1s, own_parts = [], [], [], []
                for sub in range(EC // T):
                    a = at(j * (EC // T) + sub, T)
                    if l == top:
                        if sub == 0:
                            chunk_arrived(GRAD_IN, j)
                        for d in OTHERS:
                            ge[rows_of(d), a] = g_recv[slot(d), j, :, sub * T:(sub + 1) * T].astype(BF)
                    d_res = ge[:, a].astype(F32)
                    d_msg = d_res + msg[:, a].astype(F32)
                    d_hid, d_w2, parts = mlp_back(d_msg, hidden[l, :, a], normed[l, :, a], inv[l:l + 1, a], ew2[l], vec(l, 0))
                    all_parts.append(parts)
                    d_w2s.append(d_w2)
                    d_w1s.append(dot_nt(e_in[:, a], d_hid))
                    msg[:, a] = d_hid
                    d_new = (d_res + dot(ew1[l, mat(0), :], d_hid)).astype(BF)
                    if l > 0:
                        ge[:, a] = d_new
                    else:
                        for d in OTHERS:
                            g_send[slot(d), j, :, sub * T:(sub + 1) * T] = d_new[rows_of(d)].astype(F32)
                        own_parts.append(d_new[:q])
                add_sums(sums.at[l, 0], all_parts)
                grad[l, 1] += sum(d_w2s[1:], d_w2s[0])
                grad[l, 0] += sum(d_w1s[1:], d_w1s[0])
                if l == 0:
                    @pl.when(j < hold)
                    def _():
                        for d in SEND_ORDER:
                            edge_start(GRAD_OUT, j, d)
                    place_edges(gedge_raw, beside(own_parts), 0, j)

            loop(nch, body)

        def vector_slab(l):
            def total(node, k):
                return column_sum(flip(sums[l, node, mat(k), :]))

            lat = stacked([total(node, k) for node in BOTH for k in THREE])
            biases = stacked([total(node, 3) for node in BOTH])
            n_lat = lat.shape[0]
            for d in range(GROUP):
                grad[l, VEC_SLAB, d * cols:d * cols + n_lat, :cols] = lat[:, rows_of(d)]
                grad[l, VEC_SLAB, d * cols + n_lat:d * cols + n_lat + 2, :] = biases

        def reduce_start(l, stage):
            for b in BOTH:
                core_copy(l, b, stage).start()

        def chip_sum(l, stage):
            row = lax.broadcasted_iota(jnp.int32, (cols, D), 0)
            edge_row = jnp.logical_or(row < 3, row == 6)
            core_all(l, stage).wait_recv()
            for b in BOTH:
                for k in range(SLABS)[STAGES[stage]]:
                    own = grad[l, k, rows_of(2 * b), :]
                    if k in EDGE_SLABS:
                        own = own + core_recv[l, b, k]
                    elif k == VEC_SLAB:
                        own = own + jnp.where(edge_row, core_recv[l, b, k], 0.0)
                    half[l, k, b] = own
            for i in dp_others:
                @pl.when(in_stage(lax.rem(p + i, dpn), stage))
                def _():
                    spread_copy(l, i).start()

        def dp_sum(l, stage):
            @pl.when(in_stage(p, stage))
            def _():
                total = half[l, pl.ds(seat(p) * per, per)]
                dp_all(l, 0).wait_recv()
                for i in dp_others:
                    total = total + dp_recv[l, pl.ds((i - 1) * per, per)]
                own_sum[l] = total[:, 0]
                cross_send[l] = total[:, 1]
                cross_copy(l).start()

        def cross_sum(l):
            cross_copy(l).wait_recv()
            total = own_sum[l] + cross_recv[l]
            own_sum[l] = total
            gathered[l, pl.ds(seat(p) * per, per)] = total
            for i in dp_others:
                gather_copy(l, i, p).start()

        def project(l):
            table = tables[l]

            def body(step):
                a = pl.ds(pl.multiple_of(step * TN, D), TN)
                s_bf, r_bf, v_in = s_sum[:, a].astype(BF), r_sum[:, a].astype(BF), table[:, a]
                part[layers + l, :, a] = dot(ew1[l, mat(1), :], s_bf) + dot(ew1[l, mat(2), :], r_bf)
                grad[l, 6] += dot_nt(v_in, s_bf)
                grad[l, 7] += dot_nt(v_in, r_bf)

            loop(npad // TN, body)

        for l in reversed(range(layers)):
            first_layer = l == 0
            with jax.named_scope(f'node_backward_{l}'):
                node_backward(l)
            if first_layer:
                with jax.named_scope('chip_sum_1'):
                    chip_sum(1, 0)
                    chip_sum(1, 1)
            with jax.named_scope(f'gather_back_{l}'):
                gather_back()
            if first_layer:
                edges_sent(GRAD_IN)
            with jax.named_scope(f'edge_backward_{l}'):
                edge_backward(l)
            vector_slab(l)
            reduce_start(l, 0)
            if first_layer:
                with jax.named_scope('dp_sum_1'):
                    dp_sum(1, 0)
                    dp_sum(1, 1)
            with jax.named_scope(f'sum_send_{l}'):
                segment_sum(s_sum, scol)
            if first_layer:
                with jax.named_scope('chip_sum_0'):
                    chip_sum(0, 0)
            with jax.named_scope(f'sum_recv_{l}'):
                segment_sum(r_sum, rcol)
            with jax.named_scope(f'project_{l}'):
                project(l)
            reduce_start(l, 1)
            part_copy(layers + l).start()
            if first_layer:
                with jax.named_scope('chip_sum_late'):
                    chip_sum(0, 1)
            with jax.named_scope(f'back_wait_{l}'):
                part_copy(layers + l).wait_recv()

        def final(step):
            a = pl.ds(pl.multiple_of(step * TN, D), TN)
            d_in = (d_part[:, a] + part[layers, :, a] + swap_halves(part_recv[layers, :, a])).astype(BF)
            v2[:, a] = d_in

        loop(npad // TN, final)
        dn_send[...] = v2[2 * q:3 * q, :].astype(F32)
        dn_copy = remote(dn_send, dn_recv, n_ss.at[2, 1], n_rs.at[2, 1], 2)
        dn_copy.start()
        gnode_raw[x] = v2[:q, :nodes]
        with jax.named_scope('dp_sum_0'):
            dp_sum(0, 0)

        with jax.named_scope('node_out_wait'):
            no_copy.wait_recv()
        node_raw[ox] = no_recv[:, :nodes].astype(BF)

        def place_e(j):
            for d in OTHERS:
                place_edges(edge_raw, eo_recv[slot(d), j], d, j)

        with jax.named_scope('place_edge_out'):
            for group in THREE:
                group_arrived(EDGE_OUT, group)
            loop(nch, place_e)
        with jax.named_scope('dp_sum_late'):
            dp_sum(0, 1)

        def send_rest(j):
            for d in SEND_ORDER:
                edge_start(GRAD_OUT, j, d)

        loop(nch, send_rest, hold)

        def place_g(j):
            for d in OTHERS:
                place_edges(gedge_raw, de_recv[slot(d), j], d, j)

        with jax.named_scope('place_first'):
            group_arrived(GRAD_OUT, 0)
            loop(hold, place_g)
        for l in range(layers):
            with jax.named_scope(f'cross_sum_{l}'):
                cross_sum(l)
        with jax.named_scope('d_node_wait'):
            dn_copy.wait_recv()
        gnode_raw[ox] = dn_recv[:, :nodes].astype(BF)
        with jax.named_scope('place_rest'):
            group_arrived(GRAD_OUT, 1)
            loop(last, place_g, hold)
        for l in range(layers):
            dp_all(l, 1).wait_recv()
            ew1_buf[l, 0] = gathered[l, 0]
            ew1_buf[l, 1:] = gathered[l, EARLY:]
            ew2_buf[l] = gathered[l, 1]
            nw1_buf[l] = gathered[l, 2:4]
            nw2_buf[l] = gathered[l, 4]
            small = gathered[l, VEC_SLAB]
            for k in THREE:
                evec_buf[k, l:l + 1, :] = small[k:k + 1, :cols]
                nvec_buf[k, l:l + 1, :] = small[3 + k:4 + k, :cols]
            eb1_buf[l:l + 1, :] = small[6:7]
            nb1_buf[l:l + 1, :] = small[7:8]
        for l in range(layers):
            for stage in BOTH:
                core_all(l, stage).wait_send()
            cross_copy(l).wait_send()
            dp_all(l, 0).wait_send()
            dp_all(l, 1).wait_send()
        for copy in ncop + gcop + (w_pair, w_cross, w_relay):
            copy.wait_send()
        dp_all(0, 2).wait_send()
        no_copy.wait_send()
        dn_copy.wait_send()
        for k in range(2 * layers):
            part_copy(k).wait_send()
        edges_sent(EDGE_OUT)
        with jax.named_scope('place_last'):
            group_arrived(GRAD_OUT, 2)
            loop(nch, place_g, last)
        edges_sent(GRAD_OUT)

    bf = lambda *s: pltpu.VMEM(s, BF)
    pl.run_scoped(
        scoped, bf(D, eh), bf(D, eh), bf(D, eh), bf(D, eh), bf(D, npad), bf(D, npad), bf(D, npad), bf(D, npad), bf(D, npad), bf(D, npad),
        pltpu.VMEM((eh, D), I16), pltpu.VMEM((eh, D), I16), pltpu.VMEM((eh // D * 16, D), I16), pltpu.VMEM((eh // D * 16, D), I16),
        pltpu.VMEM((T, D), I16), pltpu.VMEM((16, D), I16),
        bf(layers, 3 * D, D), bf(layers, D, 3 * D), bf(layers, D, D), bf(layers, D, D),
        bf(layers, 2 * D, D), bf(layers, D, 2 * D), bf(layers, D, D), bf(layers, D, D), pltpu.VMEM((D, D), F32))


def finish_kernel(*refs):
    count = len(refs) // 2
    sem = refs[-1]
    puts = [pltpu.make_async_copy(refs[k], refs[count + k], sem.at[k]) for k in range(count)]
    for put in puts:
        put.start()
    for put in puts:
        put.wait()


def keep_in_vmem(val):
    return pltpu.with_memory_space_constraint(val, pltpu.VMEM)


def finish(arrays):
    return pl.pallas_call(
        finish_kernel,
        name='finish',
        out_shape=[jax.ShapeDtypeStruct(a.shape, a.dtype) for a in arrays],
        in_specs=[VM] * len(arrays),
        out_specs=[HB] * len(arrays),
        scratch_shapes=[pltpu.SemaphoreType.DMA((len(arrays),))],
        compiler_params=pltpu.CompilerParams(vmem_limit_bytes=1 << 20),
    )(*[keep_in_vmem(a) for a in arrays])


def solution(mesh):
    lat_spec = P('dp', None, 'tp')
    first_spec = P(None, None, 'tp', None)
    col_spec = P(None, None, 'tp')
    param_specs = (first_spec, P(), col_spec, col_spec, first_spec, P(), col_spec, col_spec)
    in_specs = (lat_spec, lat_spec, P(), P(), lat_spec, lat_spec) + param_specs
    out_specs = (lat_spec, lat_spec, lat_spec, lat_spec) + param_specs
    shape = jax.ShapeDtypeStruct

    def local_step(node_lat, edge_lat, senders, receivers, grad_node, grad_edge, edge_w1, edge_b1, edge_w2, edge_vec, node_w1, node_b1, node_w2, node_vec):
        layers = edge_w1.shape[0]
        cols = node_lat.shape[2]
        nodes, edges = node_lat.shape[1], edge_lat.shape[1]
        npad = -(-nodes // TN) * TN
        eh = -(-edges // (2 * EC)) * EC
        nch = eh // EC
        dpn = mesh.shape['dp']
        per = SLABS // dpn
        dims = (layers, cols, nodes, edges, npad, eh, dpn)
        flat = lambda arr: jnp.swapaxes(arr, 1, 2)
        lead = lambda arr: jnp.transpose(arr, (1, 0, 2))
        args = (flat(node_lat), flat(edge_lat), flat(grad_node), flat(grad_edge), senders, receivers,
                edge_w1.reshape(-1, D), flat(edge_w2).reshape(-1, D), node_w1.reshape(-1, D), flat(node_w2).reshape(-1, D),
                lead(edge_vec), lead(node_vec), edge_b1, node_b1)
        vm, sem = pltpu.VMEM, pltpu.SemaphoreType.DMA
        wrows = -(-(HEAD + layers * LROWS) // (8 * dpn)) * 8 * dpn
        lat_n, lat_e = (2, cols, nodes), (2, cols, edges)
        outs = [RESULT(lat_n, BF), RESULT(lat_e, BF), RESULT(lat_n, BF), RESULT(lat_e, BF),
                RESULT((layers, 3, cols, D), F32), RESULT((layers, D), F32), RESULT((layers, cols, D), F32), RESULT((3, layers, cols), F32),
                RESULT((layers, 2, cols, D), F32), RESULT((layers, D), F32), RESULT((layers, cols, D), F32), RESULT((3, layers, cols), F32)]
        scratch = [
            *[vm(a.shape, a.dtype) for a in args[4:]], vm((wrows, D), F32), vm((3, wrows, D), F32),
            vm((2, cols, npad), F32), vm((3, cols, npad), F32), vm((2, cols, npad), F32), vm((3, cols, npad), F32),
            vm((cols, npad), F32), vm((cols, npad), F32), vm((cols, npad), F32), vm((cols, npad), F32),
            *[vm((3, nch, cols, EC), F32)] * 6,
            vm((2 * layers, D, npad), F32), vm((2 * layers, D, npad), F32),
            vm((layers, D, eh), F32), vm((layers, D, eh), F32), vm((8, eh), F32),
            vm((layers, D, npad), F32), vm((layers, D, npad), F32), vm((8, npad), F32),
            vm((D, npad), F32), vm((D, npad), F32), vm((D, npad), F32), vm((8, 2 * eh), jnp.int32), vm((D, D), F32), vm((layers, 2, 4 * D, D), F32),
            vm((layers, SLABS, D, D), F32), vm((layers, 2, SLABS, cols, D), F32), vm((layers, SLABS, 2, cols, D), F32),
            vm((layers, (dpn - 1) * per, 2, cols, D), F32), vm((layers, per, cols, D), F32), vm((layers, per, cols, D), F32),
            vm((layers, per, cols, D), F32), vm((layers, SLABS, cols, D), F32),
            sem((layers, 2)), sem((layers, 2)), sem((3, layers)), sem((3, layers)), sem((layers,)), sem((layers,)),
            sem((len(args),)), sem((3,)), sem((3,)), sem((3, 3)), sem((3, 3)), sem((4, 4)), sem((4, nch)),
            sem((2 * layers,)), sem((2 * layers,)), pltpu.SemaphoreType.REGULAR]
        res = pl.pallas_call(
            lambda *refs: step_kernel(dims, *refs),
            name='graph_step',
            out_shape=outs,
            in_specs=[HB] * len(args),
            out_specs=[VM] * len(outs),
            scratch_shapes=scratch,
            compiler_params=pltpu.CompilerParams(collective_id=0, has_side_effects=True, vmem_limit_bytes=VMEM_LIMIT),
        )(*args)

        res = finish(res)
        return (flat(res[0]), flat(res[1]), flat(res[2]), flat(res[3]),
                res[4], res[5], flat(res[6]), lead(res[7]), res[8], res[9], flat(res[10]), lead(res[11]))

    return jax.shard_map(local_step, mesh=mesh, in_specs=in_specs, out_specs=out_specs, check_vma=False)
```

```python
import jax
import jax.numpy as jnp
from jax import lax
from jax.experimental import pallas as pl
from jax.experimental.pallas import tpu as pltpu
from jax.sharding import PartitionSpec as P

LN_EPS = 1e-5
D = 128
T = 256
TN = 384
EC = 512
KS = 1408
BF = jnp.bfloat16
F32 = jnp.float32
I16 = jnp.int16
MESH = pl.DeviceIdType.MESH
VM = pl.BlockSpec(memory_space=pltpu.VMEM)
HB = pl.BlockSpec(memory_space=pl.ANY)
RESULT = pltpu.VMEM
GROUP = 4
BOTH = (0, 1)
THREE = (0, 1, 2)
OTHERS = (1, 2, 3)
EDGE_IN, GRAD_IN, EDGE_OUT, GRAD_OUT = range(4)
SEND_ORDER = (2, 3, 1)
LROWS = 7 * (D // 4)
HEAD = 16
LEADER = GROUP - 1
VMEM_LIMIT = 63_000_000
SLABS = 8
EARLY = 6
VEC_SLAB = 5
EDGE_SLABS = (0, 1, 6, 7)
STAGES = (slice(0, EARLY), slice(EARLY, SLABS))


def dot(a, b):
    return jnp.dot(a, b, preferred_element_type=F32)


def dot_nt(a, b):
    return lax.dot_general(a, b, (((1,), (1,)), ((), ())), preferred_element_type=F32)


def mat(k, n=1):
    return slice(k * D, (k + n) * D)


def rows_of(d):
    q = D // 4
    return slice(d * q, (d + 1) * q)


def at(step, width):
    return pl.ds(pl.multiple_of(step * width, width), width)


def loop(stop, body, start=0):
    def step(j, carry):
        body(j)
        return carry

    lax.fori_loop(start, stop, step, 0)


def column_sum(val):
    return jnp.sum(val, axis=0, keepdims=True)


def flip(val):
    return jnp.swapaxes(val, 0, 1)


def stacked(parts):
    return jnp.concatenate(parts, axis=0)


def beside(parts):
    return jnp.concatenate(parts, axis=1)


def slot(d):
    return d - 1


def sigmoid(hidden):
    return 1.0 / (1.0 + jnp.exp(-hidden))


def fold(val):
    total = val[:, mat(0)]
    for start in range(D, val.shape[1], D):
        total = total + val[:, start:start + D]
    return total


def swap_halves(val):
    return stacked([val[rows_of(d)] for d in (1, 0, 3, 2)])


def gather(table, keys, iota):
    acc = None
    nodes = table.shape[1]
    one, zero = jnp.ones((), BF), jnp.zeros((), BF)
    for base in range(0, nodes, T):
        width = min(T, nodes - base)
        ids = iota[0:width, :]
        hot = beside([jnp.where(ids == (key - jnp.asarray(base, I16)), one, zero) for key in keys])
        part = dot(table[:, base:base + width], hot)
        acc = part if acc is None else acc + part
    return acc


def scatter(acc_ref, val, cols, lanes):
    nodes = acc_ref.shape[1]
    one, zero = jnp.ones((), BF), jnp.zeros((), BF)
    row = lanes[0:1, :]
    for base in range(0, nodes, T):
        width = min(T, nodes - base)
        hot = beside([jnp.where((row + jnp.asarray(base + s, I16)) == cols, one, zero) for s in range(0, width, D)])
        acc_ref[:, base:base + width] += dot(val, hot)


def mlp_tail(hidden, w2t, vec):
    act = (hidden * sigmoid(hidden)).astype(BF)
    out = dot(w2t, act) + vec[0]
    mean = column_sum(out) / D
    centered = out - mean
    var = column_sum(centered * centered) / D
    inv = lax.rsqrt(var + LN_EPS)
    normed = centered * inv
    message = (normed * vec[1] + vec[2]).astype(BF)
    return message, normed, inv


def mlp_back(d_msg, hidden, normed, inv, w2, vec):
    d_normed = d_msg * vec[1]
    mean0 = column_sum(d_normed) / D
    mean1 = column_sum(d_normed * normed) / D
    d_out = inv * (d_normed - mean0 - normed * mean1)
    d_out_bf = d_out.astype(BF)
    sig = sigmoid(hidden)
    act = (hidden * sig).astype(BF)
    d_w2 = dot_nt(d_out_bf, act)
    d_hidden = dot(w2, d_out_bf) * (sig * (1.0 + hidden * (1.0 - sig)))
    sums = (fold(d_out), fold(d_msg * normed), fold(d_msg), fold(d_hidden))
    return d_hidden.astype(BF), d_w2, sums


def add_sums(ref, parts):
    for q in range(4):
        total = parts[0][q]
        for other in parts[1:]:
            total = total + other[q]
        ref[mat(q), :] += total


def step_kernel(dims, *refs):
    layers, cols, nodes, edges, npad, eh, dpn = dims
    nch = eh // EC
    top = layers - 1
    n_in = 14
    hbm_in = refs[:n_in]
    n_out = 12
    (node_raw, edge_raw, gnode_raw, gedge_raw, ew1_buf, eb1_buf, ew2_buf, evec_buf, nw1_buf, nb1_buf, nw2_buf, nvec_buf) = refs[n_in:n_in + n_out]
    (send_ids, recv_ids, ew1_in, ew2_in, nw1_in, nw2_in, evec_in, nvec_in, eb1_in, nb1_in, w_send, w_recv, n_send, n_recv, gn_send, gn_recv, no_send, no_recv, dn_send, dn_recv,
     e_send, g_send, e_recv, g_recv, eo_recv, de_recv, part, part_recv, hidden, normed, inv, nhid, nnrm, ninv, d_part, s_sum, r_sum,
     ids_raw, bias_cols, sums, grad, core_recv, half, dp_recv, cross_send, cross_recv, own_sum, gathered,
     core_ss, core_rs, dp_ss, dp_rs, cross_ss, cross_rs, load_sem, w_ss, w_rs, n_ss, n_rs, e_ss, e_rs, p_ss, p_rs, ready) = refs[n_in + n_out:]

    t = lax.axis_index('tp')
    p = lax.axis_index('dp')
    per = SLABS // dpn
    dp_others = range(1, dpn)
    x, c = t // 2, lax.rem(t, 2)
    ox, oc = 1 - x, 1 - c
    peer = [t, t + 1 - 2 * c, t + 2 - 4 * x, t + 3 - 2 * c - 4 * x]

    def remote(src, dst, ssem, rsem, d):
        return pltpu.make_async_remote_copy(src_ref=src, dst_ref=dst, send_sem=ssem, recv_sem=rsem,
                                            device_id={'tp': peer[d]}, device_id_type=MESH)

    small_in = (send_ids, recv_ids, ew1_in, ew2_in, nw1_in, nw2_in, evec_in, nvec_in, eb1_in, nb1_in)
    loads = [pltpu.make_async_copy(src, dst, load_sem.at[q]) for q, (src, dst) in enumerate(
        zip(hbm_in, (node_raw, edge_raw, gnode_raw, gedge_raw) + small_in))]

    def node_copies(send, recv, kind):
        return (remote(send.at[1], recv.at[0], n_ss.at[kind, 0], n_rs.at[kind, 0], 1),
                remote(send.at[0], recv.at[1], n_ss.at[kind, 1], n_rs.at[kind, 1], 2),
                remote(recv.at[1], recv.at[2], n_ss.at[kind, 2], n_rs.at[kind, 2], 1))

    piece = w_send.shape[0] // dpn

    def weight_rows(owner):
        return pl.ds(pl.multiple_of(owner * piece, 8), piece)

    w_pair = remote(w_send, w_recv.at[0], w_ss.at[0], w_rs.at[0], 1)
    w_cross = remote(w_send.at[weight_rows(p)], w_recv.at[1, weight_rows(p)], w_ss.at[1], w_rs.at[1], 2)
    w_relay = remote(w_recv.at[1], w_recv.at[2], w_ss.at[2], w_rs.at[2], 1)

    def weight_copy(i, owner):
        rows = w_recv.at[1, weight_rows(owner)]
        return dp_remote(rows, rows, 2, 0, i)

    last = nch - 1
    hold = nch - 3
    buffers = ((e_send, e_recv), (g_send, g_recv), (e_send, eo_recv), (g_send, de_recv))

    def outward(kind):
        return kind in (EDGE_OUT, GRAD_OUT)

    def edge_part(kind, index, send_sem, recv_sem, d):
        src, dst = buffers[kind]
        return remote(src.at[index], dst.at[index], e_ss.at[kind, send_sem], e_rs.at[kind, recv_sem], d)

    def by_half(half_id, j, action):
        narrow = jnp.logical_and(j == last, half_id == 1)

        @pl.when(jnp.logical_not(narrow))
        def _():
            action(slice(None))

        @pl.when(narrow)
        def _():
            action(slice(T))

    def edge_start(kind, j, d):
        other = oc if d % 2 else c
        if outward(kind):
            send_sem, recv_sem = jnp.where(j == last, 1, 0), jnp.where(j == last, 2 + slot(d), jnp.where(j < hold, 0, 1))
        else:
            send_sem, recv_sem = jnp.where(j == last, d, 0), j
        by_half(c if outward(kind) else other, j,
                lambda used: edge_part(kind, (slot(d), j, slice(None), used), send_sem, recv_sem, d).start())

    def edges_sent(kind):
        every = slice(None)
        edge_part(kind, (every, slice(0, last)), 0, 0, 1).wait_send()
        if outward(kind):
            by_half(c, last, lambda used: edge_part(kind, (every, last, every, used), 1, 0, 1).wait_send())
        else:
            for d in OTHERS:
                by_half(oc if d % 2 else c, last, lambda used: edge_part(kind, (slot(d), last, every, used), d, 0, d).wait_send())

    def chunk_arrived(kind, j):
        every = slice(None)
        by_half(c, j, lambda used: edge_part(kind, (every, j, every, used), 0, j, 1).wait_recv())

    def group_arrived(kind, group):
        every = slice(None)
        if group < 2:
            edge_part(kind, (every, (slice(0, hold), slice(hold, last))[group]), 0, group, 1).wait_recv()
        else:
            for d in OTHERS:
                by_half(oc if d % 2 else c, last, lambda used: edge_part(kind, (slot(d), last, every, used), 0, 2 + slot(d), d).wait_recv())

    def core_copy(l, b, stage):
        first, count = ((0, EARLY), (EARLY, SLABS - EARLY))[stage]
        return remote(grad.at[l, pl.ds(first, count), pl.ds((2 * b + 1) * cols, cols), :], core_recv.at[l, b, pl.ds(first, count)],
                      core_ss.at[l, stage], core_rs.at[l, stage], 1)

    def core_all(l, stage):
        part_of = core_recv.at[l, :, (slice(0, EARLY), slice(EARLY, SLABS))[stage]]
        return remote(part_of, part_of, core_ss.at[l, stage], core_rs.at[l, stage], 1)

    def seat(device):
        return lax.rem(device + dpn // 2, dpn)

    def in_stage(device, stage):
        early = (seat(device) + 1) * per <= EARLY
        return jnp.logical_not(early) if stage else early

    def dp_remote(src, dst, stage, l, i):
        return pltpu.make_async_remote_copy(src_ref=src, dst_ref=dst, send_sem=dp_ss.at[stage, l], recv_sem=dp_rs.at[stage, l],
                                            device_id={'dp': lax.rem(p + i, dpn)}, device_id_type=MESH)

    def spread_copy(l, i):
        return dp_remote(half.at[l, pl.ds(seat(lax.rem(p + i, dpn)) * per, per)], dp_recv.at[l, pl.ds((i - 1) * per, per)], 0, l, i)

    def dp_all(l, stage):
        most = (dpn - 1) * per
        part_of = (dp_recv.at[l], gathered.at[l, pl.ds(0, most)], w_recv.at[1, pl.ds(0, (dpn - 1) * piece)])[stage]
        return dp_remote(part_of, part_of, stage, l, 1)

    def cross_copy(l):
        return remote(cross_send.at[l], cross_recv.at[l], cross_ss.at[l], cross_rs.at[l], 2)

    def gather_copy(l, i, owner):
        return dp_remote(own_sum.at[l], gathered.at[l, pl.ds(seat(owner) * per, per)], 1, l, i)

    def part_copy(q):
        return remote(part.at[q], part_recv.at[q], p_ss.at[q], p_rs.at[q], 1)

    def load_nodes(raw, send, own):
        send[...] = jnp.zeros_like(send)
        send[0, :, :nodes] = raw[ox].astype(F32)
        send[1, :, :nodes] = raw[x].astype(F32)
        own[:cols, :] = send[1].astype(own.dtype)

    def load_edges(raw, send, own, kind):
        def put(j, lanes_j, val_of):
            for d in OTHERS:
                sample = x if d < 2 else ox
                send[slot(d), j] = val_of(sample, oc if d % 2 else c).astype(F32)
            own[:cols, lanes_j] = val_of(x, c)

        def chunk(j):
            put(j, at(j, EC), lambda s, h: raw[s, :, pl.ds(pl.multiple_of(h * eh + j * EC, D), EC)])
            for d in SEND_ORDER:
                edge_start(kind, j, d)

        loop(nch - 1, chunk)
        first = (nch - 1) * EC
        used = edges - eh - first
        last = pl.ds(first, EC)

        def tail(s, h):
            left = raw[s, :, pl.ds(first, EC)]
            right = beside([raw[s, :, pl.ds(eh + first, used)], jnp.zeros((cols, EC - used), BF)])
            return jnp.where(h == 0, left.astype(F32), right.astype(F32)).astype(BF)

        put(nch - 1, last, tail)
        for d in SEND_ORDER:
            edge_start(kind, nch - 1, d)

    def place_edges(raw, block, d, j):
        s = x if d < 2 else ox
        h = oc if d % 2 else c
        val = block.astype(BF)
        first = (nch - 1) * EC
        used = edges - eh - first

        @pl.when(jnp.logical_or(j < nch - 1, h == 0))
        def _():
            raw[s, :, pl.ds(pl.multiple_of(h * eh + j * EC, D), EC)] = val

        @pl.when(jnp.logical_and(j == nch - 1, h == 1))
        def _():
            raw[s, :, pl.ds(eh + first, used)] = val[:, :used]

    def scoped(e0, e1, ge, msg, v0, v1, v2, agg0, agg1, d_agg, scol, rcol, srow, rrow, iota, lanes, ew1, ew1t, ew2, ew2t, nw1, nw1t, nw2, nw2t, vecs):
        tables = (v0, v1, v2)
        aggs = (agg0, agg1)
        edges_in = (e0, e1)

        barrier = pltpu.get_barrier_semaphore()
        for d in OTHERS:
            pl.semaphore_signal(barrier, inc=1, device_id={'tp': peer[d]}, device_id_type=MESH)
        for copy in loads[:1] + loads[4:] + loads[1:4]:
            copy.start()
        loads[0].wait()
        with jax.named_scope('send_nodes'):
            load_nodes(node_raw, n_send, v0)
        ncop = node_copies(n_send, n_recv, 0)
        for copy in loads[4:]:
            copy.wait()
        q = cols
        w_send[:HEAD, :] = jnp.zeros((HEAD, D), F32)
        for k in THREE:
            w_send[k * layers:(k + 1) * layers, :cols] = evec_in[k]
            w_send[(3 + k) * layers:(4 + k) * layers, :cols] = nvec_in[k]
        for l in range(layers):
            off = HEAD + l * LROWS
            w_send[off:off + 3 * q, :] = ew1_in[l * 3 * q:(l + 1) * 3 * q, :].astype(F32)
            w_send[off + 3 * q:off + 4 * q, :] = ew2_in[l * q:(l + 1) * q, :].astype(F32)
            w_send[off + 4 * q:off + 6 * q, :] = nw1_in[l * 2 * q:(l + 1) * 2 * q, :].astype(F32)
            w_send[off + 6 * q:off + 7 * q, :] = nw2_in[l * q:(l + 1) * q, :].astype(F32)
        with jax.named_scope('barrier'):
            @pl.when(t != LEADER)
            def _():
                pl.semaphore_wait(barrier, len(OTHERS))
                pl.semaphore_signal(ready, inc=1, device_id={'tp': LEADER}, device_id_type=MESH)

            @pl.when(t == LEADER)
            def _():
                pl.semaphore_wait(ready, len(OTHERS))
                for i in dp_others:
                    pl.semaphore_signal(barrier, inc=1, device_id={'dp': lax.rem(p + i, dpn)}, device_id_type=MESH)

        w_cross.start()
        w_pair.start()
        ncop[1].start()
        ncop[0].start()
        loads[1].wait()
        with jax.named_scope('send_edges'):
            load_edges(edge_raw, e_send, e0, EDGE_IN)
        loads[2].wait()
        load_nodes(gnode_raw, gn_send, d_part)
        gcop = node_copies(gn_send, gn_recv, 1)
        gcop[1].start()
        gcop[0].start()
        loads[3].wait()
        with jax.named_scope('send_grads'):
            load_edges(gedge_raw, g_send, ge, GRAD_IN)

        with jax.named_scope('dp_barrier'):
            @pl.when(t == LEADER)
            def _():
                pl.semaphore_wait(barrier, len(OTHERS) + dpn - 1)
                for d in OTHERS:
                    pl.semaphore_signal(ready, inc=1, device_id={'tp': peer[d]}, device_id_type=MESH)

            @pl.when(t != LEADER)
            def _():
                pl.semaphore_wait(ready, 1)

        w_cross.wait_recv()
        for i in dp_others:
            weight_copy(i, p).start()

        @pl.when(c == 1)
        def _():
            for recv in (e_recv, g_recv):
                recv[:, nch - 1, :, T:] = jnp.zeros((3, cols, EC - T), F32)

        iota[...] = lax.broadcasted_iota(jnp.int32, (T, D), 0).astype(I16)
        lanes[...] = lax.broadcasted_iota(jnp.int32, (16, D), 1).astype(I16)

        ids_raw[...] = jnp.full(ids_raw.shape, -1, jnp.int32)
        for which, src in enumerate((send_ids, recv_ids)):
            ids_raw[which:which + 1, :edges] = src[...].reshape(1, edges)

        def ids(b):
            for which, (row_ref, col_ref) in enumerate(((srow, scol), (rrow, rcol))):
                wide = jnp.broadcast_to(ids_raw[which:which + 1, pl.ds(pl.multiple_of(c * eh + b * D, D), D)], (D, D))
                row_ref[at(b, 16), :] = wide[:16].astype(I16)
                col_ref[at(b, D), :] = flip(wide.astype(F32)).astype(jnp.int32).astype(I16)

        with jax.named_scope('ids'):
            loop(eh // D, ids)

        def keys(ref, step):
            return [ref[pl.ds(pl.multiple_of(step * (KS // D) * 16 + 16 * h, 16), 1), :] for h in range(KS // D)]

        bias_cols[...] = flip(stacked([eb1_in[...], nb1_in[...], jnp.zeros((D - 2 * layers, D), F32)]))

        def join_weights(l):
            off = HEAD + l * LROWS
            for d in range(GROUP):
                src = w_send if d == 0 else w_recv.at[slot(d)]
                r = slice(d * q, (d + 1) * q)
                for k in THREE:
                    ew1[l, k * D + d * q:k * D + (d + 1) * q, :] = src[off + k * q:off + (k + 1) * q, :].astype(BF)
                ew2t[l, r, :] = src[off + 3 * q:off + 4 * q, :].astype(BF)
                for k in range(2):
                    nw1[l, k * D + d * q:k * D + (d + 1) * q, :] = src[off + (4 + k) * q:off + (5 + k) * q, :].astype(BF)
                nw2t[l, r, :] = src[off + 6 * q:off + 7 * q, :].astype(BF)

            def flip_bf(mat):
                return flip(mat.astype(F32)).astype(BF)

            for k in THREE:
                ew1t[l, :, mat(k)] = flip_bf(ew1[l, mat(k), :])
            for k in range(2):
                nw1t[l, :, mat(k)] = flip_bf(nw1[l, mat(k), :])
            ew2[l] = flip_bf(ew2t[l])
            nw2[l] = flip_bf(nw2t[l])

        def wait_recvs(copies):
            copies[1].wait_recv()
            copies[2].start()
            copies[0].wait_recv()
            copies[2].wait_recv()

        with jax.named_scope('node_wait'):
            wait_recvs(ncop)
        for d in OTHERS:
            v0[rows_of(d), :] = n_recv[slot(d)].astype(BF)
        with jax.named_scope('weight_wait'):
            dp_all(0, 2).wait_recv()
            w_relay.start()
            w_pair.wait_recv()
            w_relay.wait_recv()
        rows_all = beside([w_send[:HEAD, :cols]] + [w_recv[d, :HEAD, :cols] for d in range(3)])
        vecs[...] = flip(stacked([rows_all, jnp.zeros((D - HEAD, D), F32)]))
        join_weights(0)

        def vec(l, node):
            first = 6 * node + l
            return [vecs[:, first + 2 * k:first + 2 * k + 1] for k in THREE]

        def bias(l, node):
            return bias_cols[:, node * layers + l:node * layers + l + 1]

        def hidden_of_nodes(l):
            table, b1 = tables[l], bias(l, 0)

            def body(step):
                xs = gather(table, keys(srow, step), iota).astype(BF)
                xr = gather(table, keys(rrow, step), iota).astype(BF)
                hidden[l, :, at(step, KS)] = dot(ew1t[l, :, mat(1, 2)], stacked([xs, xr])) + b1

            loop(eh // KS, body)

        def edge_forward(l):
            e_in = edges_in[l]

            def body(j):
                for sub in range(EC // T):
                    a = at(j * (EC // T) + sub, T)
                    if l == 0:
                        if sub == 0:
                            chunk_arrived(EDGE_IN, j)
                        for d in OTHERS:
                            e_in[rows_of(d), a] = e_recv[slot(d), j, :, sub * T:(sub + 1) * T].astype(BF)
                    e_val = e_in[:, a]
                    hid = hidden[l, :, a] + dot(ew1t[l, :, mat(0)], e_val)
                    hidden[l, :, a] = hid
                    message, nrm, std = mlp_tail(hid, ew2t[l], vec(l, 0))
                    normed[l, :, a] = nrm
                    inv[l:l + 1, a] = std
                    msg[:, a] = message
                    e_new = (e_val.astype(F32) + message.astype(F32)).astype(BF)
                    if l < top:
                        edges_in[l + 1][:, a] = e_new
                    else:
                        for d in OTHERS:
                            e_send[slot(d), j, :, sub * T:(sub + 1) * T] = e_new[rows_of(d)].astype(F32)
                        if sub == 0:
                            own_parts = []
                        own_parts.append(e_new[:q])
                if l == top:
                    for d in SEND_ORDER:
                        edge_start(EDGE_OUT, j, d)
                    place_edges(edge_raw, beside(own_parts), 0, j)

            loop(nch, body)

        def segment_sum(acc, ids_ref):
            acc[...] = jnp.zeros(acc.shape, F32)

            def body(step):
                scatter(acc, msg[:, at(step, KS)], ids_ref[at(step, KS), :], lanes)

            loop(eh // KS, body)

        def node_forward(l):
            table, agg, out = tables[l], aggs[l], tables[l + 1]

            def body(step):
                a = pl.ds(pl.multiple_of(step * TN, D), TN)
                v_in = table[:, a]
                agg_bf = (part[l, :, a] + swap_halves(part_recv[l, :, a])).astype(BF)
                agg[:, a] = agg_bf
                hid = dot(nw1t[l], stacked([v_in, agg_bf])) + bias(l, 1)
                nhid[l, :, a] = hid
                message, nrm, std = mlp_tail(hid, nw2t[l], vec(l, 1))
                nnrm[l, :, a] = nrm
                ninv[l:l + 1, a] = std
                out[:, a] = (v_in.astype(F32) + message.astype(F32)).astype(BF)

            loop(npad // TN, body)

        for l in range(layers):
            with jax.named_scope(f'gather_{l}'):
                hidden_of_nodes(l)
            if l == top:
                edges_sent(EDGE_IN)
            with jax.named_scope(f'edge_forward_{l}'):
                edge_forward(l)
            with jax.named_scope(f'sum_{l}'):
                segment_sum(part.at[l], rcol)
            part_copy(l).start()
            if l == 0:
                join_weights(1)
                gcop[1].wait_recv()
                gcop[2].start()
            with jax.named_scope(f'part_wait_{l}'):
                part_copy(l).wait_recv()
            with jax.named_scope(f'node_forward_{l}'):
                node_forward(l)
        no_send[...] = tables[layers][2 * q:3 * q, :].astype(F32)
        no_copy = remote(no_send, no_recv, n_ss.at[2, 0], n_rs.at[2, 0], 2)
        no_copy.start()
        node_raw[x] = tables[layers][:q, :nodes]

        grad[...] = jnp.zeros_like(grad)
        sums[...] = jnp.zeros_like(sums)
        with jax.named_scope('grad_node_wait'):
            gcop[0].wait_recv()
            gcop[2].wait_recv()
        for d in OTHERS:
            d_part[rows_of(d), :] = gn_recv[slot(d)]

        def node_backward(l):
            table, agg = tables[l], aggs[l]

            def body(step):
                a = pl.ds(pl.multiple_of(step * TN, D), TN)
                d_in = d_part[:, a]
                if l < top:
                    d_in = d_in + part[layers + l + 1, :, a] + swap_halves(part_recv[layers + l + 1, :, a])
                    d_in = d_in.astype(BF).astype(F32)
                d_hid, d_w2, parts = mlp_back(d_in, nhid[l, :, a], nnrm[l, :, a], ninv[l:l + 1, a], nw2[l], vec(l, 1))
                add_sums(sums.at[l, 1], [parts])
                grad[l, 4] += d_w2
                grad[l, 2] += dot_nt(table[:, a], d_hid)
                grad[l, 3] += dot_nt(agg[:, a], d_hid)
                d_part[:, a] = d_in + dot(nw1[l, mat(0), :], d_hid)
                d_agg[:, a] = dot(nw1[l, mat(1), :], d_hid).astype(BF)

            loop(npad // TN, body)

        def gather_back():
            def body(step):
                msg[:, at(step, KS)] = gather(d_agg, keys(rrow, step), iota).astype(BF)

            loop(eh // KS, body)

        def edge_backward(l):
            e_in = edges_in[l]

            def body(j):
                all_parts, d_w2s, d_w1s, own_parts = [], [], [], []
                for sub in range(EC // T):
                    a = at(j * (EC // T) + sub, T)
                    if l == top:
                        if sub == 0:
                            chunk_arrived(GRAD_IN, j)
                        for d in OTHERS:
                            ge[rows_of(d), a] = g_recv[slot(d), j, :, sub * T:(sub + 1) * T].astype(BF)
                    d_res = ge[:, a].astype(F32)
                    d_msg = d_res + msg[:, a].astype(F32)
                    d_hid, d_w2, parts = mlp_back(d_msg, hidden[l, :, a], normed[l, :, a], inv[l:l + 1, a], ew2[l], vec(l, 0))
                    all_parts.append(parts)
                    d_w2s.append(d_w2)
                    d_w1s.append(dot_nt(e_in[:, a], d_hid))
                    msg[:, a] = d_hid
                    d_new = (d_res + dot(ew1[l, mat(0), :], d_hid)).astype(BF)
                    if l > 0:
                        ge[:, a] = d_new
                    else:
                        for d in OTHERS:
                            g_send[slot(d), j, :, sub * T:(sub + 1) * T] = d_new[rows_of(d)].astype(F32)
                        own_parts.append(d_new[:q])
                add_sums(sums.at[l, 0], all_parts)
                grad[l, 1] += sum(d_w2s[1:], d_w2s[0])
                grad[l, 0] += sum(d_w1s[1:], d_w1s[0])
                if l == 0:
                    @pl.when(j < hold)
                    def _():
                        for d in SEND_ORDER:
                            edge_start(GRAD_OUT, j, d)
                    place_edges(gedge_raw, beside(own_parts), 0, j)

            loop(nch, body)

        def vector_slab(l):
            def total(node, k):
                return column_sum(flip(sums[l, node, mat(k), :]))

            lat = stacked([total(node, k) for node in BOTH for k in THREE])
            biases = stacked([total(node, 3) for node in BOTH])
            n_lat = lat.shape[0]
            for d in range(GROUP):
                grad[l, VEC_SLAB, d * cols:d * cols + n_lat, :cols] = lat[:, rows_of(d)]
                grad[l, VEC_SLAB, d * cols + n_lat:d * cols + n_lat + 2, :] = biases

        def reduce_start(l, stage):
            for b in BOTH:
                core_copy(l, b, stage).start()

        def chip_sum(l, stage):
            row = lax.broadcasted_iota(jnp.int32, (cols, D), 0)
            edge_row = jnp.logical_or(row < 3, row == 6)
            core_all(l, stage).wait_recv()
            for b in BOTH:
                for k in range(SLABS)[STAGES[stage]]:
                    own = grad[l, k, rows_of(2 * b), :]
                    if k in EDGE_SLABS:
                        own = own + core_recv[l, b, k]
                    elif k == VEC_SLAB:
                        own = own + jnp.where(edge_row, core_recv[l, b, k], 0.0)
                    half[l, k, b] = own
            for i in dp_others:
                @pl.when(in_stage(lax.rem(p + i, dpn), stage))
                def _():
                    spread_copy(l, i).start()

        def dp_sum(l, stage):
            @pl.when(in_stage(p, stage))
            def _():
                total = half[l, pl.ds(seat(p) * per, per)]
                dp_all(l, 0).wait_recv()
                for i in dp_others:
                    total = total + dp_recv[l, pl.ds((i - 1) * per, per)]
                own_sum[l] = total[:, 0]
                cross_send[l] = total[:, 1]
                cross_copy(l).start()

        def cross_sum(l):
            cross_copy(l).wait_recv()
            total = own_sum[l] + cross_recv[l]
            own_sum[l] = total
            gathered[l, pl.ds(seat(p) * per, per)] = total
            for i in dp_others:
                gather_copy(l, i, p).start()

        def project(l):
            table = tables[l]

            def body(step):
                a = pl.ds(pl.multiple_of(step * TN, D), TN)
                s_bf, r_bf, v_in = s_sum[:, a].astype(BF), r_sum[:, a].astype(BF), table[:, a]
                part[layers + l, :, a] = dot(ew1[l, mat(1), :], s_bf) + dot(ew1[l, mat(2), :], r_bf)
                grad[l, 6] += dot_nt(v_in, s_bf)
                grad[l, 7] += dot_nt(v_in, r_bf)

            loop(npad // TN, body)

        for l in reversed(range(layers)):
            first_layer = l == 0
            with jax.named_scope(f'node_backward_{l}'):
                node_backward(l)
            if first_layer:
                with jax.named_scope('chip_sum_1'):
                    chip_sum(1, 0)
                    chip_sum(1, 1)
            with jax.named_scope(f'gather_back_{l}'):
                gather_back()
            if first_layer:
                edges_sent(GRAD_IN)
            with jax.named_scope(f'edge_backward_{l}'):
                edge_backward(l)
            vector_slab(l)
            reduce_start(l, 0)
            if first_layer:
                with jax.named_scope('dp_sum_1'):
                    dp_sum(1, 0)
                    dp_sum(1, 1)
            with jax.named_scope(f'sum_send_{l}'):
                segment_sum(s_sum, scol)
            if first_layer:
                with jax.named_scope('chip_sum_0'):
                    chip_sum(0, 0)
            with jax.named_scope(f'sum_recv_{l}'):
                segment_sum(r_sum, rcol)
            with jax.named_scope(f'project_{l}'):
                project(l)
            reduce_start(l, 1)
            part_copy(layers + l).start()
            if first_layer:
                with jax.named_scope('chip_sum_late'):
                    chip_sum(0, 1)
                with jax.named_scope('dp_sum_0'):
                    dp_sum(0, 0)
            with jax.named_scope(f'back_wait_{l}'):
                part_copy(layers + l).wait_recv()

        def final(step):
            a = pl.ds(pl.multiple_of(step * TN, D), TN)
            d_in = (d_part[:, a] + part[layers, :, a] + swap_halves(part_recv[layers, :, a])).astype(BF)
            v2[:, a] = d_in

        loop(npad // TN, final)
        gnode_raw[x] = v2[:q, :nodes]
        with jax.named_scope('dp_sum_late'):
            dp_sum(0, 1)

        dn_send[...] = v2[2 * q:3 * q, :].astype(F32)
        dn_copy = remote(dn_send, dn_recv, n_ss.at[2, 1], n_rs.at[2, 1], 2)
        dn_copy.start()

        def send_rest(j):
            for d in SEND_ORDER:
                edge_start(GRAD_OUT, j, d)

        loop(nch, send_rest, hold)

        with jax.named_scope('node_out_wait'):
            no_copy.wait_recv()
        node_raw[ox] = no_recv[:, :nodes].astype(BF)

        def place_e(j):
            for d in OTHERS:
                place_edges(edge_raw, eo_recv[slot(d), j], d, j)

        with jax.named_scope('place_edge_out'):
            for group in THREE:
                group_arrived(EDGE_OUT, group)
            loop(nch, place_e)

        def place_g(j):
            for d in OTHERS:
                place_edges(gedge_raw, de_recv[slot(d), j], d, j)

        with jax.named_scope('place_first'):
            group_arrived(GRAD_OUT, 0)
            loop(hold, place_g)
        for l in range(layers):
            with jax.named_scope(f'cross_sum_{l}'):
                cross_sum(l)
        with jax.named_scope('d_node_wait'):
            dn_copy.wait_recv()
        gnode_raw[ox] = dn_recv[:, :nodes].astype(BF)
        with jax.named_scope('place_rest'):
            group_arrived(GRAD_OUT, 1)
            loop(last, place_g, hold)
        for l in range(layers):
            dp_all(l, 1).wait_recv()
            ew1_buf[l, 0] = gathered[l, 0]
            ew1_buf[l, 1:] = gathered[l, EARLY:]
            ew2_buf[l] = gathered[l, 1]
            nw1_buf[l] = gathered[l, 2:4]
            nw2_buf[l] = gathered[l, 4]
            small = gathered[l, VEC_SLAB]
            for k in THREE:
                evec_buf[k, l:l + 1, :] = small[k:k + 1, :cols]
                nvec_buf[k, l:l + 1, :] = small[3 + k:4 + k, :cols]
            eb1_buf[l:l + 1, :] = small[6:7]
            nb1_buf[l:l + 1, :] = small[7:8]
        for l in range(layers):
            for stage in BOTH:
                core_all(l, stage).wait_send()
            cross_copy(l).wait_send()
            dp_all(l, 0).wait_send()
            dp_all(l, 1).wait_send()
        for copy in ncop + gcop + (w_pair, w_cross, w_relay):
            copy.wait_send()
        dp_all(0, 2).wait_send()
        no_copy.wait_send()
        dn_copy.wait_send()
        for k in range(2 * layers):
            part_copy(k).wait_send()
        edges_sent(EDGE_OUT)
        with jax.named_scope('place_last'):
            group_arrived(GRAD_OUT, 2)
            loop(nch, place_g, last)
        edges_sent(GRAD_OUT)

    bf = lambda *s: pltpu.VMEM(s, BF)
    pl.run_scoped(
        scoped, bf(D, eh), bf(D, eh), bf(D, eh), bf(D, eh), bf(D, npad), bf(D, npad), bf(D, npad), bf(D, npad), bf(D, npad), bf(D, npad),
        pltpu.VMEM((eh, D), I16), pltpu.VMEM((eh, D), I16), pltpu.VMEM((eh // D * 16, D), I16), pltpu.VMEM((eh // D * 16, D), I16),
        pltpu.VMEM((T, D), I16), pltpu.VMEM((16, D), I16),
        bf(layers, 3 * D, D), bf(layers, D, 3 * D), bf(layers, D, D), bf(layers, D, D),
        bf(layers, 2 * D, D), bf(layers, D, 2 * D), bf(layers, D, D), bf(layers, D, D), pltpu.VMEM((D, D), F32))


def finish_kernel(*refs):
    count = len(refs) // 2
    sem = refs[-1]
    puts = [pltpu.make_async_copy(refs[k], refs[count + k], sem.at[k]) for k in range(count)]
    for put in puts:
        put.start()
    for put in puts:
        put.wait()


def keep_in_vmem(val):
    return pltpu.with_memory_space_constraint(val, pltpu.VMEM)


def finish(arrays):
    return pl.pallas_call(
        finish_kernel,
        name='finish',
        out_shape=[jax.ShapeDtypeStruct(a.shape, a.dtype) for a in arrays],
        in_specs=[VM] * len(arrays),
        out_specs=[HB] * len(arrays),
        scratch_shapes=[pltpu.SemaphoreType.DMA((len(arrays),))],
        compiler_params=pltpu.CompilerParams(vmem_limit_bytes=1 << 20),
    )(*[keep_in_vmem(a) for a in arrays])


def solution(mesh):
    lat_spec = P('dp', None, 'tp')
    first_spec = P(None, None, 'tp', None)
    col_spec = P(None, None, 'tp')
    param_specs = (first_spec, P(), col_spec, col_spec, first_spec, P(), col_spec, col_spec)
    in_specs = (lat_spec, lat_spec, P(), P(), lat_spec, lat_spec) + param_specs
    out_specs = (lat_spec, lat_spec, lat_spec, lat_spec) + param_specs
    shape = jax.ShapeDtypeStruct

    def local_step(node_lat, edge_lat, senders, receivers, grad_node, grad_edge, edge_w1, edge_b1, edge_w2, edge_vec, node_w1, node_b1, node_w2, node_vec):
        layers = edge_w1.shape[0]
        cols = node_lat.shape[2]
        nodes, edges = node_lat.shape[1], edge_lat.shape[1]
        npad = -(-nodes // TN) * TN
        eh = -(-edges // (2 * EC)) * EC
        nch = eh // EC
        dpn = mesh.shape['dp']
        per = SLABS // dpn
        dims = (layers, cols, nodes, edges, npad, eh, dpn)
        flat = lambda arr: jnp.swapaxes(arr, 1, 2)
        lead = lambda arr: jnp.transpose(arr, (1, 0, 2))
        args = (flat(node_lat), flat(edge_lat), flat(grad_node), flat(grad_edge), senders, receivers,
                edge_w1.reshape(-1, D), flat(edge_w2).reshape(-1, D), node_w1.reshape(-1, D), flat(node_w2).reshape(-1, D),
                lead(edge_vec), lead(node_vec), edge_b1, node_b1)
        vm, sem = pltpu.VMEM, pltpu.SemaphoreType.DMA
        wrows = -(-(HEAD + layers * LROWS) // (8 * dpn)) * 8 * dpn
        lat_n, lat_e = (2, cols, nodes), (2, cols, edges)
        outs = [RESULT(lat_n, BF), RESULT(lat_e, BF), RESULT(lat_n, BF), RESULT(lat_e, BF),
                RESULT((layers, 3, cols, D), F32), RESULT((layers, D), F32), RESULT((layers, cols, D), F32), RESULT((3, layers, cols), F32),
                RESULT((layers, 2, cols, D), F32), RESULT((layers, D), F32), RESULT((layers, cols, D), F32), RESULT((3, layers, cols), F32)]
        scratch = [
            *[vm(a.shape, a.dtype) for a in args[4:]], vm((wrows, D), F32), vm((3, wrows, D), F32),
            vm((2, cols, npad), F32), vm((3, cols, npad), F32), vm((2, cols, npad), F32), vm((3, cols, npad), F32),
            vm((cols, npad), F32), vm((cols, npad), F32), vm((cols, npad), F32), vm((cols, npad), F32),
            *[vm((3, nch, cols, EC), F32)] * 6,
            vm((2 * layers, D, npad), F32), vm((2 * layers, D, npad), F32),
            vm((layers, D, eh), F32), vm((layers, D, eh), F32), vm((8, eh), F32),
            vm((layers, D, npad), F32), vm((layers, D, npad), F32), vm((8, npad), F32),
            vm((D, npad), F32), vm((D, npad), F32), vm((D, npad), F32), vm((8, 2 * eh), jnp.int32), vm((D, D), F32), vm((layers, 2, 4 * D, D), F32),
            vm((layers, SLABS, D, D), F32), vm((layers, 2, SLABS, cols, D), F32), vm((layers, SLABS, 2, cols, D), F32),
            vm((layers, (dpn - 1) * per, 2, cols, D), F32), vm((layers, per, cols, D), F32), vm((layers, per, cols, D), F32),
            vm((layers, per, cols, D), F32), vm((layers, SLABS, cols, D), F32),
            sem((layers, 2)), sem((layers, 2)), sem((3, layers)), sem((3, layers)), sem((layers,)), sem((layers,)),
            sem((len(args),)), sem((3,)), sem((3,)), sem((3, 3)), sem((3, 3)), sem((4, 4)), sem((4, nch)),
            sem((2 * layers,)), sem((2 * layers,)), pltpu.SemaphoreType.REGULAR]
        res = pl.pallas_call(
            lambda *refs: step_kernel(dims, *refs),
            name='graph_step',
            out_shape=outs,
            in_specs=[HB] * len(args),
            out_specs=[VM] * len(outs),
            scratch_shapes=scratch,
            compiler_params=pltpu.CompilerParams(collective_id=0, has_side_effects=True, vmem_limit_bytes=VMEM_LIMIT),
        )(*args)

        res = finish(res)
        return (flat(res[0]), flat(res[1]), flat(res[2]), flat(res[3]),
                res[4], res[5], flat(res[6]), lead(res[7]), res[8], res[9], flat(res[10]), lead(res[11]))

    return jax.shard_map(local_step, mesh=mesh, in_specs=in_specs, out_specs=out_specs, check_vma=False)
```

```python
import jax
import jax.numpy as jnp
from jax import lax
from jax.experimental import pallas as pl
from jax.experimental.pallas import tpu as pltpu
from jax.sharding import PartitionSpec as P

LN_EPS = 1e-5
D = 128
T = 256
TN = 384
EC = 512
KS = 1408
BF = jnp.bfloat16
F32 = jnp.float32
I16 = jnp.int16
MESH = pl.DeviceIdType.MESH
VM = pl.BlockSpec(memory_space=pltpu.VMEM)
HB = pl.BlockSpec(memory_space=pl.ANY)
RESULT = pltpu.VMEM
GROUP = 4
BOTH = (0, 1)
THREE = (0, 1, 2)
OTHERS = (1, 2, 3)
EDGE_IN, GRAD_IN, EDGE_OUT, GRAD_OUT = range(4)
SEND_ORDER = (2, 3, 1)
LROWS = 7 * (D // 4)
HEAD = 16
LEADER = GROUP - 1
FINISH_SEMS = 40
VMEM_LIMIT = 63_000_000
SLABS = 8
EARLY = 6
VEC_SLAB = 5
EDGE_SLABS = (0, 1, 6, 7)
STAGES = (slice(0, EARLY), slice(EARLY, SLABS))


def dot(a, b):
    return jnp.dot(a, b, preferred_element_type=F32)


def dot_nt(a, b):
    return lax.dot_general(a, b, (((1,), (1,)), ((), ())), preferred_element_type=F32)


def mat(k, n=1):
    return slice(k * D, (k + n) * D)


def rows_of(d):
    q = D // 4
    return slice(d * q, (d + 1) * q)


def at(step, width):
    return pl.ds(pl.multiple_of(step * width, width), width)


def loop(stop, body, start=0):
    def step(j, carry):
        body(j)
        return carry

    lax.fori_loop(start, stop, step, 0)


def column_sum(val):
    return jnp.sum(val, axis=0, keepdims=True)


def flip(val):
    return jnp.swapaxes(val, 0, 1)


def stacked(parts):
    return jnp.concatenate(parts, axis=0)


def beside(parts):
    return jnp.concatenate(parts, axis=1)


def slot(d):
    return d - 1


def sigmoid(hidden):
    return 1.0 / (1.0 + jnp.exp(-hidden))


def fold(val):
    total = val[:, mat(0)]
    for start in range(D, val.shape[1], D):
        total = total + val[:, start:start + D]
    return total


def swap_halves(val):
    return stacked([val[rows_of(d)] for d in (1, 0, 3, 2)])


def gather(table, keys, iota):
    acc = None
    nodes = table.shape[1]
    one, zero = jnp.ones((), BF), jnp.zeros((), BF)
    for base in range(0, nodes, T):
        width = min(T, nodes - base)
        ids = iota[0:width, :]
        hot = beside([jnp.where(ids == (key - jnp.asarray(base, I16)), one, zero) for key in keys])
        part = dot(table[:, base:base + width], hot)
        acc = part if acc is None else acc + part
    return acc


def scatter(acc_ref, val, cols, lanes):
    nodes = acc_ref.shape[1]
    one, zero = jnp.ones((), BF), jnp.zeros((), BF)
    row = lanes[0:1, :]
    for base in range(0, nodes, T):
        width = min(T, nodes - base)
        hot = beside([jnp.where((row + jnp.asarray(base + s, I16)) == cols, one, zero) for s in range(0, width, D)])
        acc_ref[:, base:base + width] += dot(val, hot)


def mlp_tail(hidden, w2t, vec):
    act = (hidden * sigmoid(hidden)).astype(BF)
    out = dot(w2t, act) + vec[0]
    mean = column_sum(out) / D
    centered = out - mean
    var = column_sum(centered * centered) / D
    inv = lax.rsqrt(var + LN_EPS)
    normed = centered * inv
    message = (normed * vec[1] + vec[2]).astype(BF)
    return message, normed, inv


def mlp_back(d_msg, hidden, normed, inv, w2, vec):
    d_normed = d_msg * vec[1]
    mean0 = column_sum(d_normed) / D
    mean1 = column_sum(d_normed * normed) / D
    d_out = inv * (d_normed - mean0 - normed * mean1)
    d_out_bf = d_out.astype(BF)
    sig = sigmoid(hidden)
    act = (hidden * sig).astype(BF)
    d_w2 = dot_nt(d_out_bf, act)
    d_hidden = dot(w2, d_out_bf) * (sig * (1.0 + hidden * (1.0 - sig)))
    sums = (fold(d_out), fold(d_msg * normed), fold(d_msg), fold(d_hidden))
    return d_hidden.astype(BF), d_w2, sums


def add_sums(ref, parts):
    for q in range(4):
        total = parts[0][q]
        for other in parts[1:]:
            total = total + other[q]
        ref[mat(q), :] += total


def step_kernel(dims, *refs):
    layers, cols, nodes, edges, npad, eh, dpn = dims
    nch = eh // EC
    top = layers - 1
    n_in = 14
    hbm_in = refs[:n_in]
    n_out = 12
    (node_raw, edge_raw, gnode_raw, gedge_raw, ew1_buf, eb1_buf, ew2_buf, evec_buf, nw1_buf, nb1_buf, nw2_buf, nvec_buf) = refs[n_in:n_in + n_out]
    (send_ids, recv_ids, ew1_in, ew2_in, nw1_in, nw2_in, evec_in, nvec_in, eb1_in, nb1_in, w_send, w_recv, n_send, n_recv, gn_send, gn_recv, no_send, no_recv, dn_send, dn_recv,
     e_send, g_send, e_recv, g_recv, eo_recv, de_recv, part, part_recv, hidden, normed, inv, nhid, nnrm, ninv, d_part, s_sum, r_sum,
     ids_raw, bias_cols, sums, grad, core_recv, half, dp_recv, cross_send, cross_recv, own_sum, gathered,
     core_ss, core_rs, dp_ss, dp_rs, cross_ss, cross_rs, load_sem, w_ss, w_rs, n_ss, n_rs, e_ss, e_rs, o_rs, p_ss, p_rs, ready) = refs[n_in + n_out:]

    t = lax.axis_index('tp')
    p = lax.axis_index('dp')
    per = SLABS // dpn
    dp_others = range(1, dpn)
    x, c = t // 2, lax.rem(t, 2)
    ox, oc = 1 - x, 1 - c
    peer = [t, t + 1 - 2 * c, t + 2 - 4 * x, t + 3 - 2 * c - 4 * x]

    def remote(src, dst, ssem, rsem, d):
        return pltpu.make_async_remote_copy(src_ref=src, dst_ref=dst, send_sem=ssem, recv_sem=rsem,
                                            device_id={'tp': peer[d]}, device_id_type=MESH)

    small_in = (send_ids, recv_ids, ew1_in, ew2_in, nw1_in, nw2_in, evec_in, nvec_in, eb1_in, nb1_in)
    loads = [pltpu.make_async_copy(src, dst, load_sem.at[q]) for q, (src, dst) in enumerate(
        zip(hbm_in, (node_raw, edge_raw, gnode_raw, gedge_raw) + small_in))]

    def node_copies(send, recv, kind):
        return (remote(send.at[1], recv.at[0], n_ss.at[kind, 0], n_rs.at[kind, 0], 1),
                remote(send.at[0], recv.at[1], n_ss.at[kind, 1], n_rs.at[kind, 1], 2),
                remote(recv.at[1], recv.at[2], n_ss.at[kind, 2], n_rs.at[kind, 2], 1))

    piece = w_send.shape[0] // dpn

    def packed(l, k, count=1):
        return pl.ds(HEAD + l * LROWS + k * cols, count * cols)

    def weight_rows(owner):
        return pl.ds(pl.multiple_of(owner * piece, 8), piece)

    w_pair = remote(w_send, w_recv.at[0], w_ss.at[0], w_rs.at[0], 1)
    w_cross = remote(w_send.at[weight_rows(p)], w_recv.at[1, weight_rows(p)], w_ss.at[1], w_rs.at[1], 2)
    w_relay = remote(w_recv.at[1], w_recv.at[2], w_ss.at[2], w_rs.at[2], 1)

    def weight_copy(i, owner):
        rows = w_recv.at[1, weight_rows(owner)]
        return dp_remote(rows, rows, 2, 0, i)

    last = nch - 1
    hold = nch - 3
    buffers = ((e_send, e_recv), (g_send, g_recv), (e_send, eo_recv), (g_send, de_recv))

    def outward(kind):
        return kind in (EDGE_OUT, GRAD_OUT)

    def edge_part(kind, index, send_sem, recv_sem, d):
        src, dst = buffers[kind]
        recv_sems = o_rs.at[kind - EDGE_OUT, recv_sem] if outward(kind) else e_rs.at[kind, recv_sem]
        return remote(src.at[index], dst.at[index], e_ss.at[kind, send_sem], recv_sems, d)

    def by_half(half_id, j, action):
        narrow = jnp.logical_and(j == last, half_id == 1)

        @pl.when(jnp.logical_not(narrow))
        def _():
            action(slice(None))

        @pl.when(narrow)
        def _():
            action(slice(T))

    def edge_start(kind, j, d):
        other = oc if d % 2 else c
        if outward(kind):
            send_sem, recv_sem = jnp.where(j == last, 1, 0), jnp.where(j == last, 2 + slot(d), jnp.where(j < hold, 0, 1))
        else:
            send_sem, recv_sem = jnp.where(j == last, d, 0), j
        by_half(c if outward(kind) else other, j,
                lambda used: edge_part(kind, (slot(d), j, slice(None), used), send_sem, recv_sem, d).start())

    def edges_sent(kind):
        every = slice(None)
        edge_part(kind, (every, slice(0, last)), 0, 0, 1).wait_send()
        if outward(kind):
            by_half(c, last, lambda used: edge_part(kind, (every, last, every, used), 1, 0, 1).wait_send())
        else:
            for d in OTHERS:
                by_half(oc if d % 2 else c, last, lambda used: edge_part(kind, (slot(d), last, every, used), d, 0, d).wait_send())

    def chunk_arrived(kind, j):
        every = slice(None)
        by_half(c, j, lambda used: edge_part(kind, (every, j, every, used), 0, j, 1).wait_recv())

    def group_arrived(kind, group):
        every = slice(None)
        if group < 2:
            edge_part(kind, (every, (slice(0, hold), slice(hold, last))[group]), 0, group, 1).wait_recv()
        else:
            for d in OTHERS:
                by_half(oc if d % 2 else c, last, lambda used: edge_part(kind, (slot(d), last, every, used), 0, 2 + slot(d), d).wait_recv())

    def core_copy(l, b, stage):
        first, count = ((0, EARLY), (EARLY, SLABS - EARLY))[stage]
        return remote(grad.at[l, pl.ds(first, count), pl.ds((2 * b + 1) * cols, cols), :], core_recv.at[l, b, pl.ds(first, count)],
                      core_ss.at[l, stage], core_rs.at[l, stage], 1)

    def core_all(l, stage):
        part_of = core_recv.at[l, :, (slice(0, EARLY), slice(EARLY, SLABS))[stage]]
        return remote(part_of, part_of, core_ss.at[l, stage], core_rs.at[l, stage], 1)

    def seat(device):
        return lax.rem(device + dpn // 2, dpn)

    def in_stage(device, stage):
        early = (seat(device) + 1) * per <= EARLY
        return jnp.logical_not(early) if stage else early

    def dp_remote(src, dst, stage, l, i):
        return pltpu.make_async_remote_copy(src_ref=src, dst_ref=dst, send_sem=dp_ss.at[stage, l], recv_sem=dp_rs.at[stage, l],
                                            device_id={'dp': lax.rem(p + i, dpn)}, device_id_type=MESH)

    def spread_copy(l, i):
        return dp_remote(half.at[l, pl.ds(seat(lax.rem(p + i, dpn)) * per, per)], dp_recv.at[l, pl.ds((i - 1) * per, per)], 0, l, i)

    def dp_all(l, stage):
        most = (dpn - 1) * per
        part_of = (dp_recv.at[l], gathered.at[l, pl.ds(0, most)], w_recv.at[1, pl.ds(0, (dpn - 1) * piece)])[stage]
        return dp_remote(part_of, part_of, stage, l, 1)

    def cross_copy(l):
        return remote(cross_send.at[l], cross_recv.at[l], cross_ss.at[l], cross_rs.at[l], 2)

    def gather_copy(l, i, owner):
        return dp_remote(own_sum.at[l], gathered.at[l, pl.ds(seat(owner) * per, per)], 1, l, i)

    def part_copy(q):
        return remote(part.at[q], part_recv.at[q], p_ss.at[q], p_rs.at[q], 1)

    def load_nodes(raw, send, own):
        send[...] = jnp.zeros_like(send)
        send[0, :, :nodes] = raw[ox].astype(F32)
        send[1, :, :nodes] = raw[x].astype(F32)
        own[:cols, :] = send[1].astype(own.dtype)

    def load_edges(raw, send, own, kind):
        def put(j, lanes_j, val_of):
            for d in OTHERS:
                sample = x if d < 2 else ox
                send[slot(d), j] = val_of(sample, oc if d % 2 else c).astype(F32)
            own[:cols, lanes_j] = val_of(x, c)

        def chunk(j):
            put(j, at(j, EC), lambda s, h: raw[s, :, pl.ds(pl.multiple_of(h * eh + j * EC, D), EC)])
            for d in SEND_ORDER:
                edge_start(kind, j, d)

        loop(nch - 1, chunk)
        first = (nch - 1) * EC
        used = edges - eh - first
        last = pl.ds(first, EC)

        def tail(s, h):
            left = raw[s, :, pl.ds(first, EC)]
            right = beside([raw[s, :, pl.ds(eh + first, used)], jnp.zeros((cols, EC - used), BF)])
            return jnp.where(h == 0, left.astype(F32), right.astype(F32)).astype(BF)

        put(nch - 1, last, tail)
        for d in SEND_ORDER:
            edge_start(kind, nch - 1, d)

    def place_edges(raw, block, d, j):
        s = x if d < 2 else ox
        h = oc if d % 2 else c
        val = block.astype(BF)
        first = (nch - 1) * EC
        used = edges - eh - first

        @pl.when(jnp.logical_or(j < nch - 1, h == 0))
        def _():
            raw[s, :, pl.ds(pl.multiple_of(h * eh + j * EC, D), EC)] = val

        @pl.when(jnp.logical_and(j == nch - 1, h == 1))
        def _():
            raw[s, :, pl.ds(eh + first, used)] = val[:, :used]

    def scoped(e0, e1, ge, msg, v0, v1, v2, agg0, agg1, d_agg, scol, rcol, srow, rrow, iota, lanes, ew1, ew1t, ew2, ew2t, nw1, nw1t, nw2, nw2t, vecs):
        tables = (v0, v1, v2)
        aggs = (agg0, agg1)
        edges_in = (e0, e1)

        barrier = pltpu.get_barrier_semaphore()
        for d in OTHERS:
            pl.semaphore_signal(barrier, inc=1, device_id={'tp': peer[d]}, device_id_type=MESH)
        for copy in loads[:1] + loads[4:] + loads[1:4]:
            copy.start()
        loads[0].wait()
        with jax.named_scope('send_nodes'):
            load_nodes(node_raw, n_send, v0)
        ncop = node_copies(n_send, n_recv, 0)
        for copy in loads[4:]:
            copy.wait()
        q = cols
        w_send[:HEAD, :] = jnp.zeros((HEAD, D), F32)
        for k in THREE:
            w_send[k * layers:(k + 1) * layers, :cols] = evec_in[k]
            w_send[(3 + k) * layers:(4 + k) * layers, :cols] = nvec_in[k]
        for l in range(layers):
            w_send[packed(l, 0, 3), :] = ew1_in[pl.ds(l * 3 * q, 3 * q), :].astype(F32)
            w_send[packed(l, 3), :] = ew2_in[pl.ds(l * q, q), :].astype(F32)
            w_send[packed(l, 4, 2), :] = nw1_in[pl.ds(l * 2 * q, 2 * q), :].astype(F32)
            w_send[packed(l, 6), :] = nw2_in[pl.ds(l * q, q), :].astype(F32)
        with jax.named_scope('barrier'):
            @pl.when(t != LEADER)
            def _():
                pl.semaphore_wait(barrier, len(OTHERS))
                pl.semaphore_signal(ready, inc=1, device_id={'tp': LEADER}, device_id_type=MESH)

            @pl.when(t == LEADER)
            def _():
                pl.semaphore_wait(ready, len(OTHERS))
                for i in dp_others:
                    pl.semaphore_signal(barrier, inc=1, device_id={'dp': lax.rem(p + i, dpn)}, device_id_type=MESH)

        w_cross.start()
        w_pair.start()
        ncop[1].start()
        ncop[0].start()
        loads[1].wait()
        with jax.named_scope('send_edges'):
            load_edges(edge_raw, e_send, e0, EDGE_IN)
        loads[2].wait()
        load_nodes(gnode_raw, gn_send, d_part)
        gcop = node_copies(gn_send, gn_recv, 1)
        gcop[1].start()
        gcop[0].start()
        loads[3].wait()
        with jax.named_scope('send_grads'):
            load_edges(gedge_raw, g_send, ge, GRAD_IN)

        with jax.named_scope('dp_barrier'):
            @pl.when(t == LEADER)
            def _():
                pl.semaphore_wait(barrier, len(OTHERS) + dpn - 1)
                for d in OTHERS:
                    pl.semaphore_signal(ready, inc=1, device_id={'tp': peer[d]}, device_id_type=MESH)

            @pl.when(t != LEADER)
            def _():
                pl.semaphore_wait(ready, 1)

        w_cross.wait_recv()
        for i in dp_others:
            weight_copy(i, p).start()

        @pl.when(c == 1)
        def _():
            for recv in (e_recv, g_recv):
                recv[:, nch - 1, :, T:] = jnp.zeros((3, cols, EC - T), F32)

        iota[...] = lax.broadcasted_iota(jnp.int32, (T, D), 0).astype(I16)
        lanes[...] = lax.broadcasted_iota(jnp.int32, (16, D), 1).astype(I16)

        ids_raw[...] = jnp.full(ids_raw.shape, -1, jnp.int32)
        for which, src in enumerate((send_ids, recv_ids)):
            ids_raw[which:which + 1, :edges] = src[...].reshape(1, edges)

        def ids(b):
            for which, (row_ref, col_ref) in enumerate(((srow, scol), (rrow, rcol))):
                wide = jnp.broadcast_to(ids_raw[which:which + 1, pl.ds(pl.multiple_of(c * eh + b * D, D), D)], (D, D))
                row_ref[at(b, 16), :] = wide[:16].astype(I16)
                col_ref[at(b, D), :] = flip(wide.astype(F32)).astype(jnp.int32).astype(I16)

        with jax.named_scope('ids'):
            loop(eh // D, ids)

        def keys(ref, step):
            return [ref[pl.ds(pl.multiple_of(step * (KS // D) * 16 + 16 * h, 16), 1), :] for h in range(KS // D)]

        bias_cols[...] = flip(stacked([eb1_in[...], nb1_in[...], jnp.zeros((D - 2 * layers, D), F32)]))

        def join_weights(l):
            for d in range(GROUP):
                src = w_recv.at[slot(d)] if d else w_send
                r = rows_of(d)
                for k in THREE:
                    ew1[l, pl.ds(k * D + d * q, q), :] = src[packed(l, k), :].astype(BF)
                ew2t[l, r, :] = src[packed(l, 3), :].astype(BF)
                for k in BOTH:
                    nw1[l, pl.ds(k * D + d * q, q), :] = src[packed(l, 4 + k), :].astype(BF)
                nw2t[l, r, :] = src[packed(l, 6), :].astype(BF)

            def flip_bf(mat):
                return flip(mat.astype(F32)).astype(BF)

            for k in THREE:
                ew1t[l, :, mat(k)] = flip_bf(ew1[l, mat(k), :])
            for k in BOTH:
                nw1t[l, :, mat(k)] = flip_bf(nw1[l, mat(k), :])
            ew2[l] = flip_bf(ew2t[l])
            nw2[l] = flip_bf(nw2t[l])

        def wait_recvs(copies):
            copies[1].wait_recv()
            copies[2].start()
            copies[0].wait_recv()
            copies[2].wait_recv()

        with jax.named_scope('node_wait'):
            wait_recvs(ncop)
        for d in OTHERS:
            v0[rows_of(d), :] = n_recv[slot(d)].astype(BF)
        with jax.named_scope('weight_wait'):
            dp_all(0, 2).wait_recv()
            w_relay.start()
            w_pair.wait_recv()
            w_relay.wait_recv()
        rows_all = beside([w_send[:HEAD, :cols]] + [w_recv[d, :HEAD, :cols] for d in range(3)])
        vecs[...] = flip(stacked([rows_all, jnp.zeros((D - HEAD, D), F32)]))
        join_weights(0)

        def vec(l, node):
            first = 6 * node + l
            return [vecs[:, first + 2 * k:first + 2 * k + 1] for k in THREE]

        def bias(l, node):
            return bias_cols[:, node * layers + l:node * layers + l + 1]

        def hidden_of_nodes(l):
            table, b1 = tables[l], bias(l, 0)

            def body(step):
                xs = gather(table, keys(srow, step), iota).astype(BF)
                xr = gather(table, keys(rrow, step), iota).astype(BF)
                hidden[l, :, at(step, KS)] = dot(ew1t[l, :, mat(1, 2)], stacked([xs, xr])) + b1

            loop(eh // KS, body)

        def edge_forward(l):
            e_in = edges_in[l]

            def body(j):
                for sub in range(EC // T):
                    a = at(j * (EC // T) + sub, T)
                    if l == 0:
                        if sub == 0:
                            chunk_arrived(EDGE_IN, j)
                        for d in OTHERS:
                            e_in[rows_of(d), a] = e_recv[slot(d), j, :, sub * T:(sub + 1) * T].astype(BF)
                    e_val = e_in[:, a]
                    hid = hidden[l, :, a] + dot(ew1t[l, :, mat(0)], e_val)
                    hidden[l, :, a] = hid
                    message, nrm, std = mlp_tail(hid, ew2t[l], vec(l, 0))
                    normed[l, :, a] = nrm
                    inv[l:l + 1, a] = std
                    msg[:, a] = message
                    e_new = (e_val.astype(F32) + message.astype(F32)).astype(BF)
                    if l < top:
                        edges_in[l + 1][:, a] = e_new
                    else:
                        for d in OTHERS:
                            e_send[slot(d), j, :, sub * T:(sub + 1) * T] = e_new[rows_of(d)].astype(F32)
                        if sub == 0:
                            own_parts = []
                        own_parts.append(e_new[:q])
                if l == top:
                    for d in SEND_ORDER:
                        edge_start(EDGE_OUT, j, d)
                    place_edges(edge_raw, beside(own_parts), 0, j)

            loop(nch, body)

        def segment_sum(acc, ids_ref):
            acc[...] = jnp.zeros(acc.shape, F32)

            def body(step):
                scatter(acc, msg[:, at(step, KS)], ids_ref[at(step, KS), :], lanes)

            loop(eh // KS, body)

        def node_forward(l):
            table, agg, out = tables[l], aggs[l], tables[l + 1]

            def body(step):
                a = pl.ds(pl.multiple_of(step * TN, D), TN)
                v_in = table[:, a]
                agg_bf = (part[l, :, a] + swap_halves(part_recv[l, :, a])).astype(BF)
                agg[:, a] = agg_bf
                hid = dot(nw1t[l], stacked([v_in, agg_bf])) + bias(l, 1)
                nhid[l, :, a] = hid
                message, nrm, std = mlp_tail(hid, nw2t[l], vec(l, 1))
                nnrm[l, :, a] = nrm
                ninv[l:l + 1, a] = std
                out[:, a] = (v_in.astype(F32) + message.astype(F32)).astype(BF)

            loop(npad // TN, body)

        for l in range(layers):
            with jax.named_scope(f'gather_{l}'):
                hidden_of_nodes(l)
            if l == top:
                edges_sent(EDGE_IN)
            with jax.named_scope(f'edge_forward_{l}'):
                edge_forward(l)
            with jax.named_scope(f'sum_{l}'):
                segment_sum(part.at[l], rcol)
            part_copy(l).start()
            if l == 0:
                join_weights(1)
                gcop[1].wait_recv()
                gcop[2].start()
            with jax.named_scope(f'part_wait_{l}'):
                part_copy(l).wait_recv()
            with jax.named_scope(f'node_forward_{l}'):
                node_forward(l)
        no_send[...] = tables[layers][rows_of(2), :].astype(F32)
        no_copy = remote(no_send, no_recv, n_ss.at[2, 0], n_rs.at[2, 0], 2)
        no_copy.start()
        node_raw[x] = tables[layers][:q, :nodes]

        grad[...] = jnp.zeros_like(grad)
        sums[...] = jnp.zeros_like(sums)
        with jax.named_scope('grad_node_wait'):
            gcop[0].wait_recv()
            gcop[2].wait_recv()
        for d in OTHERS:
            d_part[rows_of(d), :] = gn_recv[slot(d)]

        def node_backward(l):
            table, agg = tables[l], aggs[l]

            def body(step):
                a = pl.ds(pl.multiple_of(step * TN, D), TN)
                d_in = d_part[:, a]
                if l < top:
                    d_in = d_in + part[layers + l + 1, :, a] + swap_halves(part_recv[layers + l + 1, :, a])
                    d_in = d_in.astype(BF).astype(F32)
                d_hid, d_w2, parts = mlp_back(d_in, nhid[l, :, a], nnrm[l, :, a], ninv[l:l + 1, a], nw2[l], vec(l, 1))
                add_sums(sums.at[l, 1], [parts])
                grad[l, 4] += d_w2
                grad[l, 2] += dot_nt(table[:, a], d_hid)
                grad[l, 3] += dot_nt(agg[:, a], d_hid)
                d_part[:, a] = d_in + dot(nw1[l, mat(0), :], d_hid)
                d_agg[:, a] = dot(nw1[l, mat(1), :], d_hid).astype(BF)

            loop(npad // TN, body)

        def gather_back():
            def body(step):
                msg[:, at(step, KS)] = gather(d_agg, keys(rrow, step), iota).astype(BF)

            loop(eh // KS, body)

        def edge_backward(l):
            e_in = edges_in[l]

            def body(j):
                all_parts, d_w2s, d_w1s, own_parts = [], [], [], []
                for sub in range(EC // T):
                    a = at(j * (EC // T) + sub, T)
                    if l == top:
                        if sub == 0:
                            chunk_arrived(GRAD_IN, j)
                        for d in OTHERS:
                            ge[rows_of(d), a] = g_recv[slot(d), j, :, sub * T:(sub + 1) * T].astype(BF)
                    d_res = ge[:, a].astype(F32)
                    d_msg = d_res + msg[:, a].astype(F32)
                    d_hid, d_w2, parts = mlp_back(d_msg, hidden[l, :, a], normed[l, :, a], inv[l:l + 1, a], ew2[l], vec(l, 0))
                    all_parts.append(parts)
                    d_w2s.append(d_w2)
                    d_w1s.append(dot_nt(e_in[:, a], d_hid))
                    msg[:, a] = d_hid
                    d_new = (d_res + dot(ew1[l, mat(0), :], d_hid)).astype(BF)
                    if l > 0:
                        ge[:, a] = d_new
                    else:
                        for d in OTHERS:
                            g_send[slot(d), j, :, sub * T:(sub + 1) * T] = d_new[rows_of(d)].astype(F32)
                        own_parts.append(d_new[:q])
                add_sums(sums.at[l, 0], all_parts)
                grad[l, 1] += sum(d_w2s[1:], d_w2s[0])
                grad[l, 0] += sum(d_w1s[1:], d_w1s[0])
                if l == 0:
                    @pl.when(j < hold)
                    def _():
                        for d in SEND_ORDER:
                            edge_start(GRAD_OUT, j, d)
                    place_edges(gedge_raw, beside(own_parts), 0, j)

            loop(nch, body)

        def vector_slab(l):
            def total(node, k):
                return column_sum(flip(sums[l, node, mat(k), :]))

            lat = stacked([total(node, k) for node in BOTH for k in THREE])
            biases = stacked([total(node, 3) for node in BOTH])
            n_lat = lat.shape[0]
            for d in range(GROUP):
                grad[l, VEC_SLAB, d * cols:d * cols + n_lat, :cols] = lat[:, rows_of(d)]
                grad[l, VEC_SLAB, d * cols + n_lat:d * cols + n_lat + 2, :] = biases

        def reduce_start(l, stage):
            for b in BOTH:
                core_copy(l, b, stage).start()

        def chip_sum(l, stage):
            row = lax.broadcasted_iota(jnp.int32, (cols, D), 0)
            edge_row = jnp.logical_or(row < 3, row == 6)
            core_all(l, stage).wait_recv()
            for b in BOTH:
                for k in range(SLABS)[STAGES[stage]]:
                    own = grad[l, k, rows_of(2 * b), :]
                    if k in EDGE_SLABS:
                        own = own + core_recv[l, b, k]
                    elif k == VEC_SLAB:
                        own = own + jnp.where(edge_row, core_recv[l, b, k], 0.0)
                    half[l, k, b] = own
            for i in dp_others:
                @pl.when(in_stage(lax.rem(p + i, dpn), stage))
                def _():
                    spread_copy(l, i).start()

        def dp_sum(l, stage):
            @pl.when(in_stage(p, stage))
            def _():
                total = half[l, pl.ds(seat(p) * per, per)]
                dp_all(l, 0).wait_recv()
                for i in dp_others:
                    total = total + dp_recv[l, pl.ds((i - 1) * per, per)]
                own_sum[l] = total[:, 0]
                cross_send[l] = total[:, 1]
                cross_copy(l).start()

        def cross_sum(l):
            cross_copy(l).wait_recv()
            total = own_sum[l] + cross_recv[l]
            own_sum[l] = total
            gathered[l, pl.ds(seat(p) * per, per)] = total
            for i in dp_others:
                gather_copy(l, i, p).start()

        def project(l):
            table = tables[l]

            def body(step):
                a = pl.ds(pl.multiple_of(step * TN, D), TN)
                s_bf, r_bf, v_in = s_sum[:, a].astype(BF), r_sum[:, a].astype(BF), table[:, a]
                part[layers + l, :, a] = dot(ew1[l, mat(1), :], s_bf) + dot(ew1[l, mat(2), :], r_bf)
                grad[l, 6] += dot_nt(v_in, s_bf)
                grad[l, 7] += dot_nt(v_in, r_bf)

            loop(npad // TN, body)

        for l in reversed(range(layers)):
            first_layer = l == 0
            with jax.named_scope(f'node_backward_{l}'):
                node_backward(l)
            if first_layer:
                with jax.named_scope('chip_sum_1'):
                    chip_sum(1, 0)
                    chip_sum(1, 1)
            with jax.named_scope(f'gather_back_{l}'):
                gather_back()
            if first_layer:
                edges_sent(GRAD_IN)
            with jax.named_scope(f'edge_backward_{l}'):
                edge_backward(l)
            vector_slab(l)
            reduce_start(l, 0)
            if first_layer:
                with jax.named_scope('dp_sum_1'):
                    dp_sum(1, 0)
                    dp_sum(1, 1)
            with jax.named_scope(f'sum_send_{l}'):
                segment_sum(s_sum, scol)
            if first_layer:
                with jax.named_scope('chip_sum_0'):
                    chip_sum(0, 0)
            with jax.named_scope(f'sum_recv_{l}'):
                segment_sum(r_sum, rcol)
            with jax.named_scope(f'project_{l}'):
                project(l)
            reduce_start(l, 1)
            part_copy(layers + l).start()
            if first_layer:
                with jax.named_scope('chip_sum_late'):
                    chip_sum(0, 1)
                with jax.named_scope('dp_sum_0'):
                    dp_sum(0, 0)
            with jax.named_scope(f'back_wait_{l}'):
                part_copy(layers + l).wait_recv()

        def final(step):
            a = pl.ds(pl.multiple_of(step * TN, D), TN)
            d_in = (d_part[:, a] + part[layers, :, a] + swap_halves(part_recv[layers, :, a])).astype(BF)
            v2[:, a] = d_in

        loop(npad // TN, final)
        gnode_raw[x] = v2[:q, :nodes]
        with jax.named_scope('dp_sum_late'):
            dp_sum(0, 1)

        dn_send[...] = v2[rows_of(2), :].astype(F32)
        dn_copy = remote(dn_send, dn_recv, n_ss.at[2, 1], n_rs.at[2, 1], 2)
        dn_copy.start()

        def send_rest(j):
            for d in SEND_ORDER:
                edge_start(GRAD_OUT, j, d)

        loop(nch, send_rest, hold)

        with jax.named_scope('node_out_wait'):
            no_copy.wait_recv()
        node_raw[ox] = no_recv[:, :nodes].astype(BF)

        def place_e(j):
            for d in OTHERS:
                place_edges(edge_raw, eo_recv[slot(d), j], d, j)

        with jax.named_scope('place_edge_out'):
            for group in THREE:
                group_arrived(EDGE_OUT, group)
            loop(nch, place_e)

        def place_g(j):
            for d in OTHERS:
                place_edges(gedge_raw, de_recv[slot(d), j], d, j)

        with jax.named_scope('place_first'):
            group_arrived(GRAD_OUT, 0)
            loop(hold, place_g)
        for l in range(layers):
            with jax.named_scope(f'cross_sum_{l}'):
                cross_sum(l)
        with jax.named_scope('d_node_wait'):
            dn_copy.wait_recv()
        gnode_raw[ox] = dn_recv[:, :nodes].astype(BF)
        with jax.named_scope('place_rest'):
            group_arrived(GRAD_OUT, 1)
            loop(last, place_g, hold)
        for l in range(layers):
            dp_all(l, 1).wait_recv()
            ew1_buf[l, 0] = gathered[l, 0]
            ew1_buf[l, 1:] = gathered[l, EARLY:]
            ew2_buf[l] = gathered[l, 1]
            nw1_buf[l] = gathered[l, 2:4]
            nw2_buf[l] = gathered[l, 4]
            small = gathered[l, VEC_SLAB]
            for k in THREE:
                evec_buf[k, l:l + 1, :] = small[k:k + 1, :cols]
                nvec_buf[k, l:l + 1, :] = small[3 + k:4 + k, :cols]
            eb1_buf[l:l + 1, :] = small[6:7]
            nb1_buf[l:l + 1, :] = small[7:8]
        for l in range(layers):
            for stage in BOTH:
                core_all(l, stage).wait_send()
            cross_copy(l).wait_send()
            dp_all(l, 0).wait_send()
            dp_all(l, 1).wait_send()
        for copy in ncop + gcop + (w_pair, w_cross, w_relay):
            copy.wait_send()
        dp_all(0, 2).wait_send()
        no_copy.wait_send()
        dn_copy.wait_send()
        for k in range(2 * layers):
            part_copy(k).wait_send()
        edges_sent(EDGE_OUT)
        with jax.named_scope('place_last'):
            group_arrived(GRAD_OUT, 2)
            loop(nch, place_g, last)
        edges_sent(GRAD_OUT)

    bf = lambda *s: pltpu.VMEM(s, BF)
    pl.run_scoped(
        scoped, bf(D, eh), bf(D, eh), bf(D, eh), bf(D, eh), bf(D, npad), bf(D, npad), bf(D, npad), bf(D, npad), bf(D, npad), bf(D, npad),
        pltpu.VMEM((eh, D), I16), pltpu.VMEM((eh, D), I16), pltpu.VMEM((eh // D * 16, D), I16), pltpu.VMEM((eh // D * 16, D), I16),
        pltpu.VMEM((T, D), I16), pltpu.VMEM((16, D), I16),
        bf(layers, 3 * D, D), bf(layers, D, 3 * D), bf(layers, D, D), bf(layers, D, D),
        bf(layers, 2 * D, D), bf(layers, D, 2 * D), bf(layers, D, D), bf(layers, D, D), pltpu.VMEM((D, D), F32))


def finish_moves(src, dst):
    if len(src.shape) != 3 or src.dtype != BF:
        return [(src, dst)]
    return [(src.at[s, pl.ds(r, 8)], dst.at[s, pl.ds(r, 8)]) for s in range(src.shape[0]) for r in range(0, src.shape[1], 8)]


def finish_kernel(*refs):
    count = len(refs) // 2
    moves = sum((finish_moves(refs[k], refs[count + k]) for k in range(count)), [])
    puts = [pltpu.make_async_copy(src, dst, refs[-1].at[k]) for k, (src, dst) in enumerate(moves)]
    for put in puts:
        put.start()
    for put in puts:
        put.wait()


def keep_in_vmem(val):
    return pltpu.with_memory_space_constraint(val, pltpu.VMEM)


def finish(arrays):
    return pl.pallas_call(
        finish_kernel,
        name='finish',
        out_shape=[jax.ShapeDtypeStruct(a.shape, a.dtype) for a in arrays],
        in_specs=[VM] * len(arrays),
        out_specs=[HB] * len(arrays),
        scratch_shapes=[pltpu.SemaphoreType.DMA((FINISH_SEMS,))],
        compiler_params=pltpu.CompilerParams(vmem_limit_bytes=1 << 20),
    )(*[keep_in_vmem(a) for a in arrays])


def solution(mesh):
    lat_spec = P('dp', None, 'tp')
    first_spec = P(None, None, 'tp', None)
    col_spec = P(None, None, 'tp')
    param_specs = (first_spec, P(), col_spec, col_spec, first_spec, P(), col_spec, col_spec)
    in_specs = (lat_spec, lat_spec, P(), P(), lat_spec, lat_spec) + param_specs
    out_specs = (lat_spec, lat_spec, lat_spec, lat_spec) + param_specs
    shape = jax.ShapeDtypeStruct

    def local_step(node_lat, edge_lat, senders, receivers, grad_node, grad_edge, edge_w1, edge_b1, edge_w2, edge_vec, node_w1, node_b1, node_w2, node_vec):
        layers = edge_w1.shape[0]
        cols = node_lat.shape[2]
        nodes, edges = node_lat.shape[1], edge_lat.shape[1]
        npad = -(-nodes // TN) * TN
        eh = -(-edges // (2 * EC)) * EC
        nch = eh // EC
        dpn = mesh.shape['dp']
        per = SLABS // dpn
        dims = (layers, cols, nodes, edges, npad, eh, dpn)
        flat = lambda arr: jnp.swapaxes(arr, 1, 2)
        lead = lambda arr: jnp.transpose(arr, (1, 0, 2))
        args = (flat(node_lat), flat(edge_lat), flat(grad_node), flat(grad_edge), senders, receivers,
                edge_w1.reshape(-1, D), flat(edge_w2).reshape(-1, D), node_w1.reshape(-1, D), flat(node_w2).reshape(-1, D),
                lead(edge_vec), lead(node_vec), edge_b1, node_b1)
        vm, sem = pltpu.VMEM, pltpu.SemaphoreType.DMA
        wrows = -(-(HEAD + layers * LROWS) // (8 * dpn)) * 8 * dpn
        lat_n, lat_e = (2, cols, nodes), (2, cols, edges)
        outs = [RESULT(lat_n, BF), RESULT(lat_e, BF), RESULT(lat_n, BF), RESULT(lat_e, BF),
                RESULT((layers, 3, cols, D), F32), RESULT((layers, D), F32), RESULT((layers, cols, D), F32), RESULT((3, layers, cols), F32),
                RESULT((layers, 2, cols, D), F32), RESULT((layers, D), F32), RESULT((layers, cols, D), F32), RESULT((3, layers, cols), F32)]
        scratch = [
            *[vm(a.shape, a.dtype) for a in args[4:]], vm((wrows, D), F32), vm((3, wrows, D), F32),
            vm((2, cols, npad), F32), vm((3, cols, npad), F32), vm((2, cols, npad), F32), vm((3, cols, npad), F32),
            vm((cols, npad), F32), vm((cols, npad), F32), vm((cols, npad), F32), vm((cols, npad), F32),
            *[vm((3, nch, cols, EC), F32)] * 6,
            vm((2 * layers, D, npad), F32), vm((2 * layers, D, npad), F32),
            vm((layers, D, eh), F32), vm((layers, D, eh), F32), vm((8, eh), F32),
            vm((layers, D, npad), F32), vm((layers, D, npad), F32), vm((8, npad), F32),
            vm((D, npad), F32), vm((D, npad), F32), vm((D, npad), F32), vm((8, 2 * eh), jnp.int32), vm((D, D), F32), vm((layers, 2, 4 * D, D), F32),
            vm((layers, SLABS, D, D), F32), vm((layers, 2, SLABS, cols, D), F32), vm((layers, SLABS, 2, cols, D), F32),
            vm((layers, (dpn - 1) * per, 2, cols, D), F32), vm((layers, per, cols, D), F32), vm((layers, per, cols, D), F32),
            vm((layers, per, cols, D), F32), vm((layers, SLABS, cols, D), F32),
            sem((layers, 2)), sem((layers, 2)), sem((3, layers)), sem((3, layers)), sem((layers,)), sem((layers,)),
            sem((len(args),)), sem((3,)), sem((3,)), sem((3, 3)), sem((3, 3)), sem((4, 4)), sem((2, nch)), sem((2, 5)),
            sem((2 * layers,)), sem((2 * layers,)), pltpu.SemaphoreType.REGULAR]
        res = pl.pallas_call(
            lambda *refs: step_kernel(dims, *refs),
            name='graph_step',
            out_shape=outs,
            in_specs=[HB] * len(args),
            out_specs=[VM] * len(outs),
            scratch_shapes=scratch,
            compiler_params=pltpu.CompilerParams(collective_id=0, has_side_effects=True, vmem_limit_bytes=VMEM_LIMIT),
        )(*args)

        res = finish(res)
        return (flat(res[0]), flat(res[1]), flat(res[2]), flat(res[3]),
                res[4], res[5], flat(res[6]), lead(res[7]), res[8], res[9], flat(res[10]), lead(res[11]))

    return jax.shard_map(local_step, mesh=mesh, in_specs=in_specs, out_specs=out_specs, check_vma=False)
```

```python
import jax
import jax.numpy as jnp
from jax import lax
from jax.experimental import pallas as pl
from jax.experimental.pallas import tpu as pltpu
from jax.sharding import PartitionSpec as P

LN_EPS = 1e-5
D = 128
T = 256
TN = 384
EC = 512
KS = 1408
BF = jnp.bfloat16
F32 = jnp.float32
I16 = jnp.int16
MESH = pl.DeviceIdType.MESH
VM = pl.BlockSpec(memory_space=pltpu.VMEM)
HB = pl.BlockSpec(memory_space=pl.ANY)
RESULT = pltpu.VMEM
GROUP = 4
BOTH = (0, 1)
THREE = (0, 1, 2)
OTHERS = (1, 2, 3)
EDGE_IN, GRAD_IN, EDGE_OUT, GRAD_OUT = range(4)
SEND_ORDER = (2, 3, 1)
LROWS = 7 * (D // 4)
HEAD = 16
LEADER = GROUP - 1
VMEM_LIMIT = 63_000_000
SLABS = 8
EARLY = 6
VEC_SLAB = 5
EDGE_SLABS = (0, 1, 6, 7)
STAGES = (slice(0, EARLY), slice(EARLY, SLABS))


def dot(a, b):
    return jnp.dot(a, b, preferred_element_type=F32)


def dot_nt(a, b):
    return lax.dot_general(a, b, (((1,), (1,)), ((), ())), preferred_element_type=F32)


def mat(k, n=1):
    return slice(k * D, (k + n) * D)


def rows_of(d):
    q = D // 4
    return slice(d * q, (d + 1) * q)


def at(step, width):
    return pl.ds(pl.multiple_of(step * width, width), width)


def loop(stop, body, start=0):
    def step(j, carry):
        body(j)
        return carry

    lax.fori_loop(start, stop, step, 0)


def column_sum(val):
    return jnp.sum(val, axis=0, keepdims=True)


def flip(val):
    return jnp.swapaxes(val, 0, 1)


def stacked(parts):
    return jnp.concatenate(parts, axis=0)


def beside(parts):
    return jnp.concatenate(parts, axis=1)


def slot(d):
    return d - 1


def sigmoid(hidden):
    return 1.0 / (1.0 + jnp.exp(-hidden))


def fold(val):
    total = val[:, mat(0)]
    for start in range(D, val.shape[1], D):
        total = total + val[:, start:start + D]
    return total


def swap_halves(val):
    return stacked([val[rows_of(d)] for d in (1, 0, 3, 2)])


def gather(table, keys, iota):
    acc = None
    nodes = table.shape[1]
    one, zero = jnp.ones((), BF), jnp.zeros((), BF)
    for base in range(0, nodes, T):
        width = min(T, nodes - base)
        ids = iota[0:width, :]
        hot = beside([jnp.where(ids == (key - jnp.asarray(base, I16)), one, zero) for key in keys])
        part = dot(table[:, base:base + width], hot)
        acc = part if acc is None else acc + part
    return acc


def scatter(acc_ref, val, cols, lanes):
    nodes = acc_ref.shape[1]
    one, zero = jnp.ones((), BF), jnp.zeros((), BF)
    row = lanes[0:1, :]
    for base in range(0, nodes, T):
        width = min(T, nodes - base)
        hot = beside([jnp.where((row + jnp.asarray(base + s, I16)) == cols, one, zero) for s in range(0, width, D)])
        acc_ref[:, base:base + width] += dot(val, hot)


def mlp_tail(hidden, w2t, vec):
    act = (hidden * sigmoid(hidden)).astype(BF)
    out = dot(w2t, act) + vec[0]
    mean = column_sum(out) / D
    centered = out - mean
    var = column_sum(centered * centered) / D
    inv = lax.rsqrt(var + LN_EPS)
    normed = centered * inv
    message = (normed * vec[1] + vec[2]).astype(BF)
    return message, normed, inv


def mlp_back(d_msg, hidden, normed, inv, w2, vec):
    d_normed = d_msg * vec[1]
    mean0 = column_sum(d_normed) / D
    mean1 = column_sum(d_normed * normed) / D
    d_out = inv * (d_normed - mean0 - normed * mean1)
    d_out_bf = d_out.astype(BF)
    sig = sigmoid(hidden)
    act = (hidden * sig).astype(BF)
    d_w2 = dot_nt(d_out_bf, act)
    d_hidden = dot(w2, d_out_bf) * (sig * (1.0 + hidden * (1.0 - sig)))
    sums = (fold(d_out), fold(d_msg * normed), fold(d_msg), fold(d_hidden))
    return d_hidden.astype(BF), d_w2, sums


def add_sums(ref, parts):
    for q in range(4):
        total = parts[0][q]
        for other in parts[1:]:
            total = total + other[q]
        ref[mat(q), :] += total


def step_kernel(dims, *refs):
    layers, cols, nodes, edges, npad, eh, dpn = dims
    nch = eh // EC
    top = layers - 1
    n_in = 14
    hbm_in = refs[:n_in]
    n_out = 12
    (node_raw, edge_raw, gnode_raw, gedge_raw, ew1_buf, eb1_buf, ew2_buf, evec_buf, nw1_buf, nb1_buf, nw2_buf, nvec_buf) = refs[n_in:n_in + n_out]
    (send_ids, recv_ids, ew1_in, ew2_in, nw1_in, nw2_in, evec_in, nvec_in, eb1_in, nb1_in, w_send, w_recv, n_send, n_recv, gn_send, gn_recv, no_send, no_recv, dn_send, dn_recv,
     e_send, g_send, e_recv, g_recv, eo_recv, de_recv, part, part_recv, hidden, normed, inv, nhid, nnrm, ninv, d_part, s_sum, r_sum,
     ids_raw, bias_cols, sums, grad, core_recv, half, dp_recv, cross_send, cross_recv, own_sum, gathered,
     core_rs, dp_rs, cross_rs, w_rs, n_rs, e_rs, o_rs, p_rs, ready, load_sem, w_ss, n_ss, e_ss, p_ss, core_ss, dp_ss, cross_ss) = refs[n_in + n_out:]

    t = lax.axis_index('tp')
    p = lax.axis_index('dp')
    per = SLABS // dpn
    dp_others = range(1, dpn)
    x, c = t // 2, lax.rem(t, 2)
    ox, oc = 1 - x, 1 - c
    peer = [t, t + 1 - 2 * c, t + 2 - 4 * x, t + 3 - 2 * c - 4 * x]

    def remote(src, dst, ssem, rsem, d):
        return pltpu.make_async_remote_copy(src_ref=src, dst_ref=dst, send_sem=ssem, recv_sem=rsem,
                                            device_id={'tp': peer[d]}, device_id_type=MESH)

    small_in = (send_ids, recv_ids, ew1_in, ew2_in, nw1_in, nw2_in, evec_in, nvec_in, eb1_in, nb1_in)
    loads = [pltpu.make_async_copy(src, dst, load_sem.at[q]) for q, (src, dst) in enumerate(
        zip(hbm_in, (node_raw, edge_raw, gnode_raw, gedge_raw) + small_in))]

    def node_copies(send, recv, kind):
        return (remote(send.at[1], recv.at[0], n_ss.at[kind, 0], n_rs.at[kind, 0], 1),
                remote(send.at[0], recv.at[1], n_ss.at[kind, 1], n_rs.at[kind, 1], 2),
                remote(recv.at[1], recv.at[2], n_ss.at[kind, 2], n_rs.at[kind, 2], 1))

    piece = w_send.shape[0] // dpn

    def packed(l, k, count=1):
        return pl.ds(HEAD + l * LROWS + k * cols, count * cols)

    def weight_rows(owner):
        return pl.ds(pl.multiple_of(owner * piece, 8), piece)

    w_pair = remote(w_send, w_recv.at[0], w_ss.at[0], w_rs.at[0], 1)
    w_cross = remote(w_send.at[weight_rows(p)], w_recv.at[1, weight_rows(p)], w_ss.at[1], w_rs.at[1], 2)
    w_relay = remote(w_recv.at[1], w_recv.at[2], w_ss.at[2], w_rs.at[2], 1)

    def weight_copy(i, owner):
        rows = w_recv.at[1, weight_rows(owner)]
        return dp_remote(rows, rows, 2, 0, i)

    last = nch - 1
    hold = nch - 3
    buffers = ((e_send, e_recv), (g_send, g_recv), (e_send, eo_recv), (g_send, de_recv))

    def outward(kind):
        return kind in (EDGE_OUT, GRAD_OUT)

    def edge_part(kind, index, send_sem, recv_sem, d):
        src, dst = buffers[kind]
        recv_sems = o_rs.at[kind - EDGE_OUT, recv_sem] if outward(kind) else e_rs.at[kind, recv_sem]
        return remote(src.at[index], dst.at[index], e_ss.at[kind, send_sem], recv_sems, d)

    def by_half(half_id, j, action):
        narrow = jnp.logical_and(j == last, half_id == 1)

        @pl.when(jnp.logical_not(narrow))
        def _():
            action(slice(None))

        @pl.when(narrow)
        def _():
            action(slice(T))

    def edge_start(kind, j, d):
        other = oc if d % 2 else c
        if outward(kind):
            send_sem, recv_sem = jnp.where(j == last, 1, 0), jnp.where(j == last, 2 + slot(d), jnp.where(j < hold, 0, 1))
        else:
            send_sem, recv_sem = jnp.where(j == last, d, 0), j
        by_half(c if outward(kind) else other, j,
                lambda used: edge_part(kind, (slot(d), j, slice(None), used), send_sem, recv_sem, d).start())

    def edges_sent(kind):
        every = slice(None)
        edge_part(kind, (every, slice(0, last)), 0, 0, 1).wait_send()
        if outward(kind):
            by_half(c, last, lambda used: edge_part(kind, (every, last, every, used), 1, 0, 1).wait_send())
        else:
            for d in OTHERS:
                by_half(oc if d % 2 else c, last, lambda used: edge_part(kind, (slot(d), last, every, used), d, 0, d).wait_send())

    def chunk_arrived(kind, j):
        every = slice(None)
        by_half(c, j, lambda used: edge_part(kind, (every, j, every, used), 0, j, 1).wait_recv())

    def group_arrived(kind, group):
        every = slice(None)
        if group < 2:
            edge_part(kind, (every, (slice(0, hold), slice(hold, last))[group]), 0, group, 1).wait_recv()
        else:
            for d in OTHERS:
                by_half(oc if d % 2 else c, last, lambda used: edge_part(kind, (slot(d), last, every, used), 0, 2 + slot(d), d).wait_recv())

    def core_copy(l, b, stage):
        first, count = ((0, EARLY), (EARLY, SLABS - EARLY))[stage]
        return remote(grad.at[l, pl.ds(first, count), pl.ds((2 * b + 1) * cols, cols), :], core_recv.at[l, b, pl.ds(first, count)],
                      core_ss.at[l, stage], core_rs.at[l, stage], 1)

    def core_all(l, stage):
        part_of = core_recv.at[l, :, (slice(0, EARLY), slice(EARLY, SLABS))[stage]]
        return remote(part_of, part_of, core_ss.at[l, stage], core_rs.at[l, stage], 1)

    def seat(device):
        return lax.rem(device + dpn // 2, dpn)

    def in_stage(device, stage):
        early = (seat(device) + 1) * per <= EARLY
        return jnp.logical_not(early) if stage else early

    def dp_remote(src, dst, stage, l, i):
        return pltpu.make_async_remote_copy(src_ref=src, dst_ref=dst, send_sem=dp_ss.at[stage, l], recv_sem=dp_rs.at[stage, l],
                                            device_id={'dp': lax.rem(p + i, dpn)}, device_id_type=MESH)

    def spread_copy(l, i):
        return dp_remote(half.at[l, pl.ds(seat(lax.rem(p + i, dpn)) * per, per)], dp_recv.at[l, pl.ds((i - 1) * per, per)], 0, l, i)

    def dp_all(l, stage):
        most = (dpn - 1) * per
        part_of = (dp_recv.at[l], gathered.at[l, pl.ds(0, most)], w_recv.at[1, pl.ds(0, (dpn - 1) * piece)])[stage]
        return dp_remote(part_of, part_of, stage, l, 1)

    def cross_copy(l):
        return remote(cross_send.at[l], cross_recv.at[l], cross_ss.at[l], cross_rs.at[l], 2)

    def gather_copy(l, i, owner):
        return dp_remote(own_sum.at[l], gathered.at[l, pl.ds(seat(owner) * per, per)], 1, l, i)

    def part_copy(q):
        return remote(part.at[q], part_recv.at[q], p_ss.at[q], p_rs.at[q], 1)

    def load_nodes(raw, send, own):
        send[...] = jnp.zeros_like(send)
        send[0, :, :nodes] = raw[ox].astype(F32)
        send[1, :, :nodes] = raw[x].astype(F32)
        own[:cols, :] = send[1].astype(own.dtype)

    def load_edges(raw, send, own, kind):
        def put(j, lanes_j, val_of):
            for d in OTHERS:
                sample = x if d < 2 else ox
                send[slot(d), j] = val_of(sample, oc if d % 2 else c).astype(F32)
            own[:cols, lanes_j] = val_of(x, c)

        def chunk(j):
            put(j, at(j, EC), lambda s, h: raw[s, :, pl.ds(pl.multiple_of(h * eh + j * EC, D), EC)])
            for d in SEND_ORDER:
                edge_start(kind, j, d)

        loop(nch - 1, chunk)
        first = (nch - 1) * EC
        used = edges - eh - first
        last = pl.ds(first, EC)

        def tail(s, h):
            left = raw[s, :, pl.ds(first, EC)]
            right = beside([raw[s, :, pl.ds(eh + first, used)], jnp.zeros((cols, EC - used), BF)])
            return jnp.where(h == 0, left.astype(F32), right.astype(F32)).astype(BF)

        put(nch - 1, last, tail)
        for d in SEND_ORDER:
            edge_start(kind, nch - 1, d)

    def place_edges(raw, block, d, j):
        s = x if d < 2 else ox
        h = oc if d % 2 else c
        val = block.astype(BF)
        first = (nch - 1) * EC
        used = edges - eh - first

        @pl.when(jnp.logical_or(j < nch - 1, h == 0))
        def _():
            raw[s, :, pl.ds(pl.multiple_of(h * eh + j * EC, D), EC)] = val

        @pl.when(jnp.logical_and(j == nch - 1, h == 1))
        def _():
            raw[s, :, pl.ds(eh + first, used)] = val[:, :used]

    def scoped(e0, e1, ge, msg, v0, v1, v2, agg0, agg1, d_agg, scol, rcol, srow, rrow, iota, lanes, ew1, ew1t, ew2, ew2t, nw1, nw1t, nw2, nw2t, vecs):
        tables = (v0, v1, v2)
        aggs = (agg0, agg1)
        edges_in = (e0, e1)

        barrier = pltpu.get_barrier_semaphore()
        for d in OTHERS:
            pl.semaphore_signal(barrier, inc=1, device_id={'tp': peer[d]}, device_id_type=MESH)
        for copy in loads[:1] + loads[4:] + loads[1:4]:
            copy.start()
        loads[0].wait()
        with jax.named_scope('send_nodes'):
            load_nodes(node_raw, n_send, v0)
        ncop = node_copies(n_send, n_recv, 0)
        for copy in loads[4:]:
            copy.wait()
        q = cols
        w_send[:HEAD, :] = jnp.zeros((HEAD, D), F32)
        for k in THREE:
            w_send[k * layers:(k + 1) * layers, :cols] = evec_in[k]
            w_send[(3 + k) * layers:(4 + k) * layers, :cols] = nvec_in[k]
        for l in range(layers):
            w_send[packed(l, 0, 3), :] = ew1_in[pl.ds(l * 3 * q, 3 * q), :].astype(F32)
            w_send[packed(l, 3), :] = ew2_in[pl.ds(l * q, q), :].astype(F32)
            w_send[packed(l, 4, 2), :] = nw1_in[pl.ds(l * 2 * q, 2 * q), :].astype(F32)
            w_send[packed(l, 6), :] = nw2_in[pl.ds(l * q, q), :].astype(F32)
        with jax.named_scope('barrier'):
            @pl.when(t != LEADER)
            def _():
                pl.semaphore_wait(barrier, len(OTHERS))
                pl.semaphore_signal(ready, inc=1, device_id={'tp': LEADER}, device_id_type=MESH)

            @pl.when(t == LEADER)
            def _():
                pl.semaphore_wait(ready, len(OTHERS))
                for i in dp_others:
                    pl.semaphore_signal(barrier, inc=1, device_id={'dp': lax.rem(p + i, dpn)}, device_id_type=MESH)

        w_cross.start()
        w_pair.start()
        ncop[1].start()
        ncop[0].start()
        loads[1].wait()
        with jax.named_scope('send_edges'):
            load_edges(edge_raw, e_send, e0, EDGE_IN)
        loads[2].wait()
        load_nodes(gnode_raw, gn_send, d_part)
        gcop = node_copies(gn_send, gn_recv, 1)
        gcop[1].start()
        gcop[0].start()
        loads[3].wait()
        with jax.named_scope('send_grads'):
            load_edges(gedge_raw, g_send, ge, GRAD_IN)

        with jax.named_scope('dp_barrier'):
            @pl.when(t == LEADER)
            def _():
                pl.semaphore_wait(barrier, len(OTHERS) + dpn - 1)
                for d in OTHERS:
                    pl.semaphore_signal(ready, inc=1, device_id={'tp': peer[d]}, device_id_type=MESH)

            @pl.when(t != LEADER)
            def _():
                pl.semaphore_wait(ready, 1)

        w_cross.wait_recv()
        for i in dp_others:
            weight_copy(i, p).start()

        @pl.when(c == 1)
        def _():
            for recv in (e_recv, g_recv):
                recv[:, nch - 1, :, T:] = jnp.zeros((3, cols, EC - T), F32)

        iota[...] = lax.broadcasted_iota(jnp.int32, (T, D), 0).astype(I16)
        lanes[...] = lax.broadcasted_iota(jnp.int32, (16, D), 1).astype(I16)

        ids_raw[...] = jnp.full(ids_raw.shape, -1, jnp.int32)
        for which, src in enumerate((send_ids, recv_ids)):
            ids_raw[which:which + 1, :edges] = src[...].reshape(1, edges)

        def ids(b):
            for which, (row_ref, col_ref) in enumerate(((srow, scol), (rrow, rcol))):
                wide = jnp.broadcast_to(ids_raw[which:which + 1, pl.ds(pl.multiple_of(c * eh + b * D, D), D)], (D, D))
                row_ref[at(b, 16), :] = wide[:16].astype(I16)
                col_ref[at(b, D), :] = flip(wide.astype(F32)).astype(jnp.int32).astype(I16)

        with jax.named_scope('ids'):
            loop(eh // D, ids)

        def keys(ref, step):
            return [ref[pl.ds(pl.multiple_of(step * (KS // D) * 16 + 16 * h, 16), 1), :] for h in range(KS // D)]

        bias_cols[...] = flip(stacked([eb1_in[...], nb1_in[...], jnp.zeros((D - 2 * layers, D), F32)]))

        def join_weights(l):
            for d in range(GROUP):
                src = w_recv.at[slot(d)] if d else w_send
                r = rows_of(d)
                for k in THREE:
                    ew1[l, pl.ds(k * D + d * q, q), :] = src[packed(l, k), :].astype(BF)
                ew2t[l, r, :] = src[packed(l, 3), :].astype(BF)
                for k in BOTH:
                    nw1[l, pl.ds(k * D + d * q, q), :] = src[packed(l, 4 + k), :].astype(BF)
                nw2t[l, r, :] = src[packed(l, 6), :].astype(BF)

            def flip_bf(mat):
                return flip(mat.astype(F32)).astype(BF)

            for k in THREE:
                ew1t[l, :, mat(k)] = flip_bf(ew1[l, mat(k), :])
            for k in BOTH:
                nw1t[l, :, mat(k)] = flip_bf(nw1[l, mat(k), :])
            ew2[l] = flip_bf(ew2t[l])
            nw2[l] = flip_bf(nw2t[l])

        def wait_recvs(copies):
            copies[1].wait_recv()
            copies[2].start()
            copies[0].wait_recv()
            copies[2].wait_recv()

        with jax.named_scope('node_wait'):
            wait_recvs(ncop)
        for d in OTHERS:
            v0[rows_of(d), :] = n_recv[slot(d)].astype(BF)
        with jax.named_scope('weight_wait'):
            dp_all(0, 2).wait_recv()
            w_relay.start()
            w_pair.wait_recv()
            w_relay.wait_recv()
        rows_all = beside([w_send[:HEAD, :cols]] + [w_recv[d, :HEAD, :cols] for d in range(3)])
        vecs[...] = flip(stacked([rows_all, jnp.zeros((D - HEAD, D), F32)]))
        join_weights(0)

        def vec(l, node):
            first = 6 * node + l
            return [vecs[:, first + 2 * k:first + 2 * k + 1] for k in THREE]

        def bias(l, node):
            return bias_cols[:, node * layers + l:node * layers + l + 1]

        def hidden_of_nodes(l):
            table, b1 = tables[l], bias(l, 0)

            def body(step):
                xs = gather(table, keys(srow, step), iota).astype(BF)
                xr = gather(table, keys(rrow, step), iota).astype(BF)
                hidden[l, :, at(step, KS)] = dot(ew1t[l, :, mat(1, 2)], stacked([xs, xr])) + b1

            loop(eh // KS, body)

        def edge_forward(l):
            e_in = edges_in[l]

            def body(j):
                for sub in range(EC // T):
                    a = at(j * (EC // T) + sub, T)
                    if l == 0:
                        if sub == 0:
                            chunk_arrived(EDGE_IN, j)
                        for d in OTHERS:
                            e_in[rows_of(d), a] = e_recv[slot(d), j, :, sub * T:(sub + 1) * T].astype(BF)
                    e_val = e_in[:, a]
                    hid = hidden[l, :, a] + dot(ew1t[l, :, mat(0)], e_val)
                    hidden[l, :, a] = hid
                    message, nrm, std = mlp_tail(hid, ew2t[l], vec(l, 0))
                    normed[l, :, a] = nrm
                    inv[l:l + 1, a] = std
                    msg[:, a] = message
                    e_new = (e_val.astype(F32) + message.astype(F32)).astype(BF)
                    if l < top:
                        edges_in[l + 1][:, a] = e_new
                    else:
                        for d in OTHERS:
                            e_send[slot(d), j, :, sub * T:(sub + 1) * T] = e_new[rows_of(d)].astype(F32)
                        if sub == 0:
                            own_parts = []
                        own_parts.append(e_new[:q])
                if l == top:
                    for d in SEND_ORDER:
                        edge_start(EDGE_OUT, j, d)
                    place_edges(edge_raw, beside(own_parts), 0, j)

            loop(nch, body)

        def segment_sum(acc, ids_ref):
            acc[...] = jnp.zeros(acc.shape, F32)

            def body(step):
                scatter(acc, msg[:, at(step, KS)], ids_ref[at(step, KS), :], lanes)

            loop(eh // KS, body)

        def node_forward(l):
            table, agg, out = tables[l], aggs[l], tables[l + 1]

            def body(step):
                a = pl.ds(pl.multiple_of(step * TN, D), TN)
                v_in = table[:, a]
                agg_bf = (part[l, :, a] + swap_halves(part_recv[l, :, a])).astype(BF)
                agg[:, a] = agg_bf
                hid = dot(nw1t[l], stacked([v_in, agg_bf])) + bias(l, 1)
                nhid[l, :, a] = hid
                message, nrm, std = mlp_tail(hid, nw2t[l], vec(l, 1))
                nnrm[l, :, a] = nrm
                ninv[l:l + 1, a] = std
                out[:, a] = (v_in.astype(F32) + message.astype(F32)).astype(BF)

            loop(npad // TN, body)

        for l in range(layers):
            with jax.named_scope(f'gather_{l}'):
                hidden_of_nodes(l)
            if l == top:
                edges_sent(EDGE_IN)
            with jax.named_scope(f'edge_forward_{l}'):
                edge_forward(l)
            with jax.named_scope(f'sum_{l}'):
                segment_sum(part.at[l], rcol)
            part_copy(l).start()
            if l == 0:
                join_weights(1)
                gcop[1].wait_recv()
                gcop[2].start()
            with jax.named_scope(f'part_wait_{l}'):
                part_copy(l).wait_recv()
            with jax.named_scope(f'node_forward_{l}'):
                node_forward(l)
        no_send[...] = tables[layers][rows_of(2), :].astype(F32)
        no_copy = remote(no_send, no_recv, n_ss.at[2, 0], n_rs.at[2, 0], 2)
        no_copy.start()
        node_raw[x] = tables[layers][:q, :nodes]

        grad[...] = jnp.zeros_like(grad)
        sums[...] = jnp.zeros_like(sums)
        with jax.named_scope('grad_node_wait'):
            gcop[0].wait_recv()
            gcop[2].wait_recv()
        for d in OTHERS:
            d_part[rows_of(d), :] = gn_recv[slot(d)]

        def node_backward(l):
            table, agg = tables[l], aggs[l]

            def body(step):
                a = pl.ds(pl.multiple_of(step * TN, D), TN)
                d_in = d_part[:, a]
                if l < top:
                    d_in = d_in + part[layers + l + 1, :, a] + swap_halves(part_recv[layers + l + 1, :, a])
                    d_in = d_in.astype(BF).astype(F32)
                d_hid, d_w2, parts = mlp_back(d_in, nhid[l, :, a], nnrm[l, :, a], ninv[l:l + 1, a], nw2[l], vec(l, 1))
                add_sums(sums.at[l, 1], [parts])
                grad[l, 4] += d_w2
                grad[l, 2] += dot_nt(table[:, a], d_hid)
                grad[l, 3] += dot_nt(agg[:, a], d_hid)
                d_part[:, a] = d_in + dot(nw1[l, mat(0), :], d_hid)
                d_agg[:, a] = dot(nw1[l, mat(1), :], d_hid).astype(BF)

            loop(npad // TN, body)

        def gather_back():
            def body(step):
                msg[:, at(step, KS)] = gather(d_agg, keys(rrow, step), iota).astype(BF)

            loop(eh // KS, body)

        def edge_backward(l):
            e_in = edges_in[l]

            def body(j):
                all_parts, d_w2s, d_w1s, own_parts = [], [], [], []
                for sub in range(EC // T):
                    a = at(j * (EC // T) + sub, T)
                    if l == top:
                        if sub == 0:
                            chunk_arrived(GRAD_IN, j)
                        for d in OTHERS:
                            ge[rows_of(d), a] = g_recv[slot(d), j, :, sub * T:(sub + 1) * T].astype(BF)
                    d_res = ge[:, a].astype(F32)
                    d_msg = d_res + msg[:, a].astype(F32)
                    d_hid, d_w2, parts = mlp_back(d_msg, hidden[l, :, a], normed[l, :, a], inv[l:l + 1, a], ew2[l], vec(l, 0))
                    all_parts.append(parts)
                    d_w2s.append(d_w2)
                    d_w1s.append(dot_nt(e_in[:, a], d_hid))
                    msg[:, a] = d_hid
                    d_new = (d_res + dot(ew1[l, mat(0), :], d_hid)).astype(BF)
                    if l > 0:
                        ge[:, a] = d_new
                    else:
                        for d in OTHERS:
                            g_send[slot(d), j, :, sub * T:(sub + 1) * T] = d_new[rows_of(d)].astype(F32)
                        own_parts.append(d_new[:q])
                add_sums(sums.at[l, 0], all_parts)
                grad[l, 1] += sum(d_w2s[1:], d_w2s[0])
                grad[l, 0] += sum(d_w1s[1:], d_w1s[0])
                if l == 0:
                    @pl.when(j < hold)
                    def _():
                        for d in SEND_ORDER:
                            edge_start(GRAD_OUT, j, d)
                    place_edges(gedge_raw, beside(own_parts), 0, j)

            loop(nch, body)

        def vector_slab(l):
            def total(node, k):
                return column_sum(flip(sums[l, node, mat(k), :]))

            lat = stacked([total(node, k) for node in BOTH for k in THREE])
            biases = stacked([total(node, 3) for node in BOTH])
            n_lat = lat.shape[0]
            for d in range(GROUP):
                grad[l, VEC_SLAB, d * cols:d * cols + n_lat, :cols] = lat[:, rows_of(d)]
                grad[l, VEC_SLAB, d * cols + n_lat:d * cols + n_lat + 2, :] = biases

        def reduce_start(l, stage):
            for b in BOTH:
                core_copy(l, b, stage).start()

        def chip_sum(l, stage):
            row = lax.broadcasted_iota(jnp.int32, (cols, D), 0)
            edge_row = jnp.logical_or(row < 3, row == 6)
            core_all(l, stage).wait_recv()
            for b in BOTH:
                for k in range(SLABS)[STAGES[stage]]:
                    own = grad[l, k, rows_of(2 * b), :]
                    if k in EDGE_SLABS:
                        own = own + core_recv[l, b, k]
                    elif k == VEC_SLAB:
                        own = own + jnp.where(edge_row, core_recv[l, b, k], 0.0)
                    half[l, k, b] = own
            for i in dp_others:
                @pl.when(in_stage(lax.rem(p + i, dpn), stage))
                def _():
                    spread_copy(l, i).start()

        def dp_sum(l, stage):
            @pl.when(in_stage(p, stage))
            def _():
                total = half[l, pl.ds(seat(p) * per, per)]
                dp_all(l, 0).wait_recv()
                for i in dp_others:
                    total = total + dp_recv[l, pl.ds((i - 1) * per, per)]
                own_sum[l] = total[:, 0]
                cross_send[l] = total[:, 1]
                cross_copy(l).start()

        def cross_sum(l):
            cross_copy(l).wait_recv()
            total = own_sum[l] + cross_recv[l]
            own_sum[l] = total
            gathered[l, pl.ds(seat(p) * per, per)] = total
            for i in dp_others:
                gather_copy(l, i, p).start()

        def project(l):
            table = tables[l]

            def body(step):
                a = pl.ds(pl.multiple_of(step * TN, D), TN)
                s_bf, r_bf, v_in = s_sum[:, a].astype(BF), r_sum[:, a].astype(BF), table[:, a]
                part[layers + l, :, a] = dot(ew1[l, mat(1), :], s_bf) + dot(ew1[l, mat(2), :], r_bf)
                grad[l, 6] += dot_nt(v_in, s_bf)
                grad[l, 7] += dot_nt(v_in, r_bf)

            loop(npad // TN, body)

        for l in reversed(range(layers)):
            first_layer = l == 0
            with jax.named_scope(f'node_backward_{l}'):
                node_backward(l)
            if first_layer:
                with jax.named_scope('chip_sum_1'):
                    chip_sum(1, 0)
                    chip_sum(1, 1)
            with jax.named_scope(f'gather_back_{l}'):
                gather_back()
            if first_layer:
                edges_sent(GRAD_IN)
            with jax.named_scope(f'edge_backward_{l}'):
                edge_backward(l)
            vector_slab(l)
            reduce_start(l, 0)
            if first_layer:
                with jax.named_scope('dp_sum_1'):
                    dp_sum(1, 0)
                    dp_sum(1, 1)
            with jax.named_scope(f'sum_send_{l}'):
                segment_sum(s_sum, scol)
            if first_layer:
                with jax.named_scope('chip_sum_0'):
                    chip_sum(0, 0)
            with jax.named_scope(f'sum_recv_{l}'):
                segment_sum(r_sum, rcol)
            with jax.named_scope(f'project_{l}'):
                project(l)
            reduce_start(l, 1)
            part_copy(layers + l).start()
            if first_layer:
                with jax.named_scope('chip_sum_late'):
                    chip_sum(0, 1)
                with jax.named_scope('dp_sum_0'):
                    dp_sum(0, 0)
            with jax.named_scope(f'back_wait_{l}'):
                part_copy(layers + l).wait_recv()

        def final(step):
            a = pl.ds(pl.multiple_of(step * TN, D), TN)
            d_in = (d_part[:, a] + part[layers, :, a] + swap_halves(part_recv[layers, :, a])).astype(BF)
            v2[:, a] = d_in

        loop(npad // TN, final)
        gnode_raw[x] = v2[:q, :nodes]
        with jax.named_scope('dp_sum_late'):
            dp_sum(0, 1)

        dn_send[...] = v2[rows_of(2), :].astype(F32)
        dn_copy = remote(dn_send, dn_recv, n_ss.at[2, 1], n_rs.at[2, 1], 2)
        dn_copy.start()

        def send_rest(j):
            for d in SEND_ORDER:
                edge_start(GRAD_OUT, j, d)

        loop(nch, send_rest, hold)

        with jax.named_scope('node_out_wait'):
            no_copy.wait_recv()
        node_raw[ox] = no_recv[:, :nodes].astype(BF)

        def place_e(j):
            for d in OTHERS:
                place_edges(edge_raw, eo_recv[slot(d), j], d, j)

        with jax.named_scope('place_edge_out'):
            for group in THREE:
                group_arrived(EDGE_OUT, group)
            loop(nch, place_e)

        def place_g(j):
            for d in OTHERS:
                place_edges(gedge_raw, de_recv[slot(d), j], d, j)

        with jax.named_scope('place_first'):
            group_arrived(GRAD_OUT, 0)
            loop(hold, place_g)
        for l in range(layers):
            with jax.named_scope(f'cross_sum_{l}'):
                cross_sum(l)
        with jax.named_scope('d_node_wait'):
            dn_copy.wait_recv()
        gnode_raw[ox] = dn_recv[:, :nodes].astype(BF)
        with jax.named_scope('place_rest'):
            group_arrived(GRAD_OUT, 1)
            loop(last, place_g, hold)
        for l in range(layers):
            dp_all(l, 1).wait_recv()
            ew1_buf[l, 0] = gathered[l, 0]
            ew1_buf[l, 1:] = gathered[l, EARLY:]
            ew2_buf[l] = gathered[l, 1]
            nw1_buf[l] = gathered[l, 2:4]
            nw2_buf[l] = gathered[l, 4]
            small = gathered[l, VEC_SLAB]
            for k in THREE:
                evec_buf[k, l:l + 1, :] = small[k:k + 1, :cols]
                nvec_buf[k, l:l + 1, :] = small[3 + k:4 + k, :cols]
            eb1_buf[l:l + 1, :] = small[6:7]
            nb1_buf[l:l + 1, :] = small[7:8]
        for l in range(layers):
            for stage in BOTH:
                core_all(l, stage).wait_send()
            cross_copy(l).wait_send()
            dp_all(l, 0).wait_send()
            dp_all(l, 1).wait_send()
        for copy in ncop + gcop + (w_pair, w_cross, w_relay):
            copy.wait_send()
        dp_all(0, 2).wait_send()
        no_copy.wait_send()
        dn_copy.wait_send()
        for k in range(2 * layers):
            part_copy(k).wait_send()
        edges_sent(EDGE_OUT)
        with jax.named_scope('place_last'):
            group_arrived(GRAD_OUT, 2)
            loop(nch, place_g, last)
        edges_sent(GRAD_OUT)

    bf = lambda *s: pltpu.VMEM(s, BF)
    pl.run_scoped(
        scoped, bf(D, eh), bf(D, eh), bf(D, eh), bf(D, eh), bf(D, npad), bf(D, npad), bf(D, npad), bf(D, npad), bf(D, npad), bf(D, npad),
        pltpu.VMEM((eh, D), I16), pltpu.VMEM((eh, D), I16), pltpu.VMEM((eh // D * 16, D), I16), pltpu.VMEM((eh // D * 16, D), I16),
        pltpu.VMEM((T, D), I16), pltpu.VMEM((16, D), I16),
        bf(layers, 3 * D, D), bf(layers, D, 3 * D), bf(layers, D, D), bf(layers, D, D),
        bf(layers, 2 * D, D), bf(layers, D, 2 * D), bf(layers, D, D), bf(layers, D, D), pltpu.VMEM((D, D), F32))


def finish_moves(src, dst):
    if len(src.shape) != 3 or src.dtype != BF:
        return [(src, dst)]
    return [(src.at[s, pl.ds(r, 8)], dst.at[s, pl.ds(r, 8)]) for s in range(src.shape[0]) for r in range(0, src.shape[1], 8)]


def finish_kernel(*refs):
    count = len(refs) // 2
    moves = sum((finish_moves(refs[k], refs[count + k]) for k in range(count)), [])
    puts = [pltpu.make_async_copy(src, dst, refs[-1]) for src, dst in moves]
    for put in puts:
        put.start()
    for put in puts:
        put.wait()


def keep_in_vmem(val):
    return pltpu.with_memory_space_constraint(val, pltpu.VMEM)


def finish(arrays):
    return pl.pallas_call(
        finish_kernel,
        name='finish',
        out_shape=[jax.ShapeDtypeStruct(a.shape, a.dtype) for a in arrays],
        in_specs=[VM] * len(arrays),
        out_specs=[HB] * len(arrays),
        scratch_shapes=[pltpu.SemaphoreType.DMA],
        compiler_params=pltpu.CompilerParams(vmem_limit_bytes=1 << 20),
    )(*[keep_in_vmem(a) for a in arrays])


def solution(mesh):
    lat_spec = P('dp', None, 'tp')
    first_spec = P(None, None, 'tp', None)
    col_spec = P(None, None, 'tp')
    param_specs = (first_spec, P(), col_spec, col_spec, first_spec, P(), col_spec, col_spec)
    in_specs = (lat_spec, lat_spec, P(), P(), lat_spec, lat_spec) + param_specs
    out_specs = (lat_spec, lat_spec, lat_spec, lat_spec) + param_specs
    shape = jax.ShapeDtypeStruct

    def local_step(node_lat, edge_lat, senders, receivers, grad_node, grad_edge, edge_w1, edge_b1, edge_w2, edge_vec, node_w1, node_b1, node_w2, node_vec):
        layers = edge_w1.shape[0]
        cols = node_lat.shape[2]
        nodes, edges = node_lat.shape[1], edge_lat.shape[1]
        npad = -(-nodes // TN) * TN
        eh = -(-edges // (2 * EC)) * EC
        nch = eh // EC
        dpn = mesh.shape['dp']
        per = SLABS // dpn
        dims = (layers, cols, nodes, edges, npad, eh, dpn)
        flat = lambda arr: jnp.swapaxes(arr, 1, 2)
        lead = lambda arr: jnp.transpose(arr, (1, 0, 2))
        args = (flat(node_lat), flat(edge_lat), flat(grad_node), flat(grad_edge), senders, receivers,
                edge_w1.reshape(-1, D), flat(edge_w2).reshape(-1, D), node_w1.reshape(-1, D), flat(node_w2).reshape(-1, D),
                lead(edge_vec), lead(node_vec), edge_b1, node_b1)
        vm, sem = pltpu.VMEM, pltpu.SemaphoreType.DMA
        wrows = -(-(HEAD + layers * LROWS) // (8 * dpn)) * 8 * dpn
        lat_n, lat_e = (2, cols, nodes), (2, cols, edges)
        outs = [RESULT(lat_n, BF), RESULT(lat_e, BF), RESULT(lat_n, BF), RESULT(lat_e, BF),
                RESULT((layers, 3, cols, D), F32), RESULT((layers, D), F32), RESULT((layers, cols, D), F32), RESULT((3, layers, cols), F32),
                RESULT((layers, 2, cols, D), F32), RESULT((layers, D), F32), RESULT((layers, cols, D), F32), RESULT((3, layers, cols), F32)]
        scratch = [
            *[vm(a.shape, a.dtype) for a in args[4:]], vm((wrows, D), F32), vm((3, wrows, D), F32),
            vm((2, cols, npad), F32), vm((3, cols, npad), F32), vm((2, cols, npad), F32), vm((3, cols, npad), F32),
            vm((cols, npad), F32), vm((cols, npad), F32), vm((cols, npad), F32), vm((cols, npad), F32),
            *[vm((3, nch, cols, EC), F32)] * 6,
            vm((2 * layers, D, npad), F32), vm((2 * layers, D, npad), F32),
            vm((layers, D, eh), F32), vm((layers, D, eh), F32), vm((8, eh), F32),
            vm((layers, D, npad), F32), vm((layers, D, npad), F32), vm((8, npad), F32),
            vm((D, npad), F32), vm((D, npad), F32), vm((D, npad), F32), vm((8, 2 * eh), jnp.int32), vm((D, D), F32), vm((layers, 2, 4 * D, D), F32),
            vm((layers, SLABS, D, D), F32), vm((layers, 2, SLABS, cols, D), F32), vm((layers, SLABS, 2, cols, D), F32),
            vm((layers, (dpn - 1) * per, 2, cols, D), F32), vm((layers, per, cols, D), F32), vm((layers, per, cols, D), F32),
            vm((layers, per, cols, D), F32), vm((layers, SLABS, cols, D), F32),
            sem((layers, 2)), sem((3, layers)), sem((layers,)), sem((3,)), sem((3, 3)), sem((2, nch)), sem((2, 5)), sem((2 * layers,)),
            pltpu.SemaphoreType.REGULAR]
        own_sems = [sem((len(args),)), sem((3,)), sem((3, 3)), sem((4, 4)), sem((2 * layers,)), sem((layers, 2)), sem((3, layers)), sem((layers,))]
        res = pl.pallas_call(
            lambda *refs: pl.run_scoped(lambda *own: step_kernel(dims, *refs, *own), *own_sems),
            name='graph_step',
            out_shape=outs,
            in_specs=[HB] * len(args),
            out_specs=[VM] * len(outs),
            scratch_shapes=scratch,
            compiler_params=pltpu.CompilerParams(collective_id=0, has_side_effects=True, vmem_limit_bytes=VMEM_LIMIT),
        )(*args)

        res = finish(res)
        return (flat(res[0]), flat(res[1]), flat(res[2]), flat(res[3]),
                res[4], res[5], flat(res[6]), lead(res[7]), res[8], res[9], flat(res[10]), lead(res[11]))

    return jax.shard_map(local_step, mesh=mesh, in_specs=in_specs, out_specs=out_specs, check_vma=False)
```

```python
import jax
import jax.numpy as jnp
from jax import lax
from jax.experimental import pallas as pl
from jax.experimental.pallas import tpu as pltpu
from jax.sharding import PartitionSpec as P

LN_EPS = 1e-5
D = 128
T = 256
TN = 384
EC = 512
KS = 1408
BF = jnp.bfloat16
F32 = jnp.float32
I16 = jnp.int16
MESH = pl.DeviceIdType.MESH
VM = pl.BlockSpec(memory_space=pltpu.VMEM)
HB = pl.BlockSpec(memory_space=pl.ANY)
RESULT = pltpu.VMEM
GROUP = 4
BOTH = (0, 1)
THREE = (0, 1, 2)
OTHERS = (1, 2, 3)
EDGE_IN, GRAD_IN, EDGE_OUT, GRAD_OUT = range(4)
SEND_ORDER = (2, 3, 1)
LROWS = 7 * (D // 4)
HEAD = 16
LEADER = GROUP - 1
VMEM_LIMIT = 63_000_000
SLABS = 8
EARLY = 6
VEC_SLAB = 5
EDGE_SLABS = (0, 1, 6, 7)
STAGES = (slice(0, EARLY), slice(EARLY, SLABS))


def dot(a, b):
    return jnp.dot(a, b, preferred_element_type=F32)


def dot_nt(a, b):
    return lax.dot_general(a, b, (((1,), (1,)), ((), ())), preferred_element_type=F32)


def mat(k, n=1):
    return slice(k * D, (k + n) * D)


def rows_of(d):
    q = D // 4
    return slice(d * q, (d + 1) * q)


def at(step, width):
    return pl.ds(pl.multiple_of(step * width, width), width)


def loop(stop, body, start=0):
    def step(j, carry):
        body(j)
        return carry

    lax.fori_loop(start, stop, step, 0)


def column_sum(val):
    return jnp.sum(val, axis=0, keepdims=True)


def flip(val):
    return jnp.swapaxes(val, 0, 1)


def stacked(parts):
    return jnp.concatenate(parts, axis=0)


def beside(parts):
    return jnp.concatenate(parts, axis=1)


def slot(d):
    return d - 1


def sigmoid(hidden):
    return 1.0 / (1.0 + jnp.exp(-hidden))


def fold(val):
    total = val[:, mat(0)]
    for start in range(D, val.shape[1], D):
        total = total + val[:, start:start + D]
    return total


def swap_halves(val):
    return stacked([val[rows_of(d)] for d in (1, 0, 3, 2)])


def gather(table, keys, iota):
    acc = None
    nodes = table.shape[1]
    one, zero = jnp.ones((), BF), jnp.zeros((), BF)
    for base in range(0, nodes, T):
        width = min(T, nodes - base)
        ids = iota[0:width, :]
        hot = beside([jnp.where(ids == (key - jnp.asarray(base, I16)), one, zero) for key in keys])
        part = dot(table[:, base:base + width], hot)
        acc = part if acc is None else acc + part
    return acc


def scatter(acc_ref, val, cols, lanes):
    nodes = acc_ref.shape[1]
    one, zero = jnp.ones((), BF), jnp.zeros((), BF)
    row = lanes[0:1, :]
    for base in range(0, nodes, T):
        width = min(T, nodes - base)
        hot = beside([jnp.where((row + jnp.asarray(base + s, I16)) == cols, one, zero) for s in range(0, width, D)])
        acc_ref[:, base:base + width] += dot(val, hot)


def mlp_tail(hidden, w2t, vec):
    act = (hidden * sigmoid(hidden)).astype(BF)
    out = dot(w2t, act) + vec[0]
    mean = column_sum(out) / D
    centered = out - mean
    var = column_sum(centered * centered) / D
    inv = lax.rsqrt(var + LN_EPS)
    normed = centered * inv
    message = (normed * vec[1] + vec[2]).astype(BF)
    return message, normed, inv


def mlp_back(d_msg, hidden, normed, inv, w2, vec):
    d_normed = d_msg * vec[1]
    mean0 = column_sum(d_normed) / D
    mean1 = column_sum(d_normed * normed) / D
    d_out = inv * (d_normed - mean0 - normed * mean1)
    d_out_bf = d_out.astype(BF)
    sig = sigmoid(hidden)
    act = (hidden * sig).astype(BF)
    d_w2 = dot_nt(d_out_bf, act)
    d_hidden = dot(w2, d_out_bf) * (sig * (1.0 + hidden * (1.0 - sig)))
    sums = (fold(d_out), fold(d_msg * normed), fold(d_msg), fold(d_hidden))
    return d_hidden.astype(BF), d_w2, sums


def add_sums(ref, parts):
    for q in range(4):
        total = parts[0][q]
        for other in parts[1:]:
            total = total + other[q]
        ref[mat(q), :] += total


def step_kernel(dims, *refs):
    layers, cols, nodes, edges, npad, eh, dpn = dims
    nch = eh // EC
    top = layers - 1
    n_in = 14
    hbm_in = refs[:n_in]
    n_out = 12
    (node_raw, edge_raw, gnode_raw, gedge_raw, ew1_buf, eb1_buf, ew2_buf, evec_buf, nw1_buf, nb1_buf, nw2_buf, nvec_buf) = refs[n_in:n_in + n_out]
    (send_ids, recv_ids, ew1_in, ew2_in, nw1_in, nw2_in, evec_in, nvec_in, eb1_in, nb1_in, w_send, w_recv, n_send, n_recv, gn_send, gn_recv, no_send, no_recv, dn_send, dn_recv,
     e_send, g_send, e_recv, g_recv, eo_recv, de_recv, part, part_recv, hidden, normed, inv, nhid, nnrm, ninv, d_part, s_sum, r_sum,
     ids_raw, bias_cols, sums, grad, core_recv, half, dp_recv, cross_send, cross_recv, own_sum, gathered,
     core_rs, dp_rs, cross_rs, w_rs, n_rs, e_rs, o_rs, p_rs, ready, load_sem, w_ss, n_ss, e_ss, p_ss, core_ss, dp_ss, cross_ss) = refs[n_in + n_out:]

    t = lax.axis_index('tp')
    p = lax.axis_index('dp')
    per = SLABS // dpn
    dp_others = range(1, dpn)
    x, c = t // 2, lax.rem(t, 2)
    ox, oc = 1 - x, 1 - c
    peer = [t, t + 1 - 2 * c, t + 2 - 4 * x, t + 3 - 2 * c - 4 * x]

    def remote(src, dst, ssem, rsem, d):
        return pltpu.make_async_remote_copy(src_ref=src, dst_ref=dst, send_sem=ssem, recv_sem=rsem,
                                            device_id={'tp': peer[d]}, device_id_type=MESH)

    small_in = (send_ids, recv_ids, ew1_in, ew2_in, nw1_in, nw2_in, evec_in, nvec_in, eb1_in, nb1_in)
    loads = [pltpu.make_async_copy(src, dst, load_sem.at[q]) for q, (src, dst) in enumerate(
        zip(hbm_in, (node_raw, edge_raw, gnode_raw, gedge_raw) + small_in))]

    def node_copies(send, recv, kind):
        return (remote(send.at[1], recv.at[0], n_ss.at[kind, 0], n_rs.at[kind, 0], 1),
                remote(send.at[0], recv.at[1], n_ss.at[kind, 1], n_rs.at[kind, 1], 2),
                remote(recv.at[1], recv.at[2], n_ss.at[kind, 2], n_rs.at[kind, 2], 1))

    piece = w_send.shape[0] // dpn

    def packed(l, k, count=1):
        return pl.ds(HEAD + l * LROWS + k * cols, count * cols)

    def weight_rows(owner):
        return pl.ds(pl.multiple_of(owner * piece, 8), piece)

    w_pair = remote(w_send, w_recv.at[0], w_ss.at[0], w_rs.at[0], 1)
    w_cross = remote(w_send.at[weight_rows(p)], w_recv.at[1, weight_rows(p)], w_ss.at[1], w_rs.at[1], 2)
    w_relay = remote(w_recv.at[1], w_recv.at[2], w_ss.at[2], w_rs.at[2], 1)

    def weight_copy(i, owner):
        rows = w_recv.at[1, weight_rows(owner)]
        return dp_remote(rows, rows, 2, 0, i)

    last = nch - 1
    hold = nch - 3
    buffers = ((e_send, e_recv), (g_send, g_recv), (e_send, eo_recv), (g_send, de_recv))

    def outward(kind):
        return kind in (EDGE_OUT, GRAD_OUT)

    def edge_part(kind, index, send_sem, recv_sem, d):
        src, dst = buffers[kind]
        recv_sems = o_rs.at[kind - EDGE_OUT, recv_sem] if outward(kind) else e_rs.at[kind, recv_sem]
        return remote(src.at[index], dst.at[index], e_ss.at[kind, send_sem], recv_sems, d)

    def by_half(half_id, j, action):
        narrow = jnp.logical_and(j == last, half_id == 1)

        @pl.when(jnp.logical_not(narrow))
        def _():
            action(slice(None))

        @pl.when(narrow)
        def _():
            action(slice(T))

    def edge_start(kind, j, d):
        other = oc if d % 2 else c
        if outward(kind):
            send_sem, recv_sem = jnp.where(j == last, 1, 0), jnp.where(j == last, 2 + slot(d), jnp.where(j < hold, 0, 1))
        else:
            send_sem, recv_sem = jnp.where(j == last, d, 0), j
        by_half(c if outward(kind) else other, j,
                lambda used: edge_part(kind, (slot(d), j, slice(None), used), send_sem, recv_sem, d).start())

    def edges_sent(kind):
        every = slice(None)
        edge_part(kind, (every, slice(0, last)), 0, 0, 1).wait_send()
        if outward(kind):
            by_half(c, last, lambda used: edge_part(kind, (every, last, every, used), 1, 0, 1).wait_send())
        else:
            for d in OTHERS:
                by_half(oc if d % 2 else c, last, lambda used: edge_part(kind, (slot(d), last, every, used), d, 0, d).wait_send())

    def chunk_arrived(kind, j):
        every = slice(None)
        by_half(c, j, lambda used: edge_part(kind, (every, j, every, used), 0, j, 1).wait_recv())

    def group_arrived(kind, group):
        every = slice(None)
        if group < 2:
            edge_part(kind, (every, (slice(0, hold), slice(hold, last))[group]), 0, group, 1).wait_recv()
        else:
            for d in OTHERS:
                by_half(oc if d % 2 else c, last, lambda used: edge_part(kind, (slot(d), last, every, used), 0, 2 + slot(d), d).wait_recv())

    def core_copy(l, b, stage):
        first, count = ((0, EARLY), (EARLY, SLABS - EARLY))[stage]
        return remote(grad.at[l, pl.ds(first, count), pl.ds((2 * b + 1) * cols, cols), :], core_recv.at[l, b, pl.ds(first, count)],
                      core_ss.at[l, stage], core_rs.at[l, stage], 1)

    def core_all(l, stage):
        part_of = core_recv.at[l, :, (slice(0, EARLY), slice(EARLY, SLABS))[stage]]
        return remote(part_of, part_of, core_ss.at[l, stage], core_rs.at[l, stage], 1)

    def seat(device):
        return lax.rem(device + dpn // 2, dpn)

    def in_stage(device, stage):
        early = (seat(device) + 1) * per <= EARLY
        return jnp.logical_not(early) if stage else early

    def dp_remote(src, dst, stage, l, i):
        return pltpu.make_async_remote_copy(src_ref=src, dst_ref=dst, send_sem=dp_ss.at[stage, l], recv_sem=dp_rs.at[stage, l],
                                            device_id={'dp': lax.rem(p + i, dpn)}, device_id_type=MESH)

    def spread_copy(l, i):
        return dp_remote(half.at[l, pl.ds(seat(lax.rem(p + i, dpn)) * per, per)], dp_recv.at[l, pl.ds((i - 1) * per, per)], 0, l, i)

    def dp_all(l, stage):
        most = (dpn - 1) * per
        part_of = (dp_recv.at[l], gathered.at[l, pl.ds(0, most)], w_recv.at[1, pl.ds(0, (dpn - 1) * piece)])[stage]
        return dp_remote(part_of, part_of, stage, l, 1)

    def cross_copy(l):
        return remote(cross_send.at[l], cross_recv.at[l], cross_ss.at[l], cross_rs.at[l], 2)

    def gather_copy(l, i, owner):
        return dp_remote(own_sum.at[l], gathered.at[l, pl.ds(seat(owner) * per, per)], 1, l, i)

    def part_copy(q):
        return remote(part.at[q], part_recv.at[q], p_ss.at[q], p_rs.at[q], 1)

    def load_nodes(raw, send, own):
        send[...] = jnp.zeros_like(send)
        send[0, :, :nodes] = raw[ox].astype(F32)
        send[1, :, :nodes] = raw[x].astype(F32)
        own[:cols, :] = send[1].astype(own.dtype)

    def load_edges(raw, send, own, kind):
        def put(j, lanes_j, val_of):
            for d in OTHERS:
                sample = x if d < 2 else ox
                send[slot(d), j] = val_of(sample, oc if d % 2 else c).astype(F32)
            own[:cols, lanes_j] = val_of(x, c)

        def chunk(j):
            put(j, at(j, EC), lambda s, h: raw[s, :, pl.ds(pl.multiple_of(h * eh + j * EC, D), EC)])
            for d in SEND_ORDER:
                edge_start(kind, j, d)

        loop(nch - 1, chunk)
        first = (nch - 1) * EC
        used = edges - eh - first
        last = pl.ds(first, EC)

        def tail(s, h):
            left = raw[s, :, pl.ds(first, EC)]
            right = beside([raw[s, :, pl.ds(eh + first, used)], jnp.zeros((cols, EC - used), BF)])
            return jnp.where(h == 0, left.astype(F32), right.astype(F32)).astype(BF)

        put(nch - 1, last, tail)
        for d in SEND_ORDER:
            edge_start(kind, nch - 1, d)

    def place_edges(raw, block, d, j):
        s = x if d < 2 else ox
        h = oc if d % 2 else c
        val = block.astype(BF)
        first = (nch - 1) * EC
        used = edges - eh - first

        @pl.when(jnp.logical_or(j < nch - 1, h == 0))
        def _():
            raw[s, :, pl.ds(pl.multiple_of(h * eh + j * EC, D), EC)] = val

        @pl.when(jnp.logical_and(j == nch - 1, h == 1))
        def _():
            raw[s, :, pl.ds(eh + first, used)] = val[:, :used]

    def scoped(e0, e1, ge, msg, v0, v1, v2, agg0, agg1, d_agg, scol, rcol, srow, rrow, iota, lanes, ew1, ew1t, ew2, ew2t, nw1, nw1t, nw2, nw2t, vecs):
        tables = (v0, v1, v2)
        aggs = (agg0, agg1)
        edges_in = (e0, e1)

        barrier = pltpu.get_barrier_semaphore()
        for d in OTHERS:
            pl.semaphore_signal(barrier, inc=1, device_id={'tp': peer[d]}, device_id_type=MESH)
        for copy in loads[:1] + loads[4:] + loads[1:4]:
            copy.start()
        loads[0].wait()
        with jax.named_scope('send_nodes'):
            load_nodes(node_raw, n_send, v0)
        ncop = node_copies(n_send, n_recv, 0)
        for copy in loads[4:]:
            copy.wait()
        q = cols
        w_send[:HEAD, :] = jnp.zeros((HEAD, D), F32)
        for k in THREE:
            w_send[k * layers:(k + 1) * layers, :cols] = evec_in[k]
            w_send[(3 + k) * layers:(4 + k) * layers, :cols] = nvec_in[k]
        for l in range(layers):
            w_send[packed(l, 0, 3), :] = ew1_in[pl.ds(l * 3 * q, 3 * q), :].astype(F32)
            w_send[packed(l, 3), :] = ew2_in[pl.ds(l * q, q), :].astype(F32)
            w_send[packed(l, 4, 2), :] = nw1_in[pl.ds(l * 2 * q, 2 * q), :].astype(F32)
            w_send[packed(l, 6), :] = nw2_in[pl.ds(l * q, q), :].astype(F32)
        with jax.named_scope('barrier'):
            @pl.when(t != LEADER)
            def _():
                pl.semaphore_wait(barrier, len(OTHERS))
                pl.semaphore_signal(ready, inc=1, device_id={'tp': LEADER}, device_id_type=MESH)

            @pl.when(t == LEADER)
            def _():
                pl.semaphore_wait(ready, len(OTHERS))
                for i in dp_others:
                    pl.semaphore_signal(barrier, inc=1, device_id={'dp': lax.rem(p + i, dpn)}, device_id_type=MESH)

        w_cross.start()
        w_pair.start()
        ncop[1].start()
        ncop[0].start()
        loads[1].wait()
        with jax.named_scope('send_edges'):
            load_edges(edge_raw, e_send, e0, EDGE_IN)
        loads[2].wait()
        load_nodes(gnode_raw, gn_send, d_part)
        gcop = node_copies(gn_send, gn_recv, 1)
        gcop[1].start()
        gcop[0].start()
        loads[3].wait()
        with jax.named_scope('send_grads'):
            load_edges(gedge_raw, g_send, ge, GRAD_IN)

        with jax.named_scope('dp_barrier'):
            @pl.when(t == LEADER)
            def _():
                pl.semaphore_wait(barrier, len(OTHERS) + dpn - 1)
                for d in OTHERS:
                    pl.semaphore_signal(ready, inc=1, device_id={'tp': peer[d]}, device_id_type=MESH)

            @pl.when(t != LEADER)
            def _():
                pl.semaphore_wait(ready, 1)

        w_cross.wait_recv()
        for i in dp_others:
            weight_copy(i, p).start()

        @pl.when(c == 1)
        def _():
            for recv in (e_recv, g_recv):
                recv[:, nch - 1, :, T:] = jnp.zeros((3, cols, EC - T), F32)

        iota[...] = lax.broadcasted_iota(jnp.int32, (T, D), 0).astype(I16)
        lanes[...] = lax.broadcasted_iota(jnp.int32, (16, D), 1).astype(I16)

        ids_raw[...] = jnp.full(ids_raw.shape, -1, jnp.int32)
        for which, src in enumerate((send_ids, recv_ids)):
            ids_raw[which:which + 1, :edges] = src[...].reshape(1, edges)

        def ids(b):
            for which, (row_ref, col_ref) in enumerate(((srow, scol), (rrow, rcol))):
                wide = jnp.broadcast_to(ids_raw[which:which + 1, pl.ds(pl.multiple_of(c * eh + b * D, D), D)], (D, D))
                row_ref[at(b, 16), :] = wide[:16].astype(I16)
                col_ref[at(b, D), :] = flip(wide.astype(F32)).astype(jnp.int32).astype(I16)

        with jax.named_scope('ids'):
            loop(eh // D, ids)

        def keys(ref, step):
            return [ref[pl.ds(pl.multiple_of(step * (KS // D) * 16 + 16 * h, 16), 1), :] for h in range(KS // D)]

        bias_cols[...] = flip(stacked([eb1_in[...], nb1_in[...], jnp.zeros((D - 2 * layers, D), F32)]))

        def join_weights(l):
            for d in range(GROUP):
                src = w_recv.at[slot(d)] if d else w_send
                r = rows_of(d)
                for k in THREE:
                    ew1[l, pl.ds(k * D + d * q, q), :] = src[packed(l, k), :].astype(BF)
                ew2t[l, r, :] = src[packed(l, 3), :].astype(BF)
                for k in BOTH:
                    nw1[l, pl.ds(k * D + d * q, q), :] = src[packed(l, 4 + k), :].astype(BF)
                nw2t[l, r, :] = src[packed(l, 6), :].astype(BF)

            def flip_bf(mat):
                return flip(mat.astype(F32)).astype(BF)

            for k in THREE:
                ew1t[l, :, mat(k)] = flip_bf(ew1[l, mat(k), :])
            for k in BOTH:
                nw1t[l, :, mat(k)] = flip_bf(nw1[l, mat(k), :])
            ew2[l] = flip_bf(ew2t[l])
            nw2[l] = flip_bf(nw2t[l])

        def wait_recvs(copies):
            copies[1].wait_recv()
            copies[2].start()
            copies[0].wait_recv()
            copies[2].wait_recv()

        with jax.named_scope('node_wait'):
            wait_recvs(ncop)
        for d in OTHERS:
            v0[rows_of(d), :] = n_recv[slot(d)].astype(BF)
        with jax.named_scope('weight_wait'):
            dp_all(0, 2).wait_recv()
            w_relay.start()
            w_pair.wait_recv()
            w_relay.wait_recv()
        rows_all = beside([w_send[:HEAD, :cols]] + [w_recv[d, :HEAD, :cols] for d in range(3)])
        vecs[...] = flip(stacked([rows_all, jnp.zeros((D - HEAD, D), F32)]))
        join_weights(0)

        def vec(l, node):
            first = 6 * node + l
            return [vecs[:, first + 2 * k:first + 2 * k + 1] for k in THREE]

        def bias(l, node):
            return bias_cols[:, node * layers + l:node * layers + l + 1]

        def hidden_of_nodes(l):
            table, b1 = tables[l], bias(l, 0)

            def body(step):
                xs = gather(table, keys(srow, step), iota).astype(BF)
                xr = gather(table, keys(rrow, step), iota).astype(BF)
                hidden[l, :, at(step, KS)] = dot(ew1t[l, :, mat(1, 2)], stacked([xs, xr])) + b1

            loop(eh // KS, body)

        def edge_forward(l):
            e_in = edges_in[l]

            def body(j):
                for sub in range(EC // T):
                    a = at(j * (EC // T) + sub, T)
                    if l == 0:
                        if sub == 0:
                            chunk_arrived(EDGE_IN, j)
                        for d in OTHERS:
                            e_in[rows_of(d), a] = e_recv[slot(d), j, :, sub * T:(sub + 1) * T].astype(BF)
                    e_val = e_in[:, a]
                    hid = hidden[l, :, a] + dot(ew1t[l, :, mat(0)], e_val)
                    hidden[l, :, a] = hid
                    message, nrm, std = mlp_tail(hid, ew2t[l], vec(l, 0))
                    normed[l, :, a] = nrm
                    inv[l:l + 1, a] = std
                    msg[:, a] = message
                    e_new = (e_val.astype(F32) + message.astype(F32)).astype(BF)
                    if l < top:
                        edges_in[l + 1][:, a] = e_new
                    else:
                        for d in OTHERS:
                            e_send[slot(d), j, :, sub * T:(sub + 1) * T] = e_new[rows_of(d)].astype(F32)
                        if sub == 0:
                            own_parts = []
                        own_parts.append(e_new[:q])
                if l == top:
                    for d in SEND_ORDER:
                        edge_start(EDGE_OUT, j, d)
                    place_edges(edge_raw, beside(own_parts), 0, j)

            loop(nch, body)

        def segment_sum(acc, ids_ref):
            acc[...] = jnp.zeros(acc.shape, F32)

            def body(step):
                scatter(acc, msg[:, at(step, KS)], ids_ref[at(step, KS), :], lanes)

            loop(eh // KS, body)

        def node_forward(l):
            table, agg, out = tables[l], aggs[l], tables[l + 1]

            def body(step):
                a = pl.ds(pl.multiple_of(step * TN, D), TN)
                v_in = table[:, a]
                agg_bf = (part[l, :, a] + swap_halves(part_recv[l, :, a])).astype(BF)
                agg[:, a] = agg_bf
                hid = dot(nw1t[l], stacked([v_in, agg_bf])) + bias(l, 1)
                nhid[l, :, a] = hid
                message, nrm, std = mlp_tail(hid, nw2t[l], vec(l, 1))
                nnrm[l, :, a] = nrm
                ninv[l:l + 1, a] = std
                out[:, a] = (v_in.astype(F32) + message.astype(F32)).astype(BF)

            loop(npad // TN, body)

        for l in range(layers):
            with jax.named_scope(f'gather_{l}'):
                hidden_of_nodes(l)
            if l == top:
                edges_sent(EDGE_IN)
            with jax.named_scope(f'edge_forward_{l}'):
                edge_forward(l)
            with jax.named_scope(f'sum_{l}'):
                segment_sum(part.at[l], rcol)
            part_copy(l).start()
            if l == 0:
                join_weights(1)
                gcop[1].wait_recv()
                gcop[2].start()
            with jax.named_scope(f'part_wait_{l}'):
                part_copy(l).wait_recv()
            with jax.named_scope(f'node_forward_{l}'):
                node_forward(l)
        no_send[...] = tables[layers][rows_of(2), :].astype(F32)
        no_copy = remote(no_send, no_recv, n_ss.at[2, 0], n_rs.at[2, 0], 2)
        no_copy.start()
        node_raw[x] = tables[layers][:q, :nodes]

        grad[...] = jnp.zeros_like(grad)
        sums[...] = jnp.zeros_like(sums)
        with jax.named_scope('grad_node_wait'):
            gcop[0].wait_recv()
            gcop[2].wait_recv()
        for d in OTHERS:
            d_part[rows_of(d), :] = gn_recv[slot(d)]

        def node_backward(l):
            table, agg = tables[l], aggs[l]

            def body(step):
                a = pl.ds(pl.multiple_of(step * TN, D), TN)
                d_in = d_part[:, a]
                if l < top:
                    d_in = d_in + part[layers + l + 1, :, a] + swap_halves(part_recv[layers + l + 1, :, a])
                    d_in = d_in.astype(BF).astype(F32)
                d_hid, d_w2, parts = mlp_back(d_in, nhid[l, :, a], nnrm[l, :, a], ninv[l:l + 1, a], nw2[l], vec(l, 1))
                add_sums(sums.at[l, 1], [parts])
                grad[l, 4] += d_w2
                grad[l, 2] += dot_nt(table[:, a], d_hid)
                grad[l, 3] += dot_nt(agg[:, a], d_hid)
                d_part[:, a] = d_in + dot(nw1[l, mat(0), :], d_hid)
                d_agg[:, a] = dot(nw1[l, mat(1), :], d_hid).astype(BF)

            loop(npad // TN, body)

        def gather_back():
            def body(step):
                msg[:, at(step, KS)] = gather(d_agg, keys(rrow, step), iota).astype(BF)

            loop(eh // KS, body)

        def edge_backward(l):
            e_in = edges_in[l]

            def body(j):
                all_parts, d_w2s, d_w1s, own_parts = [], [], [], []
                for sub in range(EC // T):
                    a = at(j * (EC // T) + sub, T)
                    if l == top:
                        if sub == 0:
                            chunk_arrived(GRAD_IN, j)
                        for d in OTHERS:
                            ge[rows_of(d), a] = g_recv[slot(d), j, :, sub * T:(sub + 1) * T].astype(BF)
                    d_res = ge[:, a].astype(F32)
                    d_msg = d_res + msg[:, a].astype(F32)
                    d_hid, d_w2, parts = mlp_back(d_msg, hidden[l, :, a], normed[l, :, a], inv[l:l + 1, a], ew2[l], vec(l, 0))
                    all_parts.append(parts)
                    d_w2s.append(d_w2)
                    d_w1s.append(dot_nt(e_in[:, a], d_hid))
                    msg[:, a] = d_hid
                    d_new = (d_res + dot(ew1[l, mat(0), :], d_hid)).astype(BF)
                    if l > 0:
                        ge[:, a] = d_new
                    else:
                        for d in OTHERS:
                            g_send[slot(d), j, :, sub * T:(sub + 1) * T] = d_new[rows_of(d)].astype(F32)
                        own_parts.append(d_new[:q])
                add_sums(sums.at[l, 0], all_parts)
                grad[l, 1] += sum(d_w2s[1:], d_w2s[0])
                grad[l, 0] += sum(d_w1s[1:], d_w1s[0])
                if l == 0:
                    @pl.when(j < hold)
                    def _():
                        for d in SEND_ORDER:
                            edge_start(GRAD_OUT, j, d)
                    place_edges(gedge_raw, beside(own_parts), 0, j)

            loop(nch, body)

        def vector_slab(l):
            def total(node, k):
                return column_sum(flip(sums[l, node, mat(k), :]))

            lat = stacked([total(node, k) for node in BOTH for k in THREE])
            biases = stacked([total(node, 3) for node in BOTH])
            n_lat = lat.shape[0]
            for d in range(GROUP):
                grad[l, VEC_SLAB, d * cols:d * cols + n_lat, :cols] = lat[:, rows_of(d)]
                grad[l, VEC_SLAB, d * cols + n_lat:d * cols + n_lat + 2, :] = biases

        def reduce_start(l, stage):
            for b in BOTH:
                core_copy(l, b, stage).start()

        def chip_sum(l, stage):
            row = lax.broadcasted_iota(jnp.int32, (cols, D), 0)
            edge_row = jnp.logical_or(row < 3, row == 6)
            core_all(l, stage).wait_recv()
            for b in BOTH:
                for k in range(SLABS)[STAGES[stage]]:
                    own = grad[l, k, rows_of(2 * b), :]
                    if k in EDGE_SLABS:
                        own = own + core_recv[l, b, k]
                    elif k == VEC_SLAB:
                        own = own + jnp.where(edge_row, core_recv[l, b, k], 0.0)
                    half[l, k, b] = own
            for i in dp_others:
                @pl.when(in_stage(lax.rem(p + i, dpn), stage))
                def _():
                    spread_copy(l, i).start()

        def dp_sum(l, stage):
            @pl.when(in_stage(p, stage))
            def _():
                total = half[l, pl.ds(seat(p) * per, per)]
                dp_all(l, 0).wait_recv()
                for i in dp_others:
                    total = total + dp_recv[l, pl.ds((i - 1) * per, per)]
                own_sum[l] = total[:, 0]
                cross_send[l] = total[:, 1]
                cross_copy(l).start()

        def cross_sum(l):
            cross_copy(l).wait_recv()
            total = own_sum[l] + cross_recv[l]
            own_sum[l] = total
            gathered[l, pl.ds(seat(p) * per, per)] = total
            for i in dp_others:
                gather_copy(l, i, p).start()

        def project(l):
            table = tables[l]

            def body(step):
                a = pl.ds(pl.multiple_of(step * TN, D), TN)
                s_bf, r_bf, v_in = s_sum[:, a].astype(BF), r_sum[:, a].astype(BF), table[:, a]
                part[layers + l, :, a] = dot(ew1[l, mat(1), :], s_bf) + dot(ew1[l, mat(2), :], r_bf)
                grad[l, 6] += dot_nt(v_in, s_bf)
                grad[l, 7] += dot_nt(v_in, r_bf)

            loop(npad // TN, body)

        for l in reversed(range(layers)):
            first_layer = l == 0
            with jax.named_scope(f'node_backward_{l}'):
                node_backward(l)
            if first_layer:
                with jax.named_scope('chip_sum_1'):
                    chip_sum(1, 0)
                    chip_sum(1, 1)
            with jax.named_scope(f'gather_back_{l}'):
                gather_back()
            if first_layer:
                edges_sent(GRAD_IN)
            with jax.named_scope(f'edge_backward_{l}'):
                edge_backward(l)
            vector_slab(l)
            reduce_start(l, 0)
            if first_layer:
                with jax.named_scope('dp_sum_1'):
                    dp_sum(1, 0)
                    dp_sum(1, 1)
            with jax.named_scope(f'sum_send_{l}'):
                segment_sum(s_sum, scol)
            if first_layer:
                with jax.named_scope('chip_sum_0'):
                    chip_sum(0, 0)
            with jax.named_scope(f'sum_recv_{l}'):
                segment_sum(r_sum, rcol)
            with jax.named_scope(f'project_{l}'):
                project(l)
            reduce_start(l, 1)
            part_copy(layers + l).start()
            if first_layer:
                with jax.named_scope('chip_sum_late'):
                    chip_sum(0, 1)
                with jax.named_scope('dp_sum_0'):
                    dp_sum(0, 0)
            with jax.named_scope(f'back_wait_{l}'):
                part_copy(layers + l).wait_recv()

        def final(step):
            a = pl.ds(pl.multiple_of(step * TN, D), TN)
            d_in = (d_part[:, a] + part[layers, :, a] + swap_halves(part_recv[layers, :, a])).astype(BF)
            v2[:, a] = d_in

        loop(npad // TN, final)
        gnode_raw[x] = v2[:q, :nodes]
        with jax.named_scope('dp_sum_late'):
            dp_sum(0, 1)

        dn_send[...] = v2[rows_of(2), :].astype(F32)
        dn_copy = remote(dn_send, dn_recv, n_ss.at[2, 1], n_rs.at[2, 1], 2)
        dn_copy.start()

        def send_rest(j):
            for d in SEND_ORDER:
                edge_start(GRAD_OUT, j, d)

        loop(nch, send_rest, hold)

        with jax.named_scope('node_out_wait'):
            no_copy.wait_recv()
        node_raw[ox] = no_recv[:, :nodes].astype(BF)

        def place_e(j):
            for d in OTHERS:
                place_edges(edge_raw, eo_recv[slot(d), j], d, j)

        with jax.named_scope('place_edge_out'):
            for group in THREE:
                group_arrived(EDGE_OUT, group)
            loop(nch, place_e)

        def place_g(j):
            for d in OTHERS:
                place_edges(gedge_raw, de_recv[slot(d), j], d, j)

        with jax.named_scope('place_first'):
            group_arrived(GRAD_OUT, 0)
            loop(hold, place_g)
        for l in range(layers):
            with jax.named_scope(f'cross_sum_{l}'):
                cross_sum(l)
        with jax.named_scope('d_node_wait'):
            dn_copy.wait_recv()
        gnode_raw[ox] = dn_recv[:, :nodes].astype(BF)
        with jax.named_scope('place_rest'):
            group_arrived(GRAD_OUT, 1)
            loop(last, place_g, hold)
        for l in range(layers):
            dp_all(l, 1).wait_recv()
            ew1_buf[l, 0] = gathered[l, 0]
            ew1_buf[l, 1:] = gathered[l, EARLY:]
            ew2_buf[l] = gathered[l, 1]
            nw1_buf[l] = gathered[l, 2:4]
            nw2_buf[l] = gathered[l, 4]
            small = gathered[l, VEC_SLAB]
            for k in THREE:
                evec_buf[k, l:l + 1, :] = small[k:k + 1, :cols]
                nvec_buf[k, l:l + 1, :] = small[3 + k:4 + k, :cols]
            eb1_buf[l:l + 1, :] = small[6:7]
            nb1_buf[l:l + 1, :] = small[7:8]
        for l in range(layers):
            for stage in BOTH:
                core_all(l, stage).wait_send()
            cross_copy(l).wait_send()
            dp_all(l, 0).wait_send()
            dp_all(l, 1).wait_send()
        for copy in ncop + gcop + (w_pair, w_cross, w_relay):
            copy.wait_send()
        dp_all(0, 2).wait_send()
        no_copy.wait_send()
        dn_copy.wait_send()
        for k in range(2 * layers):
            part_copy(k).wait_send()
        edges_sent(EDGE_OUT)
        with jax.named_scope('place_last'):
            group_arrived(GRAD_OUT, 2)
            loop(nch, place_g, last)
        edges_sent(GRAD_OUT)

    bf = lambda *s: pltpu.VMEM(s, BF)
    pl.run_scoped(
        scoped, bf(D, eh), bf(D, eh), bf(D, eh), bf(D, eh), bf(D, npad), bf(D, npad), bf(D, npad), bf(D, npad), bf(D, npad), bf(D, npad),
        pltpu.VMEM((eh, D), I16), pltpu.VMEM((eh, D), I16), pltpu.VMEM((eh // D * 16, D), I16), pltpu.VMEM((eh // D * 16, D), I16),
        pltpu.VMEM((T, D), I16), pltpu.VMEM((16, D), I16),
        bf(layers, 3 * D, D), bf(layers, D, 3 * D), bf(layers, D, D), bf(layers, D, D),
        bf(layers, 2 * D, D), bf(layers, D, 2 * D), bf(layers, D, D), bf(layers, D, D), pltpu.VMEM((D, D), F32))


def finish_moves(src, dst):
    if len(src.shape) != 3 or src.dtype != BF:
        return [(src, dst)]
    return [(src.at[s, pl.ds(r, 8)], dst.at[s, pl.ds(r, 8)]) for s in range(src.shape[0]) for r in range(0, src.shape[1], 8)]


def finish_kernel(*refs):
    count = len(refs) // 2
    moves = sum((finish_moves(refs[k], refs[count + k]) for k in range(count)), [])
    puts = [pltpu.make_async_copy(src, dst, refs[-1]) for src, dst in moves]
    for put in puts:
        put.start()
    for put in puts:
        put.wait()


def keep_in_vmem(val):
    return pltpu.with_memory_space_constraint(val, pltpu.VMEM)


def finish(arrays):
    return pl.pallas_call(
        finish_kernel,
        name='finish',
        out_shape=[jax.ShapeDtypeStruct(a.shape, a.dtype) for a in arrays],
        in_specs=[VM] * len(arrays),
        out_specs=[HB] * len(arrays),
        scratch_shapes=[pltpu.SemaphoreType.DMA],
        compiler_params=pltpu.CompilerParams(vmem_limit_bytes=1 << 20),
    )(*[keep_in_vmem(a) for a in arrays])


def solution(mesh):
    lat_spec = P('dp', None, 'tp')
    first_spec = P(None, None, 'tp', None)
    col_spec = P(None, None, 'tp')
    param_specs = (first_spec, P(), col_spec, col_spec, first_spec, P(), col_spec, col_spec)
    in_specs = (lat_spec, lat_spec, P(), P(), lat_spec, lat_spec) + param_specs
    out_specs = (lat_spec, lat_spec, lat_spec, lat_spec) + param_specs
    shape = jax.ShapeDtypeStruct

    def local_step(node_lat, edge_lat, senders, receivers, grad_node, grad_edge, edge_w1, edge_b1, edge_w2, edge_vec, node_w1, node_b1, node_w2, node_vec):
        layers = edge_w1.shape[0]
        cols = node_lat.shape[2]
        nodes, edges = node_lat.shape[1], edge_lat.shape[1]
        npad = -(-nodes // TN) * TN
        eh = -(-edges // (2 * EC)) * EC
        nch = eh // EC
        dpn = mesh.shape['dp']
        per = SLABS // dpn
        dims = (layers, cols, nodes, edges, npad, eh, dpn)
        flat = lambda arr: jnp.swapaxes(arr, 1, 2)
        lead = lambda arr: jnp.transpose(arr, (1, 0, 2))
        args = (flat(node_lat), flat(edge_lat), flat(grad_node), flat(grad_edge), senders, receivers,
                edge_w1.reshape(-1, D), flat(edge_w2).reshape(-1, D), node_w1.reshape(-1, D), flat(node_w2).reshape(-1, D),
                lead(edge_vec), lead(node_vec), edge_b1, node_b1)
        vm, sem = pltpu.VMEM, pltpu.SemaphoreType.DMA
        wrows = -(-(HEAD + layers * LROWS) // (8 * dpn)) * 8 * dpn
        lat_n, lat_e = (2, cols, nodes), (2, cols, edges)
        outs = [RESULT(lat_n, BF), RESULT(lat_e, BF), RESULT(lat_n, BF), RESULT(lat_e, BF),
                RESULT((layers, 3, cols, D), F32), RESULT((layers, D), F32), RESULT((layers, cols, D), F32), RESULT((3, layers, cols), F32),
                RESULT((layers, 2, cols, D), F32), RESULT((layers, D), F32), RESULT((layers, cols, D), F32), RESULT((3, layers, cols), F32)]
        scratch = [
            *[vm(a.shape, a.dtype) for a in args[4:]], vm((wrows, D), F32), vm((3, wrows, D), F32),
            vm((2, cols, npad), F32), vm((3, cols, npad), F32), vm((2, cols, npad), F32), vm((3, cols, npad), F32),
            vm((cols, npad), F32), vm((cols, npad), F32), vm((cols, npad), F32), vm((cols, npad), F32),
            *[vm((3, nch, cols, EC), F32)] * 6,
            vm((2 * layers, D, npad), F32), vm((2 * layers, D, npad), F32),
            vm((layers, D, eh), F32), vm((layers, D, eh), F32), vm((8, eh), F32),
            vm((layers, D, npad), F32), vm((layers, D, npad), F32), vm((8, npad), F32),
            vm((D, npad), F32), vm((D, npad), F32), vm((D, npad), F32), vm((8, 2 * eh), jnp.int32), vm((D, D), F32), vm((layers, 2, 4 * D, D), F32),
            vm((layers, SLABS, D, D), F32), vm((layers, 2, SLABS, cols, D), F32), vm((layers, SLABS, 2, cols, D), F32),
            vm((layers, (dpn - 1) * per, 2, cols, D), F32), vm((layers, per, cols, D), F32), vm((layers, per, cols, D), F32),
            vm((layers, per, cols, D), F32), vm((layers, SLABS, cols, D), F32),]
        own_sems = [
            sem((layers, 2)), sem((3, layers)), sem((layers,)), sem((3,)), sem((3, 3)), sem((2, nch)), sem((2, 5)), sem((2 * layers,)),
            pltpu.SemaphoreType.REGULAR,
            sem((len(args),)), sem((3,)), sem((3, 3)), sem((4, 4)), sem((2 * layers,)), sem((layers, 2)), sem((3, layers)), sem((layers,))]
        res = pl.pallas_call(
            lambda *refs: pl.run_scoped(lambda *own: step_kernel(dims, *refs, *own), *own_sems),
            name='graph_step',
            out_shape=outs,
            in_specs=[HB] * len(args),
            out_specs=[VM] * len(outs),
            scratch_shapes=scratch,
            compiler_params=pltpu.CompilerParams(collective_id=0, has_side_effects=True, vmem_limit_bytes=VMEM_LIMIT),
        )(*args)

        res = finish(res)
        return (flat(res[0]), flat(res[1]), flat(res[2]), flat(res[3]),
                res[4], res[5], flat(res[6]), lead(res[7]), res[8], res[9], flat(res[10]), lead(res[11]))

    return jax.shard_map(local_step, mesh=mesh, in_specs=in_specs, out_specs=out_specs, check_vma=False)
```

```python
import jax
import jax.numpy as jnp
from jax import lax
from jax.experimental import pallas as pl
from jax.experimental.pallas import tpu as pltpu
from jax.sharding import PartitionSpec as P

LN_EPS = 1e-5
D = 128
T = 256
TN = 384
EC = 512
KS = 1408
BF = jnp.bfloat16
F32 = jnp.float32
I16 = jnp.int16
MESH = pl.DeviceIdType.MESH
VM = pl.BlockSpec(memory_space=pltpu.VMEM)
HB = pl.BlockSpec(memory_space=pl.ANY)
RESULT = pltpu.VMEM
GROUP = 4
BOTH = (0, 1)
THREE = (0, 1, 2)
OTHERS = (1, 2, 3)
EDGE_IN, GRAD_IN, EDGE_OUT, GRAD_OUT = range(4)
SEND_ORDER = (2, 3, 1)
LROWS = 7 * (D // 4)
HEAD = 16
LEADER = GROUP - 1
VMEM_LIMIT = 63_000_000
SLABS = 8
EARLY = 6
VEC_SLAB = 5
EDGE_SLABS = (0, 1, 6, 7)
STAGES = (slice(0, EARLY), slice(EARLY, SLABS))


def dot(a, b):
    return jnp.dot(a, b, preferred_element_type=F32)


def dot_nt(a, b):
    return lax.dot_general(a, b, (((1,), (1,)), ((), ())), preferred_element_type=F32)


def mat(k, n=1):
    return slice(k * D, (k + n) * D)


def rows_of(d):
    q = D // 4
    return slice(d * q, (d + 1) * q)


def at(step, width):
    return pl.ds(pl.multiple_of(step * width, width), width)


def loop(stop, body, start=0):
    def step(j, carry):
        body(j)
        return carry

    lax.fori_loop(start, stop, step, 0)


def column_sum(val):
    return jnp.sum(val, axis=0, keepdims=True)


def flip(val):
    return jnp.swapaxes(val, 0, 1)


def stacked(parts):
    return jnp.concatenate(parts, axis=0)


def beside(parts):
    return jnp.concatenate(parts, axis=1)


def slot(d):
    return d - 1


def sigmoid(hidden):
    return 1.0 / (1.0 + jnp.exp(-hidden))


def fold(val):
    total = val[:, mat(0)]
    for start in range(D, val.shape[1], D):
        total = total + val[:, start:start + D]
    return total


def swap_halves(val):
    return stacked([val[rows_of(d)] for d in (1, 0, 3, 2)])


def gather(table, keys, iota):
    acc = None
    nodes = table.shape[1]
    one, zero = jnp.ones((), BF), jnp.zeros((), BF)
    for base in range(0, nodes, T):
        width = min(T, nodes - base)
        ids = iota[0:width, :]
        hot = beside([jnp.where(ids == (key - jnp.asarray(base, I16)), one, zero) for key in keys])
        part = dot(table[:, base:base + width], hot)
        acc = part if acc is None else acc + part
    return acc


def scatter(acc_ref, val, cols, lanes):
    nodes = acc_ref.shape[1]
    one, zero = jnp.ones((), BF), jnp.zeros((), BF)
    row = lanes[0:1, :]
    for base in range(0, nodes, T):
        width = min(T, nodes - base)
        hot = beside([jnp.where((row + jnp.asarray(base + s, I16)) == cols, one, zero) for s in range(0, width, D)])
        acc_ref[:, base:base + width] += dot(val, hot)


def mlp_tail(hidden, w2t, vec):
    act = (hidden * sigmoid(hidden)).astype(BF)
    out = dot(w2t, act) + vec[0]
    mean = column_sum(out) / D
    centered = out - mean
    var = column_sum(centered * centered) / D
    inv = lax.rsqrt(var + LN_EPS)
    normed = centered * inv
    message = (normed * vec[1] + vec[2]).astype(BF)
    return message, normed, inv


def mlp_back(d_msg, hidden, normed, inv, w2, vec):
    d_normed = d_msg * vec[1]
    mean0 = column_sum(d_normed) / D
    mean1 = column_sum(d_normed * normed) / D
    d_out = inv * (d_normed - mean0 - normed * mean1)
    d_out_bf = d_out.astype(BF)
    sig = sigmoid(hidden)
    act = (hidden * sig).astype(BF)
    d_w2 = dot_nt(d_out_bf, act)
    d_hidden = dot(w2, d_out_bf) * (sig * (1.0 + hidden * (1.0 - sig)))
    sums = (fold(d_out), fold(d_msg * normed), fold(d_msg), fold(d_hidden))
    return d_hidden.astype(BF), d_w2, sums


def add_sums(ref, parts):
    for q in range(4):
        total = parts[0][q]
        for other in parts[1:]:
            total = total + other[q]
        ref[mat(q), :] += total


def step_kernel(dims, *refs):
    layers, cols, nodes, edges, npad, eh, dpn = dims
    nch = eh // EC
    top = layers - 1
    n_in = 14
    hbm_in = refs[:n_in]
    n_out = 12
    (node_raw, edge_raw, gnode_raw, gedge_raw, ew1_buf, eb1_buf, ew2_buf, evec_buf, nw1_buf, nb1_buf, nw2_buf, nvec_buf) = refs[n_in:n_in + n_out]
    (send_ids, recv_ids, ew1_in, ew2_in, nw1_in, nw2_in, evec_in, nvec_in, eb1_in, nb1_in, w_send, w_recv, n_send, n_recv, gn_send, gn_recv, no_send, no_recv, dn_send, dn_recv,
     t_send, t_recv, e_send, g_send, e_recv, g_recv, eo_recv, de_recv, part, part_recv, hidden, normed, inv, nhid, nnrm, ninv, d_part, s_sum, r_sum,
     ids_raw, bias_cols, sums, grad, core_recv, half, dp_recv, cross_send, cross_recv, own_sum, gathered,
     core_rs, dp_rs, cross_rs, w_rs, n_rs, e_rs, o_rs, p_rs, ready, load_sem, w_ss, n_ss, e_ss, p_ss, core_ss, dp_ss, cross_ss) = refs[n_in + n_out:]

    t = lax.axis_index('tp')
    p = lax.axis_index('dp')
    per = SLABS // dpn
    dp_others = range(1, dpn)
    x, c = t // 2, lax.rem(t, 2)
    ox, oc = 1 - x, 1 - c
    peer = [t, t + 1 - 2 * c, t + 2 - 4 * x, t + 3 - 2 * c - 4 * x]

    def remote(src, dst, ssem, rsem, d):
        return pltpu.make_async_remote_copy(src_ref=src, dst_ref=dst, send_sem=ssem, recv_sem=rsem,
                                            device_id={'tp': peer[d]}, device_id_type=MESH)

    small_in = (send_ids, recv_ids, ew1_in, ew2_in, nw1_in, nw2_in, evec_in, nvec_in, eb1_in, nb1_in)
    loads = [pltpu.make_async_copy(src, dst, load_sem.at[q]) for q, (src, dst) in enumerate(
        zip(hbm_in, (node_raw, edge_raw, gnode_raw, gedge_raw) + small_in))]

    def node_copies(send, recv, kind):
        return (remote(send.at[1], recv.at[0], n_ss.at[kind, 0], n_rs.at[kind, 0], 1),
                remote(send.at[0], recv.at[1], n_ss.at[kind, 1], n_rs.at[kind, 1], 2),
                remote(recv.at[1], recv.at[2], n_ss.at[kind, 2], n_rs.at[kind, 2], 1))

    piece = w_send.shape[0] // dpn

    def packed(l, k, count=1):
        return pl.ds(HEAD + l * LROWS + k * cols, count * cols)

    def weight_rows(owner):
        return pl.ds(pl.multiple_of(owner * piece, 8), piece)

    w_pair = remote(w_send, w_recv.at[0], w_ss.at[0], w_rs.at[0], 1)
    w_cross = remote(w_send.at[weight_rows(p)], w_recv.at[1, weight_rows(p)], w_ss.at[1], w_rs.at[1], 2)
    w_relay = remote(w_recv.at[1], w_recv.at[2], w_ss.at[2], w_rs.at[2], 1)

    def weight_copy(i, owner):
        rows = w_recv.at[1, weight_rows(owner)]
        return dp_remote(rows, rows, 2, 0, i)

    last = nch - 1
    hold = nch - 3
    buffers = ((e_send, e_recv), (g_send, g_recv), (e_send, eo_recv), (g_send, de_recv))

    def outward(kind):
        return kind in (EDGE_OUT, GRAD_OUT)

    every = slice(None)
    ragged = pl.ds(D, D // GROUP)
    rest = [slice(g * cols // GROUP, (g + 1) * cols // GROUP) for g in range(GROUP)]

    def edge_part(kind, which, j, tail, send_sem, recv_sem, d):
        src, dst = buffers[kind]
        if tail:
            src, dst = t_send.at[kind % 2, which], t_recv.at[kind, which]
        else:
            src, dst = src.at[which, j], dst.at[which, j]
        recv_sems = o_rs.at[kind - EDGE_OUT, recv_sem] if outward(kind) else e_rs.at[kind, recv_sem]
        return remote(src, dst, e_ss.at[kind, send_sem], recv_sems, d)

    def by_half(half_id, j, action):
        narrow = jnp.logical_and(j == last, half_id == 1)

        @pl.when(jnp.logical_not(narrow))
        def _():
            action(False)

        @pl.when(narrow)
        def _():
            action(True)

    def pack_tail(kind, d):
        src, out = buffers[kind][0].at[slot(d), last], t_send.at[kind % 2, slot(d)]
        out[:cols, :] = src[:, :D]
        over = src[:, ragged]
        out[cols:, :] = beside([over[r] for r in rest])

    def unpack_tail(kind, d):
        src, out = t_recv.at[kind, slot(d)], buffers[kind][1].at[slot(d), last]
        out[:, :D] = src[:cols, :]
        over = src[cols:, :]
        out[:, ragged] = stacked([over[:, rows_of(g)] for g in range(GROUP)])

    def edge_start(kind, j, d):
        other = oc if d % 2 else c
        if outward(kind):
            send_sem, recv_sem = jnp.where(j == last, 1, 0), jnp.where(j == last, 2 + slot(d), jnp.where(j < hold, 0, 1))
        else:
            send_sem, recv_sem = jnp.where(j == last, d, 0), j

        def start(tail):
            if tail:
                pack_tail(kind, d)
            edge_part(kind, slot(d), j, tail, send_sem, recv_sem, d).start()

        by_half(c if outward(kind) else other, j, start)

    def edges_sent(kind):
        edge_part(kind, every, slice(0, last), False, 0, 0, 1).wait_send()
        if outward(kind):
            by_half(c, last, lambda tail: edge_part(kind, every, last, tail, 1, 0, 1).wait_send())
        else:
            for d in OTHERS:
                by_half(oc if d % 2 else c, last, lambda tail: edge_part(kind, slot(d), last, tail, d, 0, d).wait_send())

    def chunk_arrived(kind, j):
        def arrived(tail):
            edge_part(kind, every, j, tail, 0, j, 1).wait_recv()
            if tail:
                for d in OTHERS:
                    unpack_tail(kind, d)

        by_half(c, j, arrived)

    def group_arrived(kind, group):
        if group < 2:
            edge_part(kind, every, (slice(0, hold), slice(hold, last))[group], False, 0, group, 1).wait_recv()
        else:
            for d in OTHERS:
                def arrived(tail):
                    edge_part(kind, slot(d), last, tail, 0, 2 + slot(d), d).wait_recv()
                    if tail:
                        unpack_tail(kind, d)

                by_half(oc if d % 2 else c, last, arrived)

    def core_copy(l, b, stage):
        first, count = ((0, EARLY), (EARLY, SLABS - EARLY))[stage]
        return remote(grad.at[l, pl.ds(first, count), pl.ds((2 * b + 1) * cols, cols), :], core_recv.at[l, b, pl.ds(first, count)],
                      core_ss.at[l, stage], core_rs.at[l, stage], 1)

    def core_all(l, stage):
        part_of = core_recv.at[l, :, (slice(0, EARLY), slice(EARLY, SLABS))[stage]]
        return remote(part_of, part_of, core_ss.at[l, stage], core_rs.at[l, stage], 1)

    def seat(device):
        return lax.rem(device + dpn // 2, dpn)

    def in_stage(device, stage):
        early = (seat(device) + 1) * per <= EARLY
        return jnp.logical_not(early) if stage else early

    def dp_remote(src, dst, stage, l, i):
        return pltpu.make_async_remote_copy(src_ref=src, dst_ref=dst, send_sem=dp_ss.at[stage, l], recv_sem=dp_rs.at[stage, l],
                                            device_id={'dp': lax.rem(p + i, dpn)}, device_id_type=MESH)

    def spread_copy(l, i):
        return dp_remote(half.at[l, pl.ds(seat(lax.rem(p + i, dpn)) * per, per)], dp_recv.at[l, pl.ds((i - 1) * per, per)], 0, l, i)

    def dp_all(l, stage):
        most = (dpn - 1) * per
        part_of = (dp_recv.at[l], gathered.at[l, pl.ds(0, most)], w_recv.at[1, pl.ds(0, (dpn - 1) * piece)])[stage]
        return dp_remote(part_of, part_of, stage, l, 1)

    def cross_copy(l):
        return remote(cross_send.at[l], cross_recv.at[l], cross_ss.at[l], cross_rs.at[l], 2)

    def gather_copy(l, i, owner):
        return dp_remote(own_sum.at[l], gathered.at[l, pl.ds(seat(owner) * per, per)], 1, l, i)

    def part_copy(q):
        return remote(part.at[q], part_recv.at[q], p_ss.at[q], p_rs.at[q], 1)

    def load_nodes(raw, send, own):
        send[...] = jnp.zeros_like(send)
        send[0, :, :nodes] = raw[ox].astype(F32)
        send[1, :, :nodes] = raw[x].astype(F32)
        own[:cols, :] = send[1].astype(own.dtype)

    def load_edges(raw, send, own, kind):
        def put(j, lanes_j, val_of):
            for d in OTHERS:
                sample = x if d < 2 else ox
                send[slot(d), j] = val_of(sample, oc if d % 2 else c).astype(F32)
            own[:cols, lanes_j] = val_of(x, c)

        def chunk(j):
            put(j, at(j, EC), lambda s, h: raw[s, :, pl.ds(pl.multiple_of(h * eh + j * EC, D), EC)])
            for d in SEND_ORDER:
                edge_start(kind, j, d)

        loop(nch - 1, chunk)
        first = (nch - 1) * EC
        used = edges - eh - first
        last = pl.ds(first, EC)

        def tail(s, h):
            left = raw[s, :, pl.ds(first, EC)]
            right = beside([raw[s, :, pl.ds(eh + first, used)], jnp.zeros((cols, EC - used), BF)])
            return jnp.where(h == 0, left.astype(F32), right.astype(F32)).astype(BF)

        put(nch - 1, last, tail)
        for d in SEND_ORDER:
            edge_start(kind, nch - 1, d)

    def place_edges(raw, block, d, j):
        s = x if d < 2 else ox
        h = oc if d % 2 else c
        val = block.astype(BF)
        first = (nch - 1) * EC
        used = edges - eh - first

        @pl.when(jnp.logical_or(j < nch - 1, h == 0))
        def _():
            raw[s, :, pl.ds(pl.multiple_of(h * eh + j * EC, D), EC)] = val

        @pl.when(jnp.logical_and(j == nch - 1, h == 1))
        def _():
            raw[s, :, pl.ds(eh + first, used)] = val[:, :used]

    def scoped(e0, e1, ge, msg, v0, v1, v2, agg0, agg1, d_agg, scol, rcol, srow, rrow, iota, lanes, ew1, ew1t, ew2, ew2t, nw1, nw1t, nw2, nw2t, vecs):
        tables = (v0, v1, v2)
        aggs = (agg0, agg1)
        edges_in = (e0, e1)

        barrier = pltpu.get_barrier_semaphore()
        for d in OTHERS:
            pl.semaphore_signal(barrier, inc=1, device_id={'tp': peer[d]}, device_id_type=MESH)
        for copy in loads[:1] + loads[4:] + loads[1:4]:
            copy.start()
        loads[0].wait()
        with jax.named_scope('send_nodes'):
            load_nodes(node_raw, n_send, v0)
        ncop = node_copies(n_send, n_recv, 0)
        for copy in loads[4:]:
            copy.wait()
        q = cols
        w_send[:HEAD, :] = jnp.zeros((HEAD, D), F32)
        for k in THREE:
            w_send[k * layers:(k + 1) * layers, :cols] = evec_in[k]
            w_send[(3 + k) * layers:(4 + k) * layers, :cols] = nvec_in[k]
        for l in range(layers):
            w_send[packed(l, 0, 3), :] = ew1_in[pl.ds(l * 3 * q, 3 * q), :].astype(F32)
            w_send[packed(l, 3), :] = ew2_in[pl.ds(l * q, q), :].astype(F32)
            w_send[packed(l, 4, 2), :] = nw1_in[pl.ds(l * 2 * q, 2 * q), :].astype(F32)
            w_send[packed(l, 6), :] = nw2_in[pl.ds(l * q, q), :].astype(F32)
        with jax.named_scope('barrier'):
            @pl.when(t != LEADER)
            def _():
                pl.semaphore_wait(barrier, len(OTHERS))
                pl.semaphore_signal(ready, inc=1, device_id={'tp': LEADER}, device_id_type=MESH)

            @pl.when(t == LEADER)
            def _():
                pl.semaphore_wait(ready, len(OTHERS))
                for i in dp_others:
                    pl.semaphore_signal(barrier, inc=1, device_id={'dp': lax.rem(p + i, dpn)}, device_id_type=MESH)

        w_cross.start()
        w_pair.start()
        ncop[1].start()
        ncop[0].start()
        loads[1].wait()
        with jax.named_scope('send_edges'):
            load_edges(edge_raw, e_send, e0, EDGE_IN)
        loads[2].wait()
        load_nodes(gnode_raw, gn_send, d_part)
        gcop = node_copies(gn_send, gn_recv, 1)
        gcop[1].start()
        gcop[0].start()
        loads[3].wait()
        with jax.named_scope('send_grads'):
            load_edges(gedge_raw, g_send, ge, GRAD_IN)

        with jax.named_scope('dp_barrier'):
            @pl.when(t == LEADER)
            def _():
                pl.semaphore_wait(barrier, len(OTHERS) + dpn - 1)
                for d in OTHERS:
                    pl.semaphore_signal(ready, inc=1, device_id={'tp': peer[d]}, device_id_type=MESH)

            @pl.when(t != LEADER)
            def _():
                pl.semaphore_wait(ready, 1)

        w_cross.wait_recv()
        for i in dp_others:
            weight_copy(i, p).start()

        @pl.when(c == 1)
        def _():
            for recv in (e_recv, g_recv):
                recv[:, last, :, D:] = jnp.zeros((len(OTHERS), cols, EC - D), F32)

        iota[...] = lax.broadcasted_iota(jnp.int32, (T, D), 0).astype(I16)
        lanes[...] = lax.broadcasted_iota(jnp.int32, (16, D), 1).astype(I16)

        ids_raw[...] = jnp.full(ids_raw.shape, -1, jnp.int32)
        for which, src in enumerate((send_ids, recv_ids)):
            ids_raw[which:which + 1, :edges] = src[...].reshape(1, edges)

        def ids(b):
            for which, (row_ref, col_ref) in enumerate(((srow, scol), (rrow, rcol))):
                wide = jnp.broadcast_to(ids_raw[which:which + 1, pl.ds(pl.multiple_of(c * eh + b * D, D), D)], (D, D))
                row_ref[at(b, 16), :] = wide[:16].astype(I16)
                col_ref[at(b, D), :] = flip(wide.astype(F32)).astype(jnp.int32).astype(I16)

        with jax.named_scope('ids'):
            loop(eh // D, ids)

        def keys(ref, step):
            return [ref[pl.ds(pl.multiple_of(step * (KS // D) * 16 + 16 * h, 16), 1), :] for h in range(KS // D)]

        bias_cols[...] = flip(stacked([eb1_in[...], nb1_in[...], jnp.zeros((D - 2 * layers, D), F32)]))

        def join_weights(l):
            for d in range(GROUP):
                src = w_recv.at[slot(d)] if d else w_send
                r = rows_of(d)
                for k in THREE:
                    ew1[l, pl.ds(k * D + d * q, q), :] = src[packed(l, k), :].astype(BF)
                ew2t[l, r, :] = src[packed(l, 3), :].astype(BF)
                for k in BOTH:
                    nw1[l, pl.ds(k * D + d * q, q), :] = src[packed(l, 4 + k), :].astype(BF)
                nw2t[l, r, :] = src[packed(l, 6), :].astype(BF)

            def flip_bf(mat):
                return flip(mat.astype(F32)).astype(BF)

            for k in THREE:
                ew1t[l, :, mat(k)] = flip_bf(ew1[l, mat(k), :])
            for k in BOTH:
                nw1t[l, :, mat(k)] = flip_bf(nw1[l, mat(k), :])
            ew2[l] = flip_bf(ew2t[l])
            nw2[l] = flip_bf(nw2t[l])

        def wait_recvs(copies):
            copies[1].wait_recv()
            copies[2].start()
            copies[0].wait_recv()
            copies[2].wait_recv()

        with jax.named_scope('node_wait'):
            wait_recvs(ncop)
        for d in OTHERS:
            v0[rows_of(d), :] = n_recv[slot(d)].astype(BF)
        with jax.named_scope('weight_wait'):
            dp_all(0, 2).wait_recv()
            w_relay.start()
            w_pair.wait_recv()
            w_relay.wait_recv()
        rows_all = beside([w_send[:HEAD, :cols]] + [w_recv[d, :HEAD, :cols] for d in range(3)])
        vecs[...] = flip(stacked([rows_all, jnp.zeros((D - HEAD, D), F32)]))
        join_weights(0)

        def vec(l, node):
            first = 6 * node + l
            return [vecs[:, first + 2 * k:first + 2 * k + 1] for k in THREE]

        def bias(l, node):
            return bias_cols[:, node * layers + l:node * layers + l + 1]

        def hidden_of_nodes(l):
            table, b1 = tables[l], bias(l, 0)

            def body(step):
                xs = gather(table, keys(srow, step), iota).astype(BF)
                xr = gather(table, keys(rrow, step), iota).astype(BF)
                hidden[l, :, at(step, KS)] = dot(ew1t[l, :, mat(1, 2)], stacked([xs, xr])) + b1

            loop(eh // KS, body)

        def edge_forward(l):
            e_in = edges_in[l]

            def body(j):
                for sub in range(EC // T):
                    a = at(j * (EC // T) + sub, T)
                    if l == 0:
                        if sub == 0:
                            chunk_arrived(EDGE_IN, j)
                        for d in OTHERS:
                            e_in[rows_of(d), a] = e_recv[slot(d), j, :, sub * T:(sub + 1) * T].astype(BF)
                    e_val = e_in[:, a]
                    hid = hidden[l, :, a] + dot(ew1t[l, :, mat(0)], e_val)
                    hidden[l, :, a] = hid
                    message, nrm, std = mlp_tail(hid, ew2t[l], vec(l, 0))
                    normed[l, :, a] = nrm
                    inv[l:l + 1, a] = std
                    msg[:, a] = message
                    e_new = (e_val.astype(F32) + message.astype(F32)).astype(BF)
                    if l < top:
                        edges_in[l + 1][:, a] = e_new
                    else:
                        for d in OTHERS:
                            e_send[slot(d), j, :, sub * T:(sub + 1) * T] = e_new[rows_of(d)].astype(F32)
                        if sub == 0:
                            own_parts = []
                        own_parts.append(e_new[:q])
                if l == top:
                    for d in SEND_ORDER:
                        edge_start(EDGE_OUT, j, d)
                    place_edges(edge_raw, beside(own_parts), 0, j)

            loop(nch, body)

        def segment_sum(acc, ids_ref):
            acc[...] = jnp.zeros(acc.shape, F32)

            def body(step):
                scatter(acc, msg[:, at(step, KS)], ids_ref[at(step, KS), :], lanes)

            loop(eh // KS, body)

        def node_forward(l):
            table, agg, out = tables[l], aggs[l], tables[l + 1]

            def body(step):
                a = pl.ds(pl.multiple_of(step * TN, D), TN)
                v_in = table[:, a]
                agg_bf = (part[l, :, a] + swap_halves(part_recv[l, :, a])).astype(BF)
                agg[:, a] = agg_bf
                hid = dot(nw1t[l], stacked([v_in, agg_bf])) + bias(l, 1)
                nhid[l, :, a] = hid
                message, nrm, std = mlp_tail(hid, nw2t[l], vec(l, 1))
                nnrm[l, :, a] = nrm
                ninv[l:l + 1, a] = std
                out[:, a] = (v_in.astype(F32) + message.astype(F32)).astype(BF)

            loop(npad // TN, body)

        for l in range(layers):
            with jax.named_scope(f'gather_{l}'):
                hidden_of_nodes(l)
            if l == top:
                edges_sent(EDGE_IN)
            with jax.named_scope(f'edge_forward_{l}'):
                edge_forward(l)
            with jax.named_scope(f'sum_{l}'):
                segment_sum(part.at[l], rcol)
            part_copy(l).start()
            if l == 0:
                join_weights(1)
                gcop[1].wait_recv()
                gcop[2].start()
            with jax.named_scope(f'part_wait_{l}'):
                part_copy(l).wait_recv()
            with jax.named_scope(f'node_forward_{l}'):
                node_forward(l)
        no_send[...] = tables[layers][rows_of(2), :].astype(F32)
        no_copy = remote(no_send, no_recv, n_ss.at[2, 0], n_rs.at[2, 0], 2)
        no_copy.start()
        node_raw[x] = tables[layers][:q, :nodes]

        grad[...] = jnp.zeros_like(grad)
        sums[...] = jnp.zeros_like(sums)
        with jax.named_scope('grad_node_wait'):
            gcop[0].wait_recv()
            gcop[2].wait_recv()
        for d in OTHERS:
            d_part[rows_of(d), :] = gn_recv[slot(d)]

        def node_backward(l):
            table, agg = tables[l], aggs[l]

            def body(step):
                a = pl.ds(pl.multiple_of(step * TN, D), TN)
                d_in = d_part[:, a]
                if l < top:
                    d_in = d_in + part[layers + l + 1, :, a] + swap_halves(part_recv[layers + l + 1, :, a])
                    d_in = d_in.astype(BF).astype(F32)
                d_hid, d_w2, parts = mlp_back(d_in, nhid[l, :, a], nnrm[l, :, a], ninv[l:l + 1, a], nw2[l], vec(l, 1))
                add_sums(sums.at[l, 1], [parts])
                grad[l, 4] += d_w2
                grad[l, 2] += dot_nt(table[:, a], d_hid)
                grad[l, 3] += dot_nt(agg[:, a], d_hid)
                d_part[:, a] = d_in + dot(nw1[l, mat(0), :], d_hid)
                d_agg[:, a] = dot(nw1[l, mat(1), :], d_hid).astype(BF)

            loop(npad // TN, body)

        def gather_back():
            def body(step):
                msg[:, at(step, KS)] = gather(d_agg, keys(rrow, step), iota).astype(BF)

            loop(eh // KS, body)

        def edge_backward(l):
            e_in = edges_in[l]

            def body(j):
                all_parts, d_w2s, d_w1s, own_parts = [], [], [], []
                for sub in range(EC // T):
                    a = at(j * (EC // T) + sub, T)
                    if l == top:
                        if sub == 0:
                            chunk_arrived(GRAD_IN, j)
                        for d in OTHERS:
                            ge[rows_of(d), a] = g_recv[slot(d), j, :, sub * T:(sub + 1) * T].astype(BF)
                    d_res = ge[:, a].astype(F32)
                    d_msg = d_res + msg[:, a].astype(F32)
                    d_hid, d_w2, parts = mlp_back(d_msg, hidden[l, :, a], normed[l, :, a], inv[l:l + 1, a], ew2[l], vec(l, 0))
                    all_parts.append(parts)
                    d_w2s.append(d_w2)
                    d_w1s.append(dot_nt(e_in[:, a], d_hid))
                    msg[:, a] = d_hid
                    d_new = (d_res + dot(ew1[l, mat(0), :], d_hid)).astype(BF)
                    if l > 0:
                        ge[:, a] = d_new
                    else:
                        for d in OTHERS:
                            g_send[slot(d), j, :, sub * T:(sub + 1) * T] = d_new[rows_of(d)].astype(F32)
                        own_parts.append(d_new[:q])
                add_sums(sums.at[l, 0], all_parts)
                grad[l, 1] += sum(d_w2s[1:], d_w2s[0])
                grad[l, 0] += sum(d_w1s[1:], d_w1s[0])
                if l == 0:
                    @pl.when(j < hold)
                    def _():
                        for d in SEND_ORDER:
                            edge_start(GRAD_OUT, j, d)
                    place_edges(gedge_raw, beside(own_parts), 0, j)

            loop(nch, body)

        def vector_slab(l):
            def total(node, k):
                return column_sum(flip(sums[l, node, mat(k), :]))

            lat = stacked([total(node, k) for node in BOTH for k in THREE])
            biases = stacked([total(node, 3) for node in BOTH])
            n_lat = lat.shape[0]
            for d in range(GROUP):
                grad[l, VEC_SLAB, d * cols:d * cols + n_lat, :cols] = lat[:, rows_of(d)]
                grad[l, VEC_SLAB, d * cols + n_lat:d * cols + n_lat + 2, :] = biases

        def reduce_start(l, stage):
            for b in BOTH:
                core_copy(l, b, stage).start()

        def chip_sum(l, stage):
            row = lax.broadcasted_iota(jnp.int32, (cols, D), 0)
            edge_row = jnp.logical_or(row < 3, row == 6)
            core_all(l, stage).wait_recv()
            for b in BOTH:
                for k in range(SLABS)[STAGES[stage]]:
                    own = grad[l, k, rows_of(2 * b), :]
                    if k in EDGE_SLABS:
                        own = own + core_recv[l, b, k]
                    elif k == VEC_SLAB:
                        own = own + jnp.where(edge_row, core_recv[l, b, k], 0.0)
                    half[l, k, b] = own
            for i in dp_others:
                @pl.when(in_stage(lax.rem(p + i, dpn), stage))
                def _():
                    spread_copy(l, i).start()

        def dp_sum(l, stage):
            @pl.when(in_stage(p, stage))
            def _():
                total = half[l, pl.ds(seat(p) * per, per)]
                dp_all(l, 0).wait_recv()
                for i in dp_others:
                    total = total + dp_recv[l, pl.ds((i - 1) * per, per)]
                own_sum[l] = total[:, 0]
                cross_send[l] = total[:, 1]
                cross_copy(l).start()

        def cross_sum(l):
            cross_copy(l).wait_recv()
            total = own_sum[l] + cross_recv[l]
            own_sum[l] = total
            gathered[l, pl.ds(seat(p) * per, per)] = total
            for i in dp_others:
                gather_copy(l, i, p).start()

        def project(l):
            table = tables[l]

            def body(step):
                a = pl.ds(pl.multiple_of(step * TN, D), TN)
                s_bf, r_bf, v_in = s_sum[:, a].astype(BF), r_sum[:, a].astype(BF), table[:, a]
                part[layers + l, :, a] = dot(ew1[l, mat(1), :], s_bf) + dot(ew1[l, mat(2), :], r_bf)
                grad[l, 6] += dot_nt(v_in, s_bf)
                grad[l, 7] += dot_nt(v_in, r_bf)

            loop(npad // TN, body)

        for l in reversed(range(layers)):
            first_layer = l == 0
            with jax.named_scope(f'node_backward_{l}'):
                node_backward(l)
            if first_layer:
                with jax.named_scope('chip_sum_1'):
                    chip_sum(1, 0)
                    chip_sum(1, 1)
            with jax.named_scope(f'gather_back_{l}'):
                gather_back()
            if first_layer:
                edges_sent(GRAD_IN)
            with jax.named_scope(f'edge_backward_{l}'):
                edge_backward(l)
            vector_slab(l)
            reduce_start(l, 0)
            if first_layer:
                with jax.named_scope('dp_sum_1'):
                    dp_sum(1, 0)
                    dp_sum(1, 1)
            with jax.named_scope(f'sum_send_{l}'):
                segment_sum(s_sum, scol)
            if first_layer:
                with jax.named_scope('chip_sum_0'):
                    chip_sum(0, 0)
            with jax.named_scope(f'sum_recv_{l}'):
                segment_sum(r_sum, rcol)
            with jax.named_scope(f'project_{l}'):
                project(l)
            reduce_start(l, 1)
            part_copy(layers + l).start()
            if first_layer:
                with jax.named_scope('chip_sum_late'):
                    chip_sum(0, 1)
                with jax.named_scope('dp_sum_0'):
                    dp_sum(0, 0)
            with jax.named_scope(f'back_wait_{l}'):
                part_copy(layers + l).wait_recv()

        def final(step):
            a = pl.ds(pl.multiple_of(step * TN, D), TN)
            d_in = (d_part[:, a] + part[layers, :, a] + swap_halves(part_recv[layers, :, a])).astype(BF)
            v2[:, a] = d_in

        loop(npad // TN, final)
        gnode_raw[x] = v2[:q, :nodes]
        with jax.named_scope('dp_sum_late'):
            dp_sum(0, 1)

        dn_send[...] = v2[rows_of(2), :].astype(F32)
        dn_copy = remote(dn_send, dn_recv, n_ss.at[2, 1], n_rs.at[2, 1], 2)
        dn_copy.start()

        def send_rest(j):
            for d in SEND_ORDER:
                edge_start(GRAD_OUT, j, d)

        loop(nch, send_rest, hold)

        with jax.named_scope('node_out_wait'):
            no_copy.wait_recv()
        node_raw[ox] = no_recv[:, :nodes].astype(BF)

        def place_e(j):
            for d in OTHERS:
                place_edges(edge_raw, eo_recv[slot(d), j], d, j)

        with jax.named_scope('place_edge_out'):
            for group in THREE:
                group_arrived(EDGE_OUT, group)
            loop(nch, place_e)

        def place_g(j):
            for d in OTHERS:
                place_edges(gedge_raw, de_recv[slot(d), j], d, j)

        with jax.named_scope('place_first'):
            group_arrived(GRAD_OUT, 0)
            loop(hold, place_g)
        for l in range(layers):
            with jax.named_scope(f'cross_sum_{l}'):
                cross_sum(l)
        with jax.named_scope('d_node_wait'):
            dn_copy.wait_recv()
        gnode_raw[ox] = dn_recv[:, :nodes].astype(BF)
        with jax.named_scope('place_rest'):
            group_arrived(GRAD_OUT, 1)
            loop(last, place_g, hold)
        for l in range(layers):
            dp_all(l, 1).wait_recv()
            ew1_buf[l, 0] = gathered[l, 0]
            ew1_buf[l, 1:] = gathered[l, EARLY:]
            ew2_buf[l] = gathered[l, 1]
            nw1_buf[l] = gathered[l, 2:4]
            nw2_buf[l] = gathered[l, 4]
            small = gathered[l, VEC_SLAB]
            for k in THREE:
                evec_buf[k, l:l + 1, :] = small[k:k + 1, :cols]
                nvec_buf[k, l:l + 1, :] = small[3 + k:4 + k, :cols]
            eb1_buf[l:l + 1, :] = small[6:7]
            nb1_buf[l:l + 1, :] = small[7:8]
        for l in range(layers):
            for stage in BOTH:
                core_all(l, stage).wait_send()
            cross_copy(l).wait_send()
            dp_all(l, 0).wait_send()
            dp_all(l, 1).wait_send()
        for copy in ncop + gcop + (w_pair, w_cross, w_relay):
            copy.wait_send()
        dp_all(0, 2).wait_send()
        no_copy.wait_send()
        dn_copy.wait_send()
        for k in range(2 * layers):
            part_copy(k).wait_send()
        edges_sent(EDGE_OUT)
        with jax.named_scope('place_last'):
            group_arrived(GRAD_OUT, 2)
            loop(nch, place_g, last)
        edges_sent(GRAD_OUT)

    bf = lambda *s: pltpu.VMEM(s, BF)
    pl.run_scoped(
        scoped, bf(D, eh), bf(D, eh), bf(D, eh), bf(D, eh), bf(D, npad), bf(D, npad), bf(D, npad), bf(D, npad), bf(D, npad), bf(D, npad),
        pltpu.VMEM((eh, D), I16), pltpu.VMEM((eh, D), I16), pltpu.VMEM((eh // D * 16, D), I16), pltpu.VMEM((eh // D * 16, D), I16),
        pltpu.VMEM((T, D), I16), pltpu.VMEM((16, D), I16),
        bf(layers, 3 * D, D), bf(layers, D, 3 * D), bf(layers, D, D), bf(layers, D, D),
        bf(layers, 2 * D, D), bf(layers, D, 2 * D), bf(layers, D, D), bf(layers, D, D), pltpu.VMEM((D, D), F32))


def finish_moves(src, dst):
    if len(src.shape) != 3 or src.dtype != BF:
        return [(src, dst)]
    return [(src.at[s, pl.ds(r, 8)], dst.at[s, pl.ds(r, 8)]) for s in range(src.shape[0]) for r in range(0, src.shape[1], 8)]


def finish_kernel(*refs):
    count = len(refs) // 2
    moves = sum((finish_moves(refs[k], refs[count + k]) for k in range(count)), [])
    puts = [pltpu.make_async_copy(src, dst, refs[-1]) for src, dst in moves]
    for put in puts:
        put.start()
    for put in puts:
        put.wait()


def keep_in_vmem(val):
    return pltpu.with_memory_space_constraint(val, pltpu.VMEM)


def finish(arrays):
    return pl.pallas_call(
        finish_kernel,
        name='finish',
        out_shape=[jax.ShapeDtypeStruct(a.shape, a.dtype) for a in arrays],
        in_specs=[VM] * len(arrays),
        out_specs=[HB] * len(arrays),
        scratch_shapes=[pltpu.SemaphoreType.DMA],
        compiler_params=pltpu.CompilerParams(vmem_limit_bytes=1 << 20),
    )(*[keep_in_vmem(a) for a in arrays])


def solution(mesh):
    lat_spec = P('dp', None, 'tp')
    first_spec = P(None, None, 'tp', None)
    col_spec = P(None, None, 'tp')
    param_specs = (first_spec, P(), col_spec, col_spec, first_spec, P(), col_spec, col_spec)
    in_specs = (lat_spec, lat_spec, P(), P(), lat_spec, lat_spec) + param_specs
    out_specs = (lat_spec, lat_spec, lat_spec, lat_spec) + param_specs
    shape = jax.ShapeDtypeStruct

    def local_step(node_lat, edge_lat, senders, receivers, grad_node, grad_edge, edge_w1, edge_b1, edge_w2, edge_vec, node_w1, node_b1, node_w2, node_vec):
        layers = edge_w1.shape[0]
        cols = node_lat.shape[2]
        nodes, edges = node_lat.shape[1], edge_lat.shape[1]
        npad = -(-nodes // TN) * TN
        eh = -(-edges // (2 * EC)) * EC
        nch = eh // EC
        dpn = mesh.shape['dp']
        per = SLABS // dpn
        dims = (layers, cols, nodes, edges, npad, eh, dpn)
        flat = lambda arr: jnp.swapaxes(arr, 1, 2)
        lead = lambda arr: jnp.transpose(arr, (1, 0, 2))
        args = (flat(node_lat), flat(edge_lat), flat(grad_node), flat(grad_edge), senders, receivers,
                edge_w1.reshape(-1, D), flat(edge_w2).reshape(-1, D), node_w1.reshape(-1, D), flat(node_w2).reshape(-1, D),
                lead(edge_vec), lead(node_vec), edge_b1, node_b1)
        vm, sem = pltpu.VMEM, pltpu.SemaphoreType.DMA
        wrows = -(-(HEAD + layers * LROWS) // (8 * dpn)) * 8 * dpn
        lat_n, lat_e = (2, cols, nodes), (2, cols, edges)
        outs = [RESULT(lat_n, BF), RESULT(lat_e, BF), RESULT(lat_n, BF), RESULT(lat_e, BF),
                RESULT((layers, 3, cols, D), F32), RESULT((layers, D), F32), RESULT((layers, cols, D), F32), RESULT((3, layers, cols), F32),
                RESULT((layers, 2, cols, D), F32), RESULT((layers, D), F32), RESULT((layers, cols, D), F32), RESULT((3, layers, cols), F32)]
        scratch = [
            *[vm(a.shape, a.dtype) for a in args[4:]], vm((wrows, D), F32), vm((3, wrows, D), F32),
            vm((2, cols, npad), F32), vm((3, cols, npad), F32), vm((2, cols, npad), F32), vm((3, cols, npad), F32),
            vm((cols, npad), F32), vm((cols, npad), F32), vm((cols, npad), F32), vm((cols, npad), F32),
            vm((2, 3, cols + cols // GROUP, D), F32), vm((4, 3, cols + cols // GROUP, D), F32), *[vm((3, nch, cols, EC), F32)] * 6,
            vm((2 * layers, D, npad), F32), vm((2 * layers, D, npad), F32),
            vm((layers, D, eh), F32), vm((layers, D, eh), F32), vm((layers, eh), F32),
            vm((layers, D, npad), F32), vm((layers, D, npad), F32), vm((layers, npad), F32),
            vm((D, npad), F32), vm((D, npad), F32), vm((D, npad), F32), vm((2, 2 * eh), jnp.int32), vm((D, D), F32), vm((layers, 2, 4 * D, D), F32),
            vm((layers, SLABS, D, D), F32), vm((layers, 2, SLABS, cols, D), F32), vm((layers, SLABS, 2, cols, D), F32),
            vm((layers, (dpn - 1) * per, 2, cols, D), F32), vm((layers, per, cols, D), F32), vm((layers, per, cols, D), F32),
            vm((layers, per, cols, D), F32), vm((layers, SLABS, cols, D), F32),]
        own_sems = [
            sem((layers, 2)), sem((3, layers)), sem((layers,)), sem((3,)), sem((3, 3)), sem((2, nch)), sem((2, 5)), sem((2 * layers,)),
            pltpu.SemaphoreType.REGULAR,
            sem((len(args),)), sem((3,)), sem((3, 3)), sem((4, 4)), sem((2 * layers,)), sem((layers, 2)), sem((3, layers)), sem((layers,))]
        res = pl.pallas_call(
            lambda *refs: pl.run_scoped(lambda *own: step_kernel(dims, *refs, *own), *own_sems),
            name='graph_step',
            out_shape=outs,
            in_specs=[HB] * len(args),
            out_specs=[VM] * len(outs),
            scratch_shapes=scratch,
            compiler_params=pltpu.CompilerParams(collective_id=0, has_side_effects=True, vmem_limit_bytes=VMEM_LIMIT),
        )(*args)

        res = finish(res)
        return (flat(res[0]), flat(res[1]), flat(res[2]), flat(res[3]),
                res[4], res[5], flat(res[6]), lead(res[7]), res[8], res[9], flat(res[10]), lead(res[11]))

    return jax.shard_map(local_step, mesh=mesh, in_specs=in_specs, out_specs=out_specs, check_vma=False)
```

```python
import jax
import jax.numpy as jnp
from jax import lax
from jax.experimental import pallas as pl
from jax.experimental.pallas import tpu as pltpu
from jax.sharding import PartitionSpec as P

LN_EPS = 1e-5
D = 128
T = 256
TN = 384
EC = 512
KS = 1408
BF = jnp.bfloat16
F32 = jnp.float32
I16 = jnp.int16
MESH = pl.DeviceIdType.MESH
VM = pl.BlockSpec(memory_space=pltpu.VMEM)
HB = pl.BlockSpec(memory_space=pl.ANY)
RESULT = pltpu.VMEM
GROUP = 4
BOTH = (0, 1)
THREE = (0, 1, 2)
OTHERS = (1, 2, 3)
EDGE_IN, GRAD_IN, EDGE_OUT, GRAD_OUT = range(4)
SEND_ORDER = (2, 3, 1)
LROWS = 7 * (D // 4)
HEAD = 16
LEADER = GROUP - 1
VMEM_LIMIT = 63_000_000
SLABS = 8
EARLY = 6
PAIR = 2
VEC_SLAB = 5
EDGE_SLABS = (0, 1, 6, 7)
STAGES = (slice(0, EARLY), slice(EARLY, SLABS))


def dot(a, b):
    return jnp.dot(a, b, preferred_element_type=F32)


def dot_nt(a, b):
    return lax.dot_general(a, b, (((1,), (1,)), ((), ())), preferred_element_type=F32)


def mat(k, n=1):
    return slice(k * D, (k + n) * D)


def rows_of(d):
    q = D // 4
    return slice(d * q, (d + 1) * q)


def at(step, width):
    return pl.ds(pl.multiple_of(step * width, width), width)


def loop(stop, body, start=0):
    def step(j, carry):
        body(j)
        return carry

    lax.fori_loop(start, stop, step, 0)


def column_sum(val):
    return jnp.sum(val, axis=0, keepdims=True)


def flip(val):
    return jnp.swapaxes(val, 0, 1)


def stacked(parts):
    return jnp.concatenate(parts, axis=0)


def beside(parts):
    return jnp.concatenate(parts, axis=1)


def slot(d):
    return d - 1


def sigmoid(hidden):
    return 1.0 / (1.0 + jnp.exp(-hidden))


def fold(val):
    total = val[:, mat(0)]
    for start in range(D, val.shape[1], D):
        total = total + val[:, start:start + D]
    return total


def swap_halves(val):
    return stacked([val[rows_of(d)] for d in (1, 0, 3, 2)])


def gather(table, keys, iota):
    acc = None
    nodes = table.shape[1]
    one, zero = jnp.ones((), BF), jnp.zeros((), BF)
    for base in range(0, nodes, T):
        width = min(T, nodes - base)
        ids = iota[0:width, :]
        hot = beside([jnp.where(ids == (key - jnp.asarray(base, I16)), one, zero) for key in keys])
        part = dot(table[:, base:base + width], hot)
        acc = part if acc is None else acc + part
    return acc


def scatter(acc_ref, val, cols, lanes):
    nodes = acc_ref.shape[1]
    one, zero = jnp.ones((), BF), jnp.zeros((), BF)
    row = lanes[0:1, :]
    for base in range(0, nodes, T):
        width = min(T, nodes - base)
        hot = beside([jnp.where((row + jnp.asarray(base + s, I16)) == cols, one, zero) for s in range(0, width, D)])
        acc_ref[:, base:base + width] += dot(val, hot)


def mlp_tail(hidden, w2t, vec):
    act = (hidden * sigmoid(hidden)).astype(BF)
    out = dot(w2t, act) + vec[0]
    mean = column_sum(out) / D
    centered = out - mean
    var = column_sum(centered * centered) / D
    inv = lax.rsqrt(var + LN_EPS)
    normed = centered * inv
    message = (normed * vec[1] + vec[2]).astype(BF)
    return message, normed, inv


def mlp_back(d_msg, hidden, normed, inv, w2, vec):
    d_normed = d_msg * vec[1]
    mean0 = column_sum(d_normed) / D
    mean1 = column_sum(d_normed * normed) / D
    d_out = inv * (d_normed - mean0 - normed * mean1)
    d_out_bf = d_out.astype(BF)
    sig = sigmoid(hidden)
    act = (hidden * sig).astype(BF)
    d_w2 = dot_nt(d_out_bf, act)
    d_hidden = dot(w2, d_out_bf) * (sig * (1.0 + hidden * (1.0 - sig)))
    sums = (fold(d_out), fold(d_msg * normed), fold(d_msg), fold(d_hidden))
    return d_hidden.astype(BF), d_w2, sums


def add_sums(ref, parts):
    for q in range(4):
        total = parts[0][q]
        for other in parts[1:]:
            total = total + other[q]
        ref[mat(q), :] += total


def step_kernel(dims, *refs):
    layers, cols, nodes, edges, npad, eh, dpn = dims
    nch = eh // EC
    top = layers - 1
    n_in = 14
    hbm_in = refs[:n_in]
    n_out = 12
    (node_raw, edge_raw, gnode_raw, gedge_raw, ew1_buf, eb1_buf, ew2_buf, evec_buf, nw1_buf, nb1_buf, nw2_buf, nvec_buf) = refs[n_in:n_in + n_out]
    (send_ids, recv_ids, ew1_in, ew2_in, nw1_in, nw2_in, evec_in, nvec_in, eb1_in, nb1_in, w_send, w_recv, n_send, n_recv, gn_send, gn_recv, no_send, no_recv, dn_send, dn_recv,
     t_send, t_recv, e_send, g_send, e_recv, g_recv, eo_recv, de_recv, part, part_recv, hidden, normed, inv, nhid, nnrm, ninv, d_part, s_sum, r_sum,
     ids_raw, bias_cols, sums, grad, core_recv, half, dp_recv, cross_send, cross_recv, own_sum, gathered,
     core_rs, dp_rs, cross_rs, w_rs, n_rs, e_rs, o_rs, p_rs, ready, load_sem, w_ss, n_ss, e_ss, p_ss, core_ss, dp_ss, cross_ss) = refs[n_in + n_out:]

    t = lax.axis_index('tp')
    p = lax.axis_index('dp')
    per = SLABS // dpn
    dp_others = range(1, dpn)
    x, c = t // 2, lax.rem(t, 2)
    ox, oc = 1 - x, 1 - c
    peer = [t, t + 1 - 2 * c, t + 2 - 4 * x, t + 3 - 2 * c - 4 * x]

    def remote(src, dst, ssem, rsem, d):
        return pltpu.make_async_remote_copy(src_ref=src, dst_ref=dst, send_sem=ssem, recv_sem=rsem,
                                            device_id={'tp': peer[d]}, device_id_type=MESH)

    small_in = (send_ids, recv_ids, ew1_in, ew2_in, nw1_in, nw2_in, evec_in, nvec_in, eb1_in, nb1_in)
    loads = [pltpu.make_async_copy(src, dst, load_sem.at[q]) for q, (src, dst) in enumerate(
        zip(hbm_in, (node_raw, edge_raw, gnode_raw, gedge_raw) + small_in))]

    def node_copies(send, recv, kind):
        return (remote(send.at[1], recv.at[0], n_ss.at[kind, 0], n_rs.at[kind, 0], 1),
                remote(send.at[0], recv.at[1], n_ss.at[kind, 1], n_rs.at[kind, 1], 2),
                remote(recv.at[1], recv.at[2], n_ss.at[kind, 2], n_rs.at[kind, 2], 1))

    piece = w_send.shape[0] // dpn

    def packed(l, k, count=1):
        return pl.ds(HEAD + l * LROWS + k * cols, count * cols)

    def weight_rows(owner):
        return pl.ds(pl.multiple_of(owner * piece, 8), piece)

    w_pair = remote(w_send, w_recv.at[0], w_ss.at[0], w_rs.at[0], 1)
    w_cross = remote(w_send.at[weight_rows(p)], w_recv.at[1, weight_rows(p)], w_ss.at[1], w_rs.at[1], 2)
    w_relay = remote(w_recv.at[1], w_recv.at[2], w_ss.at[2], w_rs.at[2], 1)

    def weight_copy(i, owner):
        rows = w_recv.at[1, weight_rows(owner)]
        return dp_remote(rows, rows, 2, 0, i)

    last = nch - 1
    hold = nch - 3
    buffers = ((e_send, e_recv), (g_send, g_recv), (e_send, eo_recv), (g_send, de_recv))

    def outward(kind):
        return kind in (EDGE_OUT, GRAD_OUT)

    every = slice(None)
    ragged = pl.ds(D, D // GROUP)
    rest = [slice(g * cols // GROUP, (g + 1) * cols // GROUP) for g in range(GROUP)]

    def edge_part(kind, which, j, tail, send_sem, recv_sem, d):
        src, dst = buffers[kind]
        if tail:
            src, dst = t_send.at[kind % 2, which], t_recv.at[kind, which]
        else:
            src, dst = src.at[which, j], dst.at[which, j]
        recv_sems = o_rs.at[kind - EDGE_OUT, recv_sem] if outward(kind) else e_rs.at[kind, recv_sem]
        return remote(src, dst, e_ss.at[kind, send_sem], recv_sems, d)

    def by_half(half_id, j, action):
        narrow = jnp.logical_and(j == last, half_id == 1)

        @pl.when(jnp.logical_not(narrow))
        def _():
            action(False)

        @pl.when(narrow)
        def _():
            action(True)

    def pack_tail(kind, d):
        src, out = buffers[kind][0].at[slot(d), last], t_send.at[kind % 2, slot(d)]
        out[:cols, :] = src[:, :D]
        over = src[:, ragged]
        out[cols:, :] = beside([over[r] for r in rest])

    def unpack_tail(kind, d):
        src, out = t_recv.at[kind, slot(d)], buffers[kind][1].at[slot(d), last]
        out[:, :D] = src[:cols, :]
        over = src[cols:, :]
        out[:, ragged] = stacked([over[:, rows_of(g)] for g in range(GROUP)])

    def edge_start(kind, j, d):
        other = oc if d % 2 else c
        if outward(kind):
            send_sem, recv_sem = jnp.where(j == last, 1, 0), jnp.where(j == last, 2 + slot(d), jnp.where(j < hold, 0, 1))
        else:
            send_sem, recv_sem = d, last // PAIR

        def start(tail):
            if tail:
                pack_tail(kind, d)
            edge_part(kind, slot(d), j, tail, send_sem, recv_sem, d).start()

        by_half(c if outward(kind) else other, j, start)

    def edges_sent(kind):
        edge_part(kind, every, slice(0, last), False, 0, 0, 1).wait_send()
        if outward(kind):
            by_half(c, last, lambda tail: edge_part(kind, every, last, tail, 1, 0, 1).wait_send())
        else:
            for d in OTHERS:
                by_half(oc if d % 2 else c, last, lambda tail: edge_part(kind, slot(d), last, tail, d, 0, d).wait_send())

    def chunk_arrived(kind, j):
        @pl.when(jnp.logical_and(lax.rem(j, PAIR) == 0, j < last))
        def _():
            edge_part(kind, every, pl.ds(j, PAIR), False, 0, j // PAIR, 1).wait_recv()

        def arrived(tail):
            edge_part(kind, every, last, tail, 0, last // PAIR, 1).wait_recv()
            if tail:
                for d in OTHERS:
                    unpack_tail(kind, d)

        @pl.when(j == last)
        def _():
            by_half(c, last, arrived)

    def group_arrived(kind, group):
        if group < 2:
            edge_part(kind, every, (slice(0, hold), slice(hold, last))[group], False, 0, group, 1).wait_recv()
        else:
            for d in OTHERS:
                def arrived(tail):
                    edge_part(kind, slot(d), last, tail, 0, 2 + slot(d), d).wait_recv()
                    if tail:
                        unpack_tail(kind, d)

                by_half(oc if d % 2 else c, last, arrived)

    def core_copy(l, b, stage):
        first, count = ((0, EARLY), (EARLY, SLABS - EARLY))[stage]
        return remote(grad.at[l, pl.ds(first, count), pl.ds((2 * b + 1) * cols, cols), :], core_recv.at[l, b, pl.ds(first, count)],
                      core_ss.at[l, stage], core_rs.at[l, stage], 1)

    def core_all(l, stage):
        part_of = core_recv.at[l, :, (slice(0, EARLY), slice(EARLY, SLABS))[stage]]
        return remote(part_of, part_of, core_ss.at[l, stage], core_rs.at[l, stage], 1)

    def seat(device):
        return lax.rem(device + dpn // 2, dpn)

    def in_stage(device, stage):
        early = (seat(device) + 1) * per <= EARLY
        return jnp.logical_not(early) if stage else early

    def dp_remote(src, dst, stage, l, i):
        return pltpu.make_async_remote_copy(src_ref=src, dst_ref=dst, send_sem=dp_ss.at[stage, l], recv_sem=dp_rs.at[stage, l],
                                            device_id={'dp': lax.rem(p + i, dpn)}, device_id_type=MESH)

    def spread_copy(l, i):
        return dp_remote(half.at[l, pl.ds(seat(lax.rem(p + i, dpn)) * per, per)], dp_recv.at[l, pl.ds((i - 1) * per, per)], 0, l, i)

    def dp_all(l, stage):
        most = (dpn - 1) * per
        part_of = (dp_recv.at[l], gathered.at[l, pl.ds(0, most)], w_recv.at[1, pl.ds(0, (dpn - 1) * piece)])[stage]
        return dp_remote(part_of, part_of, stage, l, 1)

    def cross_copy(l):
        return remote(cross_send.at[l], cross_recv.at[l], cross_ss.at[l], cross_rs.at[l], 2)

    def gather_copy(l, i, owner):
        return dp_remote(own_sum.at[l], gathered.at[l, pl.ds(seat(owner) * per, per)], 1, l, i)

    def part_copy(q):
        return remote(part.at[q], part_recv.at[q], p_ss.at[q], p_rs.at[q], 1)

    def load_nodes(raw, send, own):
        send[...] = jnp.zeros_like(send)
        send[0, :, :nodes] = raw[ox].astype(F32)
        send[1, :, :nodes] = raw[x].astype(F32)
        own[:cols, :] = send[1].astype(own.dtype)

    def load_edges(raw, send, own, kind):
        def put(j, lanes_j, val_of):
            for d in OTHERS:
                sample = x if d < 2 else ox
                send[slot(d), j] = val_of(sample, oc if d % 2 else c).astype(F32)
            own[:cols, lanes_j] = val_of(x, c)

        def pair(g):
            for j in (PAIR * g, PAIR * g + 1):
                put(j, at(j, EC), lambda s, h: raw[s, :, pl.ds(pl.multiple_of(h * eh + j * EC, D), EC)])
            for d in SEND_ORDER:
                edge_part(kind, slot(d), pl.ds(PAIR * g, PAIR), False, 0, g, d).start()

        loop((nch - 1) // PAIR, pair)
        first = (nch - 1) * EC
        used = edges - eh - first
        last = pl.ds(first, EC)

        def tail(s, h):
            left = raw[s, :, pl.ds(first, EC)]
            right = beside([raw[s, :, pl.ds(eh + first, used)], jnp.zeros((cols, EC - used), BF)])
            return jnp.where(h == 0, left.astype(F32), right.astype(F32)).astype(BF)

        put(nch - 1, last, tail)
        for d in SEND_ORDER:
            edge_start(kind, nch - 1, d)

    def place_edges(raw, block, d, j):
        s = x if d < 2 else ox
        h = oc if d % 2 else c
        val = block.astype(BF)
        first = (nch - 1) * EC
        used = edges - eh - first

        @pl.when(jnp.logical_or(j < nch - 1, h == 0))
        def _():
            raw[s, :, pl.ds(pl.multiple_of(h * eh + j * EC, D), EC)] = val

        @pl.when(jnp.logical_and(j == nch - 1, h == 1))
        def _():
            raw[s, :, pl.ds(eh + first, used)] = val[:, :used]

    def scoped(e0, e1, ge, msg, v0, v1, v2, agg0, agg1, d_agg, scol, rcol, srow, rrow, iota, lanes, ew1, ew1t, ew2, ew2t, nw1, nw1t, nw2, nw2t, vecs):
        tables = (v0, v1, v2)
        aggs = (agg0, agg1)
        edges_in = (e0, e1)

        barrier = pltpu.get_barrier_semaphore()
        for d in OTHERS:
            pl.semaphore_signal(barrier, inc=1, device_id={'tp': peer[d]}, device_id_type=MESH)
        for copy in loads[:1] + loads[4:] + loads[1:4]:
            copy.start()
        loads[0].wait()
        with jax.named_scope('send_nodes'):
            load_nodes(node_raw, n_send, v0)
        ncop = node_copies(n_send, n_recv, 0)
        for copy in loads[4:]:
            copy.wait()
        q = cols
        w_send[:HEAD, :] = jnp.zeros((HEAD, D), F32)
        for k in THREE:
            w_send[k * layers:(k + 1) * layers, :cols] = evec_in[k]
            w_send[(3 + k) * layers:(4 + k) * layers, :cols] = nvec_in[k]
        for l in range(layers):
            w_send[packed(l, 0, 3), :] = ew1_in[pl.ds(l * 3 * q, 3 * q), :].astype(F32)
            w_send[packed(l, 3), :] = ew2_in[pl.ds(l * q, q), :].astype(F32)
            w_send[packed(l, 4, 2), :] = nw1_in[pl.ds(l * 2 * q, 2 * q), :].astype(F32)
            w_send[packed(l, 6), :] = nw2_in[pl.ds(l * q, q), :].astype(F32)
        with jax.named_scope('barrier'):
            @pl.when(t != LEADER)
            def _():
                pl.semaphore_wait(barrier, len(OTHERS))
                pl.semaphore_signal(ready, inc=1, device_id={'tp': LEADER}, device_id_type=MESH)

            @pl.when(t == LEADER)
            def _():
                pl.semaphore_wait(ready, len(OTHERS))
                for i in dp_others:
                    pl.semaphore_signal(barrier, inc=1, device_id={'dp': lax.rem(p + i, dpn)}, device_id_type=MESH)

        w_cross.start()
        w_pair.start()
        ncop[1].start()
        ncop[0].start()
        loads[1].wait()
        with jax.named_scope('send_edges'):
            load_edges(edge_raw, e_send, e0, EDGE_IN)
        loads[2].wait()
        load_nodes(gnode_raw, gn_send, d_part)
        gcop = node_copies(gn_send, gn_recv, 1)
        gcop[1].start()
        gcop[0].start()
        loads[3].wait()
        with jax.named_scope('send_grads'):
            load_edges(gedge_raw, g_send, ge, GRAD_IN)

        with jax.named_scope('dp_barrier'):
            @pl.when(t == LEADER)
            def _():
                pl.semaphore_wait(barrier, len(OTHERS) + dpn - 1)
                for d in OTHERS:
                    pl.semaphore_signal(ready, inc=1, device_id={'tp': peer[d]}, device_id_type=MESH)

            @pl.when(t != LEADER)
            def _():
                pl.semaphore_wait(ready, 1)

        w_cross.wait_recv()
        for i in dp_others:
            weight_copy(i, p).start()

        @pl.when(c == 1)
        def _():
            for recv in (e_recv, g_recv):
                recv[:, last, :, D:] = jnp.zeros((len(OTHERS), cols, EC - D), F32)

        iota[...] = lax.broadcasted_iota(jnp.int32, (T, D), 0).astype(I16)
        lanes[...] = lax.broadcasted_iota(jnp.int32, (16, D), 1).astype(I16)

        ids_raw[...] = jnp.full(ids_raw.shape, -1, jnp.int32)
        for which, src in enumerate((send_ids, recv_ids)):
            ids_raw[which:which + 1, :edges] = src[...].reshape(1, edges)

        def ids(b):
            for which, (row_ref, col_ref) in enumerate(((srow, scol), (rrow, rcol))):
                wide = jnp.broadcast_to(ids_raw[which:which + 1, pl.ds(pl.multiple_of(c * eh + b * D, D), D)], (D, D))
                row_ref[at(b, 16), :] = wide[:16].astype(I16)
                col_ref[at(b, D), :] = flip(wide.astype(F32)).astype(jnp.int32).astype(I16)

        with jax.named_scope('ids'):
            loop(eh // D, ids)

        def keys(ref, step):
            return [ref[pl.ds(pl.multiple_of(step * (KS // D) * 16 + 16 * h, 16), 1), :] for h in range(KS // D)]

        bias_cols[...] = flip(stacked([eb1_in[...], nb1_in[...], jnp.zeros((D - 2 * layers, D), F32)]))

        def join_weights(l):
            for d in range(GROUP):
                src = w_recv.at[slot(d)] if d else w_send
                r = rows_of(d)
                for k in THREE:
                    ew1[l, pl.ds(k * D + d * q, q), :] = src[packed(l, k), :].astype(BF)
                ew2t[l, r, :] = src[packed(l, 3), :].astype(BF)
                for k in BOTH:
                    nw1[l, pl.ds(k * D + d * q, q), :] = src[packed(l, 4 + k), :].astype(BF)
                nw2t[l, r, :] = src[packed(l, 6), :].astype(BF)

            def flip_bf(mat):
                return flip(mat.astype(F32)).astype(BF)

            for k in THREE:
                ew1t[l, :, mat(k)] = flip_bf(ew1[l, mat(k), :])
            for k in BOTH:
                nw1t[l, :, mat(k)] = flip_bf(nw1[l, mat(k), :])
            ew2[l] = flip_bf(ew2t[l])
            nw2[l] = flip_bf(nw2t[l])

        def wait_recvs(copies):
            copies[1].wait_recv()
            copies[2].start()
            copies[0].wait_recv()
            copies[2].wait_recv()

        with jax.named_scope('node_wait'):
            wait_recvs(ncop)
        for d in OTHERS:
            v0[rows_of(d), :] = n_recv[slot(d)].astype(BF)
        with jax.named_scope('weight_wait'):
            dp_all(0, 2).wait_recv()
            w_relay.start()
            w_pair.wait_recv()
            w_relay.wait_recv()
        rows_all = beside([w_send[:HEAD, :cols]] + [w_recv[d, :HEAD, :cols] for d in range(3)])
        vecs[...] = flip(stacked([rows_all, jnp.zeros((D - HEAD, D), F32)]))
        join_weights(0)

        def vec(l, node):
            first = 6 * node + l
            return [vecs[:, first + 2 * k:first + 2 * k + 1] for k in THREE]

        def bias(l, node):
            return bias_cols[:, node * layers + l:node * layers + l + 1]

        def hidden_of_nodes(l):
            table, b1 = tables[l], bias(l, 0)

            def body(step):
                xs = gather(table, keys(srow, step), iota).astype(BF)
                xr = gather(table, keys(rrow, step), iota).astype(BF)
                hidden[l, :, at(step, KS)] = dot(ew1t[l, :, mat(1, 2)], stacked([xs, xr])) + b1

            loop(eh // KS, body)

        def edge_forward(l):
            e_in = edges_in[l]

            def body(j):
                for sub in range(EC // T):
                    a = at(j * (EC // T) + sub, T)
                    if l == 0:
                        if sub == 0:
                            chunk_arrived(EDGE_IN, j)
                        for d in OTHERS:
                            e_in[rows_of(d), a] = e_recv[slot(d), j, :, sub * T:(sub + 1) * T].astype(BF)
                    e_val = e_in[:, a]
                    hid = hidden[l, :, a] + dot(ew1t[l, :, mat(0)], e_val)
                    hidden[l, :, a] = hid
                    message, nrm, std = mlp_tail(hid, ew2t[l], vec(l, 0))
                    normed[l, :, a] = nrm
                    inv[l:l + 1, a] = std
                    msg[:, a] = message
                    e_new = (e_val.astype(F32) + message.astype(F32)).astype(BF)
                    if l < top:
                        edges_in[l + 1][:, a] = e_new
                    else:
                        for d in OTHERS:
                            e_send[slot(d), j, :, sub * T:(sub + 1) * T] = e_new[rows_of(d)].astype(F32)
                        if sub == 0:
                            own_parts = []
                        own_parts.append(e_new[:q])
                if l == top:
                    for d in SEND_ORDER:
                        edge_start(EDGE_OUT, j, d)
                    place_edges(edge_raw, beside(own_parts), 0, j)

            loop(nch, body)

        def segment_sum(acc, ids_ref):
            acc[...] = jnp.zeros(acc.shape, F32)

            def body(step):
                scatter(acc, msg[:, at(step, KS)], ids_ref[at(step, KS), :], lanes)

            loop(eh // KS, body)

        def node_forward(l):
            table, agg, out = tables[l], aggs[l], tables[l + 1]

            def body(step):
                a = pl.ds(pl.multiple_of(step * TN, D), TN)
                v_in = table[:, a]
                agg_bf = (part[l, :, a] + swap_halves(part_recv[l, :, a])).astype(BF)
                agg[:, a] = agg_bf
                hid = dot(nw1t[l], stacked([v_in, agg_bf])) + bias(l, 1)
                nhid[l, :, a] = hid
                message, nrm, std = mlp_tail(hid, nw2t[l], vec(l, 1))
                nnrm[l, :, a] = nrm
                ninv[l:l + 1, a] = std
                out[:, a] = (v_in.astype(F32) + message.astype(F32)).astype(BF)

            loop(npad // TN, body)

        for l in range(layers):
            with jax.named_scope(f'gather_{l}'):
                hidden_of_nodes(l)
            if l == top:
                edges_sent(EDGE_IN)
            with jax.named_scope(f'edge_forward_{l}'):
                edge_forward(l)
            with jax.named_scope(f'sum_{l}'):
                segment_sum(part.at[l], rcol)
            part_copy(l).start()
            if l == 0:
                join_weights(1)
                gcop[1].wait_recv()
                gcop[2].start()
            with jax.named_scope(f'part_wait_{l}'):
                part_copy(l).wait_recv()
            with jax.named_scope(f'node_forward_{l}'):
                node_forward(l)
        no_send[...] = tables[layers][rows_of(2), :].astype(F32)
        no_copy = remote(no_send, no_recv, n_ss.at[2, 0], n_rs.at[2, 0], 2)
        no_copy.start()
        node_raw[x] = tables[layers][:q, :nodes]

        grad[...] = jnp.zeros_like(grad)
        sums[...] = jnp.zeros_like(sums)
        with jax.named_scope('grad_node_wait'):
            gcop[0].wait_recv()
            gcop[2].wait_recv()
        for d in OTHERS:
            d_part[rows_of(d), :] = gn_recv[slot(d)]

        def node_backward(l):
            table, agg = tables[l], aggs[l]

            def body(step):
                a = pl.ds(pl.multiple_of(step * TN, D), TN)
                d_in = d_part[:, a]
                if l < top:
                    d_in = d_in + part[layers + l + 1, :, a] + swap_halves(part_recv[layers + l + 1, :, a])
                    d_in = d_in.astype(BF).astype(F32)
                d_hid, d_w2, parts = mlp_back(d_in, nhid[l, :, a], nnrm[l, :, a], ninv[l:l + 1, a], nw2[l], vec(l, 1))
                add_sums(sums.at[l, 1], [parts])
                grad[l, 4] += d_w2
                grad[l, 2] += dot_nt(table[:, a], d_hid)
                grad[l, 3] += dot_nt(agg[:, a], d_hid)
                d_part[:, a] = d_in + dot(nw1[l, mat(0), :], d_hid)
                d_agg[:, a] = dot(nw1[l, mat(1), :], d_hid).astype(BF)

            loop(npad // TN, body)

        def gather_back():
            def body(step):
                msg[:, at(step, KS)] = gather(d_agg, keys(rrow, step), iota).astype(BF)

            loop(eh // KS, body)

        def edge_backward(l):
            e_in = edges_in[l]

            def body(j):
                all_parts, d_w2s, d_w1s, own_parts = [], [], [], []
                for sub in range(EC // T):
                    a = at(j * (EC // T) + sub, T)
                    if l == top:
                        if sub == 0:
                            chunk_arrived(GRAD_IN, j)
                        for d in OTHERS:
                            ge[rows_of(d), a] = g_recv[slot(d), j, :, sub * T:(sub + 1) * T].astype(BF)
                    d_res = ge[:, a].astype(F32)
                    d_msg = d_res + msg[:, a].astype(F32)
                    d_hid, d_w2, parts = mlp_back(d_msg, hidden[l, :, a], normed[l, :, a], inv[l:l + 1, a], ew2[l], vec(l, 0))
                    all_parts.append(parts)
                    d_w2s.append(d_w2)
                    d_w1s.append(dot_nt(e_in[:, a], d_hid))
                    msg[:, a] = d_hid
                    d_new = (d_res + dot(ew1[l, mat(0), :], d_hid)).astype(BF)
                    if l > 0:
                        ge[:, a] = d_new
                    else:
                        for d in OTHERS:
                            g_send[slot(d), j, :, sub * T:(sub + 1) * T] = d_new[rows_of(d)].astype(F32)
                        own_parts.append(d_new[:q])
                add_sums(sums.at[l, 0], all_parts)
                grad[l, 1] += sum(d_w2s[1:], d_w2s[0])
                grad[l, 0] += sum(d_w1s[1:], d_w1s[0])
                if l == 0:
                    @pl.when(j < hold)
                    def _():
                        for d in SEND_ORDER:
                            edge_start(GRAD_OUT, j, d)
                    place_edges(gedge_raw, beside(own_parts), 0, j)

            loop(nch, body)

        def vector_slab(l):
            def total(node, k):
                return column_sum(flip(sums[l, node, mat(k), :]))

            lat = stacked([total(node, k) for node in BOTH for k in THREE])
            biases = stacked([total(node, 3) for node in BOTH])
            n_lat = lat.shape[0]
            for d in range(GROUP):
                grad[l, VEC_SLAB, d * cols:d * cols + n_lat, :cols] = lat[:, rows_of(d)]
                grad[l, VEC_SLAB, d * cols + n_lat:d * cols + n_lat + 2, :] = biases

        def reduce_start(l, stage):
            for b in BOTH:
                core_copy(l, b, stage).start()

        def chip_sum(l, stage):
            row = lax.broadcasted_iota(jnp.int32, (cols, D), 0)
            edge_row = jnp.logical_or(row < 3, row == 6)
            core_all(l, stage).wait_recv()
            for b in BOTH:
                for k in range(SLABS)[STAGES[stage]]:
                    own = grad[l, k, rows_of(2 * b), :]
                    if k in EDGE_SLABS:
                        own = own + core_recv[l, b, k]
                    elif k == VEC_SLAB:
                        own = own + jnp.where(edge_row, core_recv[l, b, k], 0.0)
                    half[l, k, b] = own
            for i in dp_others:
                @pl.when(in_stage(lax.rem(p + i, dpn), stage))
                def _():
                    spread_copy(l, i).start()

        def dp_sum(l, stage):
            @pl.when(in_stage(p, stage))
            def _():
                total = half[l, pl.ds(seat(p) * per, per)]
                dp_all(l, 0).wait_recv()
                for i in dp_others:
                    total = total + dp_recv[l, pl.ds((i - 1) * per, per)]
                own_sum[l] = total[:, 0]
                cross_send[l] = total[:, 1]
                cross_copy(l).start()

        def cross_sum(l):
            cross_copy(l).wait_recv()
            total = own_sum[l] + cross_recv[l]
            own_sum[l] = total
            gathered[l, pl.ds(seat(p) * per, per)] = total
            for i in dp_others:
                gather_copy(l, i, p).start()

        def project(l):
            table = tables[l]

            def body(step):
                a = pl.ds(pl.multiple_of(step * TN, D), TN)
                s_bf, r_bf, v_in = s_sum[:, a].astype(BF), r_sum[:, a].astype(BF), table[:, a]
                part[layers + l, :, a] = dot(ew1[l, mat(1), :], s_bf) + dot(ew1[l, mat(2), :], r_bf)
                grad[l, 6] += dot_nt(v_in, s_bf)
                grad[l, 7] += dot_nt(v_in, r_bf)

            loop(npad // TN, body)

        for l in reversed(range(layers)):
            first_layer = l == 0
            with jax.named_scope(f'node_backward_{l}'):
                node_backward(l)
            if first_layer:
                with jax.named_scope('chip_sum_1'):
                    chip_sum(1, 0)
                    chip_sum(1, 1)
            with jax.named_scope(f'gather_back_{l}'):
                gather_back()
            if first_layer:
                edges_sent(GRAD_IN)
            with jax.named_scope(f'edge_backward_{l}'):
                edge_backward(l)
            vector_slab(l)
            reduce_start(l, 0)
            if first_layer:
                with jax.named_scope('dp_sum_1'):
                    dp_sum(1, 0)
                    dp_sum(1, 1)
            with jax.named_scope(f'sum_send_{l}'):
                segment_sum(s_sum, scol)
            if first_layer:
                with jax.named_scope('chip_sum_0'):
                    chip_sum(0, 0)
            with jax.named_scope(f'sum_recv_{l}'):
                segment_sum(r_sum, rcol)
            with jax.named_scope(f'project_{l}'):
                project(l)
            reduce_start(l, 1)
            part_copy(layers + l).start()
            if first_layer:
                with jax.named_scope('chip_sum_late'):
                    chip_sum(0, 1)
                with jax.named_scope('dp_sum_0'):
                    dp_sum(0, 0)
            with jax.named_scope(f'back_wait_{l}'):
                part_copy(layers + l).wait_recv()

        def final(step):
            a = pl.ds(pl.multiple_of(step * TN, D), TN)
            d_in = (d_part[:, a] + part[layers, :, a] + swap_halves(part_recv[layers, :, a])).astype(BF)
            v2[:, a] = d_in

        loop(npad // TN, final)
        gnode_raw[x] = v2[:q, :nodes]
        with jax.named_scope('dp_sum_late'):
            dp_sum(0, 1)

        dn_send[...] = v2[rows_of(2), :].astype(F32)
        dn_copy = remote(dn_send, dn_recv, n_ss.at[2, 1], n_rs.at[2, 1], 2)
        dn_copy.start()

        def send_rest(j):
            for d in SEND_ORDER:
                edge_start(GRAD_OUT, j, d)

        loop(nch, send_rest, hold)

        with jax.named_scope('node_out_wait'):
            no_copy.wait_recv()
        node_raw[ox] = no_recv[:, :nodes].astype(BF)

        def place_e(j):
            for d in OTHERS:
                place_edges(edge_raw, eo_recv[slot(d), j], d, j)

        with jax.named_scope('place_edge_out'):
            for group in THREE:
                group_arrived(EDGE_OUT, group)
            loop(nch, place_e)

        def place_g(j):
            for d in OTHERS:
                place_edges(gedge_raw, de_recv[slot(d), j], d, j)

        with jax.named_scope('place_first'):
            group_arrived(GRAD_OUT, 0)
            loop(hold, place_g)
        for l in range(layers):
            with jax.named_scope(f'cross_sum_{l}'):
                cross_sum(l)
        with jax.named_scope('d_node_wait'):
            dn_copy.wait_recv()
        gnode_raw[ox] = dn_recv[:, :nodes].astype(BF)
        with jax.named_scope('place_rest'):
            group_arrived(GRAD_OUT, 1)
            loop(last, place_g, hold)
        for l in range(layers):
            dp_all(l, 1).wait_recv()
            ew1_buf[l, 0] = gathered[l, 0]
            ew1_buf[l, 1:] = gathered[l, EARLY:]
            ew2_buf[l] = gathered[l, 1]
            nw1_buf[l] = gathered[l, 2:4]
            nw2_buf[l] = gathered[l, 4]
            small = gathered[l, VEC_SLAB]
            for k in THREE:
                evec_buf[k, l:l + 1, :] = small[k:k + 1, :cols]
                nvec_buf[k, l:l + 1, :] = small[3 + k:4 + k, :cols]
            eb1_buf[l:l + 1, :] = small[6:7]
            nb1_buf[l:l + 1, :] = small[7:8]
        for l in range(layers):
            for stage in BOTH:
                core_all(l, stage).wait_send()
            cross_copy(l).wait_send()
            dp_all(l, 0).wait_send()
            dp_all(l, 1).wait_send()
        for copy in ncop + gcop + (w_pair, w_cross, w_relay):
            copy.wait_send()
        dp_all(0, 2).wait_send()
        no_copy.wait_send()
        dn_copy.wait_send()
        for k in range(2 * layers):
            part_copy(k).wait_send()
        edges_sent(EDGE_OUT)
        with jax.named_scope('place_last'):
            group_arrived(GRAD_OUT, 2)
            loop(nch, place_g, last)
        edges_sent(GRAD_OUT)

    bf = lambda *s: pltpu.VMEM(s, BF)
    pl.run_scoped(
        scoped, bf(D, eh), bf(D, eh), bf(D, eh), bf(D, eh), bf(D, npad), bf(D, npad), bf(D, npad), bf(D, npad), bf(D, npad), bf(D, npad),
        pltpu.VMEM((eh, D), I16), pltpu.VMEM((eh, D), I16), pltpu.VMEM((eh // D * 16, D), I16), pltpu.VMEM((eh // D * 16, D), I16),
        pltpu.VMEM((T, D), I16), pltpu.VMEM((16, D), I16),
        bf(layers, 3 * D, D), bf(layers, D, 3 * D), bf(layers, D, D), bf(layers, D, D),
        bf(layers, 2 * D, D), bf(layers, D, 2 * D), bf(layers, D, D), bf(layers, D, D), pltpu.VMEM((D, D), F32))


def finish_moves(src, dst):
    if len(src.shape) != 3 or src.dtype != BF:
        return [(src, dst)]
    return [(src.at[s, pl.ds(r, 8)], dst.at[s, pl.ds(r, 8)]) for s in range(src.shape[0]) for r in range(0, src.shape[1], 8)]


def finish_kernel(*refs):
    count = len(refs) // 2
    moves = sum((finish_moves(refs[k], refs[count + k]) for k in range(count)), [])
    puts = [pltpu.make_async_copy(src, dst, refs[-1]) for src, dst in moves]
    for put in puts:
        put.start()
    for put in puts:
        put.wait()


def keep_in_vmem(val):
    return pltpu.with_memory_space_constraint(val, pltpu.VMEM)


def finish(arrays):
    return pl.pallas_call(
        finish_kernel,
        name='finish',
        out_shape=[jax.ShapeDtypeStruct(a.shape, a.dtype) for a in arrays],
        in_specs=[VM] * len(arrays),
        out_specs=[HB] * len(arrays),
        scratch_shapes=[pltpu.SemaphoreType.DMA],
        compiler_params=pltpu.CompilerParams(vmem_limit_bytes=1 << 20),
    )(*[keep_in_vmem(a) for a in arrays])


def solution(mesh):
    lat_spec = P('dp', None, 'tp')
    first_spec = P(None, None, 'tp', None)
    col_spec = P(None, None, 'tp')
    param_specs = (first_spec, P(), col_spec, col_spec, first_spec, P(), col_spec, col_spec)
    in_specs = (lat_spec, lat_spec, P(), P(), lat_spec, lat_spec) + param_specs
    out_specs = (lat_spec, lat_spec, lat_spec, lat_spec) + param_specs
    shape = jax.ShapeDtypeStruct

    def local_step(node_lat, edge_lat, senders, receivers, grad_node, grad_edge, edge_w1, edge_b1, edge_w2, edge_vec, node_w1, node_b1, node_w2, node_vec):
        layers = edge_w1.shape[0]
        cols = node_lat.shape[2]
        nodes, edges = node_lat.shape[1], edge_lat.shape[1]
        npad = -(-nodes // TN) * TN
        eh = -(-edges // (2 * EC)) * EC
        nch = eh // EC
        dpn = mesh.shape['dp']
        per = SLABS // dpn
        dims = (layers, cols, nodes, edges, npad, eh, dpn)
        flat = lambda arr: jnp.swapaxes(arr, 1, 2)
        lead = lambda arr: jnp.transpose(arr, (1, 0, 2))
        args = (flat(node_lat), flat(edge_lat), flat(grad_node), flat(grad_edge), senders, receivers,
                edge_w1.reshape(-1, D), flat(edge_w2).reshape(-1, D), node_w1.reshape(-1, D), flat(node_w2).reshape(-1, D),
                lead(edge_vec), lead(node_vec), edge_b1, node_b1)
        vm, sem = pltpu.VMEM, pltpu.SemaphoreType.DMA
        wrows = -(-(HEAD + layers * LROWS) // (8 * dpn)) * 8 * dpn
        lat_n, lat_e = (2, cols, nodes), (2, cols, edges)
        outs = [RESULT(lat_n, BF), RESULT(lat_e, BF), RESULT(lat_n, BF), RESULT(lat_e, BF),
                RESULT((layers, 3, cols, D), F32), RESULT((layers, D), F32), RESULT((layers, cols, D), F32), RESULT((3, layers, cols), F32),
                RESULT((layers, 2, cols, D), F32), RESULT((layers, D), F32), RESULT((layers, cols, D), F32), RESULT((3, layers, cols), F32)]
        scratch = [
            *[vm(a.shape, a.dtype) for a in args[4:]], vm((wrows, D), F32), vm((3, wrows, D), F32),
            vm((2, cols, npad), F32), vm((3, cols, npad), F32), vm((2, cols, npad), F32), vm((3, cols, npad), F32),
            vm((cols, npad), F32), vm((cols, npad), F32), vm((cols, npad), F32), vm((cols, npad), F32),
            vm((2, 3, cols + cols // GROUP, D), F32), vm((4, 3, cols + cols // GROUP, D), F32), *[vm((3, nch, cols, EC), F32)] * 6,
            vm((2 * layers, D, npad), F32), vm((2 * layers, D, npad), F32),
            vm((layers, D, eh), F32), vm((layers, D, eh), F32), vm((layers, eh), F32),
            vm((layers, D, npad), F32), vm((layers, D, npad), F32), vm((layers, npad), F32),
            vm((D, npad), F32), vm((D, npad), F32), vm((D, npad), F32), vm((2, 2 * eh), jnp.int32), vm((D, D), F32), vm((layers, 2, 4 * D, D), F32),
            vm((layers, SLABS, D, D), F32), vm((layers, 2, SLABS, cols, D), F32), vm((layers, SLABS, 2, cols, D), F32),
            vm((layers, (dpn - 1) * per, 2, cols, D), F32), vm((layers, per, cols, D), F32), vm((layers, per, cols, D), F32),
            vm((layers, per, cols, D), F32), vm((layers, SLABS, cols, D), F32),]
        own_sems = [
            sem((layers, 2)), sem((3, layers)), sem((layers,)), sem((3,)), sem((3, 3)), sem((2, nch // PAIR + 1)), sem((2, 5)), sem((2 * layers,)),
            pltpu.SemaphoreType.REGULAR,
            sem((len(args),)), sem((3,)), sem((3, 3)), sem((4, 4)), sem((2 * layers,)), sem((layers, 2)), sem((3, layers)), sem((layers,))]
        res = pl.pallas_call(
            lambda *refs: pl.run_scoped(lambda *own: step_kernel(dims, *refs, *own), *own_sems),
            name='graph_step',
            out_shape=outs,
            in_specs=[HB] * len(args),
            out_specs=[VM] * len(outs),
            scratch_shapes=scratch,
            compiler_params=pltpu.CompilerParams(collective_id=0, has_side_effects=True, vmem_limit_bytes=VMEM_LIMIT),
        )(*args)

        res = finish(res)
        return (flat(res[0]), flat(res[1]), flat(res[2]), flat(res[3]),
                res[4], res[5], flat(res[6]), lead(res[7]), res[8], res[9], flat(res[10]), lead(res[11]))

    return jax.shard_map(local_step, mesh=mesh, in_specs=in_specs, out_specs=out_specs, check_vma=False)
```

```python
import jax
import jax.numpy as jnp
from jax import lax
from jax.experimental import pallas as pl
from jax.experimental.pallas import tpu as pltpu
from jax.sharding import PartitionSpec as P

LN_EPS = 1e-5
D = 128
T = 256
TN = 384
EC = 512
KS = 1408
BF = jnp.bfloat16
F32 = jnp.float32
I16 = jnp.int16
MESH = pl.DeviceIdType.MESH
VM = pl.BlockSpec(memory_space=pltpu.VMEM)
HB = pl.BlockSpec(memory_space=pl.ANY)
RESULT = pltpu.VMEM
GROUP = 4
BOTH = (0, 1)
THREE = (0, 1, 2)
OTHERS = (1, 2, 3)
EDGE_IN, GRAD_IN, EDGE_OUT, GRAD_OUT = range(4)
SEND_ORDER = (2, 3, 1)
LROWS = 7 * (D // 4)
HEAD = 16
LEADER = 0
VMEM_LIMIT = 63_000_000
SLABS = 8
EARLY = 6
VEC_SLAB = 5
EDGE_SLABS = (0, 1, 6, 7)
STAGES = (slice(0, EARLY), slice(EARLY, SLABS))


def dot(a, b):
    return jnp.dot(a, b, preferred_element_type=F32)


def dot_nt(a, b):
    return lax.dot_general(a, b, (((1,), (1,)), ((), ())), preferred_element_type=F32)


def mat(k, n=1):
    return slice(k * D, (k + n) * D)


def rows_of(d):
    q = D // 4
    return slice(d * q, (d + 1) * q)


def at(step, width):
    return pl.ds(pl.multiple_of(step * width, width), width)


def loop(stop, body, start=0):
    def step(j, carry):
        body(j)
        return carry

    lax.fori_loop(start, stop, step, 0)


def column_sum(val):
    return jnp.sum(val, axis=0, keepdims=True)


def flip(val):
    return jnp.swapaxes(val, 0, 1)


def stacked(parts):
    return jnp.concatenate(parts, axis=0)


def beside(parts):
    return jnp.concatenate(parts, axis=1)


def slot(d):
    return d - 1


def sigmoid(hidden):
    return 1.0 / (1.0 + jnp.exp(-hidden))


def fold(val):
    total = val[:, mat(0)]
    for start in range(D, val.shape[1], D):
        total = total + val[:, start:start + D]
    return total


def swap_halves(val):
    return stacked([val[rows_of(d)] for d in (1, 0, 3, 2)])


def gather(table, keys, iota):
    acc = None
    nodes = table.shape[1]
    one, zero = jnp.ones((), BF), jnp.zeros((), BF)
    for base in range(0, nodes, T):
        width = min(T, nodes - base)
        ids = iota[0:width, :]
        hot = beside([jnp.where(ids == (key - jnp.asarray(base, I16)), one, zero) for key in keys])
        part = dot(table[:, base:base + width], hot)
        acc = part if acc is None else acc + part
    return acc


def scatter(acc_ref, val, cols, lanes):
    nodes = acc_ref.shape[1]
    one, zero = jnp.ones((), BF), jnp.zeros((), BF)
    row = lanes[0:1, :]
    for base in range(0, nodes, T):
        width = min(T, nodes - base)
        hot = beside([jnp.where((row + jnp.asarray(base + s, I16)) == cols, one, zero) for s in range(0, width, D)])
        acc_ref[:, base:base + width] += dot(val, hot)


def mlp_tail(hidden, w2t, vec):
    act = (hidden * sigmoid(hidden)).astype(BF)
    out = dot(w2t, act) + vec[0]
    mean = column_sum(out) / D
    centered = out - mean
    var = column_sum(centered * centered) / D
    inv = lax.rsqrt(var + LN_EPS)
    normed = centered * inv
    message = (normed * vec[1] + vec[2]).astype(BF)
    return message, normed, inv


def mlp_back(d_msg, hidden, normed, inv, w2, vec):
    d_normed = d_msg * vec[1]
    mean0 = column_sum(d_normed) / D
    mean1 = column_sum(d_normed * normed) / D
    d_out = inv * (d_normed - mean0 - normed * mean1)
    d_out_bf = d_out.astype(BF)
    sig = sigmoid(hidden)
    act = (hidden * sig).astype(BF)
    d_w2 = dot_nt(d_out_bf, act)
    d_hidden = dot(w2, d_out_bf) * (sig * (1.0 + hidden * (1.0 - sig)))
    sums = (fold(d_out), fold(d_msg * normed), fold(d_msg), fold(d_hidden))
    return d_hidden.astype(BF), d_w2, sums


def add_sums(ref, parts):
    for q in range(4):
        total = parts[0][q]
        for other in parts[1:]:
            total = total + other[q]
        ref[mat(q), :] += total


def step_kernel(dims, *refs):
    layers, cols, nodes, edges, npad, eh, dpn = dims
    nch = eh // EC
    top = layers - 1
    n_in = 14
    hbm_in = refs[:n_in]
    n_out = 12
    (node_raw, edge_raw, gnode_raw, gedge_raw, ew1_buf, eb1_buf, ew2_buf, evec_buf, nw1_buf, nb1_buf, nw2_buf, nvec_buf) = refs[n_in:n_in + n_out]
    (send_ids, recv_ids, ew1_in, ew2_in, nw1_in, nw2_in, evec_in, nvec_in, eb1_in, nb1_in, w_send, w_recv, n_send, n_recv, gn_send, gn_recv, no_send, no_recv, dn_send, dn_recv,
     t_send, t_recv, e_send, g_send, e_recv, g_recv, eo_recv, de_recv, part, part_recv, hidden, normed, inv, nhid, nnrm, ninv, d_part, s_sum, r_sum,
     ids_raw, bias_cols, sums, grad, core_recv, half, dp_recv, cross_send, cross_recv, own_sum, gathered,
     core_rs, dp_rs, cross_rs, w_rs, n_rs, e_rs, o_rs, p_rs, ready, load_sem, w_ss, n_ss, e_ss, p_ss, core_ss, dp_ss, cross_ss) = refs[n_in + n_out:]

    t = lax.axis_index('tp')
    p = lax.axis_index('dp')
    per = SLABS // dpn
    dp_others = range(1, dpn)
    x, c = t // 2, lax.rem(t, 2)
    ox, oc = 1 - x, 1 - c
    peer = [t, t + 1 - 2 * c, t + 2 - 4 * x, t + 3 - 2 * c - 4 * x]

    def remote(src, dst, ssem, rsem, d):
        return pltpu.make_async_remote_copy(src_ref=src, dst_ref=dst, send_sem=ssem, recv_sem=rsem,
                                            device_id={'tp': peer[d]}, device_id_type=MESH)

    small_in = (send_ids, recv_ids, ew1_in, ew2_in, nw1_in, nw2_in, evec_in, nvec_in, eb1_in, nb1_in)
    loads = [pltpu.make_async_copy(src, dst, load_sem.at[q]) for q, (src, dst) in enumerate(
        zip(hbm_in, (node_raw, edge_raw, gnode_raw, gedge_raw) + small_in))]

    def node_copies(send, recv, kind):
        return (remote(send.at[1], recv.at[0], n_ss.at[kind, 0], n_rs.at[kind, 0], 1),
                remote(send.at[0], recv.at[1], n_ss.at[kind, 1], n_rs.at[kind, 1], 2),
                remote(recv.at[1], recv.at[2], n_ss.at[kind, 2], n_rs.at[kind, 2], 1))

    piece = w_send.shape[0] // dpn

    def packed(l, k, count=1):
        return pl.ds(HEAD + l * LROWS + k * cols, count * cols)

    def weight_rows(owner):
        return pl.ds(pl.multiple_of(owner * piece, 8), piece)

    w_pair = remote(w_send, w_recv.at[0], w_ss.at[0], w_rs.at[0], 1)
    w_cross = remote(w_send.at[weight_rows(p)], w_recv.at[1, weight_rows(p)], w_ss.at[1], w_rs.at[1], 2)
    w_relay = remote(w_recv.at[1], w_recv.at[2], w_ss.at[2], w_rs.at[2], 1)

    def weight_copy(i, owner):
        rows = w_recv.at[1, weight_rows(owner)]
        return dp_remote(rows, rows, 2, 0, i)

    last = nch - 1
    hold = nch - 3
    buffers = ((e_send, e_recv), (g_send, g_recv), (e_send, eo_recv), (g_send, de_recv))

    def outward(kind):
        return kind in (EDGE_OUT, GRAD_OUT)

    every = slice(None)
    ragged = pl.ds(D, D // GROUP)
    rest = [slice(g * cols // GROUP, (g + 1) * cols // GROUP) for g in range(GROUP)]

    def edge_part(kind, which, j, tail, send_sem, recv_sem, d):
        src, dst = buffers[kind]
        if tail:
            src, dst = t_send.at[kind % 2, which], t_recv.at[kind, which]
        else:
            src, dst = src.at[which, j], dst.at[which, j]
        recv_sems = o_rs.at[kind - EDGE_OUT, recv_sem] if outward(kind) else e_rs.at[kind, recv_sem]
        return remote(src, dst, e_ss.at[kind, send_sem], recv_sems, d)

    def by_half(half_id, j, action):
        narrow = jnp.logical_and(j == last, half_id == 1)

        @pl.when(jnp.logical_not(narrow))
        def _():
            action(False)

        @pl.when(narrow)
        def _():
            action(True)

    def pack_tail(kind, d):
        src, out = buffers[kind][0].at[slot(d), last], t_send.at[kind % 2, slot(d)]
        out[:cols, :] = src[:, :D]
        over = src[:, ragged]
        out[cols:, :] = beside([over[r] for r in rest])

    def unpack_tail(kind, d):
        src, out = t_recv.at[kind, slot(d)], buffers[kind][1].at[slot(d), last]
        out[:, :D] = src[:cols, :]
        over = src[cols:, :]
        out[:, ragged] = stacked([over[:, rows_of(g)] for g in range(GROUP)])

    def edge_start(kind, j, d):
        other = oc if d % 2 else c
        if outward(kind):
            send_sem, recv_sem = jnp.where(j == last, 1, 0), jnp.where(j == last, 2 + slot(d), jnp.where(j < hold, 0, 1))
        else:
            send_sem, recv_sem = jnp.where(j == last, d, 0), j

        def start(tail):
            if tail:
                pack_tail(kind, d)
            edge_part(kind, slot(d), j, tail, send_sem, recv_sem, d).start()

        by_half(c if outward(kind) else other, j, start)

    def edges_sent(kind):
        edge_part(kind, every, slice(0, last), False, 0, 0, 1).wait_send()
        if outward(kind):
            by_half(c, last, lambda tail: edge_part(kind, every, last, tail, 1, 0, 1).wait_send())
        else:
            for d in OTHERS:
                by_half(oc if d % 2 else c, last, lambda tail: edge_part(kind, slot(d), last, tail, d, 0, d).wait_send())

    def chunk_arrived(kind, j):
        def arrived(tail):
            edge_part(kind, every, j, tail, 0, j, 1).wait_recv()
            if tail:
                for d in OTHERS:
                    unpack_tail(kind, d)

        by_half(c, j, arrived)

    def group_arrived(kind, group):
        if group < 2:
            edge_part(kind, every, (slice(0, hold), slice(hold, last))[group], False, 0, group, 1).wait_recv()
        else:
            for d in OTHERS:
                def arrived(tail):
                    edge_part(kind, slot(d), last, tail, 0, 2 + slot(d), d).wait_recv()
                    if tail:
                        unpack_tail(kind, d)

                by_half(oc if d % 2 else c, last, arrived)

    def core_copy(l, b, stage):
        first, count = ((0, EARLY), (EARLY, SLABS - EARLY))[stage]
        return remote(grad.at[l, pl.ds(first, count), pl.ds((2 * b + 1) * cols, cols), :], core_recv.at[l, b, pl.ds(first, count)],
                      core_ss.at[l, stage], core_rs.at[l, stage], 1)

    def core_all(l, stage):
        part_of = core_recv.at[l, :, (slice(0, EARLY), slice(EARLY, SLABS))[stage]]
        return remote(part_of, part_of, core_ss.at[l, stage], core_rs.at[l, stage], 1)

    def seat(device):
        return lax.rem(device + dpn // 2, dpn)

    def in_stage(device, stage):
        early = (seat(device) + 1) * per <= EARLY
        return jnp.logical_not(early) if stage else early

    def dp_remote(src, dst, stage, l, i):
        return pltpu.make_async_remote_copy(src_ref=src, dst_ref=dst, send_sem=dp_ss.at[stage, l], recv_sem=dp_rs.at[stage, l],
                                            device_id={'dp': lax.rem(p + i, dpn)}, device_id_type=MESH)

    def spread_copy(l, i):
        return dp_remote(half.at[l, pl.ds(seat(lax.rem(p + i, dpn)) * per, per)], dp_recv.at[l, pl.ds((i - 1) * per, per)], 0, l, i)

    def dp_all(l, stage):
        most = (dpn - 1) * per
        part_of = (dp_recv.at[l], gathered.at[l, pl.ds(0, most)], w_recv.at[1, pl.ds(0, (dpn - 1) * piece)])[stage]
        return dp_remote(part_of, part_of, stage, l, 1)

    def cross_copy(l):
        return remote(cross_send.at[l], cross_recv.at[l], cross_ss.at[l], cross_rs.at[l], 2)

    def gather_copy(l, i, owner):
        return dp_remote(own_sum.at[l], gathered.at[l, pl.ds(seat(owner) * per, per)], 1, l, i)

    def part_copy(q):
        return remote(part.at[q], part_recv.at[q], p_ss.at[q], p_rs.at[q], 1)

    def load_nodes(raw, send, own):
        send[...] = jnp.zeros_like(send)
        send[0, :, :nodes] = raw[ox].astype(F32)
        send[1, :, :nodes] = raw[x].astype(F32)
        own[:cols, :] = send[1].astype(own.dtype)

    def load_edges(raw, send, own, kind):
        def put(j, lanes_j, val_of):
            for d in OTHERS:
                sample = x if d < 2 else ox
                send[slot(d), j] = val_of(sample, oc if d % 2 else c).astype(F32)
            own[:cols, lanes_j] = val_of(x, c)

        def chunk(j):
            put(j, at(j, EC), lambda s, h: raw[s, :, pl.ds(pl.multiple_of(h * eh + j * EC, D), EC)])
            for d in SEND_ORDER:
                edge_start(kind, j, d)

        loop(nch - 1, chunk)
        first = (nch - 1) * EC
        used = edges - eh - first
        last = pl.ds(first, EC)

        def tail(s, h):
            left = raw[s, :, pl.ds(first, EC)]
            right = beside([raw[s, :, pl.ds(eh + first, used)], jnp.zeros((cols, EC - used), BF)])
            return jnp.where(h == 0, left.astype(F32), right.astype(F32)).astype(BF)

        put(nch - 1, last, tail)
        for d in SEND_ORDER:
            edge_start(kind, nch - 1, d)

    def place_edges(raw, block, d, j):
        s = x if d < 2 else ox
        h = oc if d % 2 else c
        val = block.astype(BF)
        first = (nch - 1) * EC
        used = edges - eh - first

        @pl.when(jnp.logical_or(j < nch - 1, h == 0))
        def _():
            raw[s, :, pl.ds(pl.multiple_of(h * eh + j * EC, D), EC)] = val

        @pl.when(jnp.logical_and(j == nch - 1, h == 1))
        def _():
            raw[s, :, pl.ds(eh + first, used)] = val[:, :used]

    def scoped(e0, e1, ge, msg, v0, v1, v2, agg0, agg1, d_agg, scol, rcol, srow, rrow, iota, lanes, ew1, ew1t, ew2, ew2t, nw1, nw1t, nw2, nw2t, vecs):
        tables = (v0, v1, v2)
        aggs = (agg0, agg1)
        edges_in = (e0, e1)

        barrier = pltpu.get_barrier_semaphore()
        for d in OTHERS:
            pl.semaphore_signal(barrier, inc=1, device_id={'tp': peer[d]}, device_id_type=MESH)
        for copy in loads[:1] + loads[4:] + loads[1:4]:
            copy.start()
        loads[0].wait()
        with jax.named_scope('send_nodes'):
            load_nodes(node_raw, n_send, v0)
        ncop = node_copies(n_send, n_recv, 0)
        for copy in loads[4:]:
            copy.wait()
        q = cols
        w_send[:HEAD, :] = jnp.zeros((HEAD, D), F32)
        for k in THREE:
            w_send[k * layers:(k + 1) * layers, :cols] = evec_in[k]
            w_send[(3 + k) * layers:(4 + k) * layers, :cols] = nvec_in[k]
        for l in range(layers):
            w_send[packed(l, 0, 3), :] = ew1_in[pl.ds(l * 3 * q, 3 * q), :].astype(F32)
            w_send[packed(l, 3), :] = ew2_in[pl.ds(l * q, q), :].astype(F32)
            w_send[packed(l, 4, 2), :] = nw1_in[pl.ds(l * 2 * q, 2 * q), :].astype(F32)
            w_send[packed(l, 6), :] = nw2_in[pl.ds(l * q, q), :].astype(F32)
        with jax.named_scope('barrier'):
            @pl.when(t != LEADER)
            def _():
                pl.semaphore_wait(barrier, len(OTHERS))
                pl.semaphore_signal(ready, inc=1, device_id={'tp': LEADER}, device_id_type=MESH)

            @pl.when(t == LEADER)
            def _():
                pl.semaphore_wait(ready, len(OTHERS))
                for i in dp_others:
                    pl.semaphore_signal(barrier, inc=1, device_id={'dp': lax.rem(p + i, dpn)}, device_id_type=MESH)

        w_cross.start()
        w_pair.start()
        ncop[1].start()
        ncop[0].start()
        loads[1].wait()
        with jax.named_scope('send_edges'):
            load_edges(edge_raw, e_send, e0, EDGE_IN)
        loads[2].wait()
        load_nodes(gnode_raw, gn_send, d_part)
        gcop = node_copies(gn_send, gn_recv, 1)
        gcop[1].start()
        gcop[0].start()
        loads[3].wait()
        with jax.named_scope('send_grads'):
            load_edges(gedge_raw, g_send, ge, GRAD_IN)

        with jax.named_scope('dp_barrier'):
            @pl.when(t == LEADER)
            def _():
                pl.semaphore_wait(barrier, len(OTHERS) + dpn - 1)
                for d in OTHERS:
                    pl.semaphore_signal(ready, inc=1, device_id={'tp': peer[d]}, device_id_type=MESH)

            @pl.when(t != LEADER)
            def _():
                pl.semaphore_wait(ready, 1)

        w_cross.wait_recv()
        for i in dp_others:
            weight_copy(i, p).start()

        @pl.when(c == 1)
        def _():
            for recv in (e_recv, g_recv):
                recv[:, last, :, D:] = jnp.zeros((len(OTHERS), cols, EC - D), F32)

        iota[...] = lax.broadcasted_iota(jnp.int32, (T, D), 0).astype(I16)
        lanes[...] = lax.broadcasted_iota(jnp.int32, (16, D), 1).astype(I16)

        ids_raw[...] = jnp.full(ids_raw.shape, -1, jnp.int32)
        for which, src in enumerate((send_ids, recv_ids)):
            ids_raw[which:which + 1, :edges] = src[...].reshape(1, edges)

        def ids(b):
            for which, (row_ref, col_ref) in enumerate(((srow, scol), (rrow, rcol))):
                wide = jnp.broadcast_to(ids_raw[which:which + 1, pl.ds(pl.multiple_of(c * eh + b * D, D), D)], (D, D))
                row_ref[at(b, 16), :] = wide[:16].astype(I16)
                col_ref[at(b, D), :] = flip(wide.astype(F32)).astype(jnp.int32).astype(I16)

        with jax.named_scope('ids'):
            loop(eh // D, ids)

        def keys(ref, step):
            return [ref[pl.ds(pl.multiple_of(step * (KS // D) * 16 + 16 * h, 16), 1), :] for h in range(KS // D)]

        bias_cols[...] = flip(stacked([eb1_in[...], nb1_in[...], jnp.zeros((D - 2 * layers, D), F32)]))

        def join_weights(l):
            for d in range(GROUP):
                src = w_recv.at[slot(d)] if d else w_send
                r = rows_of(d)
                for k in THREE:
                    ew1[l, pl.ds(k * D + d * q, q), :] = src[packed(l, k), :].astype(BF)
                ew2t[l, r, :] = src[packed(l, 3), :].astype(BF)
                for k in BOTH:
                    nw1[l, pl.ds(k * D + d * q, q), :] = src[packed(l, 4 + k), :].astype(BF)
                nw2t[l, r, :] = src[packed(l, 6), :].astype(BF)

            def flip_bf(mat):
                return flip(mat.astype(F32)).astype(BF)

            for k in THREE:
                ew1t[l, :, mat(k)] = flip_bf(ew1[l, mat(k), :])
            for k in BOTH:
                nw1t[l, :, mat(k)] = flip_bf(nw1[l, mat(k), :])
            ew2[l] = flip_bf(ew2t[l])
            nw2[l] = flip_bf(nw2t[l])

        def wait_recvs(copies):
            copies[1].wait_recv()
            copies[2].start()
            copies[0].wait_recv()
            copies[2].wait_recv()

        with jax.named_scope('node_wait'):
            wait_recvs(ncop)
        for d in OTHERS:
            v0[rows_of(d), :] = n_recv[slot(d)].astype(BF)
        with jax.named_scope('weight_wait'):
            dp_all(0, 2).wait_recv()
            w_relay.start()
            w_pair.wait_recv()
            w_relay.wait_recv()
        rows_all = beside([w_send[:HEAD, :cols]] + [w_recv[d, :HEAD, :cols] for d in range(3)])
        vecs[...] = flip(stacked([rows_all, jnp.zeros((D - HEAD, D), F32)]))
        join_weights(0)

        def vec(l, node):
            first = 6 * node + l
            return [vecs[:, first + 2 * k:first + 2 * k + 1] for k in THREE]

        def bias(l, node):
            return bias_cols[:, node * layers + l:node * layers + l + 1]

        def hidden_of_nodes(l):
            table, b1 = tables[l], bias(l, 0)

            def body(step):
                xs = gather(table, keys(srow, step), iota).astype(BF)
                xr = gather(table, keys(rrow, step), iota).astype(BF)
                hidden[l, :, at(step, KS)] = dot(ew1t[l, :, mat(1, 2)], stacked([xs, xr])) + b1

            loop(eh // KS, body)

        def edge_forward(l):
            e_in = edges_in[l]

            def body(j):
                for sub in range(EC // T):
                    a = at(j * (EC // T) + sub, T)
                    if l == 0:
                        if sub == 0:
                            chunk_arrived(EDGE_IN, j)
                        for d in OTHERS:
                            e_in[rows_of(d), a] = e_recv[slot(d), j, :, sub * T:(sub + 1) * T].astype(BF)
                    e_val = e_in[:, a]
                    hid = hidden[l, :, a] + dot(ew1t[l, :, mat(0)], e_val)
                    hidden[l, :, a] = hid
                    message, nrm, std = mlp_tail(hid, ew2t[l], vec(l, 0))
                    normed[l, :, a] = nrm
                    inv[l:l + 1, a] = std
                    msg[:, a] = message
                    e_new = (e_val.astype(F32) + message.astype(F32)).astype(BF)
                    if l < top:
                        edges_in[l + 1][:, a] = e_new
                    else:
                        for d in OTHERS:
                            e_send[slot(d), j, :, sub * T:(sub + 1) * T] = e_new[rows_of(d)].astype(F32)
                        if sub == 0:
                            own_parts = []
                        own_parts.append(e_new[:q])
                if l == top:
                    for d in SEND_ORDER:
                        edge_start(EDGE_OUT, j, d)
                    place_edges(edge_raw, beside(own_parts), 0, j)

            loop(nch, body)

        def segment_sum(acc, ids_ref):
            acc[...] = jnp.zeros(acc.shape, F32)

            def body(step):
                scatter(acc, msg[:, at(step, KS)], ids_ref[at(step, KS), :], lanes)

            loop(eh // KS, body)

        def node_forward(l):
            table, agg, out = tables[l], aggs[l], tables[l + 1]

            def body(step):
                a = pl.ds(pl.multiple_of(step * TN, D), TN)
                v_in = table[:, a]
                agg_bf = (part[l, :, a] + swap_halves(part_recv[l, :, a])).astype(BF)
                agg[:, a] = agg_bf
                hid = dot(nw1t[l], stacked([v_in, agg_bf])) + bias(l, 1)
                nhid[l, :, a] = hid
                message, nrm, std = mlp_tail(hid, nw2t[l], vec(l, 1))
                nnrm[l, :, a] = nrm
                ninv[l:l + 1, a] = std
                out[:, a] = (v_in.astype(F32) + message.astype(F32)).astype(BF)

            loop(npad // TN, body)

        for l in range(layers):
            with jax.named_scope(f'gather_{l}'):
                hidden_of_nodes(l)
            if l == top:
                edges_sent(EDGE_IN)
            with jax.named_scope(f'edge_forward_{l}'):
                edge_forward(l)
            with jax.named_scope(f'sum_{l}'):
                segment_sum(part.at[l], rcol)
            part_copy(l).start()
            if l == 0:
                join_weights(1)
                gcop[1].wait_recv()
                gcop[2].start()
            with jax.named_scope(f'part_wait_{l}'):
                part_copy(l).wait_recv()
            with jax.named_scope(f'node_forward_{l}'):
                node_forward(l)
        no_send[...] = tables[layers][rows_of(2), :].astype(F32)
        no_copy = remote(no_send, no_recv, n_ss.at[2, 0], n_rs.at[2, 0], 2)
        no_copy.start()
        node_raw[x] = tables[layers][:q, :nodes]

        grad[...] = jnp.zeros_like(grad)
        sums[...] = jnp.zeros_like(sums)
        with jax.named_scope('grad_node_wait'):
            gcop[0].wait_recv()
            gcop[2].wait_recv()
        for d in OTHERS:
            d_part[rows_of(d), :] = gn_recv[slot(d)]

        def node_backward(l):
            table, agg = tables[l], aggs[l]

            def body(step):
                a = pl.ds(pl.multiple_of(step * TN, D), TN)
                d_in = d_part[:, a]
                if l < top:
                    d_in = d_in + part[layers + l + 1, :, a] + swap_halves(part_recv[layers + l + 1, :, a])
                    d_in = d_in.astype(BF).astype(F32)
                d_hid, d_w2, parts = mlp_back(d_in, nhid[l, :, a], nnrm[l, :, a], ninv[l:l + 1, a], nw2[l], vec(l, 1))
                add_sums(sums.at[l, 1], [parts])
                grad[l, 4] += d_w2
                grad[l, 2] += dot_nt(table[:, a], d_hid)
                grad[l, 3] += dot_nt(agg[:, a], d_hid)
                d_part[:, a] = d_in + dot(nw1[l, mat(0), :], d_hid)
                d_agg[:, a] = dot(nw1[l, mat(1), :], d_hid).astype(BF)

            loop(npad // TN, body)

        def gather_back():
            def body(step):
                msg[:, at(step, KS)] = gather(d_agg, keys(rrow, step), iota).astype(BF)

            loop(eh // KS, body)

        def edge_backward(l):
            e_in = edges_in[l]

            def body(j):
                all_parts, d_w2s, d_w1s, own_parts = [], [], [], []
                for sub in range(EC // T):
                    a = at(j * (EC // T) + sub, T)
                    if l == top:
                        if sub == 0:
                            chunk_arrived(GRAD_IN, j)
                        for d in OTHERS:
                            ge[rows_of(d), a] = g_recv[slot(d), j, :, sub * T:(sub + 1) * T].astype(BF)
                    d_res = ge[:, a].astype(F32)
                    d_msg = d_res + msg[:, a].astype(F32)
                    d_hid, d_w2, parts = mlp_back(d_msg, hidden[l, :, a], normed[l, :, a], inv[l:l + 1, a], ew2[l], vec(l, 0))
                    all_parts.append(parts)
                    d_w2s.append(d_w2)
                    d_w1s.append(dot_nt(e_in[:, a], d_hid))
                    msg[:, a] = d_hid
                    d_new = (d_res + dot(ew1[l, mat(0), :], d_hid)).astype(BF)
                    if l > 0:
                        ge[:, a] = d_new
                    else:
                        for d in OTHERS:
                            g_send[slot(d), j, :, sub * T:(sub + 1) * T] = d_new[rows_of(d)].astype(F32)
                        own_parts.append(d_new[:q])
                add_sums(sums.at[l, 0], all_parts)
                grad[l, 1] += sum(d_w2s[1:], d_w2s[0])
                grad[l, 0] += sum(d_w1s[1:], d_w1s[0])
                if l == 0:
                    @pl.when(j < hold)
                    def _():
                        for d in SEND_ORDER:
                            edge_start(GRAD_OUT, j, d)
                    place_edges(gedge_raw, beside(own_parts), 0, j)

            loop(nch, body)

        def vector_slab(l):
            def total(node, k):
                return column_sum(flip(sums[l, node, mat(k), :]))

            lat = stacked([total(node, k) for node in BOTH for k in THREE])
            biases = stacked([total(node, 3) for node in BOTH])
            n_lat = lat.shape[0]
            for d in range(GROUP):
                grad[l, VEC_SLAB, d * cols:d * cols + n_lat, :cols] = lat[:, rows_of(d)]
                grad[l, VEC_SLAB, d * cols + n_lat:d * cols + n_lat + 2, :] = biases

        def reduce_start(l, stage):
            for b in BOTH:
                core_copy(l, b, stage).start()

        def chip_sum(l, stage):
            row = lax.broadcasted_iota(jnp.int32, (cols, D), 0)
            edge_row = jnp.logical_or(row < 3, row == 6)
            core_all(l, stage).wait_recv()
            for b in BOTH:
                for k in range(SLABS)[STAGES[stage]]:
                    own = grad[l, k, rows_of(2 * b), :]
                    if k in EDGE_SLABS:
                        own = own + core_recv[l, b, k]
                    elif k == VEC_SLAB:
                        own = own + jnp.where(edge_row, core_recv[l, b, k], 0.0)
                    half[l, k, b] = own
            for i in dp_others:
                @pl.when(in_stage(lax.rem(p + i, dpn), stage))
                def _():
                    spread_copy(l, i).start()

        def dp_sum(l, stage):
            @pl.when(in_stage(p, stage))
            def _():
                total = half[l, pl.ds(seat(p) * per, per)]
                dp_all(l, 0).wait_recv()
                for i in dp_others:
                    total = total + dp_recv[l, pl.ds((i - 1) * per, per)]
                own_sum[l] = total[:, 0]
                cross_send[l] = total[:, 1]
                cross_copy(l).start()

        def cross_sum(l):
            cross_copy(l).wait_recv()
            total = own_sum[l] + cross_recv[l]
            own_sum[l] = total
            gathered[l, pl.ds(seat(p) * per, per)] = total
            for i in dp_others:
                gather_copy(l, i, p).start()

        def project(l):
            table = tables[l]

            def body(step):
                a = pl.ds(pl.multiple_of(step * TN, D), TN)
                s_bf, r_bf, v_in = s_sum[:, a].astype(BF), r_sum[:, a].astype(BF), table[:, a]
                part[layers + l, :, a] = dot(ew1[l, mat(1), :], s_bf) + dot(ew1[l, mat(2), :], r_bf)
                grad[l, 6] += dot_nt(v_in, s_bf)
                grad[l, 7] += dot_nt(v_in, r_bf)

            loop(npad // TN, body)

        for l in reversed(range(layers)):
            first_layer = l == 0
            with jax.named_scope(f'node_backward_{l}'):
                node_backward(l)
            if first_layer:
                with jax.named_scope('chip_sum_1'):
                    chip_sum(1, 0)
                    chip_sum(1, 1)
            with jax.named_scope(f'gather_back_{l}'):
                gather_back()
            if first_layer:
                edges_sent(GRAD_IN)
            with jax.named_scope(f'edge_backward_{l}'):
                edge_backward(l)
            vector_slab(l)
            reduce_start(l, 0)
            if first_layer:
                with jax.named_scope('dp_sum_1'):
                    dp_sum(1, 0)
                    dp_sum(1, 1)
            with jax.named_scope(f'sum_send_{l}'):
                segment_sum(s_sum, scol)
            if first_layer:
                with jax.named_scope('chip_sum_0'):
                    chip_sum(0, 0)
            with jax.named_scope(f'sum_recv_{l}'):
                segment_sum(r_sum, rcol)
            with jax.named_scope(f'project_{l}'):
                project(l)
            reduce_start(l, 1)
            part_copy(layers + l).start()
            if first_layer:
                with jax.named_scope('chip_sum_late'):
                    chip_sum(0, 1)
                with jax.named_scope('dp_sum_0'):
                    dp_sum(0, 0)
            with jax.named_scope(f'back_wait_{l}'):
                part_copy(layers + l).wait_recv()

        def final(step):
            a = pl.ds(pl.multiple_of(step * TN, D), TN)
            d_in = (d_part[:, a] + part[layers, :, a] + swap_halves(part_recv[layers, :, a])).astype(BF)
            v2[:, a] = d_in

        loop(npad // TN, final)
        gnode_raw[x] = v2[:q, :nodes]
        with jax.named_scope('dp_sum_late'):
            dp_sum(0, 1)

        dn_send[...] = v2[rows_of(2), :].astype(F32)
        dn_copy = remote(dn_send, dn_recv, n_ss.at[2, 1], n_rs.at[2, 1], 2)
        dn_copy.start()

        def send_rest(j):
            for d in SEND_ORDER:
                edge_start(GRAD_OUT, j, d)

        loop(nch, send_rest, hold)

        with jax.named_scope('node_out_wait'):
            no_copy.wait_recv()
        node_raw[ox] = no_recv[:, :nodes].astype(BF)

        def place_e(j):
            for d in OTHERS:
                place_edges(edge_raw, eo_recv[slot(d), j], d, j)

        with jax.named_scope('place_edge_out'):
            for group in THREE:
                group_arrived(EDGE_OUT, group)
            loop(nch, place_e)

        def place_g(j):
            for d in OTHERS:
                place_edges(gedge_raw, de_recv[slot(d), j], d, j)

        with jax.named_scope('place_first'):
            group_arrived(GRAD_OUT, 0)
            loop(hold, place_g)
        for l in range(layers):
            with jax.named_scope(f'cross_sum_{l}'):
                cross_sum(l)
        with jax.named_scope('d_node_wait'):
            dn_copy.wait_recv()
        gnode_raw[ox] = dn_recv[:, :nodes].astype(BF)
        with jax.named_scope('place_rest'):
            group_arrived(GRAD_OUT, 1)
            loop(last, place_g, hold)
        for l in range(layers):
            dp_all(l, 1).wait_recv()
            ew1_buf[l, 0] = gathered[l, 0]
            ew1_buf[l, 1:] = gathered[l, EARLY:]
            ew2_buf[l] = gathered[l, 1]
            nw1_buf[l] = gathered[l, 2:4]
            nw2_buf[l] = gathered[l, 4]
            small = gathered[l, VEC_SLAB]
            for k in THREE:
                evec_buf[k, l:l + 1, :] = small[k:k + 1, :cols]
                nvec_buf[k, l:l + 1, :] = small[3 + k:4 + k, :cols]
            eb1_buf[l:l + 1, :] = small[6:7]
            nb1_buf[l:l + 1, :] = small[7:8]
        for l in range(layers):
            for stage in BOTH:
                core_all(l, stage).wait_send()
            cross_copy(l).wait_send()
            dp_all(l, 0).wait_send()
            dp_all(l, 1).wait_send()
        for copy in ncop + gcop + (w_pair, w_cross, w_relay):
            copy.wait_send()
        dp_all(0, 2).wait_send()
        no_copy.wait_send()
        dn_copy.wait_send()
        for k in range(2 * layers):
            part_copy(k).wait_send()
        edges_sent(EDGE_OUT)
        with jax.named_scope('place_last'):
            group_arrived(GRAD_OUT, 2)
            loop(nch, place_g, last)
        edges_sent(GRAD_OUT)

    bf = lambda *s: pltpu.VMEM(s, BF)
    pl.run_scoped(
        scoped, bf(D, eh), bf(D, eh), bf(D, eh), bf(D, eh), bf(D, npad), bf(D, npad), bf(D, npad), bf(D, npad), bf(D, npad), bf(D, npad),
        pltpu.VMEM((eh, D), I16), pltpu.VMEM((eh, D), I16), pltpu.VMEM((eh // D * 16, D), I16), pltpu.VMEM((eh // D * 16, D), I16),
        pltpu.VMEM((T, D), I16), pltpu.VMEM((16, D), I16),
        bf(layers, 3 * D, D), bf(layers, D, 3 * D), bf(layers, D, D), bf(layers, D, D),
        bf(layers, 2 * D, D), bf(layers, D, 2 * D), bf(layers, D, D), bf(layers, D, D), pltpu.VMEM((D, D), F32))


def finish_moves(src, dst):
    if len(src.shape) != 3 or src.dtype != BF:
        return [(src, dst)]
    return [(src.at[s, pl.ds(r, 8)], dst.at[s, pl.ds(r, 8)]) for s in range(src.shape[0]) for r in range(0, src.shape[1], 8)]


def finish_kernel(*refs):
    count = len(refs) // 2
    moves = sum((finish_moves(refs[k], refs[count + k]) for k in range(count)), [])
    puts = [pltpu.make_async_copy(src, dst, refs[-1]) for src, dst in moves]
    for put in puts:
        put.start()
    for put in puts:
        put.wait()


def keep_in_vmem(val):
    return pltpu.with_memory_space_constraint(val, pltpu.VMEM)


def finish(arrays):
    return pl.pallas_call(
        finish_kernel,
        name='finish',
        out_shape=[jax.ShapeDtypeStruct(a.shape, a.dtype) for a in arrays],
        in_specs=[VM] * len(arrays),
        out_specs=[HB] * len(arrays),
        scratch_shapes=[pltpu.SemaphoreType.DMA],
        compiler_params=pltpu.CompilerParams(vmem_limit_bytes=1 << 20),
    )(*[keep_in_vmem(a) for a in arrays])


def solution(mesh):
    lat_spec = P('dp', None, 'tp')
    first_spec = P(None, None, 'tp', None)
    col_spec = P(None, None, 'tp')
    param_specs = (first_spec, P(), col_spec, col_spec, first_spec, P(), col_spec, col_spec)
    in_specs = (lat_spec, lat_spec, P(), P(), lat_spec, lat_spec) + param_specs
    out_specs = (lat_spec, lat_spec, lat_spec, lat_spec) + param_specs
    shape = jax.ShapeDtypeStruct

    def local_step(node_lat, edge_lat, senders, receivers, grad_node, grad_edge, edge_w1, edge_b1, edge_w2, edge_vec, node_w1, node_b1, node_w2, node_vec):
        layers = edge_w1.shape[0]
        cols = node_lat.shape[2]
        nodes, edges = node_lat.shape[1], edge_lat.shape[1]
        npad = -(-nodes // TN) * TN
        eh = -(-edges // (2 * EC)) * EC
        nch = eh // EC
        dpn = mesh.shape['dp']
        per = SLABS // dpn
        dims = (layers, cols, nodes, edges, npad, eh, dpn)
        flat = lambda arr: jnp.swapaxes(arr, 1, 2)
        lead = lambda arr: jnp.transpose(arr, (1, 0, 2))
        args = (flat(node_lat), flat(edge_lat), flat(grad_node), flat(grad_edge), senders, receivers,
                edge_w1.reshape(-1, D), flat(edge_w2).reshape(-1, D), node_w1.reshape(-1, D), flat(node_w2).reshape(-1, D),
                lead(edge_vec), lead(node_vec), edge_b1, node_b1)
        vm, sem = pltpu.VMEM, pltpu.SemaphoreType.DMA
        wrows = -(-(HEAD + layers * LROWS) // (8 * dpn)) * 8 * dpn
        lat_n, lat_e = (2, cols, nodes), (2, cols, edges)
        outs = [RESULT(lat_n, BF), RESULT(lat_e, BF), RESULT(lat_n, BF), RESULT(lat_e, BF),
                RESULT((layers, 3, cols, D), F32), RESULT((layers, D), F32), RESULT((layers, cols, D), F32), RESULT((3, layers, cols), F32),
                RESULT((layers, 2, cols, D), F32), RESULT((layers, D), F32), RESULT((layers, cols, D), F32), RESULT((3, layers, cols), F32)]
        scratch = [
            *[vm(a.shape, a.dtype) for a in args[4:]], vm((wrows, D), F32), vm((3, wrows, D), F32),
            vm((2, cols, npad), F32), vm((3, cols, npad), F32), vm((2, cols, npad), F32), vm((3, cols, npad), F32),
            vm((cols, npad), F32), vm((cols, npad), F32), vm((cols, npad), F32), vm((cols, npad), F32),
            vm((2, 3, cols + cols // GROUP, D), F32), vm((4, 3, cols + cols // GROUP, D), F32), *[vm((3, nch, cols, EC), F32)] * 6,
            vm((2 * layers, D, npad), F32), vm((2 * layers, D, npad), F32),
            vm((layers, D, eh), F32), vm((layers, D, eh), F32), vm((layers, eh), F32),
            vm((layers, D, npad), F32), vm((layers, D, npad), F32), vm((layers, npad), F32),
            vm((D, npad), F32), vm((D, npad), F32), vm((D, npad), F32), vm((2, 2 * eh), jnp.int32), vm((D, D), F32), vm((layers, 2, 4 * D, D), F32),
            vm((layers, SLABS, D, D), F32), vm((layers, 2, SLABS, cols, D), F32), vm((layers, SLABS, 2, cols, D), F32),
            vm((layers, (dpn - 1) * per, 2, cols, D), F32), vm((layers, per, cols, D), F32), vm((layers, per, cols, D), F32),
            vm((layers, per, cols, D), F32), vm((layers, SLABS, cols, D), F32),]
        own_sems = [
            sem((layers, 2)), sem((3, layers)), sem((layers,)), sem((3,)), sem((3, 3)), sem((2, nch)), sem((2, 5)), sem((2 * layers,)),
            pltpu.SemaphoreType.REGULAR,
            sem((len(args),)), sem((3,)), sem((3, 3)), sem((4, 4)), sem((2 * layers,)), sem((layers, 2)), sem((3, layers)), sem((layers,))]
        res = pl.pallas_call(
            lambda *refs: pl.run_scoped(lambda *own: step_kernel(dims, *refs, *own), *own_sems),
            name='graph_step',
            out_shape=outs,
            in_specs=[HB] * len(args),
            out_specs=[VM] * len(outs),
            scratch_shapes=scratch,
            compiler_params=pltpu.CompilerParams(collective_id=0, has_side_effects=True, vmem_limit_bytes=VMEM_LIMIT),
        )(*args)

        res = finish(res)
        return (flat(res[0]), flat(res[1]), flat(res[2]), flat(res[3]),
                res[4], res[5], flat(res[6]), lead(res[7]), res[8], res[9], flat(res[10]), lead(res[11]))

    return jax.shard_map(local_step, mesh=mesh, in_specs=in_specs, out_specs=out_specs, check_vma=False)
```

```python
import jax
import jax.numpy as jnp
from jax import lax
from jax.experimental import pallas as pl
from jax.experimental.pallas import tpu as pltpu
from jax.sharding import PartitionSpec as P

LN_EPS = 1e-5
D = 128
T = 256
TN = 384
EC = 512
KS = 1408
BF = jnp.bfloat16
F32 = jnp.float32
I16 = jnp.int16
MESH = pl.DeviceIdType.MESH
VM = pl.BlockSpec(memory_space=pltpu.VMEM)
HB = pl.BlockSpec(memory_space=pl.ANY)
RESULT = pltpu.VMEM
GROUP = 4
BOTH = (0, 1)
THREE = (0, 1, 2)
OTHERS = (1, 2, 3)
EDGE_IN, GRAD_IN, EDGE_OUT, GRAD_OUT = range(4)
SEND_ORDER = (2, 3, 1)
LROWS = 7 * (D // 4)
HEAD = 16
LEADER = GROUP - 1
HELPER = LEADER - 1
VMEM_LIMIT = 63_000_000
SLABS = 8
EARLY = 6
VEC_SLAB = 5
EDGE_SLABS = (0, 1, 6, 7)
STAGES = (slice(0, EARLY), slice(EARLY, SLABS))


def dot(a, b):
    return jnp.dot(a, b, preferred_element_type=F32)


def dot_nt(a, b):
    return lax.dot_general(a, b, (((1,), (1,)), ((), ())), preferred_element_type=F32)


def mat(k, n=1):
    return slice(k * D, (k + n) * D)


def rows_of(d):
    q = D // 4
    return slice(d * q, (d + 1) * q)


def at(step, width):
    return pl.ds(pl.multiple_of(step * width, width), width)


def loop(stop, body, start=0):
    def step(j, carry):
        body(j)
        return carry

    lax.fori_loop(start, stop, step, 0)


def column_sum(val):
    return jnp.sum(val, axis=0, keepdims=True)


def flip(val):
    return jnp.swapaxes(val, 0, 1)


def stacked(parts):
    return jnp.concatenate(parts, axis=0)


def beside(parts):
    return jnp.concatenate(parts, axis=1)


def slot(d):
    return d - 1


def sigmoid(hidden):
    return 1.0 / (1.0 + jnp.exp(-hidden))


def fold(val):
    total = val[:, mat(0)]
    for start in range(D, val.shape[1], D):
        total = total + val[:, start:start + D]
    return total


def swap_halves(val):
    return stacked([val[rows_of(d)] for d in (1, 0, 3, 2)])


def gather(table, keys, iota):
    acc = None
    nodes = table.shape[1]
    one, zero = jnp.ones((), BF), jnp.zeros((), BF)
    for base in range(0, nodes, T):
        width = min(T, nodes - base)
        ids = iota[0:width, :]
        hot = beside([jnp.where(ids == (key - jnp.asarray(base, I16)), one, zero) for key in keys])
        part = dot(table[:, base:base + width], hot)
        acc = part if acc is None else acc + part
    return acc


def scatter(acc_ref, val, cols, lanes):
    nodes = acc_ref.shape[1]
    one, zero = jnp.ones((), BF), jnp.zeros((), BF)
    row = lanes[0:1, :]
    for base in range(0, nodes, T):
        width = min(T, nodes - base)
        hot = beside([jnp.where((row + jnp.asarray(base + s, I16)) == cols, one, zero) for s in range(0, width, D)])
        acc_ref[:, base:base + width] += dot(val, hot)


def mlp_tail(hidden, w2t, vec):
    act = (hidden * sigmoid(hidden)).astype(BF)
    out = dot(w2t, act) + vec[0]
    mean = column_sum(out) / D
    centered = out - mean
    var = column_sum(centered * centered) / D
    inv = lax.rsqrt(var + LN_EPS)
    normed = centered * inv
    message = (normed * vec[1] + vec[2]).astype(BF)
    return message, normed, inv


def mlp_back(d_msg, hidden, normed, inv, w2, vec):
    d_normed = d_msg * vec[1]
    mean0 = column_sum(d_normed) / D
    mean1 = column_sum(d_normed * normed) / D
    d_out = inv * (d_normed - mean0 - normed * mean1)
    d_out_bf = d_out.astype(BF)
    sig = sigmoid(hidden)
    act = (hidden * sig).astype(BF)
    d_w2 = dot_nt(d_out_bf, act)
    d_hidden = dot(w2, d_out_bf) * (sig * (1.0 + hidden * (1.0 - sig)))
    sums = (fold(d_out), fold(d_msg * normed), fold(d_msg), fold(d_hidden))
    return d_hidden.astype(BF), d_w2, sums


def add_sums(ref, parts):
    for q in range(4):
        total = parts[0][q]
        for other in parts[1:]:
            total = total + other[q]
        ref[mat(q), :] += total


def step_kernel(dims, *refs):
    layers, cols, nodes, edges, npad, eh, dpn = dims
    nch = eh // EC
    top = layers - 1
    n_in = 14
    hbm_in = refs[:n_in]
    n_out = 12
    (node_raw, edge_raw, gnode_raw, gedge_raw, ew1_buf, eb1_buf, ew2_buf, evec_buf, nw1_buf, nb1_buf, nw2_buf, nvec_buf) = refs[n_in:n_in + n_out]
    (send_ids, recv_ids, ew1_in, ew2_in, nw1_in, nw2_in, evec_in, nvec_in, eb1_in, nb1_in, w_send, w_recv, n_send, n_recv, gn_send, gn_recv, no_send, no_recv, dn_send, dn_recv,
     t_send, t_recv, e_send, g_send, e_recv, g_recv, eo_recv, de_recv, part, part_recv, hidden, normed, inv, nhid, nnrm, ninv, d_part, s_sum, r_sum,
     ids_raw, bias_cols, sums, grad, core_recv, half, dp_recv, cross_send, cross_recv, own_sum, gathered,
     core_rs, dp_rs, cross_rs, w_rs, n_rs, e_rs, o_rs, p_rs, ready, load_sem, w_ss, n_ss, e_ss, p_ss, core_ss, dp_ss, cross_ss) = refs[n_in + n_out:]

    t = lax.axis_index('tp')
    p = lax.axis_index('dp')
    per = SLABS // dpn
    dp_others = range(1, dpn)
    x, c = t // 2, lax.rem(t, 2)
    ox, oc = 1 - x, 1 - c
    peer = [t, t + 1 - 2 * c, t + 2 - 4 * x, t + 3 - 2 * c - 4 * x]

    def remote(src, dst, ssem, rsem, d):
        return pltpu.make_async_remote_copy(src_ref=src, dst_ref=dst, send_sem=ssem, recv_sem=rsem,
                                            device_id={'tp': peer[d]}, device_id_type=MESH)

    small_in = (send_ids, recv_ids, ew1_in, ew2_in, nw1_in, nw2_in, evec_in, nvec_in, eb1_in, nb1_in)
    loads = [pltpu.make_async_copy(src, dst, load_sem.at[q]) for q, (src, dst) in enumerate(
        zip(hbm_in, (node_raw, edge_raw, gnode_raw, gedge_raw) + small_in))]

    def node_copies(send, recv, kind):
        return (remote(send.at[1], recv.at[0], n_ss.at[kind, 0], n_rs.at[kind, 0], 1),
                remote(send.at[0], recv.at[1], n_ss.at[kind, 1], n_rs.at[kind, 1], 2),
                remote(recv.at[1], recv.at[2], n_ss.at[kind, 2], n_rs.at[kind, 2], 1))

    piece = w_send.shape[0] // dpn

    def packed(l, k, count=1):
        return pl.ds(HEAD + l * LROWS + k * cols, count * cols)

    def weight_rows(owner):
        return pl.ds(pl.multiple_of(owner * piece, 8), piece)

    w_pair = remote(w_send, w_recv.at[0], w_ss.at[0], w_rs.at[0], 1)
    w_cross = remote(w_send.at[weight_rows(p)], w_recv.at[1, weight_rows(p)], w_ss.at[1], w_rs.at[1], 2)
    w_relay = remote(w_recv.at[1], w_recv.at[2], w_ss.at[2], w_rs.at[2], 1)

    def weight_copy(i, owner):
        rows = w_recv.at[1, weight_rows(owner)]
        return dp_remote(rows, rows, 2, 0, i)

    last = nch - 1
    hold = nch - 3
    buffers = ((e_send, e_recv), (g_send, g_recv), (e_send, eo_recv), (g_send, de_recv))

    def outward(kind):
        return kind in (EDGE_OUT, GRAD_OUT)

    every = slice(None)
    ragged = pl.ds(D, D // GROUP)
    rest = [slice(g * cols // GROUP, (g + 1) * cols // GROUP) for g in range(GROUP)]

    def edge_part(kind, which, j, tail, send_sem, recv_sem, d):
        src, dst = buffers[kind]
        if tail:
            src, dst = t_send.at[kind % 2, which], t_recv.at[kind, which]
        else:
            src, dst = src.at[which, j], dst.at[which, j]
        recv_sems = o_rs.at[kind - EDGE_OUT, recv_sem] if outward(kind) else e_rs.at[kind, recv_sem]
        return remote(src, dst, e_ss.at[kind, send_sem], recv_sems, d)

    def by_half(half_id, j, action):
        narrow = jnp.logical_and(j == last, half_id == 1)

        @pl.when(jnp.logical_not(narrow))
        def _():
            action(False)

        @pl.when(narrow)
        def _():
            action(True)

    def pack_tail(kind, d):
        src, out = buffers[kind][0].at[slot(d), last], t_send.at[kind % 2, slot(d)]
        out[:cols, :] = src[:, :D]
        over = src[:, ragged]
        out[cols:, :] = beside([over[r] for r in rest])

    def unpack_tail(kind, d):
        src, out = t_recv.at[kind, slot(d)], buffers[kind][1].at[slot(d), last]
        out[:, :D] = src[:cols, :]
        over = src[cols:, :]
        out[:, ragged] = stacked([over[:, rows_of(g)] for g in range(GROUP)])

    def edge_start(kind, j, d):
        other = oc if d % 2 else c
        if outward(kind):
            send_sem, recv_sem = jnp.where(j == last, 1, 0), jnp.where(j == last, 2 + slot(d), jnp.where(j < hold, 0, 1))
        else:
            send_sem, recv_sem = jnp.where(j == last, d, 0), j

        def start(tail):
            if tail:
                pack_tail(kind, d)
            edge_part(kind, slot(d), j, tail, send_sem, recv_sem, d).start()

        by_half(c if outward(kind) else other, j, start)

    def edges_sent(kind):
        edge_part(kind, every, slice(0, last), False, 0, 0, 1).wait_send()
        if outward(kind):
            by_half(c, last, lambda tail: edge_part(kind, every, last, tail, 1, 0, 1).wait_send())
        else:
            for d in OTHERS:
                by_half(oc if d % 2 else c, last, lambda tail: edge_part(kind, slot(d), last, tail, d, 0, d).wait_send())

    def chunk_arrived(kind, j):
        def arrived(tail):
            edge_part(kind, every, j, tail, 0, j, 1).wait_recv()
            if tail:
                for d in OTHERS:
                    unpack_tail(kind, d)

        by_half(c, j, arrived)

    def group_arrived(kind, group):
        if group < 2:
            edge_part(kind, every, (slice(0, hold), slice(hold, last))[group], False, 0, group, 1).wait_recv()
        else:
            for d in OTHERS:
                def arrived(tail):
                    edge_part(kind, slot(d), last, tail, 0, 2 + slot(d), d).wait_recv()
                    if tail:
                        unpack_tail(kind, d)

                by_half(oc if d % 2 else c, last, arrived)

    def core_copy(l, b, stage):
        first, count = ((0, EARLY), (EARLY, SLABS - EARLY))[stage]
        return remote(grad.at[l, pl.ds(first, count), pl.ds((2 * b + 1) * cols, cols), :], core_recv.at[l, b, pl.ds(first, count)],
                      core_ss.at[l, stage], core_rs.at[l, stage], 1)

    def core_all(l, stage):
        part_of = core_recv.at[l, :, (slice(0, EARLY), slice(EARLY, SLABS))[stage]]
        return remote(part_of, part_of, core_ss.at[l, stage], core_rs.at[l, stage], 1)

    def seat(device):
        return lax.rem(device + dpn // 2, dpn)

    def in_stage(device, stage):
        early = (seat(device) + 1) * per <= EARLY
        return jnp.logical_not(early) if stage else early

    def dp_remote(src, dst, stage, l, i):
        return pltpu.make_async_remote_copy(src_ref=src, dst_ref=dst, send_sem=dp_ss.at[stage, l], recv_sem=dp_rs.at[stage, l],
                                            device_id={'dp': lax.rem(p + i, dpn)}, device_id_type=MESH)

    def spread_copy(l, i):
        return dp_remote(half.at[l, pl.ds(seat(lax.rem(p + i, dpn)) * per, per)], dp_recv.at[l, pl.ds((i - 1) * per, per)], 0, l, i)

    def dp_all(l, stage):
        most = (dpn - 1) * per
        part_of = (dp_recv.at[l], gathered.at[l, pl.ds(0, most)], w_recv.at[1, pl.ds(0, (dpn - 1) * piece)])[stage]
        return dp_remote(part_of, part_of, stage, l, 1)

    def cross_copy(l):
        return remote(cross_send.at[l], cross_recv.at[l], cross_ss.at[l], cross_rs.at[l], 2)

    def gather_copy(l, i, owner):
        return dp_remote(own_sum.at[l], gathered.at[l, pl.ds(seat(owner) * per, per)], 1, l, i)

    def part_copy(q):
        return remote(part.at[q], part_recv.at[q], p_ss.at[q], p_rs.at[q], 1)

    def load_nodes(raw, send, own):
        send[...] = jnp.zeros_like(send)
        send[0, :, :nodes] = raw[ox].astype(F32)
        send[1, :, :nodes] = raw[x].astype(F32)
        own[:cols, :] = send[1].astype(own.dtype)

    def load_edges(raw, send, own, kind):
        def put(j, lanes_j, val_of):
            for d in OTHERS:
                sample = x if d < 2 else ox
                send[slot(d), j] = val_of(sample, oc if d % 2 else c).astype(F32)
            own[:cols, lanes_j] = val_of(x, c)

        def chunk(j):
            put(j, at(j, EC), lambda s, h: raw[s, :, pl.ds(pl.multiple_of(h * eh + j * EC, D), EC)])
            for d in SEND_ORDER:
                edge_start(kind, j, d)

        loop(nch - 1, chunk)
        first = (nch - 1) * EC
        used = edges - eh - first
        last = pl.ds(first, EC)

        def tail(s, h):
            left = raw[s, :, pl.ds(first, EC)]
            right = beside([raw[s, :, pl.ds(eh + first, used)], jnp.zeros((cols, EC - used), BF)])
            return jnp.where(h == 0, left.astype(F32), right.astype(F32)).astype(BF)

        put(nch - 1, last, tail)
        for d in SEND_ORDER:
            edge_start(kind, nch - 1, d)

    def place_edges(raw, block, d, j):
        s = x if d < 2 else ox
        h = oc if d % 2 else c
        val = block.astype(BF)
        first = (nch - 1) * EC
        used = edges - eh - first

        @pl.when(jnp.logical_or(j < nch - 1, h == 0))
        def _():
            raw[s, :, pl.ds(pl.multiple_of(h * eh + j * EC, D), EC)] = val

        @pl.when(jnp.logical_and(j == nch - 1, h == 1))
        def _():
            raw[s, :, pl.ds(eh + first, used)] = val[:, :used]

    def scoped(e0, e1, ge, msg, v0, v1, v2, agg0, agg1, d_agg, scol, rcol, srow, rrow, iota, lanes, ew1, ew1t, ew2, ew2t, nw1, nw1t, nw2, nw2t, vecs):
        tables = (v0, v1, v2)
        aggs = (agg0, agg1)
        edges_in = (e0, e1)

        barrier = pltpu.get_barrier_semaphore()
        for d in OTHERS:
            pl.semaphore_signal(barrier, inc=1, device_id={'tp': peer[d]}, device_id_type=MESH)
        for copy in loads[:1] + loads[4:] + loads[1:4]:
            copy.start()
        loads[0].wait()
        with jax.named_scope('send_nodes'):
            load_nodes(node_raw, n_send, v0)
        ncop = node_copies(n_send, n_recv, 0)
        for copy in loads[4:]:
            copy.wait()
        q = cols
        w_send[:HEAD, :] = jnp.zeros((HEAD, D), F32)
        for k in THREE:
            w_send[k * layers:(k + 1) * layers, :cols] = evec_in[k]
            w_send[(3 + k) * layers:(4 + k) * layers, :cols] = nvec_in[k]
        for l in range(layers):
            w_send[packed(l, 0, 3), :] = ew1_in[pl.ds(l * 3 * q, 3 * q), :].astype(F32)
            w_send[packed(l, 3), :] = ew2_in[pl.ds(l * q, q), :].astype(F32)
            w_send[packed(l, 4, 2), :] = nw1_in[pl.ds(l * 2 * q, 2 * q), :].astype(F32)
            w_send[packed(l, 6), :] = nw2_in[pl.ds(l * q, q), :].astype(F32)
        with jax.named_scope('barrier'):
            @pl.when(t != LEADER)
            def _():
                pl.semaphore_wait(barrier, len(OTHERS))

            @pl.when(t == HELPER)
            def _():
                pl.semaphore_signal(ready, inc=1, device_id={'tp': LEADER}, device_id_type=MESH)

            @pl.when(t == LEADER)
            def _():
                pl.semaphore_wait(ready, 1)

        w_cross.start()
        w_pair.start()
        ncop[1].start()
        ncop[0].start()
        loads[1].wait()
        with jax.named_scope('send_edges'):
            load_edges(edge_raw, e_send, e0, EDGE_IN)
        loads[2].wait()
        load_nodes(gnode_raw, gn_send, d_part)
        gcop = node_copies(gn_send, gn_recv, 1)
        gcop[1].start()
        gcop[0].start()
        loads[3].wait()
        with jax.named_scope('send_grads'):
            load_edges(gedge_raw, g_send, ge, GRAD_IN)

        with jax.named_scope('dp_barrier'):
            @pl.when(t == LEADER)
            def _():
                for i in dp_others:
                    pl.semaphore_signal(barrier, inc=1, device_id={'dp': lax.rem(p + i, dpn)}, device_id_type=MESH)
                pl.semaphore_wait(barrier, len(OTHERS) + dpn - 1)
                for d in OTHERS:
                    pl.semaphore_signal(ready, inc=1, device_id={'tp': peer[d]}, device_id_type=MESH)

            @pl.when(t != LEADER)
            def _():
                pl.semaphore_wait(ready, 1)

        w_cross.wait_recv()
        for i in dp_others:
            weight_copy(i, p).start()

        @pl.when(c == 1)
        def _():
            for recv in (e_recv, g_recv):
                recv[:, last, :, D:] = jnp.zeros((len(OTHERS), cols, EC - D), F32)

        iota[...] = lax.broadcasted_iota(jnp.int32, (T, D), 0).astype(I16)
        lanes[...] = lax.broadcasted_iota(jnp.int32, (16, D), 1).astype(I16)

        ids_raw[...] = jnp.full(ids_raw.shape, -1, jnp.int32)
        for which, src in enumerate((send_ids, recv_ids)):
            ids_raw[which:which + 1, :edges] = src[...].reshape(1, edges)

        def ids(b):
            for which, (row_ref, col_ref) in enumerate(((srow, scol), (rrow, rcol))):
                wide = jnp.broadcast_to(ids_raw[which:which + 1, pl.ds(pl.multiple_of(c * eh + b * D, D), D)], (D, D))
                row_ref[at(b, 16), :] = wide[:16].astype(I16)
                col_ref[at(b, D), :] = flip(wide.astype(F32)).astype(jnp.int32).astype(I16)

        with jax.named_scope('ids'):
            loop(eh // D, ids)

        def keys(ref, step):
            return [ref[pl.ds(pl.multiple_of(step * (KS // D) * 16 + 16 * h, 16), 1), :] for h in range(KS // D)]

        bias_cols[...] = flip(stacked([eb1_in[...], nb1_in[...], jnp.zeros((D - 2 * layers, D), F32)]))

        def join_weights(l):
            for d in range(GROUP):
                src = w_recv.at[slot(d)] if d else w_send
                r = rows_of(d)
                for k in THREE:
                    ew1[l, pl.ds(k * D + d * q, q), :] = src[packed(l, k), :].astype(BF)
                ew2t[l, r, :] = src[packed(l, 3), :].astype(BF)
                for k in BOTH:
                    nw1[l, pl.ds(k * D + d * q, q), :] = src[packed(l, 4 + k), :].astype(BF)
                nw2t[l, r, :] = src[packed(l, 6), :].astype(BF)

            def flip_bf(mat):
                return flip(mat.astype(F32)).astype(BF)

            for k in THREE:
                ew1t[l, :, mat(k)] = flip_bf(ew1[l, mat(k), :])
            for k in BOTH:
                nw1t[l, :, mat(k)] = flip_bf(nw1[l, mat(k), :])
            ew2[l] = flip_bf(ew2t[l])
            nw2[l] = flip_bf(nw2t[l])

        def wait_recvs(copies):
            copies[1].wait_recv()
            copies[2].start()
            copies[0].wait_recv()
            copies[2].wait_recv()

        with jax.named_scope('node_wait'):
            wait_recvs(ncop)
        for d in OTHERS:
            v0[rows_of(d), :] = n_recv[slot(d)].astype(BF)
        with jax.named_scope('weight_wait'):
            dp_all(0, 2).wait_recv()
            w_relay.start()
            w_pair.wait_recv()
            w_relay.wait_recv()
        rows_all = beside([w_send[:HEAD, :cols]] + [w_recv[d, :HEAD, :cols] for d in range(3)])
        vecs[...] = flip(stacked([rows_all, jnp.zeros((D - HEAD, D), F32)]))
        join_weights(0)

        def vec(l, node):
            first = 6 * node + l
            return [vecs[:, first + 2 * k:first + 2 * k + 1] for k in THREE]

        def bias(l, node):
            return bias_cols[:, node * layers + l:node * layers + l + 1]

        def hidden_of_nodes(l):
            table, b1 = tables[l], bias(l, 0)

            def body(step):
                xs = gather(table, keys(srow, step), iota).astype(BF)
                xr = gather(table, keys(rrow, step), iota).astype(BF)
                hidden[l, :, at(step, KS)] = dot(ew1t[l, :, mat(1, 2)], stacked([xs, xr])) + b1

            loop(eh // KS, body)

        def edge_forward(l):
            e_in = edges_in[l]

            def body(j):
                for sub in range(EC // T):
                    a = at(j * (EC // T) + sub, T)
                    if l == 0:
                        if sub == 0:
                            chunk_arrived(EDGE_IN, j)
                        for d in OTHERS:
                            e_in[rows_of(d), a] = e_recv[slot(d), j, :, sub * T:(sub + 1) * T].astype(BF)
                    e_val = e_in[:, a]
                    hid = hidden[l, :, a] + dot(ew1t[l, :, mat(0)], e_val)
                    hidden[l, :, a] = hid
                    message, nrm, std = mlp_tail(hid, ew2t[l], vec(l, 0))
                    normed[l, :, a] = nrm
                    inv[l:l + 1, a] = std
                    msg[:, a] = message
                    e_new = (e_val.astype(F32) + message.astype(F32)).astype(BF)
                    if l < top:
                        edges_in[l + 1][:, a] = e_new
                    else:
                        for d in OTHERS:
                            e_send[slot(d), j, :, sub * T:(sub + 1) * T] = e_new[rows_of(d)].astype(F32)
                        if sub == 0:
                            own_parts = []
                        own_parts.append(e_new[:q])
                if l == top:
                    for d in SEND_ORDER:
                        edge_start(EDGE_OUT, j, d)
                    place_edges(edge_raw, beside(own_parts), 0, j)

            loop(nch, body)

        def segment_sum(acc, ids_ref):
            acc[...] = jnp.zeros(acc.shape, F32)

            def body(step):
                scatter(acc, msg[:, at(step, KS)], ids_ref[at(step, KS), :], lanes)

            loop(eh // KS, body)

        def node_forward(l):
            table, agg, out = tables[l], aggs[l], tables[l + 1]

            def body(step):
                a = pl.ds(pl.multiple_of(step * TN, D), TN)
                v_in = table[:, a]
                agg_bf = (part[l, :, a] + swap_halves(part_recv[l, :, a])).astype(BF)
                agg[:, a] = agg_bf
                hid = dot(nw1t[l], stacked([v_in, agg_bf])) + bias(l, 1)
                nhid[l, :, a] = hid
                message, nrm, std = mlp_tail(hid, nw2t[l], vec(l, 1))
                nnrm[l, :, a] = nrm
                ninv[l:l + 1, a] = std
                out[:, a] = (v_in.astype(F32) + message.astype(F32)).astype(BF)

            loop(npad // TN, body)

        for l in range(layers):
            with jax.named_scope(f'gather_{l}'):
                hidden_of_nodes(l)
            if l == top:
                edges_sent(EDGE_IN)
            with jax.named_scope(f'edge_forward_{l}'):
                edge_forward(l)
            with jax.named_scope(f'sum_{l}'):
                segment_sum(part.at[l], rcol)
            part_copy(l).start()
            if l == 0:
                join_weights(1)
                gcop[1].wait_recv()
                gcop[2].start()
            with jax.named_scope(f'part_wait_{l}'):
                part_copy(l).wait_recv()
            with jax.named_scope(f'node_forward_{l}'):
                node_forward(l)
        no_send[...] = tables[layers][rows_of(2), :].astype(F32)
        no_copy = remote(no_send, no_recv, n_ss.at[2, 0], n_rs.at[2, 0], 2)
        no_copy.start()
        node_raw[x] = tables[layers][:q, :nodes]

        grad[...] = jnp.zeros_like(grad)
        sums[...] = jnp.zeros_like(sums)
        with jax.named_scope('grad_node_wait'):
            gcop[0].wait_recv()
            gcop[2].wait_recv()
        for d in OTHERS:
            d_part[rows_of(d), :] = gn_recv[slot(d)]

        def node_backward(l):
            table, agg = tables[l], aggs[l]

            def body(step):
                a = pl.ds(pl.multiple_of(step * TN, D), TN)
                d_in = d_part[:, a]
                if l < top:
                    d_in = d_in + part[layers + l + 1, :, a] + swap_halves(part_recv[layers + l + 1, :, a])
                    d_in = d_in.astype(BF).astype(F32)
                d_hid, d_w2, parts = mlp_back(d_in, nhid[l, :, a], nnrm[l, :, a], ninv[l:l + 1, a], nw2[l], vec(l, 1))
                add_sums(sums.at[l, 1], [parts])
                grad[l, 4] += d_w2
                grad[l, 2] += dot_nt(table[:, a], d_hid)
                grad[l, 3] += dot_nt(agg[:, a], d_hid)
                d_part[:, a] = d_in + dot(nw1[l, mat(0), :], d_hid)
                d_agg[:, a] = dot(nw1[l, mat(1), :], d_hid).astype(BF)

            loop(npad // TN, body)

        def gather_back():
            def body(step):
                msg[:, at(step, KS)] = gather(d_agg, keys(rrow, step), iota).astype(BF)

            loop(eh // KS, body)

        def edge_backward(l):
            e_in = edges_in[l]

            def body(j):
                all_parts, d_w2s, d_w1s, own_parts = [], [], [], []
                for sub in range(EC // T):
                    a = at(j * (EC // T) + sub, T)
                    if l == top:
                        if sub == 0:
                            chunk_arrived(GRAD_IN, j)
                        for d in OTHERS:
                            ge[rows_of(d), a] = g_recv[slot(d), j, :, sub * T:(sub + 1) * T].astype(BF)
                    d_res = ge[:, a].astype(F32)
                    d_msg = d_res + msg[:, a].astype(F32)
                    d_hid, d_w2, parts = mlp_back(d_msg, hidden[l, :, a], normed[l, :, a], inv[l:l + 1, a], ew2[l], vec(l, 0))
                    all_parts.append(parts)
                    d_w2s.append(d_w2)
                    d_w1s.append(dot_nt(e_in[:, a], d_hid))
                    msg[:, a] = d_hid
                    d_new = (d_res + dot(ew1[l, mat(0), :], d_hid)).astype(BF)
                    if l > 0:
                        ge[:, a] = d_new
                    else:
                        for d in OTHERS:
                            g_send[slot(d), j, :, sub * T:(sub + 1) * T] = d_new[rows_of(d)].astype(F32)
                        own_parts.append(d_new[:q])
                add_sums(sums.at[l, 0], all_parts)
                grad[l, 1] += sum(d_w2s[1:], d_w2s[0])
                grad[l, 0] += sum(d_w1s[1:], d_w1s[0])
                if l == 0:
                    @pl.when(j < hold)
                    def _():
                        for d in SEND_ORDER:
                            edge_start(GRAD_OUT, j, d)
                    place_edges(gedge_raw, beside(own_parts), 0, j)

            loop(nch, body)

        def vector_slab(l):
            def total(node, k):
                return column_sum(flip(sums[l, node, mat(k), :]))

            lat = stacked([total(node, k) for node in BOTH for k in THREE])
            biases = stacked([total(node, 3) for node in BOTH])
            n_lat = lat.shape[0]
            for d in range(GROUP):
                grad[l, VEC_SLAB, d * cols:d * cols + n_lat, :cols] = lat[:, rows_of(d)]
                grad[l, VEC_SLAB, d * cols + n_lat:d * cols + n_lat + 2, :] = biases

        def reduce_start(l, stage):
            for b in BOTH:
                core_copy(l, b, stage).start()

        def chip_sum(l, stage):
            row = lax.broadcasted_iota(jnp.int32, (cols, D), 0)
            edge_row = jnp.logical_or(row < 3, row == 6)
            core_all(l, stage).wait_recv()
            for b in BOTH:
                for k in range(SLABS)[STAGES[stage]]:
                    own = grad[l, k, rows_of(2 * b), :]
                    if k in EDGE_SLABS:
                        own = own + core_recv[l, b, k]
                    elif k == VEC_SLAB:
                        own = own + jnp.where(edge_row, core_recv[l, b, k], 0.0)
                    half[l, k, b] = own
            for i in dp_others:
                @pl.when(in_stage(lax.rem(p + i, dpn), stage))
                def _():
                    spread_copy(l, i).start()

        def dp_sum(l, stage):
            @pl.when(in_stage(p, stage))
            def _():
                total = half[l, pl.ds(seat(p) * per, per)]
                dp_all(l, 0).wait_recv()
                for i in dp_others:
                    total = total + dp_recv[l, pl.ds((i - 1) * per, per)]
                own_sum[l] = total[:, 0]
                cross_send[l] = total[:, 1]
                cross_copy(l).start()

        def cross_sum(l):
            cross_copy(l).wait_recv()
            total = own_sum[l] + cross_recv[l]
            own_sum[l] = total
            gathered[l, pl.ds(seat(p) * per, per)] = total
            for i in dp_others:
                gather_copy(l, i, p).start()

        def project(l):
            table = tables[l]

            def body(step):
                a = pl.ds(pl.multiple_of(step * TN, D), TN)
                s_bf, r_bf, v_in = s_sum[:, a].astype(BF), r_sum[:, a].astype(BF), table[:, a]
                part[layers + l, :, a] = dot(ew1[l, mat(1), :], s_bf) + dot(ew1[l, mat(2), :], r_bf)
                grad[l, 6] += dot_nt(v_in, s_bf)
                grad[l, 7] += dot_nt(v_in, r_bf)

            loop(npad // TN, body)

        for l in reversed(range(layers)):
            first_layer = l == 0
            with jax.named_scope(f'node_backward_{l}'):
                node_backward(l)
            if first_layer:
                with jax.named_scope('chip_sum_1'):
                    chip_sum(1, 0)
                    chip_sum(1, 1)
            with jax.named_scope(f'gather_back_{l}'):
                gather_back()
            if first_layer:
                edges_sent(GRAD_IN)
            with jax.named_scope(f'edge_backward_{l}'):
                edge_backward(l)
            vector_slab(l)
            reduce_start(l, 0)
            if first_layer:
                with jax.named_scope('dp_sum_1'):
                    dp_sum(1, 0)
                    dp_sum(1, 1)
            with jax.named_scope(f'sum_send_{l}'):
                segment_sum(s_sum, scol)
            if first_layer:
                with jax.named_scope('chip_sum_0'):
                    chip_sum(0, 0)
            with jax.named_scope(f'sum_recv_{l}'):
                segment_sum(r_sum, rcol)
            with jax.named_scope(f'project_{l}'):
                project(l)
            reduce_start(l, 1)
            part_copy(layers + l).start()
            if first_layer:
                with jax.named_scope('chip_sum_late'):
                    chip_sum(0, 1)
                with jax.named_scope('dp_sum_0'):
                    dp_sum(0, 0)
            with jax.named_scope(f'back_wait_{l}'):
                part_copy(layers + l).wait_recv()

        def final(step):
            a = pl.ds(pl.multiple_of(step * TN, D), TN)
            d_in = (d_part[:, a] + part[layers, :, a] + swap_halves(part_recv[layers, :, a])).astype(BF)
            v2[:, a] = d_in

        loop(npad // TN, final)
        gnode_raw[x] = v2[:q, :nodes]
        with jax.named_scope('dp_sum_late'):
            dp_sum(0, 1)

        dn_send[...] = v2[rows_of(2), :].astype(F32)
        dn_copy = remote(dn_send, dn_recv, n_ss.at[2, 1], n_rs.at[2, 1], 2)
        dn_copy.start()

        def send_rest(j):
            for d in SEND_ORDER:
                edge_start(GRAD_OUT, j, d)

        loop(nch, send_rest, hold)

        with jax.named_scope('node_out_wait'):
            no_copy.wait_recv()
        node_raw[ox] = no_recv[:, :nodes].astype(BF)

        def place_e(j):
            for d in OTHERS:
                place_edges(edge_raw, eo_recv[slot(d), j], d, j)

        with jax.named_scope('place_edge_out'):
            for group in THREE:
                group_arrived(EDGE_OUT, group)
            loop(nch, place_e)

        def place_g(j):
            for d in OTHERS:
                place_edges(gedge_raw, de_recv[slot(d), j], d, j)

        with jax.named_scope('place_first'):
            group_arrived(GRAD_OUT, 0)
            loop(hold, place_g)
        for l in range(layers):
            with jax.named_scope(f'cross_sum_{l}'):
                cross_sum(l)
        with jax.named_scope('d_node_wait'):
            dn_copy.wait_recv()
        gnode_raw[ox] = dn_recv[:, :nodes].astype(BF)
        with jax.named_scope('place_rest'):
            group_arrived(GRAD_OUT, 1)
            loop(last, place_g, hold)
        for l in range(layers):
            dp_all(l, 1).wait_recv()
            ew1_buf[l, 0] = gathered[l, 0]
            ew1_buf[l, 1:] = gathered[l, EARLY:]
            ew2_buf[l] = gathered[l, 1]
            nw1_buf[l] = gathered[l, 2:4]
            nw2_buf[l] = gathered[l, 4]
            small = gathered[l, VEC_SLAB]
            for k in THREE:
                evec_buf[k, l:l + 1, :] = small[k:k + 1, :cols]
                nvec_buf[k, l:l + 1, :] = small[3 + k:4 + k, :cols]
            eb1_buf[l:l + 1, :] = small[6:7]
            nb1_buf[l:l + 1, :] = small[7:8]
        for l in range(layers):
            for stage in BOTH:
                core_all(l, stage).wait_send()
            cross_copy(l).wait_send()
            dp_all(l, 0).wait_send()
            dp_all(l, 1).wait_send()
        for copy in ncop + gcop + (w_pair, w_cross, w_relay):
            copy.wait_send()
        dp_all(0, 2).wait_send()
        no_copy.wait_send()
        dn_copy.wait_send()
        for k in range(2 * layers):
            part_copy(k).wait_send()
        edges_sent(EDGE_OUT)
        with jax.named_scope('place_last'):
            group_arrived(GRAD_OUT, 2)
            loop(nch, place_g, last)
        edges_sent(GRAD_OUT)

    bf = lambda *s: pltpu.VMEM(s, BF)
    pl.run_scoped(
        scoped, bf(D, eh), bf(D, eh), bf(D, eh), bf(D, eh), bf(D, npad), bf(D, npad), bf(D, npad), bf(D, npad), bf(D, npad), bf(D, npad),
        pltpu.VMEM((eh, D), I16), pltpu.VMEM((eh, D), I16), pltpu.VMEM((eh // D * 16, D), I16), pltpu.VMEM((eh // D * 16, D), I16),
        pltpu.VMEM((T, D), I16), pltpu.VMEM((16, D), I16),
        bf(layers, 3 * D, D), bf(layers, D, 3 * D), bf(layers, D, D), bf(layers, D, D),
        bf(layers, 2 * D, D), bf(layers, D, 2 * D), bf(layers, D, D), bf(layers, D, D), pltpu.VMEM((D, D), F32))


def finish_moves(src, dst):
    if len(src.shape) != 3 or src.dtype != BF:
        return [(src, dst)]
    return [(src.at[s, pl.ds(r, 8)], dst.at[s, pl.ds(r, 8)]) for s in range(src.shape[0]) for r in range(0, src.shape[1], 8)]


def finish_kernel(*refs):
    count = len(refs) // 2
    moves = sum((finish_moves(refs[k], refs[count + k]) for k in range(count)), [])
    puts = [pltpu.make_async_copy(src, dst, refs[-1]) for src, dst in moves]
    for put in puts:
        put.start()
    for put in puts:
        put.wait()


def keep_in_vmem(val):
    return pltpu.with_memory_space_constraint(val, pltpu.VMEM)


def finish(arrays):
    return pl.pallas_call(
        finish_kernel,
        name='finish',
        out_shape=[jax.ShapeDtypeStruct(a.shape, a.dtype) for a in arrays],
        in_specs=[VM] * len(arrays),
        out_specs=[HB] * len(arrays),
        scratch_shapes=[pltpu.SemaphoreType.DMA],
        compiler_params=pltpu.CompilerParams(vmem_limit_bytes=1 << 20),
    )(*[keep_in_vmem(a) for a in arrays])


def solution(mesh):
    lat_spec = P('dp', None, 'tp')
    first_spec = P(None, None, 'tp', None)
    col_spec = P(None, None, 'tp')
    param_specs = (first_spec, P(), col_spec, col_spec, first_spec, P(), col_spec, col_spec)
    in_specs = (lat_spec, lat_spec, P(), P(), lat_spec, lat_spec) + param_specs
    out_specs = (lat_spec, lat_spec, lat_spec, lat_spec) + param_specs
    shape = jax.ShapeDtypeStruct

    def local_step(node_lat, edge_lat, senders, receivers, grad_node, grad_edge, edge_w1, edge_b1, edge_w2, edge_vec, node_w1, node_b1, node_w2, node_vec):
        layers = edge_w1.shape[0]
        cols = node_lat.shape[2]
        nodes, edges = node_lat.shape[1], edge_lat.shape[1]
        npad = -(-nodes // TN) * TN
        eh = -(-edges // (2 * EC)) * EC
        nch = eh // EC
        dpn = mesh.shape['dp']
        per = SLABS // dpn
        dims = (layers, cols, nodes, edges, npad, eh, dpn)
        flat = lambda arr: jnp.swapaxes(arr, 1, 2)
        lead = lambda arr: jnp.transpose(arr, (1, 0, 2))
        args = (flat(node_lat), flat(edge_lat), flat(grad_node), flat(grad_edge), senders, receivers,
                edge_w1.reshape(-1, D), flat(edge_w2).reshape(-1, D), node_w1.reshape(-1, D), flat(node_w2).reshape(-1, D),
                lead(edge_vec), lead(node_vec), edge_b1, node_b1)
        vm, sem = pltpu.VMEM, pltpu.SemaphoreType.DMA
        wrows = -(-(HEAD + layers * LROWS) // (8 * dpn)) * 8 * dpn
        lat_n, lat_e = (2, cols, nodes), (2, cols, edges)
        outs = [RESULT(lat_n, BF), RESULT(lat_e, BF), RESULT(lat_n, BF), RESULT(lat_e, BF),
                RESULT((layers, 3, cols, D), F32), RESULT((layers, D), F32), RESULT((layers, cols, D), F32), RESULT((3, layers, cols), F32),
                RESULT((layers, 2, cols, D), F32), RESULT((layers, D), F32), RESULT((layers, cols, D), F32), RESULT((3, layers, cols), F32)]
        scratch = [
            *[vm(a.shape, a.dtype) for a in args[4:]], vm((wrows, D), F32), vm((3, wrows, D), F32),
            vm((2, cols, npad), F32), vm((3, cols, npad), F32), vm((2, cols, npad), F32), vm((3, cols, npad), F32),
            vm((cols, npad), F32), vm((cols, npad), F32), vm((cols, npad), F32), vm((cols, npad), F32),
            vm((2, 3, cols + cols // GROUP, D), F32), vm((4, 3, cols + cols // GROUP, D), F32), *[vm((3, nch, cols, EC), F32)] * 6,
            vm((2 * layers, D, npad), F32), vm((2 * layers, D, npad), F32),
            vm((layers, D, eh), F32), vm((layers, D, eh), F32), vm((layers, eh), F32),
            vm((layers, D, npad), F32), vm((layers, D, npad), F32), vm((layers, npad), F32),
            vm((D, npad), F32), vm((D, npad), F32), vm((D, npad), F32), vm((2, 2 * eh), jnp.int32), vm((D, D), F32), vm((layers, 2, 4 * D, D), F32),
            vm((layers, SLABS, D, D), F32), vm((layers, 2, SLABS, cols, D), F32), vm((layers, SLABS, 2, cols, D), F32),
            vm((layers, (dpn - 1) * per, 2, cols, D), F32), vm((layers, per, cols, D), F32), vm((layers, per, cols, D), F32),
            vm((layers, per, cols, D), F32), vm((layers, SLABS, cols, D), F32),]
        own_sems = [
            sem((layers, 2)), sem((3, layers)), sem((layers,)), sem((3,)), sem((3, 3)), sem((2, nch)), sem((2, 5)), sem((2 * layers,)),
            pltpu.SemaphoreType.REGULAR,
            sem((len(args),)), sem((3,)), sem((3, 3)), sem((4, 4)), sem((2 * layers,)), sem((layers, 2)), sem((3, layers)), sem((layers,))]
        res = pl.pallas_call(
            lambda *refs: pl.run_scoped(lambda *own: step_kernel(dims, *refs, *own), *own_sems),
            name='graph_step',
            out_shape=outs,
            in_specs=[HB] * len(args),
            out_specs=[VM] * len(outs),
            scratch_shapes=scratch,
            compiler_params=pltpu.CompilerParams(collective_id=0, has_side_effects=True, vmem_limit_bytes=VMEM_LIMIT),
        )(*args)

        res = finish(res)
        return (flat(res[0]), flat(res[1]), flat(res[2]), flat(res[3]),
                res[4], res[5], flat(res[6]), lead(res[7]), res[8], res[9], flat(res[10]), lead(res[11]))

    return jax.shard_map(local_step, mesh=mesh, in_specs=in_specs, out_specs=out_specs, check_vma=False)
```

```python
import jax
import jax.numpy as jnp
from jax import lax
from jax.experimental import pallas as pl
from jax.experimental.pallas import tpu as pltpu
from jax.sharding import PartitionSpec as P

LN_EPS = 1e-5
D = 128
T = 256
TN = 384
EC = 512
KS = 1408
BF = jnp.bfloat16
F32 = jnp.float32
I16 = jnp.int16
MESH = pl.DeviceIdType.MESH
VM = pl.BlockSpec(memory_space=pltpu.VMEM)
HB = pl.BlockSpec(memory_space=pl.ANY)
RESULT = pltpu.VMEM
GROUP = 4
BOTH = (0, 1)
THREE = (0, 1, 2)
OTHERS = (1, 2, 3)
EDGE_IN, GRAD_IN, EDGE_OUT, GRAD_OUT = range(4)
SEND_ORDER = (2, 3, 1)
LROWS = 7 * (D // 4)
HEAD = 16
LEADER = GROUP - 1
HELPER = LEADER - 1
VMEM_LIMIT = 63_000_000
SLABS = 8
EARLY = 6
VEC_SLAB = 5
EDGE_SLABS = (0, 1, 6, 7)
STAGES = (slice(0, EARLY), slice(EARLY, SLABS))


def dot(a, b):
    return jnp.dot(a, b, preferred_element_type=F32)


def dot_nt(a, b):
    return lax.dot_general(a, b, (((1,), (1,)), ((), ())), preferred_element_type=F32)


def mat(k, n=1):
    return slice(k * D, (k + n) * D)


def rows_of(d):
    q = D // 4
    return slice(d * q, (d + 1) * q)


def at(step, width):
    return pl.ds(pl.multiple_of(step * width, width), width)


def loop(stop, body, start=0):
    def step(j, carry):
        body(j)
        return carry

    lax.fori_loop(start, stop, step, 0)


def column_sum(val):
    return jnp.sum(val, axis=0, keepdims=True)


def flip(val):
    return jnp.swapaxes(val, 0, 1)


def stacked(parts):
    return jnp.concatenate(parts, axis=0)


def beside(parts):
    return jnp.concatenate(parts, axis=1)


def slot(d):
    return d - 1


def sigmoid(hidden):
    return 1.0 / (1.0 + jnp.exp(-hidden))


def fold(val):
    total = val[:, mat(0)]
    for start in range(D, val.shape[1], D):
        total = total + val[:, start:start + D]
    return total


def swap_halves(val):
    return stacked([val[rows_of(d)] for d in (1, 0, 3, 2)])


def gather(table, keys, iota):
    acc = None
    nodes = table.shape[1]
    one, zero = jnp.ones((), BF), jnp.zeros((), BF)
    for base in range(0, nodes, T):
        width = min(T, nodes - base)
        ids = iota[0:width, :]
        hot = beside([jnp.where(ids == (key - jnp.asarray(base, I16)), one, zero) for key in keys])
        part = dot(table[:, base:base + width], hot)
        acc = part if acc is None else acc + part
    return acc


def scatter(acc_ref, val, cols, lanes):
    nodes = acc_ref.shape[1]
    one, zero = jnp.ones((), BF), jnp.zeros((), BF)
    row = lanes[0:1, :]
    for base in range(0, nodes, T):
        width = min(T, nodes - base)
        hot = beside([jnp.where((row + jnp.asarray(base + s, I16)) == cols, one, zero) for s in range(0, width, D)])
        acc_ref[:, base:base + width] += dot(val, hot)


def mlp_tail(hidden, w2t, vec):
    act = (hidden * sigmoid(hidden)).astype(BF)
    out = dot(w2t, act) + vec[0]
    mean = column_sum(out) / D
    centered = out - mean
    var = column_sum(centered * centered) / D
    inv = lax.rsqrt(var + LN_EPS)
    normed = centered * inv
    message = (normed * vec[1] + vec[2]).astype(BF)
    return message, normed, inv


def mlp_back(d_msg, hidden, normed, inv, w2, vec):
    d_normed = d_msg * vec[1]
    mean0 = column_sum(d_normed) / D
    mean1 = column_sum(d_normed * normed) / D
    d_out = inv * (d_normed - mean0 - normed * mean1)
    d_out_bf = d_out.astype(BF)
    sig = sigmoid(hidden)
    act = (hidden * sig).astype(BF)
    d_w2 = dot_nt(d_out_bf, act)
    d_hidden = dot(w2, d_out_bf) * (sig * (1.0 + hidden * (1.0 - sig)))
    sums = (fold(d_out), fold(d_msg * normed), fold(d_msg), fold(d_hidden))
    return d_hidden.astype(BF), d_w2, sums


def add_sums(ref, parts):
    for q in range(4):
        total = parts[0][q]
        for other in parts[1:]:
            total = total + other[q]
        ref[mat(q), :] += total


def step_kernel(dims, *refs):
    layers, cols, nodes, edges, npad, eh, dpn = dims
    nch = eh // EC
    top = layers - 1
    n_in = 14
    hbm_in = refs[:n_in]
    n_out = 12
    (node_raw, edge_raw, gnode_raw, gedge_raw, ew1_buf, eb1_buf, ew2_buf, evec_buf, nw1_buf, nb1_buf, nw2_buf, nvec_buf) = refs[n_in:n_in + n_out]
    (send_ids, recv_ids, ew1_in, ew2_in, nw1_in, nw2_in, evec_in, nvec_in, eb1_in, nb1_in, w_send, w_recv, n_send, n_recv, gn_send, gn_recv, no_send, no_recv, dn_send, dn_recv,
     node_pad, t_send, t_recv, e_send, g_send, e_recv, g_recv, eo_recv, de_recv, part, part_recv, hidden, normed, inv, nhid, nnrm, ninv, d_part, s_sum, r_sum,
     ids_raw, bias_cols, sums, grad, core_recv, half, dp_recv, cross_send, cross_recv, own_sum, gathered,
     core_rs, dp_rs, cross_rs, w_rs, n_rs, e_rs, o_rs, p_rs, ready, load_sem, w_ss, n_ss, e_ss, p_ss, core_ss, dp_ss, cross_ss) = refs[n_in + n_out:]

    t = lax.axis_index('tp')
    p = lax.axis_index('dp')
    per = SLABS // dpn
    dp_others = range(1, dpn)
    x, c = t // 2, lax.rem(t, 2)
    ox, oc = 1 - x, 1 - c
    peer = [t, t + 1 - 2 * c, t + 2 - 4 * x, t + 3 - 2 * c - 4 * x]

    def remote(src, dst, ssem, rsem, d):
        return pltpu.make_async_remote_copy(src_ref=src, dst_ref=dst, send_sem=ssem, recv_sem=rsem,
                                            device_id={'tp': peer[d]}, device_id_type=MESH)

    small_in = (send_ids, recv_ids, ew1_in, ew2_in, nw1_in, nw2_in, evec_in, nvec_in, eb1_in, nb1_in)
    loads = [pltpu.make_async_copy(src, dst, load_sem.at[q]) for q, (src, dst) in enumerate(
        zip(hbm_in, (node_raw, edge_raw, gnode_raw, gedge_raw) + small_in))]

    def node_copies(send, recv, kind):
        return (remote(send.at[1], recv.at[0], n_ss.at[kind, 0], n_rs.at[kind, 0], 1),
                remote(send.at[0], recv.at[1], n_ss.at[kind, 1], n_rs.at[kind, 1], 2),
                remote(recv.at[1], recv.at[2], n_ss.at[kind, 2], n_rs.at[kind, 2], 1))

    piece = w_send.shape[0] // dpn

    def packed(l, k, count=1):
        return pl.ds(HEAD + l * LROWS + k * cols, count * cols)

    def weight_rows(owner):
        return pl.ds(pl.multiple_of(owner * piece, 8), piece)

    w_pair = remote(w_send, w_recv.at[0], w_ss.at[0], w_rs.at[0], 1)
    w_cross = remote(w_send.at[weight_rows(p)], w_recv.at[1, weight_rows(p)], w_ss.at[1], w_rs.at[1], 2)
    w_relay = remote(w_recv.at[1], w_recv.at[2], w_ss.at[2], w_rs.at[2], 1)

    def weight_copy(i, owner):
        rows = w_recv.at[1, weight_rows(owner)]
        return dp_remote(rows, rows, 2, 0, i)

    last = nch - 1
    hold = nch - 3
    buffers = ((e_send, e_recv), (g_send, g_recv), (e_send, eo_recv), (g_send, de_recv))

    def outward(kind):
        return kind in (EDGE_OUT, GRAD_OUT)

    every = slice(None)
    ragged = pl.ds(D, D // GROUP)
    rest = [slice(g * cols // GROUP, (g + 1) * cols // GROUP) for g in range(GROUP)]

    def edge_part(kind, which, j, tail, send_sem, recv_sem, d):
        src, dst = buffers[kind]
        if tail:
            src, dst = t_send.at[kind % 2, which], t_recv.at[kind, which]
        else:
            src, dst = src.at[which, j], dst.at[which, j]
        recv_sems = o_rs.at[kind - EDGE_OUT, recv_sem] if outward(kind) else e_rs.at[kind, recv_sem]
        return remote(src, dst, e_ss.at[kind, send_sem], recv_sems, d)

    def by_half(half_id, j, action):
        narrow = jnp.logical_and(j == last, half_id == 1)

        @pl.when(jnp.logical_not(narrow))
        def _():
            action(False)

        @pl.when(narrow)
        def _():
            action(True)

    def pack_tail(kind, d):
        src, out = buffers[kind][0].at[slot(d), last], t_send.at[kind % 2, slot(d)]
        out[:cols, :] = src[:, :D]
        over = src[:, ragged]
        out[cols:, :] = beside([over[r] for r in rest])

    def unpack_tail(kind, d):
        src, out = t_recv.at[kind, slot(d)], buffers[kind][1].at[slot(d), last]
        out[:, :D] = src[:cols, :]
        over = src[cols:, :]
        out[:, ragged] = stacked([over[:, rows_of(g)] for g in range(GROUP)])

    def edge_start(kind, j, d):
        other = oc if d % 2 else c
        if outward(kind):
            send_sem, recv_sem = jnp.where(j == last, 1, 0), jnp.where(j == last, 2 + slot(d), jnp.where(j < hold, 0, 1))
        else:
            send_sem, recv_sem = jnp.where(j == last, d, 0), j

        def start(tail):
            if tail:
                pack_tail(kind, d)
            edge_part(kind, slot(d), j, tail, send_sem, recv_sem, d).start()

        by_half(c if outward(kind) else other, j, start)

    def edges_sent(kind):
        edge_part(kind, every, slice(0, last), False, 0, 0, 1).wait_send()
        if outward(kind):
            by_half(c, last, lambda tail: edge_part(kind, every, last, tail, 1, 0, 1).wait_send())
        else:
            for d in OTHERS:
                by_half(oc if d % 2 else c, last, lambda tail: edge_part(kind, slot(d), last, tail, d, 0, d).wait_send())

    def chunk_arrived(kind, j):
        def arrived(tail):
            edge_part(kind, every, j, tail, 0, j, 1).wait_recv()
            if tail:
                for d in OTHERS:
                    unpack_tail(kind, d)

        by_half(c, j, arrived)

    def group_arrived(kind, group):
        if group < 2:
            edge_part(kind, every, (slice(0, hold), slice(hold, last))[group], False, 0, group, 1).wait_recv()
        else:
            for d in OTHERS:
                def arrived(tail):
                    edge_part(kind, slot(d), last, tail, 0, 2 + slot(d), d).wait_recv()
                    if tail:
                        unpack_tail(kind, d)

                by_half(oc if d % 2 else c, last, arrived)

    def core_copy(l, b, stage):
        first, count = ((0, EARLY), (EARLY, SLABS - EARLY))[stage]
        return remote(grad.at[l, pl.ds(first, count), pl.ds((2 * b + 1) * cols, cols), :], core_recv.at[l, b, pl.ds(first, count)],
                      core_ss.at[l, stage], core_rs.at[l, stage], 1)

    def core_all(l, stage):
        part_of = core_recv.at[l, :, (slice(0, EARLY), slice(EARLY, SLABS))[stage]]
        return remote(part_of, part_of, core_ss.at[l, stage], core_rs.at[l, stage], 1)

    def seat(device):
        return lax.rem(device + dpn // 2, dpn)

    def in_stage(device, stage):
        early = (seat(device) + 1) * per <= EARLY
        return jnp.logical_not(early) if stage else early

    def dp_remote(src, dst, stage, l, i):
        return pltpu.make_async_remote_copy(src_ref=src, dst_ref=dst, send_sem=dp_ss.at[stage, l], recv_sem=dp_rs.at[stage, l],
                                            device_id={'dp': lax.rem(p + i, dpn)}, device_id_type=MESH)

    def spread_copy(l, i):
        return dp_remote(half.at[l, pl.ds(seat(lax.rem(p + i, dpn)) * per, per)], dp_recv.at[l, pl.ds((i - 1) * per, per)], 0, l, i)

    def dp_all(l, stage):
        most = (dpn - 1) * per
        part_of = (dp_recv.at[l], gathered.at[l, pl.ds(0, most)], w_recv.at[1, pl.ds(0, (dpn - 1) * piece)])[stage]
        return dp_remote(part_of, part_of, stage, l, 1)

    def cross_copy(l):
        return remote(cross_send.at[l], cross_recv.at[l], cross_ss.at[l], cross_rs.at[l], 2)

    def gather_copy(l, i, owner):
        return dp_remote(own_sum.at[l], gathered.at[l, pl.ds(seat(owner) * per, per)], 1, l, i)

    def part_piece(q, a):
        return remote(part.at[q, :, a], part_recv.at[q, :, a], p_ss.at[q], p_rs.at[q], 1)

    def part_copy(q):
        return remote(part.at[q], part_recv.at[q], p_ss.at[q], p_rs.at[q], 1)

    wide = D // GROUP
    tiles = nodes // D
    over = range(tiles * D, nodes, wide)

    def node_rows(k):
        return slice(k * cols, (k + 1) * cols) if k < tiles else pl.ds(tiles * cols + (k - tiles) * cols // GROUP, cols // GROUP)

    def pack_nodes(take, out):
        for k in range(tiles):
            out[node_rows(k), :] = take(k * D, D)
        for k, start in enumerate(over):
            val = take(start, wide)
            out[node_rows(tiles + k), :] = beside([val[r] for r in rest])

    def unpack_nodes(src, put):
        for k in range(tiles):
            put(k * D, src[node_rows(k), :])
        for k, start in enumerate(over):
            val = src[node_rows(tiles + k), :]
            put(start, stacked([val[:, rows_of(g)] for g in range(GROUP)]))

    def put_rows(ref, rows):
        def put(start, val):
            ref[rows, start:start + val.shape[1]] = val.astype(ref.dtype)

        return put

    def put_output(ref):
        def put(start, val):
            used = min(val.shape[1], nodes - start)
            ref[ox, :, start:start + used] = val[:, :used].astype(ref.dtype)

        return put

    def take_rows(ref, rows):
        return lambda start, width: ref[rows, start:start + width].astype(F32)

    def load_nodes(raw, send, own):
        own[...] = jnp.zeros_like(own)
        node_pad[...] = jnp.zeros_like(node_pad)
        for which, sample in enumerate((ox, x)):
            node_pad[:, :nodes] = raw[sample].astype(F32)
            pack_nodes(take_rows(node_pad, every), send.at[which])
        own[:cols, :] = node_pad[...].astype(own.dtype)

    def load_edges(raw, send, own, kind):
        def put(j, lanes_j, val_of):
            for d in OTHERS:
                sample = x if d < 2 else ox
                send[slot(d), j] = val_of(sample, oc if d % 2 else c).astype(F32)
            own[:cols, lanes_j] = val_of(x, c)

        def chunk(j):
            put(j, at(j, EC), lambda s, h: raw[s, :, pl.ds(pl.multiple_of(h * eh + j * EC, D), EC)])
            for d in SEND_ORDER:
                edge_start(kind, j, d)

        loop(nch - 1, chunk)
        first = (nch - 1) * EC
        used = edges - eh - first
        last = pl.ds(first, EC)

        def tail(s, h):
            left = raw[s, :, pl.ds(first, EC)]
            right = beside([raw[s, :, pl.ds(eh + first, used)], jnp.zeros((cols, EC - used), BF)])
            return jnp.where(h == 0, left.astype(F32), right.astype(F32)).astype(BF)

        put(nch - 1, last, tail)
        for d in SEND_ORDER:
            edge_start(kind, nch - 1, d)

    def place_edges(raw, block, d, j):
        s = x if d < 2 else ox
        h = oc if d % 2 else c
        val = block.astype(BF)
        first = (nch - 1) * EC
        used = edges - eh - first

        @pl.when(jnp.logical_or(j < nch - 1, h == 0))
        def _():
            raw[s, :, pl.ds(pl.multiple_of(h * eh + j * EC, D), EC)] = val

        @pl.when(jnp.logical_and(j == nch - 1, h == 1))
        def _():
            raw[s, :, pl.ds(eh + first, used)] = val[:, :used]

    def scoped(e0, e1, ge, msg, v0, v1, v2, agg0, agg1, d_agg, scol, rcol, srow, rrow, iota, lanes, ew1, ew1t, ew2, ew2t, nw1, nw1t, nw2, nw2t, vecs):
        tables = (v0, v1, v2)
        aggs = (agg0, agg1)
        edges_in = (e0, e1)

        barrier = pltpu.get_barrier_semaphore()
        for d in OTHERS:
            pl.semaphore_signal(barrier, device_id={'tp': peer[d]}, device_id_type=MESH)
        for copy in loads[:1] + loads[4:] + loads[1:4]:
            copy.start()
        loads[0].wait()
        with jax.named_scope('send_nodes'):
            load_nodes(node_raw, n_send, v0)
        ncop = node_copies(n_send, n_recv, 0)
        for copy in loads[4:]:
            copy.wait()
        q = cols
        w_send[:HEAD, :] = jnp.zeros((HEAD, D), F32)
        for k in THREE:
            w_send[k * layers:(k + 1) * layers, :cols] = evec_in[k]
            w_send[(3 + k) * layers:(4 + k) * layers, :cols] = nvec_in[k]
        for l in range(layers):
            w_send[packed(l, 0, 3), :] = ew1_in[pl.ds(l * 3 * q, 3 * q), :].astype(F32)
            w_send[packed(l, 3), :] = ew2_in[pl.ds(l * q, q), :].astype(F32)
            w_send[packed(l, 4, 2), :] = nw1_in[pl.ds(l * 2 * q, 2 * q), :].astype(F32)
            w_send[packed(l, 6), :] = nw2_in[pl.ds(l * q, q), :].astype(F32)
        with jax.named_scope('barrier'):
            @pl.when(t != LEADER)
            def _():
                pl.semaphore_wait(barrier, len(OTHERS))

            @pl.when(t == HELPER)
            def _():
                pl.semaphore_signal(ready, device_id={'tp': LEADER}, device_id_type=MESH)

            @pl.when(t == LEADER)
            def _():
                pl.semaphore_wait(ready, 1)

        w_cross.start()
        w_pair.start()
        ncop[1].start()
        ncop[0].start()
        loads[1].wait()
        with jax.named_scope('send_edges'):
            load_edges(edge_raw, e_send, e0, EDGE_IN)
        loads[2].wait()
        load_nodes(gnode_raw, gn_send, d_part)
        gcop = node_copies(gn_send, gn_recv, 1)
        gcop[1].start()
        gcop[0].start()
        loads[3].wait()
        with jax.named_scope('send_grads'):
            load_edges(gedge_raw, g_send, ge, GRAD_IN)

        with jax.named_scope('dp_barrier'):
            @pl.when(t == LEADER)
            def _():
                for i in dp_others:
                    pl.semaphore_signal(barrier, device_id={'dp': lax.rem(p + i, dpn)}, device_id_type=MESH)
                pl.semaphore_wait(barrier, len(OTHERS) + dpn - 1)
                for d in OTHERS:
                    pl.semaphore_signal(ready, device_id={'tp': peer[d]}, device_id_type=MESH)

            @pl.when(t != LEADER)
            def _():
                pl.semaphore_wait(ready, 1)

        w_cross.wait_recv()
        for i in dp_others:
            weight_copy(i, p).start()

        @pl.when(c == 1)
        def _():
            for recv in (e_recv, g_recv):
                recv[:, last, :, D:] = jnp.zeros((len(OTHERS), cols, EC - D), F32)

        iota[...] = lax.broadcasted_iota(jnp.int32, (T, D), 0).astype(I16)
        lanes[...] = lax.broadcasted_iota(jnp.int32, (16, D), 1).astype(I16)

        ids_raw[...] = jnp.full(ids_raw.shape, -1, jnp.int32)
        for which, src in enumerate((send_ids, recv_ids)):
            ids_raw[which:which + 1, :edges] = src[...].reshape(1, edges)

        def ids(b):
            for which, (row_ref, col_ref) in enumerate(((srow, scol), (rrow, rcol))):
                wide = jnp.broadcast_to(ids_raw[which:which + 1, pl.ds(pl.multiple_of(c * eh + b * D, D), D)], (D, D))
                row_ref[at(b, 16), :] = wide[:16].astype(I16)
                col_ref[at(b, D), :] = flip(wide.astype(F32)).astype(jnp.int32).astype(I16)

        with jax.named_scope('ids'):
            loop(eh // D, ids)

        def keys(ref, step):
            return [ref[pl.ds(pl.multiple_of(step * (KS // D) * 16 + 16 * h, 16), 1), :] for h in range(KS // D)]

        bias_cols[...] = flip(stacked([eb1_in[...], nb1_in[...], jnp.zeros((D - 2 * layers, D), F32)]))

        def join_weights(l):
            for d in range(GROUP):
                src = w_recv.at[slot(d)] if d else w_send
                r = rows_of(d)
                for k in THREE:
                    ew1[l, pl.ds(k * D + d * q, q), :] = src[packed(l, k), :].astype(BF)
                ew2t[l, r, :] = src[packed(l, 3), :].astype(BF)
                for k in BOTH:
                    nw1[l, pl.ds(k * D + d * q, q), :] = src[packed(l, 4 + k), :].astype(BF)
                nw2t[l, r, :] = src[packed(l, 6), :].astype(BF)

            def flip_bf(mat):
                return flip(mat.astype(F32)).astype(BF)

            for k in THREE:
                ew1t[l, :, mat(k)] = flip_bf(ew1[l, mat(k), :])
            for k in BOTH:
                nw1t[l, :, mat(k)] = flip_bf(nw1[l, mat(k), :])
            ew2[l] = flip_bf(ew2t[l])
            nw2[l] = flip_bf(nw2t[l])

        def wait_recvs(copies):
            copies[1].wait_recv()
            copies[2].start()
            copies[0].wait_recv()
            copies[2].wait_recv()

        with jax.named_scope('node_wait'):
            wait_recvs(ncop)
        for d in OTHERS:
            unpack_nodes(n_recv.at[slot(d)], put_rows(v0, rows_of(d)))
        with jax.named_scope('weight_wait'):
            dp_all(0, 2).wait_recv()
            w_relay.start()
            w_pair.wait_recv()
            w_relay.wait_recv()
        rows_all = beside([w_send[:HEAD, :cols]] + [w_recv[d, :HEAD, :cols] for d in range(3)])
        vecs[...] = flip(stacked([rows_all, jnp.zeros((D - HEAD, D), F32)]))
        join_weights(0)

        def vec(l, node):
            first = 6 * node + l
            return [vecs[:, first + 2 * k:first + 2 * k + 1] for k in THREE]

        def bias(l, node):
            return bias_cols[:, node * layers + l:node * layers + l + 1]

        def hidden_of_nodes(l):
            table, b1 = tables[l], bias(l, 0)

            def body(step):
                xs = gather(table, keys(srow, step), iota).astype(BF)
                xr = gather(table, keys(rrow, step), iota).astype(BF)
                hidden[l, :, at(step, KS)] = dot(ew1t[l, :, mat(1, 2)], stacked([xs, xr])) + b1

            loop(eh // KS, body)

        def edge_forward(l):
            e_in = edges_in[l]

            def body(j):
                for sub in range(EC // T):
                    a = at(j * (EC // T) + sub, T)
                    if l == 0:
                        if sub == 0:
                            chunk_arrived(EDGE_IN, j)
                        for d in OTHERS:
                            e_in[rows_of(d), a] = e_recv[slot(d), j, :, sub * T:(sub + 1) * T].astype(BF)
                    e_val = e_in[:, a]
                    hid = hidden[l, :, a] + dot(ew1t[l, :, mat(0)], e_val)
                    hidden[l, :, a] = hid
                    message, nrm, std = mlp_tail(hid, ew2t[l], vec(l, 0))
                    normed[l, :, a] = nrm
                    inv[l:l + 1, a] = std
                    msg[:, a] = message
                    e_new = (e_val.astype(F32) + message.astype(F32)).astype(BF)
                    if l < top:
                        edges_in[l + 1][:, a] = e_new
                    else:
                        for d in OTHERS:
                            e_send[slot(d), j, :, sub * T:(sub + 1) * T] = e_new[rows_of(d)].astype(F32)
                        if sub == 0:
                            own_parts = []
                        own_parts.append(e_new[:q])
                if l == top:
                    for d in SEND_ORDER:
                        edge_start(EDGE_OUT, j, d)
                    place_edges(edge_raw, beside(own_parts), 0, j)

            loop(nch, body)

        def segment_sum(acc, ids_ref):
            acc[...] = jnp.zeros(acc.shape, F32)

            def body(step):
                scatter(acc, msg[:, at(step, KS)], ids_ref[at(step, KS), :], lanes)

            loop(eh // KS, body)

        def node_forward(l):
            table, agg, out = tables[l], aggs[l], tables[l + 1]

            def body(step):
                a = pl.ds(pl.multiple_of(step * TN, D), TN)
                v_in = table[:, a]
                agg_bf = (part[l, :, a] + swap_halves(part_recv[l, :, a])).astype(BF)
                agg[:, a] = agg_bf
                hid = dot(nw1t[l], stacked([v_in, agg_bf])) + bias(l, 1)
                nhid[l, :, a] = hid
                message, nrm, std = mlp_tail(hid, nw2t[l], vec(l, 1))
                nnrm[l, :, a] = nrm
                ninv[l:l + 1, a] = std
                out[:, a] = (v_in.astype(F32) + message.astype(F32)).astype(BF)

            loop(npad // TN, body)

        for l in range(layers):
            with jax.named_scope(f'gather_{l}'):
                hidden_of_nodes(l)
            if l == top:
                edges_sent(EDGE_IN)
            with jax.named_scope(f'edge_forward_{l}'):
                edge_forward(l)
            with jax.named_scope(f'sum_{l}'):
                segment_sum(part.at[l], rcol)
            part_copy(l).start()
            if l == 0:
                join_weights(1)
                gcop[1].wait_recv()
                gcop[2].start()
            with jax.named_scope(f'part_wait_{l}'):
                part_copy(l).wait_recv()
            with jax.named_scope(f'node_forward_{l}'):
                node_forward(l)
        pack_nodes(take_rows(tables[layers], rows_of(2)), no_send)
        no_copy = remote(no_send, no_recv, n_ss.at[2, 0], n_rs.at[2, 0], 2)
        no_copy.start()
        node_raw[x] = tables[layers][:q, :nodes]

        grad[...] = jnp.zeros_like(grad)
        sums[...] = jnp.zeros_like(sums)
        with jax.named_scope('grad_node_wait'):
            gcop[0].wait_recv()
            gcop[2].wait_recv()
        for d in OTHERS:
            unpack_nodes(gn_recv.at[slot(d)], put_rows(d_part, rows_of(d)))

        def node_backward(l):
            table, agg = tables[l], aggs[l]

            def body(step):
                a = pl.ds(pl.multiple_of(step * TN, D), TN)
                d_in = d_part[:, a]
                if l < top:
                    d_in = d_in + part[layers + l + 1, :, a] + swap_halves(part_recv[layers + l + 1, :, a])
                    d_in = d_in.astype(BF).astype(F32)
                d_hid, d_w2, parts = mlp_back(d_in, nhid[l, :, a], nnrm[l, :, a], ninv[l:l + 1, a], nw2[l], vec(l, 1))
                add_sums(sums.at[l, 1], [parts])
                grad[l, 4] += d_w2
                grad[l, 2] += dot_nt(table[:, a], d_hid)
                grad[l, 3] += dot_nt(agg[:, a], d_hid)
                d_part[:, a] = d_in + dot(nw1[l, mat(0), :], d_hid)
                d_agg[:, a] = dot(nw1[l, mat(1), :], d_hid).astype(BF)

            loop(npad // TN, body)

        def gather_back():
            def body(step):
                msg[:, at(step, KS)] = gather(d_agg, keys(rrow, step), iota).astype(BF)

            loop(eh // KS, body)

        def edge_backward(l):
            e_in = edges_in[l]

            def body(j):
                all_parts, d_w2s, d_w1s, own_parts = [], [], [], []
                for sub in range(EC // T):
                    a = at(j * (EC // T) + sub, T)
                    if l == top:
                        if sub == 0:
                            chunk_arrived(GRAD_IN, j)
                        for d in OTHERS:
                            ge[rows_of(d), a] = g_recv[slot(d), j, :, sub * T:(sub + 1) * T].astype(BF)
                    d_res = ge[:, a].astype(F32)
                    d_msg = d_res + msg[:, a].astype(F32)
                    d_hid, d_w2, parts = mlp_back(d_msg, hidden[l, :, a], normed[l, :, a], inv[l:l + 1, a], ew2[l], vec(l, 0))
                    all_parts.append(parts)
                    d_w2s.append(d_w2)
                    d_w1s.append(dot_nt(e_in[:, a], d_hid))
                    msg[:, a] = d_hid
                    d_new = (d_res + dot(ew1[l, mat(0), :], d_hid)).astype(BF)
                    if l > 0:
                        ge[:, a] = d_new
                    else:
                        for d in OTHERS:
                            g_send[slot(d), j, :, sub * T:(sub + 1) * T] = d_new[rows_of(d)].astype(F32)
                        own_parts.append(d_new[:q])
                add_sums(sums.at[l, 0], all_parts)
                grad[l, 1] += sum(d_w2s[1:], d_w2s[0])
                grad[l, 0] += sum(d_w1s[1:], d_w1s[0])
                if l == 0:
                    @pl.when(j < hold)
                    def _():
                        for d in SEND_ORDER:
                            edge_start(GRAD_OUT, j, d)
                    place_edges(gedge_raw, beside(own_parts), 0, j)

            loop(nch, body)

        def vector_slab(l):
            def total(node, k):
                return column_sum(flip(sums[l, node, mat(k), :]))

            lat = stacked([total(node, k) for node in BOTH for k in THREE])
            biases = stacked([total(node, 3) for node in BOTH])
            n_lat = lat.shape[0]
            for d in range(GROUP):
                grad[l, VEC_SLAB, d * cols:d * cols + n_lat, :cols] = lat[:, rows_of(d)]
                grad[l, VEC_SLAB, d * cols + n_lat:d * cols + n_lat + 2, :] = biases

        def reduce_start(l, stage):
            for b in BOTH:
                core_copy(l, b, stage).start()

        def chip_sum(l, stage):
            row = lax.broadcasted_iota(jnp.int32, (cols, D), 0)
            edge_row = jnp.logical_or(row < 3, row == 6)
            core_all(l, stage).wait_recv()
            for b in BOTH:
                for k in range(SLABS)[STAGES[stage]]:
                    own = grad[l, k, rows_of(2 * b), :]
                    if k in EDGE_SLABS:
                        own = own + core_recv[l, b, k]
                    elif k == VEC_SLAB:
                        own = own + jnp.where(edge_row, core_recv[l, b, k], 0.0)
                    half[l, k, b] = own
            for i in dp_others:
                @pl.when(in_stage(lax.rem(p + i, dpn), stage))
                def _():
                    spread_copy(l, i).start()

        def dp_sum(l, stage):
            @pl.when(in_stage(p, stage))
            def _():
                total = half[l, pl.ds(seat(p) * per, per)]
                dp_all(l, 0).wait_recv()
                for i in dp_others:
                    total = total + dp_recv[l, pl.ds((i - 1) * per, per)]
                own_sum[l] = total[:, 0]
                cross_send[l] = total[:, 1]
                cross_copy(l).start()

        def cross_sum(l):
            cross_copy(l).wait_recv()
            total = own_sum[l] + cross_recv[l]
            own_sum[l] = total
            gathered[l, pl.ds(seat(p) * per, per)] = total
            for i in dp_others:
                gather_copy(l, i, p).start()

        def project(l):
            table = tables[l]

            def body(step):
                a = pl.ds(pl.multiple_of(step * TN, D), TN)
                s_bf, r_bf, v_in = s_sum[:, a].astype(BF), r_sum[:, a].astype(BF), table[:, a]
                part[layers + l, :, a] = dot(ew1[l, mat(1), :], s_bf) + dot(ew1[l, mat(2), :], r_bf)
                if l > 0:
                    part_piece(layers + l, a).start()
                grad[l, 6] += dot_nt(v_in, s_bf)
                grad[l, 7] += dot_nt(v_in, r_bf)

            loop(npad // TN, body)

        for l in reversed(range(layers)):
            first_layer = l == 0
            with jax.named_scope(f'node_backward_{l}'):
                node_backward(l)
            if first_layer:
                with jax.named_scope('chip_sum_1'):
                    chip_sum(1, 0)
                    chip_sum(1, 1)
            with jax.named_scope(f'gather_back_{l}'):
                gather_back()
            if first_layer:
                edges_sent(GRAD_IN)
            with jax.named_scope(f'edge_backward_{l}'):
                edge_backward(l)
            vector_slab(l)
            reduce_start(l, 0)
            if first_layer:
                with jax.named_scope('dp_sum_1'):
                    dp_sum(1, 0)
                    dp_sum(1, 1)
            with jax.named_scope(f'sum_send_{l}'):
                segment_sum(s_sum, scol)
            if first_layer:
                with jax.named_scope('chip_sum_0'):
                    chip_sum(0, 0)
            with jax.named_scope(f'sum_recv_{l}'):
                segment_sum(r_sum, rcol)
            with jax.named_scope(f'project_{l}'):
                project(l)
            reduce_start(l, 1)
            if first_layer:
                part_copy(layers + l).start()
            if first_layer:
                with jax.named_scope('chip_sum_late'):
                    chip_sum(0, 1)
                with jax.named_scope('dp_sum_0'):
                    dp_sum(0, 0)
            with jax.named_scope(f'back_wait_{l}'):
                part_copy(layers + l).wait_recv()

        def final(step):
            a = pl.ds(pl.multiple_of(step * TN, D), TN)
            d_in = (d_part[:, a] + part[layers, :, a] + swap_halves(part_recv[layers, :, a])).astype(BF)
            v2[:, a] = d_in

        loop(npad // TN, final)
        gnode_raw[x] = v2[:q, :nodes]
        with jax.named_scope('dp_sum_late'):
            dp_sum(0, 1)

        pack_nodes(take_rows(v2, rows_of(2)), dn_send)
        dn_copy = remote(dn_send, dn_recv, n_ss.at[2, 1], n_rs.at[2, 1], 2)
        dn_copy.start()

        def send_rest(j):
            for d in SEND_ORDER:
                edge_start(GRAD_OUT, j, d)

        loop(nch, send_rest, hold)

        with jax.named_scope('node_out_wait'):
            no_copy.wait_recv()
        unpack_nodes(no_recv, put_output(node_raw))

        def place_e(j):
            for d in OTHERS:
                place_edges(edge_raw, eo_recv[slot(d), j], d, j)

        with jax.named_scope('place_edge_out'):
            for group in THREE:
                group_arrived(EDGE_OUT, group)
            loop(nch, place_e)

        def place_g(j):
            for d in OTHERS:
                place_edges(gedge_raw, de_recv[slot(d), j], d, j)

        with jax.named_scope('place_first'):
            group_arrived(GRAD_OUT, 0)
            loop(hold, place_g)
        for l in range(layers):
            with jax.named_scope(f'cross_sum_{l}'):
                cross_sum(l)
        with jax.named_scope('d_node_wait'):
            dn_copy.wait_recv()
        unpack_nodes(dn_recv, put_output(gnode_raw))
        with jax.named_scope('place_rest'):
            group_arrived(GRAD_OUT, 1)
            loop(last, place_g, hold)
        for l in range(layers):
            dp_all(l, 1).wait_recv()
            ew1_buf[l, 0] = gathered[l, 0]
            ew1_buf[l, 1:] = gathered[l, EARLY:]
            ew2_buf[l] = gathered[l, 1]
            nw1_buf[l] = gathered[l, 2:4]
            nw2_buf[l] = gathered[l, 4]
            small = gathered[l, VEC_SLAB]
            for k in THREE:
                evec_buf[k, l:l + 1, :] = small[k:k + 1, :cols]
                nvec_buf[k, l:l + 1, :] = small[3 + k:4 + k, :cols]
            eb1_buf[l:l + 1, :] = small[6:7]
            nb1_buf[l:l + 1, :] = small[7:8]
        for l in range(layers):
            for stage in BOTH:
                core_all(l, stage).wait_send()
            cross_copy(l).wait_send()
            dp_all(l, 0).wait_send()
            dp_all(l, 1).wait_send()
        for copy in ncop + gcop + (w_pair, w_cross, w_relay):
            copy.wait_send()
        dp_all(0, 2).wait_send()
        no_copy.wait_send()
        dn_copy.wait_send()
        for k in range(2 * layers):
            part_copy(k).wait_send()
        edges_sent(EDGE_OUT)
        with jax.named_scope('place_last'):
            group_arrived(GRAD_OUT, 2)
            loop(nch, place_g, last)
        edges_sent(GRAD_OUT)

    bf = lambda *s: pltpu.VMEM(s, BF)
    pl.run_scoped(
        scoped, bf(D, eh), bf(D, eh), bf(D, eh), bf(D, eh), bf(D, npad), bf(D, npad), bf(D, npad), bf(D, npad), bf(D, npad), bf(D, npad),
        pltpu.VMEM((eh, D), I16), pltpu.VMEM((eh, D), I16), pltpu.VMEM((eh // D * 16, D), I16), pltpu.VMEM((eh // D * 16, D), I16),
        pltpu.VMEM((T, D), I16), pltpu.VMEM((16, D), I16),
        bf(layers, 3 * D, D), bf(layers, D, 3 * D), bf(layers, D, D), bf(layers, D, D),
        bf(layers, 2 * D, D), bf(layers, D, 2 * D), bf(layers, D, D), bf(layers, D, D), pltpu.VMEM((D, D), F32))


def finish_moves(src, dst):
    if len(src.shape) != 3 or src.dtype != BF:
        return [(src, dst)]
    return [(src.at[s, pl.ds(r, 8)], dst.at[s, pl.ds(r, 8)]) for s in range(src.shape[0]) for r in range(0, src.shape[1], 8)]


def finish_kernel(*refs):
    count = len(refs) // 2
    moves = sum((finish_moves(refs[k], refs[count + k]) for k in range(count)), [])
    puts = [pltpu.make_async_copy(src, dst, refs[-1]) for src, dst in moves]
    for put in puts:
        put.start()
    for put in puts:
        put.wait()


def keep_in_vmem(val):
    return pltpu.with_memory_space_constraint(val, pltpu.VMEM)


def finish(arrays):
    return pl.pallas_call(
        finish_kernel,
        name='finish',
        out_shape=[jax.ShapeDtypeStruct(a.shape, a.dtype) for a in arrays],
        in_specs=[VM] * len(arrays),
        out_specs=[HB] * len(arrays),
        scratch_shapes=[pltpu.SemaphoreType.DMA],
        compiler_params=pltpu.CompilerParams(vmem_limit_bytes=1 << 20),
    )(*[keep_in_vmem(a) for a in arrays])


def solution(mesh):
    lat_spec = P('dp', None, 'tp')
    first_spec = P(None, None, 'tp', None)
    col_spec = P(None, None, 'tp')
    param_specs = (first_spec, P(), col_spec, col_spec, first_spec, P(), col_spec, col_spec)
    in_specs = (lat_spec, lat_spec, P(), P(), lat_spec, lat_spec) + param_specs
    out_specs = (lat_spec, lat_spec, lat_spec, lat_spec) + param_specs
    shape = jax.ShapeDtypeStruct

    def local_step(node_lat, edge_lat, senders, receivers, grad_node, grad_edge, edge_w1, edge_b1, edge_w2, edge_vec, node_w1, node_b1, node_w2, node_vec):
        layers = edge_w1.shape[0]
        cols = node_lat.shape[2]
        nodes, edges = node_lat.shape[1], edge_lat.shape[1]
        npad = -(-nodes // TN) * TN
        eh = -(-edges // (2 * EC)) * EC
        nch = eh // EC
        dpn = mesh.shape['dp']
        per = SLABS // dpn
        dims = (layers, cols, nodes, edges, npad, eh, dpn)
        flat = lambda arr: jnp.swapaxes(arr, 1, 2)
        lead = lambda arr: jnp.transpose(arr, (1, 0, 2))
        args = (flat(node_lat), flat(edge_lat), flat(grad_node), flat(grad_edge), senders, receivers,
                edge_w1.reshape(-1, D), flat(edge_w2).reshape(-1, D), node_w1.reshape(-1, D), flat(node_w2).reshape(-1, D),
                lead(edge_vec), lead(node_vec), edge_b1, node_b1)
        vm, sem = pltpu.VMEM, pltpu.SemaphoreType.DMA
        packed = nodes // D * cols + -(-(nodes % D) * GROUP // D) * cols // GROUP
        wrows = -(-(HEAD + layers * LROWS) // (8 * dpn)) * 8 * dpn
        lat_n, lat_e = (2, cols, nodes), (2, cols, edges)
        outs = [RESULT(lat_n, BF), RESULT(lat_e, BF), RESULT(lat_n, BF), RESULT(lat_e, BF),
                RESULT((layers, 3, cols, D), F32), RESULT((layers, D), F32), RESULT((layers, cols, D), F32), RESULT((3, layers, cols), F32),
                RESULT((layers, 2, cols, D), F32), RESULT((layers, D), F32), RESULT((layers, cols, D), F32), RESULT((3, layers, cols), F32)]
        scratch = [
            *[vm(a.shape, a.dtype) for a in args[4:]], vm((wrows, D), F32), vm((3, wrows, D), F32),
            *[vm((many, packed, D), F32) for many in (2, 3, 2, 3)], *[vm((packed, D), F32)] * 4, vm((cols, npad), F32),
            vm((2, 3, cols + cols // GROUP, D), F32), vm((4, 3, cols + cols // GROUP, D), F32), *[vm((3, nch, cols, EC), F32)] * 6,
            vm((2 * layers, D, npad), F32), vm((2 * layers, D, npad), F32),
            vm((layers, D, eh), F32), vm((layers, D, eh), F32), vm((layers, eh), F32),
            vm((layers, D, npad), F32), vm((layers, D, npad), F32), vm((layers, npad), F32),
            vm((D, npad), F32), vm((D, npad), F32), vm((D, npad), F32), vm((2, 2 * eh), jnp.int32), vm((D, D), F32), vm((layers, 2, 4 * D, D), F32),
            vm((layers, SLABS, D, D), F32), vm((layers, 2, SLABS, cols, D), F32), vm((layers, SLABS, 2, cols, D), F32),
            vm((layers, (dpn - 1) * per, 2, cols, D), F32), vm((layers, per, cols, D), F32), vm((layers, per, cols, D), F32),
            vm((layers, per, cols, D), F32), vm((layers, SLABS, cols, D), F32),]
        own_sems = [
            sem((layers, 2)), sem((3, layers)), sem((layers,)), sem((3,)), sem((3, 3)), sem((2, nch)), sem((2, 5)), sem((2 * layers,)),
            pltpu.SemaphoreType.REGULAR,
            sem((len(args),)), sem((3,)), sem((3, 3)), sem((4, 4)), sem((2 * layers,)), sem((layers, 2)), sem((3, layers)), sem((layers,))]
        res = pl.pallas_call(
            lambda *refs: pl.run_scoped(lambda *own: step_kernel(dims, *refs, *own), *own_sems),
            name='graph_step',
            out_shape=outs,
            in_specs=[HB] * len(args),
            out_specs=[VM] * len(outs),
            scratch_shapes=scratch,
            compiler_params=pltpu.CompilerParams(collective_id=0, has_side_effects=True, vmem_limit_bytes=VMEM_LIMIT),
        )(*args)

        res = finish(res)
        return (flat(res[0]), flat(res[1]), flat(res[2]), flat(res[3]),
                res[4], res[5], flat(res[6]), lead(res[7]), res[8], res[9], flat(res[10]), lead(res[11]))

    return jax.shard_map(local_step, mesh=mesh, in_specs=in_specs, out_specs=out_specs, check_vma=False)
```

```python
import jax
import jax.numpy as jnp
from jax import lax
from jax.experimental import pallas as pl
from jax.experimental.pallas import tpu as pltpu
from jax.sharding import PartitionSpec as P

LN_EPS = 1e-5
D = 128
T = 256
TN = 384
EC = 512
KS = 1408
BF = jnp.bfloat16
F32 = jnp.float32
I16 = jnp.int16
MESH = pl.DeviceIdType.MESH
VM = pl.BlockSpec(memory_space=pltpu.VMEM)
HB = pl.BlockSpec(memory_space=pl.ANY)
RESULT = pltpu.VMEM
GROUP = 4
BOTH = (0, 1)
THREE = (0, 1, 2)
OTHERS = (1, 2, 3)
EDGE_IN, GRAD_IN, EDGE_OUT, GRAD_OUT = range(4)
SEND_ORDER = (2, 3, 1)
LROWS = 7 * (D // 4)
HEAD = 16
LEADER = GROUP - 1
HELPER = LEADER - 1
VMEM_LIMIT = 63_000_000
SLABS = 8
EARLY = 6
VEC_SLAB = 5
EDGE_SLABS = (0, 1, 6, 7)
STAGES = (slice(0, EARLY), slice(EARLY, SLABS))


def dot(a, b):
    return jnp.dot(a, b, preferred_element_type=F32)


def dot_nt(a, b):
    return lax.dot_general(a, b, (((1,), (1,)), ((), ())), preferred_element_type=F32)


def mat(k, n=1):
    return slice(k * D, (k + n) * D)


def rows_of(d):
    q = D // 4
    return slice(d * q, (d + 1) * q)


def at(step, width):
    return pl.ds(pl.multiple_of(step * width, width), width)


def loop(stop, body, start=0):
    def step(j, carry):
        body(j)
        return carry

    lax.fori_loop(start, stop, step, 0)


def column_sum(val):
    return jnp.sum(val, axis=0, keepdims=True)


def flip(val):
    return jnp.swapaxes(val, 0, 1)


def stacked(parts):
    return jnp.concatenate(parts, axis=0)


def beside(parts):
    return jnp.concatenate(parts, axis=1)


def slot(d):
    return d - 1


def sigmoid(hidden):
    return 1.0 / (1.0 + jnp.exp(-hidden))


def fold(val):
    total = val[:, mat(0)]
    for start in range(D, val.shape[1], D):
        total = total + val[:, start:start + D]
    return total


def swap_halves(val):
    return stacked([val[rows_of(d)] for d in (1, 0, 3, 2)])


def gather(table, keys, iota):
    acc = None
    nodes = table.shape[1]
    one, zero = jnp.ones((), BF), jnp.zeros((), BF)
    for base in range(0, nodes, T):
        width = min(T, nodes - base)
        ids = iota[0:width, :]
        hot = beside([jnp.where(ids == (key - jnp.asarray(base, I16)), one, zero) for key in keys])
        part = dot(table[:, base:base + width], hot)
        acc = part if acc is None else acc + part
    return acc


def scatter(acc_ref, val, cols, lanes):
    nodes = acc_ref.shape[1]
    one, zero = jnp.ones((), BF), jnp.zeros((), BF)
    row = lanes[0:1, :]
    for base in range(0, nodes, T):
        width = min(T, nodes - base)
        hot = beside([jnp.where((row + jnp.asarray(base + s, I16)) == cols, one, zero) for s in range(0, width, D)])
        acc_ref[:, base:base + width] += dot(val, hot)


def mlp_tail(hidden, w2t, vec):
    act = (hidden * sigmoid(hidden)).astype(BF)
    out = dot(w2t, act) + vec[0]
    mean = column_sum(out) / D
    centered = out - mean
    var = column_sum(centered * centered) / D
    inv = lax.rsqrt(var + LN_EPS)
    normed = centered * inv
    message = (normed * vec[1] + vec[2]).astype(BF)
    return message, normed, inv


def mlp_back(d_msg, hidden, normed, inv, w2, vec):
    d_normed = d_msg * vec[1]
    mean0 = column_sum(d_normed) / D
    mean1 = column_sum(d_normed * normed) / D
    d_out = inv * (d_normed - mean0 - normed * mean1)
    d_out_bf = d_out.astype(BF)
    sig = sigmoid(hidden)
    act = (hidden * sig).astype(BF)
    d_w2 = dot_nt(d_out_bf, act)
    d_hidden = dot(w2, d_out_bf) * (sig * (1.0 + hidden * (1.0 - sig)))
    sums = (fold(d_out), fold(d_msg * normed), fold(d_msg), fold(d_hidden))
    return d_hidden.astype(BF), d_w2, sums


def add_sums(ref, parts):
    for q in range(4):
        total = parts[0][q]
        for other in parts[1:]:
            total = total + other[q]
        ref[mat(q), :] += total


def step_kernel(dims, *refs):
    layers, cols, nodes, edges, npad, eh, dpn = dims
    nch = eh // EC
    top = layers - 1
    n_in = 14
    hbm_in = refs[:n_in]
    n_out = 12
    (node_raw, edge_raw, gnode_raw, gedge_raw, ew1_buf, eb1_buf, ew2_buf, evec_buf, nw1_buf, nb1_buf, nw2_buf, nvec_buf) = refs[n_in:n_in + n_out]
    (send_ids, recv_ids, ew1_in, ew2_in, nw1_in, nw2_in, evec_in, nvec_in, eb1_in, nb1_in, w_send, w_recv, n_send, n_recv, gn_send, gn_recv, no_send, no_recv, dn_send, dn_recv,
     node_pad, t_send, t_recv, e_send, g_send, e_recv, g_recv, eo_recv, de_recv, part, part_recv, hidden, normed, inv, nhid, nnrm, ninv, d_part, s_sum, r_sum,
     ids_raw, bias_cols, sums, grad, core_recv, half, dp_recv, cross_send, cross_recv, own_sum, gathered,
     core_rs, dp_rs, cross_rs, w_rs, n_rs, e_rs, o_rs, p_rs, ready, load_sem, w_ss, n_ss, e_ss, p_ss, core_ss, dp_ss, cross_ss) = refs[n_in + n_out:]

    t = lax.axis_index('tp')
    p = lax.axis_index('dp')
    per = SLABS // dpn
    dp_others = range(1, dpn)
    x, c = t // 2, lax.rem(t, 2)
    ox, oc = 1 - x, 1 - c
    peer = [t, t + 1 - 2 * c, t + 2 - 4 * x, t + 3 - 2 * c - 4 * x]

    def remote(src, dst, ssem, rsem, d):
        return pltpu.make_async_remote_copy(src_ref=src, dst_ref=dst, send_sem=ssem, recv_sem=rsem,
                                            device_id={'tp': peer[d]}, device_id_type=MESH)

    small_in = (send_ids, recv_ids, ew1_in, ew2_in, nw1_in, nw2_in, evec_in, nvec_in, eb1_in, nb1_in)
    loads = [pltpu.make_async_copy(src, dst, load_sem.at[q]) for q, (src, dst) in enumerate(
        zip((hbm_in[0].at[x],) + hbm_in[1:], (node_raw.at[x], edge_raw, gnode_raw, gedge_raw) + small_in))]
    first_load = pltpu.make_async_copy(hbm_in[0].at[ox], node_raw.at[ox], load_sem.at[n_in])

    def node_copies(send, recv, kind):
        return (remote(send.at[1], recv.at[0], n_ss.at[kind, 0], n_rs.at[kind, 0], 1),
                remote(send.at[0], recv.at[1], n_ss.at[kind, 1], n_rs.at[kind, 1], 2),
                remote(recv.at[1], recv.at[2], n_ss.at[kind, 2], n_rs.at[kind, 2], 1))

    piece = w_send.shape[0] // dpn

    def packed(l, k, count=1):
        return pl.ds(HEAD + l * LROWS + k * cols, count * cols)

    def weight_rows(owner):
        return pl.ds(pl.multiple_of(owner * piece, 8), piece)

    w_pair = remote(w_send, w_recv.at[0], w_ss.at[0], w_rs.at[0], 1)
    w_cross = remote(w_send.at[weight_rows(p)], w_recv.at[1, weight_rows(p)], w_ss.at[1], w_rs.at[1], 2)
    w_relay = remote(w_recv.at[1], w_recv.at[2], w_ss.at[2], w_rs.at[2], 1)

    def weight_copy(i, owner):
        rows = w_recv.at[1, weight_rows(owner)]
        return dp_remote(rows, rows, 2, 0, i)

    last = nch - 1
    hold = nch - 3
    buffers = ((e_send, e_recv), (g_send, g_recv), (e_send, eo_recv), (g_send, de_recv))

    def outward(kind):
        return kind in (EDGE_OUT, GRAD_OUT)

    every = slice(None)
    ragged = pl.ds(D, D // GROUP)
    rest = [slice(g * cols // GROUP, (g + 1) * cols // GROUP) for g in range(GROUP)]

    def edge_part(kind, which, j, tail, send_sem, recv_sem, d):
        src, dst = buffers[kind]
        if tail:
            src, dst = t_send.at[kind % 2, which], t_recv.at[kind, which]
        else:
            src, dst = src.at[which, j], dst.at[which, j]
        recv_sems = o_rs.at[kind - EDGE_OUT, recv_sem] if outward(kind) else e_rs.at[kind, recv_sem]
        return remote(src, dst, e_ss.at[kind, send_sem], recv_sems, d)

    def by_half(half_id, j, action):
        narrow = jnp.logical_and(j == last, half_id == 1)

        @pl.when(jnp.logical_not(narrow))
        def _():
            action(False)

        @pl.when(narrow)
        def _():
            action(True)

    def pack_tail(kind, d):
        src, out = buffers[kind][0].at[slot(d), last], t_send.at[kind % 2, slot(d)]
        out[:cols, :] = src[:, :D]
        over = src[:, ragged]
        out[cols:, :] = beside([over[r] for r in rest])

    def unpack_tail(kind, d):
        src, out = t_recv.at[kind, slot(d)], buffers[kind][1].at[slot(d), last]
        out[:, :D] = src[:cols, :]
        over = src[cols:, :]
        out[:, ragged] = stacked([over[:, rows_of(g)] for g in range(GROUP)])

    def edge_start(kind, j, d):
        other = oc if d % 2 else c
        if outward(kind):
            send_sem, recv_sem = jnp.where(j == last, 1, 0), jnp.where(j == last, 2 + slot(d), jnp.where(j < hold, 0, 1))
        else:
            send_sem, recv_sem = jnp.where(j == last, d, 0), j

        def start(tail):
            if tail:
                pack_tail(kind, d)
            edge_part(kind, slot(d), j, tail, send_sem, recv_sem, d).start()

        by_half(c if outward(kind) else other, j, start)

    def edges_sent(kind):
        edge_part(kind, every, slice(0, last), False, 0, 0, 1).wait_send()
        if outward(kind):
            by_half(c, last, lambda tail: edge_part(kind, every, last, tail, 1, 0, 1).wait_send())
        else:
            for d in OTHERS:
                by_half(oc if d % 2 else c, last, lambda tail: edge_part(kind, slot(d), last, tail, d, 0, d).wait_send())

    def chunk_arrived(kind, j):
        def arrived(tail):
            edge_part(kind, every, j, tail, 0, j, 1).wait_recv()
            if tail:
                for d in OTHERS:
                    unpack_tail(kind, d)

        by_half(c, j, arrived)

    def group_arrived(kind, group):
        if group < 2:
            edge_part(kind, every, (slice(0, hold), slice(hold, last))[group], False, 0, group, 1).wait_recv()
        else:
            for d in OTHERS:
                def arrived(tail):
                    edge_part(kind, slot(d), last, tail, 0, 2 + slot(d), d).wait_recv()
                    if tail:
                        unpack_tail(kind, d)

                by_half(oc if d % 2 else c, last, arrived)

    def core_copy(l, b, stage):
        first, count = ((0, EARLY), (EARLY, SLABS - EARLY))[stage]
        return remote(grad.at[l, pl.ds(first, count), pl.ds((2 * b + 1) * cols, cols), :], core_recv.at[l, b, pl.ds(first, count)],
                      core_ss.at[l, stage], core_rs.at[l, stage], 1)

    def core_all(l, stage):
        part_of = core_recv.at[l, :, (slice(0, EARLY), slice(EARLY, SLABS))[stage]]
        return remote(part_of, part_of, core_ss.at[l, stage], core_rs.at[l, stage], 1)

    def seat(device):
        return lax.rem(device + dpn // 2, dpn)

    def in_stage(device, stage):
        early = (seat(device) + 1) * per <= EARLY
        return jnp.logical_not(early) if stage else early

    def dp_remote(src, dst, stage, l, i):
        return pltpu.make_async_remote_copy(src_ref=src, dst_ref=dst, send_sem=dp_ss.at[stage, l], recv_sem=dp_rs.at[stage, l],
                                            device_id={'dp': lax.rem(p + i, dpn)}, device_id_type=MESH)

    def spread_copy(l, i):
        return dp_remote(half.at[l, pl.ds(seat(lax.rem(p + i, dpn)) * per, per)], dp_recv.at[l, pl.ds((i - 1) * per, per)], 0, l, i)

    def dp_all(l, stage):
        most = (dpn - 1) * per
        part_of = (dp_recv.at[l], gathered.at[l, pl.ds(0, most)], w_recv.at[1, pl.ds(0, (dpn - 1) * piece)])[stage]
        return dp_remote(part_of, part_of, stage, l, 1)

    def cross_copy(l):
        return remote(cross_send.at[l], cross_recv.at[l], cross_ss.at[l], cross_rs.at[l], 2)

    def gather_copy(l, i, owner):
        return dp_remote(own_sum.at[l], gathered.at[l, pl.ds(seat(owner) * per, per)], 1, l, i)

    def part_piece(q, a):
        return remote(part.at[q, :, a], part_recv.at[q, :, a], p_ss.at[q], p_rs.at[q], 1)

    def part_copy(q):
        return remote(part.at[q], part_recv.at[q], p_ss.at[q], p_rs.at[q], 1)

    wide = D // GROUP
    tiles = nodes // D
    over = range(tiles * D, nodes, wide)

    def node_rows(k):
        return slice(k * cols, (k + 1) * cols) if k < tiles else pl.ds(tiles * cols + (k - tiles) * cols // GROUP, cols // GROUP)

    def pack_nodes(take, out):
        for k in range(tiles):
            out[node_rows(k), :] = take(k * D, D)
        for k, start in enumerate(over):
            val = take(start, wide)
            out[node_rows(tiles + k), :] = beside([val[r] for r in rest])

    def unpack_nodes(src, put):
        for k in range(tiles):
            put(k * D, src[node_rows(k), :])
        for k, start in enumerate(over):
            val = src[node_rows(tiles + k), :]
            put(start, stacked([val[:, rows_of(g)] for g in range(GROUP)]))

    def put_rows(ref, rows):
        def put(start, val):
            ref[rows, start:start + val.shape[1]] = val.astype(ref.dtype)

        return put

    def put_output(ref):
        def put(start, val):
            used = min(val.shape[1], nodes - start)
            ref[ox, :, start:start + used] = val[:, :used].astype(ref.dtype)

        return put

    def take_rows(ref, rows):
        return lambda start, width: ref[rows, start:start + width].astype(F32)

    def load_nodes(raw, sample, out):
        node_pad[:, :nodes] = raw[sample].astype(F32)
        pack_nodes(take_rows(node_pad, every), out)

    def keep_nodes(own):
        own[...] = jnp.zeros_like(own)
        own[:cols, :] = node_pad[...].astype(own.dtype)

    def load_edges(raw, send, own, kind):
        def put(j, lanes_j, val_of):
            for d in OTHERS:
                sample = x if d < 2 else ox
                send[slot(d), j] = val_of(sample, oc if d % 2 else c).astype(F32)
            own[:cols, lanes_j] = val_of(x, c)

        def chunk(j):
            put(j, at(j, EC), lambda s, h: raw[s, :, pl.ds(pl.multiple_of(h * eh + j * EC, D), EC)])
            for d in SEND_ORDER:
                edge_start(kind, j, d)

        loop(nch - 1, chunk)
        first = (nch - 1) * EC
        used = edges - eh - first
        last = pl.ds(first, EC)

        def tail(s, h):
            left = raw[s, :, pl.ds(first, EC)]
            right = beside([raw[s, :, pl.ds(eh + first, used)], jnp.zeros((cols, EC - used), BF)])
            return jnp.where(h == 0, left.astype(F32), right.astype(F32)).astype(BF)

        put(nch - 1, last, tail)
        for d in SEND_ORDER:
            edge_start(kind, nch - 1, d)

    def place_edges(raw, block, d, j):
        s = x if d < 2 else ox
        h = oc if d % 2 else c
        val = block.astype(BF)
        first = (nch - 1) * EC
        used = edges - eh - first

        @pl.when(jnp.logical_or(j < nch - 1, h == 0))
        def _():
            raw[s, :, pl.ds(pl.multiple_of(h * eh + j * EC, D), EC)] = val

        @pl.when(jnp.logical_and(j == nch - 1, h == 1))
        def _():
            raw[s, :, pl.ds(eh + first, used)] = val[:, :used]

    def scoped(e0, e1, ge, msg, v0, v1, v2, agg0, agg1, d_agg, scol, rcol, srow, rrow, iota, lanes, ew1, ew1t, ew2, ew2t, nw1, nw1t, nw2, nw2t, vecs):
        tables = (v0, v1, v2)
        aggs = (agg0, agg1)
        edges_in = (e0, e1)

        barrier = pltpu.get_barrier_semaphore()
        for d in OTHERS:
            pl.semaphore_signal(barrier, device_id={'tp': peer[d]}, device_id_type=MESH)
        for copy in [first_load] + loads[:1] + loads[4:] + loads[1:4]:
            copy.start()
        node_pad[...] = jnp.zeros_like(node_pad)
        with jax.named_scope('barrier'):
            @pl.when(t != LEADER)
            def _():
                pl.semaphore_wait(barrier, len(OTHERS))

            @pl.when(t == HELPER)
            def _():
                pl.semaphore_signal(ready, device_id={'tp': LEADER}, device_id_type=MESH)

            @pl.when(t == LEADER)
            def _():
                pl.semaphore_wait(ready, 1)

        first_load.wait()
        with jax.named_scope('send_nodes'):
            load_nodes(node_raw, ox, n_send.at[0])
        ncop = node_copies(n_send, n_recv, 0)
        ncop[1].start()
        loads[0].wait()
        load_nodes(node_raw, x, n_send.at[1])
        keep_nodes(v0)
        ncop[0].start()
        for copy in loads[4:]:
            copy.wait()
        q = cols
        w_send[:HEAD, :] = jnp.zeros((HEAD, D), F32)
        for k in THREE:
            w_send[k * layers:(k + 1) * layers, :cols] = evec_in[k]
            w_send[(3 + k) * layers:(4 + k) * layers, :cols] = nvec_in[k]
        for l in range(layers):
            w_send[packed(l, 0, 3), :] = ew1_in[pl.ds(l * 3 * q, 3 * q), :].astype(F32)
            w_send[packed(l, 3), :] = ew2_in[pl.ds(l * q, q), :].astype(F32)
            w_send[packed(l, 4, 2), :] = nw1_in[pl.ds(l * 2 * q, 2 * q), :].astype(F32)
            w_send[packed(l, 6), :] = nw2_in[pl.ds(l * q, q), :].astype(F32)
        w_cross.start()
        w_pair.start()
        loads[1].wait()
        with jax.named_scope('send_edges'):
            load_edges(edge_raw, e_send, e0, EDGE_IN)
        loads[2].wait()
        load_nodes(gnode_raw, ox, gn_send.at[0])
        load_nodes(gnode_raw, x, gn_send.at[1])
        keep_nodes(d_part)
        gcop = node_copies(gn_send, gn_recv, 1)
        gcop[1].start()
        gcop[0].start()
        loads[3].wait()
        with jax.named_scope('send_grads'):
            load_edges(gedge_raw, g_send, ge, GRAD_IN)

        with jax.named_scope('dp_barrier'):
            @pl.when(t == LEADER)
            def _():
                for i in dp_others:
                    pl.semaphore_signal(barrier, device_id={'dp': lax.rem(p + i, dpn)}, device_id_type=MESH)
                pl.semaphore_wait(barrier, len(OTHERS) + dpn - 1)
                for d in OTHERS:
                    pl.semaphore_signal(ready, device_id={'tp': peer[d]}, device_id_type=MESH)

            @pl.when(t != LEADER)
            def _():
                pl.semaphore_wait(ready, 1)

        w_cross.wait_recv()
        for i in dp_others:
            weight_copy(i, p).start()

        @pl.when(c == 1)
        def _():
            for recv in (e_recv, g_recv):
                recv[:, last, :, D:] = jnp.zeros((len(OTHERS), cols, EC - D), F32)

        iota[...] = lax.broadcasted_iota(jnp.int32, (T, D), 0).astype(I16)
        lanes[...] = lax.broadcasted_iota(jnp.int32, (16, D), 1).astype(I16)

        ids_raw[...] = jnp.full(ids_raw.shape, -1, jnp.int32)
        for which, src in enumerate((send_ids, recv_ids)):
            ids_raw[which:which + 1, :edges] = src[...].reshape(1, edges)

        def ids(b):
            for which, (row_ref, col_ref) in enumerate(((srow, scol), (rrow, rcol))):
                wide = jnp.broadcast_to(ids_raw[which:which + 1, pl.ds(pl.multiple_of(c * eh + b * D, D), D)], (D, D))
                row_ref[at(b, 16), :] = wide[:16].astype(I16)
                col_ref[at(b, D), :] = flip(wide.astype(F32)).astype(jnp.int32).astype(I16)

        with jax.named_scope('ids'):
            loop(eh // D, ids)

        def keys(ref, step):
            return [ref[pl.ds(pl.multiple_of(step * (KS // D) * 16 + 16 * h, 16), 1), :] for h in range(KS // D)]

        bias_cols[...] = flip(stacked([eb1_in[...], nb1_in[...], jnp.zeros((D - 2 * layers, D), F32)]))

        def join_weights(l):
            for d in range(GROUP):
                src = w_recv.at[slot(d)] if d else w_send
                r = rows_of(d)
                for k in THREE:
                    ew1[l, pl.ds(k * D + d * q, q), :] = src[packed(l, k), :].astype(BF)
                ew2t[l, r, :] = src[packed(l, 3), :].astype(BF)
                for k in BOTH:
                    nw1[l, pl.ds(k * D + d * q, q), :] = src[packed(l, 4 + k), :].astype(BF)
                nw2t[l, r, :] = src[packed(l, 6), :].astype(BF)

            def flip_bf(mat):
                return flip(mat.astype(F32)).astype(BF)

            for k in THREE:
                ew1t[l, :, mat(k)] = flip_bf(ew1[l, mat(k), :])
            for k in BOTH:
                nw1t[l, :, mat(k)] = flip_bf(nw1[l, mat(k), :])
            ew2[l] = flip_bf(ew2t[l])
            nw2[l] = flip_bf(nw2t[l])

        def wait_recvs(copies):
            copies[1].wait_recv()
            copies[2].start()
            copies[0].wait_recv()
            copies[2].wait_recv()

        with jax.named_scope('node_wait'):
            wait_recvs(ncop)
        for d in OTHERS:
            unpack_nodes(n_recv.at[slot(d)], put_rows(v0, rows_of(d)))
        with jax.named_scope('weight_wait'):
            dp_all(0, 2).wait_recv()
            w_relay.start()
            w_pair.wait_recv()
            w_relay.wait_recv()
        rows_all = beside([w_send[:HEAD, :cols]] + [w_recv[d, :HEAD, :cols] for d in range(3)])
        vecs[...] = flip(stacked([rows_all, jnp.zeros((D - HEAD, D), F32)]))
        join_weights(0)

        def vec(l, node):
            first = 6 * node + l
            return [vecs[:, first + 2 * k:first + 2 * k + 1] for k in THREE]

        def bias(l, node):
            return bias_cols[:, node * layers + l:node * layers + l + 1]

        def hidden_of_nodes(l):
            table, b1 = tables[l], bias(l, 0)

            def body(step):
                xs = gather(table, keys(srow, step), iota).astype(BF)
                xr = gather(table, keys(rrow, step), iota).astype(BF)
                hidden[l, :, at(step, KS)] = dot(ew1t[l, :, mat(1, 2)], stacked([xs, xr])) + b1

            loop(eh // KS, body)

        def edge_forward(l):
            e_in = edges_in[l]

            def body(j):
                for sub in range(EC // T):
                    a = at(j * (EC // T) + sub, T)
                    if l == 0:
                        if sub == 0:
                            chunk_arrived(EDGE_IN, j)
                        for d in OTHERS:
                            e_in[rows_of(d), a] = e_recv[slot(d), j, :, sub * T:(sub + 1) * T].astype(BF)
                    e_val = e_in[:, a]
                    hid = hidden[l, :, a] + dot(ew1t[l, :, mat(0)], e_val)
                    hidden[l, :, a] = hid
                    message, nrm, std = mlp_tail(hid, ew2t[l], vec(l, 0))
                    normed[l, :, a] = nrm
                    inv[l:l + 1, a] = std
                    msg[:, a] = message
                    e_new = (e_val.astype(F32) + message.astype(F32)).astype(BF)
                    if l < top:
                        edges_in[l + 1][:, a] = e_new
                    else:
                        for d in OTHERS:
                            e_send[slot(d), j, :, sub * T:(sub + 1) * T] = e_new[rows_of(d)].astype(F32)
                        if sub == 0:
                            own_parts = []
                        own_parts.append(e_new[:q])
                if l == top:
                    for d in SEND_ORDER:
                        edge_start(EDGE_OUT, j, d)
                    place_edges(edge_raw, beside(own_parts), 0, j)

            loop(nch, body)

        def segment_sum(acc, ids_ref):
            acc[...] = jnp.zeros(acc.shape, F32)

            def body(step):
                scatter(acc, msg[:, at(step, KS)], ids_ref[at(step, KS), :], lanes)

            loop(eh // KS, body)

        def node_forward(l):
            table, agg, out = tables[l], aggs[l], tables[l + 1]

            def body(step):
                a = pl.ds(pl.multiple_of(step * TN, D), TN)
                v_in = table[:, a]
                agg_bf = (part[l, :, a] + swap_halves(part_recv[l, :, a])).astype(BF)
                agg[:, a] = agg_bf
                hid = dot(nw1t[l], stacked([v_in, agg_bf])) + bias(l, 1)
                nhid[l, :, a] = hid
                message, nrm, std = mlp_tail(hid, nw2t[l], vec(l, 1))
                nnrm[l, :, a] = nrm
                ninv[l:l + 1, a] = std
                out[:, a] = (v_in.astype(F32) + message.astype(F32)).astype(BF)

            loop(npad // TN, body)

        for l in range(layers):
            with jax.named_scope(f'gather_{l}'):
                hidden_of_nodes(l)
            if l == top:
                edges_sent(EDGE_IN)
            with jax.named_scope(f'edge_forward_{l}'):
                edge_forward(l)
            with jax.named_scope(f'sum_{l}'):
                segment_sum(part.at[l], rcol)
            part_copy(l).start()
            if l == 0:
                join_weights(1)
                gcop[1].wait_recv()
                gcop[2].start()
            with jax.named_scope(f'part_wait_{l}'):
                part_copy(l).wait_recv()
            with jax.named_scope(f'node_forward_{l}'):
                node_forward(l)
        pack_nodes(take_rows(tables[layers], rows_of(2)), no_send)
        no_copy = remote(no_send, no_recv, n_ss.at[2, 0], n_rs.at[2, 0], 2)
        no_copy.start()
        node_raw[x] = tables[layers][:q, :nodes]

        grad[...] = jnp.zeros_like(grad)
        sums[...] = jnp.zeros_like(sums)
        with jax.named_scope('grad_node_wait'):
            gcop[0].wait_recv()
            gcop[2].wait_recv()
        for d in OTHERS:
            unpack_nodes(gn_recv.at[slot(d)], put_rows(d_part, rows_of(d)))

        def node_backward(l):
            table, agg = tables[l], aggs[l]

            def body(step):
                a = pl.ds(pl.multiple_of(step * TN, D), TN)
                d_in = d_part[:, a]
                if l < top:
                    d_in = d_in + part[layers + l + 1, :, a] + swap_halves(part_recv[layers + l + 1, :, a])
                    d_in = d_in.astype(BF).astype(F32)
                d_hid, d_w2, parts = mlp_back(d_in, nhid[l, :, a], nnrm[l, :, a], ninv[l:l + 1, a], nw2[l], vec(l, 1))
                add_sums(sums.at[l, 1], [parts])
                grad[l, 4] += d_w2
                grad[l, 2] += dot_nt(table[:, a], d_hid)
                grad[l, 3] += dot_nt(agg[:, a], d_hid)
                d_part[:, a] = d_in + dot(nw1[l, mat(0), :], d_hid)
                d_agg[:, a] = dot(nw1[l, mat(1), :], d_hid).astype(BF)

            loop(npad // TN, body)

        def gather_back():
            def body(step):
                msg[:, at(step, KS)] = gather(d_agg, keys(rrow, step), iota).astype(BF)

            loop(eh // KS, body)

        def edge_backward(l):
            e_in = edges_in[l]

            def body(j):
                all_parts, d_w2s, d_w1s, own_parts = [], [], [], []
                for sub in range(EC // T):
                    a = at(j * (EC // T) + sub, T)
                    if l == top:
                        if sub == 0:
                            chunk_arrived(GRAD_IN, j)
                        for d in OTHERS:
                            ge[rows_of(d), a] = g_recv[slot(d), j, :, sub * T:(sub + 1) * T].astype(BF)
                    d_res = ge[:, a].astype(F32)
                    d_msg = d_res + msg[:, a].astype(F32)
                    d_hid, d_w2, parts = mlp_back(d_msg, hidden[l, :, a], normed[l, :, a], inv[l:l + 1, a], ew2[l], vec(l, 0))
                    all_parts.append(parts)
                    d_w2s.append(d_w2)
                    d_w1s.append(dot_nt(e_in[:, a], d_hid))
                    msg[:, a] = d_hid
                    d_new = (d_res + dot(ew1[l, mat(0), :], d_hid)).astype(BF)
                    if l > 0:
                        ge[:, a] = d_new
                    else:
                        for d in OTHERS:
                            g_send[slot(d), j, :, sub * T:(sub + 1) * T] = d_new[rows_of(d)].astype(F32)
                        own_parts.append(d_new[:q])
                add_sums(sums.at[l, 0], all_parts)
                grad[l, 1] += sum(d_w2s[1:], d_w2s[0])
                grad[l, 0] += sum(d_w1s[1:], d_w1s[0])
                if l == 0:
                    @pl.when(j < hold)
                    def _():
                        for d in SEND_ORDER:
                            edge_start(GRAD_OUT, j, d)
                    place_edges(gedge_raw, beside(own_parts), 0, j)

            loop(nch, body)

        def vector_slab(l):
            def total(node, k):
                return column_sum(flip(sums[l, node, mat(k), :]))

            lat = stacked([total(node, k) for node in BOTH for k in THREE])
            biases = stacked([total(node, 3) for node in BOTH])
            n_lat = lat.shape[0]
            for d in range(GROUP):
                grad[l, VEC_SLAB, d * cols:d * cols + n_lat, :cols] = lat[:, rows_of(d)]
                grad[l, VEC_SLAB, d * cols + n_lat:d * cols + n_lat + 2, :] = biases

        def reduce_start(l, stage):
            for b in BOTH:
                core_copy(l, b, stage).start()

        def chip_sum(l, stage):
            row = lax.broadcasted_iota(jnp.int32, (cols, D), 0)
            edge_row = jnp.logical_or(row < 3, row == 6)
            core_all(l, stage).wait_recv()
            for b in BOTH:
                for k in range(SLABS)[STAGES[stage]]:
                    own = grad[l, k, rows_of(2 * b), :]
                    if k in EDGE_SLABS:
                        own = own + core_recv[l, b, k]
                    elif k == VEC_SLAB:
                        own = own + jnp.where(edge_row, core_recv[l, b, k], 0.0)
                    half[l, k, b] = own
            for i in dp_others:
                @pl.when(in_stage(lax.rem(p + i, dpn), stage))
                def _():
                    spread_copy(l, i).start()

        def dp_sum(l, stage):
            @pl.when(in_stage(p, stage))
            def _():
                total = half[l, pl.ds(seat(p) * per, per)]
                dp_all(l, 0).wait_recv()
                for i in dp_others:
                    total = total + dp_recv[l, pl.ds((i - 1) * per, per)]
                own_sum[l] = total[:, 0]
                cross_send[l] = total[:, 1]
                cross_copy(l).start()

        def cross_sum(l):
            cross_copy(l).wait_recv()
            total = own_sum[l] + cross_recv[l]
            own_sum[l] = total
            gathered[l, pl.ds(seat(p) * per, per)] = total
            for i in dp_others:
                gather_copy(l, i, p).start()

        def project(l):
            table = tables[l]

            def body(step):
                a = pl.ds(pl.multiple_of(step * TN, D), TN)
                s_bf, r_bf, v_in = s_sum[:, a].astype(BF), r_sum[:, a].astype(BF), table[:, a]
                part[layers + l, :, a] = dot(ew1[l, mat(1), :], s_bf) + dot(ew1[l, mat(2), :], r_bf)
                if l > 0:
                    part_piece(layers + l, a).start()
                grad[l, 6] += dot_nt(v_in, s_bf)
                grad[l, 7] += dot_nt(v_in, r_bf)

            loop(npad // TN, body)

        for l in reversed(range(layers)):
            first_layer = l == 0
            with jax.named_scope(f'node_backward_{l}'):
                node_backward(l)
            if first_layer:
                with jax.named_scope('chip_sum_1'):
                    chip_sum(1, 0)
                    chip_sum(1, 1)
            with jax.named_scope(f'gather_back_{l}'):
                gather_back()
            if first_layer:
                edges_sent(GRAD_IN)
            with jax.named_scope(f'edge_backward_{l}'):
                edge_backward(l)
            vector_slab(l)
            reduce_start(l, 0)
            if first_layer:
                with jax.named_scope('dp_sum_1'):
                    dp_sum(1, 0)
                    dp_sum(1, 1)
            with jax.named_scope(f'sum_send_{l}'):
                segment_sum(s_sum, scol)
            if first_layer:
                with jax.named_scope('chip_sum_0'):
                    chip_sum(0, 0)
            with jax.named_scope(f'sum_recv_{l}'):
                segment_sum(r_sum, rcol)
            with jax.named_scope(f'project_{l}'):
                project(l)
            reduce_start(l, 1)
            if first_layer:
                part_copy(layers + l).start()
            if first_layer:
                with jax.named_scope('chip_sum_late'):
                    chip_sum(0, 1)
                with jax.named_scope('dp_sum_0'):
                    dp_sum(0, 0)
            with jax.named_scope(f'back_wait_{l}'):
                part_copy(layers + l).wait_recv()

        def final(step):
            a = pl.ds(pl.multiple_of(step * TN, D), TN)
            d_in = (d_part[:, a] + part[layers, :, a] + swap_halves(part_recv[layers, :, a])).astype(BF)
            v2[:, a] = d_in

        loop(npad // TN, final)
        gnode_raw[x] = v2[:q, :nodes]
        with jax.named_scope('dp_sum_late'):
            dp_sum(0, 1)

        pack_nodes(take_rows(v2, rows_of(2)), dn_send)
        dn_copy = remote(dn_send, dn_recv, n_ss.at[2, 1], n_rs.at[2, 1], 2)
        dn_copy.start()

        def send_rest(j):
            for d in SEND_ORDER:
                edge_start(GRAD_OUT, j, d)

        loop(nch, send_rest, hold)

        with jax.named_scope('node_out_wait'):
            no_copy.wait_recv()
        unpack_nodes(no_recv, put_output(node_raw))

        def place_e(j):
            for d in OTHERS:
                place_edges(edge_raw, eo_recv[slot(d), j], d, j)

        with jax.named_scope('place_edge_out'):
            for group in THREE:
                group_arrived(EDGE_OUT, group)
            loop(nch, place_e)

        def place_g(j):
            for d in OTHERS:
                place_edges(gedge_raw, de_recv[slot(d), j], d, j)

        with jax.named_scope('place_first'):
            group_arrived(GRAD_OUT, 0)
            loop(hold, place_g)
        for l in range(layers):
            with jax.named_scope(f'cross_sum_{l}'):
                cross_sum(l)
        with jax.named_scope('d_node_wait'):
            dn_copy.wait_recv()
        unpack_nodes(dn_recv, put_output(gnode_raw))
        with jax.named_scope('place_rest'):
            group_arrived(GRAD_OUT, 1)
            loop(last, place_g, hold)
        for l in range(layers):
            dp_all(l, 1).wait_recv()
            ew1_buf[l, 0] = gathered[l, 0]
            ew1_buf[l, 1:] = gathered[l, EARLY:]
            ew2_buf[l] = gathered[l, 1]
            nw1_buf[l] = gathered[l, 2:4]
            nw2_buf[l] = gathered[l, 4]
            small = gathered[l, VEC_SLAB]
            for k in THREE:
                evec_buf[k, l:l + 1, :] = small[k:k + 1, :cols]
                nvec_buf[k, l:l + 1, :] = small[3 + k:4 + k, :cols]
            eb1_buf[l:l + 1, :] = small[6:7]
            nb1_buf[l:l + 1, :] = small[7:8]
        for l in range(layers):
            for stage in BOTH:
                core_all(l, stage).wait_send()
            cross_copy(l).wait_send()
            dp_all(l, 0).wait_send()
            dp_all(l, 1).wait_send()
        for copy in ncop + gcop + (w_pair, w_cross, w_relay):
            copy.wait_send()
        dp_all(0, 2).wait_send()
        no_copy.wait_send()
        dn_copy.wait_send()
        for k in range(2 * layers):
            part_copy(k).wait_send()
        edges_sent(EDGE_OUT)
        with jax.named_scope('place_last'):
            group_arrived(GRAD_OUT, 2)
            loop(nch, place_g, last)
        edges_sent(GRAD_OUT)

    bf = lambda *s: pltpu.VMEM(s, BF)
    pl.run_scoped(
        scoped, bf(D, eh), bf(D, eh), bf(D, eh), bf(D, eh), bf(D, npad), bf(D, npad), bf(D, npad), bf(D, npad), bf(D, npad), bf(D, npad),
        pltpu.VMEM((eh, D), I16), pltpu.VMEM((eh, D), I16), pltpu.VMEM((eh // D * 16, D), I16), pltpu.VMEM((eh // D * 16, D), I16),
        pltpu.VMEM((T, D), I16), pltpu.VMEM((16, D), I16),
        bf(layers, 3 * D, D), bf(layers, D, 3 * D), bf(layers, D, D), bf(layers, D, D),
        bf(layers, 2 * D, D), bf(layers, D, 2 * D), bf(layers, D, D), bf(layers, D, D), pltpu.VMEM((D, D), F32))


def finish_moves(src, dst):
    if len(src.shape) != 3 or src.dtype != BF:
        return [(src, dst)]
    return [(src.at[s, pl.ds(r, 8)], dst.at[s, pl.ds(r, 8)]) for s in range(src.shape[0]) for r in range(0, src.shape[1], 8)]


def finish_kernel(*refs):
    count = len(refs) // 2
    moves = sum((finish_moves(refs[k], refs[count + k]) for k in range(count)), [])
    puts = [pltpu.make_async_copy(src, dst, refs[-1]) for src, dst in moves]
    for put in puts:
        put.start()
    for put in puts:
        put.wait()


def keep_in_vmem(val):
    return pltpu.with_memory_space_constraint(val, pltpu.VMEM)


def finish(arrays):
    return pl.pallas_call(
        finish_kernel,
        name='finish',
        out_shape=[jax.ShapeDtypeStruct(a.shape, a.dtype) for a in arrays],
        in_specs=[VM] * len(arrays),
        out_specs=[HB] * len(arrays),
        scratch_shapes=[pltpu.SemaphoreType.DMA],
        compiler_params=pltpu.CompilerParams(vmem_limit_bytes=1 << 20),
    )(*[keep_in_vmem(a) for a in arrays])


def solution(mesh):
    lat_spec = P('dp', None, 'tp')
    first_spec = P(None, None, 'tp', None)
    col_spec = P(None, None, 'tp')
    param_specs = (first_spec, P(), col_spec, col_spec, first_spec, P(), col_spec, col_spec)
    in_specs = (lat_spec, lat_spec, P(), P(), lat_spec, lat_spec) + param_specs
    out_specs = (lat_spec, lat_spec, lat_spec, lat_spec) + param_specs
    shape = jax.ShapeDtypeStruct

    def local_step(node_lat, edge_lat, senders, receivers, grad_node, grad_edge, edge_w1, edge_b1, edge_w2, edge_vec, node_w1, node_b1, node_w2, node_vec):
        layers = edge_w1.shape[0]
        cols = node_lat.shape[2]
        nodes, edges = node_lat.shape[1], edge_lat.shape[1]
        npad = -(-nodes // TN) * TN
        eh = -(-edges // (2 * EC)) * EC
        nch = eh // EC
        dpn = mesh.shape['dp']
        per = SLABS // dpn
        dims = (layers, cols, nodes, edges, npad, eh, dpn)
        flat = lambda arr: jnp.swapaxes(arr, 1, 2)
        lead = lambda arr: jnp.transpose(arr, (1, 0, 2))
        args = (flat(node_lat), flat(edge_lat), flat(grad_node), flat(grad_edge), senders, receivers,
                edge_w1.reshape(-1, D), flat(edge_w2).reshape(-1, D), node_w1.reshape(-1, D), flat(node_w2).reshape(-1, D),
                lead(edge_vec), lead(node_vec), edge_b1, node_b1)
        vm, sem = pltpu.VMEM, pltpu.SemaphoreType.DMA
        packed = nodes // D * cols + -(-(nodes % D) * GROUP // D) * cols // GROUP
        wrows = -(-(HEAD + layers * LROWS) // (8 * dpn)) * 8 * dpn
        lat_n, lat_e = (2, cols, nodes), (2, cols, edges)
        outs = [RESULT(lat_n, BF), RESULT(lat_e, BF), RESULT(lat_n, BF), RESULT(lat_e, BF),
                RESULT((layers, 3, cols, D), F32), RESULT((layers, D), F32), RESULT((layers, cols, D), F32), RESULT((3, layers, cols), F32),
                RESULT((layers, 2, cols, D), F32), RESULT((layers, D), F32), RESULT((layers, cols, D), F32), RESULT((3, layers, cols), F32)]
        scratch = [
            *[vm(a.shape, a.dtype) for a in args[4:]], vm((wrows, D), F32), vm((3, wrows, D), F32),
            *[vm((many, packed, D), F32) for many in (2, 3, 2, 3)], *[vm((packed, D), F32)] * 4, vm((cols, npad), F32),
            vm((2, 3, cols + cols // GROUP, D), F32), vm((4, 3, cols + cols // GROUP, D), F32), *[vm((3, nch, cols, EC), F32)] * 6,
            vm((2 * layers, D, npad), F32), vm((2 * layers, D, npad), F32),
            vm((layers, D, eh), F32), vm((layers, D, eh), F32), vm((layers, eh), F32),
            vm((layers, D, npad), F32), vm((layers, D, npad), F32), vm((layers, npad), F32),
            vm((D, npad), F32), vm((D, npad), F32), vm((D, npad), F32), vm((2, 2 * eh), jnp.int32), vm((D, D), F32), vm((layers, 2, 4 * D, D), F32),
            vm((layers, SLABS, D, D), F32), vm((layers, 2, SLABS, cols, D), F32), vm((layers, SLABS, 2, cols, D), F32),
            vm((layers, (dpn - 1) * per, 2, cols, D), F32), vm((layers, per, cols, D), F32), vm((layers, per, cols, D), F32),
            vm((layers, per, cols, D), F32), vm((layers, SLABS, cols, D), F32),]
        own_sems = [
            sem((layers, 2)), sem((3, layers)), sem((layers,)), sem((3,)), sem((3, 3)), sem((2, nch)), sem((2, 5)), sem((2 * layers,)),
            pltpu.SemaphoreType.REGULAR,
            sem((len(args) + 1,)), sem((3,)), sem((3, 3)), sem((4, 4)), sem((2 * layers,)), sem((layers, 2)), sem((3, layers)), sem((layers,))]
        res = pl.pallas_call(
            lambda *refs: pl.run_scoped(lambda *own: step_kernel(dims, *refs, *own), *own_sems),
            name='graph_step',
            out_shape=outs,
            in_specs=[HB] * len(args),
            out_specs=[VM] * len(outs),
            scratch_shapes=scratch,
            compiler_params=pltpu.CompilerParams(collective_id=0, has_side_effects=True, vmem_limit_bytes=VMEM_LIMIT),
        )(*args)

        res = finish(res)
        return (flat(res[0]), flat(res[1]), flat(res[2]), flat(res[3]),
                res[4], res[5], flat(res[6]), lead(res[7]), res[8], res[9], flat(res[10]), lead(res[11]))

    return jax.shard_map(local_step, mesh=mesh, in_specs=in_specs, out_specs=out_specs, check_vma=False)
```

```python
import jax
import jax.numpy as jnp
from jax import lax
from jax.experimental import pallas as pl
from jax.experimental.pallas import tpu as pltpu
from jax.sharding import PartitionSpec as P

LN_EPS = 1e-5
D = 128
T = 256
TN = 384
EC = 512
KS = 1408
BF = jnp.bfloat16
F32 = jnp.float32
I16 = jnp.int16
MESH = pl.DeviceIdType.MESH
VM = pl.BlockSpec(memory_space=pltpu.VMEM)
HB = pl.BlockSpec(memory_space=pl.ANY)
RESULT = pltpu.VMEM
GROUP = 4
BOTH = (0, 1)
THREE = (0, 1, 2)
OTHERS = (1, 2, 3)
EDGE_IN, GRAD_IN, EDGE_OUT, GRAD_OUT = range(4)
SEND_ORDER = (2, 3, 1)
LROWS = 7 * (D // 4)
HEAD = 16
LEADER = GROUP - 1
HELPER = LEADER - 1
VMEM_LIMIT = 63_000_000
SLABS = 8
EARLY = 6
VEC_SLAB = 5
EDGE_SLABS = (0, 1, 6, 7)
STAGES = (slice(0, EARLY), slice(EARLY, SLABS))


def dot(a, b):
    return jnp.dot(a, b, preferred_element_type=F32)


def dot_nt(a, b):
    return lax.dot_general(a, b, (((1,), (1,)), ((), ())), preferred_element_type=F32)


def mat(k, n=1):
    return slice(k * D, (k + n) * D)


def rows_of(d):
    q = D // 4
    return slice(d * q, (d + 1) * q)


def at(step, width):
    return pl.ds(pl.multiple_of(step * width, width), width)


def loop(stop, body, start=0):
    def step(j, carry):
        body(j)
        return carry

    lax.fori_loop(start, stop, step, 0)


def column_sum(val):
    return jnp.sum(val, axis=0, keepdims=True)


def flip(val):
    return jnp.swapaxes(val, 0, 1)


def stacked(parts):
    return jnp.concatenate(parts, axis=0)


def beside(parts):
    return jnp.concatenate(parts, axis=1)


def slot(d):
    return d - 1


def sigmoid(hidden):
    return 1.0 / (1.0 + jnp.exp(-hidden))


def fold(val):
    total = val[:, mat(0)]
    for start in range(D, val.shape[1], D):
        total = total + val[:, start:start + D]
    return total


def swap_halves(val):
    return stacked([val[rows_of(d)] for d in (1, 0, 3, 2)])


def gather(table, keys, iota):
    acc = None
    nodes = table.shape[1]
    one, zero = jnp.ones((), BF), jnp.zeros((), BF)
    for base in range(0, nodes, T):
        width = min(T, nodes - base)
        ids = iota[0:width, :]
        hot = beside([jnp.where(ids == (key - jnp.asarray(base, I16)), one, zero) for key in keys])
        part = dot(table[:, base:base + width], hot)
        acc = part if acc is None else acc + part
    return acc


def scatter(acc_ref, val, cols, lanes):
    nodes = acc_ref.shape[1]
    one, zero = jnp.ones((), BF), jnp.zeros((), BF)
    row = lanes[0:1, :]
    for base in range(0, nodes, T):
        width = min(T, nodes - base)
        hot = beside([jnp.where((row + jnp.asarray(base + s, I16)) == cols, one, zero) for s in range(0, width, D)])
        acc_ref[:, base:base + width] += dot(val, hot)


def mlp_tail(hidden, w2t, vec):
    act = (hidden * sigmoid(hidden)).astype(BF)
    out = dot(w2t, act) + vec[0]
    mean = column_sum(out) / D
    centered = out - mean
    var = column_sum(centered * centered) / D
    inv = lax.rsqrt(var + LN_EPS)
    normed = centered * inv
    message = (normed * vec[1] + vec[2]).astype(BF)
    return message, normed, inv


def mlp_back(d_msg, hidden, normed, inv, w2, vec):
    d_normed = d_msg * vec[1]
    mean0 = column_sum(d_normed) / D
    mean1 = column_sum(d_normed * normed) / D
    d_out = inv * (d_normed - mean0 - normed * mean1)
    d_out_bf = d_out.astype(BF)
    sig = sigmoid(hidden)
    act = (hidden * sig).astype(BF)
    d_w2 = dot_nt(d_out_bf, act)
    d_hidden = dot(w2, d_out_bf) * (sig * (1.0 + hidden * (1.0 - sig)))
    sums = (fold(d_out), fold(d_msg * normed), fold(d_msg), fold(d_hidden))
    return d_hidden.astype(BF), d_w2, sums


def add_sums(ref, parts):
    for q in range(4):
        total = parts[0][q]
        for other in parts[1:]:
            total = total + other[q]
        ref[mat(q), :] += total


def step_kernel(dims, *refs):
    layers, cols, nodes, edges, npad, eh, dpn = dims
    nch = eh // EC
    top = layers - 1
    n_in = 14
    hbm_in = refs[:n_in]
    n_out = 12
    (node_raw, edge_raw, gnode_raw, gedge_raw, ew1_buf, eb1_buf, ew2_buf, evec_buf, nw1_buf, nb1_buf, nw2_buf, nvec_buf) = refs[n_in:n_in + n_out]
    (send_ids, recv_ids, ew1_in, ew2_in, nw1_in, nw2_in, evec_in, nvec_in, eb1_in, nb1_in, w_send, w_recv, n_send, n_recv, gn_send, gn_recv, no_recv, dn_recv,
     node_pad, t_send, t_recv, e_send, g_send, e_recv, g_recv, eo_recv, de_recv, part, part_recv, hidden, normed, inv, nhid, nnrm, ninv, d_part, s_sum, r_sum,
     ids_raw, bias_cols, sums, grad, core_recv, half, dp_recv, cross_send, cross_recv, own_sum, gathered,
     core_rs, dp_rs, cross_rs, w_rs, n_rs, e_rs, o_rs, p_rs, ready, load_sem, w_ss, n_ss, e_ss, p_ss, core_ss, dp_ss, cross_ss) = refs[n_in + n_out:]

    t = lax.axis_index('tp')
    p = lax.axis_index('dp')
    per = SLABS // dpn
    dp_others = range(1, dpn)
    x, c = t // 2, lax.rem(t, 2)
    ox, oc = 1 - x, 1 - c
    mate, across = t + oc - c, t + 2 * (ox - x)
    peer = [t, mate, across, mate + across - t]

    def remote(src, dst, ssem, rsem, d):
        return pltpu.make_async_remote_copy(src_ref=src, dst_ref=dst, send_sem=ssem, recv_sem=rsem,
                                            device_id={'tp': peer[d]}, device_id_type=MESH)

    small_in = (send_ids, recv_ids, ew1_in, ew2_in, nw1_in, nw2_in, evec_in, nvec_in, eb1_in, nb1_in)
    loads = [pltpu.make_async_copy(src, dst, load_sem.at[q]) for q, (src, dst) in enumerate(
        zip((hbm_in[0].at[x],) + hbm_in[1:], (node_raw.at[x], edge_raw, gnode_raw, gedge_raw) + small_in))]
    node_load, edge_load, gnode_load, gedge_load, *small_loads = loads
    first_load = pltpu.make_async_copy(hbm_in[0].at[ox], node_raw.at[ox], load_sem.at[n_in])

    def node_copies(send, recv, kind):
        return (remote(send.at[1], recv.at[0], n_ss.at[kind, 0], n_rs.at[kind, 0], 1),
                remote(send.at[0], recv.at[1], n_ss.at[kind, 1], n_rs.at[kind, 1], 2),
                remote(recv.at[1], recv.at[2], n_ss.at[kind, 2], n_rs.at[kind, 2], 1))

    piece = w_send.shape[0] // dpn

    def packed(l, k, count=1):
        return pl.ds(HEAD + l * LROWS + k * cols, count * cols)

    def weight_rows(owner):
        return pl.ds(pl.multiple_of(owner * piece, 8), piece)

    w_pair = remote(w_send, w_recv.at[0], w_ss.at[0], w_rs.at[0], 1)
    w_cross = remote(w_send.at[weight_rows(p)], w_recv.at[1, weight_rows(p)], w_ss.at[1], w_rs.at[1], 2)
    w_relay = remote(w_recv.at[1], w_recv.at[2], w_ss.at[2], w_rs.at[2], 1)

    def weight_copy(i, owner):
        rows = w_recv.at[1, weight_rows(owner)]
        return dp_remote(rows, rows, 2, 0, i)

    last = nch - 1
    hold = nch - 3
    share = 2 * (eh - last * EC - D - D // GROUP) * cols // D
    share = min(share, no_recv.shape[0] // 16 * 8)
    buffers = ((e_send, e_recv), (g_send, g_recv), (e_send, eo_recv), (g_send, de_recv))

    def outward(kind):
        return kind in (EDGE_OUT, GRAD_OUT)

    every = slice(None)
    ragged = pl.ds(D, D // GROUP)
    rest = [slice(g * cols // GROUP, (g + 1) * cols // GROUP) for g in range(GROUP)]

    def edge_part(kind, which, j, tail, send_sem, recv_sem, d):
        src, dst = buffers[kind]
        if tail:
            src, dst = t_send.at[kind % 2, which], t_recv.at[kind, which]
        else:
            src, dst = src.at[which, j], dst.at[which, j]
        recv_sems = o_rs.at[kind - EDGE_OUT, recv_sem] if outward(kind) else e_rs.at[kind, recv_sem]
        return remote(src, dst, e_ss.at[kind, send_sem], recv_sems, d)

    def by_half(half_id, j, action):
        narrow = jnp.logical_and(j == last, half_id == 1)

        @pl.when(jnp.logical_not(narrow))
        def _():
            action(False)

        @pl.when(narrow)
        def _():
            action(True)

    def pack_tail(kind, d):
        src, out = buffers[kind][0].at[slot(d), last], t_send.at[kind % 2, slot(d)]
        out[:cols, :] = src[:, :D]
        over = src[:, ragged]
        out[cols:, :] = beside([over[r] for r in rest])

    def unpack_tail(kind, d):
        src, out = t_recv.at[kind, slot(d)], buffers[kind][1].at[slot(d), last]
        out[:, :D] = src[:cols, :]
        over = src[cols:, :]
        out[:, ragged] = stacked([over[:, rows_of(g)] for g in range(GROUP)])

    def edge_start(kind, j, d):
        other = oc if d % 2 else c
        if outward(kind):
            send_sem, recv_sem = jnp.where(j == last, 1, 0), jnp.where(j == last, 2 + slot(d), jnp.where(j < hold, 0, 1))
        else:
            send_sem, recv_sem = jnp.where(j == last, d, 0), j

        def start(tail):
            if tail:
                pack_tail(kind, d)
            edge_part(kind, slot(d), j, tail, send_sem, recv_sem, d).start()

        by_half(c if outward(kind) else other, j, start)

    def edges_sent(kind):
        edge_part(kind, every, slice(0, last), False, 0, 0, 1).wait_send()
        if outward(kind):
            by_half(c, last, lambda tail: edge_part(kind, every, last, tail, 1, 0, 1).wait_send())
        else:
            for d in OTHERS:
                by_half(oc if d % 2 else c, last, lambda tail: edge_part(kind, slot(d), last, tail, d, 0, d).wait_send())

    def chunk_arrived(kind, j):
        def arrived(tail):
            edge_part(kind, every, j, tail, 0, j, 1).wait_recv()
            if tail:
                for d in OTHERS:
                    unpack_tail(kind, d)

        by_half(c, j, arrived)

    def group_arrived(kind, group):
        if group < 2:
            edge_part(kind, every, (slice(0, hold), slice(hold, last))[group], False, 0, group, 1).wait_recv()
        else:
            for d in OTHERS:
                def arrived(tail):
                    edge_part(kind, slot(d), last, tail, 0, 2 + slot(d), d).wait_recv()
                    if tail:
                        unpack_tail(kind, d)

                by_half(oc if d % 2 else c, last, arrived)

    def core_copy(l, b, stage):
        return remote(grad.at[l, STAGES[stage], pl.ds((2 * b + 1) * cols, cols), :], core_recv.at[l, b, STAGES[stage]],
                      core_ss.at[l, stage], core_rs.at[l, stage], 1)

    def core_all(l, stage):
        part_of = core_recv.at[l, :, STAGES[stage]]
        return remote(part_of, part_of, core_ss.at[l, stage], core_rs.at[l, stage], 1)

    def seat(device):
        return lax.rem(device + dpn // 2, dpn)

    def in_stage(device, stage):
        early = (seat(device) + 1) * per <= EARLY
        return jnp.logical_not(early) if stage else early

    def dp_remote(src, dst, stage, l, i):
        return pltpu.make_async_remote_copy(src_ref=src, dst_ref=dst, send_sem=dp_ss.at[stage, l], recv_sem=dp_rs.at[stage, l],
                                            device_id={'dp': lax.rem(p + i, dpn)}, device_id_type=MESH)

    def spread_copy(l, i):
        return dp_remote(half.at[l, pl.ds(seat(lax.rem(p + i, dpn)) * per, per)], dp_recv.at[l, pl.ds((i - 1) * per, per)], 0, l, i)

    def dp_all(l, stage):
        most = (dpn - 1) * per
        part_of = (dp_recv.at[l], gathered.at[l, slice(most)], w_recv.at[1, slice((dpn - 1) * piece)])[stage]
        return dp_remote(part_of, part_of, stage, l, 1)

    def cross_copy(l):
        return remote(cross_send.at[l], cross_recv.at[l], cross_ss.at[l], cross_rs.at[l], 2)

    def gather_copy(l, i, owner):
        return dp_remote(own_sum.at[l], gathered.at[l, pl.ds(seat(owner) * per, per)], 1, l, i)

    def output_copies(action):
        block, more = n_send.at[0], n_send.at[1]
        most = slice(block.shape[0] - share)
        end = pl.ds(block.shape[0] - share, share)
        sems = n_ss.at[2, 0], n_rs.at[2, 0]
        extra = remote(more.at[end], no_recv.at[end], n_ss.at[2, 2], n_rs.at[2, 2], 3)
        first_core = c == 0

        @pl.when(first_core)
        def _():
            getattr(remote(block.at[most], no_recv.at[most], *sems, 2), action)()
            if action == 'wait_recv':
                extra.wait_recv()

        @pl.when(jnp.logical_not(first_core))
        def _():
            getattr(remote(block, no_recv, *sems, 2), action)()
            if action != 'wait_recv':
                getattr(extra, action)()

    def part_piece(q, a):
        return remote(part.at[q, :, a], part_recv.at[q, :, a], p_ss.at[q], p_rs.at[q], 1)

    def part_copy(q):
        return remote(part.at[q], part_recv.at[q], p_ss.at[q], p_rs.at[q], 1)

    wide = D // GROUP
    tiles = nodes // D
    over = range(tiles * D, nodes, wide)

    def node_rows(k):
        return slice(k * cols, (k + 1) * cols) if k < tiles else pl.ds(tiles * cols + (k - tiles) * cols // GROUP, cols // GROUP)

    def pack_nodes(take, out):
        for k in range(tiles):
            out[node_rows(k), :] = take(k * D, D)
        for k, start in enumerate(over):
            val = take(start, wide)
            out[node_rows(tiles + k), :] = beside([val[r] for r in rest])

    def unpack_nodes(src, put):
        for k in range(tiles):
            put(k * D, src[node_rows(k), :])
        for k, start in enumerate(over):
            val = src[node_rows(tiles + k), :]
            put(start, stacked([val[:, rows_of(g)] for g in range(GROUP)]))

    def put_rows(ref, rows):
        def put(start, val):
            ref[rows, start:start + val.shape[1]] = val.astype(ref.dtype)

        return put

    def put_output(ref):
        def put(start, val):
            used = min(val.shape[1], nodes - start)
            ref[ox, :, start:start + used] = val[:, :used].astype(ref.dtype)

        return put

    def take_rows(ref, rows):
        return lambda start, width: ref[rows, start:start + width].astype(F32)

    def load_nodes(raw, sample, out):
        node_pad[:, :nodes] = raw[sample].astype(F32)
        pack_nodes(take_rows(node_pad, every), out)

    def keep_nodes(own):
        own[...] = jnp.zeros_like(own)
        own[:cols, :] = node_pad[...].astype(own.dtype)

    def load_edges(raw, send, own, kind):
        def put(j, lanes_j, val_of):
            for d in OTHERS:
                sample = x if d < 2 else ox
                send[slot(d), j] = val_of(sample, oc if d % 2 else c).astype(F32)
            own[:cols, lanes_j] = val_of(x, c)

        def chunk(j):
            put(j, at(j, EC), lambda s, h: raw[s, :, pl.ds(pl.multiple_of(h * eh + j * EC, D), EC)])
            for d in SEND_ORDER:
                edge_start(kind, j, d)

        loop(nch - 1, chunk)
        first = (nch - 1) * EC
        used = edges - eh - first
        last = pl.ds(first, EC)

        def tail(s, h):
            left = raw[s, :, pl.ds(first, EC)]
            right = beside([raw[s, :, pl.ds(eh + first, used)], jnp.zeros((cols, EC - used), BF)])
            return jnp.where(h == 0, left.astype(F32), right.astype(F32)).astype(BF)

        put(nch - 1, last, tail)
        for d in SEND_ORDER:
            edge_start(kind, nch - 1, d)

    def place_edges(raw, block, d, j):
        s = x if d < 2 else ox
        h = oc if d % 2 else c
        val = block.astype(BF)
        first = (nch - 1) * EC
        used = edges - eh - first

        @pl.when(jnp.logical_or(j < nch - 1, h == 0))
        def _():
            raw[s, :, pl.ds(pl.multiple_of(h * eh + j * EC, D), EC)] = val

        @pl.when(jnp.logical_and(j == nch - 1, h == 1))
        def _():
            raw[s, :, pl.ds(eh + first, used)] = val[:, :used]

    def scoped(e0, e1, ge, msg, v0, v1, v2, agg0, agg1, d_agg, scol, rcol, srow, rrow, iota, lanes, ew1, ew1t, ew2, ew2t, nw1, nw1t, nw2, nw2t, vecs):
        tables = (v0, v1, v2)
        aggs = (agg0, agg1)
        edges_in = (e0, e1)

        barrier = pltpu.get_barrier_semaphore()
        for d in OTHERS:
            pl.semaphore_signal(barrier, device_id={'tp': peer[d]}, device_id_type=MESH)
        for copy in (first_load, node_load, *small_loads, edge_load, gnode_load, gedge_load):
            copy.start()
        node_pad[...] = jnp.zeros_like(node_pad)
        with jax.named_scope('barrier'):
            @pl.when(t != LEADER)
            def _():
                pl.semaphore_wait(barrier, len(OTHERS))

            @pl.when(t == HELPER)
            def _():
                pl.semaphore_signal(ready, device_id={'tp': LEADER}, device_id_type=MESH)

            @pl.when(t == LEADER)
            def _():
                pl.semaphore_wait(ready, 1)

        first_load.wait()
        with jax.named_scope('send_nodes'):
            load_nodes(node_raw, ox, n_send.at[0])
        ncop = node_copies(n_send, n_recv, 0)
        ncop[1].start()
        node_load.wait()
        load_nodes(node_raw, x, n_send.at[1])
        keep_nodes(v0)
        ncop[0].start()
        for copy in small_loads:
            copy.wait()
        q = cols
        w_send[:HEAD, :] = jnp.zeros((HEAD, D), F32)
        for k in THREE:
            w_send[k * layers:(k + 1) * layers, :cols] = evec_in[k]
            w_send[(3 + k) * layers:(4 + k) * layers, :cols] = nvec_in[k]
        for l in range(layers):
            w_send[packed(l, 0, 3), :] = ew1_in[pl.ds(l * 3 * q, 3 * q), :].astype(F32)
            w_send[packed(l, 3), :] = ew2_in[pl.ds(l * q, q), :].astype(F32)
            w_send[packed(l, 4, 2), :] = nw1_in[pl.ds(l * 2 * q, 2 * q), :].astype(F32)
            w_send[packed(l, 6), :] = nw2_in[pl.ds(l * q, q), :].astype(F32)
        w_cross.start()
        w_pair.start()
        edge_load.wait()
        with jax.named_scope('send_edges'):
            load_edges(edge_raw, e_send, e0, EDGE_IN)
        gnode_load.wait()
        load_nodes(gnode_raw, ox, gn_send.at[0])
        load_nodes(gnode_raw, x, gn_send.at[1])
        keep_nodes(d_part)
        gcop = node_copies(gn_send, gn_recv, 1)
        gcop[1].start()
        gcop[0].start()
        gedge_load.wait()
        with jax.named_scope('send_grads'):
            load_edges(gedge_raw, g_send, ge, GRAD_IN)

        with jax.named_scope('dp_barrier'):
            @pl.when(t == LEADER)
            def _():
                for i in dp_others:
                    pl.semaphore_signal(barrier, device_id={'dp': lax.rem(p + i, dpn)}, device_id_type=MESH)
                pl.semaphore_wait(barrier, len(OTHERS) + dpn - 1)
                for d in OTHERS:
                    pl.semaphore_signal(ready, device_id={'tp': peer[d]}, device_id_type=MESH)

            @pl.when(t != LEADER)
            def _():
                pl.semaphore_wait(ready, 1)

        w_cross.wait_recv()
        for i in dp_others:
            weight_copy(i, p).start()

        @pl.when(c == 1)
        def _():
            for recv in (e_recv, g_recv):
                recv[:, last, :, D:] = jnp.zeros((len(OTHERS), cols, EC - D), F32)

        iota[...] = lax.broadcasted_iota(jnp.int32, (T, D), 0).astype(I16)
        lanes[...] = lax.broadcasted_iota(jnp.int32, (16, D), 1).astype(I16)

        ids_raw[...] = jnp.full(ids_raw.shape, -1, jnp.int32)
        for which, src in enumerate((send_ids, recv_ids)):
            ids_raw[which:which + 1, :edges] = src[...].reshape(1, edges)

        def ids(b):
            for which, (row_ref, col_ref) in enumerate(((srow, scol), (rrow, rcol))):
                wide = jnp.broadcast_to(ids_raw[which:which + 1, pl.ds(pl.multiple_of(c * eh + b * D, D), D)], (D, D))
                row_ref[at(b, 16), :] = wide[:16].astype(I16)
                col_ref[at(b, D), :] = flip(wide.astype(F32)).astype(jnp.int32).astype(I16)

        with jax.named_scope('ids'):
            loop(eh // D, ids)

        def keys(ref, step):
            return [ref[pl.ds(pl.multiple_of(step * (KS // D) * 16 + 16 * h, 16), 1), :] for h in range(KS // D)]

        bias_cols[...] = flip(stacked([eb1_in[...], nb1_in[...], jnp.zeros((D - 2 * layers, D), F32)]))

        def join_weights(l):
            for d in range(GROUP):
                src = w_recv.at[slot(d)] if d else w_send
                r = rows_of(d)
                for k in THREE:
                    ew1[l, pl.ds(k * D + d * q, q), :] = src[packed(l, k), :].astype(BF)
                ew2t[l, r, :] = src[packed(l, 3), :].astype(BF)
                for k in BOTH:
                    nw1[l, pl.ds(k * D + d * q, q), :] = src[packed(l, 4 + k), :].astype(BF)
                nw2t[l, r, :] = src[packed(l, 6), :].astype(BF)

            def flip_bf(mat):
                return flip(mat.astype(F32)).astype(BF)

            for k in THREE:
                ew1t[l, :, mat(k)] = flip_bf(ew1[l, mat(k), :])
            for k in BOTH:
                nw1t[l, :, mat(k)] = flip_bf(nw1[l, mat(k), :])
            ew2[l] = flip_bf(ew2t[l])
            nw2[l] = flip_bf(nw2t[l])

        def wait_recvs(copies):
            copies[1].wait_recv()
            copies[2].start()
            copies[0].wait_recv()
            copies[2].wait_recv()

        with jax.named_scope('node_wait'):
            wait_recvs(ncop)
        for d in OTHERS:
            unpack_nodes(n_recv.at[slot(d)], put_rows(v0, rows_of(d)))
        with jax.named_scope('weight_wait'):
            dp_all(0, 2).wait_recv()
            w_relay.start()
            w_pair.wait_recv()
            w_relay.wait_recv()
        rows_all = beside([w_send[:HEAD, :cols]] + [w_recv[d, :HEAD, :cols] for d in range(3)])
        vecs[...] = flip(stacked([rows_all, jnp.zeros((D - HEAD, D), F32)]))
        join_weights(0)

        def vec(l, node):
            first = 6 * node + l
            return [vecs[:, first + 2 * k:first + 2 * k + 1] for k in THREE]

        def bias(l, node):
            return bias_cols[:, node * layers + l:node * layers + l + 1]

        def hidden_of_nodes(l):
            table, b1 = tables[l], bias(l, 0)

            def body(step):
                xs = gather(table, keys(srow, step), iota).astype(BF)
                xr = gather(table, keys(rrow, step), iota).astype(BF)
                hidden[l, :, at(step, KS)] = dot(ew1t[l, :, mat(1, 2)], stacked([xs, xr])) + b1

            loop(eh // KS, body)

        def edge_forward(l):
            e_in = edges_in[l]

            def body(j):
                for sub in range(EC // T):
                    a = at(j * (EC // T) + sub, T)
                    if l == 0:
                        if sub == 0:
                            chunk_arrived(EDGE_IN, j)
                        for d in OTHERS:
                            e_in[rows_of(d), a] = e_recv[slot(d), j, :, sub * T:(sub + 1) * T].astype(BF)
                    e_val = e_in[:, a]
                    hid = hidden[l, :, a] + dot(ew1t[l, :, mat(0)], e_val)
                    hidden[l, :, a] = hid
                    message, nrm, std = mlp_tail(hid, ew2t[l], vec(l, 0))
                    normed[l, :, a] = nrm
                    inv[l:l + 1, a] = std
                    msg[:, a] = message
                    e_new = (e_val.astype(F32) + message.astype(F32)).astype(BF)
                    if l < top:
                        edges_in[l + 1][:, a] = e_new
                    else:
                        for d in OTHERS:
                            e_send[slot(d), j, :, sub * T:(sub + 1) * T] = e_new[rows_of(d)].astype(F32)
                        if sub == 0:
                            own_parts = []
                        own_parts.append(e_new[:q])
                if l == top:
                    for d in SEND_ORDER:
                        edge_start(EDGE_OUT, j, d)
                    place_edges(edge_raw, beside(own_parts), 0, j)

            loop(nch, body)

        def segment_sum(acc, ids_ref):
            acc[...] = jnp.zeros(acc.shape, F32)

            def body(step):
                scatter(acc, msg[:, at(step, KS)], ids_ref[at(step, KS), :], lanes)

            loop(eh // KS, body)

        def node_forward(l):
            table, agg, out = tables[l], aggs[l], tables[l + 1]

            def body(step):
                a = pl.ds(pl.multiple_of(step * TN, D), TN)
                v_in = table[:, a]
                agg_bf = (part[l, :, a] + swap_halves(part_recv[l, :, a])).astype(BF)
                agg[:, a] = agg_bf
                hid = dot(nw1t[l], stacked([v_in, agg_bf])) + bias(l, 1)
                nhid[l, :, a] = hid
                message, nrm, std = mlp_tail(hid, nw2t[l], vec(l, 1))
                nnrm[l, :, a] = nrm
                ninv[l:l + 1, a] = std
                out[:, a] = (v_in.astype(F32) + message.astype(F32)).astype(BF)

            loop(npad // TN, body)

        for l in range(layers):
            with jax.named_scope(f'gather_{l}'):
                hidden_of_nodes(l)
            if l == top:
                edges_sent(EDGE_IN)
            with jax.named_scope(f'edge_forward_{l}'):
                edge_forward(l)
            with jax.named_scope(f'sum_{l}'):
                segment_sum(part.at[l], rcol)
            part_copy(l).start()
            if l == 0:
                join_weights(1)
                gcop[1].wait_recv()
                gcop[2].start()
            with jax.named_scope(f'part_wait_{l}'):
                part_copy(l).wait_recv()
            with jax.named_scope(f'node_forward_{l}'):
                node_forward(l)
        for copy in ncop[:2]:
            copy.wait_send()
        for which in BOTH:
            pack_nodes(take_rows(tables[layers], rows_of(2 + which)), n_send.at[which])
        output_copies('start')
        node_raw[x] = tables[layers][:q, :nodes]

        grad[...] = jnp.zeros_like(grad)
        sums[...] = jnp.zeros_like(sums)
        with jax.named_scope('grad_node_wait'):
            gcop[0].wait_recv()
            gcop[2].wait_recv()
        for d in OTHERS:
            unpack_nodes(gn_recv.at[slot(d)], put_rows(d_part, rows_of(d)))

        def node_backward(l):
            table, agg = tables[l], aggs[l]

            def body(step):
                a = pl.ds(pl.multiple_of(step * TN, D), TN)
                d_in = d_part[:, a]
                if l < top:
                    d_in = d_in + part[layers + l + 1, :, a] + swap_halves(part_recv[layers + l + 1, :, a])
                    d_in = d_in.astype(BF).astype(F32)
                d_hid, d_w2, parts = mlp_back(d_in, nhid[l, :, a], nnrm[l, :, a], ninv[l:l + 1, a], nw2[l], vec(l, 1))
                add_sums(sums.at[l, 1], [parts])
                grad[l, 4] += d_w2
                grad[l, 2] += dot_nt(table[:, a], d_hid)
                grad[l, 3] += dot_nt(agg[:, a], d_hid)
                d_part[:, a] = d_in + dot(nw1[l, mat(0), :], d_hid)
                d_agg[:, a] = dot(nw1[l, mat(1), :], d_hid).astype(BF)

            loop(npad // TN, body)

        def gather_back():
            def body(step):
                msg[:, at(step, KS)] = gather(d_agg, keys(rrow, step), iota).astype(BF)

            loop(eh // KS, body)

        def edge_backward(l):
            e_in = edges_in[l]

            def body(j):
                all_parts, d_w2s, d_w1s, own_parts = [], [], [], []
                for sub in range(EC // T):
                    a = at(j * (EC // T) + sub, T)
                    if l == top:
                        if sub == 0:
                            chunk_arrived(GRAD_IN, j)
                        for d in OTHERS:
                            ge[rows_of(d), a] = g_recv[slot(d), j, :, sub * T:(sub + 1) * T].astype(BF)
                    d_res = ge[:, a].astype(F32)
                    d_msg = d_res + msg[:, a].astype(F32)
                    d_hid, d_w2, parts = mlp_back(d_msg, hidden[l, :, a], normed[l, :, a], inv[l:l + 1, a], ew2[l], vec(l, 0))
                    all_parts.append(parts)
                    d_w2s.append(d_w2)
                    d_w1s.append(dot_nt(e_in[:, a], d_hid))
                    msg[:, a] = d_hid
                    d_new = (d_res + dot(ew1[l, mat(0), :], d_hid)).astype(BF)
                    if l > 0:
                        ge[:, a] = d_new
                    else:
                        for d in OTHERS:
                            g_send[slot(d), j, :, sub * T:(sub + 1) * T] = d_new[rows_of(d)].astype(F32)
                        own_parts.append(d_new[:q])
                add_sums(sums.at[l, 0], all_parts)
                grad[l, 1] += sum(d_w2s[1:], d_w2s[0])
                grad[l, 0] += sum(d_w1s[1:], d_w1s[0])
                if l == 0:
                    @pl.when(j < hold)
                    def _():
                        for d in SEND_ORDER:
                            edge_start(GRAD_OUT, j, d)
                    place_edges(gedge_raw, beside(own_parts), 0, j)

            loop(nch, body)

        def vector_slab(l):
            def total(node, k):
                return column_sum(flip(sums[l, node, mat(k), :]))

            lat = stacked([total(node, k) for node in BOTH for k in THREE])
            biases = stacked([total(node, 3) for node in BOTH])
            n_lat = lat.shape[0]
            for d in range(GROUP):
                grad[l, VEC_SLAB, d * cols:d * cols + n_lat, :cols] = lat[:, rows_of(d)]
                grad[l, VEC_SLAB, d * cols + n_lat:d * cols + n_lat + 2, :] = biases

        def reduce_start(l, stage):
            for b in BOTH:
                core_copy(l, b, stage).start()

        def chip_sum(l, stage):
            row = lax.broadcasted_iota(jnp.int32, (cols, D), 0)
            edge_row = jnp.logical_or(row < 3, row == 6)
            core_all(l, stage).wait_recv()
            for b in BOTH:
                for k in range(SLABS)[STAGES[stage]]:
                    own = grad[l, k, rows_of(2 * b), :]
                    if k in EDGE_SLABS:
                        own = own + core_recv[l, b, k]
                    elif k == VEC_SLAB:
                        other = core_recv[l, b, k]
                        own = own + jnp.where(edge_row, other, 0.0)
                        own = jnp.where(jnp.logical_and(row == 7, c == 1), other, own)
                    half[l, k, b] = own
            for i in dp_others:
                @pl.when(in_stage(lax.rem(p + i, dpn), stage))
                def _():
                    spread_copy(l, i).start()

        def dp_sum(l, stage):
            @pl.when(in_stage(p, stage))
            def _():
                total = half[l, pl.ds(seat(p) * per, per)]
                dp_all(l, 0).wait_recv()
                for i in dp_others:
                    total = total + dp_recv[l, pl.ds((i - 1) * per, per)]
                own_sum[l] = total[:, 0]
                cross_send[l] = total[:, 1]
                cross_copy(l).start()

        def cross_sum(l):
            cross_copy(l).wait_recv()
            total = own_sum[l] + cross_recv[l]
            own_sum[l] = total
            gathered[l, pl.ds(seat(p) * per, per)] = total
            for i in dp_others:
                gather_copy(l, i, p).start()

        def project(l):
            table = tables[l]

            def body(step):
                a = pl.ds(pl.multiple_of(step * TN, D), TN)
                s_bf, r_bf, v_in = s_sum[:, a].astype(BF), r_sum[:, a].astype(BF), table[:, a]
                part[layers + l, :, a] = dot(ew1[l, mat(1), :], s_bf) + dot(ew1[l, mat(2), :], r_bf)
                if l > 0:
                    part_piece(layers + l, a).start()
                grad[l, 6] += dot_nt(v_in, s_bf)
                grad[l, 7] += dot_nt(v_in, r_bf)

            loop(npad // TN, body)

        for l in reversed(range(layers)):
            first_layer = l == 0
            with jax.named_scope(f'node_backward_{l}'):
                node_backward(l)
            if first_layer:
                with jax.named_scope('chip_sum_1'):
                    chip_sum(1, 0)
                    chip_sum(1, 1)
            with jax.named_scope(f'gather_back_{l}'):
                gather_back()
            if first_layer:
                edges_sent(GRAD_IN)
            with jax.named_scope(f'edge_backward_{l}'):
                edge_backward(l)
            vector_slab(l)
            reduce_start(l, 0)
            if first_layer:
                with jax.named_scope('dp_sum_1'):
                    dp_sum(1, 0)
                    dp_sum(1, 1)
            with jax.named_scope(f'sum_send_{l}'):
                segment_sum(s_sum, scol)
            if first_layer:
                with jax.named_scope('chip_sum_0'):
                    chip_sum(0, 0)
            with jax.named_scope(f'sum_recv_{l}'):
                segment_sum(r_sum, rcol)
            with jax.named_scope(f'project_{l}'):
                project(l)
            reduce_start(l, 1)
            if first_layer:
                part_copy(layers + l).start()
            if first_layer:
                with jax.named_scope('chip_sum_late'):
                    chip_sum(0, 1)
                with jax.named_scope('dp_sum_0'):
                    dp_sum(0, 0)
            with jax.named_scope(f'back_wait_{l}'):
                part_copy(layers + l).wait_recv()

        def final(step):
            a = pl.ds(pl.multiple_of(step * TN, D), TN)
            d_in = (d_part[:, a] + part[layers, :, a] + swap_halves(part_recv[layers, :, a])).astype(BF)
            v2[:, a] = d_in

        loop(npad // TN, final)
        gnode_raw[x] = v2[:q, :nodes]
        with jax.named_scope('dp_sum_late'):
            dp_sum(0, 1)

        gcop[1].wait_send()
        dn_send = gn_send.at[0]
        pack_nodes(take_rows(v2, rows_of(2)), dn_send)
        dn_copy = remote(dn_send, dn_recv, n_ss.at[2, 1], n_rs.at[2, 1], 2)
        dn_copy.start()

        def send_rest(j):
            for d in SEND_ORDER:
                edge_start(GRAD_OUT, j, d)

        loop(nch, send_rest, hold)

        with jax.named_scope('node_out_wait'):
            output_copies('wait_recv')
        unpack_nodes(no_recv, put_output(node_raw))

        def place_e(j):
            for d in OTHERS:
                place_edges(edge_raw, eo_recv[slot(d), j], d, j)

        with jax.named_scope('place_edge_out'):
            for group in THREE:
                group_arrived(EDGE_OUT, group)
            loop(nch, place_e)

        def place_g(j):
            for d in OTHERS:
                place_edges(gedge_raw, de_recv[slot(d), j], d, j)

        with jax.named_scope('place_first'):
            group_arrived(GRAD_OUT, 0)
            loop(hold, place_g)
        for l in range(layers):
            with jax.named_scope(f'cross_sum_{l}'):
                cross_sum(l)
        with jax.named_scope('d_node_wait'):
            dn_copy.wait_recv()
        unpack_nodes(dn_recv, put_output(gnode_raw))
        with jax.named_scope('place_rest'):
            group_arrived(GRAD_OUT, 1)
            loop(last, place_g, hold)
        for l in range(layers):
            dp_all(l, 1).wait_recv()
            ew1_buf[l, 0] = gathered[l, 0]
            ew1_buf[l, 1:] = gathered[l, EARLY:]
            ew2_buf[l] = gathered[l, 1]
            nw1_buf[l] = gathered[l, 2:4]
            nw2_buf[l] = gathered[l, 4]
            small = gathered[l, VEC_SLAB]
            for k in THREE:
                evec_buf[k, l:l + 1, :] = small[k:k + 1, :cols]
                nvec_buf[k, l:l + 1, :] = small[3 + k:4 + k, :cols]
            eb1_buf[l:l + 1, :] = small[6:7]
            nb1_buf[l:l + 1, :] = small[7:8]
        for l in range(layers):
            for stage in BOTH:
                core_all(l, stage).wait_send()
            cross_copy(l).wait_send()
            dp_all(l, 0).wait_send()
            dp_all(l, 1).wait_send()
        for copy in (ncop[2], gcop[0], gcop[2], w_pair, w_cross, w_relay):
            copy.wait_send()
        dp_all(0, 2).wait_send()
        output_copies('wait_send')
        dn_copy.wait_send()
        for k in range(2 * layers):
            part_copy(k).wait_send()
        edges_sent(EDGE_OUT)
        with jax.named_scope('place_last'):
            group_arrived(GRAD_OUT, 2)
            loop(nch, place_g, last)
        edges_sent(GRAD_OUT)

    bf = lambda *s: pltpu.VMEM(s, BF)
    pl.run_scoped(
        scoped, bf(D, eh), bf(D, eh), bf(D, eh), bf(D, eh), bf(D, npad), bf(D, npad), bf(D, npad), bf(D, npad), bf(D, npad), bf(D, npad),
        pltpu.VMEM((eh, D), I16), pltpu.VMEM((eh, D), I16), pltpu.VMEM((eh // D * 16, D), I16), pltpu.VMEM((eh // D * 16, D), I16),
        pltpu.VMEM((T, D), I16), pltpu.VMEM((16, D), I16),
        bf(layers, 3 * D, D), bf(layers, D, 3 * D), bf(layers, D, D), bf(layers, D, D),
        bf(layers, 2 * D, D), bf(layers, D, 2 * D), bf(layers, D, D), bf(layers, D, D), pltpu.VMEM((D, D), F32))


def finish_moves(src, dst):
    if len(src.shape) != 3 or src.dtype != BF:
        return [(src, dst)]
    return [(src.at[s, pl.ds(r, 8)], dst.at[s, pl.ds(r, 8)]) for s in range(src.shape[0]) for r in range(0, src.shape[1], 8)]


def finish_kernel(*refs):
    count = len(refs) // 2
    moves = sum((finish_moves(refs[k], refs[count + k]) for k in range(count)), [])
    puts = [pltpu.make_async_copy(src, dst, refs[-1]) for src, dst in moves]
    for put in puts:
        put.start()
    for put in puts:
        put.wait()


def keep_in_vmem(val):
    return pltpu.with_memory_space_constraint(val, pltpu.VMEM)


def finish(arrays):
    return pl.pallas_call(
        finish_kernel,
        name='finish',
        out_shape=[jax.ShapeDtypeStruct(a.shape, a.dtype) for a in arrays],
        in_specs=[VM] * len(arrays),
        out_specs=[HB] * len(arrays),
        scratch_shapes=[pltpu.SemaphoreType.DMA],
        compiler_params=pltpu.CompilerParams(vmem_limit_bytes=1 << 20),
    )(*[keep_in_vmem(a) for a in arrays])


def solution(mesh):
    lat_spec = P('dp', None, 'tp')
    first_spec = P(None, None, 'tp', None)
    col_spec = P(None, None, 'tp')
    param_specs = (first_spec, P(), col_spec, col_spec, first_spec, P(), col_spec, col_spec)
    in_specs = (lat_spec, lat_spec, P(), P(), lat_spec, lat_spec) + param_specs
    out_specs = (lat_spec, lat_spec, lat_spec, lat_spec) + param_specs
    shape = jax.ShapeDtypeStruct

    def local_step(node_lat, edge_lat, senders, receivers, grad_node, grad_edge, edge_w1, edge_b1, edge_w2, edge_vec, node_w1, node_b1, node_w2, node_vec):
        layers = edge_w1.shape[0]
        cols = node_lat.shape[2]
        nodes, edges = node_lat.shape[1], edge_lat.shape[1]
        npad = -(-nodes // TN) * TN
        eh = -(-edges // (2 * EC)) * EC
        nch = eh // EC
        dpn = mesh.shape['dp']
        per = SLABS // dpn
        dims = (layers, cols, nodes, edges, npad, eh, dpn)
        flat = lambda arr: jnp.swapaxes(arr, 1, 2)
        lead = lambda arr: jnp.transpose(arr, (1, 0, 2))
        args = (flat(node_lat), flat(edge_lat), flat(grad_node), flat(grad_edge), senders, receivers,
                edge_w1.reshape(-1, D), flat(edge_w2).reshape(-1, D), node_w1.reshape(-1, D), flat(node_w2).reshape(-1, D),
                lead(edge_vec), lead(node_vec), edge_b1, node_b1)
        vm, sem = pltpu.VMEM, pltpu.SemaphoreType.DMA
        packed = nodes // D * cols + -(-(nodes % D) * GROUP // D) * cols // GROUP
        wrows = -(-(HEAD + layers * LROWS) // (8 * dpn)) * 8 * dpn
        lat_n, lat_e = (2, cols, nodes), (2, cols, edges)
        outs = [RESULT(lat_n, BF), RESULT(lat_e, BF), RESULT(lat_n, BF), RESULT(lat_e, BF),
                RESULT((layers, 3, cols, D), F32), RESULT((layers, D), F32), RESULT((layers, cols, D), F32), RESULT((3, layers, cols), F32),
                RESULT((layers, 2, cols, D), F32), RESULT((layers, D), F32), RESULT((layers, cols, D), F32), RESULT((3, layers, cols), F32)]
        scratch = [
            *[vm(a.shape, a.dtype) for a in args[4:]], vm((wrows, D), F32), vm((3, wrows, D), F32),
            *[vm((many, packed, D), F32) for many in (2, 3, 2, 3)], *[vm((packed, D), F32)] * 2, vm((cols, npad), F32),
            vm((2, 3, cols + cols // GROUP, D), F32), vm((4, 3, cols + cols // GROUP, D), F32), *[vm((3, nch, cols, EC), F32)] * 6,
            vm((2 * layers, D, npad), F32), vm((2 * layers, D, npad), F32),
            vm((layers, D, eh), F32), vm((layers, D, eh), F32), vm((layers, eh), F32),
            vm((layers, D, npad), F32), vm((layers, D, npad), F32), vm((layers, npad), F32),
            vm((D, npad), F32), vm((D, npad), F32), vm((D, npad), F32), vm((2, 2 * eh), jnp.int32), vm((D, D), F32), vm((layers, 2, 4 * D, D), F32),
            vm((layers, SLABS, D, D), F32), vm((layers, 2, SLABS, cols, D), F32), vm((layers, SLABS, 2, cols, D), F32),
            vm((layers, (dpn - 1) * per, 2, cols, D), F32), vm((layers, per, cols, D), F32), vm((layers, per, cols, D), F32),
            vm((layers, per, cols, D), F32), vm((layers, SLABS, cols, D), F32),]
        own_sems = [
            sem((layers, 2)), sem((3, layers)), sem((layers,)), sem((3,)), sem((3, 3)), sem((2, nch)), sem((2, 5)), sem((2 * layers,)),
            pltpu.SemaphoreType.REGULAR,
            sem((len(args) + 1,)), sem((3,)), sem((3, 3)), sem((4, 4)), sem((2 * layers,)), sem((layers, 2)), sem((3, layers)), sem((layers,))]
        res = pl.pallas_call(
            lambda *refs: pl.run_scoped(lambda *own: step_kernel(dims, *refs, *own), *own_sems),
            name='graph_step',
            out_shape=outs,
            in_specs=[HB] * len(args),
            out_specs=[VM] * len(outs),
            scratch_shapes=scratch,
            compiler_params=pltpu.CompilerParams(collective_id=0, has_side_effects=True, vmem_limit_bytes=VMEM_LIMIT),
        )(*args)

        res = finish(res)
        return (flat(res[0]), flat(res[1]), flat(res[2]), flat(res[3]),
                res[4], res[5], flat(res[6]), lead(res[7]), res[8], res[9], flat(res[10]), lead(res[11]))

    return jax.shard_map(local_step, mesh=mesh, in_specs=in_specs, out_specs=out_specs, check_vma=False)
```

```python
import jax
import jax.numpy as jnp
from jax import lax
from jax.experimental import pallas as pl
from jax.experimental.pallas import tpu as pltpu
from jax.sharding import PartitionSpec as P

LN_EPS = 1e-5
D = 128
T = 256
TN = 384
EC = 512
KS = 1408
BF = jnp.bfloat16
F32 = jnp.float32
I16 = jnp.int16
MESH = pl.DeviceIdType.MESH
VM = pl.BlockSpec(memory_space=pltpu.VMEM)
HB = pl.BlockSpec(memory_space=pl.ANY)
RESULT = pltpu.VMEM
GROUP = 4
BOTH = (0, 1)
THREE = (0, 1, 2)
OTHERS = (1, 2, 3)
EDGE_IN, GRAD_IN, EDGE_OUT, GRAD_OUT = range(4)
SEND_ORDER = (2, 3, 1)
LROWS = 7 * (D // 4)
HEAD = 16
LEADER = GROUP - 1
HELPER = LEADER - 1
VMEM_LIMIT = 63_000_000
SLABS = 8
EARLY = 6
VEC_SLAB = 5
EDGE_SLABS = (0, 1, 6, 7)
STAGES = (slice(0, EARLY), slice(EARLY, SLABS))


def dot(a, b):
    return jnp.dot(a, b, preferred_element_type=F32)


def dot_nt(a, b):
    return lax.dot_general(a, b, (((1,), (1,)), ((), ())), preferred_element_type=F32)


def mat(k, n=1):
    return slice(k * D, (k + n) * D)


def rows_of(d):
    q = D // 4
    return slice(d * q, (d + 1) * q)


def at(step, width):
    return pl.ds(pl.multiple_of(step * width, width), width)


def loop(stop, body, start=0):
    def step(j, carry):
        body(j)
        return carry

    lax.fori_loop(start, stop, step, 0)


def column_sum(val):
    return jnp.sum(val, axis=0, keepdims=True)


def flip(val):
    return jnp.swapaxes(val, 0, 1)


def stacked(parts):
    return jnp.concatenate(parts, axis=0)


def beside(parts):
    return jnp.concatenate(parts, axis=1)


def slot(d):
    return d - 1


def sigmoid(hidden):
    return 1.0 / (1.0 + jnp.exp(-hidden))


def fold(val):
    total = val[:, mat(0)]
    for start in range(D, val.shape[1], D):
        total = total + val[:, start:start + D]
    return total


def swap_halves(val):
    return stacked([val[rows_of(d)] for d in (1, 0, 3, 2)])


def gather(table, keys, iota):
    acc = None
    nodes = table.shape[1]
    one, zero = jnp.ones((), BF), jnp.zeros((), BF)
    for base in range(0, nodes, T):
        width = min(T, nodes - base)
        ids = iota[0:width, :]
        hot = beside([jnp.where(ids == (key - jnp.asarray(base, I16)), one, zero) for key in keys])
        part = dot(table[:, base:base + width], hot)
        acc = part if acc is None else acc + part
    return acc


def scatter(acc_ref, val, cols, lanes):
    nodes = acc_ref.shape[1]
    one, zero = jnp.ones((), BF), jnp.zeros((), BF)
    row = lanes[0:1, :]
    for base in range(0, nodes, T):
        width = min(T, nodes - base)
        hot = beside([jnp.where((row + jnp.asarray(base + s, I16)) == cols, one, zero) for s in range(0, width, D)])
        acc_ref[:, base:base + width] += dot(val, hot)


def mlp_tail(hidden, w2t, vec):
    act = (hidden * sigmoid(hidden)).astype(BF)
    out = dot(w2t, act) + vec[0]
    mean = column_sum(out) / D
    centered = out - mean
    var = column_sum(centered * centered) / D
    inv = lax.rsqrt(var + LN_EPS)
    normed = centered * inv
    message = (normed * vec[1] + vec[2]).astype(BF)
    return message, normed, inv


def mlp_back(d_msg, hidden, normed, inv, w2, vec):
    d_normed = d_msg * vec[1]
    mean0 = column_sum(d_normed) / D
    mean1 = column_sum(d_normed * normed) / D
    d_out = inv * (d_normed - mean0 - normed * mean1)
    d_out_bf = d_out.astype(BF)
    sig = sigmoid(hidden)
    act = (hidden * sig).astype(BF)
    d_w2 = dot_nt(d_out_bf, act)
    d_hidden = dot(w2, d_out_bf) * (sig * (1.0 + hidden * (1.0 - sig)))
    sums = (fold(d_out), fold(d_msg * normed), fold(d_msg), fold(d_hidden))
    return d_hidden.astype(BF), d_w2, sums


def add_sums(ref, parts):
    for q in range(4):
        total = parts[0][q]
        for other in parts[1:]:
            total = total + other[q]
        ref[mat(q), :] += total


def step_kernel(dims, *refs):
    layers, cols, nodes, edges, npad, eh, dpn = dims
    nch = eh // EC
    top = layers - 1
    n_in = 14
    hbm_in = refs[:n_in]
    n_out = 12
    (node_raw, edge_raw, gnode_raw, gedge_raw, ew1_buf, eb1_buf, ew2_buf, evec_buf, nw1_buf, nb1_buf, nw2_buf, nvec_buf) = refs[n_in:n_in + n_out]
    (send_ids, recv_ids, ew1_in, ew2_in, nw1_in, nw2_in, evec_in, nvec_in, eb1_in, nb1_in, w_send, w_recv, n_send, n_recv, gn_send, gn_recv, no_recv, dn_recv,
     node_pad, t_send, t_recv, e_send, g_send, e_recv, g_recv, eo_recv, de_recv, part, part_recv, hidden, normed, inv, nhid, nnrm, ninv, d_part, s_sum, r_sum,
     ids_raw, bias_cols, sums, grad, core_recv, half, dp_recv, cross_send, cross_recv, own_sum, gathered,
     core_rs, dp_rs, cross_rs, w_rs, n_rs, e_rs, o_rs, p_rs, ready, load_sem, w_ss, n_ss, e_ss, p_ss, core_ss, dp_ss, cross_ss) = refs[n_in + n_out:]

    t = lax.axis_index('tp')
    p = lax.axis_index('dp')
    per = SLABS // dpn
    dp_others = range(1, dpn)
    x, c = t // 2, lax.rem(t, 2)
    ox, oc = 1 - x, 1 - c
    mate, across = t + oc - c, t + 2 * (ox - x)
    peer = [t, mate, across, mate + across - t]

    def remote(src, dst, ssem, rsem, d):
        return pltpu.make_async_remote_copy(src_ref=src, dst_ref=dst, send_sem=ssem, recv_sem=rsem,
                                            device_id={'tp': peer[d]}, device_id_type=MESH)

    small_in = (send_ids, recv_ids, ew1_in, ew2_in, nw1_in, nw2_in, evec_in, nvec_in, eb1_in, nb1_in)
    loads = [pltpu.make_async_copy(src, dst, load_sem.at[q]) for q, (src, dst) in enumerate(
        zip((hbm_in[0].at[x],) + hbm_in[1:], (node_raw.at[x], edge_raw, gnode_raw, gedge_raw) + small_in))]
    node_load, edge_load, gnode_load, gedge_load, *small_loads = loads
    first_load = pltpu.make_async_copy(hbm_in[0].at[ox], node_raw.at[ox], load_sem.at[n_in])

    def node_copies(send, recv, kind):
        return (remote(send.at[1], recv.at[0], n_ss.at[kind, 0], n_rs.at[kind, 0], 1),
                remote(send.at[0], recv.at[1], n_ss.at[kind, 1], n_rs.at[kind, 1], 2),
                remote(recv.at[1], recv.at[2], n_ss.at[kind, 2], n_rs.at[kind, 2], 1))

    piece = w_send.shape[0] // (dpn - 1)
    brings = p > 0

    def packed(l, k, count=1):
        return pl.ds(HEAD + l * LROWS + k * cols, count * cols)

    def weight_rows(owner):
        return pl.ds(pl.multiple_of((owner - 1) * piece, 8), piece)

    w_pair = remote(w_send, w_recv.at[0], w_ss.at[0], w_rs.at[0], 1)
    w_cross = remote(w_send.at[weight_rows(p)], w_recv.at[1, weight_rows(p)], w_ss.at[1], w_rs.at[1], 2)
    w_relay = remote(w_recv.at[1], w_recv.at[2], w_ss.at[2], w_rs.at[2], 1)

    def weight_copy(i, owner):
        rows = w_recv.at[1, weight_rows(owner)]
        return dp_remote(rows, rows, 2, 0, i)

    last = nch - 1
    hold = nch - 3
    share = 2 * (eh - last * EC - D - D // GROUP) * cols // D
    share = min(share, no_recv.shape[0] // 16 * 8)
    buffers = ((e_send, e_recv), (g_send, g_recv), (e_send, eo_recv), (g_send, de_recv))

    def outward(kind):
        return kind in (EDGE_OUT, GRAD_OUT)

    every = slice(None)
    ragged = pl.ds(D, D // GROUP)
    rest = [slice(g * cols // GROUP, (g + 1) * cols // GROUP) for g in range(GROUP)]

    def edge_part(kind, which, j, tail, send_sem, recv_sem, d):
        src, dst = buffers[kind]
        if tail:
            src, dst = t_send.at[kind % 2, which], t_recv.at[kind, which]
        else:
            src, dst = src.at[which, j], dst.at[which, j]
        recv_sems = o_rs.at[kind - EDGE_OUT, recv_sem] if outward(kind) else e_rs.at[kind, recv_sem]
        return remote(src, dst, e_ss.at[kind, send_sem], recv_sems, d)

    def by_half(half_id, j, action):
        narrow = jnp.logical_and(j == last, half_id == 1)

        @pl.when(jnp.logical_not(narrow))
        def _():
            action(False)

        @pl.when(narrow)
        def _():
            action(True)

    def pack_tail(kind, d):
        src, out = buffers[kind][0].at[slot(d), last], t_send.at[kind % 2, slot(d)]
        out[:cols, :] = src[:, :D]
        over = src[:, ragged]
        out[cols:, :] = beside([over[r] for r in rest])

    def unpack_tail(kind, d):
        src, out = t_recv.at[kind, slot(d)], buffers[kind][1].at[slot(d), last]
        out[:, :D] = src[:cols, :]
        over = src[cols:, :]
        out[:, ragged] = stacked([over[:, rows_of(g)] for g in range(GROUP)])

    def edge_start(kind, j, d):
        other = oc if d % 2 else c
        if outward(kind):
            at_last = j == last
            send_sem = jnp.asarray(at_last, jnp.int32)
            recv_sem = jnp.where(at_last, 2 + slot(d), jnp.asarray(j >= hold, jnp.int32))
        else:
            send_sem, recv_sem = jnp.where(j == last, d, 0), j

        def start(tail):
            if tail:
                pack_tail(kind, d)
            edge_part(kind, slot(d), j, tail, send_sem, recv_sem, d).start()

        by_half(c if outward(kind) else other, j, start)

    def edges_sent(kind):
        edge_part(kind, every, slice(0, last), False, 0, 0, 1).wait_send()
        if outward(kind):
            by_half(c, last, lambda tail: edge_part(kind, every, last, tail, 1, 0, 1).wait_send())
        else:
            for d in OTHERS:
                by_half(oc if d % 2 else c, last, lambda tail: edge_part(kind, slot(d), last, tail, d, 0, d).wait_send())

    def chunk_arrived(kind, j):
        def arrived(tail):
            edge_part(kind, every, j, tail, 0, j, 1).wait_recv()
            if tail:
                for d in OTHERS:
                    unpack_tail(kind, d)

        by_half(c, j, arrived)

    def group_arrived(kind, group):
        if group < 2:
            edge_part(kind, every, (slice(0, hold), slice(hold, last))[group], False, 0, group, 1).wait_recv()
        else:
            for d in OTHERS:
                def arrived(tail):
                    edge_part(kind, slot(d), last, tail, 0, 2 + slot(d), d).wait_recv()
                    if tail:
                        unpack_tail(kind, d)

                by_half(oc if d % 2 else c, last, arrived)

    def core_copy(l, b, stage):
        return remote(grad.at[l, STAGES[stage], pl.ds((2 * b + 1) * cols, cols), :], core_recv.at[l, b, STAGES[stage]],
                      core_ss.at[l, stage], core_rs.at[l, stage], 1)

    def core_all(l, stage):
        part_of = core_recv.at[l, :, STAGES[stage]]
        return remote(part_of, part_of, core_ss.at[l, stage], core_rs.at[l, stage], 1)

    def seat(device):
        return lax.rem(device + dpn // 2, dpn)

    def in_stage(device, stage):
        early = (seat(device) + 1) * per <= EARLY
        return jnp.logical_not(early) if stage else early

    def dp_remote(src, dst, stage, l, i):
        return pltpu.make_async_remote_copy(src_ref=src, dst_ref=dst, send_sem=dp_ss.at[stage, l], recv_sem=dp_rs.at[stage, l],
                                            device_id={'dp': lax.rem(p + i, dpn)}, device_id_type=MESH)

    def spread_copy(l, i):
        return dp_remote(half.at[l, pl.ds(seat(lax.rem(p + i, dpn)) * per, per)], dp_recv.at[l, pl.ds((i - 1) * per, per)], 0, l, i)

    def dp_all(l, stage):
        part_of = (dp_recv.at[l], gathered.at[l, slice((dpn - 1) * per)])[stage]
        return dp_remote(part_of, part_of, stage, l, 1)

    def pieces(count):
        part_of = w_recv.at[1, slice(count * piece)]
        return dp_remote(part_of, part_of, 2, 0, 1)

    def cross_copy(l):
        return remote(cross_send.at[l], cross_recv.at[l], cross_ss.at[l], cross_rs.at[l], 2)

    def gather_copy(l, i, owner):
        return dp_remote(own_sum.at[l], gathered.at[l, pl.ds(seat(owner) * per, per)], 1, l, i)

    def output_copies(action):
        block, more = n_send.at[0], n_send.at[1]
        most = slice(block.shape[0] - share)
        end = pl.ds(block.shape[0] - share, share)
        sems = n_ss.at[2, 0], n_rs.at[2, 0]
        extra = remote(more.at[end], no_recv.at[end], n_ss.at[2, 2], n_rs.at[2, 2], 3)
        first_core = c == 0

        @pl.when(first_core)
        def _():
            getattr(remote(block.at[most], no_recv.at[most], *sems, 2), action)()
            if action == 'wait_recv':
                extra.wait_recv()

        @pl.when(jnp.logical_not(first_core))
        def _():
            getattr(remote(block, no_recv, *sems, 2), action)()
            if action != 'wait_recv':
                getattr(extra, action)()

    def part_piece(q, a):
        return remote(part.at[q, :, a], part_recv.at[q, :, a], p_ss.at[q], p_rs.at[q], 1)

    def part_copy(q):
        return remote(part.at[q], part_recv.at[q], p_ss.at[q], p_rs.at[q], 1)

    wide = D // GROUP
    tiles = nodes // D
    over = range(tiles * D, nodes, wide)

    def node_rows(k):
        return slice(k * cols, (k + 1) * cols) if k < tiles else pl.ds(tiles * cols + (k - tiles) * cols // GROUP, cols // GROUP)

    def pack_nodes(take, out):
        for k in range(tiles):
            out[node_rows(k), :] = take(k * D, D)
        for k, start in enumerate(over):
            val = take(start, wide)
            out[node_rows(tiles + k), :] = beside([val[r] for r in rest])

    def unpack_nodes(src, put):
        for k in range(tiles):
            put(k * D, src[node_rows(k), :])
        for k, start in enumerate(over):
            val = src[node_rows(tiles + k), :]
            put(start, stacked([val[:, rows_of(g)] for g in range(GROUP)]))

    def put_rows(ref, rows):
        def put(start, val):
            ref[rows, start:start + val.shape[1]] = val.astype(ref.dtype)

        return put

    def put_output(ref):
        def put(start, val):
            used = min(val.shape[1], nodes - start)
            ref[ox, :, start:start + used] = val[:, :used].astype(ref.dtype)

        return put

    def take_rows(ref, rows):
        return lambda start, width: ref[rows, start:start + width].astype(F32)

    def load_nodes(raw, sample, out):
        node_pad[:, :nodes] = raw[sample].astype(F32)
        pack_nodes(take_rows(node_pad, every), out)

    def keep_nodes(own):
        own[...] = jnp.zeros_like(own)
        own[:cols, :] = node_pad[...].astype(own.dtype)

    def load_edges(raw, send, own, kind):
        def put(j, lanes_j, val_of):
            for d in OTHERS:
                sample = x if d < 2 else ox
                send[slot(d), j] = val_of(sample, oc if d % 2 else c).astype(F32)
            own[:cols, lanes_j] = val_of(x, c)

        def chunk(j):
            put(j, at(j, EC), lambda s, h: raw[s, :, pl.ds(pl.multiple_of(h * eh + j * EC, D), EC)])
            for d in SEND_ORDER:
                edge_start(kind, j, d)

        loop(nch - 1, chunk)
        first = (nch - 1) * EC
        used = edges - eh - first
        last = pl.ds(first, EC)

        def tail(s, h):
            left = raw[s, :, pl.ds(first, EC)]
            right = beside([raw[s, :, pl.ds(eh + first, used)], jnp.zeros((cols, EC - used), BF)])
            return jnp.where(h == 0, left.astype(F32), right.astype(F32)).astype(BF)

        put(nch - 1, last, tail)
        for d in SEND_ORDER:
            edge_start(kind, nch - 1, d)

    def place_edges(raw, block, d, j):
        s = x if d < 2 else ox
        h = oc if d % 2 else c
        val = block.astype(BF)
        first = (nch - 1) * EC
        used = edges - eh - first

        @pl.when(jnp.logical_or(j < nch - 1, h == 0))
        def _():
            raw[s, :, pl.ds(pl.multiple_of(h * eh + j * EC, D), EC)] = val

        @pl.when(jnp.logical_and(j == nch - 1, h == 1))
        def _():
            raw[s, :, pl.ds(eh + first, used)] = val[:, :used]

    def scoped(e0, e1, ge, msg, v0, v1, v2, agg0, agg1, d_agg, scol, rcol, srow, rrow, iota, lanes, ew1, ew1t, ew2, ew2t, nw1, nw1t, nw2, nw2t, vecs):
        tables = (v0, v1, v2)
        aggs = (agg0, agg1)
        edges_in = (e0, e1)

        barrier = pltpu.get_barrier_semaphore()
        for d in OTHERS:
            pl.semaphore_signal(barrier, device_id={'tp': peer[d]}, device_id_type=MESH)
        for copy in (first_load, node_load, *small_loads, edge_load, gnode_load, gedge_load):
            copy.start()
        node_pad[...] = jnp.zeros_like(node_pad)
        with jax.named_scope('barrier'):
            @pl.when(t != LEADER)
            def _():
                pl.semaphore_wait(barrier, len(OTHERS))

            @pl.when(t == HELPER)
            def _():
                pl.semaphore_signal(ready, device_id={'tp': LEADER}, device_id_type=MESH)

            @pl.when(t == LEADER)
            def _():
                pl.semaphore_wait(ready)

        first_load.wait()
        with jax.named_scope('send_nodes'):
            load_nodes(node_raw, ox, n_send.at[0])
        ncop = node_copies(n_send, n_recv, 0)
        ncop[1].start()
        node_load.wait()
        load_nodes(node_raw, x, n_send.at[1])
        keep_nodes(v0)
        ncop[0].start()
        for copy in small_loads:
            copy.wait()
        q = cols
        w_send[:HEAD, :] = jnp.zeros((HEAD, D), F32)
        for k in THREE:
            w_send[k * layers:(k + 1) * layers, :cols] = evec_in[k]
            w_send[(3 + k) * layers:(4 + k) * layers, :cols] = nvec_in[k]
        for l in range(layers):
            w_send[packed(l, 0, 3), :] = ew1_in[pl.ds(l * 3 * q, 3 * q), :].astype(F32)
            w_send[packed(l, 3), :] = ew2_in[pl.ds(l * q, q), :].astype(F32)
            w_send[packed(l, 4, 2), :] = nw1_in[pl.ds(l * 2 * q, 2 * q), :].astype(F32)
            w_send[packed(l, 6), :] = nw2_in[pl.ds(l * q, q), :].astype(F32)
        pl.when(brings)(w_cross.start)
        w_pair.start()
        edge_load.wait()
        with jax.named_scope('send_edges'):
            load_edges(edge_raw, e_send, e0, EDGE_IN)
        gnode_load.wait()
        load_nodes(gnode_raw, ox, gn_send.at[0])
        load_nodes(gnode_raw, x, gn_send.at[1])
        keep_nodes(d_part)
        gcop = node_copies(gn_send, gn_recv, 1)
        gcop[1].start()
        gcop[0].start()
        gedge_load.wait()
        with jax.named_scope('send_grads'):
            load_edges(gedge_raw, g_send, ge, GRAD_IN)

        with jax.named_scope('dp_barrier'):
            @pl.when(t == LEADER)
            def _():
                for i in dp_others:
                    pl.semaphore_signal(barrier, device_id={'dp': lax.rem(p + i, dpn)}, device_id_type=MESH)
                pl.semaphore_wait(barrier, len(OTHERS) + dpn - 1)
                for d in OTHERS:
                    pl.semaphore_signal(ready, device_id={'tp': peer[d]}, device_id_type=MESH)

            @pl.when(t != LEADER)
            def _():
                pl.semaphore_wait(ready)

        @pl.when(brings)
        def _():
            w_cross.wait_recv()
            for i in dp_others:
                weight_copy(i, p).start()

        @pl.when(c == 1)
        def _():
            for recv in (e_recv, g_recv):
                recv[:, last, :, D:] = jnp.zeros((len(OTHERS), cols, EC - D), F32)

        iota[...] = lax.broadcasted_iota(jnp.int32, (T, D), 0).astype(I16)
        lanes[...] = lax.broadcasted_iota(jnp.int32, (16, D), 1).astype(I16)

        ids_raw[...] = jnp.full(ids_raw.shape, -1, jnp.int32)
        for which, src in enumerate((send_ids, recv_ids)):
            ids_raw[which:which + 1, :edges] = src[...].reshape(1, edges)

        def ids(b):
            for which, (row_ref, col_ref) in enumerate(((srow, scol), (rrow, rcol))):
                wide = jnp.broadcast_to(ids_raw[which:which + 1, pl.ds(pl.multiple_of(c * eh + b * D, D), D)], (D, D))
                row_ref[at(b, 16), :] = wide[:16].astype(I16)
                col_ref[at(b, D), :] = flip(wide.astype(F32)).astype(jnp.int32).astype(I16)

        with jax.named_scope('ids'):
            loop(eh // D, ids)

        def keys(ref, step):
            return [ref[pl.ds(pl.multiple_of(step * (KS // D) * 16 + 16 * h, 16), 1), :] for h in range(KS // D)]

        bias_cols[...] = flip(stacked([eb1_in[...], nb1_in[...], jnp.zeros((D - 2 * layers, D), F32)]))

        def join_weights(l):
            for d in range(GROUP):
                src = w_recv.at[slot(d)] if d else w_send
                r = rows_of(d)
                for k in THREE:
                    ew1[l, pl.ds(k * D + d * q, q), :] = src[packed(l, k), :].astype(BF)
                ew2t[l, r, :] = src[packed(l, 3), :].astype(BF)
                for k in BOTH:
                    nw1[l, pl.ds(k * D + d * q, q), :] = src[packed(l, 4 + k), :].astype(BF)
                nw2t[l, r, :] = src[packed(l, 6), :].astype(BF)

            def flip_bf(mat):
                return flip(mat.astype(F32)).astype(BF)

            for k in THREE:
                ew1t[l, :, mat(k)] = flip_bf(ew1[l, mat(k), :])
            for k in BOTH:
                nw1t[l, :, mat(k)] = flip_bf(nw1[l, mat(k), :])
            ew2[l] = flip_bf(ew2t[l])
            nw2[l] = flip_bf(nw2t[l])

        def wait_recvs(copies):
            copies[1].wait_recv()
            copies[2].start()
            copies[0].wait_recv()
            copies[2].wait_recv()

        with jax.named_scope('node_wait'):
            wait_recvs(ncop)
        for d in OTHERS:
            unpack_nodes(n_recv.at[slot(d)], put_rows(v0, rows_of(d)))
        with jax.named_scope('weight_wait'):
            pl.when(jnp.logical_not(brings))(pieces(dpn - 1).wait_recv)
            if dpn > 2:
                pl.when(brings)(pieces(dpn - 2).wait_recv)
            w_relay.start()
            w_pair.wait_recv()
            w_relay.wait_recv()
        rows_all = beside([w_send[:HEAD, :cols]] + [w_recv[d, :HEAD, :cols] for d in range(3)])
        vecs[...] = flip(stacked([rows_all, jnp.zeros((D - HEAD, D), F32)]))
        join_weights(0)

        def vec(l, node):
            first = 6 * node + l
            return [vecs[:, first + 2 * k:first + 2 * k + 1] for k in THREE]

        def bias(l, node):
            return bias_cols[:, node * layers + l:node * layers + l + 1]

        def hidden_of_nodes(l):
            table, b1 = tables[l], bias(l, 0)

            def body(step):
                xs = gather(table, keys(srow, step), iota).astype(BF)
                xr = gather(table, keys(rrow, step), iota).astype(BF)
                hidden[l, :, at(step, KS)] = dot(ew1t[l, :, mat(1, 2)], stacked([xs, xr])) + b1

            loop(eh // KS, body)

        def edge_forward(l):
            e_in = edges_in[l]

            def body(j):
                for sub in range(EC // T):
                    a = at(j * (EC // T) + sub, T)
                    if l == 0:
                        if sub == 0:
                            chunk_arrived(EDGE_IN, j)
                        for d in OTHERS:
                            e_in[rows_of(d), a] = e_recv[slot(d), j, :, sub * T:(sub + 1) * T].astype(BF)
                    e_val = e_in[:, a]
                    hid = hidden[l, :, a] + dot(ew1t[l, :, mat(0)], e_val)
                    hidden[l, :, a] = hid
                    message, nrm, std = mlp_tail(hid, ew2t[l], vec(l, 0))
                    normed[l, :, a] = nrm
                    inv[l:l + 1, a] = std
                    msg[:, a] = message
                    e_new = (e_val.astype(F32) + message.astype(F32)).astype(BF)
                    if l < top:
                        edges_in[l + 1][:, a] = e_new
                    else:
                        for d in OTHERS:
                            e_send[slot(d), j, :, sub * T:(sub + 1) * T] = e_new[rows_of(d)].astype(F32)
                        if sub == 0:
                            own_parts = []
                        own_parts.append(e_new[:q])
                if l == top:
                    for d in SEND_ORDER:
                        edge_start(EDGE_OUT, j, d)
                    place_edges(edge_raw, beside(own_parts), 0, j)

            loop(nch, body)

        def segment_sum(acc, ids_ref):
            acc[...] = jnp.zeros(acc.shape, F32)

            def body(step):
                scatter(acc, msg[:, at(step, KS)], ids_ref[at(step, KS), :], lanes)

            loop(eh // KS, body)

        def node_forward(l):
            table, agg, out = tables[l], aggs[l], tables[l + 1]

            def body(step):
                a = pl.ds(pl.multiple_of(step * TN, D), TN)
                v_in = table[:, a]
                agg_bf = (part[l, :, a] + swap_halves(part_recv[l, :, a])).astype(BF)
                agg[:, a] = agg_bf
                hid = dot(nw1t[l], stacked([v_in, agg_bf])) + bias(l, 1)
                nhid[l, :, a] = hid
                message, nrm, std = mlp_tail(hid, nw2t[l], vec(l, 1))
                nnrm[l, :, a] = nrm
                ninv[l:l + 1, a] = std
                out[:, a] = (v_in.astype(F32) + message.astype(F32)).astype(BF)

            loop(npad // TN, body)

        for l in range(layers):
            with jax.named_scope(f'gather_{l}'):
                hidden_of_nodes(l)
            if l == top:
                edges_sent(EDGE_IN)
            with jax.named_scope(f'edge_forward_{l}'):
                edge_forward(l)
            with jax.named_scope(f'sum_{l}'):
                segment_sum(part.at[l], rcol)
            part_copy(l).start()
            if l == 0:
                join_weights(1)
                gcop[1].wait_recv()
                gcop[2].start()
            with jax.named_scope(f'part_wait_{l}'):
                part_copy(l).wait_recv()
            with jax.named_scope(f'node_forward_{l}'):
                node_forward(l)
        for copy in ncop[:2]:
            copy.wait_send()
        for which in BOTH:
            pack_nodes(take_rows(tables[layers], rows_of(2 + which)), n_send.at[which])
        output_copies('start')
        node_raw[x] = tables[layers][:q, :nodes]

        grad[...] = jnp.zeros_like(grad)
        sums[...] = jnp.zeros_like(sums)
        with jax.named_scope('grad_node_wait'):
            gcop[0].wait_recv()
            gcop[2].wait_recv()
        for d in OTHERS:
            unpack_nodes(gn_recv.at[slot(d)], put_rows(d_part, rows_of(d)))

        def node_backward(l):
            table, agg = tables[l], aggs[l]

            def body(step):
                a = pl.ds(pl.multiple_of(step * TN, D), TN)
                d_in = d_part[:, a]
                if l < top:
                    d_in = d_in + part[layers + l + 1, :, a] + swap_halves(part_recv[layers + l + 1, :, a])
                    d_in = d_in.astype(BF).astype(F32)
                d_hid, d_w2, parts = mlp_back(d_in, nhid[l, :, a], nnrm[l, :, a], ninv[l:l + 1, a], nw2[l], vec(l, 1))
                add_sums(sums.at[l, 1], [parts])
                grad[l, 4] += d_w2
                grad[l, 2] += dot_nt(table[:, a], d_hid)
                grad[l, 3] += dot_nt(agg[:, a], d_hid)
                d_part[:, a] = d_in + dot(nw1[l, mat(0), :], d_hid)
                d_agg[:, a] = dot(nw1[l, mat(1), :], d_hid).astype(BF)

            loop(npad // TN, body)

        def gather_back():
            def body(step):
                msg[:, at(step, KS)] = gather(d_agg, keys(rrow, step), iota).astype(BF)

            loop(eh // KS, body)

        def edge_backward(l):
            e_in = edges_in[l]

            def body(j):
                all_parts, d_w2s, d_w1s, own_parts = [], [], [], []
                for sub in range(EC // T):
                    a = at(j * (EC // T) + sub, T)
                    if l == top:
                        if sub == 0:
                            chunk_arrived(GRAD_IN, j)
                        for d in OTHERS:
                            ge[rows_of(d), a] = g_recv[slot(d), j, :, sub * T:(sub + 1) * T].astype(BF)
                    d_res = ge[:, a].astype(F32)
                    d_msg = d_res + msg[:, a].astype(F32)
                    d_hid, d_w2, parts = mlp_back(d_msg, hidden[l, :, a], normed[l, :, a], inv[l:l + 1, a], ew2[l], vec(l, 0))
                    all_parts.append(parts)
                    d_w2s.append(d_w2)
                    d_w1s.append(dot_nt(e_in[:, a], d_hid))
                    msg[:, a] = d_hid
                    d_new = (d_res + dot(ew1[l, mat(0), :], d_hid)).astype(BF)
                    if l > 0:
                        ge[:, a] = d_new
                    else:
                        for d in OTHERS:
                            g_send[slot(d), j, :, sub * T:(sub + 1) * T] = d_new[rows_of(d)].astype(F32)
                        own_parts.append(d_new[:q])
                add_sums(sums.at[l, 0], all_parts)
                grad[l, 1] += sum(d_w2s[1:], d_w2s[0])
                grad[l, 0] += sum(d_w1s[1:], d_w1s[0])
                if l == 0:
                    @pl.when(j < hold)
                    def _():
                        for d in SEND_ORDER:
                            edge_start(GRAD_OUT, j, d)
                    place_edges(gedge_raw, beside(own_parts), 0, j)

            loop(nch, body)

        def vector_slab(l):
            def total(node, k):
                return column_sum(flip(sums[l, node, mat(k), :]))

            lat = stacked([total(node, k) for node in BOTH for k in THREE])
            biases = stacked([total(node, 3) for node in BOTH])
            n_lat = lat.shape[0]
            for d in range(GROUP):
                grad[l, VEC_SLAB, d * cols:d * cols + n_lat, :cols] = lat[:, rows_of(d)]
                grad[l, VEC_SLAB, d * cols + n_lat:d * cols + n_lat + 2, :] = biases

        def reduce_start(l, stage):
            for b in BOTH:
                core_copy(l, b, stage).start()

        def chip_sum(l, stage):
            row = lax.broadcasted_iota(jnp.int32, (cols, D), 0)
            edge_row = jnp.logical_or(row < 3, row == 6)
            core_all(l, stage).wait_recv()
            for b in BOTH:
                for k in range(SLABS)[STAGES[stage]]:
                    own = grad[l, k, rows_of(2 * b), :]
                    if k in EDGE_SLABS:
                        own = own + core_recv[l, b, k]
                    elif k == VEC_SLAB:
                        other = core_recv[l, b, k]
                        own = own + jnp.where(edge_row, other, 0.0)
                        own = jnp.where(jnp.logical_and(row == 7, c == 1), other, own)
                    half[l, k, b] = own
            for i in dp_others:
                @pl.when(in_stage(lax.rem(p + i, dpn), stage))
                def _():
                    spread_copy(l, i).start()

        def dp_sum(l, stage):
            @pl.when(in_stage(p, stage))
            def _():
                total = half[l, pl.ds(seat(p) * per, per)]
                dp_all(l, 0).wait_recv()
                for i in dp_others:
                    total = total + dp_recv[l, pl.ds((i - 1) * per, per)]
                own_sum[l] = total[:, 0]
                cross_send[l] = total[:, 1]
                cross_copy(l).start()

        def cross_sum(l):
            cross_copy(l).wait_recv()
            total = own_sum[l] + cross_recv[l]
            own_sum[l] = total
            gathered[l, pl.ds(seat(p) * per, per)] = total
            for i in dp_others:
                gather_copy(l, i, p).start()

        def project(l):
            table = tables[l]

            def body(step):
                a = pl.ds(pl.multiple_of(step * TN, D), TN)
                s_bf, r_bf, v_in = s_sum[:, a].astype(BF), r_sum[:, a].astype(BF), table[:, a]
                part[layers + l, :, a] = dot(ew1[l, mat(1), :], s_bf) + dot(ew1[l, mat(2), :], r_bf)
                if l > 0:
                    part_piece(layers + l, a).start()
                grad[l, 6] += dot_nt(v_in, s_bf)
                grad[l, 7] += dot_nt(v_in, r_bf)

            loop(npad // TN, body)

        for l in reversed(range(layers)):
            first_layer = l == 0
            with jax.named_scope(f'node_backward_{l}'):
                node_backward(l)
            if first_layer:
                with jax.named_scope('chip_sum_1'):
                    chip_sum(1, 0)
                    chip_sum(1, 1)
            with jax.named_scope(f'gather_back_{l}'):
                gather_back()
            if first_layer:
                edges_sent(GRAD_IN)
            with jax.named_scope(f'edge_backward_{l}'):
                edge_backward(l)
            vector_slab(l)
            reduce_start(l, 0)
            if first_layer:
                with jax.named_scope('dp_sum_1'):
                    dp_sum(1, 0)
                    dp_sum(1, 1)
            with jax.named_scope(f'sum_send_{l}'):
                segment_sum(s_sum, scol)
            if first_layer:
                with jax.named_scope('chip_sum_0'):
                    chip_sum(0, 0)
            with jax.named_scope(f'sum_recv_{l}'):
                segment_sum(r_sum, rcol)
            with jax.named_scope(f'project_{l}'):
                project(l)
            reduce_start(l, 1)
            if first_layer:
                part_copy(layers + l).start()
            if first_layer:
                with jax.named_scope('chip_sum_late'):
                    chip_sum(0, 1)
                with jax.named_scope('dp_sum_0'):
                    dp_sum(0, 0)
            with jax.named_scope(f'back_wait_{l}'):
                part_copy(layers + l).wait_recv()

        def final(step):
            a = pl.ds(pl.multiple_of(step * TN, D), TN)
            d_in = (d_part[:, a] + part[layers, :, a] + swap_halves(part_recv[layers, :, a])).astype(BF)
            v2[:, a] = d_in

        loop(npad // TN, final)
        gnode_raw[x] = v2[:q, :nodes]
        with jax.named_scope('dp_sum_late'):
            dp_sum(0, 1)

        gcop[1].wait_send()
        dn_send = gn_send.at[0]
        pack_nodes(take_rows(v2, rows_of(2)), dn_send)
        dn_copy = remote(dn_send, dn_recv, n_ss.at[2, 1], n_rs.at[2, 1], 2)
        dn_copy.start()

        def send_rest(j):
            for d in SEND_ORDER:
                edge_start(GRAD_OUT, j, d)

        loop(nch, send_rest, hold)

        with jax.named_scope('node_out_wait'):
            output_copies('wait_recv')
        unpack_nodes(no_recv, put_output(node_raw))

        def place_e(j):
            for d in OTHERS:
                place_edges(edge_raw, eo_recv[slot(d), j], d, j)

        with jax.named_scope('place_edge_out'):
            for group in THREE:
                group_arrived(EDGE_OUT, group)
            loop(nch, place_e)

        def place_g(j):
            for d in OTHERS:
                place_edges(gedge_raw, de_recv[slot(d), j], d, j)

        with jax.named_scope('place_first'):
            group_arrived(GRAD_OUT, 0)
            loop(hold, place_g)
        for l in range(layers):
            with jax.named_scope(f'cross_sum_{l}'):
                cross_sum(l)
        with jax.named_scope('d_node_wait'):
            dn_copy.wait_recv()
        unpack_nodes(dn_recv, put_output(gnode_raw))
        with jax.named_scope('place_rest'):
            group_arrived(GRAD_OUT, 1)
            loop(last, place_g, hold)
        for l in range(layers):
            dp_all(l, 1).wait_recv()
            ew1_buf[l, 0] = gathered[l, 0]
            ew1_buf[l, 1:] = gathered[l, EARLY:]
            ew2_buf[l] = gathered[l, 1]
            nw1_buf[l] = gathered[l, 2:4]
            nw2_buf[l] = gathered[l, 4]
            small = gathered[l, VEC_SLAB]
            for k in THREE:
                evec_buf[k, l:l + 1, :] = small[k:k + 1, :cols]
                nvec_buf[k, l:l + 1, :] = small[3 + k:4 + k, :cols]
            eb1_buf[l:l + 1, :] = small[6:7]
            nb1_buf[l:l + 1, :] = small[7:8]
        for l in range(layers):
            for stage in BOTH:
                core_all(l, stage).wait_send()
            cross_copy(l).wait_send()
            dp_all(l, 0).wait_send()
            dp_all(l, 1).wait_send()
        for copy in (ncop[2], gcop[0], gcop[2], w_pair, w_relay):
            copy.wait_send()

        @pl.when(brings)
        def _():
            w_cross.wait_send()
            pieces(dpn - 1).wait_send()

        output_copies('wait_send')
        dn_copy.wait_send()
        for k in range(2 * layers):
            part_copy(k).wait_send()
        edges_sent(EDGE_OUT)
        with jax.named_scope('place_last'):
            group_arrived(GRAD_OUT, 2)
            loop(nch, place_g, last)
        edges_sent(GRAD_OUT)

    bf = lambda *s: pltpu.VMEM(s, BF)
    pl.run_scoped(
        scoped, bf(D, eh), bf(D, eh), bf(D, eh), bf(D, eh), bf(D, npad), bf(D, npad), bf(D, npad), bf(D, npad), bf(D, npad), bf(D, npad),
        pltpu.VMEM((eh, D), I16), pltpu.VMEM((eh, D), I16), pltpu.VMEM((eh // D * 16, D), I16), pltpu.VMEM((eh // D * 16, D), I16),
        pltpu.VMEM((T, D), I16), pltpu.VMEM((16, D), I16),
        bf(layers, 3 * D, D), bf(layers, D, 3 * D), bf(layers, D, D), bf(layers, D, D),
        bf(layers, 2 * D, D), bf(layers, D, 2 * D), bf(layers, D, D), bf(layers, D, D), pltpu.VMEM((D, D), F32))


def finish_moves(src, dst):
    if len(src.shape) != 3 or src.dtype != BF:
        return [(src, dst)]
    return [(src.at[s, pl.ds(r, 8)], dst.at[s, pl.ds(r, 8)]) for s in range(src.shape[0]) for r in range(0, src.shape[1], 8)]


def finish_kernel(*refs):
    count = len(refs) // 2
    moves = sum((finish_moves(refs[k], refs[count + k]) for k in range(count)), [])
    puts = [pltpu.make_async_copy(src, dst, refs[-1]) for src, dst in moves]
    for put in puts:
        put.start()
    for put in puts:
        put.wait()


def keep_in_vmem(val):
    return pltpu.with_memory_space_constraint(val, pltpu.VMEM)


def finish(arrays):
    return pl.pallas_call(
        finish_kernel,
        name='finish',
        out_shape=[jax.ShapeDtypeStruct(a.shape, a.dtype) for a in arrays],
        in_specs=[VM] * len(arrays),
        out_specs=[HB] * len(arrays),
        scratch_shapes=[pltpu.SemaphoreType.DMA],
        compiler_params=pltpu.CompilerParams(vmem_limit_bytes=1 << 20),
    )(*[keep_in_vmem(a) for a in arrays])


def solution(mesh):
    lat_spec = P('dp', None, 'tp')
    first_spec = P(None, None, 'tp', None)
    col_spec = P(None, None, 'tp')
    param_specs = (first_spec, P(), col_spec, col_spec, first_spec, P(), col_spec, col_spec)
    in_specs = (lat_spec, lat_spec, P(), P(), lat_spec, lat_spec) + param_specs
    out_specs = (lat_spec, lat_spec, lat_spec, lat_spec) + param_specs
    shape = jax.ShapeDtypeStruct

    def local_step(node_lat, edge_lat, senders, receivers, grad_node, grad_edge, edge_w1, edge_b1, edge_w2, edge_vec, node_w1, node_b1, node_w2, node_vec):
        layers = edge_w1.shape[0]
        cols = node_lat.shape[2]
        nodes, edges = node_lat.shape[1], edge_lat.shape[1]
        npad = -(-nodes // TN) * TN
        eh = -(-edges // (2 * EC)) * EC
        nch = eh // EC
        dpn = mesh.shape['dp']
        per = SLABS // dpn
        dims = (layers, cols, nodes, edges, npad, eh, dpn)
        flat = lambda arr: jnp.swapaxes(arr, 1, 2)
        lead = lambda arr: jnp.transpose(arr, (1, 0, 2))
        args = (flat(node_lat), flat(edge_lat), flat(grad_node), flat(grad_edge), senders, receivers,
                edge_w1.reshape(-1, D), flat(edge_w2).reshape(-1, D), node_w1.reshape(-1, D), flat(node_w2).reshape(-1, D),
                lead(edge_vec), lead(node_vec), edge_b1, node_b1)
        vm, sem = pltpu.VMEM, pltpu.SemaphoreType.DMA
        packed = nodes // D * cols + -(-(nodes % D) * GROUP // D) * cols // GROUP
        wrows = -(-(HEAD + layers * LROWS) // (8 * (dpn - 1))) * 8 * (dpn - 1)
        lat_n, lat_e = (2, cols, nodes), (2, cols, edges)
        outs = [RESULT(lat_n, BF), RESULT(lat_e, BF), RESULT(lat_n, BF), RESULT(lat_e, BF),
                RESULT((layers, 3, cols, D), F32), RESULT((layers, D), F32), RESULT((layers, cols, D), F32), RESULT((3, layers, cols), F32),
                RESULT((layers, 2, cols, D), F32), RESULT((layers, D), F32), RESULT((layers, cols, D), F32), RESULT((3, layers, cols), F32)]
        scratch = [
            *[vm(a.shape, a.dtype) for a in args[4:]], vm((wrows, D), F32), vm((3, wrows, D), F32),
            *[vm((many, packed, D), F32) for many in (2, 3, 2, 3)], *[vm((packed, D), F32)] * 2, vm((cols, npad), F32),
            *[vm((kinds, len(OTHERS), cols + cols // GROUP, D), F32) for kinds in (2, GROUP)], *[vm((len(OTHERS), nch, cols, EC), F32)] * 6,
            vm((2 * layers, D, npad), F32), vm((2 * layers, D, npad), F32),
            vm((layers, D, eh), F32), vm((layers, D, eh), F32), vm((layers, eh), F32),
            vm((layers, D, npad), F32), vm((layers, D, npad), F32), vm((layers, npad), F32),
            vm((D, npad), F32), vm((D, npad), F32), vm((D, npad), F32), vm((2, 2 * eh), jnp.int32), vm((D, D), F32), vm((layers, 2, 4 * D, D), F32),
            vm((layers, SLABS, D, D), F32), vm((layers, 2, SLABS, cols, D), F32), vm((layers, SLABS, 2, cols, D), F32),
            vm((layers, (dpn - 1) * per, 2, cols, D), F32), vm((layers, per, cols, D), F32), vm((layers, per, cols, D), F32),
            vm((layers, per, cols, D), F32), vm((layers, SLABS, cols, D), F32),]
        own_sems = [
            sem((layers, 2)), sem((3, layers)), sem((layers,)), sem((3,)), sem((3, 3)), sem((2, nch)), sem((2, 5)), sem((2 * layers,)),
            pltpu.SemaphoreType.REGULAR,
            sem((len(args) + 1,)), sem((3,)), sem((3, 3)), sem((4, 4)), sem((2 * layers,)), sem((layers, 2)), sem((3, layers)), sem((layers,))]
        res = pl.pallas_call(
            lambda *refs: pl.run_scoped(lambda *own: step_kernel(dims, *refs, *own), *own_sems),
            name='graph_step',
            out_shape=outs,
            in_specs=[HB] * len(args),
            out_specs=[VM] * len(outs),
            scratch_shapes=scratch,
            compiler_params=pltpu.CompilerParams(collective_id=0, has_side_effects=True, vmem_limit_bytes=VMEM_LIMIT),
        )(*args)

        res = finish(res)
        return (flat(res[0]), flat(res[1]), flat(res[2]), flat(res[3]),
                res[4], res[5], flat(res[6]), lead(res[7]), res[8], res[9], flat(res[10]), lead(res[11]))

    return jax.shard_map(local_step, mesh=mesh, in_specs=in_specs, out_specs=out_specs, check_vma=False)
```

```python
import jax
import jax.numpy as jnp
from jax import lax
from jax.experimental import pallas as pl
from jax.experimental.pallas import tpu as pltpu
from jax.sharding import PartitionSpec as P

LN_EPS = 1e-5
D = 128
T = 256
TN = 384
EC = 512
KS = 2816
BF = jnp.bfloat16
F32 = jnp.float32
I16 = jnp.int16
MESH = pl.DeviceIdType.MESH
VM = pl.BlockSpec(memory_space=pltpu.VMEM)
HB = pl.BlockSpec(memory_space=pl.ANY)
RESULT = pltpu.VMEM
GROUP = 4
BOTH = (0, 1)
THREE = (0, 1, 2)
OTHERS = (1, 2, 3)
EDGE_IN, GRAD_IN, EDGE_OUT, GRAD_OUT = range(4)
SEND_ORDER = (2, 3, 1)
LROWS = 7 * (D // 4)
HEAD = 16
LEADER = GROUP - 1
HELPER = LEADER - 1
VMEM_LIMIT = 63_000_000
SLABS = 8
EARLY = 6
VEC_SLAB = 5
EDGE_SLABS = (0, 1, 6, 7)
STAGES = (slice(0, EARLY), slice(EARLY, SLABS))


def dot(a, b):
    return jnp.dot(a, b, preferred_element_type=F32)


def dot_nt(a, b):
    return lax.dot_general(a, b, (((1,), (1,)), ((), ())), preferred_element_type=F32)


def mat(k, n=1):
    return slice(k * D, (k + n) * D)


def rows_of(d):
    q = D // 4
    return slice(d * q, (d + 1) * q)


def at(step, width):
    return pl.ds(pl.multiple_of(step * width, width), width)


def loop(stop, body, start=0):
    def step(j, carry):
        body(j)
        return carry

    lax.fori_loop(start, stop, step, 0)


def column_sum(val):
    return jnp.sum(val, axis=0, keepdims=True)


def flip(val):
    return jnp.swapaxes(val, 0, 1)


def stacked(parts):
    return jnp.concatenate(parts, axis=0)


def beside(parts):
    return jnp.concatenate(parts, axis=1)


def slot(d):
    return d - 1


def sigmoid(hidden):
    return 1.0 / (1.0 + jnp.exp(-hidden))


def fold(val):
    total = val[:, mat(0)]
    for start in range(D, val.shape[1], D):
        total = total + val[:, start:start + D]
    return total


def swap_halves(val):
    return stacked([val[rows_of(d)] for d in (1, 0, 3, 2)])


def gather(table, keys, iota):
    acc = None
    nodes = table.shape[1]
    one, zero = jnp.ones((), BF), jnp.zeros((), BF)
    for base in range(0, nodes, T):
        width = min(T, nodes - base)
        ids = iota[0:width, :]
        hot = beside([jnp.where(ids == (key - jnp.asarray(base, I16)), one, zero) for key in keys])
        part = dot(table[:, base:base + width], hot)
        acc = part if acc is None else acc + part
    return acc


def scatter(acc_ref, val, cols, lanes):
    nodes = acc_ref.shape[1]
    one, zero = jnp.ones((), BF), jnp.zeros((), BF)
    row = lanes[0:1, :]
    for base in range(0, nodes, T):
        width = min(T, nodes - base)
        hot = beside([jnp.where((row + jnp.asarray(base + s, I16)) == cols, one, zero) for s in range(0, width, D)])
        acc_ref[:, base:base + width] += dot(val, hot)


def mlp_tail(hidden, w2t, vec):
    act = (hidden * sigmoid(hidden)).astype(BF)
    out = dot(w2t, act) + vec[0]
    mean = column_sum(out) / D
    centered = out - mean
    var = column_sum(centered * centered) / D
    inv = lax.rsqrt(var + LN_EPS)
    normed = centered * inv
    message = (normed * vec[1] + vec[2]).astype(BF)
    return message, normed, inv


def mlp_back(d_msg, hidden, normed, inv, w2, vec):
    d_normed = d_msg * vec[1]
    mean0 = column_sum(d_normed) / D
    mean1 = column_sum(d_normed * normed) / D
    d_out = inv * (d_normed - mean0 - normed * mean1)
    d_out_bf = d_out.astype(BF)
    sig = sigmoid(hidden)
    act = (hidden * sig).astype(BF)
    d_w2 = dot_nt(d_out_bf, act)
    d_hidden = dot(w2, d_out_bf) * (sig * (1.0 + hidden * (1.0 - sig)))
    sums = (fold(d_out), fold(d_msg * normed), fold(d_msg), fold(d_hidden))
    return d_hidden.astype(BF), d_w2, sums


def add_sums(ref, parts):
    for q in range(4):
        total = parts[0][q]
        for other in parts[1:]:
            total = total + other[q]
        ref[mat(q), :] += total


def step_kernel(dims, *refs):
    layers, cols, nodes, edges, npad, eh, dpn = dims
    nch = eh // EC
    top = layers - 1
    n_in = 14
    hbm_in = refs[:n_in]
    n_out = 12
    (node_raw, edge_raw, gnode_raw, gedge_raw, ew1_buf, eb1_buf, ew2_buf, evec_buf, nw1_buf, nb1_buf, nw2_buf, nvec_buf) = refs[n_in:n_in + n_out]
    (send_ids, recv_ids, ew1_in, ew2_in, nw1_in, nw2_in, evec_in, nvec_in, eb1_in, nb1_in, w_send, w_recv, n_send, n_recv, gn_send, gn_recv, no_recv, dn_recv,
     node_pad, t_send, t_recv, e_send, g_send, e_recv, g_recv, eo_recv, de_recv, part, part_recv, hidden, normed, inv, nhid, nnrm, ninv, d_part,
     ids_raw, bias_cols, sums, grad, core_recv, half, dp_recv, cross_send, cross_recv, own_sum, gathered,
     core_rs, dp_rs, cross_rs, w_rs, n_rs, e_rs, o_rs, p_rs, ready, load_sem, w_ss, n_ss, e_ss, p_ss, core_ss, dp_ss, cross_ss) = refs[n_in + n_out:]

    t = lax.axis_index('tp')
    p = lax.axis_index('dp')
    per = SLABS // dpn
    dp_others = range(1, dpn)
    x, c = t // 2, lax.rem(t, 2)
    ox, oc = 1 - x, 1 - c
    mate, across = t + oc - c, t + 2 * (ox - x)
    peer = [t, mate, across, mate + across - t]

    def remote(src, dst, ssem, rsem, d):
        return pltpu.make_async_remote_copy(src_ref=src, dst_ref=dst, send_sem=ssem, recv_sem=rsem,
                                            device_id={'tp': peer[d]}, device_id_type=MESH)

    small_in = (send_ids, recv_ids, ew1_in, ew2_in, nw1_in, nw2_in, evec_in, nvec_in, eb1_in, nb1_in)
    loads = [pltpu.make_async_copy(src, dst, load_sem.at[q]) for q, (src, dst) in enumerate(
        zip((hbm_in[0].at[x],) + hbm_in[1:], (node_raw.at[x], edge_raw, gnode_raw, gedge_raw) + small_in))]
    node_load, edge_load, gnode_load, gedge_load, *small_loads = loads
    first_load = pltpu.make_async_copy(hbm_in[0].at[ox], node_raw.at[ox], load_sem.at[n_in])

    def node_copies(send, recv, kind):
        return (remote(send.at[1], recv.at[0], n_ss.at[kind, 0], n_rs.at[kind, 0], 1),
                remote(send.at[0], recv.at[1], n_ss.at[kind, 1], n_rs.at[kind, 1], 2),
                remote(recv.at[1], recv.at[2], n_ss.at[kind, 2], n_rs.at[kind, 2], 1))

    piece = w_send.shape[0] // (dpn - 1)
    brings = p > 0

    def packed(l, k, count=1):
        return pl.ds(HEAD + l * LROWS + k * cols, count * cols)

    def weight_rows(owner):
        return pl.ds(pl.multiple_of((owner - 1) * piece, 8), piece)

    w_pair = remote(w_send, w_recv.at[0], w_ss.at[0], w_rs.at[0], 1)
    w_cross = remote(w_send.at[weight_rows(p)], w_recv.at[1, weight_rows(p)], w_ss.at[1], w_rs.at[1], 2)
    w_relay = remote(w_recv.at[1], w_recv.at[2], w_ss.at[2], w_rs.at[2], 1)

    def weight_copy(i, owner):
        rows = w_recv.at[1, weight_rows(owner)]
        return dp_remote(rows, rows, 2, 0, i)

    last = nch - 1
    hold = nch - 3
    share = 2 * (eh - last * EC - D - D // GROUP) * cols // D
    share = min(share, no_recv.shape[0] // 16 * 8)
    buffers = ((e_send, e_recv), (g_send, g_recv), (e_send, eo_recv), (g_send, de_recv))

    def outward(kind):
        return kind in (EDGE_OUT, GRAD_OUT)

    every = slice(None)
    ragged = pl.ds(D, D // GROUP)
    rest = [slice(g * cols // GROUP, (g + 1) * cols // GROUP) for g in range(GROUP)]

    def edge_part(kind, which, j, tail, send_sem, recv_sem, d):
        src, dst = buffers[kind]
        if tail:
            src, dst = t_send.at[kind % 2, which], t_recv.at[kind, which]
        else:
            src, dst = src.at[which, j], dst.at[which, j]
        recv_sems = o_rs.at[kind - EDGE_OUT, recv_sem] if outward(kind) else e_rs.at[kind, recv_sem]
        return remote(src, dst, e_ss.at[kind, send_sem], recv_sems, d)

    def by_half(half_id, j, action):
        narrow = jnp.logical_and(j == last, half_id == 1)

        @pl.when(jnp.logical_not(narrow))
        def _():
            action(False)

        @pl.when(narrow)
        def _():
            action(True)

    def pack_tail(kind, d):
        src, out = buffers[kind][0].at[slot(d), last], t_send.at[kind % 2, slot(d)]
        out[:cols, :] = src[:, :D]
        over = src[:, ragged]
        out[cols:, :] = beside([over[r] for r in rest])

    def unpack_tail(kind, d):
        src, out = t_recv.at[kind, slot(d)], buffers[kind][1].at[slot(d), last]
        out[:, :D] = src[:cols, :]
        over = src[cols:, :]
        out[:, ragged] = stacked([over[:, rows_of(g)] for g in range(GROUP)])

    def edge_start(kind, j, d):
        other = oc if d % 2 else c
        if outward(kind):
            at_last = j == last
            send_sem = jnp.asarray(at_last, jnp.int32)
            recv_sem = jnp.where(at_last, 2 + slot(d), jnp.asarray(j >= hold, jnp.int32))
        else:
            send_sem, recv_sem = jnp.where(j == last, d, 0), j

        def start(tail):
            if tail:
                pack_tail(kind, d)
            edge_part(kind, slot(d), j, tail, send_sem, recv_sem, d).start()

        by_half(c if outward(kind) else other, j, start)

    def edges_sent(kind):
        edge_part(kind, every, slice(0, last), False, 0, 0, 1).wait_send()
        if outward(kind):
            by_half(c, last, lambda tail: edge_part(kind, every, last, tail, 1, 0, 1).wait_send())
        else:
            for d in OTHERS:
                by_half(oc if d % 2 else c, last, lambda tail: edge_part(kind, slot(d), last, tail, d, 0, d).wait_send())

    def chunk_arrived(kind, j):
        def arrived(tail):
            edge_part(kind, every, j, tail, 0, j, 1).wait_recv()
            if tail:
                for d in OTHERS:
                    unpack_tail(kind, d)

        by_half(c, j, arrived)

    def group_arrived(kind, group):
        if group < 2:
            edge_part(kind, every, (slice(0, hold), slice(hold, last))[group], False, 0, group, 1).wait_recv()
        else:
            for d in OTHERS:
                def arrived(tail):
                    edge_part(kind, slot(d), last, tail, 0, 2 + slot(d), d).wait_recv()
                    if tail:
                        unpack_tail(kind, d)

                by_half(oc if d % 2 else c, last, arrived)

    def core_copy(l, b, stage):
        return remote(grad.at[l, STAGES[stage], pl.ds((2 * b + 1) * cols, cols), :], core_recv.at[l, b, STAGES[stage]],
                      core_ss.at[l, stage], core_rs.at[l, stage], 1)

    def core_all(l, stage):
        part_of = core_recv.at[l, :, STAGES[stage]]
        return remote(part_of, part_of, core_ss.at[l, stage], core_rs.at[l, stage], 1)

    def seat(device):
        return lax.rem(device + dpn // 2, dpn)

    def in_stage(device, stage):
        early = (seat(device) + 1) * per <= EARLY
        return jnp.logical_not(early) if stage else early

    def dp_remote(src, dst, stage, l, i):
        return pltpu.make_async_remote_copy(src_ref=src, dst_ref=dst, send_sem=dp_ss.at[stage, l], recv_sem=dp_rs.at[stage, l],
                                            device_id={'dp': lax.rem(p + i, dpn)}, device_id_type=MESH)

    def spread_copy(l, i):
        return dp_remote(half.at[l, pl.ds(seat(lax.rem(p + i, dpn)) * per, per)], dp_recv.at[l, pl.ds((i - 1) * per, per)], 0, l, i)

    def dp_all(l, stage):
        part_of = (dp_recv.at[l], gathered.at[l, slice((dpn - 1) * per)])[stage]
        return dp_remote(part_of, part_of, stage, l, 1)

    def pieces(count):
        part_of = w_recv.at[1, slice(count * piece)]
        return dp_remote(part_of, part_of, 2, 0, 1)

    def cross_copy(l):
        return remote(cross_send.at[l], cross_recv.at[l], cross_ss.at[l], cross_rs.at[l], 2)

    def gather_copy(l, i, owner):
        return dp_remote(own_sum.at[l], gathered.at[l, pl.ds(seat(owner) * per, per)], 1, l, i)

    def output_copies(action):
        block, more = n_send.at[0], n_send.at[1]
        most = slice(block.shape[0] - share)
        end = pl.ds(block.shape[0] - share, share)
        sems = n_ss.at[2, 0], n_rs.at[2, 0]
        extra = remote(more.at[end], no_recv.at[end], n_ss.at[2, 2], n_rs.at[2, 2], 3)
        first_core = c == 0

        @pl.when(first_core)
        def _():
            getattr(remote(block.at[most], no_recv.at[most], *sems, 2), action)()
            if action == 'wait_recv':
                extra.wait_recv()

        @pl.when(jnp.logical_not(first_core))
        def _():
            getattr(remote(block, no_recv, *sems, 2), action)()
            if action != 'wait_recv':
                getattr(extra, action)()

    def part_piece(q, a):
        return remote(part.at[q, :, a], part_recv.at[q, :, a], p_ss.at[q], p_rs.at[q], 1)

    def part_copy(q):
        return remote(part.at[q], part_recv.at[q], p_ss.at[q], p_rs.at[q], 1)

    wide = D // GROUP
    tiles = nodes // D
    over = range(tiles * D, nodes, wide)

    def node_rows(k):
        return slice(k * cols, (k + 1) * cols) if k < tiles else pl.ds(tiles * cols + (k - tiles) * cols // GROUP, cols // GROUP)

    def pack_nodes(take, out):
        for k in range(tiles):
            out[node_rows(k), :] = take(k * D, D)
        for k, start in enumerate(over):
            val = take(start, wide)
            out[node_rows(tiles + k), :] = beside([val[r] for r in rest])

    def unpack_nodes(src, put):
        for k in range(tiles):
            put(k * D, src[node_rows(k), :])
        for k, start in enumerate(over):
            val = src[node_rows(tiles + k), :]
            put(start, stacked([val[:, rows_of(g)] for g in range(GROUP)]))

    def put_rows(ref, rows):
        def put(start, val):
            ref[rows, start:start + val.shape[1]] = val.astype(ref.dtype)

        return put

    def put_output(ref):
        def put(start, val):
            used = min(val.shape[1], nodes - start)
            ref[ox, :, start:start + used] = val[:, :used].astype(ref.dtype)

        return put

    def take_rows(ref, rows):
        return lambda start, width: ref[rows, start:start + width].astype(F32)

    def load_nodes(raw, sample, out):
        node_pad[:, :nodes] = raw[sample].astype(F32)
        pack_nodes(take_rows(node_pad, every), out)

    def keep_nodes(own):
        own[...] = jnp.zeros_like(own)
        own[:cols, :] = node_pad[...].astype(own.dtype)

    def load_edges(raw, send, own, kind):
        def put(j, lanes_j, val_of):
            for d in OTHERS:
                sample = x if d < 2 else ox
                send[slot(d), j] = val_of(sample, oc if d % 2 else c).astype(F32)
            own[:cols, lanes_j] = val_of(x, c)

        def chunk(j):
            put(j, at(j, EC), lambda s, h: raw[s, :, pl.ds(pl.multiple_of(h * eh + j * EC, D), EC)])
            for d in SEND_ORDER:
                edge_start(kind, j, d)

        loop(nch - 1, chunk)
        first = (nch - 1) * EC
        used = edges - eh - first
        last = pl.ds(first, EC)

        def tail(s, h):
            left = raw[s, :, pl.ds(first, EC)]
            right = beside([raw[s, :, pl.ds(eh + first, used)], jnp.zeros((cols, EC - used), BF)])
            return jnp.where(h == 0, left.astype(F32), right.astype(F32)).astype(BF)

        put(nch - 1, last, tail)
        for d in SEND_ORDER:
            edge_start(kind, nch - 1, d)

    def place_edges(raw, block, d, j):
        s = x if d < 2 else ox
        h = oc if d % 2 else c
        val = block.astype(BF)
        first = (nch - 1) * EC
        used = edges - eh - first

        @pl.when(jnp.logical_or(j < nch - 1, h == 0))
        def _():
            raw[s, :, pl.ds(pl.multiple_of(h * eh + j * EC, D), EC)] = val

        @pl.when(jnp.logical_and(j == nch - 1, h == 1))
        def _():
            raw[s, :, pl.ds(eh + first, used)] = val[:, :used]

    def scoped(e0, e1, ge, msg, v0, v1, v2, agg0, agg1, d_agg, scol, rcol, srow, rrow, iota, lanes, ew1, ew1t, ew2, ew2t, nw1, nw1t, nw2, nw2t, vecs):
        tables = (v0, v1, v2)
        aggs = (agg0, agg1)
        edges_in = (e0, e1)

        barrier = pltpu.get_barrier_semaphore()
        for d in OTHERS:
            pl.semaphore_signal(barrier, device_id={'tp': peer[d]}, device_id_type=MESH)
        for copy in (first_load, node_load, *small_loads, edge_load, gnode_load, gedge_load):
            copy.start()
        node_pad[...] = jnp.zeros_like(node_pad)
        with jax.named_scope('barrier'):
            @pl.when(t != LEADER)
            def _():
                pl.semaphore_wait(barrier, len(OTHERS))

            @pl.when(t == HELPER)
            def _():
                pl.semaphore_signal(ready, device_id={'tp': LEADER}, device_id_type=MESH)

            @pl.when(t == LEADER)
            def _():
                pl.semaphore_wait(ready)

        first_load.wait()
        with jax.named_scope('send_nodes'):
            load_nodes(node_raw, ox, n_send.at[0])
        ncop = node_copies(n_send, n_recv, 0)
        ncop[1].start()
        node_load.wait()
        load_nodes(node_raw, x, n_send.at[1])
        keep_nodes(v0)
        ncop[0].start()
        for copy in small_loads:
            copy.wait()
        q = cols
        w_send[:HEAD, :] = jnp.zeros((HEAD, D), F32)
        for k in THREE:
            w_send[k * layers:(k + 1) * layers, :cols] = evec_in[k]
            w_send[(3 + k) * layers:(4 + k) * layers, :cols] = nvec_in[k]
        for l in range(layers):
            w_send[packed(l, 0, 3), :] = ew1_in[pl.ds(l * 3 * q, 3 * q), :].astype(F32)
            w_send[packed(l, 3), :] = ew2_in[pl.ds(l * q, q), :].astype(F32)
            w_send[packed(l, 4, 2), :] = nw1_in[pl.ds(l * 2 * q, 2 * q), :].astype(F32)
            w_send[packed(l, 6), :] = nw2_in[pl.ds(l * q, q), :].astype(F32)
        pl.when(brings)(w_cross.start)
        w_pair.start()
        edge_load.wait()
        with jax.named_scope('send_edges'):
            load_edges(edge_raw, e_send, e0, EDGE_IN)
        gnode_load.wait()
        load_nodes(gnode_raw, ox, gn_send.at[0])
        load_nodes(gnode_raw, x, gn_send.at[1])
        keep_nodes(d_part)
        gcop = node_copies(gn_send, gn_recv, 1)
        gcop[1].start()
        gcop[0].start()
        gedge_load.wait()
        with jax.named_scope('send_grads'):
            load_edges(gedge_raw, g_send, ge, GRAD_IN)

        with jax.named_scope('dp_barrier'):
            @pl.when(t == LEADER)
            def _():
                for i in dp_others:
                    pl.semaphore_signal(barrier, device_id={'dp': lax.rem(p + i, dpn)}, device_id_type=MESH)
                pl.semaphore_wait(barrier, len(OTHERS) + dpn - 1)
                for d in OTHERS:
                    pl.semaphore_signal(ready, device_id={'tp': peer[d]}, device_id_type=MESH)

            @pl.when(t != LEADER)
            def _():
                pl.semaphore_wait(ready)

        @pl.when(brings)
        def _():
            w_cross.wait_recv()
            for i in dp_others:
                weight_copy(i, p).start()

        @pl.when(c == 1)
        def _():
            for recv in (e_recv, g_recv):
                recv[:, last, :, D:] = jnp.zeros((len(OTHERS), cols, EC - D), F32)

        iota[...] = lax.broadcasted_iota(jnp.int32, (T, D), 0).astype(I16)
        lanes[...] = lax.broadcasted_iota(jnp.int32, (16, D), 1).astype(I16)

        ids_raw[...] = jnp.full(ids_raw.shape, -1, jnp.int32)
        for which, src in enumerate((send_ids, recv_ids)):
            ids_raw[which:which + 1, :edges] = src[...].reshape(1, edges)

        def ids(b):
            for which, (row_ref, col_ref) in enumerate(((srow, scol), (rrow, rcol))):
                wide = jnp.broadcast_to(ids_raw[which:which + 1, pl.ds(pl.multiple_of(c * eh + b * D, D), D)], (D, D))
                row_ref[at(b, 16), :] = wide[:16].astype(I16)
                col_ref[at(b, D), :] = flip(wide.astype(F32)).astype(jnp.int32).astype(I16)

        with jax.named_scope('ids'):
            loop(eh // D, ids)

        def keys(ref, step):
            return [ref[pl.ds(pl.multiple_of(step * (KS // D) * 16 + 16 * h, 16), 1), :] for h in range(KS // D)]

        bias_cols[...] = flip(stacked([eb1_in[...], nb1_in[...], jnp.zeros((D - 2 * layers, D), F32)]))

        def join_weights(l):
            for d in range(GROUP):
                src = w_recv.at[slot(d)] if d else w_send
                r = rows_of(d)
                for k in THREE:
                    ew1[l, pl.ds(k * D + d * q, q), :] = src[packed(l, k), :].astype(BF)
                ew2t[l, r, :] = src[packed(l, 3), :].astype(BF)
                for k in BOTH:
                    nw1[l, pl.ds(k * D + d * q, q), :] = src[packed(l, 4 + k), :].astype(BF)
                nw2t[l, r, :] = src[packed(l, 6), :].astype(BF)

            def flip_bf(mat):
                return flip(mat.astype(F32)).astype(BF)

            for k in THREE:
                ew1t[l, :, mat(k)] = flip_bf(ew1[l, mat(k), :])
            for k in BOTH:
                nw1t[l, :, mat(k)] = flip_bf(nw1[l, mat(k), :])
            ew2[l] = flip_bf(ew2t[l])
            nw2[l] = flip_bf(nw2t[l])

        def wait_recvs(copies):
            copies[1].wait_recv()
            copies[2].start()
            copies[0].wait_recv()
            copies[2].wait_recv()

        with jax.named_scope('node_wait'):
            wait_recvs(ncop)
        for d in OTHERS:
            unpack_nodes(n_recv.at[slot(d)], put_rows(v0, rows_of(d)))
        with jax.named_scope('weight_wait'):
            pl.when(jnp.logical_not(brings))(pieces(dpn - 1).wait_recv)
            if dpn > 2:
                pl.when(brings)(pieces(dpn - 2).wait_recv)
            w_relay.start()
            w_pair.wait_recv()
            w_relay.wait_recv()
        rows_all = beside([w_send[:HEAD, :cols]] + [w_recv[d, :HEAD, :cols] for d in range(3)])
        vecs[...] = flip(stacked([rows_all, jnp.zeros((D - HEAD, D), F32)]))
        join_weights(0)

        def vec(l, node):
            first = 6 * node + l
            return [vecs[:, first + 2 * k:first + 2 * k + 1] for k in THREE]

        def bias(l, node):
            return bias_cols[:, node * layers + l:node * layers + l + 1]

        def hidden_of_nodes(l):
            table, b1 = tables[l], bias(l, 0)

            def body(step):
                xs = gather(table, keys(srow, step), iota).astype(BF)
                xr = gather(table, keys(rrow, step), iota).astype(BF)
                hidden[l, :, at(step, KS)] = dot(ew1t[l, :, mat(1, 2)], stacked([xs, xr])) + b1

            loop(eh // KS, body)

        def edge_forward(l):
            e_in = edges_in[l]

            def body(j):
                for sub in range(EC // T):
                    a = at(j * (EC // T) + sub, T)
                    if l == 0:
                        if sub == 0:
                            chunk_arrived(EDGE_IN, j)
                        for d in OTHERS:
                            e_in[rows_of(d), a] = e_recv[slot(d), j, :, sub * T:(sub + 1) * T].astype(BF)
                    e_val = e_in[:, a]
                    hid = hidden[l, :, a] + dot(ew1t[l, :, mat(0)], e_val)
                    hidden[l, :, a] = hid
                    message, nrm, std = mlp_tail(hid, ew2t[l], vec(l, 0))
                    normed[l, :, a] = nrm
                    inv[l:l + 1, a] = std
                    msg[:, a] = message
                    e_new = (e_val.astype(F32) + message.astype(F32)).astype(BF)
                    if l < top:
                        edges_in[l + 1][:, a] = e_new
                    else:
                        for d in OTHERS:
                            e_send[slot(d), j, :, sub * T:(sub + 1) * T] = e_new[rows_of(d)].astype(F32)
                        if sub == 0:
                            own_parts = []
                        own_parts.append(e_new[:q])
                if l == top:
                    for d in SEND_ORDER:
                        edge_start(EDGE_OUT, j, d)
                    place_edges(edge_raw, beside(own_parts), 0, j)

            loop(nch, body)

        def segment_sum(acc, ids_ref):
            acc[...] = jnp.zeros(acc.shape, F32)

            def body(step):
                scatter(acc, msg[:, at(step, KS)], ids_ref[at(step, KS), :], lanes)

            loop(eh // KS, body)

        def node_forward(l):
            table, agg, out = tables[l], aggs[l], tables[l + 1]

            def body(step):
                a = pl.ds(pl.multiple_of(step * TN, D), TN)
                v_in = table[:, a]
                agg_bf = (part[l, :, a] + swap_halves(part_recv[l, :, a])).astype(BF)
                agg[:, a] = agg_bf
                hid = dot(nw1t[l], stacked([v_in, agg_bf])) + bias(l, 1)
                nhid[l, :, a] = hid
                message, nrm, std = mlp_tail(hid, nw2t[l], vec(l, 1))
                nnrm[l, :, a] = nrm
                ninv[l:l + 1, a] = std
                out[:, a] = (v_in.astype(F32) + message.astype(F32)).astype(BF)

            loop(npad // TN, body)

        for l in range(layers):
            with jax.named_scope(f'gather_{l}'):
                hidden_of_nodes(l)
            if l == top:
                edges_sent(EDGE_IN)
            with jax.named_scope(f'edge_forward_{l}'):
                edge_forward(l)
            with jax.named_scope(f'sum_{l}'):
                segment_sum(part.at[l], rcol)
            part_copy(l).start()
            if l == 0:
                join_weights(1)
                gcop[1].wait_recv()
                gcop[2].start()
            with jax.named_scope(f'part_wait_{l}'):
                part_copy(l).wait_recv()
            with jax.named_scope(f'node_forward_{l}'):
                node_forward(l)
        for copy in ncop[:2]:
            copy.wait_send()
        for which in BOTH:
            pack_nodes(take_rows(tables[layers], rows_of(2 + which)), n_send.at[which])
        output_copies('start')
        node_raw[x] = tables[layers][:q, :nodes]

        for k in range(layers):
            part_copy(k).wait_send()
        s_sum, r_sum = (part.at[k] for k in BOTH)
        grad[...] = jnp.zeros_like(grad)
        sums[...] = jnp.zeros_like(sums)
        with jax.named_scope('grad_node_wait'):
            gcop[0].wait_recv()
            gcop[2].wait_recv()
        for d in OTHERS:
            unpack_nodes(gn_recv.at[slot(d)], put_rows(d_part, rows_of(d)))

        def node_backward(l):
            table, agg = tables[l], aggs[l]

            def body(step):
                a = pl.ds(pl.multiple_of(step * TN, D), TN)
                d_in = d_part[:, a]
                if l < top:
                    d_in = d_in + part[layers + l + 1, :, a] + swap_halves(part_recv[layers + l + 1, :, a])
                    d_in = d_in.astype(BF).astype(F32)
                d_hid, d_w2, parts = mlp_back(d_in, nhid[l, :, a], nnrm[l, :, a], ninv[l:l + 1, a], nw2[l], vec(l, 1))
                add_sums(sums.at[l, 1], [parts])
                grad[l, 4] += d_w2
                grad[l, 2] += dot_nt(table[:, a], d_hid)
                grad[l, 3] += dot_nt(agg[:, a], d_hid)
                d_part[:, a] = d_in + dot(nw1[l, mat(0), :], d_hid)
                d_agg[:, a] = dot(nw1[l, mat(1), :], d_hid).astype(BF)

            loop(npad // TN, body)

        def gather_back():
            def body(step):
                msg[:, at(step, KS)] = gather(d_agg, keys(rrow, step), iota).astype(BF)

            loop(eh // KS, body)

        def edge_backward(l):
            e_in = edges_in[l]

            def body(j):
                all_parts, d_w2s, d_w1s, own_parts = [], [], [], []
                for sub in range(EC // T):
                    a = at(j * (EC // T) + sub, T)
                    if l == top:
                        if sub == 0:
                            chunk_arrived(GRAD_IN, j)
                        for d in OTHERS:
                            ge[rows_of(d), a] = g_recv[slot(d), j, :, sub * T:(sub + 1) * T].astype(BF)
                    d_res = ge[:, a].astype(F32)
                    d_msg = d_res + msg[:, a].astype(F32)
                    d_hid, d_w2, parts = mlp_back(d_msg, hidden[l, :, a], normed[l, :, a], inv[l:l + 1, a], ew2[l], vec(l, 0))
                    all_parts.append(parts)
                    d_w2s.append(d_w2)
                    d_w1s.append(dot_nt(e_in[:, a], d_hid))
                    msg[:, a] = d_hid
                    d_new = (d_res + dot(ew1[l, mat(0), :], d_hid)).astype(BF)
                    if l > 0:
                        ge[:, a] = d_new
                    else:
                        for d in OTHERS:
                            g_send[slot(d), j, :, sub * T:(sub + 1) * T] = d_new[rows_of(d)].astype(F32)
                        own_parts.append(d_new[:q])
                add_sums(sums.at[l, 0], all_parts)
                grad[l, 1] += sum(d_w2s[1:], d_w2s[0])
                grad[l, 0] += sum(d_w1s[1:], d_w1s[0])
                if l == 0:
                    @pl.when(j < hold)
                    def _():
                        for d in SEND_ORDER:
                            edge_start(GRAD_OUT, j, d)
                    place_edges(gedge_raw, beside(own_parts), 0, j)

            loop(nch, body)

        def vector_slab(l):
            def total(node, k):
                return column_sum(flip(sums[l, node, mat(k), :]))

            lat = stacked([total(node, k) for node in BOTH for k in THREE])
            biases = stacked([total(node, 3) for node in BOTH])
            n_lat = lat.shape[0]
            for d in range(GROUP):
                grad[l, VEC_SLAB, d * cols:d * cols + n_lat, :cols] = lat[:, rows_of(d)]
                grad[l, VEC_SLAB, d * cols + n_lat:d * cols + n_lat + 2, :] = biases

        def reduce_start(l, stage):
            for b in BOTH:
                core_copy(l, b, stage).start()

        def chip_sum(l, stage):
            row = lax.broadcasted_iota(jnp.int32, (cols, D), 0)
            edge_row = jnp.logical_or(row < 3, row == 6)
            core_all(l, stage).wait_recv()
            for b in BOTH:
                for k in range(SLABS)[STAGES[stage]]:
                    own = grad[l, k, rows_of(2 * b), :]
                    if k in EDGE_SLABS:
                        own = own + core_recv[l, b, k]
                    elif k == VEC_SLAB:
                        other = core_recv[l, b, k]
                        own = own + jnp.where(edge_row, other, 0.0)
                        own = jnp.where(jnp.logical_and(row == 7, c == 1), other, own)
                    half[l, k, b] = own
            for i in dp_others:
                @pl.when(in_stage(lax.rem(p + i, dpn), stage))
                def _():
                    spread_copy(l, i).start()

        def dp_sum(l, stage):
            @pl.when(in_stage(p, stage))
            def _():
                total = half[l, pl.ds(seat(p) * per, per)]
                dp_all(l, 0).wait_recv()
                for i in dp_others:
                    total = total + dp_recv[l, pl.ds((i - 1) * per, per)]
                own_sum[l] = total[:, 0]
                cross_send[l] = total[:, 1]
                cross_copy(l).start()

        def cross_sum(l):
            cross_copy(l).wait_recv()
            total = own_sum[l] + cross_recv[l]
            own_sum[l] = total
            gathered[l, pl.ds(seat(p) * per, per)] = total
            for i in dp_others:
                gather_copy(l, i, p).start()

        def project(l):
            table = tables[l]

            def body(step):
                a = pl.ds(pl.multiple_of(step * TN, D), TN)
                s_bf, r_bf, v_in = s_sum[:, a].astype(BF), r_sum[:, a].astype(BF), table[:, a]
                part[layers + l, :, a] = dot(ew1[l, mat(1), :], s_bf) + dot(ew1[l, mat(2), :], r_bf)
                if l > 0:
                    part_piece(layers + l, a).start()
                grad[l, 6] += dot_nt(v_in, s_bf)
                grad[l, 7] += dot_nt(v_in, r_bf)

            loop(npad // TN, body)

        for l in reversed(range(layers)):
            first_layer = l == 0
            with jax.named_scope(f'node_backward_{l}'):
                node_backward(l)
            if first_layer:
                with jax.named_scope('chip_sum_1'):
                    chip_sum(1, 0)
                    chip_sum(1, 1)
            with jax.named_scope(f'gather_back_{l}'):
                gather_back()
            if first_layer:
                edges_sent(GRAD_IN)
            with jax.named_scope(f'edge_backward_{l}'):
                edge_backward(l)
            vector_slab(l)
            reduce_start(l, 0)
            if first_layer:
                with jax.named_scope('dp_sum_1'):
                    dp_sum(1, 0)
                    dp_sum(1, 1)
            with jax.named_scope(f'sum_send_{l}'):
                segment_sum(s_sum, scol)
            if first_layer:
                with jax.named_scope('chip_sum_0'):
                    chip_sum(0, 0)
            with jax.named_scope(f'sum_recv_{l}'):
                segment_sum(r_sum, rcol)
            with jax.named_scope(f'project_{l}'):
                project(l)
            reduce_start(l, 1)
            if first_layer:
                part_copy(layers + l).start()
            if first_layer:
                with jax.named_scope('chip_sum_late'):
                    chip_sum(0, 1)
                with jax.named_scope('dp_sum_0'):
                    dp_sum(0, 0)
            with jax.named_scope(f'back_wait_{l}'):
                part_copy(layers + l).wait_recv()

        def final(step):
            a = pl.ds(pl.multiple_of(step * TN, D), TN)
            d_in = (d_part[:, a] + part[layers, :, a] + swap_halves(part_recv[layers, :, a])).astype(BF)
            v2[:, a] = d_in

        loop(npad // TN, final)
        gnode_raw[x] = v2[:q, :nodes]
        with jax.named_scope('dp_sum_late'):
            dp_sum(0, 1)

        gcop[1].wait_send()
        dn_send = gn_send.at[0]
        pack_nodes(take_rows(v2, rows_of(2)), dn_send)
        dn_copy = remote(dn_send, dn_recv, n_ss.at[2, 1], n_rs.at[2, 1], 2)
        dn_copy.start()

        def send_rest(j):
            for d in SEND_ORDER:
                edge_start(GRAD_OUT, j, d)

        loop(nch, send_rest, hold)

        with jax.named_scope('node_out_wait'):
            output_copies('wait_recv')
        unpack_nodes(no_recv, put_output(node_raw))

        def place_e(j):
            for d in OTHERS:
                place_edges(edge_raw, eo_recv[slot(d), j], d, j)

        with jax.named_scope('place_edge_out'):
            for group in THREE:
                group_arrived(EDGE_OUT, group)
            loop(nch, place_e)

        def place_g(j):
            for d in OTHERS:
                place_edges(gedge_raw, de_recv[slot(d), j], d, j)

        with jax.named_scope('place_first'):
            group_arrived(GRAD_OUT, 0)
            loop(hold, place_g)
        for l in range(layers):
            with jax.named_scope(f'cross_sum_{l}'):
                cross_sum(l)
        with jax.named_scope('d_node_wait'):
            dn_copy.wait_recv()
        unpack_nodes(dn_recv, put_output(gnode_raw))
        with jax.named_scope('place_rest'):
            group_arrived(GRAD_OUT, 1)
            loop(last, place_g, hold)
        for l in range(layers):
            dp_all(l, 1).wait_recv()
            ew1_buf[l, 0] = gathered[l, 0]
            ew1_buf[l, 1:] = gathered[l, EARLY:]
            ew2_buf[l] = gathered[l, 1]
            nw1_buf[l] = gathered[l, 2:4]
            nw2_buf[l] = gathered[l, 4]
            small = gathered[l, VEC_SLAB]
            for k in THREE:
                evec_buf[k, l:l + 1, :] = small[k:k + 1, :cols]
                nvec_buf[k, l:l + 1, :] = small[3 + k:4 + k, :cols]
            eb1_buf[l:l + 1, :] = small[6:7]
            nb1_buf[l:l + 1, :] = small[7:8]
        for l in range(layers):
            for stage in BOTH:
                core_all(l, stage).wait_send()
            cross_copy(l).wait_send()
            dp_all(l, 0).wait_send()
            dp_all(l, 1).wait_send()
        for copy in (ncop[2], gcop[0], gcop[2], w_pair, w_relay):
            copy.wait_send()

        @pl.when(brings)
        def _():
            w_cross.wait_send()
            pieces(dpn - 1).wait_send()

        output_copies('wait_send')
        dn_copy.wait_send()
        for k in range(layers, 2 * layers):
            part_copy(k).wait_send()
        edges_sent(EDGE_OUT)
        with jax.named_scope('place_last'):
            group_arrived(GRAD_OUT, 2)
            loop(nch, place_g, last)
        edges_sent(GRAD_OUT)

    bf = lambda *s: pltpu.VMEM(s, BF)
    pl.run_scoped(
        scoped, bf(D, eh), bf(D, eh), bf(D, eh), bf(D, eh), bf(D, npad), bf(D, npad), bf(D, npad), bf(D, npad), bf(D, npad), bf(D, npad),
        pltpu.VMEM((eh, D), I16), pltpu.VMEM((eh, D), I16), pltpu.VMEM((eh // D * 16, D), I16), pltpu.VMEM((eh // D * 16, D), I16),
        pltpu.VMEM((T, D), I16), pltpu.VMEM((16, D), I16),
        bf(layers, 3 * D, D), bf(layers, D, 3 * D), bf(layers, D, D), bf(layers, D, D),
        bf(layers, 2 * D, D), bf(layers, D, 2 * D), bf(layers, D, D), bf(layers, D, D), pltpu.VMEM((D, D), F32))


def finish_moves(src, dst):
    if len(src.shape) != 3 or src.dtype != BF:
        return [(src, dst)]
    return [(src.at[s, pl.ds(r, 8)], dst.at[s, pl.ds(r, 8)]) for s in range(src.shape[0]) for r in range(0, src.shape[1], 8)]


def finish_kernel(*refs):
    count = len(refs) // 2
    moves = sum((finish_moves(refs[k], refs[count + k]) for k in range(count)), [])
    puts = [pltpu.make_async_copy(src, dst, refs[-1]) for src, dst in moves]
    for put in puts:
        put.start()
    for put in puts:
        put.wait()


def keep_in_vmem(val):
    return pltpu.with_memory_space_constraint(val, pltpu.VMEM)


def finish(arrays):
    return pl.pallas_call(
        finish_kernel,
        name='finish',
        out_shape=[jax.ShapeDtypeStruct(a.shape, a.dtype) for a in arrays],
        in_specs=[VM] * len(arrays),
        out_specs=[HB] * len(arrays),
        scratch_shapes=[pltpu.SemaphoreType.DMA],
        compiler_params=pltpu.CompilerParams(vmem_limit_bytes=1 << 20),
    )(*[keep_in_vmem(a) for a in arrays])


def solution(mesh):
    lat_spec = P('dp', None, 'tp')
    first_spec = P(None, None, 'tp', None)
    col_spec = P(None, None, 'tp')
    param_specs = (first_spec, P(), col_spec, col_spec, first_spec, P(), col_spec, col_spec)
    in_specs = (lat_spec, lat_spec, P(), P(), lat_spec, lat_spec) + param_specs
    out_specs = (lat_spec, lat_spec, lat_spec, lat_spec) + param_specs
    shape = jax.ShapeDtypeStruct

    def local_step(node_lat, edge_lat, senders, receivers, grad_node, grad_edge, edge_w1, edge_b1, edge_w2, edge_vec, node_w1, node_b1, node_w2, node_vec):
        layers = edge_w1.shape[0]
        cols = node_lat.shape[2]
        nodes, edges = node_lat.shape[1], edge_lat.shape[1]
        npad = -(-nodes // TN) * TN
        eh = -(-edges // (2 * EC)) * EC
        nch = eh // EC
        dpn = mesh.shape['dp']
        per = SLABS // dpn
        dims = (layers, cols, nodes, edges, npad, eh, dpn)
        flat = lambda arr: jnp.swapaxes(arr, 1, 2)
        lead = lambda arr: jnp.transpose(arr, (1, 0, 2))
        args = (flat(node_lat), flat(edge_lat), flat(grad_node), flat(grad_edge), senders, receivers,
                edge_w1.reshape(-1, D), flat(edge_w2).reshape(-1, D), node_w1.reshape(-1, D), flat(node_w2).reshape(-1, D),
                lead(edge_vec), lead(node_vec), edge_b1, node_b1)
        vm, sem = pltpu.VMEM, pltpu.SemaphoreType.DMA
        packed = nodes // D * cols + -(-(nodes % D) * GROUP // D) * cols // GROUP
        wrows = -(-(HEAD + layers * LROWS) // (8 * (dpn - 1))) * 8 * (dpn - 1)
        lat_n, lat_e = (2, cols, nodes), (2, cols, edges)
        outs = [RESULT(lat_n, BF), RESULT(lat_e, BF), RESULT(lat_n, BF), RESULT(lat_e, BF),
                RESULT((layers, 3, cols, D), F32), RESULT((layers, D), F32), RESULT((layers, cols, D), F32), RESULT((3, layers, cols), F32),
                RESULT((layers, 2, cols, D), F32), RESULT((layers, D), F32), RESULT((layers, cols, D), F32), RESULT((3, layers, cols), F32)]
        scratch = [
            *[vm(a.shape, a.dtype) for a in args[4:]], vm((wrows, D), F32), vm((3, wrows, D), F32),
            *[vm((many, packed, D), F32) for many in (2, 3, 2, 3)], *[vm((packed, D), F32)] * 2, vm((cols, npad), F32),
            *[vm((kinds, len(OTHERS), cols + cols // GROUP, D), F32) for kinds in (2, GROUP)], *[vm((len(OTHERS), nch, cols, EC), F32)] * 6,
            vm((2 * layers, D, npad), F32), vm((2 * layers, D, npad), F32),
            vm((layers, D, eh), F32), vm((layers, D, eh), F32), vm((layers, eh), F32),
            vm((layers, D, npad), F32), vm((layers, D, npad), F32), vm((layers, npad), F32),
            vm((D, npad), F32), vm((2, 2 * eh), jnp.int32), vm((D, D), F32), vm((layers, 2, 4 * D, D), F32),
            vm((layers, SLABS, D, D), F32), vm((layers, 2, SLABS, cols, D), F32), vm((layers, SLABS, 2, cols, D), F32),
            vm((layers, (dpn - 1) * per, 2, cols, D), F32), vm((layers, per, cols, D), F32), vm((layers, per, cols, D), F32),
            vm((layers, per, cols, D), F32), vm((layers, SLABS, cols, D), F32),]
        own_sems = [
            sem((layers, 2)), sem((3, layers)), sem((layers,)), sem((3,)), sem((3, 3)), sem((2, nch)), sem((2, 5)), sem((2 * layers,)),
            pltpu.SemaphoreType.REGULAR,
            sem((len(args) + 1,)), sem((3,)), sem((3, 3)), sem((4, 4)), sem((2 * layers,)), sem((layers, 2)), sem((3, layers)), sem((layers,))]
        res = pl.pallas_call(
            lambda *refs: pl.run_scoped(lambda *own: step_kernel(dims, *refs, *own), *own_sems),
            name='graph_step',
            out_shape=outs,
            in_specs=[HB] * len(args),
            out_specs=[VM] * len(outs),
            scratch_shapes=scratch,
            compiler_params=pltpu.CompilerParams(collective_id=0, has_side_effects=True, vmem_limit_bytes=VMEM_LIMIT),
        )(*args)

        res = finish(res)
        return (flat(res[0]), flat(res[1]), flat(res[2]), flat(res[3]),
                res[4], res[5], flat(res[6]), lead(res[7]), res[8], res[9], flat(res[10]), lead(res[11]))

    return jax.shard_map(local_step, mesh=mesh, in_specs=in_specs, out_specs=out_specs, check_vma=False)
```

```python
import jax
import jax.numpy as jnp
from jax import lax
from jax.experimental import pallas as pl
from jax.experimental.pallas import tpu as pltpu
from jax.sharding import PartitionSpec as P

LN_EPS = 1e-5
D = 128
T = 256
TN = 384
EC = 512
KS = 2816
BF = jnp.bfloat16
F32 = jnp.float32
I16 = jnp.int16
MESH = pl.DeviceIdType.MESH
VM = pl.BlockSpec(memory_space=pltpu.VMEM)
HB = pl.BlockSpec(memory_space=pl.ANY)
RESULT = pltpu.VMEM
GROUP = 4
BOTH = (0, 1)
THREE = (0, 1, 2)
OTHERS = (1, 2, 3)
EDGE_IN, GRAD_IN, EDGE_OUT, GRAD_OUT = range(4)
SEND_ORDER = (2, 3, 1)
LROWS = 7 * (D // 4)
HEAD = 8
LEADER = GROUP - 1
HELPER = LEADER - 1
VMEM_LIMIT = 63_000_000
SLABS = 8
EARLY = 6
VEC_SLAB = 5
EDGE_SLABS = (0, 1, 6, 7)
STAGES = (slice(0, EARLY), slice(EARLY, SLABS))


def dot(a, b):
    return jnp.dot(a, b, preferred_element_type=F32)


def dot_nt(a, b):
    return lax.dot_general(a, b, (((1,), (1,)), ((), ())), preferred_element_type=F32)


def mat(k, n=1):
    return slice(k * D, (k + n) * D)


def rows_of(d):
    q = D // 4
    return slice(d * q, (d + 1) * q)


def at(step, width):
    return pl.ds(pl.multiple_of(step * width, width), width)


def loop(stop, body, start=0):
    def step(j, carry):
        body(j)
        return carry

    lax.fori_loop(start, stop, step, 0)


def column_sum(val):
    return jnp.sum(val, axis=0, keepdims=True)


def flip(val):
    return jnp.swapaxes(val, 0, 1)


def stacked(parts):
    return jnp.concatenate(parts, axis=0)


def beside(parts):
    return jnp.concatenate(parts, axis=1)


def slot(d):
    return d - 1


def sigmoid(hidden):
    return 1.0 / (1.0 + jnp.exp(-hidden))


def fold(val):
    total = val[:, mat(0)]
    for start in range(D, val.shape[1], D):
        total = total + val[:, start:start + D]
    return total


def swap_halves(val):
    return stacked([val[rows_of(d)] for d in (1, 0, 3, 2)])


def gather(table, keys, iota):
    acc = None
    nodes = table.shape[1]
    one, zero = jnp.ones((), BF), jnp.zeros((), BF)
    for base in range(0, nodes, T):
        width = min(T, nodes - base)
        ids = iota[0:width, :]
        hot = beside([jnp.where(ids == (key - jnp.asarray(base, I16)), one, zero) for key in keys])
        part = dot(table[:, base:base + width], hot)
        acc = part if acc is None else acc + part
    return acc


def scatter(acc_ref, val, cols, lanes):
    nodes = acc_ref.shape[1]
    one, zero = jnp.ones((), BF), jnp.zeros((), BF)
    row = lanes[0:1, :]
    for base in range(0, nodes, T):
        width = min(T, nodes - base)
        hot = beside([jnp.where((row + jnp.asarray(base + s, I16)) == cols, one, zero) for s in range(0, width, D)])
        acc_ref[:, base:base + width] += dot(val, hot)


def mlp_tail(hidden, w2t, vec):
    act = (hidden * sigmoid(hidden)).astype(BF)
    out = dot(w2t, act) + vec[0]
    mean = column_sum(out) / D
    centered = out - mean
    var = column_sum(centered * centered) / D
    inv = lax.rsqrt(var + LN_EPS)
    normed = centered * inv
    message = (normed * vec[1] + vec[2]).astype(BF)
    return message, normed, inv


def mlp_back(d_msg, hidden, normed, inv, w2, vec):
    d_normed = d_msg * vec[1]
    mean0 = column_sum(d_normed) / D
    mean1 = column_sum(d_normed * normed) / D
    d_out = inv * (d_normed - mean0 - normed * mean1)
    d_out_bf = d_out.astype(BF)
    sig = sigmoid(hidden)
    act = (hidden * sig).astype(BF)
    d_w2 = dot_nt(d_out_bf, act)
    d_hidden = dot(w2, d_out_bf) * (sig * (1.0 + hidden * (1.0 - sig)))
    sums = (fold(d_out), fold(d_msg * normed), fold(d_msg), fold(d_hidden))
    return d_hidden.astype(BF), d_w2, sums


def add_sums(ref, parts):
    for q in range(4):
        total = parts[0][q]
        for other in parts[1:]:
            total = total + other[q]
        ref[mat(q), :] += total


def step_kernel(dims, *refs):
    layers, cols, nodes, edges, npad, eh, dpn = dims
    nch = eh // EC
    top = layers - 1
    n_in = 14
    hbm_in = refs[:n_in]
    n_out = 12
    (node_raw, edge_raw, gnode_raw, gedge_raw, ew1_buf, eb1_buf, ew2_buf, evec_buf, nw1_buf, nb1_buf, nw2_buf, nvec_buf) = refs[n_in:n_in + n_out]
    (send_ids, recv_ids, ew1_in, ew2_in, nw1_in, nw2_in, evec_in, nvec_in, eb1_in, nb1_in, w_send, w_recv, n_send, n_recv, gn_send, gn_recv, no_recv, dn_recv,
     node_pad, t_send, t_recv, e_send, g_send, e_recv, g_recv, eo_recv, de_recv, part, part_recv, hidden, normed, inv, nhid, nnrm, ninv, d_part,
     ids_raw, bias_cols, sums, grad, core_recv, half, dp_recv, cross_send, cross_recv, own_sum, gathered,
     core_rs, dp_rs, cross_rs, w_rs, n_rs, e_rs, o_rs, p_rs, ready, load_sem, w_ss, n_ss, e_ss, p_ss, core_ss, dp_ss, cross_ss) = refs[n_in + n_out:]

    t = lax.axis_index('tp')
    p = lax.axis_index('dp')
    per = SLABS // dpn
    dp_others = range(1, dpn)
    x, c = t // 2, lax.rem(t, 2)
    ox, oc = 1 - x, 1 - c
    mate, across = t + oc - c, t + 2 * (ox - x)
    peer = [t, mate, across, mate + across - t]

    def remote(src, dst, ssem, rsem, d):
        return pltpu.make_async_remote_copy(src_ref=src, dst_ref=dst, send_sem=ssem, recv_sem=rsem,
                                            device_id={'tp': peer[d]}, device_id_type=MESH)

    small_in = (send_ids, recv_ids, ew1_in, ew2_in, nw1_in, nw2_in, evec_in, nvec_in, eb1_in, nb1_in)
    loads = [pltpu.make_async_copy(src, dst, load_sem.at[q]) for q, (src, dst) in enumerate(
        zip((hbm_in[0].at[x],) + hbm_in[1:], (node_raw.at[x], edge_raw, gnode_raw, gedge_raw) + small_in))]
    node_load, edge_load, gnode_load, gedge_load, *small_loads = loads
    first_load = pltpu.make_async_copy(hbm_in[0].at[ox], node_raw.at[ox], load_sem.at[n_in])

    def node_copies(send, recv, kind):
        return (remote(send.at[1], recv.at[0], n_ss.at[kind, 0], n_rs.at[kind, 0], 1),
                remote(send.at[0], recv.at[1], n_ss.at[kind, 1], n_rs.at[kind, 1], 2),
                remote(recv.at[1], recv.at[2], n_ss.at[kind, 2], n_rs.at[kind, 2], 1))

    piece = (w_send.shape[0] - HEAD) // (dpn - 1)
    brings = p > 0

    def packed(l, k, count=1):
        return pl.ds(HEAD + l * LROWS + k * cols, count * cols)

    def by_share(action):
        @pl.when(brings)
        def _():
            action(pl.ds(pl.multiple_of(HEAD + (p - 1) * piece, HEAD), piece))

        @pl.when(jnp.logical_not(brings))
        def _():
            action(slice(HEAD))

    w_pair = remote(w_send, w_recv.at[0], w_ss.at[0], w_rs.at[0], 1)
    def w_cross(rows):
        return remote(w_send.at[rows], w_recv.at[1, rows], w_ss.at[1], w_rs.at[1], 2)

    w_relay = remote(w_recv.at[1], w_recv.at[2], w_ss.at[2], w_rs.at[2], 1)

    def weight_copy(i, rows):
        rows = w_recv.at[1, rows]
        return dp_remote(rows, rows, 2, 0, i)

    last = nch - 1
    hold = nch - 3
    share = 2 * (eh - last * EC - D - D // GROUP) * cols // D
    share = min(share, no_recv.shape[0] // 16 * 8)
    buffers = ((e_send, e_recv), (g_send, g_recv), (e_send, eo_recv), (g_send, de_recv))

    def outward(kind):
        return kind in (EDGE_OUT, GRAD_OUT)

    every = slice(None)
    ragged = pl.ds(D, D // GROUP)
    rest = [slice(g * cols // GROUP, (g + 1) * cols // GROUP) for g in range(GROUP)]

    def edge_part(kind, which, j, tail, send_sem, recv_sem, d):
        src, dst = buffers[kind]
        if tail:
            src, dst = t_send.at[kind % 2, which], t_recv.at[kind, which]
        else:
            src, dst = src.at[which, j], dst.at[which, j]
        recv_sems = o_rs.at[kind - EDGE_OUT, recv_sem] if outward(kind) else e_rs.at[kind, recv_sem]
        return remote(src, dst, e_ss.at[kind, send_sem], recv_sems, d)

    def by_half(half_id, j, action):
        narrow = jnp.logical_and(j == last, half_id == 1)

        @pl.when(jnp.logical_not(narrow))
        def _():
            action(False)

        @pl.when(narrow)
        def _():
            action(True)

    def pack_tail(kind, d):
        src, out = buffers[kind][0].at[slot(d), last], t_send.at[kind % 2, slot(d)]
        out[:cols, :] = src[:, :D]
        over = src[:, ragged]
        out[cols:, :] = beside([over[r] for r in rest])

    def unpack_tail(kind, d):
        src, out = t_recv.at[kind, slot(d)], buffers[kind][1].at[slot(d), last]
        out[:, :D] = src[:cols, :]
        over = src[cols:, :]
        out[:, ragged] = stacked([over[:, rows_of(g)] for g in range(GROUP)])

    def edge_start(kind, j, d):
        other = oc if d % 2 else c
        if outward(kind):
            at_last = j == last
            send_sem = jnp.asarray(at_last, jnp.int32)
            recv_sem = jnp.where(at_last, 2 + slot(d), jnp.asarray(j >= hold, jnp.int32))
        else:
            send_sem, recv_sem = jnp.where(j == last, d, 0), j

        def start(tail):
            if tail:
                pack_tail(kind, d)
            edge_part(kind, slot(d), j, tail, send_sem, recv_sem, d).start()

        by_half(c if outward(kind) else other, j, start)

    def edges_sent(kind):
        edge_part(kind, every, slice(0, last), False, 0, 0, 1).wait_send()
        if outward(kind):
            by_half(c, last, lambda tail: edge_part(kind, every, last, tail, 1, 0, 1).wait_send())
        else:
            for d in OTHERS:
                by_half(oc if d % 2 else c, last, lambda tail: edge_part(kind, slot(d), last, tail, d, 0, d).wait_send())

    def chunk_arrived(kind, j):
        def arrived(tail):
            edge_part(kind, every, j, tail, 0, j, 1).wait_recv()
            if tail:
                for d in OTHERS:
                    unpack_tail(kind, d)

        by_half(c, j, arrived)

    def group_arrived(kind, group):
        if group < 2:
            edge_part(kind, every, (slice(0, hold), slice(hold, last))[group], False, 0, group, 1).wait_recv()
        else:
            for d in OTHERS:
                def arrived(tail):
                    edge_part(kind, slot(d), last, tail, 0, 2 + slot(d), d).wait_recv()
                    if tail:
                        unpack_tail(kind, d)

                by_half(oc if d % 2 else c, last, arrived)

    def core_copy(l, b, stage):
        return remote(grad.at[l, STAGES[stage], pl.ds((2 * b + 1) * cols, cols), :], core_recv.at[l, b, STAGES[stage]],
                      core_ss.at[l, stage], core_rs.at[l, stage], 1)

    def core_all(l, stage):
        part_of = core_recv.at[l, :, STAGES[stage]]
        return remote(part_of, part_of, core_ss.at[l, stage], core_rs.at[l, stage], 1)

    def seat(device):
        return lax.rem(device + dpn // 2, dpn)

    def in_stage(device, stage):
        early = (seat(device) + 1) * per <= EARLY
        return jnp.logical_not(early) if stage else early

    def dp_remote(src, dst, stage, l, i):
        return pltpu.make_async_remote_copy(src_ref=src, dst_ref=dst, send_sem=dp_ss.at[stage, l], recv_sem=dp_rs.at[stage, l],
                                            device_id={'dp': lax.rem(p + i, dpn)}, device_id_type=MESH)

    def spread_copy(l, i):
        return dp_remote(half.at[l, pl.ds(seat(lax.rem(p + i, dpn)) * per, per)], dp_recv.at[l, pl.ds((i - 1) * per, per)], 0, l, i)

    def dp_all(l, stage):
        part_of = (dp_recv.at[l], gathered.at[l, slice((dpn - 1) * per)])[stage]
        return dp_remote(part_of, part_of, stage, l, 1)

    def weight_part(rows):
        part_of = w_recv.at[1, slice(rows)]
        return dp_remote(part_of, part_of, 2, 0, 1)

    def cross_copy(l):
        return remote(cross_send.at[l], cross_recv.at[l], cross_ss.at[l], cross_rs.at[l], 2)

    def gather_copy(l, i, owner):
        return dp_remote(own_sum.at[l], gathered.at[l, pl.ds(seat(owner) * per, per)], 1, l, i)

    def output_copies(action):
        block, more = n_send.at[0], n_send.at[1]
        most = slice(block.shape[0] - share)
        end = pl.ds(block.shape[0] - share, share)
        sems = n_ss.at[2, 0], n_rs.at[2, 0]
        extra = remote(more.at[end], no_recv.at[end], n_ss.at[2, 2], n_rs.at[2, 2], 3)
        first_core = c == 0

        @pl.when(first_core)
        def _():
            getattr(remote(block.at[most], no_recv.at[most], *sems, 2), action)()
            if action == 'wait_recv':
                extra.wait_recv()

        @pl.when(jnp.logical_not(first_core))
        def _():
            getattr(remote(block, no_recv, *sems, 2), action)()
            if action != 'wait_recv':
                getattr(extra, action)()

    def part_piece(q, a):
        return remote(part.at[q, :, a], part_recv.at[q, :, a], p_ss.at[q], p_rs.at[q], 1)

    def part_copy(q):
        return remote(part.at[q], part_recv.at[q], p_ss.at[q], p_rs.at[q], 1)

    wide = D // GROUP
    tiles = nodes // D
    over = range(tiles * D, nodes, wide)

    def node_rows(k):
        return slice(k * cols, (k + 1) * cols) if k < tiles else pl.ds(tiles * cols + (k - tiles) * cols // GROUP, cols // GROUP)

    def pack_nodes(take, out):
        for k in range(tiles):
            out[node_rows(k), :] = take(k * D, D)
        for k, start in enumerate(over):
            val = take(start, wide)
            out[node_rows(tiles + k), :] = beside([val[r] for r in rest])

    def unpack_nodes(src, put):
        for k in range(tiles):
            put(k * D, src[node_rows(k), :])
        for k, start in enumerate(over):
            val = src[node_rows(tiles + k), :]
            put(start, stacked([val[:, rows_of(g)] for g in range(GROUP)]))

    def put_rows(ref, rows):
        def put(start, val):
            ref[rows, start:start + val.shape[1]] = val.astype(ref.dtype)

        return put

    def put_output(ref):
        def put(start, val):
            used = min(val.shape[1], nodes - start)
            ref[ox, :, start:start + used] = val[:, :used].astype(ref.dtype)

        return put

    def take_rows(ref, rows):
        return lambda start, width: ref[rows, start:start + width].astype(F32)

    def load_nodes(raw, sample, out):
        node_pad[:, :nodes] = raw[sample].astype(F32)
        pack_nodes(take_rows(node_pad, every), out)

    def keep_nodes(own):
        own[...] = jnp.zeros_like(own)
        own[:cols, :] = node_pad[...].astype(own.dtype)

    def load_edges(raw, send, own, kind):
        def put(j, lanes_j, val_of):
            for d in OTHERS:
                sample = x if d < 2 else ox
                send[slot(d), j] = val_of(sample, oc if d % 2 else c).astype(F32)
            own[:cols, lanes_j] = val_of(x, c)

        def chunk(j):
            put(j, at(j, EC), lambda s, h: raw[s, :, pl.ds(pl.multiple_of(h * eh + j * EC, D), EC)])
            for d in SEND_ORDER:
                edge_start(kind, j, d)

        loop(nch - 1, chunk)
        first = (nch - 1) * EC
        used = edges - eh - first
        last = pl.ds(first, EC)

        def tail(s, h):
            left = raw[s, :, pl.ds(first, EC)]
            right = beside([raw[s, :, pl.ds(eh + first, used)], jnp.zeros((cols, EC - used), BF)])
            return jnp.where(h == 0, left.astype(F32), right.astype(F32)).astype(BF)

        put(nch - 1, last, tail)
        for d in SEND_ORDER:
            edge_start(kind, nch - 1, d)

    def place_edges(raw, block, d, j):
        s = x if d < 2 else ox
        h = oc if d % 2 else c
        val = block.astype(BF)
        first = (nch - 1) * EC
        used = edges - eh - first

        @pl.when(jnp.logical_or(j < nch - 1, h == 0))
        def _():
            raw[s, :, pl.ds(pl.multiple_of(h * eh + j * EC, D), EC)] = val

        @pl.when(jnp.logical_and(j == nch - 1, h == 1))
        def _():
            raw[s, :, pl.ds(eh + first, used)] = val[:, :used]

    def scoped(e0, e1, ge, msg, v0, v1, v2, agg0, agg1, d_agg, scol, rcol, srow, rrow, iota, lanes, ew1, ew1t, ew2, ew2t, nw1, nw1t, nw2, nw2t, vecs):
        tables = (v0, v1, v2)
        aggs = (agg0, agg1)
        edges_in = (e0, e1)

        barrier = pltpu.get_barrier_semaphore()
        for d in OTHERS:
            pl.semaphore_signal(barrier, device_id={'tp': peer[d]}, device_id_type=MESH)
        for copy in (first_load, node_load, *small_loads, edge_load, gnode_load, gedge_load):
            copy.start()
        node_pad[...] = jnp.zeros_like(node_pad)
        with jax.named_scope('barrier'):
            @pl.when(t != LEADER)
            def _():
                pl.semaphore_wait(barrier, len(OTHERS))

            @pl.when(t == HELPER)
            def _():
                pl.semaphore_signal(ready, device_id={'tp': LEADER}, device_id_type=MESH)

            @pl.when(t == LEADER)
            def _():
                pl.semaphore_wait(ready)

        first_load.wait()
        with jax.named_scope('send_nodes'):
            load_nodes(node_raw, ox, n_send.at[0])
        ncop = node_copies(n_send, n_recv, 0)
        ncop[1].start()
        node_load.wait()
        load_nodes(node_raw, x, n_send.at[1])
        keep_nodes(v0)
        ncop[0].start()
        for copy in small_loads:
            copy.wait()
        q = cols
        w_send[:HEAD, :] = jnp.zeros((HEAD, D), F32)
        for k in THREE:
            w_send[k:k + 1, :] = beside([src[k, l:l + 1, :] for src in (evec_in, nvec_in) for l in range(layers)])
        for l in range(layers):
            w_send[packed(l, 0, 3), :] = ew1_in[pl.ds(l * 3 * q, 3 * q), :].astype(F32)
            w_send[packed(l, 3), :] = ew2_in[pl.ds(l * q, q), :].astype(F32)
            w_send[packed(l, 4, 2), :] = nw1_in[pl.ds(l * 2 * q, 2 * q), :].astype(F32)
            w_send[packed(l, 6), :] = nw2_in[pl.ds(l * q, q), :].astype(F32)
        by_share(lambda rows: w_cross(rows).start())
        w_pair.start()
        edge_load.wait()
        with jax.named_scope('send_edges'):
            load_edges(edge_raw, e_send, e0, EDGE_IN)
        gnode_load.wait()
        load_nodes(gnode_raw, ox, gn_send.at[0])
        load_nodes(gnode_raw, x, gn_send.at[1])
        keep_nodes(d_part)
        gcop = node_copies(gn_send, gn_recv, 1)
        gcop[1].start()
        gcop[0].start()
        gedge_load.wait()
        with jax.named_scope('send_grads'):
            load_edges(gedge_raw, g_send, ge, GRAD_IN)

        with jax.named_scope('dp_barrier'):
            @pl.when(t == LEADER)
            def _():
                for i in dp_others:
                    pl.semaphore_signal(barrier, device_id={'dp': lax.rem(p + i, dpn)}, device_id_type=MESH)
                pl.semaphore_wait(barrier, len(OTHERS) + dpn - 1)
                for d in OTHERS:
                    pl.semaphore_signal(ready, device_id={'tp': peer[d]}, device_id_type=MESH)

            @pl.when(t != LEADER)
            def _():
                pl.semaphore_wait(ready)

        def hand_on(rows):
            w_cross(rows).wait_recv()
            for i in dp_others:
                weight_copy(i, rows).start()

        by_share(hand_on)

        @pl.when(c == 1)
        def _():
            for recv in (e_recv, g_recv):
                recv[:, last, :, D:] = jnp.zeros((len(OTHERS), cols, EC - D), F32)

        iota[...] = lax.broadcasted_iota(jnp.int32, (T, D), 0).astype(I16)
        lanes[...] = lax.broadcasted_iota(jnp.int32, (16, D), 1).astype(I16)

        ids_raw[...] = jnp.full(ids_raw.shape, -1, jnp.int32)
        for which, src in enumerate((send_ids, recv_ids)):
            ids_raw[which:which + 1, :edges] = src[...].reshape(1, edges)

        def ids(b):
            for which, (row_ref, col_ref) in enumerate(((srow, scol), (rrow, rcol))):
                wide = jnp.broadcast_to(ids_raw[which:which + 1, pl.ds(pl.multiple_of(c * eh + b * D, D), D)], (D, D))
                row_ref[at(b, 16), :] = wide[:16].astype(I16)
                col_ref[at(b, D), :] = flip(wide.astype(F32)).astype(jnp.int32).astype(I16)

        with jax.named_scope('ids'):
            loop(eh // D, ids)

        def keys(ref, step):
            return [ref[pl.ds(pl.multiple_of(step * (KS // D) * 16 + 16 * h, 16), 1), :] for h in range(KS // D)]

        bias_cols[...] = flip(stacked([eb1_in[...], nb1_in[...], jnp.zeros((D - 2 * layers, D), F32)]))

        def join_weights(l):
            for d in range(GROUP):
                src = w_recv.at[slot(d)] if d else w_send
                r = rows_of(d)
                for k in THREE:
                    ew1[l, pl.ds(k * D + d * q, q), :] = src[packed(l, k), :].astype(BF)
                ew2t[l, r, :] = src[packed(l, 3), :].astype(BF)
                for k in BOTH:
                    nw1[l, pl.ds(k * D + d * q, q), :] = src[packed(l, 4 + k), :].astype(BF)
                nw2t[l, r, :] = src[packed(l, 6), :].astype(BF)

            def flip_bf(mat):
                return flip(mat.astype(F32)).astype(BF)

            for k in THREE:
                ew1t[l, :, mat(k)] = flip_bf(ew1[l, mat(k), :])
            for k in BOTH:
                nw1t[l, :, mat(k)] = flip_bf(nw1[l, mat(k), :])
            ew2[l] = flip_bf(ew2t[l])
            nw2[l] = flip_bf(nw2t[l])

        def wait_recvs(copies):
            copies[1].wait_recv()
            copies[2].start()
            copies[0].wait_recv()
            copies[2].wait_recv()

        with jax.named_scope('node_wait'):
            wait_recvs(ncop)
        for d in OTHERS:
            unpack_nodes(n_recv.at[slot(d)], put_rows(v0, rows_of(d)))
        with jax.named_scope('weight_wait'):
            pl.when(jnp.logical_not(brings))(weight_part(w_send.shape[0] - HEAD).wait_recv)
            pl.when(brings)(weight_part(w_send.shape[0] - piece).wait_recv)
            w_relay.start()
            w_pair.wait_recv()
            w_relay.wait_recv()
        blocks = [w_send] + [w_recv.at[d] for d in THREE]
        rows_all = beside([stacked([src[:HEAD, rows_of(g)] for g in range(GROUP)]) for src in blocks])
        vecs[...] = flip(stacked([rows_all, jnp.zeros((D - rows_all.shape[0], D), F32)]))
        join_weights(0)

        def vec(l, node):
            first = (node * layers + l) * HEAD
            return [vecs[:, first + k:first + k + 1] for k in THREE]

        def bias(l, node):
            return bias_cols[:, node * layers + l:node * layers + l + 1]

        def hidden_of_nodes(l):
            table, b1 = tables[l], bias(l, 0)

            def body(step):
                xs = gather(table, keys(srow, step), iota).astype(BF)
                xr = gather(table, keys(rrow, step), iota).astype(BF)
                hidden[l, :, at(step, KS)] = dot(ew1t[l, :, mat(1, 2)], stacked([xs, xr])) + b1

            loop(eh // KS, body)

        def edge_forward(l):
            e_in = edges_in[l]

            def body(j):
                for sub in range(EC // T):
                    a = at(j * (EC // T) + sub, T)
                    if l == 0:
                        if sub == 0:
                            chunk_arrived(EDGE_IN, j)
                        for d in OTHERS:
                            e_in[rows_of(d), a] = e_recv[slot(d), j, :, sub * T:(sub + 1) * T].astype(BF)
                    e_val = e_in[:, a]
                    hid = hidden[l, :, a] + dot(ew1t[l, :, mat(0)], e_val)
                    hidden[l, :, a] = hid
                    message, nrm, std = mlp_tail(hid, ew2t[l], vec(l, 0))
                    normed[l, :, a] = nrm
                    inv[l:l + 1, a] = std
                    msg[:, a] = message
                    e_new = (e_val.astype(F32) + message.astype(F32)).astype(BF)
                    if l < top:
                        edges_in[l + 1][:, a] = e_new
                    else:
                        for d in OTHERS:
                            e_send[slot(d), j, :, sub * T:(sub + 1) * T] = e_new[rows_of(d)].astype(F32)
                        if sub == 0:
                            own_parts = []
                        own_parts.append(e_new[:q])
                if l == top:
                    for d in SEND_ORDER:
                        edge_start(EDGE_OUT, j, d)
                    place_edges(edge_raw, beside(own_parts), 0, j)

            loop(nch, body)

        def segment_sum(acc, ids_ref):
            acc[...] = jnp.zeros(acc.shape, F32)

            def body(step):
                scatter(acc, msg[:, at(step, KS)], ids_ref[at(step, KS), :], lanes)

            loop(eh // KS, body)

        def node_forward(l):
            table, agg, out = tables[l], aggs[l], tables[l + 1]

            def body(step):
                a = pl.ds(pl.multiple_of(step * TN, D), TN)
                v_in = table[:, a]
                agg_bf = (part[l, :, a] + swap_halves(part_recv[l, :, a])).astype(BF)
                agg[:, a] = agg_bf
                hid = dot(nw1t[l], stacked([v_in, agg_bf])) + bias(l, 1)
                nhid[l, :, a] = hid
                message, nrm, std = mlp_tail(hid, nw2t[l], vec(l, 1))
                nnrm[l, :, a] = nrm
                ninv[l:l + 1, a] = std
                out[:, a] = (v_in.astype(F32) + message.astype(F32)).astype(BF)

            loop(npad // TN, body)

        for l in range(layers):
            with jax.named_scope(f'gather_{l}'):
                hidden_of_nodes(l)
            if l == top:
                edges_sent(EDGE_IN)
            with jax.named_scope(f'edge_forward_{l}'):
                edge_forward(l)
            with jax.named_scope(f'sum_{l}'):
                segment_sum(part.at[l], rcol)
            part_copy(l).start()
            if l == 0:
                join_weights(1)
                gcop[1].wait_recv()
                gcop[2].start()
            with jax.named_scope(f'part_wait_{l}'):
                part_copy(l).wait_recv()
            with jax.named_scope(f'node_forward_{l}'):
                node_forward(l)
        for copy in ncop[:2]:
            copy.wait_send()
        for which in BOTH:
            pack_nodes(take_rows(tables[layers], rows_of(2 + which)), n_send.at[which])
        output_copies('start')
        node_raw[x] = tables[layers][:q, :nodes]

        for k in range(layers):
            part_copy(k).wait_send()
        s_sum, r_sum = (part.at[k] for k in BOTH)
        grad[...] = jnp.zeros_like(grad)
        sums[...] = jnp.zeros_like(sums)
        with jax.named_scope('grad_node_wait'):
            gcop[0].wait_recv()
            gcop[2].wait_recv()
        for d in OTHERS:
            unpack_nodes(gn_recv.at[slot(d)], put_rows(d_part, rows_of(d)))

        def node_backward(l):
            table, agg = tables[l], aggs[l]

            def body(step):
                a = pl.ds(pl.multiple_of(step * TN, D), TN)
                d_in = d_part[:, a]
                if l < top:
                    d_in = d_in + part[layers + l + 1, :, a] + swap_halves(part_recv[layers + l + 1, :, a])
                    d_in = d_in.astype(BF).astype(F32)
                d_hid, d_w2, parts = mlp_back(d_in, nhid[l, :, a], nnrm[l, :, a], ninv[l:l + 1, a], nw2[l], vec(l, 1))
                add_sums(sums.at[l, 1], [parts])
                grad[l, 4] += d_w2
                grad[l, 2] += dot_nt(table[:, a], d_hid)
                grad[l, 3] += dot_nt(agg[:, a], d_hid)
                d_part[:, a] = d_in + dot(nw1[l, mat(0), :], d_hid)
                d_agg[:, a] = dot(nw1[l, mat(1), :], d_hid).astype(BF)

            loop(npad // TN, body)

        def gather_back():
            def body(step):
                msg[:, at(step, KS)] = gather(d_agg, keys(rrow, step), iota).astype(BF)

            loop(eh // KS, body)

        def edge_backward(l):
            e_in = edges_in[l]

            def body(j):
                all_parts, d_w2s, d_w1s, own_parts = [], [], [], []
                for sub in range(EC // T):
                    a = at(j * (EC // T) + sub, T)
                    if l == top:
                        if sub == 0:
                            chunk_arrived(GRAD_IN, j)
                        for d in OTHERS:
                            ge[rows_of(d), a] = g_recv[slot(d), j, :, sub * T:(sub + 1) * T].astype(BF)
                    d_res = ge[:, a].astype(F32)
                    d_msg = d_res + msg[:, a].astype(F32)
                    d_hid, d_w2, parts = mlp_back(d_msg, hidden[l, :, a], normed[l, :, a], inv[l:l + 1, a], ew2[l], vec(l, 0))
                    all_parts.append(parts)
                    d_w2s.append(d_w2)
                    d_w1s.append(dot_nt(e_in[:, a], d_hid))
                    msg[:, a] = d_hid
                    d_new = (d_res + dot(ew1[l, mat(0), :], d_hid)).astype(BF)
                    if l > 0:
                        ge[:, a] = d_new
                    else:
                        for d in OTHERS:
                            g_send[slot(d), j, :, sub * T:(sub + 1) * T] = d_new[rows_of(d)].astype(F32)
                        own_parts.append(d_new[:q])
                add_sums(sums.at[l, 0], all_parts)
                grad[l, 1] += sum(d_w2s[1:], d_w2s[0])
                grad[l, 0] += sum(d_w1s[1:], d_w1s[0])
                if l == 0:
                    @pl.when(j < hold)
                    def _():
                        for d in SEND_ORDER:
                            edge_start(GRAD_OUT, j, d)
                    place_edges(gedge_raw, beside(own_parts), 0, j)

            loop(nch, body)

        def vector_slab(l):
            def total(node, k):
                return column_sum(flip(sums[l, node, mat(k), :]))

            lat = stacked([total(node, k) for node in BOTH for k in THREE])
            biases = stacked([total(node, 3) for node in BOTH])
            n_lat = lat.shape[0]
            for d in range(GROUP):
                grad[l, VEC_SLAB, d * cols:d * cols + n_lat, :cols] = lat[:, rows_of(d)]
                grad[l, VEC_SLAB, d * cols + n_lat:d * cols + n_lat + 2, :] = biases

        def reduce_start(l, stage):
            for b in BOTH:
                core_copy(l, b, stage).start()

        def chip_sum(l, stage):
            row = lax.broadcasted_iota(jnp.int32, (cols, D), 0)
            edge_row = jnp.logical_or(row < 3, row == 6)
            core_all(l, stage).wait_recv()
            for b in BOTH:
                for k in range(SLABS)[STAGES[stage]]:
                    own = grad[l, k, rows_of(2 * b), :]
                    if k in EDGE_SLABS:
                        own = own + core_recv[l, b, k]
                    elif k == VEC_SLAB:
                        other = core_recv[l, b, k]
                        own = own + jnp.where(edge_row, other, 0.0)
                        own = jnp.where(jnp.logical_and(row == 7, c == 1), other, own)
                    half[l, k, b] = own
            for i in dp_others:
                @pl.when(in_stage(lax.rem(p + i, dpn), stage))
                def _():
                    spread_copy(l, i).start()

        def dp_sum(l, stage):
            @pl.when(in_stage(p, stage))
            def _():
                total = half[l, pl.ds(seat(p) * per, per)]
                dp_all(l, 0).wait_recv()
                for i in dp_others:
                    total = total + dp_recv[l, pl.ds((i - 1) * per, per)]
                own_sum[l] = total[:, 0]
                cross_send[l] = total[:, 1]
                cross_copy(l).start()

        def cross_sum(l):
            cross_copy(l).wait_recv()
            total = own_sum[l] + cross_recv[l]
            own_sum[l] = total
            gathered[l, pl.ds(seat(p) * per, per)] = total
            for i in dp_others:
                gather_copy(l, i, p).start()

        def project(l):
            table = tables[l]

            def body(step):
                a = pl.ds(pl.multiple_of(step * TN, D), TN)
                s_bf, r_bf, v_in = s_sum[:, a].astype(BF), r_sum[:, a].astype(BF), table[:, a]
                part[layers + l, :, a] = dot(ew1[l, mat(1), :], s_bf) + dot(ew1[l, mat(2), :], r_bf)
                if l > 0:
                    part_piece(layers + l, a).start()
                grad[l, 6] += dot_nt(v_in, s_bf)
                grad[l, 7] += dot_nt(v_in, r_bf)

            loop(npad // TN, body)

        for l in reversed(range(layers)):
            first_layer = l == 0
            with jax.named_scope(f'node_backward_{l}'):
                node_backward(l)
            if first_layer:
                with jax.named_scope('chip_sum_1'):
                    chip_sum(1, 0)
                    chip_sum(1, 1)
            with jax.named_scope(f'gather_back_{l}'):
                gather_back()
            if first_layer:
                edges_sent(GRAD_IN)
            with jax.named_scope(f'edge_backward_{l}'):
                edge_backward(l)
            vector_slab(l)
            reduce_start(l, 0)
            if first_layer:
                with jax.named_scope('dp_sum_1'):
                    dp_sum(1, 0)
                    dp_sum(1, 1)
            with jax.named_scope(f'sum_send_{l}'):
                segment_sum(s_sum, scol)
            if first_layer:
                with jax.named_scope('chip_sum_0'):
                    chip_sum(0, 0)
            with jax.named_scope(f'sum_recv_{l}'):
                segment_sum(r_sum, rcol)
            with jax.named_scope(f'project_{l}'):
                project(l)
            reduce_start(l, 1)
            if first_layer:
                part_copy(layers + l).start()
            if first_layer:
                with jax.named_scope('chip_sum_late'):
                    chip_sum(0, 1)
                with jax.named_scope('dp_sum_0'):
                    dp_sum(0, 0)
            with jax.named_scope(f'back_wait_{l}'):
                part_copy(layers + l).wait_recv()

        def final(step):
            a = pl.ds(pl.multiple_of(step * TN, D), TN)
            d_in = (d_part[:, a] + part[layers, :, a] + swap_halves(part_recv[layers, :, a])).astype(BF)
            v2[:, a] = d_in

        loop(npad // TN, final)
        gnode_raw[x] = v2[:q, :nodes]
        with jax.named_scope('dp_sum_late'):
            dp_sum(0, 1)

        gcop[1].wait_send()
        dn_send = gn_send.at[0]
        pack_nodes(take_rows(v2, rows_of(2)), dn_send)
        dn_copy = remote(dn_send, dn_recv, n_ss.at[2, 1], n_rs.at[2, 1], 2)
        dn_copy.start()

        def send_rest(j):
            for d in SEND_ORDER:
                edge_start(GRAD_OUT, j, d)

        loop(nch, send_rest, hold)

        with jax.named_scope('node_out_wait'):
            output_copies('wait_recv')
        unpack_nodes(no_recv, put_output(node_raw))

        def place_e(j):
            for d in OTHERS:
                place_edges(edge_raw, eo_recv[slot(d), j], d, j)

        with jax.named_scope('place_edge_out'):
            for group in THREE:
                group_arrived(EDGE_OUT, group)
            loop(nch, place_e)

        def place_g(j):
            for d in OTHERS:
                place_edges(gedge_raw, de_recv[slot(d), j], d, j)

        with jax.named_scope('place_first'):
            group_arrived(GRAD_OUT, 0)
            loop(hold, place_g)
        for l in range(layers):
            with jax.named_scope(f'cross_sum_{l}'):
                cross_sum(l)
        with jax.named_scope('d_node_wait'):
            dn_copy.wait_recv()
        unpack_nodes(dn_recv, put_output(gnode_raw))
        with jax.named_scope('place_rest'):
            group_arrived(GRAD_OUT, 1)
            loop(last, place_g, hold)
        for l in range(layers):
            dp_all(l, 1).wait_recv()
            ew1_buf[l, 0] = gathered[l, 0]
            ew1_buf[l, 1:] = gathered[l, EARLY:]
            ew2_buf[l] = gathered[l, 1]
            nw1_buf[l] = gathered[l, 2:4]
            nw2_buf[l] = gathered[l, 4]
            small = gathered[l, VEC_SLAB]
            for k in THREE:
                evec_buf[k, l:l + 1, :] = small[k:k + 1, :cols]
                nvec_buf[k, l:l + 1, :] = small[3 + k:4 + k, :cols]
            eb1_buf[l:l + 1, :] = small[6:7]
            nb1_buf[l:l + 1, :] = small[7:8]
        for l in range(layers):
            for stage in BOTH:
                core_all(l, stage).wait_send()
            cross_copy(l).wait_send()
            dp_all(l, 0).wait_send()
            dp_all(l, 1).wait_send()
        for copy in (ncop[2], gcop[0], gcop[2], w_pair, w_relay):
            copy.wait_send()

        by_share(lambda rows: w_cross(rows).wait_send())
        pl.when(brings)(weight_part((dpn - 1) * piece).wait_send)
        pl.when(jnp.logical_not(brings))(weight_part((dpn - 1) * HEAD).wait_send)

        output_copies('wait_send')
        dn_copy.wait_send()
        for k in range(layers, 2 * layers):
            part_copy(k).wait_send()
        edges_sent(EDGE_OUT)
        with jax.named_scope('place_last'):
            group_arrived(GRAD_OUT, 2)
            loop(nch, place_g, last)
        edges_sent(GRAD_OUT)

    bf = lambda *s: pltpu.VMEM(s, BF)
    pl.run_scoped(
        scoped, bf(D, eh), bf(D, eh), bf(D, eh), bf(D, eh), bf(D, npad), bf(D, npad), bf(D, npad), bf(D, npad), bf(D, npad), bf(D, npad),
        pltpu.VMEM((eh, D), I16), pltpu.VMEM((eh, D), I16), pltpu.VMEM((eh // D * 16, D), I16), pltpu.VMEM((eh // D * 16, D), I16),
        pltpu.VMEM((T, D), I16), pltpu.VMEM((16, D), I16),
        bf(layers, 3 * D, D), bf(layers, D, 3 * D), bf(layers, D, D), bf(layers, D, D),
        bf(layers, 2 * D, D), bf(layers, D, 2 * D), bf(layers, D, D), bf(layers, D, D), pltpu.VMEM((D, D), F32))


def finish_moves(src, dst):
    if len(src.shape) != 3 or src.dtype != BF:
        return [(src, dst)]
    return [(src.at[s, pl.ds(r, 8)], dst.at[s, pl.ds(r, 8)]) for s in range(src.shape[0]) for r in range(0, src.shape[1], 8)]


def finish_kernel(*refs):
    count = len(refs) // 2
    moves = sum((finish_moves(refs[k], refs[count + k]) for k in range(count)), [])
    puts = [pltpu.make_async_copy(src, dst, refs[-1]) for src, dst in moves]
    for put in puts:
        put.start()
    for put in puts:
        put.wait()


def keep_in_vmem(val):
    return pltpu.with_memory_space_constraint(val, pltpu.VMEM)


def finish(arrays):
    return pl.pallas_call(
        finish_kernel,
        name='finish',
        out_shape=[jax.ShapeDtypeStruct(a.shape, a.dtype) for a in arrays],
        in_specs=[VM] * len(arrays),
        out_specs=[HB] * len(arrays),
        scratch_shapes=[pltpu.SemaphoreType.DMA],
        compiler_params=pltpu.CompilerParams(vmem_limit_bytes=1 << 20),
    )(*[keep_in_vmem(a) for a in arrays])


def solution(mesh):
    lat_spec = P('dp', None, 'tp')
    first_spec = P(None, None, 'tp', None)
    col_spec = P(None, None, 'tp')
    param_specs = (first_spec, P(), col_spec, col_spec, first_spec, P(), col_spec, col_spec)
    in_specs = (lat_spec, lat_spec, P(), P(), lat_spec, lat_spec) + param_specs
    out_specs = (lat_spec, lat_spec, lat_spec, lat_spec) + param_specs
    shape = jax.ShapeDtypeStruct

    def local_step(node_lat, edge_lat, senders, receivers, grad_node, grad_edge, edge_w1, edge_b1, edge_w2, edge_vec, node_w1, node_b1, node_w2, node_vec):
        layers = edge_w1.shape[0]
        cols = node_lat.shape[2]
        nodes, edges = node_lat.shape[1], edge_lat.shape[1]
        npad = -(-nodes // TN) * TN
        eh = -(-edges // (2 * EC)) * EC
        nch = eh // EC
        dpn = mesh.shape['dp']
        per = SLABS // dpn
        dims = (layers, cols, nodes, edges, npad, eh, dpn)
        flat = lambda arr: jnp.swapaxes(arr, 1, 2)
        lead = lambda arr: jnp.transpose(arr, (1, 0, 2))
        args = (flat(node_lat), flat(edge_lat), flat(grad_node), flat(grad_edge), senders, receivers,
                edge_w1.reshape(-1, D), flat(edge_w2).reshape(-1, D), node_w1.reshape(-1, D), flat(node_w2).reshape(-1, D),
                lead(edge_vec), lead(node_vec), edge_b1, node_b1)
        vm, sem = pltpu.VMEM, pltpu.SemaphoreType.DMA
        packed = nodes // D * cols + -(-(nodes % D) * GROUP // D) * cols // GROUP
        wrows = HEAD + layers * LROWS
        lat_n, lat_e = (2, cols, nodes), (2, cols, edges)
        outs = [RESULT(lat_n, BF), RESULT(lat_e, BF), RESULT(lat_n, BF), RESULT(lat_e, BF),
                RESULT((layers, 3, cols, D), F32), RESULT((layers, D), F32), RESULT((layers, cols, D), F32), RESULT((3, layers, cols), F32),
                RESULT((layers, 2, cols, D), F32), RESULT((layers, D), F32), RESULT((layers, cols, D), F32), RESULT((3, layers, cols), F32)]
        scratch = [
            *[vm(a.shape, a.dtype) for a in args[4:]], vm((wrows, D), F32), vm((3, wrows, D), F32),
            *[vm((many, packed, D), F32) for many in (2, 3, 2, 3)], *[vm((packed, D), F32)] * 2, vm((cols, npad), F32),
            *[vm((kinds, len(OTHERS), cols + cols // GROUP, D), F32) for kinds in (2, GROUP)], *[vm((len(OTHERS), nch, cols, EC), F32)] * 6,
            vm((2 * layers, D, npad), F32), vm((2 * layers, D, npad), F32),
            vm((layers, D, eh), F32), vm((layers, D, eh), F32), vm((layers, eh), F32),
            vm((layers, D, npad), F32), vm((layers, D, npad), F32), vm((layers, npad), F32),
            vm((D, npad), F32), vm((2, 2 * eh), jnp.int32), vm((D, D), F32), vm((layers, 2, 4 * D, D), F32),
            vm((layers, SLABS, D, D), F32), vm((layers, 2, SLABS, cols, D), F32), vm((layers, SLABS, 2, cols, D), F32),
            vm((layers, (dpn - 1) * per, 2, cols, D), F32), vm((layers, per, cols, D), F32), vm((layers, per, cols, D), F32),
            vm((layers, per, cols, D), F32), vm((layers, SLABS, cols, D), F32),]
        own_sems = [
            sem((layers, 2)), sem((3, layers)), sem((layers,)), sem((3,)), sem((3, 3)), sem((2, nch)), sem((2, 5)), sem((2 * layers,)),
            pltpu.SemaphoreType.REGULAR,
            sem((len(args) + 1,)), sem((3,)), sem((3, 3)), sem((4, 4)), sem((2 * layers,)), sem((layers, 2)), sem((3, layers)), sem((layers,))]
        res = pl.pallas_call(
            lambda *refs: pl.run_scoped(lambda *own: step_kernel(dims, *refs, *own), *own_sems),
            name='graph_step',
            out_shape=outs,
            in_specs=[HB] * len(args),
            out_specs=[VM] * len(outs),
            scratch_shapes=scratch,
            compiler_params=pltpu.CompilerParams(collective_id=0, has_side_effects=True, vmem_limit_bytes=VMEM_LIMIT),
        )(*args)

        res = finish(res)
        return (flat(res[0]), flat(res[1]), flat(res[2]), flat(res[3]),
                res[4], res[5], flat(res[6]), lead(res[7]), res[8], res[9], flat(res[10]), lead(res[11]))

    return jax.shard_map(local_step, mesh=mesh, in_specs=in_specs, out_specs=out_specs, check_vma=False)
```

```python
import jax
import jax.numpy as jnp
from jax import lax
from jax.experimental import pallas as pl
from jax.experimental.pallas import tpu as pltpu
from jax.sharding import PartitionSpec as P

LN_EPS = 1e-5
D = 128
T = 256
TN = 384
EC = 512
KS = 2816
BF = jnp.bfloat16
F32 = jnp.float32
I16 = jnp.int16
MESH = pl.DeviceIdType.MESH
VM = pl.BlockSpec(memory_space=pltpu.VMEM)
HB = pl.BlockSpec(memory_space=pl.ANY)
RESULT = pltpu.VMEM
GROUP = 4
BOTH = (0, 1)
THREE = (0, 1, 2)
OTHERS = (1, 2, 3)
EDGE_IN, GRAD_IN, EDGE_OUT, GRAD_OUT = range(4)
SEND_ORDER = (2, 3, 1)
LROWS = 7 * (D // 4)
HEAD = 8
LEADER = GROUP - 1
HELPER = LEADER - 1
VMEM_LIMIT = 63_000_000
SLABS = 8
EARLY = 6
VEC_SLAB = 5
EDGE_SLABS = (0, 1, 6, 7)
STAGES = (slice(0, EARLY), slice(EARLY, SLABS))


def dot(a, b):
    return jnp.dot(a, b, preferred_element_type=F32)


def dot_nt(a, b):
    return lax.dot_general(a, b, (((1,), (1,)), ((), ())), preferred_element_type=F32)


def mat(k, n=1):
    return slice(k * D, (k + n) * D)


def rows_of(d):
    q = D // 4
    return slice(d * q, (d + 1) * q)


def at(step, width):
    return pl.ds(pl.multiple_of(step * width, width), width)


def loop(stop, body, start=0):
    def step(j, carry):
        body(j)
        return carry

    lax.fori_loop(start, stop, step, 0)


def column_sum(val):
    return jnp.sum(val, axis=0, keepdims=True)


def flip(val):
    return jnp.swapaxes(val, 0, 1)


def stacked(parts):
    return jnp.concatenate(parts, axis=0)


def beside(parts):
    return jnp.concatenate(parts, axis=1)


def slot(d):
    return d - 1


def sigmoid(hidden):
    return 1.0 / (1.0 + jnp.exp(-hidden))


def fold(val):
    total = val[:, mat(0)]
    for start in range(D, val.shape[1], D):
        total = total + val[:, start:start + D]
    return total


def swap_halves(val):
    return stacked([val[rows_of(d)] for d in (1, 0, 3, 2)])


def gather(table, keys, iota):
    acc = None
    nodes = table.shape[1]
    one, zero = jnp.ones((), BF), jnp.zeros((), BF)
    for base in range(0, nodes, T):
        width = min(T, nodes - base)
        ids = iota[0:width, :]
        hot = beside([jnp.where(ids == (key - jnp.asarray(base, I16)), one, zero) for key in keys])
        part = dot(table[:, base:base + width], hot)
        acc = part if acc is None else acc + part
    return acc


def scatter(acc_ref, val, cols, lanes):
    nodes = acc_ref.shape[1]
    one, zero = jnp.ones((), BF), jnp.zeros((), BF)
    row = lanes[0:1, :]
    for base in range(0, nodes, T):
        width = min(T, nodes - base)
        hot = beside([jnp.where((row + jnp.asarray(base + s, I16)) == cols, one, zero) for s in range(0, width, D)])
        acc_ref[:, base:base + width] += dot(val, hot)


def mlp_tail(hidden, w2t, vec):
    act = (hidden * sigmoid(hidden)).astype(BF)
    out = dot(w2t, act) + vec[0]
    mean = column_sum(out) / D
    centered = out - mean
    var = column_sum(centered * centered) / D
    inv = lax.rsqrt(var + LN_EPS)
    normed = centered * inv
    message = (normed * vec[1] + vec[2]).astype(BF)
    return message, normed, inv


def mlp_back(d_msg, hidden, normed, inv, w2, vec):
    d_normed = d_msg * vec[1]
    mean0 = column_sum(d_normed) / D
    mean1 = column_sum(d_normed * normed) / D
    d_out = inv * (d_normed - mean0 - normed * mean1)
    d_out_bf = d_out.astype(BF)
    sig = sigmoid(hidden)
    act = (hidden * sig).astype(BF)
    d_w2 = dot_nt(d_out_bf, act)
    d_hidden = dot(w2, d_out_bf) * (sig * (1.0 + hidden * (1.0 - sig)))
    sums = (fold(d_out), fold(d_msg * normed), fold(d_msg), fold(d_hidden))
    return d_hidden.astype(BF), d_w2, sums


def add_sums(ref, parts):
    for q in range(4):
        total = parts[0][q]
        for other in parts[1:]:
            total = total + other[q]
        ref[mat(q), :] += total


def step_kernel(dims, *refs):
    layers, cols, nodes, edges, npad, eh, dpn = dims
    nch = eh // EC
    top = layers - 1
    n_in = 14
    hbm_in = refs[:n_in]
    n_out = 12
    (node_raw, edge_raw, gnode_raw, gedge_raw, ew1_buf, eb1_buf, ew2_buf, evec_buf, nw1_buf, nb1_buf, nw2_buf, nvec_buf) = refs[n_in:n_in + n_out]
    (send_ids, recv_ids, ew1_in, ew2_in, nw1_in, nw2_in, evec_in, nvec_in, eb1_in, nb1_in, w_send, w_recv, n_send, n_recv, gn_send, gn_recv, no_recv, dn_recv,
     node_pad, t_send, t_recv, e_send, g_send, e_recv, g_recv, eo_recv, de_recv, part, part_recv, hidden, normed, inv, nhid, nnrm, ninv, d_part,
     ids_raw, bias_cols, sums, grad, core_recv, half, dp_recv, cross_send, cross_recv, own_sum, gathered,
     core_rs, dp_rs, cross_rs, w_rs, n_rs, e_rs, o_rs, p_rs, ready, load_sem, w_ss, n_ss, e_ss, p_ss, core_ss, dp_ss, cross_ss) = refs[n_in + n_out:]

    t = lax.axis_index('tp')
    p = lax.axis_index('dp')
    per = SLABS // dpn
    dp_others = range(1, dpn)
    x, c = t // 2, lax.rem(t, 2)
    ox, oc = 1 - x, 1 - c
    mate, across = t + oc - c, t + 2 * (ox - x)
    peer = [t, mate, across, mate + across - t]

    def remote(src, dst, ssem, rsem, d):
        return pltpu.make_async_remote_copy(src_ref=src, dst_ref=dst, send_sem=ssem, recv_sem=rsem,
                                            device_id={'tp': peer[d]}, device_id_type=MESH)

    small_in = (send_ids, recv_ids, ew1_in, ew2_in, nw1_in, nw2_in, evec_in, nvec_in, eb1_in, nb1_in)
    loads = [pltpu.make_async_copy(src, dst, load_sem.at[q]) for q, (src, dst) in enumerate(
        zip((hbm_in[0].at[x],) + hbm_in[1:], (node_raw.at[x], edge_raw, gnode_raw, gedge_raw) + small_in))]
    node_load, edge_load, gnode_load, gedge_load, *small_loads = loads
    first_load = pltpu.make_async_copy(hbm_in[0].at[ox], node_raw.at[ox], load_sem.at[n_in])

    def node_copies(send, recv, kind):
        return (remote(send.at[1], recv.at[0], n_ss.at[kind, 0], n_rs.at[kind, 0], 1),
                remote(send.at[0], recv.at[1], n_ss.at[kind, 1], n_rs.at[kind, 1], 2),
                remote(recv.at[1], recv.at[2], n_ss.at[kind, 2], n_rs.at[kind, 2], 1))

    piece = (w_send.shape[0] - HEAD) // (dpn - 1)
    brings = p > 0

    def packed(l, k, count=1):
        return pl.ds(HEAD + l * LROWS + k * cols, count * cols)

    def by_share(action):
        @pl.when(brings)
        def _():
            action(pl.ds(pl.multiple_of(HEAD + (p - 1) * piece, HEAD), piece))

        @pl.when(jnp.logical_not(brings))
        def _():
            action(slice(HEAD))

    w_pair = remote(w_send, w_recv.at[0], w_ss.at[0], w_rs.at[0], 1)
    def w_cross(rows):
        return remote(w_send.at[rows], w_recv.at[1, rows], w_ss.at[1], w_rs.at[1], 2)

    w_relay = remote(w_recv.at[1], w_recv.at[2], w_ss.at[2], w_rs.at[2], 1)

    def weight_copy(i, rows):
        rows = w_recv.at[1, rows]
        return dp_remote(rows, rows, 2, 0, i)

    last = nch - 1
    hold = nch - 3
    share = 2 * (eh - last * EC - D - D // GROUP) * cols // D
    share = min(share, no_recv.shape[0] // 16 * 8)
    buffers = ((e_send, e_recv), (g_send, g_recv), (e_send, eo_recv), (g_send, de_recv))

    def outward(kind):
        return kind in (EDGE_OUT, GRAD_OUT)

    every = slice(None)
    ragged = pl.ds(D, D // GROUP)
    rest = [slice(g * cols // GROUP, (g + 1) * cols // GROUP) for g in range(GROUP)]

    def edge_part(kind, which, j, tail, send_sem, recv_sem, d):
        src, dst = buffers[kind]
        if tail:
            src, dst = t_send.at[kind % 2, which], t_recv.at[kind, which]
        else:
            src, dst = src.at[which, j], dst.at[which, j]
        recv_sems = o_rs.at[kind - EDGE_OUT, recv_sem] if outward(kind) else e_rs.at[kind, recv_sem]
        return remote(src, dst, e_ss.at[kind, send_sem], recv_sems, d)

    def by_half(half_id, j, action):
        narrow = jnp.logical_and(j == last, half_id == 1)

        @pl.when(jnp.logical_not(narrow))
        def _():
            action(False)

        @pl.when(narrow)
        def _():
            action(True)

    def pack_tail(kind, d):
        src, out = buffers[kind][0].at[slot(d), last], t_send.at[kind % 2, slot(d)]
        out[:cols, :] = src[:, :D]
        over = src[:, ragged]
        out[cols:, :] = beside([over[r] for r in rest])

    def unpack_tail(kind, d):
        src, out = t_recv.at[kind, slot(d)], buffers[kind][1].at[slot(d), last]
        out[:, :D] = src[:cols, :]
        over = src[cols:, :]
        out[:, ragged] = stacked([over[:, rows_of(g)] for g in range(GROUP)])

    def edge_start(kind, j, d):
        other = oc if d % 2 else c
        if outward(kind):
            at_last = j == last
            send_sem = jnp.asarray(at_last, jnp.int32)
            recv_sem = jnp.where(at_last, 2 + slot(d), jnp.asarray(j >= hold, jnp.int32))
        else:
            send_sem, recv_sem = jnp.where(j == last, d, 0), j

        def start(tail):
            if tail:
                pack_tail(kind, d)
            edge_part(kind, slot(d), j, tail, send_sem, recv_sem, d).start()

        by_half(c if outward(kind) else other, j, start)

    def edges_sent(kind):
        edge_part(kind, every, slice(0, last), False, 0, 0, 1).wait_send()
        if outward(kind):
            by_half(c, last, lambda tail: edge_part(kind, every, last, tail, 1, 0, 1).wait_send())
        else:
            for d in OTHERS:
                by_half(oc if d % 2 else c, last, lambda tail: edge_part(kind, slot(d), last, tail, d, 0, d).wait_send())

    def chunk_arrived(kind, j):
        def arrived(tail):
            edge_part(kind, every, j, tail, 0, j, 1).wait_recv()
            if tail:
                for d in OTHERS:
                    unpack_tail(kind, d)

        by_half(c, j, arrived)

    def group_arrived(kind, group):
        if group < 2:
            edge_part(kind, every, (slice(0, hold), slice(hold, last))[group], False, 0, group, 1).wait_recv()
        else:
            for d in OTHERS:
                last_arrived(kind, d)

    def last_arrived(kind, d):
        def arrived(tail):
            edge_part(kind, slot(d), last, tail, 0, 2 + slot(d), d).wait_recv()
            if tail:
                unpack_tail(kind, d)

        by_half(oc if d % 2 else c, last, arrived)

    def core_copy(l, b, stage):
        return remote(grad.at[l, STAGES[stage], pl.ds((2 * b + 1) * cols, cols), :], core_recv.at[l, b, STAGES[stage]],
                      core_ss.at[l, stage], core_rs.at[l, stage], 1)

    def core_all(l, stage):
        part_of = core_recv.at[l, :, STAGES[stage]]
        return remote(part_of, part_of, core_ss.at[l, stage], core_rs.at[l, stage], 1)

    def seat(device):
        return lax.rem(device + dpn // 2, dpn)

    def in_stage(device, stage):
        early = (seat(device) + 1) * per <= EARLY
        return jnp.logical_not(early) if stage else early

    def dp_remote(src, dst, stage, l, i):
        return pltpu.make_async_remote_copy(src_ref=src, dst_ref=dst, send_sem=dp_ss.at[stage, l], recv_sem=dp_rs.at[stage, l],
                                            device_id={'dp': lax.rem(p + i, dpn)}, device_id_type=MESH)

    def spread_copy(l, i):
        return dp_remote(half.at[l, pl.ds(seat(lax.rem(p + i, dpn)) * per, per)], dp_recv.at[l, pl.ds((i - 1) * per, per)], 0, l, i)

    def dp_all(l, stage):
        part_of = (dp_recv.at[l], gathered.at[l, slice((dpn - 1) * per)])[stage]
        return dp_remote(part_of, part_of, stage, l, 1)

    def weight_part(rows):
        part_of = w_recv.at[1, slice(rows)]
        return dp_remote(part_of, part_of, 2, 0, 1)

    def cross_copy(l):
        return remote(cross_send.at[l], cross_recv.at[l], cross_ss.at[l], cross_rs.at[l], 2)

    def gather_copy(l, i, owner):
        return dp_remote(own_sum.at[l], gathered.at[l, pl.ds(seat(owner) * per, per)], 1, l, i)

    def output_copies(action):
        block, more = n_send.at[0], n_send.at[1]
        most = slice(block.shape[0] - share)
        end = pl.ds(block.shape[0] - share, share)
        sems = n_ss.at[2, 0], n_rs.at[2, 0]
        extra = remote(more.at[end], no_recv.at[end], n_ss.at[2, 2], n_rs.at[2, 2], 3)
        first_core = c == 0

        @pl.when(first_core)
        def _():
            getattr(remote(block.at[most], no_recv.at[most], *sems, 2), action)()
            if action == 'wait_recv':
                extra.wait_recv()

        @pl.when(jnp.logical_not(first_core))
        def _():
            getattr(remote(block, no_recv, *sems, 2), action)()
            if action != 'wait_recv':
                getattr(extra, action)()

    def part_piece(q, a):
        return remote(part.at[q, :, a], part_recv.at[q, :, a], p_ss.at[q], p_rs.at[q], 1)

    def part_copy(q):
        return remote(part.at[q], part_recv.at[q], p_ss.at[q], p_rs.at[q], 1)

    wide = D // GROUP
    tiles = nodes // D
    over = range(tiles * D, nodes, wide)

    def node_rows(k):
        return slice(k * cols, (k + 1) * cols) if k < tiles else pl.ds(tiles * cols + (k - tiles) * cols // GROUP, cols // GROUP)

    def pack_tiles(take, out, which):
        for k in which:
            out[node_rows(k), :] = take(k * D, D)

    def pack_nodes(take, out, first=0):
        pack_tiles(take, out, range(first, tiles))
        for k, start in enumerate(over):
            val = take(start, wide)
            out[node_rows(tiles + k), :] = beside([val[r] for r in rest])

    def unpack_nodes(src, put):
        for k in range(tiles):
            put(k * D, src[node_rows(k), :])
        for k, start in enumerate(over):
            val = src[node_rows(tiles + k), :]
            put(start, stacked([val[:, rows_of(g)] for g in range(GROUP)]))

    def put_rows(ref, rows):
        def put(start, val):
            ref[rows, start:start + val.shape[1]] = val.astype(ref.dtype)

        return put

    def put_output(ref):
        def put(start, val):
            used = min(val.shape[1], nodes - start)
            ref[ox, :, start:start + used] = val[:, :used].astype(ref.dtype)

        return put

    def take_raw(raw, sample):
        def take(start, width):
            used = min(width, nodes - start)
            val = raw[sample, :, start:start + used].astype(F32)
            return val if used == width else beside([val, jnp.zeros((cols, width - used), F32)])

        return take

    def take_rows(ref, rows):
        return lambda start, width: ref[rows, start:start + width].astype(F32)

    def load_nodes(raw, sample, out):
        node_pad[:, :nodes] = raw[sample].astype(F32)
        pack_nodes(take_rows(node_pad, every), out)

    def keep_nodes(own):
        own[...] = jnp.zeros_like(own)
        own[:cols, :] = node_pad[...].astype(own.dtype)

    def load_edges(raw, send, own, kind):
        def put(j, lanes_j, val_of):
            for d in OTHERS:
                sample = x if d < 2 else ox
                send[slot(d), j] = val_of(sample, oc if d % 2 else c).astype(F32)
            own[:cols, lanes_j] = val_of(x, c)

        def chunk(j):
            put(j, at(j, EC), lambda s, h: raw[s, :, pl.ds(pl.multiple_of(h * eh + j * EC, D), EC)])
            for d in SEND_ORDER:
                edge_start(kind, j, d)

        loop(nch - 1, chunk)
        first = (nch - 1) * EC
        used = edges - eh - first
        last = pl.ds(first, EC)

        def tail(s, h):
            left = raw[s, :, pl.ds(first, EC)]
            right = beside([raw[s, :, pl.ds(eh + first, used)], jnp.zeros((cols, EC - used), BF)])
            return jnp.where(h == 0, left.astype(F32), right.astype(F32)).astype(BF)

        put(nch - 1, last, tail)
        for d in SEND_ORDER:
            edge_start(kind, nch - 1, d)

    def place_edges(raw, block, d, j):
        s = x if d < 2 else ox
        h = oc if d % 2 else c
        val = block.astype(BF)
        first = (nch - 1) * EC
        used = edges - eh - first

        @pl.when(jnp.logical_or(j < nch - 1, h == 0))
        def _():
            raw[s, :, pl.ds(pl.multiple_of(h * eh + j * EC, D), EC)] = val

        @pl.when(jnp.logical_and(j == nch - 1, h == 1))
        def _():
            raw[s, :, pl.ds(eh + first, used)] = val[:, :used]

    def scoped(e0, e1, ge, msg, v0, v1, v2, agg0, agg1, d_agg, scol, rcol, srow, rrow, iota, lanes, ew1, ew1t, ew2, ew2t, nw1, nw1t, nw2, nw2t, vecs):
        tables = (v0, v1, v2)
        aggs = (agg0, agg1)
        edges_in = (e0, e1)

        barrier = pltpu.get_barrier_semaphore()
        for d in OTHERS:
            pl.semaphore_signal(barrier, device_id={'tp': peer[d]}, device_id_type=MESH)
        for copy in (first_load, node_load, *small_loads, edge_load, gnode_load, gedge_load):
            copy.start()
        node_pad[...] = jnp.zeros_like(node_pad)
        with jax.named_scope('barrier'):
            @pl.when(t != LEADER)
            def _():
                pl.semaphore_wait(barrier, len(OTHERS))

            @pl.when(t == HELPER)
            def _():
                pl.semaphore_signal(ready, device_id={'tp': LEADER}, device_id_type=MESH)

            @pl.when(t == LEADER)
            def _():
                pl.semaphore_wait(ready)

        first_load.wait()
        ncop = node_copies(n_send, n_recv, 0)
        early = tiles // 2
        take, out = take_raw(node_raw, ox), n_send.at[0]
        pack_tiles(take, out, range(early))

        def send_part(rows):
            remote(out.at[rows], n_recv.at[1, rows], n_ss.at[0, 1], n_rs.at[0, 1], 2).start()

        send_part(slice(early * cols))
        pack_nodes(take, out, early)
        send_part(slice(early * cols, out.shape[0]))
        node_load.wait()
        load_nodes(node_raw, x, n_send.at[1])
        keep_nodes(v0)
        ncop[0].start()
        for copy in small_loads:
            copy.wait()
        q = cols
        w_send[:HEAD, :] = jnp.zeros((HEAD, D), F32)
        for k in THREE:
            w_send[k:k + 1, :] = beside([src[k, l:l + 1, :] for src in (evec_in, nvec_in) for l in range(layers)])
        for l in range(layers):
            w_send[packed(l, 0, 3), :] = ew1_in[pl.ds(l * 3 * q, 3 * q), :].astype(F32)
            w_send[packed(l, 3), :] = ew2_in[pl.ds(l * q, q), :].astype(F32)
            w_send[packed(l, 4, 2), :] = nw1_in[pl.ds(l * 2 * q, 2 * q), :].astype(F32)
            w_send[packed(l, 6), :] = nw2_in[pl.ds(l * q, q), :].astype(F32)
        by_share(lambda rows: w_cross(rows).start())
        w_pair.start()
        edge_load.wait()
        with jax.named_scope('send_edges'):
            load_edges(edge_raw, e_send, e0, EDGE_IN)
        gnode_load.wait()
        load_nodes(gnode_raw, ox, gn_send.at[0])
        load_nodes(gnode_raw, x, gn_send.at[1])
        keep_nodes(d_part)
        gcop = node_copies(gn_send, gn_recv, 1)
        gcop[1].start()
        gcop[0].start()
        gedge_load.wait()
        with jax.named_scope('send_grads'):
            load_edges(gedge_raw, g_send, ge, GRAD_IN)

        with jax.named_scope('dp_barrier'):
            @pl.when(t == LEADER)
            def _():
                for i in dp_others:
                    pl.semaphore_signal(barrier, device_id={'dp': lax.rem(p + i, dpn)}, device_id_type=MESH)
                pl.semaphore_wait(barrier, len(OTHERS) + dpn - 1)
                for d in OTHERS:
                    pl.semaphore_signal(ready, device_id={'tp': peer[d]}, device_id_type=MESH)

            @pl.when(t != LEADER)
            def _():
                pl.semaphore_wait(ready)

        def hand_on(rows):
            w_cross(rows).wait_recv()
            for i in dp_others:
                weight_copy(i, rows).start()

        by_share(hand_on)

        @pl.when(c == 1)
        def _():
            for recv in (e_recv, g_recv):
                recv[:, last, :, D:] = jnp.zeros((len(OTHERS), cols, EC - D), F32)

        iota[...] = lax.broadcasted_iota(jnp.int32, (T, D), 0).astype(I16)
        lanes[...] = lax.broadcasted_iota(jnp.int32, (16, D), 1).astype(I16)

        ids_raw[...] = jnp.full(ids_raw.shape, -1, jnp.int32)
        for which, src in enumerate((send_ids, recv_ids)):
            ids_raw[which:which + 1, :edges] = src[...].reshape(1, edges)

        def ids(b):
            for which, (row_ref, col_ref) in enumerate(((srow, scol), (rrow, rcol))):
                wide = jnp.broadcast_to(ids_raw[which:which + 1, pl.ds(pl.multiple_of(c * eh + b * D, D), D)], (D, D))
                row_ref[at(b, 16), :] = wide[:16].astype(I16)
                col_ref[at(b, D), :] = flip(wide.astype(F32)).astype(jnp.int32).astype(I16)

        with jax.named_scope('ids'):
            loop(eh // D, ids)

        def keys(ref, step):
            return [ref[pl.ds(pl.multiple_of(step * (KS // D) * 16 + 16 * h, 16), 1), :] for h in range(KS // D)]

        bias_cols[...] = flip(stacked([eb1_in[...], nb1_in[...], jnp.zeros((D - 2 * layers, D), F32)]))

        def join_weights(l):
            for d in range(GROUP):
                src = w_recv.at[slot(d)] if d else w_send
                r = rows_of(d)
                for k in THREE:
                    ew1[l, pl.ds(k * D + d * q, q), :] = src[packed(l, k), :].astype(BF)
                ew2t[l, r, :] = src[packed(l, 3), :].astype(BF)
                for k in BOTH:
                    nw1[l, pl.ds(k * D + d * q, q), :] = src[packed(l, 4 + k), :].astype(BF)
                nw2t[l, r, :] = src[packed(l, 6), :].astype(BF)

            def flip_bf(mat):
                return flip(mat.astype(F32)).astype(BF)

            for k in THREE:
                ew1t[l, :, mat(k)] = flip_bf(ew1[l, mat(k), :])
            for k in BOTH:
                nw1t[l, :, mat(k)] = flip_bf(nw1[l, mat(k), :])
            ew2[l] = flip_bf(ew2t[l])
            nw2[l] = flip_bf(nw2t[l])

        def wait_recvs(copies):
            copies[1].wait_recv()
            copies[2].start()
            copies[0].wait_recv()
            copies[2].wait_recv()

        with jax.named_scope('node_wait'):
            wait_recvs(ncop)
        for d in OTHERS:
            unpack_nodes(n_recv.at[slot(d)], put_rows(v0, rows_of(d)))
        with jax.named_scope('weight_wait'):
            pl.when(jnp.logical_not(brings))(weight_part(w_send.shape[0] - HEAD).wait_recv)
            pl.when(brings)(weight_part(w_send.shape[0] - piece).wait_recv)
            w_relay.start()
            w_pair.wait_recv()
            w_relay.wait_recv()
        blocks = [w_send] + [w_recv.at[d] for d in THREE]
        rows_all = beside([stacked([src[:HEAD, rows_of(g)] for g in range(GROUP)]) for src in blocks])
        vecs[...] = flip(stacked([rows_all, jnp.zeros((D - rows_all.shape[0], D), F32)]))
        join_weights(0)

        def vec(l, node):
            first = (node * layers + l) * HEAD
            return [vecs[:, first + k:first + k + 1] for k in THREE]

        def bias(l, node):
            return bias_cols[:, node * layers + l:node * layers + l + 1]

        def hidden_of_nodes(l):
            table, b1 = tables[l], bias(l, 0)

            def body(step):
                xs = gather(table, keys(srow, step), iota).astype(BF)
                xr = gather(table, keys(rrow, step), iota).astype(BF)
                hidden[l, :, at(step, KS)] = dot(ew1t[l, :, mat(1, 2)], stacked([xs, xr])) + b1

            loop(eh // KS, body)

        def edge_forward(l):
            e_in = edges_in[l]

            def body(j):
                for sub in range(EC // T):
                    a = at(j * (EC // T) + sub, T)
                    if l == 0:
                        if sub == 0:
                            chunk_arrived(EDGE_IN, j)
                        for d in OTHERS:
                            e_in[rows_of(d), a] = e_recv[slot(d), j, :, sub * T:(sub + 1) * T].astype(BF)
                    e_val = e_in[:, a]
                    hid = hidden[l, :, a] + dot(ew1t[l, :, mat(0)], e_val)
                    hidden[l, :, a] = hid
                    message, nrm, std = mlp_tail(hid, ew2t[l], vec(l, 0))
                    normed[l, :, a] = nrm
                    inv[l:l + 1, a] = std
                    msg[:, a] = message
                    e_new = (e_val.astype(F32) + message.astype(F32)).astype(BF)
                    if l < top:
                        edges_in[l + 1][:, a] = e_new
                    else:
                        for d in OTHERS:
                            e_send[slot(d), j, :, sub * T:(sub + 1) * T] = e_new[rows_of(d)].astype(F32)
                        if sub == 0:
                            own_parts = []
                        own_parts.append(e_new[:q])
                if l == top:
                    for d in SEND_ORDER:
                        edge_start(EDGE_OUT, j, d)
                    place_edges(edge_raw, beside(own_parts), 0, j)

            loop(nch, body)

        def segment_sum(acc, ids_ref):
            acc[...] = jnp.zeros(acc.shape, F32)

            def body(step):
                scatter(acc, msg[:, at(step, KS)], ids_ref[at(step, KS), :], lanes)

            loop(eh // KS, body)

        def node_forward(l):
            table, agg, out = tables[l], aggs[l], tables[l + 1]

            def body(step):
                a = pl.ds(pl.multiple_of(step * TN, D), TN)
                v_in = table[:, a]
                agg_bf = (part[l, :, a] + swap_halves(part_recv[l, :, a])).astype(BF)
                agg[:, a] = agg_bf
                hid = dot(nw1t[l], stacked([v_in, agg_bf])) + bias(l, 1)
                nhid[l, :, a] = hid
                message, nrm, std = mlp_tail(hid, nw2t[l], vec(l, 1))
                nnrm[l, :, a] = nrm
                ninv[l:l + 1, a] = std
                out[:, a] = (v_in.astype(F32) + message.astype(F32)).astype(BF)

            loop(npad // TN, body)

        for l in range(layers):
            with jax.named_scope(f'gather_{l}'):
                hidden_of_nodes(l)
            if l == top:
                edges_sent(EDGE_IN)
            with jax.named_scope(f'edge_forward_{l}'):
                edge_forward(l)
            with jax.named_scope(f'sum_{l}'):
                segment_sum(part.at[l], rcol)
            part_copy(l).start()
            if l == 0:
                join_weights(1)
                gcop[1].wait_recv()
                gcop[2].start()
            with jax.named_scope(f'part_wait_{l}'):
                part_copy(l).wait_recv()
            with jax.named_scope(f'node_forward_{l}'):
                node_forward(l)
        for copy in ncop[:2]:
            copy.wait_send()
        for which in BOTH:
            pack_nodes(take_rows(tables[layers], rows_of(2 + which)), n_send.at[which])
        output_copies('start')
        node_raw[x] = tables[layers][:q, :nodes]

        for k in range(layers):
            part_copy(k).wait_send()
        s_sum, r_sum = (part.at[k] for k in BOTH)
        grad[...] = jnp.zeros_like(grad)
        sums[...] = jnp.zeros_like(sums)
        with jax.named_scope('grad_node_wait'):
            gcop[0].wait_recv()
            gcop[2].wait_recv()
        for d in OTHERS:
            unpack_nodes(gn_recv.at[slot(d)], put_rows(d_part, rows_of(d)))

        def node_backward(l):
            table, agg = tables[l], aggs[l]

            def body(step):
                a = pl.ds(pl.multiple_of(step * TN, D), TN)
                d_in = d_part[:, a]
                if l < top:
                    d_in = d_in + part[layers + l + 1, :, a] + swap_halves(part_recv[layers + l + 1, :, a])
                    d_in = d_in.astype(BF).astype(F32)
                d_hid, d_w2, parts = mlp_back(d_in, nhid[l, :, a], nnrm[l, :, a], ninv[l:l + 1, a], nw2[l], vec(l, 1))
                add_sums(sums.at[l, 1], [parts])
                grad[l, 4] += d_w2
                grad[l, 2] += dot_nt(table[:, a], d_hid)
                grad[l, 3] += dot_nt(agg[:, a], d_hid)
                d_part[:, a] = d_in + dot(nw1[l, mat(0), :], d_hid)
                d_agg[:, a] = dot(nw1[l, mat(1), :], d_hid).astype(BF)

            loop(npad // TN, body)

        def gather_back():
            def body(step):
                msg[:, at(step, KS)] = gather(d_agg, keys(rrow, step), iota).astype(BF)

            loop(eh // KS, body)

        def edge_backward(l):
            e_in = edges_in[l]

            def body(j):
                all_parts, d_w2s, d_w1s, own_parts = [], [], [], []
                for sub in range(EC // T):
                    a = at(j * (EC // T) + sub, T)
                    if l == top:
                        if sub == 0:
                            chunk_arrived(GRAD_IN, j)
                        for d in OTHERS:
                            ge[rows_of(d), a] = g_recv[slot(d), j, :, sub * T:(sub + 1) * T].astype(BF)
                    d_res = ge[:, a].astype(F32)
                    d_msg = d_res + msg[:, a].astype(F32)
                    d_hid, d_w2, parts = mlp_back(d_msg, hidden[l, :, a], normed[l, :, a], inv[l:l + 1, a], ew2[l], vec(l, 0))
                    all_parts.append(parts)
                    d_w2s.append(d_w2)
                    d_w1s.append(dot_nt(e_in[:, a], d_hid))
                    msg[:, a] = d_hid
                    d_new = (d_res + dot(ew1[l, mat(0), :], d_hid)).astype(BF)
                    if l > 0:
                        ge[:, a] = d_new
                    else:
                        for d in OTHERS:
                            g_send[slot(d), j, :, sub * T:(sub + 1) * T] = d_new[rows_of(d)].astype(F32)
                        own_parts.append(d_new[:q])
                add_sums(sums.at[l, 0], all_parts)
                grad[l, 1] += sum(d_w2s[1:], d_w2s[0])
                grad[l, 0] += sum(d_w1s[1:], d_w1s[0])
                if l == 0:
                    @pl.when(j < hold)
                    def _():
                        for d in SEND_ORDER:
                            edge_start(GRAD_OUT, j, d)
                    place_edges(gedge_raw, beside(own_parts), 0, j)

            loop(nch, body)

        def vector_slab(l):
            def total(node, k):
                return column_sum(flip(sums[l, node, mat(k), :]))

            lat = stacked([total(node, k) for node in BOTH for k in THREE])
            biases = stacked([total(node, 3) for node in BOTH])
            n_lat = lat.shape[0]
            for d in range(GROUP):
                grad[l, VEC_SLAB, d * cols:d * cols + n_lat, :cols] = lat[:, rows_of(d)]
                grad[l, VEC_SLAB, d * cols + n_lat:d * cols + n_lat + 2, :] = biases

        def reduce_start(l, stage):
            for b in BOTH:
                core_copy(l, b, stage).start()

        def chip_sum(l, stage):
            row = lax.broadcasted_iota(jnp.int32, (cols, D), 0)
            edge_row = jnp.logical_or(row < 3, row == 6)
            core_all(l, stage).wait_recv()
            for b in BOTH:
                for k in range(SLABS)[STAGES[stage]]:
                    own = grad[l, k, rows_of(2 * b), :]
                    if k in EDGE_SLABS:
                        own = own + core_recv[l, b, k]
                    elif k == VEC_SLAB:
                        other = core_recv[l, b, k]
                        own = own + jnp.where(edge_row, other, 0.0)
                        own = jnp.where(jnp.logical_and(row == 7, c == 1), other, own)
                    half[l, k, b] = own
            for i in dp_others:
                @pl.when(in_stage(lax.rem(p + i, dpn), stage))
                def _():
                    spread_copy(l, i).start()

        def dp_sum(l, stage):
            @pl.when(in_stage(p, stage))
            def _():
                total = half[l, pl.ds(seat(p) * per, per)]
                dp_all(l, 0).wait_recv()
                for i in dp_others:
                    total = total + dp_recv[l, pl.ds((i - 1) * per, per)]
                own_sum[l] = total[:, 0]
                cross_send[l] = total[:, 1]
                cross_copy(l).start()

        def cross_sum(l):
            cross_copy(l).wait_recv()
            total = own_sum[l] + cross_recv[l]
            own_sum[l] = total
            gathered[l, pl.ds(seat(p) * per, per)] = total
            for i in dp_others:
                gather_copy(l, i, p).start()

        def project(l):
            table = tables[l]

            def body(step):
                a = pl.ds(pl.multiple_of(step * TN, D), TN)
                s_bf, r_bf, v_in = s_sum[:, a].astype(BF), r_sum[:, a].astype(BF), table[:, a]
                part[layers + l, :, a] = dot(ew1[l, mat(1), :], s_bf) + dot(ew1[l, mat(2), :], r_bf)
                if l > 0:
                    part_piece(layers + l, a).start()
                grad[l, 6] += dot_nt(v_in, s_bf)
                grad[l, 7] += dot_nt(v_in, r_bf)

            loop(npad // TN, body)

        for l in reversed(range(layers)):
            first_layer = l == 0
            with jax.named_scope(f'node_backward_{l}'):
                node_backward(l)
            if first_layer:
                with jax.named_scope('chip_sum_1'):
                    chip_sum(1, 0)
                    chip_sum(1, 1)
            with jax.named_scope(f'gather_back_{l}'):
                gather_back()
            if first_layer:
                edges_sent(GRAD_IN)
            with jax.named_scope(f'edge_backward_{l}'):
                edge_backward(l)
            vector_slab(l)
            reduce_start(l, 0)
            if first_layer:
                with jax.named_scope('dp_sum_1'):
                    dp_sum(1, 0)
                    dp_sum(1, 1)
            with jax.named_scope(f'sum_send_{l}'):
                segment_sum(s_sum, scol)
            if first_layer:
                with jax.named_scope('chip_sum_0'):
                    chip_sum(0, 0)
            with jax.named_scope(f'sum_recv_{l}'):
                segment_sum(r_sum, rcol)
            with jax.named_scope(f'project_{l}'):
                project(l)
            reduce_start(l, 1)
            if first_layer:
                part_copy(layers + l).start()
            if first_layer:
                with jax.named_scope('chip_sum_late'):
                    chip_sum(0, 1)
                with jax.named_scope('dp_sum_0'):
                    dp_sum(0, 0)
            with jax.named_scope(f'back_wait_{l}'):
                part_copy(layers + l).wait_recv()

        def final(step):
            a = pl.ds(pl.multiple_of(step * TN, D), TN)
            d_in = (d_part[:, a] + part[layers, :, a] + swap_halves(part_recv[layers, :, a])).astype(BF)
            v2[:, a] = d_in

        loop(npad // TN, final)
        gnode_raw[x] = v2[:q, :nodes]
        with jax.named_scope('dp_sum_late'):
            dp_sum(0, 1)

        gcop[1].wait_send()
        dn_send = gn_send.at[0]
        pack_nodes(take_rows(v2, rows_of(2)), dn_send)
        dn_copy = remote(dn_send, dn_recv, n_ss.at[2, 1], n_rs.at[2, 1], 2)
        dn_copy.start()

        def send_rest(j):
            for d in SEND_ORDER:
                edge_start(GRAD_OUT, j, d)

        loop(nch, send_rest, hold)

        with jax.named_scope('node_out_wait'):
            output_copies('wait_recv')
        unpack_nodes(no_recv, put_output(node_raw))

        def place_e(j):
            for d in OTHERS:
                place_edges(edge_raw, eo_recv[slot(d), j], d, j)

        with jax.named_scope('place_edge_out'):
            for group in THREE:
                group_arrived(EDGE_OUT, group)
            loop(nch, place_e)

        def place_g(j):
            for d in OTHERS:
                place_edges(gedge_raw, de_recv[slot(d), j], d, j)

        with jax.named_scope('place_first'):
            group_arrived(GRAD_OUT, 0)
            loop(hold, place_g)
        for l in range(layers):
            with jax.named_scope(f'cross_sum_{l}'):
                cross_sum(l)
        with jax.named_scope('d_node_wait'):
            dn_copy.wait_recv()
        unpack_nodes(dn_recv, put_output(gnode_raw))
        with jax.named_scope('place_rest'):
            group_arrived(GRAD_OUT, 1)
            loop(last, place_g, hold)
        for l in range(layers):
            dp_all(l, 1).wait_recv()
            ew1_buf[l, 0] = gathered[l, 0]
            ew1_buf[l, 1:] = gathered[l, EARLY:]
            ew2_buf[l] = gathered[l, 1]
            nw1_buf[l] = gathered[l, 2:4]
            nw2_buf[l] = gathered[l, 4]
            small = gathered[l, VEC_SLAB]
            for k in THREE:
                evec_buf[k, l:l + 1, :] = small[k:k + 1, :cols]
                nvec_buf[k, l:l + 1, :] = small[3 + k:4 + k, :cols]
            eb1_buf[l:l + 1, :] = small[6:7]
            nb1_buf[l:l + 1, :] = small[7:8]
        for l in range(layers):
            for stage in BOTH:
                core_all(l, stage).wait_send()
            cross_copy(l).wait_send()
            dp_all(l, 0).wait_send()
            dp_all(l, 1).wait_send()
        for copy in (ncop[2], gcop[0], gcop[2], w_pair, w_relay):
            copy.wait_send()

        by_share(lambda rows: w_cross(rows).wait_send())
        pl.when(brings)(weight_part((dpn - 1) * piece).wait_send)
        pl.when(jnp.logical_not(brings))(weight_part((dpn - 1) * HEAD).wait_send)

        output_copies('wait_send')
        dn_copy.wait_send()
        for k in range(layers, 2 * layers):
            part_copy(k).wait_send()
        edges_sent(EDGE_OUT)
        with jax.named_scope('place_last'):
            for d in (1, 2, 3):
                last_arrived(GRAD_OUT, d)
                place_edges(gedge_raw, de_recv[slot(d), last], d, last)
        edges_sent(GRAD_OUT)

    bf = lambda *s: pltpu.VMEM(s, BF)
    pl.run_scoped(
        scoped, bf(D, eh), bf(D, eh), bf(D, eh), bf(D, eh), bf(D, npad), bf(D, npad), bf(D, npad), bf(D, npad), bf(D, npad), bf(D, npad),
        pltpu.VMEM((eh, D), I16), pltpu.VMEM((eh, D), I16), pltpu.VMEM((eh // D * 16, D), I16), pltpu.VMEM((eh // D * 16, D), I16),
        pltpu.VMEM((T, D), I16), pltpu.VMEM((16, D), I16),
        bf(layers, 3 * D, D), bf(layers, D, 3 * D), bf(layers, D, D), bf(layers, D, D),
        bf(layers, 2 * D, D), bf(layers, D, 2 * D), bf(layers, D, D), bf(layers, D, D), pltpu.VMEM((D, D), F32))


def finish_moves(src, dst):
    if len(src.shape) != 3 or src.dtype != BF:
        return [(src, dst)]
    return [(src.at[s, pl.ds(r, 8)], dst.at[s, pl.ds(r, 8)]) for s in range(src.shape[0]) for r in range(0, src.shape[1], 8)]


def finish_kernel(*refs):
    count = len(refs) // 2
    moves = sum((finish_moves(refs[k], refs[count + k]) for k in range(count)), [])
    puts = [pltpu.make_async_copy(src, dst, refs[-1]) for src, dst in moves]
    for put in puts:
        put.start()
    for put in puts:
        put.wait()


def keep_in_vmem(val):
    return pltpu.with_memory_space_constraint(val, pltpu.VMEM)


def finish(arrays):
    return pl.pallas_call(
        finish_kernel,
        name='finish',
        out_shape=[jax.ShapeDtypeStruct(a.shape, a.dtype) for a in arrays],
        in_specs=[VM] * len(arrays),
        out_specs=[HB] * len(arrays),
        scratch_shapes=[pltpu.SemaphoreType.DMA],
        compiler_params=pltpu.CompilerParams(vmem_limit_bytes=1 << 20),
    )(*[keep_in_vmem(a) for a in arrays])


def solution(mesh):
    lat_spec = P('dp', None, 'tp')
    first_spec = P(None, None, 'tp', None)
    col_spec = P(None, None, 'tp')
    param_specs = (first_spec, P(), col_spec, col_spec, first_spec, P(), col_spec, col_spec)
    in_specs = (lat_spec, lat_spec, P(), P(), lat_spec, lat_spec) + param_specs
    out_specs = (lat_spec, lat_spec, lat_spec, lat_spec) + param_specs
    shape = jax.ShapeDtypeStruct

    def local_step(node_lat, edge_lat, senders, receivers, grad_node, grad_edge, edge_w1, edge_b1, edge_w2, edge_vec, node_w1, node_b1, node_w2, node_vec):
        layers = edge_w1.shape[0]
        cols = node_lat.shape[2]
        nodes, edges = node_lat.shape[1], edge_lat.shape[1]
        npad = -(-nodes // TN) * TN
        eh = -(-edges // (2 * EC)) * EC
        nch = eh // EC
        dpn = mesh.shape['dp']
        per = SLABS // dpn
        dims = (layers, cols, nodes, edges, npad, eh, dpn)
        flat = lambda arr: jnp.swapaxes(arr, 1, 2)
        lead = lambda arr: jnp.transpose(arr, (1, 0, 2))
        args = (flat(node_lat), flat(edge_lat), flat(grad_node), flat(grad_edge), senders, receivers,
                edge_w1.reshape(-1, D), flat(edge_w2).reshape(-1, D), node_w1.reshape(-1, D), flat(node_w2).reshape(-1, D),
                lead(edge_vec), lead(node_vec), edge_b1, node_b1)
        vm, sem = pltpu.VMEM, pltpu.SemaphoreType.DMA
        packed = nodes // D * cols + -(-(nodes % D) * GROUP // D) * cols // GROUP
        wrows = HEAD + layers * LROWS
        lat_n, lat_e = (2, cols, nodes), (2, cols, edges)
        outs = [RESULT(lat_n, BF), RESULT(lat_e, BF), RESULT(lat_n, BF), RESULT(lat_e, BF),
                RESULT((layers, 3, cols, D), F32), RESULT((layers, D), F32), RESULT((layers, cols, D), F32), RESULT((3, layers, cols), F32),
                RESULT((layers, 2, cols, D), F32), RESULT((layers, D), F32), RESULT((layers, cols, D), F32), RESULT((3, layers, cols), F32)]
        scratch = [
            *[vm(a.shape, a.dtype) for a in args[4:]], vm((wrows, D), F32), vm((3, wrows, D), F32),
            *[vm((many, packed, D), F32) for many in (2, 3, 2, 3)], *[vm((packed, D), F32)] * 2, vm((cols, npad), F32),
            *[vm((kinds, len(OTHERS), cols + cols // GROUP, D), F32) for kinds in (2, GROUP)], *[vm((len(OTHERS), nch, cols, EC), F32)] * 6,
            vm((2 * layers, D, npad), F32), vm((2 * layers, D, npad), F32),
            vm((layers, D, eh), F32), vm((layers, D, eh), F32), vm((layers, eh), F32),
            vm((layers, D, npad), F32), vm((layers, D, npad), F32), vm((layers, npad), F32),
            vm((D, npad), F32), vm((2, 2 * eh), jnp.int32), vm((D, D), F32), vm((layers, 2, 4 * D, D), F32),
            vm((layers, SLABS, D, D), F32), vm((layers, 2, SLABS, cols, D), F32), vm((layers, SLABS, 2, cols, D), F32),
            vm((layers, (dpn - 1) * per, 2, cols, D), F32), vm((layers, per, cols, D), F32), vm((layers, per, cols, D), F32),
            vm((layers, per, cols, D), F32), vm((layers, SLABS, cols, D), F32),]
        own_sems = [
            sem((layers, 2)), sem((3, layers)), sem((layers,)), sem((3,)), sem((3, 3)), sem((2, nch)), sem((2, 5)), sem((2 * layers,)),
            pltpu.SemaphoreType.REGULAR,
            sem((len(args) + 1,)), sem((3,)), sem((3, 3)), sem((4, 4)), sem((2 * layers,)), sem((layers, 2)), sem((3, layers)), sem((layers,))]
        res = pl.pallas_call(
            lambda *refs: pl.run_scoped(lambda *own: step_kernel(dims, *refs, *own), *own_sems),
            name='graph_step',
            out_shape=outs,
            in_specs=[HB] * len(args),
            out_specs=[VM] * len(outs),
            scratch_shapes=scratch,
            compiler_params=pltpu.CompilerParams(collective_id=0, has_side_effects=True, vmem_limit_bytes=VMEM_LIMIT),
        )(*args)

        res = finish(res)
        return (flat(res[0]), flat(res[1]), flat(res[2]), flat(res[3]),
                res[4], res[5], flat(res[6]), lead(res[7]), res[8], res[9], flat(res[10]), lead(res[11]))

    return jax.shard_map(local_step, mesh=mesh, in_specs=in_specs, out_specs=out_specs, check_vma=False)
```

```python
import jax
import jax.numpy as jnp
from jax import lax
from jax.experimental import pallas as pl
from jax.experimental.pallas import tpu as pltpu
from jax.sharding import PartitionSpec as P

LN_EPS = 1e-5
D = 128
T = 256
TN = 384
EC = 512
KS = 2816
BF = jnp.bfloat16
F32 = jnp.float32
I16 = jnp.int16
MESH = pl.DeviceIdType.MESH
VM = pl.BlockSpec(memory_space=pltpu.VMEM)
HB = pl.BlockSpec(memory_space=pl.ANY)
RESULT = pltpu.VMEM
GROUP = 4
BOTH = (0, 1)
THREE = (0, 1, 2)
OTHERS = (1, 2, 3)
EDGE_IN, GRAD_IN, EDGE_OUT, GRAD_OUT = range(4)
SEND_ORDER = (2, 3, 1)
LROWS = 7 * (D // 4)
HEAD = 8
LEADER = GROUP - 1
HELPER = LEADER - 1
VMEM_LIMIT = 63_000_000
SLABS = 8
EARLY = 6
VEC_SLAB = 5
EDGE_SLABS = (0, 1, 6, 7)
STAGES = (slice(0, EARLY), slice(EARLY, SLABS))


def dot(a, b):
    return jnp.dot(a, b, preferred_element_type=F32)


def dot_nt(a, b):
    return lax.dot_general(a, b, (((1,), (1,)), ((), ())), preferred_element_type=F32)


def mat(k, n=1):
    return slice(k * D, (k + n) * D)


def rows_of(d):
    q = D // 4
    return slice(d * q, (d + 1) * q)


def at(step, width):
    return pl.ds(pl.multiple_of(step * width, width), width)


def loop(stop, body, start=0):
    def step(j, carry):
        body(j)
        return carry

    lax.fori_loop(start, stop, step, 0)


def column_sum(val):
    return jnp.sum(val, axis=0, keepdims=True)


def flip(val):
    return jnp.swapaxes(val, 0, 1)


def stacked(parts):
    return jnp.concatenate(parts, axis=0)


def beside(parts):
    return jnp.concatenate(parts, axis=1)


def slot(d):
    return d - 1


def sigmoid(hidden):
    return 1.0 / (1.0 + jnp.exp(-hidden))


def fold(val):
    total = val[:, mat(0)]
    for start in range(D, val.shape[1], D):
        total = total + val[:, start:start + D]
    return total


def swap_halves(val):
    return stacked([val[rows_of(d)] for d in (1, 0, 3, 2)])


def gather(table, keys, iota):
    acc = None
    nodes = table.shape[1]
    one, zero = jnp.ones((), BF), jnp.zeros((), BF)
    for base in range(0, nodes, T):
        width = min(T, nodes - base)
        ids = iota[0:width, :]
        hot = beside([jnp.where(ids == (key - jnp.asarray(base, I16)), one, zero) for key in keys])
        part = dot(table[:, base:base + width], hot)
        acc = part if acc is None else acc + part
    return acc


def scatter(acc_ref, val, cols, lanes):
    nodes = acc_ref.shape[1]
    one, zero = jnp.ones((), BF), jnp.zeros((), BF)
    row = lanes[0:1, :]
    for base in range(0, nodes, T):
        width = min(T, nodes - base)
        hot = beside([jnp.where((row + jnp.asarray(base + s, I16)) == cols, one, zero) for s in range(0, width, D)])
        acc_ref[:, base:base + width] += dot(val, hot)


def mlp_tail(hidden, w2t, vec):
    act = (hidden * sigmoid(hidden)).astype(BF)
    out = dot(w2t, act) + vec[0]
    mean = column_sum(out) / D
    centered = out - mean
    var = column_sum(centered * centered) / D
    inv = lax.rsqrt(var + LN_EPS)
    normed = centered * inv
    message = (normed * vec[1] + vec[2]).astype(BF)
    return message, normed, inv


def mlp_back(d_msg, hidden, normed, inv, w2, vec):
    d_normed = d_msg * vec[1]
    mean0 = column_sum(d_normed) / D
    mean1 = column_sum(d_normed * normed) / D
    d_out = inv * (d_normed - mean0 - normed * mean1)
    d_out_bf = d_out.astype(BF)
    sig = sigmoid(hidden)
    act = (hidden * sig).astype(BF)
    d_w2 = dot_nt(d_out_bf, act)
    d_hidden = dot(w2, d_out_bf) * (sig * (1.0 + hidden * (1.0 - sig)))
    sums = (fold(d_out), fold(d_msg * normed), fold(d_msg), fold(d_hidden))
    return d_hidden.astype(BF), d_w2, sums


def add_sums(ref, parts):
    for q in range(4):
        total = parts[0][q]
        for other in parts[1:]:
            total = total + other[q]
        ref[mat(q), :] += total


def step_kernel(dims, *refs):
    layers, cols, nodes, edges, npad, eh, dpn = dims
    nch = eh // EC
    top = layers - 1
    n_in = 14
    hbm_in = refs[:n_in]
    n_out = 12
    (node_raw, edge_raw, gnode_raw, gedge_raw, ew1_buf, eb1_buf, ew2_buf, evec_buf, nw1_buf, nb1_buf, nw2_buf, nvec_buf) = refs[n_in:n_in + n_out]
    (send_ids, recv_ids, ew1_in, ew2_in, nw1_in, nw2_in, evec_in, nvec_in, eb1_in, nb1_in, w_send, w_recv, n_send, n_recv, gn_send, gn_recv, no_recv, dn_recv,
     node_pad, t_send, t_recv, e_send, g_send, e_recv, g_recv, eo_recv, de_recv, part, part_recv, hidden, normed, inv, nhid, nnrm, ninv, d_part,
     ids_raw, bias_cols, sums, grad, core_recv, half, dp_recv, cross_send, cross_recv, own_sum, gathered,
     core_rs, dp_rs, cross_rs, w_rs, n_rs, e_rs, o_rs, p_rs, ready, load_sem, w_ss, n_ss, e_ss, p_ss, core_ss, dp_ss, cross_ss) = refs[n_in + n_out:]

    t = lax.axis_index('tp')
    p = lax.axis_index('dp')
    per = SLABS // dpn
    dp_others = range(1, dpn)
    x, c = t // 2, lax.rem(t, 2)
    ox, oc = 1 - x, 1 - c
    mate, across = t + oc - c, t + 2 * (ox - x)
    peer = [t, mate, across, mate + across - t]

    def remote(src, dst, ssem, rsem, d):
        return pltpu.make_async_remote_copy(src_ref=src, dst_ref=dst, send_sem=ssem, recv_sem=rsem,
                                            device_id={'tp': peer[d]}, device_id_type=MESH)

    small_in = (send_ids, recv_ids, ew1_in, ew2_in, nw1_in, nw2_in, evec_in, nvec_in, eb1_in, nb1_in)
    loads = [pltpu.make_async_copy(src, dst, load_sem.at[q]) for q, (src, dst) in enumerate(
        zip((hbm_in[0].at[x],) + hbm_in[1:], (node_raw.at[x], edge_raw, gnode_raw, gedge_raw) + small_in))]
    node_load, edge_load, gnode_load, gedge_load, *small_loads = loads
    first_load = pltpu.make_async_copy(hbm_in[0].at[ox], node_raw.at[ox], load_sem.at[n_in])

    def node_copies(send, recv, kind):
        return (remote(send.at[1], recv.at[0], n_ss.at[kind, 0], n_rs.at[kind, 0], 1),
                remote(send.at[0], recv.at[1], n_ss.at[kind, 1], n_rs.at[kind, 1], 2),
                remote(recv.at[1], recv.at[2], n_ss.at[kind, 2], n_rs.at[kind, 2], 1))

    piece = (w_send.shape[0] - HEAD) // (dpn - 1)
    brings = p > 0

    def packed(l, k, count=1):
        return pl.ds(HEAD + l * LROWS + k * cols, count * cols)

    def by_share(action):
        @pl.when(brings)
        def _():
            action(pl.ds(pl.multiple_of(HEAD + (p - 1) * piece, HEAD), piece))

        @pl.when(jnp.logical_not(brings))
        def _():
            action(slice(HEAD))

    w_pair = remote(w_send, w_recv.at[0], w_ss.at[0], w_rs.at[0], 1)
    def w_cross(rows):
        return remote(w_send.at[rows], w_recv.at[1, rows], w_ss.at[1], w_rs.at[1], 2)

    w_relay = remote(w_recv.at[1], w_recv.at[2], w_ss.at[2], w_rs.at[2], 1)

    def weight_copy(i, rows):
        rows = w_recv.at[1, rows]
        return dp_remote(rows, rows, 2, 0, i)

    last = nch - 1
    hold = nch - 3
    share = 2 * (eh - last * EC - D - D // GROUP) * cols // D
    share = min(share, no_recv.shape[0] // 16 * 8)
    buffers = ((e_send, e_recv), (g_send, g_recv), (e_send, eo_recv), (g_send, de_recv))

    def outward(kind):
        return kind in (EDGE_OUT, GRAD_OUT)

    every = slice(None)
    ragged = pl.ds(D, D // GROUP)
    rest = [slice(g * cols // GROUP, (g + 1) * cols // GROUP) for g in range(GROUP)]

    def edge_part(kind, which, j, tail, send_sem, recv_sem, d):
        src, dst = buffers[kind]
        if tail:
            src, dst = t_send.at[kind % 2, which], t_recv.at[kind, which]
        else:
            src, dst = src.at[which, j], dst.at[which, j]
        recv_sems = o_rs.at[kind - EDGE_OUT, recv_sem] if outward(kind) else e_rs.at[kind, recv_sem]
        return remote(src, dst, e_ss.at[kind, send_sem], recv_sems, d)

    def by_half(half_id, j, action):
        narrow = jnp.logical_and(j == last, half_id == 1)

        @pl.when(jnp.logical_not(narrow))
        def _():
            action(False)

        @pl.when(narrow)
        def _():
            action(True)

    def pack_tail(kind, d):
        src, out = buffers[kind][0].at[slot(d), last], t_send.at[kind % 2, slot(d)]
        out[:cols, :] = src[:, :D]
        over = src[:, ragged]
        out[cols:, :] = beside([over[r] for r in rest])

    def unpack_tail(kind, d):
        src, out = t_recv.at[kind, slot(d)], buffers[kind][1].at[slot(d), last]
        out[:, :D] = src[:cols, :]
        over = src[cols:, :]
        out[:, ragged] = stacked([over[:, rows_of(g)] for g in range(GROUP)])

    def edge_start(kind, j, d):
        other = oc if d % 2 else c
        if outward(kind):
            at_last = j == last
            send_sem = jnp.asarray(at_last, jnp.int32)
            recv_sem = jnp.where(at_last, 2 + slot(d), jnp.asarray(j >= hold, jnp.int32))
        else:
            send_sem, recv_sem = jnp.where(j == last, d, 0), j

        def start(tail):
            if tail:
                pack_tail(kind, d)
            edge_part(kind, slot(d), j, tail, send_sem, recv_sem, d).start()

        by_half(c if outward(kind) else other, j, start)

    def edges_sent(kind):
        edge_part(kind, every, slice(0, last), False, 0, 0, 1).wait_send()
        if outward(kind):
            by_half(c, last, lambda tail: edge_part(kind, every, last, tail, 1, 0, 1).wait_send())
        else:
            for d in OTHERS:
                by_half(oc if d % 2 else c, last, lambda tail: edge_part(kind, slot(d), last, tail, d, 0, d).wait_send())

    def chunk_arrived(kind, j):
        def arrived(tail):
            edge_part(kind, every, j, tail, 0, j, 1).wait_recv()
            if tail:
                for d in OTHERS:
                    unpack_tail(kind, d)

        by_half(c, j, arrived)

    def group_arrived(kind, group):
        if group < 2:
            edge_part(kind, every, (slice(0, hold), slice(hold, last))[group], False, 0, group, 1).wait_recv()
        else:
            for d in OTHERS:
                last_arrived(kind, d)

    def last_arrived(kind, d):
        def arrived(tail):
            edge_part(kind, slot(d), last, tail, 0, 2 + slot(d), d).wait_recv()
            if tail:
                unpack_tail(kind, d)

        by_half(oc if d % 2 else c, last, arrived)

    def core_copy(l, b, stage):
        return remote(grad.at[l, STAGES[stage], pl.ds((2 * b + 1) * cols, cols), :], core_recv.at[l, b, STAGES[stage]],
                      core_ss.at[l, stage], core_rs.at[l, stage], 1)

    def core_all(l, stage):
        part_of = core_recv.at[l, :, STAGES[stage]]
        return remote(part_of, part_of, core_ss.at[l, stage], core_rs.at[l, stage], 1)

    def seat(device):
        return lax.rem(device + dpn // 2, dpn)

    def in_stage(device, stage):
        early = (seat(device) + 1) * per <= EARLY
        return jnp.logical_not(early) if stage else early

    def dp_remote(src, dst, stage, l, i):
        return pltpu.make_async_remote_copy(src_ref=src, dst_ref=dst, send_sem=dp_ss.at[stage, l], recv_sem=dp_rs.at[stage, l],
                                            device_id={'dp': lax.rem(p + i, dpn)}, device_id_type=MESH)

    def spread_copy(l, i):
        return dp_remote(half.at[l, pl.ds(seat(lax.rem(p + i, dpn)) * per, per)], dp_recv.at[l, pl.ds((i - 1) * per, per)], 0, l, i)

    def dp_all(l, stage):
        part_of = (dp_recv.at[l], gathered.at[l, slice((dpn - 1) * per)])[stage]
        return dp_remote(part_of, part_of, stage, l, 1)

    def weight_part(rows):
        part_of = w_recv.at[1, slice(rows)]
        return dp_remote(part_of, part_of, 2, 0, 1)

    def cross_copy(l):
        return remote(cross_send.at[l], cross_recv.at[l], cross_ss.at[l], cross_rs.at[l], 2)

    def gather_copy(l, i, owner):
        return dp_remote(own_sum.at[l], gathered.at[l, pl.ds(seat(owner) * per, per)], 1, l, i)

    def output_copies(action):
        block, more = n_send.at[0], n_send.at[1]
        most = slice(block.shape[0] - share)
        end = pl.ds(block.shape[0] - share, share)
        sems = n_ss.at[2, 0], n_rs.at[2, 0]
        extra = remote(more.at[end], no_recv.at[end], n_ss.at[2, 2], n_rs.at[2, 2], 3)
        first_core = c == 0

        @pl.when(first_core)
        def _():
            getattr(remote(block.at[most], no_recv.at[most], *sems, 2), action)()
            if action == 'wait_recv':
                extra.wait_recv()

        @pl.when(jnp.logical_not(first_core))
        def _():
            getattr(remote(block, no_recv, *sems, 2), action)()
            if action != 'wait_recv':
                getattr(extra, action)()

    def part_piece(q, a):
        return remote(part.at[q, :, a], part_recv.at[q, :, a], p_ss.at[q], p_rs.at[q], 1)

    def part_copy(q):
        return remote(part.at[q], part_recv.at[q], p_ss.at[q], p_rs.at[q], 1)

    wide = D // GROUP
    tiles = nodes // D
    over = range(tiles * D, nodes, wide)

    def node_rows(k):
        return slice(k * cols, (k + 1) * cols) if k < tiles else pl.ds(tiles * cols + (k - tiles) * cols // GROUP, cols // GROUP)

    def pack_tiles(take, out, which):
        for k in which:
            out[node_rows(k), :] = take(k * D, D)

    def pack_nodes(take, out, first=0):
        pack_tiles(take, out, range(first, tiles))
        for k, start in enumerate(over):
            val = take(start, wide)
            out[node_rows(tiles + k), :] = beside([val[r] for r in rest])

    def unpack_nodes(src, put):
        for k in range(tiles):
            put(k * D, src[node_rows(k), :])
        for k, start in enumerate(over):
            val = src[node_rows(tiles + k), :]
            put(start, stacked([val[:, rows_of(g)] for g in range(GROUP)]))

    def put_rows(ref, rows):
        def put(start, val):
            ref[rows, start:start + val.shape[1]] = val.astype(ref.dtype)

        return put

    def put_output(ref):
        def put(start, val):
            used = min(val.shape[1], nodes - start)
            ref[ox, :, start:start + used] = val[:, :used].astype(ref.dtype)

        return put

    def take_raw(raw, sample):
        def take(start, width):
            used = min(width, nodes - start)
            val = raw[sample, :, start:start + used].astype(F32)
            return val if used == width else beside([val, jnp.zeros((cols, width - used), F32)])

        return take

    def take_rows(ref, rows):
        return lambda start, width: ref[rows, start:start + width].astype(F32)

    def load_nodes(raw, sample, out):
        node_pad[:, :nodes] = raw[sample].astype(F32)
        pack_nodes(take_rows(node_pad, every), out)

    def keep_nodes(own):
        own[...] = jnp.zeros_like(own)
        own[:cols, :] = node_pad[...].astype(own.dtype)

    def load_edges(raw, send, own, kind):
        def put(j, lanes_j, val_of):
            for d in OTHERS:
                sample = x if d < 2 else ox
                send[slot(d), j] = val_of(sample, oc if d % 2 else c).astype(F32)
            own[:cols, lanes_j] = val_of(x, c)

        def chunk(j):
            put(j, at(j, EC), lambda s, h: raw[s, :, pl.ds(pl.multiple_of(h * eh + j * EC, D), EC)])
            for d in SEND_ORDER:
                edge_start(kind, j, d)

        loop(nch - 1, chunk)
        first = (nch - 1) * EC
        used = edges - eh - first
        last = pl.ds(first, EC)

        def tail(s, h):
            left = raw[s, :, pl.ds(first, EC)]
            right = beside([raw[s, :, pl.ds(eh + first, used)], jnp.zeros((cols, EC - used), BF)])
            return jnp.where(h == 0, left.astype(F32), right.astype(F32)).astype(BF)

        put(nch - 1, last, tail)
        for d in SEND_ORDER:
            edge_start(kind, nch - 1, d)

    def place_edges(raw, block, d, j):
        s = x if d < 2 else ox
        h = oc if d % 2 else c
        val = block.astype(BF)
        first = (nch - 1) * EC
        used = edges - eh - first

        @pl.when(jnp.logical_or(j < nch - 1, h == 0))
        def _():
            raw[s, :, pl.ds(pl.multiple_of(h * eh + j * EC, D), EC)] = val

        @pl.when(jnp.logical_and(j == nch - 1, h == 1))
        def _():
            raw[s, :, pl.ds(eh + first, used)] = val[:, :used]

    def scoped(e0, e1, ge, msg, v0, v1, v2, agg0, agg1, d_agg, scol, rcol, srow, rrow, iota, lanes, ew1, ew1t, ew2, ew2t, nw1, nw1t, nw2, nw2t, vecs):
        tables = (v0, v1, v2)
        aggs = (agg0, agg1)
        edges_in = (e0, e1)

        barrier = pltpu.get_barrier_semaphore()
        for d in OTHERS:
            pl.semaphore_signal(barrier, device_id={'tp': peer[d]}, device_id_type=MESH)
        for copy in (first_load, node_load, *small_loads, edge_load, gnode_load, gedge_load):
            copy.start()
        node_pad[...] = jnp.zeros_like(node_pad)
        with jax.named_scope('barrier'):
            @pl.when(t != LEADER)
            def _():
                pl.semaphore_wait(barrier, len(OTHERS))

            @pl.when(t == HELPER)
            def _():
                pl.semaphore_signal(ready, device_id={'tp': LEADER}, device_id_type=MESH)

            @pl.when(t == LEADER)
            def _():
                pl.semaphore_wait(ready)

        first_load.wait()
        ncop = node_copies(n_send, n_recv, 0)
        early = 2
        take, out = take_raw(node_raw, ox), n_send.at[0]
        pack_tiles(take, out, range(early))

        def send_part(rows):
            remote(out.at[rows], n_recv.at[1, rows], n_ss.at[0, 1], n_rs.at[0, 1], 2).start()

        send_part(slice(early * cols))
        pack_nodes(take, out, early)
        send_part(slice(early * cols, out.shape[0]))
        node_load.wait()
        load_nodes(node_raw, x, n_send.at[1])
        keep_nodes(v0)
        ncop[0].start()
        for copy in small_loads:
            copy.wait()
        q = cols
        w_send[:HEAD, :] = jnp.zeros((HEAD, D), F32)
        for k in THREE:
            w_send[k:k + 1, :] = beside([src[k, l:l + 1, :] for src in (evec_in, nvec_in) for l in range(layers)])
        for l in range(layers):
            w_send[packed(l, 0, 3), :] = ew1_in[pl.ds(l * 3 * q, 3 * q), :].astype(F32)
            w_send[packed(l, 3), :] = ew2_in[pl.ds(l * q, q), :].astype(F32)
            w_send[packed(l, 4, 2), :] = nw1_in[pl.ds(l * 2 * q, 2 * q), :].astype(F32)
            w_send[packed(l, 6), :] = nw2_in[pl.ds(l * q, q), :].astype(F32)
        by_share(lambda rows: w_cross(rows).start())
        w_pair.start()
        edge_load.wait()
        with jax.named_scope('send_edges'):
            load_edges(edge_raw, e_send, e0, EDGE_IN)
        gnode_load.wait()
        load_nodes(gnode_raw, ox, gn_send.at[0])
        load_nodes(gnode_raw, x, gn_send.at[1])
        keep_nodes(d_part)
        gcop = node_copies(gn_send, gn_recv, 1)
        gcop[1].start()
        gcop[0].start()
        gedge_load.wait()
        with jax.named_scope('send_grads'):
            load_edges(gedge_raw, g_send, ge, GRAD_IN)

        with jax.named_scope('dp_barrier'):
            @pl.when(t == LEADER)
            def _():
                for i in dp_others:
                    pl.semaphore_signal(barrier, device_id={'dp': lax.rem(p + i, dpn)}, device_id_type=MESH)
                pl.semaphore_wait(barrier, len(OTHERS) + dpn - 1)
                for d in OTHERS:
                    pl.semaphore_signal(ready, device_id={'tp': peer[d]}, device_id_type=MESH)

            @pl.when(t != LEADER)
            def _():
                pl.semaphore_wait(ready)

        def hand_on(rows):
            w_cross(rows).wait_recv()
            for i in dp_others:
                weight_copy(i, rows).start()

        by_share(hand_on)

        @pl.when(c == 1)
        def _():
            for recv in (e_recv, g_recv):
                recv[:, last, :, D:] = jnp.zeros((len(OTHERS), cols, EC - D), F32)

        iota[...] = lax.broadcasted_iota(jnp.int32, (T, D), 0).astype(I16)
        lanes[...] = lax.broadcasted_iota(jnp.int32, (16, D), 1).astype(I16)

        ids_raw[...] = jnp.full(ids_raw.shape, -1, jnp.int32)
        for which, src in enumerate((send_ids, recv_ids)):
            ids_raw[which:which + 1, :edges] = src[...].reshape(1, edges)

        def ids(b):
            for which, (row_ref, col_ref) in enumerate(((srow, scol), (rrow, rcol))):
                wide = jnp.broadcast_to(ids_raw[which:which + 1, pl.ds(pl.multiple_of(c * eh + b * D, D), D)], (D, D))
                row_ref[at(b, 16), :] = wide[:16].astype(I16)
                col_ref[at(b, D), :] = flip(wide.astype(F32)).astype(jnp.int32).astype(I16)

        with jax.named_scope('ids'):
            loop(eh // D, ids)

        def keys(ref, step):
            return [ref[pl.ds(pl.multiple_of(step * (KS // D) * 16 + 16 * h, 16), 1), :] for h in range(KS // D)]

        bias_cols[...] = flip(stacked([eb1_in[...], nb1_in[...], jnp.zeros((D - 2 * layers, D), F32)]))

        def join_weights(l):
            for d in range(GROUP):
                src = w_recv.at[slot(d)] if d else w_send
                r = rows_of(d)
                for k in THREE:
                    ew1[l, pl.ds(k * D + d * q, q), :] = src[packed(l, k), :].astype(BF)
                ew2t[l, r, :] = src[packed(l, 3), :].astype(BF)
                for k in BOTH:
                    nw1[l, pl.ds(k * D + d * q, q), :] = src[packed(l, 4 + k), :].astype(BF)
                nw2t[l, r, :] = src[packed(l, 6), :].astype(BF)

            def flip_bf(mat):
                return flip(mat.astype(F32)).astype(BF)

            for k in THREE:
                ew1t[l, :, mat(k)] = flip_bf(ew1[l, mat(k), :])
            for k in BOTH:
                nw1t[l, :, mat(k)] = flip_bf(nw1[l, mat(k), :])
            ew2[l] = flip_bf(ew2t[l])
            nw2[l] = flip_bf(nw2t[l])

        def wait_recvs(copies):
            copies[1].wait_recv()
            copies[2].start()
            copies[0].wait_recv()
            copies[2].wait_recv()

        with jax.named_scope('node_wait'):
            wait_recvs(ncop)
        for d in OTHERS:
            unpack_nodes(n_recv.at[slot(d)], put_rows(v0, rows_of(d)))
        with jax.named_scope('weight_wait'):
            pl.when(jnp.logical_not(brings))(weight_part(w_send.shape[0] - HEAD).wait_recv)
            pl.when(brings)(weight_part(w_send.shape[0] - piece).wait_recv)
            w_relay.start()
            w_pair.wait_recv()
            w_relay.wait_recv()
        blocks = [w_send] + [w_recv.at[d] for d in THREE]
        rows_all = beside([stacked([src[:HEAD, rows_of(g)] for g in range(GROUP)]) for src in blocks])
        vecs[...] = flip(stacked([rows_all, jnp.zeros((D - rows_all.shape[0], D), F32)]))
        join_weights(0)

        def vec(l, node):
            first = (node * layers + l) * HEAD
            return [vecs[:, first + k:first + k + 1] for k in THREE]

        def bias(l, node):
            return bias_cols[:, node * layers + l:node * layers + l + 1]

        def hidden_of_nodes(l):
            table, b1 = tables[l], bias(l, 0)

            def body(step):
                xs = gather(table, keys(srow, step), iota).astype(BF)
                xr = gather(table, keys(rrow, step), iota).astype(BF)
                hidden[l, :, at(step, KS)] = dot(ew1t[l, :, mat(1, 2)], stacked([xs, xr])) + b1

            loop(eh // KS, body)

        def edge_forward(l):
            e_in = edges_in[l]

            def body(j):
                for sub in range(EC // T):
                    a = at(j * (EC // T) + sub, T)
                    if l == 0:
                        if sub == 0:
                            chunk_arrived(EDGE_IN, j)
                        for d in OTHERS:
                            e_in[rows_of(d), a] = e_recv[slot(d), j, :, sub * T:(sub + 1) * T].astype(BF)
                    e_val = e_in[:, a]
                    hid = hidden[l, :, a] + dot(ew1t[l, :, mat(0)], e_val)
                    hidden[l, :, a] = hid
                    message, nrm, std = mlp_tail(hid, ew2t[l], vec(l, 0))
                    normed[l, :, a] = nrm
                    inv[l:l + 1, a] = std
                    msg[:, a] = message
                    e_new = (e_val.astype(F32) + message.astype(F32)).astype(BF)
                    if l < top:
                        edges_in[l + 1][:, a] = e_new
                    else:
                        for d in OTHERS:
                            e_send[slot(d), j, :, sub * T:(sub + 1) * T] = e_new[rows_of(d)].astype(F32)
                        if sub == 0:
                            own_parts = []
                        own_parts.append(e_new[:q])
                if l == top:
                    for d in SEND_ORDER:
                        edge_start(EDGE_OUT, j, d)
                    place_edges(edge_raw, beside(own_parts), 0, j)

            loop(nch, body)

        def segment_sum(acc, ids_ref):
            acc[...] = jnp.zeros(acc.shape, F32)

            def body(step):
                scatter(acc, msg[:, at(step, KS)], ids_ref[at(step, KS), :], lanes)

            loop(eh // KS, body)

        def node_forward(l):
            table, agg, out = tables[l], aggs[l], tables[l + 1]

            def body(step):
                a = pl.ds(pl.multiple_of(step * TN, D), TN)
                v_in = table[:, a]
                agg_bf = (part[l, :, a] + swap_halves(part_recv[l, :, a])).astype(BF)
                agg[:, a] = agg_bf
                hid = dot(nw1t[l], stacked([v_in, agg_bf])) + bias(l, 1)
                nhid[l, :, a] = hid
                message, nrm, std = mlp_tail(hid, nw2t[l], vec(l, 1))
                nnrm[l, :, a] = nrm
                ninv[l:l + 1, a] = std
                out[:, a] = (v_in.astype(F32) + message.astype(F32)).astype(BF)

            loop(npad // TN, body)

        for l in range(layers):
            with jax.named_scope(f'gather_{l}'):
                hidden_of_nodes(l)
            if l == top:
                edges_sent(EDGE_IN)
            with jax.named_scope(f'edge_forward_{l}'):
                edge_forward(l)
            with jax.named_scope(f'sum_{l}'):
                segment_sum(part.at[l], rcol)
            part_copy(l).start()
            if l == 0:
                join_weights(1)
                gcop[1].wait_recv()
                gcop[2].start()
            with jax.named_scope(f'part_wait_{l}'):
                part_copy(l).wait_recv()
            with jax.named_scope(f'node_forward_{l}'):
                node_forward(l)
        for copy in ncop[:2]:
            copy.wait_send()
        for which in BOTH:
            pack_nodes(take_rows(tables[layers], rows_of(2 + which)), n_send.at[which])
        output_copies('start')
        node_raw[x] = tables[layers][:q, :nodes]

        for k in range(layers):
            part_copy(k).wait_send()
        s_sum, r_sum = (part.at[k] for k in BOTH)
        grad[...] = jnp.zeros_like(grad)
        sums[...] = jnp.zeros_like(sums)
        with jax.named_scope('grad_node_wait'):
            gcop[0].wait_recv()
            gcop[2].wait_recv()
        for d in OTHERS:
            unpack_nodes(gn_recv.at[slot(d)], put_rows(d_part, rows_of(d)))

        def node_backward(l):
            table, agg = tables[l], aggs[l]

            def body(step):
                a = pl.ds(pl.multiple_of(step * TN, D), TN)
                d_in = d_part[:, a]
                if l < top:
                    d_in = d_in + part[layers + l + 1, :, a] + swap_halves(part_recv[layers + l + 1, :, a])
                    d_in = d_in.astype(BF).astype(F32)
                d_hid, d_w2, parts = mlp_back(d_in, nhid[l, :, a], nnrm[l, :, a], ninv[l:l + 1, a], nw2[l], vec(l, 1))
                add_sums(sums.at[l, 1], [parts])
                grad[l, 4] += d_w2
                grad[l, 2] += dot_nt(table[:, a], d_hid)
                grad[l, 3] += dot_nt(agg[:, a], d_hid)
                d_part[:, a] = d_in + dot(nw1[l, mat(0), :], d_hid)
                d_agg[:, a] = dot(nw1[l, mat(1), :], d_hid).astype(BF)

            loop(npad // TN, body)

        def gather_back():
            def body(step):
                msg[:, at(step, KS)] = gather(d_agg, keys(rrow, step), iota).astype(BF)

            loop(eh // KS, body)

        def edge_backward(l):
            e_in = edges_in[l]

            def body(j):
                all_parts, d_w2s, d_w1s, own_parts = [], [], [], []
                for sub in range(EC // T):
                    a = at(j * (EC // T) + sub, T)
                    if l == top:
                        if sub == 0:
                            chunk_arrived(GRAD_IN, j)
                        for d in OTHERS:
                            ge[rows_of(d), a] = g_recv[slot(d), j, :, sub * T:(sub + 1) * T].astype(BF)
                    d_res = ge[:, a].astype(F32)
                    d_msg = d_res + msg[:, a].astype(F32)
                    d_hid, d_w2, parts = mlp_back(d_msg, hidden[l, :, a], normed[l, :, a], inv[l:l + 1, a], ew2[l], vec(l, 0))
                    all_parts.append(parts)
                    d_w2s.append(d_w2)
                    d_w1s.append(dot_nt(e_in[:, a], d_hid))
                    msg[:, a] = d_hid
                    d_new = (d_res + dot(ew1[l, mat(0), :], d_hid)).astype(BF)
                    if l > 0:
                        ge[:, a] = d_new
                    else:
                        for d in OTHERS:
                            g_send[slot(d), j, :, sub * T:(sub + 1) * T] = d_new[rows_of(d)].astype(F32)
                        own_parts.append(d_new[:q])
                add_sums(sums.at[l, 0], all_parts)
                grad[l, 1] += sum(d_w2s[1:], d_w2s[0])
                grad[l, 0] += sum(d_w1s[1:], d_w1s[0])
                if l == 0:
                    @pl.when(j < hold)
                    def _():
                        for d in SEND_ORDER:
                            edge_start(GRAD_OUT, j, d)
                    place_edges(gedge_raw, beside(own_parts), 0, j)

            loop(nch, body)

        def vector_slab(l):
            def total(node, k):
                return column_sum(flip(sums[l, node, mat(k), :]))

            lat = stacked([total(node, k) for node in BOTH for k in THREE])
            biases = stacked([total(node, 3) for node in BOTH])
            n_lat = lat.shape[0]
            for d in range(GROUP):
                grad[l, VEC_SLAB, d * cols:d * cols + n_lat, :cols] = lat[:, rows_of(d)]
                grad[l, VEC_SLAB, d * cols + n_lat:d * cols + n_lat + 2, :] = biases

        def reduce_start(l, stage):
            for b in BOTH:
                core_copy(l, b, stage).start()

        def chip_sum(l, stage):
            row = lax.broadcasted_iota(jnp.int32, (cols, D), 0)
            edge_row = jnp.logical_or(row < 3, row == 6)
            core_all(l, stage).wait_recv()
            for b in BOTH:
                for k in range(SLABS)[STAGES[stage]]:
                    own = grad[l, k, rows_of(2 * b), :]
                    if k in EDGE_SLABS:
                        own = own + core_recv[l, b, k]
                    elif k == VEC_SLAB:
                        other = core_recv[l, b, k]
                        own = own + jnp.where(edge_row, other, 0.0)
                        own = jnp.where(jnp.logical_and(row == 7, c == 1), other, own)
                    half[l, k, b] = own
            for i in dp_others:
                @pl.when(in_stage(lax.rem(p + i, dpn), stage))
                def _():
                    spread_copy(l, i).start()

        def dp_sum(l, stage):
            @pl.when(in_stage(p, stage))
            def _():
                total = half[l, pl.ds(seat(p) * per, per)]
                dp_all(l, 0).wait_recv()
                for i in dp_others:
                    total = total + dp_recv[l, pl.ds((i - 1) * per, per)]
                own_sum[l] = total[:, 0]
                cross_send[l] = total[:, 1]
                cross_copy(l).start()

        def cross_sum(l):
            cross_copy(l).wait_recv()
            total = own_sum[l] + cross_recv[l]
            own_sum[l] = total
            gathered[l, pl.ds(seat(p) * per, per)] = total
            for i in dp_others:
                gather_copy(l, i, p).start()

        def project(l):
            table = tables[l]

            def body(step):
                a = pl.ds(pl.multiple_of(step * TN, D), TN)
                s_bf, r_bf, v_in = s_sum[:, a].astype(BF), r_sum[:, a].astype(BF), table[:, a]
                part[layers + l, :, a] = dot(ew1[l, mat(1), :], s_bf) + dot(ew1[l, mat(2), :], r_bf)
                if l > 0:
                    part_piece(layers + l, a).start()
                grad[l, 6] += dot_nt(v_in, s_bf)
                grad[l, 7] += dot_nt(v_in, r_bf)

            loop(npad // TN, body)

        for l in reversed(range(layers)):
            first_layer = l == 0
            with jax.named_scope(f'node_backward_{l}'):
                node_backward(l)
            if first_layer:
                with jax.named_scope('chip_sum_1'):
                    chip_sum(1, 0)
                    chip_sum(1, 1)
            with jax.named_scope(f'gather_back_{l}'):
                gather_back()
            if first_layer:
                edges_sent(GRAD_IN)
            with jax.named_scope(f'edge_backward_{l}'):
                edge_backward(l)
            vector_slab(l)
            reduce_start(l, 0)
            if first_layer:
                with jax.named_scope('dp_sum_1'):
                    dp_sum(1, 0)
                    dp_sum(1, 1)
            with jax.named_scope(f'sum_send_{l}'):
                segment_sum(s_sum, scol)
            if first_layer:
                with jax.named_scope('chip_sum_0'):
                    chip_sum(0, 0)
            with jax.named_scope(f'sum_recv_{l}'):
                segment_sum(r_sum, rcol)
            with jax.named_scope(f'project_{l}'):
                project(l)
            reduce_start(l, 1)
            if first_layer:
                part_copy(layers + l).start()
            if first_layer:
                with jax.named_scope('chip_sum_late'):
                    chip_sum(0, 1)
                with jax.named_scope('dp_sum_0'):
                    dp_sum(0, 0)
            with jax.named_scope(f'back_wait_{l}'):
                part_copy(layers + l).wait_recv()

        def final(step):
            a = pl.ds(pl.multiple_of(step * TN, D), TN)
            d_in = (d_part[:, a] + part[layers, :, a] + swap_halves(part_recv[layers, :, a])).astype(BF)
            v2[:, a] = d_in

        loop(npad // TN, final)
        gnode_raw[x] = v2[:q, :nodes]
        with jax.named_scope('dp_sum_late'):
            dp_sum(0, 1)

        gcop[1].wait_send()
        dn_send = gn_send.at[0]
        pack_nodes(take_rows(v2, rows_of(2)), dn_send)
        dn_copy = remote(dn_send, dn_recv, n_ss.at[2, 1], n_rs.at[2, 1], 2)
        dn_copy.start()

        def send_rest(j):
            for d in SEND_ORDER:
                edge_start(GRAD_OUT, j, d)

        loop(nch, send_rest, hold)

        with jax.named_scope('node_out_wait'):
            output_copies('wait_recv')
        unpack_nodes(no_recv, put_output(node_raw))

        def place_e(j):
            for d in OTHERS:
                place_edges(edge_raw, eo_recv[slot(d), j], d, j)

        with jax.named_scope('place_edge_out'):
            for group in THREE:
                group_arrived(EDGE_OUT, group)
            loop(nch, place_e)

        def place_g(j):
            for d in OTHERS:
                place_edges(gedge_raw, de_recv[slot(d), j], d, j)

        with jax.named_scope('place_first'):
            group_arrived(GRAD_OUT, 0)
            loop(hold, place_g)
        for l in range(layers):
            with jax.named_scope(f'cross_sum_{l}'):
                cross_sum(l)
        with jax.named_scope('d_node_wait'):
            dn_copy.wait_recv()
        unpack_nodes(dn_recv, put_output(gnode_raw))
        with jax.named_scope('place_rest'):
            group_arrived(GRAD_OUT, 1)
            loop(last, place_g, hold)
        for l in range(layers):
            dp_all(l, 1).wait_recv()
            ew1_buf[l, 0] = gathered[l, 0]
            ew1_buf[l, 1:] = gathered[l, EARLY:]
            ew2_buf[l] = gathered[l, 1]
            nw1_buf[l] = gathered[l, 2:4]
            nw2_buf[l] = gathered[l, 4]
            small = gathered[l, VEC_SLAB]
            for k in THREE:
                evec_buf[k, l:l + 1, :] = small[k:k + 1, :cols]
                nvec_buf[k, l:l + 1, :] = small[3 + k:4 + k, :cols]
            eb1_buf[l:l + 1, :] = small[6:7]
            nb1_buf[l:l + 1, :] = small[7:8]
        for l in range(layers):
            for stage in BOTH:
                core_all(l, stage).wait_send()
            cross_copy(l).wait_send()
            dp_all(l, 0).wait_send()
            dp_all(l, 1).wait_send()
        for copy in (ncop[2], gcop[0], gcop[2], w_pair, w_relay):
            copy.wait_send()

        by_share(lambda rows: w_cross(rows).wait_send())
        pl.when(brings)(weight_part((dpn - 1) * piece).wait_send)
        pl.when(jnp.logical_not(brings))(weight_part((dpn - 1) * HEAD).wait_send)

        output_copies('wait_send')
        dn_copy.wait_send()
        for k in range(layers, 2 * layers):
            part_copy(k).wait_send()
        edges_sent(EDGE_OUT)
        with jax.named_scope('place_last'):
            for d in (1, 2, 3):
                last_arrived(GRAD_OUT, d)
                place_edges(gedge_raw, de_recv[slot(d), last], d, last)
        edges_sent(GRAD_OUT)

    bf = lambda *s: pltpu.VMEM(s, BF)
    pl.run_scoped(
        scoped, bf(D, eh), bf(D, eh), bf(D, eh), bf(D, eh), bf(D, npad), bf(D, npad), bf(D, npad), bf(D, npad), bf(D, npad), bf(D, npad),
        pltpu.VMEM((eh, D), I16), pltpu.VMEM((eh, D), I16), pltpu.VMEM((eh // D * 16, D), I16), pltpu.VMEM((eh // D * 16, D), I16),
        pltpu.VMEM((T, D), I16), pltpu.VMEM((16, D), I16),
        bf(layers, 3 * D, D), bf(layers, D, 3 * D), bf(layers, D, D), bf(layers, D, D),
        bf(layers, 2 * D, D), bf(layers, D, 2 * D), bf(layers, D, D), bf(layers, D, D), pltpu.VMEM((D, D), F32))


def finish_moves(src, dst):
    if len(src.shape) != 3 or src.dtype != BF:
        return [(src, dst)]
    return [(src.at[s, pl.ds(r, 8)], dst.at[s, pl.ds(r, 8)]) for s in range(src.shape[0]) for r in range(0, src.shape[1], 8)]


def finish_kernel(*refs):
    count = len(refs) // 2
    moves = sum((finish_moves(refs[k], refs[count + k]) for k in range(count)), [])
    puts = [pltpu.make_async_copy(src, dst, refs[-1]) for src, dst in moves]
    for put in puts:
        put.start()
    for put in puts:
        put.wait()


def keep_in_vmem(val):
    return pltpu.with_memory_space_constraint(val, pltpu.VMEM)


def finish(arrays):
    return pl.pallas_call(
        finish_kernel,
        name='finish',
        out_shape=[jax.ShapeDtypeStruct(a.shape, a.dtype) for a in arrays],
        in_specs=[VM] * len(arrays),
        out_specs=[HB] * len(arrays),
        scratch_shapes=[pltpu.SemaphoreType.DMA],
        compiler_params=pltpu.CompilerParams(vmem_limit_bytes=1 << 20),
    )(*[keep_in_vmem(a) for a in arrays])


def solution(mesh):
    lat_spec = P('dp', None, 'tp')
    first_spec = P(None, None, 'tp', None)
    col_spec = P(None, None, 'tp')
    param_specs = (first_spec, P(), col_spec, col_spec, first_spec, P(), col_spec, col_spec)
    in_specs = (lat_spec, lat_spec, P(), P(), lat_spec, lat_spec) + param_specs
    out_specs = (lat_spec, lat_spec, lat_spec, lat_spec) + param_specs
    shape = jax.ShapeDtypeStruct

    def local_step(node_lat, edge_lat, senders, receivers, grad_node, grad_edge, edge_w1, edge_b1, edge_w2, edge_vec, node_w1, node_b1, node_w2, node_vec):
        layers = edge_w1.shape[0]
        cols = node_lat.shape[2]
        nodes, edges = node_lat.shape[1], edge_lat.shape[1]
        npad = -(-nodes // TN) * TN
        eh = -(-edges // (2 * EC)) * EC
        nch = eh // EC
        dpn = mesh.shape['dp']
        per = SLABS // dpn
        dims = (layers, cols, nodes, edges, npad, eh, dpn)
        flat = lambda arr: jnp.swapaxes(arr, 1, 2)
        lead = lambda arr: jnp.transpose(arr, (1, 0, 2))
        args = (flat(node_lat), flat(edge_lat), flat(grad_node), flat(grad_edge), senders, receivers,
                edge_w1.reshape(-1, D), flat(edge_w2).reshape(-1, D), node_w1.reshape(-1, D), flat(node_w2).reshape(-1, D),
                lead(edge_vec), lead(node_vec), edge_b1, node_b1)
        vm, sem = pltpu.VMEM, pltpu.SemaphoreType.DMA
        packed = nodes // D * cols + -(-(nodes % D) * GROUP // D) * cols // GROUP
        wrows = HEAD + layers * LROWS
        lat_n, lat_e = (2, cols, nodes), (2, cols, edges)
        outs = [RESULT(lat_n, BF), RESULT(lat_e, BF), RESULT(lat_n, BF), RESULT(lat_e, BF),
                RESULT((layers, 3, cols, D), F32), RESULT((layers, D), F32), RESULT((layers, cols, D), F32), RESULT((3, layers, cols), F32),
                RESULT((layers, 2, cols, D), F32), RESULT((layers, D), F32), RESULT((layers, cols, D), F32), RESULT((3, layers, cols), F32)]
        scratch = [
            *[vm(a.shape, a.dtype) for a in args[4:]], vm((wrows, D), F32), vm((3, wrows, D), F32),
            *[vm((many, packed, D), F32) for many in (2, 3, 2, 3)], *[vm((packed, D), F32)] * 2, vm((cols, npad), F32),
            *[vm((kinds, len(OTHERS), cols + cols // GROUP, D), F32) for kinds in (2, GROUP)], *[vm((len(OTHERS), nch, cols, EC), F32)] * 6,
            vm((2 * layers, D, npad), F32), vm((2 * layers, D, npad), F32),
            vm((layers, D, eh), F32), vm((layers, D, eh), F32), vm((layers, eh), F32),
            vm((layers, D, npad), F32), vm((layers, D, npad), F32), vm((layers, npad), F32),
            vm((D, npad), F32), vm((2, 2 * eh), jnp.int32), vm((D, D), F32), vm((layers, 2, 4 * D, D), F32),
            vm((layers, SLABS, D, D), F32), vm((layers, 2, SLABS, cols, D), F32), vm((layers, SLABS, 2, cols, D), F32),
            vm((layers, (dpn - 1) * per, 2, cols, D), F32), vm((layers, per, cols, D), F32), vm((layers, per, cols, D), F32),
            vm((layers, per, cols, D), F32), vm((layers, SLABS, cols, D), F32),]
        own_sems = [
            sem((layers, 2)), sem((3, layers)), sem((layers,)), sem((3,)), sem((3, 3)), sem((2, nch)), sem((2, 5)), sem((2 * layers,)),
            pltpu.SemaphoreType.REGULAR,
            sem((len(args) + 1,)), sem((3,)), sem((3, 3)), sem((4, 4)), sem((2 * layers,)), sem((layers, 2)), sem((3, layers)), sem((layers,))]
        res = pl.pallas_call(
            lambda *refs: pl.run_scoped(lambda *own: step_kernel(dims, *refs, *own), *own_sems),
            name='graph_step',
            out_shape=outs,
            in_specs=[HB] * len(args),
            out_specs=[VM] * len(outs),
            scratch_shapes=scratch,
            compiler_params=pltpu.CompilerParams(collective_id=0, has_side_effects=True, vmem_limit_bytes=VMEM_LIMIT),
        )(*args)

        res = finish(res)
        return (flat(res[0]), flat(res[1]), flat(res[2]), flat(res[3]),
                res[4], res[5], flat(res[6]), lead(res[7]), res[8], res[9], flat(res[10]), lead(res[11]))

    return jax.shard_map(local_step, mesh=mesh, in_specs=in_specs, out_specs=out_specs, check_vma=False)
```
